32 devices in a mesh: ctx: 8 (over z, y), fsdp: 4 (over x, core).
Axes of the slice: x: 2, y: 2, z: 4, core: 2. Of those that a mesh axis runs over, the one named last changes fastest.
Arguments:
- hidden: bfloat16 [4, 1024, 1536], P('fsdp', 'ctx'), may hold values from -6 to 6
- routes: int32 [4, 1024, 8], P('fsdp', 'ctx'), may hold values from 0 to 31, all different within a row; in each aligned block of 128 rows (0 to 127, 128 to 255, ..., all dimensions but the last counted through in order) at most 40 rows name the same one
- attn_norm: bfloat16 [1536], P(('ctx', 'fsdp')), may hold values from 0.5 to 1.5
- ffn_norm: bfloat16 [1536], P(('ctx', 'fsdp')), may hold values from 0.5 to 1.5
- w_q: bfloat16 [1536, 1536], P(('ctx', 'fsdp')), may hold values from -0.625 to 0.625
- key_weight: bfloat16 [1536, 512], P(('ctx', 'fsdp')), may hold values from -0.625 to 0.625
- value_weight: bfloat16 [1536, 512], P(('ctx', 'fsdp')), may hold values from -0.15625 to 0.15625
- w_o: bfloat16 [1536, 1536], P(('ctx', 'fsdp')), may hold values from -1.75 to 1.75
- router: bfloat16 [1536, 32], P(('ctx', 'fsdp')), may hold values from -0.3125 to 0.3125
- expert_in: bfloat16 [32, 1536, 1024], P('ctx', 'fsdp'), may hold values from -0.15625 to 0.15625
- expert_out: bfloat16 [32, 1536, 512], P('ctx', 'fsdp'), may hold values from -0.25 to 0.25
- cotangent: float32 [4, 1024, 1536], P('fsdp', 'ctx'), may hold values from -6 to 6
Outputs:
- layer_out: bfloat16 [4, 1024, 1536], P('fsdp', 'ctx')
- grad_hidden: float32 [4, 1024, 1536], P('fsdp', 'ctx')
- grad_attn_norm: float32 [1536], P(('ctx', 'fsdp'))
- grad_ffn_norm: float32 [1536], P(('ctx', 'fsdp'))
- grad_w_q: float32 [1536, 1536], P(('ctx', 'fsdp'))
- grad_w_k: float32 [1536, 512], P(('ctx', 'fsdp'))
- grad_w_v: float32 [1536, 512], P(('ctx', 'fsdp'))
- grad_w_o: float32 [1536, 1536], P(('ctx', 'fsdp'))
- grad_router: float32 [1536, 32], P(('ctx', 'fsdp'))
- grad_expert_in: float32 [32, 1536, 1024], P('ctx', 'fsdp')
- grad_expert_out: float32 [32, 1536, 512], P('ctx', 'fsdp')
The draws below stay inside these ranges and needn't reach their ends.
Inputs may be any that keep to these rules, and one draw needn't show every extreme that they name: `routes`: in the tokens of one block of 128, no expert is named more than 40 times, a bound that some block reaches.
All inputs are finite; a program needn't handle non-finite values.
Results may differ from the reference program's by a relative error of at most 0.033.
Values may be sent and summed in bfloat16 or wider, within the bound.
A program may use at most 256 MiB of HBM per device.

```python
import math
import jax
import jax.numpy as jnp
import numpy as np
from jax import lax

MODEL_WIDTH = 1536
QUERY_HEADS = 24
KEY_VALUE_HEADS = 8
HEAD_SIZE = 64
EXPERT_HIDDEN = 512
EXPERT_COUNT = 32
TOP = 8
TOK_DEV = 128
CAP = 40
SEQ_LEN = 1024
SEQS = 4
N_CTX = 8


def block_levels(stream_key, dims, cuts, low, high):
    loudness = 1.0
    for axis_at, parts in cuts:
        heights = jax.random.uniform(jax.random.fold_in(jax.random.fold_in(stream_key, 6), axis_at), (parts,), jnp.float32, low / len(cuts), high / len(cuts))
        loudness = loudness * jnp.repeat(jnp.exp(heights), dims[axis_at] // parts).reshape((-1,) + (1,) * (len(dims) - 1 - axis_at))
    return loudness


def shared_out(key, own, number, rows, count, top, most, skew):
    order = jax.random.permutation(key, count)
    crowded, ordinary = load_shares(count, rows * top, most, skew, True), load_shares(count, rows * top, most, skew, False)
    places = jnp.arange(count)

    def named(sizes, offset_by):
        used = int((sizes > 0).sum())
        fixed = max(1, used // 4)
        shifted = fixed + (places - fixed + offset_by * (used - fixed)) % max(1, count - fixed)
        return jnp.zeros((count,), jnp.int32).at[order[jnp.where(places < fixed, places, shifted)]].set(jnp.asarray(sizes, jnp.int32))

    sizes = jnp.where(number % 4 == 0, named(crowded, number // 4), named(ordinary, number - number // 4 - 1))
    mixed = jax.random.permutation(jax.random.fold_in(own, 3), count)
    source_of, receiver = mixed[0:count // 2 * 2:2], mixed[1:count // 2 * 2:2]
    slack = jnp.minimum(sizes[source_of] - 1, most - sizes[receiver]) // 2
    slack = jnp.where((source_of == order[0]) | (receiver == order[0]) | (sizes[receiver] == 0), 0, jnp.maximum(slack, 0))
    shifted = jax.random.randint(jax.random.fold_in(own, 4), (count // 2,), 0, 1 << 20) % (slack + 1)
    sizes = sizes.at[source_of].add(-shifted).at[receiver].add(shifted)
    members = jnp.searchsorted(jnp.cumsum(sizes), jnp.arange(rows * top), side="right").astype(jnp.int32)
    grid = members.reshape(top, rows).T
    grid = grid[jax.random.permutation(jax.random.fold_in(own, 1), rows)]
    offset_by = jax.random.randint(jax.random.fold_in(own, 2), (rows, 1), 0, top)
    return jnp.take_along_axis(grid, (jnp.arange(top)[None, :] + offset_by) % top, axis=1)


def load_shares(count, total, bound, lean, full):
    weights = [(1 << 20) // math.isqrt(standing ** lean) + 1 for standing in range(1, count + 1)]
    largest = bound if full else min(bound, max(-(-total // count), total * weights[0] // sum(weights)))
    least = 1 if total - largest >= count - 1 else 0
    given, rest = [largest] + [least] * (count - 1), total - largest - least * (count - 1)
    while rest > 0:
        movable = [i for i in range(1, count) if given[i] < largest] or [i for i in range(1, count) if given[i] < bound]
        pool, budget = sum([weights[i] for i in movable]), rest
        for i in movable:
            extra = min(bound - given[i], max(1, budget * weights[i] // pool), rest)
            given[i] = given[i] + extra
            rest = rest - extra
    return np.array(given)


def normal_values(stream_key, shape, scale, reach, cuts=(), kind=jnp.bfloat16):
    drawn = scale * jax.random.normal(stream_key, shape, jnp.float32)
    if cuts:
        drawn = drawn * block_levels(stream_key, shape, cuts, -0.22, 0.18)
    return jnp.clip(drawn, -reach, reach).astype(kind)


def setup_inputs(seed: int = 0) -> dict:
    streams_of = jax.random.split(jax.random.key(seed), 13)
    hidden = normal_values(streams_of[0], (SEQS, SEQ_LEN, MODEL_WIDTH), 1.0, 6.0, ((0, 4), (1, 8)))
    routes_keys = jax.random.split(jax.random.fold_in(streams_of[1], 1), SEQS * SEQ_LEN // TOK_DEV)
    routes_turns = jax.random.permutation(jax.random.fold_in(streams_of[1], 3), SEQS * SEQ_LEN // TOK_DEV)
    routes = jax.vmap(lambda own, number: shared_out(jax.random.fold_in(streams_of[1], 2), own, number, TOK_DEV, EXPERT_COUNT, TOP, CAP, 1))(routes_keys, routes_turns).reshape((SEQS, SEQ_LEN, TOP))
    attn_norm = jnp.clip(1.0 + 0.1 * jax.random.normal(streams_of[2], (MODEL_WIDTH,), jnp.float32), 0.5, 1.5).astype(jnp.bfloat16)
    ffn_norm = jnp.clip(1.0 + 0.1 * jax.random.normal(streams_of[3], (MODEL_WIDTH,), jnp.float32), 0.5, 1.5).astype(jnp.bfloat16)
    w_q = normal_values(streams_of[4], (MODEL_WIDTH, QUERY_HEADS * HEAD_SIZE), (MODEL_WIDTH // 16) ** -0.5, 0.625, ((0, 32),))
    key_weight = normal_values(streams_of[5], (MODEL_WIDTH, KEY_VALUE_HEADS * HEAD_SIZE), (MODEL_WIDTH // 16) ** -0.5, 0.625, ((0, 32),))
    value_weight = normal_values(streams_of[6], (MODEL_WIDTH, KEY_VALUE_HEADS * HEAD_SIZE), MODEL_WIDTH ** -0.5, 0.15625, ((0, 32),))
    w_o = normal_values(streams_of[7], (QUERY_HEADS * HEAD_SIZE, MODEL_WIDTH), (max(1, 8 * QUERY_HEADS * HEAD_SIZE // (TOK_DEV * N_CTX))) ** -0.5, 1.75, ((0, 32),))
    router = normal_values(streams_of[8], (MODEL_WIDTH, EXPERT_COUNT), (MODEL_WIDTH // 4) ** -0.5, 0.3125, ((0, 32),))
    expert_in = normal_values(streams_of[9], (EXPERT_COUNT, MODEL_WIDTH, 2 * EXPERT_HIDDEN), MODEL_WIDTH ** -0.5, 0.15625, ((0, 8), (1, 4)))
    expert_out = normal_values(streams_of[10], (EXPERT_COUNT, MODEL_WIDTH, EXPERT_HIDDEN), EXPERT_HIDDEN ** -0.5, 0.25, ((0, 8), (1, 4)))
    cotangent = normal_values(streams_of[11], (SEQS, SEQ_LEN, MODEL_WIDTH), 1.0, 6.0, ((0, 4), (1, 8)), jnp.float32)
    return dict(hidden=hidden, routes=routes, attn_norm=attn_norm, ffn_norm=ffn_norm, w_q=w_q, key_weight=key_weight, value_weight=value_weight, w_o=w_o, router=router, expert_in=expert_in, expert_out=expert_out, cotangent=cotangent)


norm_eps = 1e-06
attn_scale = 0.015625
rope_base = 10000.0
highest = lax.Precision.HIGHEST

def rope_tables(positions):
    half = HEAD_SIZE // 2
    frequency = jnp.power(jnp.float32(rope_base), -2.0 * jnp.arange(half, dtype=jnp.float32) / HEAD_SIZE)
    angle = positions.astype(jnp.float32)[:, None] * frequency[None, :]
    return (jnp.cos(angle)[:, None, :], jnp.sin(angle)[:, None, :])

def rotate_pairs(value_tensor, cosine_table, sine_table):
    half = value_tensor.shape[-1] // 2
    first = value_tensor[..., :half]
    second = value_tensor[..., half:]
    return jnp.concatenate([first * cosine_table - second * sine_table, second * cosine_table + first * sine_table], axis=-1)

def rms_forward(wide, gain):
    inverse = lax.rsqrt(lax.optimization_barrier(jnp.mean(wide * wide, axis=-1, keepdims=True)) + norm_eps)
    unit = wide * inverse
    return (unit, inverse, (unit * gain.astype(jnp.float32)).astype(jnp.bfloat16))

def rms_backward(grad, unit, inverse, gain):
    scaled = grad * gain.astype(jnp.float32)
    back = inverse * (scaled - unit * lax.optimization_barrier(jnp.mean(scaled * unit, axis=-1, keepdims=True)))
    return (back, lax.optimization_barrier(jnp.sum(grad * unit, axis=0)))

def round_half(value_tensor):
    return lax.optimization_barrier(value_tensor.astype(jnp.bfloat16)).astype(jnp.float32)

def attention_forward(query_rows, key_tensor, value_tensor):
    sequence_length = query_rows.shape[0]
    span = min(256, sequence_length)
    key_pos = jnp.arange(sequence_length, dtype=jnp.int32)
    keys_wide = key_tensor.astype(jnp.float32)
    values_wide = value_tensor.astype(jnp.float32)

    def block_step(carry, index):
        start = index * span
        query_block = lax.dynamic_slice_in_dim(query_rows, start, span, 0).astype(jnp.float32)
        scores = jnp.einsum('tkgd,nkd->kgtn', query_block, keys_wide, precision=highest) * attn_scale
        visible = key_pos[None, :] <= (start + jnp.arange(span, dtype=jnp.int32))[:, None]
        scores = jnp.where(visible, scores, -jnp.inf)
        log_sum_rows = jax.nn.logsumexp(scores, axis=-1)
        probs = round_half(jnp.exp(scores - log_sum_rows[..., None]))
        out_block = jnp.einsum('kgtn,nkd->tkgd', probs, values_wide, precision=highest).astype(jnp.bfloat16)
        return (carry, (out_block, log_sum_rows))
    _, (outs, log_sum_table) = lax.scan(block_step, None, jnp.arange(sequence_length // span, dtype=jnp.int32))
    attention_output = outs.reshape(sequence_length, QUERY_HEADS * HEAD_SIZE)
    log_sum_rows = jnp.transpose(log_sum_table, (1, 2, 0, 3)).reshape(KEY_VALUE_HEADS, QUERY_HEADS // KEY_VALUE_HEADS, sequence_length)
    return (attention_output, log_sum_rows)

def attention_backward(query_rows, key_tensor, value_tensor, grad_out, log_sum_rows, delta_rows):
    sequence_length = query_rows.shape[0]
    span = min(256, sequence_length)
    key_pos = jnp.arange(sequence_length, dtype=jnp.int32)
    keys_wide = key_tensor.astype(jnp.float32)
    values_wide = value_tensor.astype(jnp.float32)

    def block_step(carry, index):
        grad_keys, grad_values = carry
        start = index * span
        query_block = lax.dynamic_slice_in_dim(query_rows, start, span, 0).astype(jnp.float32)
        grad_block = lax.dynamic_slice_in_dim(grad_out, start, span, 0).astype(jnp.float32)
        logsum_block = lax.dynamic_slice_in_dim(log_sum_rows, start, span, 2)
        delta_block = lax.dynamic_slice_in_dim(delta_rows, start, span, 2)
        scores = jnp.einsum('tkgd,nkd->kgtn', query_block, keys_wide, precision=highest) * attn_scale
        visible = key_pos[None, :] <= (start + jnp.arange(span, dtype=jnp.int32))[:, None]
        weights_full = jnp.where(visible, jnp.exp(scores - logsum_block[..., None]), 0.0)
        grad_probs = jnp.einsum('tkgd,nkd->kgtn', grad_block, values_wide, precision=highest)
        grad_scores = round_half(weights_full * (grad_probs - delta_block[..., None]))
        grad_query = attn_scale * jnp.einsum('kgtn,nkd->tkgd', grad_scores, keys_wide, precision=highest)
        grad_keys = grad_keys + attn_scale * jnp.einsum('kgtn,tkgd->nkd', grad_scores, query_block, precision=highest)
        grad_values = grad_values + jnp.einsum('kgtn,tkgd->nkd', round_half(weights_full), grad_block, precision=highest)
        return ((grad_keys, grad_values), grad_query)
    zero_state = jnp.zeros((sequence_length, KEY_VALUE_HEADS, HEAD_SIZE), jnp.float32)
    (grad_keys, grad_values), grad_queries = lax.scan(block_step, (zero_state, zero_state), jnp.arange(sequence_length // span, dtype=jnp.int32))
    return (grad_queries.reshape(sequence_length, QUERY_HEADS, HEAD_SIZE), grad_keys, grad_values)

def expert_slots(route):
    sequence_length = route.shape[0]
    per_block = route.reshape(-1, TOK_DEV * TOP)
    indicator = (per_block[..., None] == jnp.arange(EXPERT_COUNT, dtype=jnp.int32)).astype(jnp.int32)
    slot = lax.optimization_barrier(jnp.sum(indicator * (jnp.cumsum(indicator, axis=1) - 1), axis=-1))
    block_index = jnp.arange(per_block.shape[0], dtype=jnp.int32)[:, None]
    return (block_index * CAP + slot).reshape(sequence_length, TOP).astype(jnp.int32)

def reference(hidden, routes, attn_norm, ffn_norm, w_q, key_weight, value_weight, w_o, router, expert_in, expert_out, cotangent):
    query_group = QUERY_HEADS // KEY_VALUE_HEADS

    def one_sequence(carry, inputs):
        hidden_seq, route, cot_seq = inputs
        sequence_length = hidden_seq.shape[0]
        positions = jnp.arange(sequence_length, dtype=jnp.int32)
        cosine_table, sine_table = rope_tables(positions)
        wide = hidden_seq.astype(jnp.float32)
        attn_unit, inverse_one, attention_input = rms_forward(wide, attn_norm)
        query_linear = jnp.dot(attention_input, w_q, preferred_element_type=jnp.float32).reshape(sequence_length, QUERY_HEADS, HEAD_SIZE)
        query_rows = rotate_pairs(query_linear, cosine_table, sine_table).astype(jnp.bfloat16).reshape(sequence_length, KEY_VALUE_HEADS, query_group, HEAD_SIZE)
        key_linear = jnp.dot(attention_input, key_weight, preferred_element_type=jnp.float32).reshape(sequence_length, KEY_VALUE_HEADS, HEAD_SIZE)
        key_tensor = rotate_pairs(key_linear, cosine_table, sine_table).astype(jnp.bfloat16)
        value_tensor = jnp.dot(attention_input, value_weight, preferred_element_type=jnp.float32).astype(jnp.bfloat16).reshape(sequence_length, KEY_VALUE_HEADS, HEAD_SIZE)
        attention_output, log_sum_rows = attention_forward(query_rows, key_tensor, value_tensor)
        mixed = wide + jnp.dot(attention_output, w_o, preferred_element_type=jnp.float32)
        ffn_unit, inverse_two, ffn_in = rms_forward(mixed, ffn_norm)
        logits = jnp.dot(ffn_in, router, preferred_element_type=jnp.float32)
        chosen = jnp.take_along_axis(logits, route, axis=1)
        gates = jax.nn.softmax(chosen, axis=-1)
        row = expert_slots(route)
        owner = jnp.full((EXPERT_COUNT, row.shape[0] // TOK_DEV * CAP), sequence_length * TOP, jnp.int32)
        owner = owner.at[route.reshape(-1), row.reshape(-1)].set(jnp.arange(sequence_length * TOP, dtype=jnp.int32))
        ffn_pad = jnp.concatenate([ffn_in, jnp.zeros((1, MODEL_WIDTH), jnp.bfloat16)], axis=0)

        def expert_forward(inputs_e):
            owners, weight_in, weight_out = inputs_e
            rows = ffn_pad[owners // TOP]
            act = jnp.dot(rows, weight_in, preferred_element_type=jnp.float32)
            gate_part = act[:, :EXPERT_HIDDEN]
            up_part = act[:, EXPERT_HIDDEN:]
            inner = (gate_part * jax.nn.sigmoid(gate_part) * up_part).astype(jnp.bfloat16)
            return lax.dot_general(inner, weight_out, (((1,), (1,)), ((), ())), preferred_element_type=jnp.float32).astype(jnp.bfloat16)
        expert_rows = lax.map(expert_forward, (owner, expert_in, expert_out))
        picked = expert_rows[route, row].astype(jnp.float32)
        layer_out = (mixed + lax.optimization_barrier(jnp.sum(gates[..., None] * picked, axis=1))).astype(jnp.bfloat16)
        grad_gate = lax.optimization_barrier(jnp.sum(cot_seq[:, None, :] * picked, axis=-1))
        slot_grads = (gates[..., None] * cot_seq[:, None, :]).astype(jnp.bfloat16).reshape(sequence_length * TOP, MODEL_WIDTH)
        slot_pad = jnp.concatenate([slot_grads, jnp.zeros((1, MODEL_WIDTH), jnp.bfloat16)], axis=0)

        def expert_backward(inputs_e):
            owners, weight_in, weight_out = inputs_e
            rows = ffn_pad[owners // TOP]
            incoming = slot_pad[owners]
            act = jnp.dot(rows, weight_in, preferred_element_type=jnp.float32)
            gate_part = act[:, :EXPERT_HIDDEN]
            up_part = act[:, EXPERT_HIDDEN:]
            sigma = jax.nn.sigmoid(gate_part)
            inner = (gate_part * sigma * up_part).astype(jnp.bfloat16)
            grad_out_w = lax.dot_general(incoming, inner, (((0,), (0,)), ((), ())), preferred_element_type=jnp.float32)
            grad_inner = jnp.dot(incoming, weight_out, preferred_element_type=jnp.float32)
            grad_act = jnp.concatenate([grad_inner * up_part * sigma * (1.0 + gate_part * (1.0 - sigma)), grad_inner * gate_part * sigma], axis=1).astype(jnp.bfloat16)
            grad_in_w = lax.dot_general(rows, grad_act, (((0,), (0,)), ((), ())), preferred_element_type=jnp.float32)
            grad_rows = lax.dot_general(grad_act, weight_in, (((1,), (1,)), ((), ())), preferred_element_type=jnp.float32).astype(jnp.bfloat16)
            return (grad_in_w, grad_out_w, grad_rows)
        grad_in_all, grad_out_all, grad_rows_all = lax.map(expert_backward, (owner, expert_in, expert_out))
        grad_chosen = gates * (grad_gate - lax.optimization_barrier(jnp.sum(gates * grad_gate, axis=-1, keepdims=True)))
        grad_logits = jnp.zeros((sequence_length, EXPERT_COUNT), jnp.float32).at[jnp.arange(sequence_length, dtype=jnp.int32)[:, None], route].add(grad_chosen).astype(jnp.bfloat16)
        grad_router_seq = lax.dot_general(ffn_in, grad_logits, (((0,), (0,)), ((), ())), preferred_element_type=jnp.float32)
        grad_ffn_in = lax.dot_general(grad_logits, router, (((1,), (1,)), ((), ())), preferred_element_type=jnp.float32)
        grad_ffn_in = grad_ffn_in + lax.optimization_barrier(jnp.sum(grad_rows_all[route, row].astype(jnp.float32), axis=1))
        back_two, grad_ffn_gain = rms_backward(grad_ffn_in, ffn_unit, inverse_two, ffn_norm)
        grad_mixed = cot_seq + back_two
        grad_attn = grad_mixed.astype(jnp.bfloat16)
        grad_wo_seq = lax.dot_general(attention_output, grad_attn, (((0,), (0,)), ((), ())), preferred_element_type=jnp.float32)
        attention_output_gradient = lax.dot_general(grad_attn, w_o, (((1,), (1,)), ((), ())), preferred_element_type=jnp.float32).astype(jnp.bfloat16)
        head_gradient = attention_output_gradient.reshape(sequence_length, KEY_VALUE_HEADS, query_group, HEAD_SIZE)
        delta_rows = lax.optimization_barrier(jnp.sum(head_gradient.astype(jnp.float32) * attention_output.reshape(sequence_length, KEY_VALUE_HEADS, query_group, HEAD_SIZE).astype(jnp.float32), axis=-1))
        delta_rows = jnp.transpose(delta_rows, (1, 2, 0))
        grad_q, key_gradient, value_gradient = attention_backward(query_rows, key_tensor, value_tensor, head_gradient, log_sum_rows, delta_rows)
        query_back = rotate_pairs(grad_q, cosine_table, -sine_table).astype(jnp.bfloat16).reshape(sequence_length, QUERY_HEADS * HEAD_SIZE)
        key_backward_rows = rotate_pairs(key_gradient, cosine_table, -sine_table).astype(jnp.bfloat16).reshape(sequence_length, KEY_VALUE_HEADS * HEAD_SIZE)
        value_backward_rows = value_gradient.astype(jnp.bfloat16).reshape(sequence_length, KEY_VALUE_HEADS * HEAD_SIZE)
        contract_rows = (((0,), (0,)), ((), ()))
        contract_cols = (((1,), (1,)), ((), ()))
        grad_wq_seq = lax.dot_general(attention_input, query_back, contract_rows, preferred_element_type=jnp.float32)
        grad_wk_seq = lax.dot_general(attention_input, key_backward_rows, contract_rows, preferred_element_type=jnp.float32)
        grad_wv_seq = lax.dot_general(attention_input, value_backward_rows, contract_rows, preferred_element_type=jnp.float32)
        grad_attn_in = lax.dot_general(query_back, w_q, contract_cols, preferred_element_type=jnp.float32)
        grad_attn_in = grad_attn_in + lax.dot_general(key_backward_rows, key_weight, contract_cols, preferred_element_type=jnp.float32)
        grad_attn_in = grad_attn_in + lax.dot_general(value_backward_rows, value_weight, contract_cols, preferred_element_type=jnp.float32)
        back_one, grad_attn_gain = rms_backward(grad_attn_in, attn_unit, inverse_one, attn_norm)
        grad_input = grad_mixed + back_one
        updates = (grad_attn_gain, grad_ffn_gain, grad_wq_seq, grad_wk_seq, grad_wv_seq, grad_wo_seq, grad_router_seq, grad_in_all, grad_out_all)
        new_carry = tuple((total + part for total, part in zip(carry, updates)))
        return (new_carry, (layer_out, grad_input))
    initial_state = (jnp.zeros((MODEL_WIDTH,), jnp.float32), jnp.zeros((MODEL_WIDTH,), jnp.float32), jnp.zeros((MODEL_WIDTH, QUERY_HEADS * HEAD_SIZE), jnp.float32), jnp.zeros((MODEL_WIDTH, KEY_VALUE_HEADS * HEAD_SIZE), jnp.float32), jnp.zeros((MODEL_WIDTH, KEY_VALUE_HEADS * HEAD_SIZE), jnp.float32), jnp.zeros((QUERY_HEADS * HEAD_SIZE, MODEL_WIDTH), jnp.float32), jnp.zeros((MODEL_WIDTH, EXPERT_COUNT), jnp.float32), jnp.zeros((EXPERT_COUNT, MODEL_WIDTH, 2 * EXPERT_HIDDEN), jnp.float32), jnp.zeros((EXPERT_COUNT, MODEL_WIDTH, EXPERT_HIDDEN), jnp.float32))
    totals, (layer_out, grad_hidden) = lax.scan(one_sequence, initial_state, (hidden, routes, cotangent))
    return (layer_out, grad_hidden, totals[0], totals[1], totals[2], totals[3], totals[4], totals[5], totals[6], totals[7], totals[8])
```

```python
import functools
import itertools

import jax
import jax.numpy as jnp
from jax import lax
from jax.experimental import pallas as pl
from jax.experimental.pallas import tpu as pltpu
from jax.sharding import PartitionSpec as P


NY = 2
NZ = 4
NX = 2
NC = 2
DEV = pl.DeviceIdType.MESH
CTX, FSDP = "ctx", "fsdp"
Z, Y, X, C = 0, 1, 2, 3
SIZES = {Z: NZ, Y: NY, X: NX, C: NC}
UP, DOWN = 4, 5


class Plan:
    def __init__(self, ref, order, index, rows=None):
        self.ref, self.order, self.index, self.rows = ref, order, index, rows
        self.blocks = 1
        for d in index:
            self.blocks *= SIZES[d]


class Place:
    def __init__(self):
        ctx = lax.axis_index(CTX)
        fsdp = lax.axis_index(FSDP)
        self.at = {Z: ctx // NY, Y: ctx % NY, X: fsdp // NC, C: fsdp % NC}
        z = self.at[Z]
        low = z < NZ // 2
        base = jnp.where(low, z, NZ - 1 - z)
        near = [base, 1 - base, jnp.int32(2), jnp.int32(3)]
        self.order = [z] + [jnp.where(low, k, NZ - 1 - k) for k in near[1:]]

    def device(self, dim, value):
        spot = dict(self.at)
        spot[dim] = value
        return (spot[Z] * NY + spot[Y], spot[X] * NC + spot[C])

    def across(self, dim):
        return self.device(dim, 1 - self.at[dim])

    def along(self, step):
        return self.device(Z, self.at[Z] + step)

    def coords(self, z_from, flips):
        spot = {d: (1 - self.at[d] if d in flips else self.at[d]) for d in (Y, X, C)}
        spot[Z] = z_from
        return spot


def flat_index(spot, dims):
    index = 0
    for d in dims:
        index = index * SIZES[d] + spot[d]
    return index


def subsets(dims):
    return [c for n in range(len(dims) + 1) for c in itertools.combinations(dims, n)]


def greet(place, dims):
    barrier = pltpu.get_barrier_semaphore()
    z = place.at[Z]
    count = jnp.int32(0)
    for d in dims:
        if d == Z:
            @pl.when(z > 0)
            def _():
                pl.semaphore_signal(barrier, inc=1, device_id=place.along(-1), device_id_type=DEV)

            @pl.when(z < NZ - 1)
            def _():
                pl.semaphore_signal(barrier, inc=1, device_id=place.along(1), device_id_type=DEV)

            count = count + jnp.where(z > 0, 1, 0) + jnp.where(z < NZ - 1, 1, 0)
        else:
            pl.semaphore_signal(barrier, inc=1, device_id=place.across(d), device_id_type=DEV)
            count = count + 1
    pl.semaphore_wait(barrier, count)


def gather_events(order):
    pairs = [d for d in order if d != Z]
    events = [(k, f) for k in range(NZ) for f in subsets(pairs)]
    return sorted(events, key=lambda e: (e[0] + len(e[1]), len(e[1])))


def gather_sends(order, k, flips):
    z_at = order.index(Z)
    last = max([order.index(d) for d in flips] + ([z_at] if k > 0 else []) + [-1])
    out = []
    for position, d in enumerate(order):
        if position > last:
            out.extend([UP, DOWN] if d == Z else [d])
    if k > 0 and last == z_at:
        out.extend([UP, DOWN])
    return out


def gather_kernel(plans, n_in, *refs):
    ins, outs = refs[:n_in], refs[n_in : 2 * n_in]
    send_sem, recv_sem, own_sem = refs[2 * n_in :]
    place = Place()
    z = place.at[Z]
    greet(place, sorted({d for p in plans for d in p.order}))
    pending = []
    slot = 0
    queue = []
    for n, plan in enumerate(plans):
        for rank, event in enumerate(gather_events(plan.order)):
            queue.append((rank / len(gather_events(plan.order)), n, event))
    queue.sort(key=lambda q: (q[0], q[1]))
    bases = [sum(p.blocks for p in plans[:n]) for n in range(len(plans))]
    for _, n, (k, flips) in queue:
        plan = plans[n]
        src = ins[plan.ref]
        out = outs[plan.ref]
        rows = plan.rows
        z_from = place.order[k]
        spot = place.coords(z_from, flips)
        index = flat_index(spot, plan.index)
        target = out.at[index] if rows is None else out.at[index, pl.ds(rows[0], rows[1])]
        sem = recv_sem.at[bases[n] + index]
        own = k == 0 and not flips
        source = (src if rows is None else src.at[pl.ds(rows[0], rows[1])]) if own else target
        if not own:
            pltpu.make_async_remote_copy(
                src_ref=target, dst_ref=target, send_sem=own_sem.at[0], recv_sem=sem,
                device_id=place.across(C), device_id_type=DEV,
            ).wait_recv()
        for way in gather_sends(plan.order, k, flips):
            if way in (UP, DOWN):
                step = 1 if way == UP else -1
                go = z < NZ - 1 if way == UP else z > 0
                if k > 0:
                    go = jnp.logical_and(go, z_from < z if way == UP else z_from > z)
                dest = place.device(Z, jnp.clip(z + step, 0, NZ - 1))
            else:
                go, dest = None, place.across(way)
            copy = pltpu.make_async_remote_copy(
                src_ref=source, dst_ref=target, send_sem=send_sem.at[slot], recv_sem=sem,
                device_id=dest, device_id_type=DEV,
            )
            slot += 1
            if go is None:
                copy.start()
            else:
                pl.when(go)(copy.start)
            pending.append((go, copy.wait_send))
        if own:
            copy = pltpu.make_async_copy(source, target, own_sem.at[1 + n])
            copy.start()
            pending.append((None, copy.wait))
    for go, wait in pending:
        if go is None:
            wait()
        else:
            pl.when(go)(wait)


def gather(arrays, plans, collective_id, name):
    n = len(arrays)
    sends = sum(len(gather_sends(p.order, k, f)) for p in plans for k, f in gather_events(p.order))
    blocks = {p.ref: p.blocks for p in plans}
    return pl.pallas_call(
        functools.partial(gather_kernel, plans, n),
        out_shape=[jax.ShapeDtypeStruct((blocks[i],) + a.shape, a.dtype) for i, a in enumerate(arrays)],
        in_specs=[pl.BlockSpec(memory_space=pltpu.VMEM)] * n,
        out_specs=[pl.BlockSpec(memory_space=pl.ANY)] * n,
        scratch_shapes=[
            pltpu.SemaphoreType.DMA((sends,)),
            pltpu.SemaphoreType.DMA((sum(p.blocks for p in plans),)),
            pltpu.SemaphoreType.DMA((1 + len(plans),)),
        ],
        compiler_params=pltpu.CompilerParams(collective_id=collective_id, has_side_effects=True),
        name=name,
    )(*arrays)


def add_into(acc, other):
    acc[...] = (acc[...].astype(jnp.float32) + other[...].astype(jnp.float32)).astype(acc.dtype)


def reduce_kernel(plans, n_in, *refs):
    ins, outs = refs[:n_in], refs[n_in : 2 * n_in]
    rest = list(refs[2 * n_in :])
    send_sem, recv_sem, own_sem = rest[:3]
    buffers = rest[3:]
    place = Place()
    z = place.at[Z]
    greet(place, sorted({d for p in plans for d in p.order} | {Z}))
    pending = []
    slots = [0, 0]

    def push(source, target, sem, dest):
        copy = pltpu.make_async_remote_copy(
            src_ref=source, dst_ref=target, send_sem=send_sem.at[slots[0]], recv_sem=sem,
            device_id=dest, device_id_type=DEV,
        )
        slots[0] += 1
        copy.start()
        pending.append(copy)

    def arrived(target, sem):
        pltpu.make_async_remote_copy(
            src_ref=target, dst_ref=target, send_sem=own_sem.at[0], recv_sem=sem,
            device_id=place.across(C), device_id_type=DEV,
        ).wait_recv()

    work = []
    far = list(reversed(range(NZ)))
    own_slot = 1
    state = []
    base = 0
    for n, plan in enumerate(plans):
        dims = plan.order
        acc = buffers[0]
        levels = buffers[1 : 1 + len(dims)]
        chain = buffers[1 + len(dims)]
        buffers = buffers[2 + len(dims) :]
        kept = [subsets(dims[p + 1 :]) for p in range(len(dims))]
        counts = [NZ * len(f) for f in kept]
        level_base = [base + sum(counts[:p]) for p in range(len(dims))]
        chain_base = base + sum(counts)
        base = chain_base + 2 * NZ
        state.append((acc, levels, chain, kept, level_base, chain_base))
        own_copies = {}
        src = ins[plan.ref]
        for k in far:
            for f in kept[0]:
                gone = flat_index(place.coords(place.order[k], (dims[0],) + f), plan.index)
                spot = place.order[k] * len(kept[0]) + kept[0].index(f)
                work.append((0, n, k, f, gone, spot))
                mine = flat_index(place.coords(place.order[k], f), plan.index)
                copy = pltpu.make_async_copy(src.at[mine], acc.at[spot], own_sem.at[own_slot])
                own_slot += 1
                own_copies[(k, f)] = copy
        state[-1] += (own_copies,)
    for _, n, k, f, gone, spot in sorted(work, key=lambda w: (-w[2],)):
        plan = plans[n]
        acc, levels, chain, kept, level_base, chain_base, own_copies = state[n]
        push(ins[plan.ref].at[gone], levels[0].at[spot], recv_sem.at[level_base[0] + spot], place.across(plan.order[0]))
        own_copies[(k, f)].start()

    def level_step(n, p, k):
        plan = plans[n]
        dims = plan.order
        acc, levels, chain, kept, level_base, chain_base, own_copies = state[n]
        for f in sorted(kept[p], key=lambda f: -len(f)):
            spot = place.order[k] * len(kept[p]) + kept[p].index(f)
            at = place.order[k] * len(kept[0]) + kept[0].index(f)
            if p == 0:
                own_copies[(k, f)].wait()
            arrived(levels[p].at[spot], recv_sem.at[level_base[p] + spot])
            add_into(acc.at[at], levels[p].at[spot])
            later = p + 1
            if later < len(dims) and dims[later] in f:
                left = tuple(d for d in f if d != dims[later])
                there = place.order[k] * len(kept[later]) + kept[later].index(left)
                push(
                    acc.at[at], levels[later].at[there],
                    recv_sem.at[level_base[later] + there], place.across(dims[later]),
                )

    def chain_step(n, k):
        plan = plans[n]
        acc, levels, chain, kept, level_base, chain_base, own_copies = state[n]
        dest = place.order[k]
        up = dest > z
        lane = jnp.where(up, 0, 1)
        at = dest * len(kept[0])
        spot = lane * NZ + dest

        @pl.when(jnp.where(up, z > 0, z < NZ - 1))
        def _():
            arrived(chain.at[spot], recv_sem.at[chain_base + spot])
            add_into(acc.at[at], chain.at[spot])

        push(acc.at[at], chain.at[spot], recv_sem.at[chain_base + spot], place.along(jnp.where(up, 1, -1)))

    most = max(len(p.order) for p in plans)
    for step in range(NZ + most):
        for n, plan in enumerate(plans):
            for p in range(len(plan.order)):
                if 0 <= step - p < NZ:
                    level_step(n, p, far[step - p])
            p = len(plan.order)
            if 0 <= step - p < NZ - 1:
                chain_step(n, far[step - p])
    for n, plan in enumerate(plans):
        acc, levels, chain, kept, level_base, chain_base, own_copies = state[n]
        at = z * len(kept[0])

        @pl.when(z > 0)
        def _():
            spot = z
            arrived(chain.at[spot], recv_sem.at[chain_base + spot])
            add_into(acc.at[at], chain.at[spot])

        @pl.when(z < NZ - 1)
        def _():
            spot = NZ + z
            arrived(chain.at[spot], recv_sem.at[chain_base + spot])
            add_into(acc.at[at], chain.at[spot])

        outs[plan.ref][...] = acc[at].astype(outs[plan.ref].dtype)
    for copy in pending:
        copy.wait_send()


def reduce_scatter(arrays, plans, out_dtypes, collective_id, name):
    n = len(arrays)
    scratch = []
    sends = recvs = owns = 0
    for p in plans:
        a = arrays[p.ref]
        block = a.shape[1:]
        kept = [len(subsets(p.order[q + 1 :])) for q in range(len(p.order))]
        scratch.append(pltpu.VMEM((NZ * kept[0],) + block, a.dtype))
        for q in kept:
            scratch.append(pltpu.VMEM((NZ * q,) + block, a.dtype))
        scratch.append(pltpu.VMEM((2 * NZ,) + block, a.dtype))
        sends += NZ * sum(kept) + NZ - 1
        recvs += NZ * sum(kept) + 2 * NZ
        owns += NZ * kept[0]
    return pl.pallas_call(
        functools.partial(reduce_kernel, plans, n),
        out_shape=[jax.ShapeDtypeStruct(a.shape[1:], d) for a, d in zip(arrays, out_dtypes)],
        in_specs=[pl.BlockSpec(memory_space=pl.ANY)] * n,
        out_specs=[pl.BlockSpec(memory_space=pltpu.VMEM)] * n,
        scratch_shapes=[
            pltpu.SemaphoreType.DMA((sends,)),
            pltpu.SemaphoreType.DMA((recvs,)),
            pltpu.SemaphoreType.DMA((1 + owns,)),
        ]
        + scratch,
        compiler_params=pltpu.CompilerParams(
            collective_id=collective_id, has_side_effects=True, vmem_limit_bytes=60 * 1024 * 1024
        ),
        name=name,
    )(*arrays)


MODEL_WIDTH = 1536
QUERY_HEADS = 24
KEY_VALUE_HEADS = 8
HEAD_SIZE = 64
EXPERT_HIDDEN = 512
EXPERT_COUNT = 32
TOP = 8
CAP = 40


norm_eps = 1e-06
attn_scale = 0.015625
rope_base = 10000.0
masked_logits = -1e30


def rope_tables(positions):
    half = HEAD_SIZE // 2
    frequency = jnp.power(
        jnp.float32(rope_base), -2.0 * jnp.arange(half, dtype=jnp.float32) / HEAD_SIZE
    )
    angle = positions.astype(jnp.float32)[:, None] * frequency[None, :]
    return (jnp.cos(angle)[:, None, :], jnp.sin(angle)[:, None, :])


def rotate_pairs(value_tensor, cosine_table, sine_table):
    half = value_tensor.shape[-1] // 2
    first = value_tensor[..., :half]
    second = value_tensor[..., half:]
    return jnp.concatenate(
        [first * cosine_table - second * sine_table, second * cosine_table + first * sine_table],
        axis=-1,
    )


def rms_forward(wide, gain):
    inverse = lax.rsqrt(jnp.mean(wide * wide, axis=-1, keepdims=True) + norm_eps)
    unit = wide * inverse
    return (unit, inverse, (unit * gain.astype(jnp.float32)).astype(jnp.bfloat16))


def rms_backward(grad, unit, inverse, gain):
    scaled = grad * gain.astype(jnp.float32)
    back = inverse * (scaled - unit * jnp.mean(scaled * unit, axis=-1, keepdims=True))
    return (back, jnp.sum(grad * unit, axis=0))


def piece_scores(query_rows, key_section, positions):
    token_count = key_section.shape[0]
    key_tensor = key_section.reshape(token_count, KEY_VALUE_HEADS, HEAD_SIZE)
    scores = (
        jnp.einsum("tkgd,nkd->kgtn", query_rows, key_tensor, preferred_element_type=jnp.float32)
        * attn_scale
    )
    visible = jnp.arange(token_count, dtype=jnp.int32)[None, :] <= positions[:, None]
    return (jnp.where(visible, scores, masked_logits), visible, key_tensor)


def local(
    hidden,
    routes,
    attn_norm,
    ffn_norm,
    w_q,
    key_weight,
    value_weight,
    w_o,
    router,
    expert_in,
    expert_out,
    cotangent,
):
    token_rows = hidden.shape[1]
    query_group = QUERY_HEADS // KEY_VALUE_HEADS
    ctx_size = lax.axis_size(CTX)
    sequence_length = token_rows * ctx_size
    positions = lax.axis_index(CTX) * token_rows + jnp.arange(token_rows, dtype=jnp.int32)
    cosine_table, sine_table = rope_tables(positions)
    contract_rows = (((0,), (0,)), ((), ()))
    contract_cols = (((1,), (1,)), ((), ()))
    layer = (
        lax.all_gather(attn_norm, (CTX, FSDP), axis=0, tiled=True),
        lax.all_gather(ffn_norm, (CTX, FSDP), axis=0, tiled=True),
        lax.all_gather(w_q, (CTX, FSDP), axis=0, tiled=True),
        lax.all_gather(key_weight, (CTX, FSDP), axis=0, tiled=True),
        lax.all_gather(value_weight, (CTX, FSDP), axis=0, tiled=True),
        lax.all_gather(w_o, (CTX, FSDP), axis=0, tiled=True),
        lax.all_gather(router, (CTX, FSDP), axis=0, tiled=True),
    )
    attn_gain, ffn_gain, query_w, key_weight_matrix, value_w, output_w, router_w = layer
    experts = (
        lax.all_gather(expert_in, FSDP, axis=1, tiled=True),
        lax.all_gather(expert_out, FSDP, axis=1, tiled=True),
    )
    weight_in, weight_out = experts
    wide = hidden[0].astype(jnp.float32)
    attn_unit, inverse_one, attention_input = rms_forward(wide, attn_gain)
    query_linear = jnp.dot(attention_input, query_w, preferred_element_type=jnp.float32).reshape(
        token_rows, QUERY_HEADS, HEAD_SIZE
    )
    query_rows = (
        rotate_pairs(query_linear, cosine_table, sine_table)
        .astype(jnp.bfloat16)
        .reshape(token_rows, KEY_VALUE_HEADS, query_group, HEAD_SIZE)
    )
    key_linear = jnp.dot(
        attention_input, key_weight_matrix, preferred_element_type=jnp.float32
    ).reshape(token_rows, KEY_VALUE_HEADS, HEAD_SIZE)
    key_matrix_rows = (
        rotate_pairs(key_linear, cosine_table, sine_table)
        .astype(jnp.bfloat16)
        .reshape(token_rows, KEY_VALUE_HEADS * HEAD_SIZE)
    )
    value_rows = jnp.dot(attention_input, value_w, preferred_element_type=jnp.float32).astype(
        jnp.bfloat16
    )
    init_state = (
        jnp.full((KEY_VALUE_HEADS, query_group, token_rows), masked_logits, jnp.float32),
        jnp.zeros((KEY_VALUE_HEADS, query_group, token_rows), jnp.float32),
        jnp.zeros((KEY_VALUE_HEADS, query_group, token_rows, HEAD_SIZE), jnp.float32),
    )
    key_section = lax.all_gather(key_matrix_rows, CTX, axis=0, tiled=True)
    value_section = lax.all_gather(value_rows, CTX, axis=0, tiled=True)

    def compute(current):
        best, total, weighted = current
        scores, visible, key_tensor = piece_scores(query_rows, key_section, positions)
        value_tensor = value_section.reshape(value_section.shape[0], KEY_VALUE_HEADS, HEAD_SIZE)
        new_best = jnp.maximum(best, jnp.max(scores, axis=-1))
        weights = jnp.where(visible, jnp.exp(scores - new_best[..., None]), 0.0)
        total = jnp.sum(weights, axis=-1)
        weighted = jnp.einsum(
            "kgtn,nkd->kgtd",
            weights.astype(jnp.bfloat16),
            value_tensor,
            preferred_element_type=jnp.float32,
        )
        return (new_best, total, weighted)

    best, total, weighted = lax.cond(
        jnp.int32(0) <= positions[-1], compute, lambda current: current, init_state
    )
    log_sum_rows = best + jnp.log(total)
    attention_output = (
        jnp.transpose(weighted / total[..., None], (2, 0, 1, 3))
        .reshape(token_rows, QUERY_HEADS * HEAD_SIZE)
        .astype(jnp.bfloat16)
    )
    mixed = wide + jnp.dot(attention_output, output_w, preferred_element_type=jnp.float32)
    ffn_unit, inverse_two, ffn_in = rms_forward(mixed, ffn_gain)
    logits = jnp.dot(ffn_in, router_w, preferred_element_type=jnp.float32)
    route = routes[0]
    indicator = (route[:, :, None] == jnp.arange(EXPERT_COUNT, dtype=jnp.int32)).astype(jnp.float32)
    chosen = jnp.sum(indicator * logits[:, None, :], axis=-1)
    gates = jax.nn.softmax(chosen, axis=-1)
    flat_route = route.reshape(-1)
    counter = (flat_route[:, None] == jnp.arange(EXPERT_COUNT, dtype=jnp.int32)).astype(jnp.int32)
    slot = jnp.sum(counter * (jnp.cumsum(counter, axis=0) - 1), axis=1)
    target = flat_route * CAP + slot
    owner = (
        jnp.full((EXPERT_COUNT * CAP,), token_rows * TOP, jnp.int32)
        .at[target]
        .set(jnp.arange(token_rows * TOP, dtype=jnp.int32))
    )
    ffn_pad = jnp.concatenate([ffn_in, jnp.zeros((1, MODEL_WIDTH), jnp.bfloat16)], axis=0)
    local_experts = weight_in.shape[0]
    outgoing = ffn_pad[owner // TOP].reshape(ctx_size, local_experts, CAP, MODEL_WIDTH)
    received = lax.all_to_all(outgoing, CTX, split_axis=0, concat_axis=2, tiled=True)[0]
    act = jnp.einsum("erd,edf->erf", received, weight_in, preferred_element_type=jnp.float32)
    gate_part = act[..., :EXPERT_HIDDEN]
    up_part = act[..., EXPERT_HIDDEN:]
    sigma = jax.nn.sigmoid(gate_part)
    inner = (gate_part * sigma * up_part).astype(jnp.bfloat16)
    produced = jnp.einsum(
        "erf,edf->erd", inner, weight_out, preferred_element_type=jnp.float32
    ).astype(jnp.bfloat16)
    returned = lax.all_to_all(
        produced[None], CTX, split_axis=2, concat_axis=0, tiled=True
    ).reshape(EXPERT_COUNT * CAP, MODEL_WIDTH)
    picked = returned[target].reshape(token_rows, TOP, MODEL_WIDTH)
    layer_out = (mixed + jnp.sum(gates[..., None] * picked, axis=1)).astype(jnp.bfloat16)
    cot = cotangent[0]
    layer = (
        lax.all_gather(attn_norm, (CTX, FSDP), axis=0, tiled=True),
        lax.all_gather(ffn_norm, (CTX, FSDP), axis=0, tiled=True),
        lax.all_gather(w_q, (CTX, FSDP), axis=0, tiled=True),
        lax.all_gather(key_weight, (CTX, FSDP), axis=0, tiled=True),
        lax.all_gather(value_weight, (CTX, FSDP), axis=0, tiled=True),
        lax.all_gather(w_o, (CTX, FSDP), axis=0, tiled=True),
        lax.all_gather(router, (CTX, FSDP), axis=0, tiled=True),
    )
    attn_gain, ffn_gain, query_w, key_weight_matrix, value_w, output_w, router_w = layer
    experts = (
        lax.all_gather(expert_in, FSDP, axis=1, tiled=True),
        lax.all_gather(expert_out, FSDP, axis=1, tiled=True),
    )
    weight_in, weight_out = experts
    grad_gate = jnp.sum(cot[:, None, :] * picked, axis=-1)
    slot_grads = (
        (gates[..., None] * cot[:, None, :])
        .astype(jnp.bfloat16)
        .reshape(token_rows * TOP, MODEL_WIDTH)
    )
    slot_pad = jnp.concatenate([slot_grads, jnp.zeros((1, MODEL_WIDTH), jnp.bfloat16)], axis=0)
    grad_outgoing = slot_pad[owner].reshape(ctx_size, local_experts, CAP, MODEL_WIDTH)
    grad_received = lax.all_to_all(grad_outgoing, CTX, split_axis=0, concat_axis=2, tiled=True)[0]
    grad_w_out = jnp.einsum(
        "erd,erf->edf", grad_received, inner, preferred_element_type=jnp.float32
    )
    grad_inner = jnp.einsum(
        "erd,edf->erf", grad_received, weight_out, preferred_element_type=jnp.float32
    )
    grad_act = jnp.concatenate(
        [
            grad_inner * up_part * sigma * (1.0 + gate_part * (1.0 - sigma)),
            grad_inner * gate_part * sigma,
        ],
        axis=-1,
    ).astype(jnp.bfloat16)
    grad_w_in = jnp.einsum("erd,erf->edf", received, grad_act, preferred_element_type=jnp.float32)
    grad_rows = jnp.einsum(
        "erf,edf->erd", grad_act, weight_in, preferred_element_type=jnp.float32
    ).astype(jnp.bfloat16)
    grad_back = lax.all_to_all(
        grad_rows[None], CTX, split_axis=2, concat_axis=0, tiled=True
    ).reshape(EXPERT_COUNT * CAP, MODEL_WIDTH)
    grad_expert_in, grad_expert_out = (
        lax.psum_scatter(
            grad_w_in.astype(jnp.bfloat16), FSDP, scatter_dimension=1, tiled=True
        ).astype(jnp.float32),
        lax.psum_scatter(
            grad_w_out.astype(jnp.bfloat16), FSDP, scatter_dimension=1, tiled=True
        ).astype(jnp.float32),
    )
    grad_chosen = gates * (grad_gate - jnp.sum(gates * grad_gate, axis=-1, keepdims=True))
    grad_logits = jnp.sum(indicator * grad_chosen[..., None], axis=1).astype(jnp.bfloat16)
    grad_router_part = lax.dot_general(
        ffn_in, grad_logits, contract_rows, preferred_element_type=jnp.float32
    )
    grad_ffn_in = lax.dot_general(
        grad_logits, router_w, contract_cols, preferred_element_type=jnp.float32
    )
    grad_ffn_in = grad_ffn_in + jnp.sum(
        grad_back[target].reshape(token_rows, TOP, MODEL_WIDTH), axis=1, dtype=jnp.float32
    )
    back_two, grad_ffn_gain = rms_backward(grad_ffn_in, ffn_unit, inverse_two, ffn_gain)
    grad_mixed = cot + back_two
    grad_attn = grad_mixed.astype(jnp.bfloat16)
    grad_wo_part = lax.dot_general(
        attention_output, grad_attn, contract_rows, preferred_element_type=jnp.float32
    )
    attention_output_gradient = lax.dot_general(
        grad_attn, output_w, contract_cols, preferred_element_type=jnp.float32
    ).astype(jnp.bfloat16)
    head_gradient = attention_output_gradient.reshape(
        token_rows, KEY_VALUE_HEADS, query_group, HEAD_SIZE
    )
    delta_rows = jnp.sum(
        head_gradient.astype(jnp.float32)
        * attention_output.reshape(token_rows, KEY_VALUE_HEADS, query_group, HEAD_SIZE).astype(
            jnp.float32
        ),
        axis=-1,
    )
    delta_rows = jnp.transpose(delta_rows, (1, 2, 0))
    init_back = (
        jnp.zeros((token_rows, KEY_VALUE_HEADS, query_group, HEAD_SIZE), jnp.float32),
        jnp.zeros((sequence_length, 2 * KEY_VALUE_HEADS * HEAD_SIZE), jnp.float32),
    )
    attend_key_section = lax.all_gather(key_matrix_rows, CTX, axis=0, tiled=True)
    attend_value_section = lax.all_gather(value_rows, CTX, axis=0, tiled=True)

    def compute(current):
        token_count = attend_key_section.shape[0]
        scores, visible, key_tensor = piece_scores(query_rows, attend_key_section, positions)
        value_tensor = attend_value_section.reshape(token_count, KEY_VALUE_HEADS, HEAD_SIZE)
        weights_full = jnp.where(visible, jnp.exp(scores - log_sum_rows[..., None]), 0.0)
        grad_probs = jnp.einsum(
            "tkgd,nkd->kgtn", head_gradient, value_tensor, preferred_element_type=jnp.float32
        )
        grad_scores = (weights_full * (grad_probs - delta_rows[..., None])).astype(jnp.bfloat16)
        grad_query = attn_scale * jnp.einsum(
            "kgtn,nkd->tkgd", grad_scores, key_tensor, preferred_element_type=jnp.float32
        )
        key_portion = attn_scale * jnp.einsum(
            "kgtn,tkgd->nkd", grad_scores, query_rows, preferred_element_type=jnp.float32
        )
        value_portion = jnp.einsum(
            "kgtn,tkgd->nkd",
            weights_full.astype(jnp.bfloat16),
            head_gradient,
            preferred_element_type=jnp.float32,
        )
        update = jnp.concatenate(
            [
                key_portion.reshape(token_count, KEY_VALUE_HEADS * HEAD_SIZE),
                value_portion.reshape(token_count, KEY_VALUE_HEADS * HEAD_SIZE),
            ],
            axis=1,
        )
        return (grad_query, update)

    grad_query, grad_keys_full = lax.cond(
        jnp.int32(0) <= positions[-1], compute, lambda current: current, init_back
    )
    local_gradients = lax.psum_scatter(
        grad_keys_full.astype(jnp.bfloat16), CTX, scatter_dimension=0, tiled=True
    ).astype(jnp.float32)
    query_back = (
        rotate_pairs(
            grad_query.reshape(token_rows, QUERY_HEADS, HEAD_SIZE), cosine_table, -sine_table
        )
        .astype(jnp.bfloat16)
        .reshape(token_rows, QUERY_HEADS * HEAD_SIZE)
    )
    key_backward_rows = (
        rotate_pairs(
            local_gradients[:, : KEY_VALUE_HEADS * HEAD_SIZE].reshape(
                token_rows, KEY_VALUE_HEADS, HEAD_SIZE
            ),
            cosine_table,
            -sine_table,
        )
        .astype(jnp.bfloat16)
        .reshape(token_rows, KEY_VALUE_HEADS * HEAD_SIZE)
    )
    value_backward_rows = local_gradients[:, KEY_VALUE_HEADS * HEAD_SIZE :].astype(jnp.bfloat16)
    grad_wq_part = lax.dot_general(
        attention_input, query_back, contract_rows, preferred_element_type=jnp.float32
    )
    grad_wk_part = lax.dot_general(
        attention_input, key_backward_rows, contract_rows, preferred_element_type=jnp.float32
    )
    grad_wv_part = lax.dot_general(
        attention_input, value_backward_rows, contract_rows, preferred_element_type=jnp.float32
    )
    grad_attn_in = lax.dot_general(
        query_back, query_w, contract_cols, preferred_element_type=jnp.float32
    )
    grad_attn_in = grad_attn_in + lax.dot_general(
        key_backward_rows, key_weight_matrix, contract_cols, preferred_element_type=jnp.float32
    )
    grad_attn_in = grad_attn_in + lax.dot_general(
        value_backward_rows, value_w, contract_cols, preferred_element_type=jnp.float32
    )
    back_one, grad_attn_gain = rms_backward(grad_attn_in, attn_unit, inverse_one, attn_gain)
    grad_input = grad_mixed + back_one
    partial_sums = (
        lax.psum_scatter(
            grad_attn_gain.astype(jnp.bfloat16), CTX, scatter_dimension=0, tiled=True
        ).astype(jnp.float32),
        lax.psum_scatter(
            grad_ffn_gain.astype(jnp.bfloat16), CTX, scatter_dimension=0, tiled=True
        ).astype(jnp.float32),
        lax.psum_scatter(
            grad_wq_part.astype(jnp.bfloat16), CTX, scatter_dimension=0, tiled=True
        ).astype(jnp.float32),
        lax.psum_scatter(
            grad_wk_part.astype(jnp.bfloat16), CTX, scatter_dimension=0, tiled=True
        ).astype(jnp.float32),
        lax.psum_scatter(
            grad_wv_part.astype(jnp.bfloat16), CTX, scatter_dimension=0, tiled=True
        ).astype(jnp.float32),
        lax.psum_scatter(
            grad_wo_part.astype(jnp.bfloat16), CTX, scatter_dimension=0, tiled=True
        ).astype(jnp.float32),
        lax.psum_scatter(
            grad_router_part.astype(jnp.bfloat16), CTX, scatter_dimension=0, tiled=True
        ).astype(jnp.float32),
    )
    summed = (
        lax.psum_scatter(
            partial_sums[0].astype(jnp.bfloat16), FSDP, scatter_dimension=0, tiled=True
        ).astype(jnp.float32),
        lax.psum_scatter(
            partial_sums[1].astype(jnp.bfloat16), FSDP, scatter_dimension=0, tiled=True
        ).astype(jnp.float32),
        lax.psum_scatter(
            partial_sums[2].astype(jnp.bfloat16), FSDP, scatter_dimension=0, tiled=True
        ).astype(jnp.float32),
        lax.psum_scatter(
            partial_sums[3].astype(jnp.bfloat16), FSDP, scatter_dimension=0, tiled=True
        ).astype(jnp.float32),
        lax.psum_scatter(
            partial_sums[4].astype(jnp.bfloat16), FSDP, scatter_dimension=0, tiled=True
        ).astype(jnp.float32),
        lax.psum_scatter(
            partial_sums[5].astype(jnp.bfloat16), FSDP, scatter_dimension=0, tiled=True
        ).astype(jnp.float32),
        lax.psum_scatter(
            partial_sums[6].astype(jnp.bfloat16), FSDP, scatter_dimension=0, tiled=True
        ).astype(jnp.float32),
    )
    return (
        layer_out[None],
        grad_input[None],
        summed[0],
        summed[1],
        summed[2],
        summed[3],
        summed[4],
        summed[5],
        summed[6],
        grad_expert_in,
        grad_expert_out,
    )


def swap(a, flip):
    return lax.ppermute(a, FSDP, [(i, i ^ flip) for i in range(NX * NC)])


def fast(
    hidden,
    routes,
    attn_norm,
    ffn_norm,
    w_q,
    key_weight,
    value_weight,
    w_o,
    router,
    expert_in,
    expert_out,
    cotangent,
):
    tokens = hidden.shape[1]
    group = QUERY_HEADS // KEY_VALUE_HEADS
    ctx_size = NZ * NY
    ctx = lax.axis_index(CTX)
    fsdp = lax.axis_index(FSDP)
    core = fsdp % NC
    rows = w_q.shape[0]
    quarter = expert_in.shape[1]
    kv_width = KEY_VALUE_HEADS * HEAD_SIZE
    q_width = QUERY_HEADS * HEAD_SIZE
    held = expert_in.shape[0] // NC
    bf = jnp.bfloat16
    f32 = jnp.float32
    positions = ctx * tokens + jnp.arange(tokens, dtype=jnp.int32)
    cosine_table, sine_table = rope_tables(positions)
    contract_rows = (((0,), (0,)), ((), ()))
    contract_cols = (((1,), (1,)), ((), ()))
    wide = hidden[0].astype(f32)
    cot = cotangent[0]

    def picked(w):
        pair = w.reshape(NC, held, *w.shape[1:])
        return (
            lax.dynamic_index_in_dim(pair, core, 0, False),
            lax.dynamic_index_in_dim(pair, 1 - core, 0, False),
        )

    def spread(mine, other):
        parts = jnp.stack([mine, swap(other, 1), swap(mine, 2), swap(other, 3)])
        order = jnp.arange(NX * NC) ^ fsdp
        whole = jnp.take(parts, order, axis=0)
        return jnp.transpose(whole, (1, 0, 2, 3)).reshape(held, NX * NC * quarter, mine.shape[2])

    pack_one = jnp.concatenate([w_q, key_weight, value_weight], axis=1)
    pack_two = jnp.concatenate(
        [w_o, router, attn_norm[:, None], ffn_norm[:, None], jnp.zeros((rows, 94), bf)], axis=1
    )
    one, two, cots = gather(
        [pack_one, pack_two, cot.astype(bf)],
        [
            Plan(0, (Z, Y, X, C,), (Z, Y, X, C,)),
            Plan(1, (Z, X, Y, C,), (Z, Y, X, C,)),
            Plan(2, (Z, Y, C,), (C, Z, Y,), rows=(0, tokens // 2)),
            Plan(2, (Y, Z, C,), (C, Z, Y,), rows=(tokens // 2, tokens // 2)),
        ],
        0,
        "gather_weights",
    )
    one, experts = lax.optimization_barrier((one, picked(expert_in) + picked(expert_out)))
    weight_in = spread(*experts[:2])
    weight_out = spread(*experts[2:])
    one = one.reshape(MODEL_WIDTH, -1)
    two = two.reshape(MODEL_WIDTH, -1)
    output_w = two[:, :MODEL_WIDTH]
    small = two[:, MODEL_WIDTH:]
    router_w = small[:, :EXPERT_COUNT]
    gains = lax.dot_general(
        jnp.eye(128, dtype=bf), small, contract_cols, preferred_element_type=f32
    )
    attn_gain, ffn_gain = gains[EXPERT_COUNT], gains[EXPERT_COUNT + 1]

    attn_unit, inverse_one, attention_input = rms_forward(wide, attn_gain)
    linear = jnp.dot(attention_input, one, preferred_element_type=f32)
    query_rows = (
        rotate_pairs(linear[:, :q_width].reshape(tokens, QUERY_HEADS, HEAD_SIZE), cosine_table, sine_table)
        .astype(bf)
        .reshape(tokens, KEY_VALUE_HEADS, group, HEAD_SIZE)
    )
    key_rows = (
        rotate_pairs(
            linear[:, q_width : q_width + kv_width].reshape(tokens, KEY_VALUE_HEADS, HEAD_SIZE),
            cosine_table,
            sine_table,
        )
        .astype(bf)
        .reshape(tokens, kv_width)
    )
    value_rows = linear[:, q_width + kv_width :].astype(bf)
    (kv,) = gather(
        [jnp.concatenate([key_rows, value_rows], axis=1)],
        [Plan(0, (Z, Y,), (Z, Y,))],
        1,
        "gather_keys",
    )
    kv = kv.reshape(ctx_size * tokens, 2 * kv_width)
    key_section, value_section = kv[:, :kv_width], kv[:, kv_width:]
    value_tensor = value_section.reshape(ctx_size * tokens, KEY_VALUE_HEADS, HEAD_SIZE)
    scores, visible, key_tensor = piece_scores(query_rows, key_section, positions)
    best = jnp.max(scores, axis=-1)
    weights = jnp.where(visible, jnp.exp(scores - best[..., None]), 0.0)
    total = jnp.sum(weights, axis=-1)
    weighted = jnp.einsum(
        "kgtn,nkd->kgtd", weights.astype(bf), value_tensor, preferred_element_type=f32
    )
    log_sum_rows = best + jnp.log(total)
    attention_output = (
        jnp.transpose(weighted / total[..., None], (2, 0, 1, 3)).reshape(tokens, q_width).astype(bf)
    )
    mixed = wide + jnp.dot(attention_output, output_w, preferred_element_type=f32)
    ffn_unit, inverse_two, ffn_in = rms_forward(mixed, ffn_gain)
    logits = jnp.dot(ffn_in, router_w, preferred_element_type=f32)
    route = routes[0]
    indicator = (route[:, :, None] == jnp.arange(EXPERT_COUNT, dtype=jnp.int32)).astype(f32)
    chosen = jnp.sum(indicator * logits[:, None, :], axis=-1)
    gates = jax.nn.softmax(chosen, axis=-1)
    gate_map = jnp.sum(indicator * (gates[..., None] + 1.0), axis=1) - 1.0

    payload = jnp.concatenate(
        [ffn_in, gate_map.astype(bf), jnp.zeros((tokens, 128 - EXPERT_COUNT), bf)], axis=1
    )
    cut = tokens * 3 // 4
    (all_tokens,) = gather(
        [payload],
        [
            Plan(0, (Z, Y, C,), (C, Z, Y,), rows=(0, cut)),
            Plan(0, (Y, Z, C,), (C, Z, Y,), rows=(cut, tokens - cut)),
        ],
        2,
        "gather_tokens",
    )
    blocks = NC * ctx_size
    inputs = all_tokens[:, :, :MODEL_WIDTH]
    first = (ctx * NC + core) * held
    own_gates = lax.dynamic_slice_in_dim(
        all_tokens[:, :, MODEL_WIDTH : MODEL_WIDTH + EXPERT_COUNT], first, held, axis=2
    ).astype(f32)
    chosen_here = own_gates >= 0.0
    before = (
        jnp.arange(tokens)[:, None] > jnp.arange(tokens)[None, :]
    ).astype(bf)
    slot = jnp.einsum(
        "ts,bse->bet", before, chosen_here.astype(bf), preferred_element_type=f32
    ).astype(jnp.int32)
    place_of = (
        (slot[:, :, None, :] == jnp.arange(CAP, dtype=jnp.int32)[None, None, :, None])
        & jnp.transpose(chosen_here, (0, 2, 1))[:, :, None, :]
    )
    pick = place_of.astype(bf)
    gate_t = jnp.transpose(own_gates, (0, 2, 1))
    row_gate = jnp.sum(jnp.where(place_of, gate_t[:, :, None, :], 0.0), axis=-1)
    row_gate = jnp.transpose(row_gate, (1, 0, 2)).reshape(held, blocks * CAP, 1)
    received = jnp.einsum("best,btd->ebsd", pick, inputs, preferred_element_type=f32).astype(bf)
    received = received.reshape(held, blocks * CAP, MODEL_WIDTH)
    cot_rows = jnp.einsum("best,btd->ebsd", pick, cots, preferred_element_type=f32).astype(bf)
    cot_rows = cot_rows.reshape(held, blocks * CAP, MODEL_WIDTH)
    act = jnp.einsum("erd,edf->erf", received, weight_in, preferred_element_type=f32)
    gate_part = act[..., :EXPERT_HIDDEN]
    up_part = act[..., EXPERT_HIDDEN:]
    sigma = jax.nn.sigmoid(gate_part)
    inner = gate_part * sigma * up_part
    scaled_inner = (inner * row_gate).astype(bf)
    produced = jnp.einsum(
        "erf,edf->erd", scaled_inner, weight_out, preferred_element_type=f32
    ).astype(bf)
    raw_inner = jnp.einsum("erd,edf->erf", cot_rows, weight_out, preferred_element_type=f32)
    row_grad_gate = jnp.sum(raw_inner * inner, axis=-1).reshape(held, blocks, CAP)
    grad_inner = raw_inner * row_gate
    grad_w_out = jnp.einsum("erd,erf->edf", cot_rows, scaled_inner, preferred_element_type=f32)
    grad_act = jnp.concatenate(
        [
            grad_inner * up_part * sigma * (1.0 + gate_part * (1.0 - sigma)),
            grad_inner * gate_part * sigma,
        ],
        axis=-1,
    ).astype(bf)
    grad_w_in = jnp.einsum("erd,erf->edf", received, grad_act, preferred_element_type=f32)
    grad_rows = jnp.einsum("erf,edf->erd", grad_act, weight_in, preferred_element_type=f32).astype(bf)
    out_part = jnp.einsum(
        "best,ebsd->btd",
        pick,
        produced.reshape(held, blocks, CAP, MODEL_WIDTH),
        preferred_element_type=f32,
    ).astype(bf)
    in_part = jnp.einsum(
        "best,ebsd->btd",
        pick,
        grad_rows.reshape(held, blocks, CAP, MODEL_WIDTH),
        preferred_element_type=f32,
    ).astype(bf)
    gate_grads = jnp.sum(
        jnp.where(place_of, jnp.transpose(row_grad_gate, (1, 0, 2))[..., None], 0.0), axis=2
    )
    gate_grads = jnp.transpose(gate_grads, (0, 2, 1))
    columns = jnp.arange(EXPERT_COUNT, dtype=jnp.int32)
    spread_gates = sum(
        jnp.where(columns == first + e, gate_grads[:, :, e : e + 1], 0.0) for e in range(held)
    )
    high = spread_gates.astype(bf)
    low = (spread_gates - high.astype(f32)).astype(bf)
    in_part = jnp.concatenate(
        [in_part, high, low, jnp.zeros((blocks, tokens, 128 - 2 * EXPERT_COUNT), bf)], axis=2
    )

    def cut_up(g):
        whole = g.astype(bf).reshape(held, NX * NC, quarter, g.shape[2])
        return [lax.dynamic_index_in_dim(whole, fsdp ^ j, 1, False) for j in range(NX * NC)]

    def collect(parts):
        mine = parts[0].astype(f32) + swap(parts[2], 2).astype(f32)
        other = swap(parts[1], 1).astype(f32) + swap(parts[3], 3).astype(f32)
        return jnp.where(
            core == 0, jnp.concatenate([mine, other]), jnp.concatenate([other, mine])
        )

    in_part, out_part, pieces = lax.optimization_barrier(
        (in_part, out_part, (cut_up(grad_w_in), cut_up(grad_w_out)))
    )
    grad_expert_in = collect(pieces[0])
    grad_expert_out = collect(pieces[1])

    gin, moe_out = reduce_scatter(
        [in_part, out_part],
        [Plan(0, (C, Y,), (C, Z, Y,)), Plan(1, (C, Y,), (C, Z, Y,))],
        [f32, f32],
        3,
        "return_tokens",
    )
    layer_out = (mixed + moe_out).astype(bf)
    grad_gate_map = gin[:, MODEL_WIDTH : MODEL_WIDTH + EXPERT_COUNT] + gin[
        :, MODEL_WIDTH + EXPERT_COUNT : MODEL_WIDTH + 2 * EXPERT_COUNT
    ]
    grad_gate = jnp.sum(indicator * grad_gate_map[:, None, :], axis=-1)
    grad_chosen = gates * (grad_gate - jnp.sum(gates * grad_gate, axis=-1, keepdims=True))
    grad_logits = jnp.sum(indicator * grad_chosen[..., None], axis=1).astype(bf)
    grad_router_part = lax.dot_general(
        ffn_in, grad_logits, contract_rows, preferred_element_type=f32
    )
    grad_ffn_in = gin[:, :MODEL_WIDTH] + lax.dot_general(
        grad_logits, router_w, contract_cols, preferred_element_type=f32
    )
    back_two, _ = rms_backward(grad_ffn_in, ffn_unit, inverse_two, ffn_gain)
    grad_mixed = cot + back_two
    grad_attn = grad_mixed.astype(bf)
    grad_wo_part = lax.dot_general(
        attention_output, grad_attn, contract_rows, preferred_element_type=f32
    )
    attention_output_gradient = lax.dot_general(
        grad_attn, output_w, contract_cols, preferred_element_type=f32
    ).astype(bf)
    head_gradient = attention_output_gradient.reshape(tokens, KEY_VALUE_HEADS, group, HEAD_SIZE)
    delta_rows = jnp.sum(
        head_gradient.astype(f32)
        * attention_output.reshape(tokens, KEY_VALUE_HEADS, group, HEAD_SIZE).astype(f32),
        axis=-1,
    )
    delta_rows = jnp.transpose(delta_rows, (1, 2, 0))
    weights_full = jnp.where(visible, jnp.exp(scores - log_sum_rows[..., None]), 0.0)
    grad_probs = jnp.einsum(
        "tkgd,nkd->kgtn", head_gradient, value_tensor, preferred_element_type=f32
    )
    grad_scores = (weights_full * (grad_probs - delta_rows[..., None])).astype(bf)
    grad_query = attn_scale * jnp.einsum(
        "kgtn,nkd->tkgd", grad_scores, key_tensor, preferred_element_type=f32
    )
    key_portion = attn_scale * jnp.einsum(
        "kgtn,tkgd->nkd", grad_scores, query_rows, preferred_element_type=f32
    )
    value_portion = jnp.einsum(
        "kgtn,tkgd->nkd", weights_full.astype(bf), head_gradient, preferred_element_type=f32
    )
    update = jnp.concatenate(
        [
            key_portion.astype(bf).reshape(ctx_size, tokens, kv_width),
            value_portion.astype(bf).reshape(ctx_size, tokens, kv_width),
        ],
        axis=2,
    )
    (local_gradients,) = reduce_scatter(
        [update], [Plan(0, (Y,), (Z, Y,))], [f32], 4, "return_keys"
    )
    query_back = (
        rotate_pairs(
            grad_query.reshape(tokens, QUERY_HEADS, HEAD_SIZE), cosine_table, -sine_table
        )
        .astype(bf)
        .reshape(tokens, q_width)
    )
    key_back = (
        rotate_pairs(
            local_gradients[:, :kv_width].reshape(tokens, KEY_VALUE_HEADS, HEAD_SIZE),
            cosine_table,
            -sine_table,
        )
        .astype(bf)
        .reshape(tokens, kv_width)
    )
    back = jnp.concatenate([query_back, key_back, local_gradients[:, kv_width:].astype(bf)], axis=1)
    grad_one = lax.dot_general(attention_input, back, contract_rows, preferred_element_type=f32)
    grad_attn_in = lax.dot_general(back, one, contract_cols, preferred_element_type=f32)
    back_one, _ = rms_backward(grad_attn_in, attn_unit, inverse_one, attn_gain)
    grad_input = grad_mixed + back_one
    attn_gain_grad = jnp.sum(grad_attn_in * attn_unit, axis=0)
    ffn_gain_grad = jnp.sum(grad_ffn_in * ffn_unit, axis=0)
    grad_two = jnp.concatenate(
        [
            grad_wo_part,
            grad_router_part,
            attn_gain_grad[:, None],
            ffn_gain_grad[:, None],
            jnp.zeros((MODEL_WIDTH, 94), f32),
        ],
        axis=1,
    )
    sum_one, sum_two = reduce_scatter(
        [
            grad_one.astype(bf).reshape(-1, rows, grad_one.shape[1]),
            grad_two.astype(bf).reshape(-1, rows, grad_two.shape[1]),
        ],
        [Plan(0, (C, X, Y,), (Z, Y, X, C,)), Plan(1, (C, Y, X,), (Z, Y, X, C,))],
        [f32, f32],
        5,
        "return_weights",
    )
    at = MODEL_WIDTH + EXPERT_COUNT
    return (
        layer_out[None],
        grad_input[None],
        sum_two[:, at],
        sum_two[:, at + 1],
        sum_one[:, :q_width],
        sum_one[:, q_width : q_width + kv_width],
        sum_one[:, q_width + kv_width :],
        sum_two[:, :MODEL_WIDTH],
        sum_two[:, MODEL_WIDTH:at],
        grad_expert_in,
        grad_expert_out,
    )


def solution(mesh):
    placed = (
        P(FSDP, CTX, None),
        P(FSDP, CTX, None),
        P((CTX, FSDP)),
        P((CTX, FSDP)),
        P((CTX, FSDP), None),
        P((CTX, FSDP), None),
        P((CTX, FSDP), None),
        P((CTX, FSDP), None),
        P((CTX, FSDP), None),
        P(CTX, FSDP, None),
        P(CTX, FSDP, None),
        P(FSDP, CTX, None),
    )
    small = mesh.shape[CTX] == NZ * NY and mesh.shape[FSDP] == NX * NC
    return jax.shard_map(
        fast if small else local,
        mesh=mesh,
        in_specs=placed,
        out_specs=(
            P(FSDP, CTX, None),
            P(FSDP, CTX, None),
            P((CTX, FSDP)),
            P((CTX, FSDP)),
            P((CTX, FSDP), None),
            P((CTX, FSDP), None),
            P((CTX, FSDP), None),
            P((CTX, FSDP), None),
            P((CTX, FSDP), None),
            P(CTX, FSDP, None),
            P(CTX, FSDP, None),
        ),
        check_vma=False,
    )
```

```python
import functools
import itertools

import jax
import jax.numpy as jnp
from jax import lax
from jax.experimental import pallas as pl
from jax.experimental.pallas import tpu as pltpu
from jax.sharding import PartitionSpec as P


NY = 2
NZ = 4
NX = 2
NC = 2
DEV = pl.DeviceIdType.MESH
CTX, FSDP = "ctx", "fsdp"
Z, Y, X, C = 0, 1, 2, 3
SIZES = {Z: NZ, Y: NY, X: NX, C: NC}
UP, DOWN = 4, 5


class Plan:
    def __init__(self, ref, order, index, rows=None):
        self.ref, self.order, self.index, self.rows = ref, order, index, rows
        self.blocks = 1
        for d in index:
            self.blocks *= SIZES[d]


class Place:
    def __init__(self):
        ctx = lax.axis_index(CTX)
        fsdp = lax.axis_index(FSDP)
        self.at = {Z: ctx // NY, Y: ctx % NY, X: fsdp // NC, C: fsdp % NC}
        z = self.at[Z]
        low = z < NZ // 2
        base = jnp.where(low, z, NZ - 1 - z)
        near = [base, 1 - base, jnp.int32(2), jnp.int32(3)]
        self.order = [z] + [jnp.where(low, k, NZ - 1 - k) for k in near[1:]]

    def device(self, dim, value):
        spot = dict(self.at)
        spot[dim] = value
        return (spot[Z] * NY + spot[Y], spot[X] * NC + spot[C])

    def across(self, dim):
        return self.device(dim, 1 - self.at[dim])

    def along(self, step):
        return self.device(Z, self.at[Z] + step)

    def coords(self, z_from, flips):
        spot = {d: (1 - self.at[d] if d in flips else self.at[d]) for d in (Y, X, C)}
        spot[Z] = z_from
        return spot


def flat_index(spot, dims):
    index = 0
    for d in dims:
        index = index * SIZES[d] + spot[d]
    return index


def subsets(dims):
    return [c for n in range(len(dims) + 1) for c in itertools.combinations(dims, n)]


def greet(place, dims):
    barrier = pltpu.get_barrier_semaphore()
    z = place.at[Z]
    count = jnp.int32(0)
    for d in dims:
        if d == Z:
            @pl.when(z > 0)
            def _():
                pl.semaphore_signal(barrier, inc=1, device_id=place.along(-1), device_id_type=DEV)

            @pl.when(z < NZ - 1)
            def _():
                pl.semaphore_signal(barrier, inc=1, device_id=place.along(1), device_id_type=DEV)

            count = count + jnp.where(z > 0, 1, 0) + jnp.where(z < NZ - 1, 1, 0)
        else:
            pl.semaphore_signal(barrier, inc=1, device_id=place.across(d), device_id_type=DEV)
            count = count + 1
    pl.semaphore_wait(barrier, count)


def gather_events(order):
    pairs = [d for d in order if d != Z]
    events = [(k, f) for k in range(NZ) for f in subsets(pairs)]
    return sorted(events, key=lambda e: (e[0] + len(e[1]), len(e[1])))


def gather_sends(order, k, flips):
    z_at = order.index(Z)
    last = max([order.index(d) for d in flips] + ([z_at] if k > 0 else []) + [-1])
    out = []
    for position, d in enumerate(order):
        if position > last:
            out.extend([UP, DOWN] if d == Z else [d])
    if k > 0 and last == z_at:
        out.extend([UP, DOWN])
    return out


def gather_kernel(plans, n_in, *refs):
    ins, outs = refs[:n_in], refs[n_in : 2 * n_in]
    send_sem, recv_sem, own_sem = refs[2 * n_in :]
    place = Place()
    z = place.at[Z]
    greet(place, sorted({d for p in plans for d in p.order}))
    pending = []
    slot = 0
    queue = []
    for n, plan in enumerate(plans):
        for rank, event in enumerate(gather_events(plan.order)):
            queue.append((rank / len(gather_events(plan.order)), n, event))
    queue.sort(key=lambda q: (q[0], q[1]))
    bases = [sum(p.blocks for p in plans[:n]) for n in range(len(plans))]
    for _, n, (k, flips) in queue:
        plan = plans[n]
        src = ins[plan.ref]
        out = outs[plan.ref]
        rows = plan.rows
        z_from = place.order[k]
        spot = place.coords(z_from, flips)
        index = flat_index(spot, plan.index)
        target = out.at[index] if rows is None else out.at[index, pl.ds(rows[0], rows[1])]
        sem = recv_sem.at[bases[n] + index]
        own = k == 0 and not flips
        source = (src if rows is None else src.at[pl.ds(rows[0], rows[1])]) if own else target
        if not own:
            pltpu.make_async_remote_copy(
                src_ref=target, dst_ref=target, send_sem=own_sem.at[0], recv_sem=sem,
                device_id=place.across(C), device_id_type=DEV,
            ).wait_recv()
        for way in gather_sends(plan.order, k, flips):
            if way in (UP, DOWN):
                step = 1 if way == UP else -1
                go = z < NZ - 1 if way == UP else z > 0
                if k > 0:
                    go = jnp.logical_and(go, z_from < z if way == UP else z_from > z)
                dest = place.device(Z, jnp.clip(z + step, 0, NZ - 1))
            else:
                go, dest = None, place.across(way)
            copy = pltpu.make_async_remote_copy(
                src_ref=source, dst_ref=target, send_sem=send_sem.at[slot], recv_sem=sem,
                device_id=dest, device_id_type=DEV,
            )
            slot += 1
            if go is None:
                copy.start()
            else:
                pl.when(go)(copy.start)
            pending.append((go, copy.wait_send))
        if own:
            copy = pltpu.make_async_copy(source, target, own_sem.at[1 + n])
            copy.start()
            pending.append((None, copy.wait))
    for go, wait in pending:
        if go is None:
            wait()
        else:
            pl.when(go)(wait)


def gather(arrays, plans, collective_id, name):
    n = len(arrays)
    sends = sum(len(gather_sends(p.order, k, f)) for p in plans for k, f in gather_events(p.order))
    blocks = {p.ref: p.blocks for p in plans}
    return pl.pallas_call(
        functools.partial(gather_kernel, plans, n),
        out_shape=[jax.ShapeDtypeStruct((blocks[i],) + a.shape, a.dtype) for i, a in enumerate(arrays)],
        in_specs=[pl.BlockSpec(memory_space=pltpu.VMEM)] * n,
        out_specs=[pl.BlockSpec(memory_space=pl.ANY)] * n,
        scratch_shapes=[
            pltpu.SemaphoreType.DMA((sends,)),
            pltpu.SemaphoreType.DMA((sum(p.blocks for p in plans),)),
            pltpu.SemaphoreType.DMA((1 + len(plans),)),
        ],
        compiler_params=pltpu.CompilerParams(collective_id=collective_id, has_side_effects=True),
        name=name,
    )(*arrays)


def add_into(acc, other):
    acc[...] = (acc[...].astype(jnp.float32) + other[...].astype(jnp.float32)).astype(acc.dtype)


def reduce_kernel(plans, n_in, *refs):
    ins, outs = refs[:n_in], refs[n_in : 2 * n_in]
    rest = list(refs[2 * n_in :])
    send_sem, recv_sem, own_sem = rest[:3]
    buffers = rest[3:]
    place = Place()
    z = place.at[Z]
    greet(place, sorted({d for p in plans for d in p.order} | {Z}))
    pending = []
    slots = [0, 0]

    def push(source, target, sem, dest):
        copy = pltpu.make_async_remote_copy(
            src_ref=source, dst_ref=target, send_sem=send_sem.at[slots[0]], recv_sem=sem,
            device_id=dest, device_id_type=DEV,
        )
        slots[0] += 1
        copy.start()
        pending.append(copy)

    def arrived(target, sem):
        pltpu.make_async_remote_copy(
            src_ref=target, dst_ref=target, send_sem=own_sem.at[0], recv_sem=sem,
            device_id=place.across(C), device_id_type=DEV,
        ).wait_recv()

    work = []
    far = list(reversed(range(NZ)))
    own_slot = 1
    state = []
    base = 0
    for n, plan in enumerate(plans):
        dims = plan.order
        acc = buffers[0]
        levels = buffers[1 : 1 + len(dims)]
        chain = buffers[1 + len(dims)]
        buffers = buffers[2 + len(dims) :]
        kept = [subsets(dims[p + 1 :]) for p in range(len(dims))]
        counts = [NZ * len(f) for f in kept]
        level_base = [base + sum(counts[:p]) for p in range(len(dims))]
        chain_base = base + sum(counts)
        base = chain_base + 2 * NZ
        state.append((acc, levels, chain, kept, level_base, chain_base))
        own_copies = {}
        src = ins[plan.ref]
        for k in far:
            for f in kept[0]:
                gone = flat_index(place.coords(place.order[k], (dims[0],) + f), plan.index)
                spot = place.order[k] * len(kept[0]) + kept[0].index(f)
                work.append((0, n, k, f, gone, spot))
                mine = flat_index(place.coords(place.order[k], f), plan.index)
                copy = pltpu.make_async_copy(src.at[mine], acc.at[spot], own_sem.at[own_slot])
                own_slot += 1
                own_copies[(k, f)] = copy
        state[-1] += (own_copies,)
    for _, n, k, f, gone, spot in sorted(work, key=lambda w: (-w[2],)):
        plan = plans[n]
        acc, levels, chain, kept, level_base, chain_base, own_copies = state[n]
        push(ins[plan.ref].at[gone], levels[0].at[spot], recv_sem.at[level_base[0] + spot], place.across(plan.order[0]))
        own_copies[(k, f)].start()

    def level_step(n, p, k):
        plan = plans[n]
        dims = plan.order
        acc, levels, chain, kept, level_base, chain_base, own_copies = state[n]
        for f in sorted(kept[p], key=lambda f: -len(f)):
            spot = place.order[k] * len(kept[p]) + kept[p].index(f)
            at = place.order[k] * len(kept[0]) + kept[0].index(f)
            if p == 0:
                own_copies[(k, f)].wait()
            arrived(levels[p].at[spot], recv_sem.at[level_base[p] + spot])
            add_into(acc.at[at], levels[p].at[spot])
            later = p + 1
            if later < len(dims) and dims[later] in f:
                left = tuple(d for d in f if d != dims[later])
                there = place.order[k] * len(kept[later]) + kept[later].index(left)
                push(
                    acc.at[at], levels[later].at[there],
                    recv_sem.at[level_base[later] + there], place.across(dims[later]),
                )

    def chain_step(n, k):
        plan = plans[n]
        acc, levels, chain, kept, level_base, chain_base, own_copies = state[n]
        dest = place.order[k]
        up = dest > z
        lane = jnp.where(up, 0, 1)
        at = dest * len(kept[0])
        spot = lane * NZ + dest

        @pl.when(jnp.where(up, z > 0, z < NZ - 1))
        def _():
            arrived(chain.at[spot], recv_sem.at[chain_base + spot])
            add_into(acc.at[at], chain.at[spot])

        push(acc.at[at], chain.at[spot], recv_sem.at[chain_base + spot], place.along(jnp.where(up, 1, -1)))

    most = max(len(p.order) for p in plans)
    for step in range(NZ + most):
        for n, plan in enumerate(plans):
            for p in range(len(plan.order)):
                if 0 <= step - p < NZ:
                    level_step(n, p, far[step - p])
            p = len(plan.order)
            if 0 <= step - p < NZ - 1:
                chain_step(n, far[step - p])
    for n, plan in enumerate(plans):
        acc, levels, chain, kept, level_base, chain_base, own_copies = state[n]
        at = z * len(kept[0])

        @pl.when(z > 0)
        def _():
            spot = z
            arrived(chain.at[spot], recv_sem.at[chain_base + spot])
            add_into(acc.at[at], chain.at[spot])

        @pl.when(z < NZ - 1)
        def _():
            spot = NZ + z
            arrived(chain.at[spot], recv_sem.at[chain_base + spot])
            add_into(acc.at[at], chain.at[spot])

        outs[plan.ref][...] = acc[at].astype(outs[plan.ref].dtype)
    for copy in pending:
        copy.wait_send()


def reduce_scatter(arrays, plans, out_dtypes, collective_id, name):
    n = len(arrays)
    scratch = []
    sends = recvs = owns = 0
    for p in plans:
        a = arrays[p.ref]
        block = a.shape[1:]
        kept = [len(subsets(p.order[q + 1 :])) for q in range(len(p.order))]
        scratch.append(pltpu.VMEM((NZ * kept[0],) + block, a.dtype))
        for q in kept:
            scratch.append(pltpu.VMEM((NZ * q,) + block, a.dtype))
        scratch.append(pltpu.VMEM((2 * NZ,) + block, a.dtype))
        sends += NZ * sum(kept) + NZ - 1
        recvs += NZ * sum(kept) + 2 * NZ
        owns += NZ * kept[0]
    return pl.pallas_call(
        functools.partial(reduce_kernel, plans, n),
        out_shape=[jax.ShapeDtypeStruct(a.shape[1:], d) for a, d in zip(arrays, out_dtypes)],
        in_specs=[pl.BlockSpec(memory_space=pl.ANY)] * n,
        out_specs=[pl.BlockSpec(memory_space=pltpu.VMEM)] * n,
        scratch_shapes=[
            pltpu.SemaphoreType.DMA((sends,)),
            pltpu.SemaphoreType.DMA((recvs,)),
            pltpu.SemaphoreType.DMA((1 + owns,)),
        ]
        + scratch,
        compiler_params=pltpu.CompilerParams(
            collective_id=collective_id, has_side_effects=True, vmem_limit_bytes=60 * 1024 * 1024
        ),
        name=name,
    )(*arrays)


class Gather:
    def __init__(self, place, plan, src, out, send_sem, recv_sem, spare_sem, slot, base):
        self.place, self.plan, self.src, self.out = place, plan, src, out
        self.send_sem, self.recv_sem, self.spare_sem = send_sem, recv_sem, spare_sem
        self.slot, self.base = slot, base
        self.pending = []

    @staticmethod
    def sends(plan):
        return sum(len(gather_sends(plan.order, k, f)) for k, f in gather_events(plan.order))

    def step(self, k, flips):
        place, plan = self.place, self.plan
        z = place.at[Z]
        z_from = place.order[k]
        index = flat_index(place.coords(z_from, flips), plan.index)
        rows = plan.rows
        target = self.out.at[index] if rows is None else self.out.at[index, pl.ds(rows[0], rows[1])]
        sem = self.recv_sem.at[self.base + index]
        own = k == 0 and not flips
        source = target
        if own:
            source = self.src if rows is None else self.src.at[pl.ds(rows[0], rows[1])]
        else:
            pltpu.make_async_remote_copy(
                src_ref=target, dst_ref=target, send_sem=self.spare_sem, recv_sem=sem,
                device_id=place.across(C), device_id_type=DEV,
            ).wait_recv()
        for way in gather_sends(plan.order, k, flips):
            if way in (UP, DOWN):
                step = 1 if way == UP else -1
                go = z < NZ - 1 if way == UP else z > 0
                if k > 0:
                    go = jnp.logical_and(go, z_from < z if way == UP else z_from > z)
                dest = place.device(Z, jnp.clip(z + step, 0, NZ - 1))
            else:
                go, dest = None, place.across(way)
            copy = pltpu.make_async_remote_copy(
                src_ref=source, dst_ref=target, send_sem=self.send_sem.at[self.slot], recv_sem=sem,
                device_id=dest, device_id_type=DEV,
            )
            self.slot += 1
            if go is None:
                copy.start()
            else:
                pl.when(go)(copy.start)
            self.pending.append((go, copy.wait_send))

    def finish(self):
        for go, wait in self.pending:
            if go is None:
                wait()
            else:
                pl.when(go)(wait)


class Reduce:
    def __init__(self, place, plan, held, levels, chain, send_sem, recv_sem, spare_sem):
        self.place, self.plan, self.held, self.levels, self.chain = place, plan, held, levels, chain
        self.send_sem, self.recv_sem, self.spare_sem = send_sem, recv_sem, spare_sem
        dims = plan.order
        self.kept = [subsets(dims[p + 1 :]) for p in range(len(dims))]
        self.base = [NZ * sum(len(f) for f in self.kept[:p]) for p in range(len(dims) + 1)]
        self.slot = 0
        self.pending = []

    @staticmethod
    def counts(plan):
        kept = [NZ * len(subsets(plan.order[p + 1 :])) for p in range(len(plan.order))]
        return kept, sum(kept) + NZ - 1, sum(kept) + NZ + 1

    def push(self, source, target, sem, dest):
        copy = pltpu.make_async_remote_copy(
            src_ref=source, dst_ref=target, send_sem=self.send_sem.at[self.slot], recv_sem=sem,
            device_id=dest, device_id_type=DEV,
        )
        self.slot += 1
        copy.start()
        self.pending.append(copy)

    def arrived(self, target, sem):
        pltpu.make_async_remote_copy(
            src_ref=target, dst_ref=target, send_sem=self.spare_sem, recv_sem=sem,
            device_id=self.place.across(C), device_id_type=DEV,
        ).wait_recv()

    def block(self, k, flips):
        return flat_index(self.place.coords(self.place.order[k], flips), self.plan.index)

    def first(self, k):
        dim = self.plan.order[0]
        for n, f in enumerate(self.kept[0]):
            spot = self.place.order[k] * len(self.kept[0]) + n
            self.push(
                self.held.at[self.block(k, (dim,) + f)], self.levels[0].at[spot],
                self.recv_sem.at[spot], self.place.across(dim),
            )

    def level(self, p, k):
        dims = self.plan.order
        z_to = self.place.order[k]
        for f in sorted(self.kept[p], key=lambda f: -len(f)):
            spot = z_to * len(self.kept[p]) + self.kept[p].index(f)
            mine = self.held.at[self.block(k, f)]
            self.arrived(self.levels[p].at[spot], self.recv_sem.at[self.base[p] + spot])
            add_into(mine, self.levels[p].at[spot])
            later = p + 1
            if later < len(dims) and dims[later] in f:
                left = tuple(d for d in f if d != dims[later])
                there = z_to * len(self.kept[later]) + self.kept[later].index(left)
                self.push(
                    mine, self.levels[later].at[there],
                    self.recv_sem.at[self.base[later] + there], self.place.across(dims[later]),
                )

    def along(self, k):
        z = self.place.at[Z]
        dest = self.place.order[k]
        up = dest > z
        spot = dest + jnp.where(up, 1, 0)
        mine = self.held.at[self.block(k, ())]
        sem = self.recv_sem.at[self.base[-1] + spot]

        @pl.when(jnp.where(up, z > 0, z < NZ - 1))
        def _():
            self.arrived(self.chain.at[spot], sem)
            add_into(mine, self.chain.at[spot])

        self.push(mine, self.chain.at[spot], sem, self.place.along(jnp.where(up, 1, -1)))

    def last(self, out):
        z = self.place.at[Z]
        mine = self.held.at[self.block(0, ())]
        for go, spot in ((z > 0, z + 1), (z < NZ - 1, z)):

            @pl.when(go)
            def _():
                self.arrived(self.chain.at[spot], self.recv_sem.at[self.base[-1] + spot])
                add_into(mine, self.chain.at[spot])

        out[...] = mine[...].astype(out.dtype)

    def steps(self):
        depth = len(self.plan.order)
        far = list(reversed(range(NZ)))
        out = []
        for t in range(NZ + depth):
            for p in range(depth):
                if 0 <= t - p < NZ:
                    out.append(functools.partial(self.level, p, far[t - p]))
            if 0 <= t - depth < NZ - 1:
                out.append(functools.partial(self.along, far[t - depth]))
        return out

    def finish(self):
        for copy in self.pending:
            copy.wait_send()


def tile_up(n, m):
    return (n + m - 1) // m * m


def columns_of(width, chunk=512):
    return [(i, min(chunk, width - i)) for i in range(0, width, chunk)]


def moe_kernel(plans, back, width, hidden, cap, *refs):
    payload, cots, w_own, w_core, w_x, w_both = refs[:6]
    gin_out, moe_out = refs[6:8]
    grads = refs[8:12]
    (
        seen, cot_seen, weights, taken, cot_taken, rows_buf, scaled, grad_act, pick, stage,
        lvl_a0, lvl_a1, chain_a, lvl_b0, lvl_b1, chain_b,
        send_sem, recv_sem, spare_sem, send_a, recv_a, send_b, recv_b, load_sem, store_sem,
    ) = refs[12:]
    bf, f32 = jnp.bfloat16, jnp.float32
    place = Place()
    count = payload.shape[0]
    pair = 2 * cap
    wide = width + 128
    quarter = width // (NX * NC)
    half = NZ * pair
    lanes = pick.shape[2]
    held = weights.shape[0]
    fsdp = place.at[X] * NC + place.at[C]
    first = (((place.at[Z] * NY + place.at[Y]) * NC) + place.at[C]) * held

    loads = []
    for j, ref in enumerate((w_own, w_core, w_x, w_both)):
        rows = pl.ds(pl.multiple_of((fsdp ^ j) * quarter, quarter), quarter)
        for e in range(held):
            loads.append(pltpu.make_async_copy(ref.at[e], weights.at[e, rows], load_sem.at[len(loads)]))
    base_of = lambda h, k: (jnp.where(h == 0, place.at[C], 1 - place.at[C]) * NZ + place.order[k]) * NY
    cot_loads = {}
    for k in range(NZ):
        for h in range(2):
            at = pl.ds(base_of(h, k), NY)
            cot_loads[(h, k)] = pltpu.make_async_copy(cots.at[at], cot_seen.at[at], load_sem.at[len(loads) + len(cot_loads)])

    greet(place, (Z, Y, C))
    ways = []
    send_at = 0
    for n, plan in enumerate(plans):
        ways.append(Gather(place, plan, payload, seen, send_sem, recv_sem, spare_sem, send_at, n * plan.blocks))
        send_at += Gather.sends(plan)
    for way in ways:
        way.step(0, ())
    for key in cot_loads:
        cot_loads[key].start()
    for copy in loads:
        copy.start()
    seen[flat_index(place.at, plans[0].index)] = payload[...]

    row_id = lax.broadcasted_iota(jnp.int32, (NY * count, NY * count), 0)
    col_id = lax.broadcasted_iota(jnp.int32, (NY * count, NY * count), 1)
    earlier = jnp.logical_and(col_id < row_id, col_id // count == row_id // count).astype(bf)
    lane_id = lax.broadcasted_iota(jnp.int32, (1, 128), 1)
    here = [(lane_id == first + e).astype(f32) for e in range(held)]
    pick_lane = lax.broadcasted_iota(jnp.int32, (NY * count, lanes), 1).astype(f32)
    y_shift = (lax.broadcasted_iota(jnp.int32, (NY * count, 1), 0) // count * cap).astype(f32)

    def dispatch(source, target, h, k, cols):
        at = pl.ds(base_of(h, k), NY)
        r = (h * NZ + k) * pair
        for c0, cn in cols:
            block = source[at, :, c0 : c0 + cn].reshape(NY * count, cn)
            got = lax.dot_general(
                pick[h * NZ + k], block, (((0,), (0,)), ((), ())), preferred_element_type=f32
            ).astype(bf)
            for e in range(held):
                target[e, r : r + pair, c0 : c0 + cn] = got[e * pair : (e + 1) * pair]

    def cot_chunk(h, k):
        cot_loads[(h, k)].wait()
        at = pl.ds(base_of(h, k), NY)
        chosen = cot_seen[at, :, width:wide].reshape(NY * count, 128)
        before = jnp.dot(earlier, chosen, preferred_element_type=f32)
        picked = None
        for e in range(held):
            is_here = jnp.sum(chosen.astype(f32) * here[e], axis=1, keepdims=True)
            slot = jnp.sum(before * here[e], axis=1, keepdims=True) + y_shift + e * pair
            target = jnp.where(is_here > 0.5, slot, -1.0)
            hit = pick_lane == target
            picked = hit if picked is None else jnp.logical_or(picked, hit)
        pick[h * NZ + k] = picked.astype(f32).astype(bf)
        dispatch(cot_seen, cot_taken, h, k, columns_of(width))

    def hidden_chunk(h, e, n, tile):
        rows = pl.ds(h * half, half)
        tokens_in = taken[e, rows, :width]
        gate = jnp.sum(taken[e, rows, width:wide].astype(f32) * here[e], axis=1, keepdims=True)
        col = n * tile
        g = jnp.dot(tokens_in, weights[e, :, col : col + tile], preferred_element_type=f32)
        u = jnp.dot(tokens_in, weights[e, :, hidden + col : hidden + col + tile], preferred_element_type=f32)
        raw = jnp.dot(
            cot_taken[e, rows, :], weights[e, :, 2 * hidden + col : 2 * hidden + col + tile], preferred_element_type=f32
        )
        s = jax.nn.sigmoid(g)
        gs = g * s
        inner = gs * u
        scaled[e, rows, col : col + tile] = (inner * gate).astype(bf)
        grad_inner = raw * gate
        grad_act[e, rows, col : col + tile] = (grad_inner * u * s * (1.0 + g * (1.0 - s))).astype(bf)
        grad_act[e, rows, hidden + col : hidden + col + tile] = (grad_inner * gs).astype(bf)
        return jnp.sum(raw * inner, axis=1, keepdims=True)

    def hidden_part(h, e):
        tile = min(256, hidden)
        gate_grad = sum(hidden_chunk(h, e, n, tile) for n in range(hidden // tile))
        high = gate_grad.astype(bf).astype(f32)
        there = pl.ds(h * half, half)
        apart = (lane_id == EXPERT_COUNT + first + e).astype(f32)
        rows_buf[e, there, width:wide] = (high * here[e] + (gate_grad - high) * apart).astype(bf)

    def project(h, e, left, weight_cols):
        rows = pl.ds(h * half, half)
        lo, n = weight_cols
        for c0, cn in columns_of(width):
            rows_buf[e, rows, c0 : c0 + cn] = lax.dot_general(
                left[e, rows, :], weights[e, c0 : c0 + cn, lo : lo + n], (((1,), (1,)), ((), ())), preferred_element_type=f32
            ).astype(bf)

    def combine(target, h, k, cols):
        at = pl.ds(base_of(h, k), NY)
        r = (h * NZ + k) * pair
        for c0, cn in cols:
            parts = [rows_buf[e, r : r + pair, c0 : c0 + cn] for e in range(held)]
            if lanes > held * pair:
                parts.append(jnp.zeros((lanes - held * pair, cn), bf))
            got = jnp.dot(pick[h * NZ + k], jnp.concatenate(parts, axis=0), preferred_element_type=f32)
            target[at, :, c0 : c0 + cn] = got.astype(bf).reshape(NY, count, cn)

    stores = []

    def weight_grad(e, j):
        rows = pl.ds(pl.multiple_of((fsdp ^ j) * quarter, 128), quarter)
        slot = len(stores) % 2
        if len(stores) >= 2:
            stores[-2].wait()
        for c0, cn in columns_of(2 * hidden):
            stage[slot, :, c0 : c0 + cn] = lax.dot_general(
                taken[e, :, rows], grad_act[e, :, c0 : c0 + cn], (((0,), (0,)), ((), ())), preferred_element_type=f32
            ).astype(bf)
        stage[slot, :, 2 * hidden :] = lax.dot_general(
            cot_taken[e, :, rows], scaled[e], (((0,), (0,)), ((), ())), preferred_element_type=f32
        ).astype(bf)
        copy = pltpu.make_async_copy(stage.at[slot], grads[j].at[e], store_sem.at[len(stores)])
        copy.start()
        stores.append(copy)

    work = [functools.partial(cot_chunk, h, k) for h in range(NC) for k in range(NZ)]
    all_cols = columns_of(width) + [(width, 128)]
    ready = {(h, k): 0 for h in range(NC) for k in range(NZ)}
    ready[(0, 0)] = 1
    for k, flips in gather_events(plans[0].order)[1:]:
        for way in ways:
            way.step(k, flips)
        key = (1 if C in flips else 0, k)
        ready[key] += 1
        if ready[key] == NY:
            work.append(functools.partial(dispatch, seen, taken, *key, all_cols))
        for _ in range(min(len(work), 1 if k < NZ - 1 else 2)):
            work.pop(0)()
    for chunk in work:
        chunk()
    for copy in loads:
        copy.wait()
    for h in range(NC):
        for e in range(held):
            hidden_part(h, e)
    for way in ways:
        way.finish()

    far = list(reversed(range(NZ)))
    spare = spare_sem
    out_way = Reduce(place, back, seen.at[:, :, pl.ds(0, width)], (lvl_a0, lvl_a1), chain_a, send_a, recv_a, spare)
    in_way = Reduce(place, back, cot_seen, (lvl_b0, lvl_b1), chain_b, send_b, recv_b, spare)
    out_steps, in_steps = out_way.steps(), in_way.steps()

    def out_step():
        if out_steps:
            out_steps.pop(0)()

    for h in reversed(range(NC)):
        for e in range(held):
            project(h, e, scaled, (2 * hidden, hidden))
        for k in far:
            combine(seen, h, k, columns_of(width))
            if h == 1:
                out_way.first(k)
    for h in reversed(range(NC)):
        for e in range(held):
            project(h, e, grad_act, (0, 2 * hidden))
            out_step()
        for k in far:
            combine(cot_seen, h, k, all_cols)
            if h == 1:
                in_way.first(k)
            out_step()
    grad_work = [functools.partial(weight_grad, e, j) for j in reversed(range(NX * NC)) for e in range(held)]
    while out_steps or in_steps or grad_work:
        if grad_work:
            grad_work.pop(0)()
        out_step()
        if in_steps:
            in_steps.pop(0)()
        if in_steps:
            in_steps.pop(0)()
    out_way.last(moe_out)
    in_way.last(gin_out)
    for copy in stores[-2:]:
        copy.wait()
    out_way.finish()
    in_way.finish()


def moe(payload, cots, parts, cap, collective_id):
    count, wide = payload.shape
    width = wide - 128
    held, quarter, columns = parts[0].shape
    hidden = columns // 3
    cut = count * 3 // 4
    plans = [
        Plan(0, (Z, Y, C), (C, Z, Y), rows=(0, cut)),
        Plan(0, (Y, Z, C), (C, Z, Y), rows=(cut, count - cut)),
    ]
    back = Plan(0, (C, Y), (C, Z, Y))
    levels, sends, recvs = Reduce.counts(back)
    blocks = NC * NZ * NY
    pair = NY * cap
    rows = blocks // NY * pair
    lanes = tile_up(held * pair, 128)
    bf, f32 = jnp.bfloat16, jnp.float32
    whole = pl.BlockSpec(memory_space=pltpu.VMEM)
    apart = pl.BlockSpec(memory_space=pl.ANY)
    dma = pltpu.SemaphoreType.DMA
    return pl.pallas_call(
        functools.partial(moe_kernel, plans, back, width, hidden, cap),
        out_shape=[
            jax.ShapeDtypeStruct((count, wide), f32),
            jax.ShapeDtypeStruct((count, width), f32),
        ]
        + [jax.ShapeDtypeStruct((held, quarter, columns), bf)] * (NX * NC),
        in_specs=[whole] + [apart] * 5,
        out_specs=[whole] * 2 + [apart] * (NX * NC),
        scratch_shapes=[
            pltpu.VMEM((blocks, count, wide), bf),
            pltpu.VMEM((blocks, count, wide), bf),
            pltpu.VMEM((held, NX * NC * quarter, columns), bf),
            pltpu.VMEM((held, rows, wide), bf),
            pltpu.VMEM((held, rows, width), bf),
            pltpu.VMEM((held, rows, wide), bf),
            pltpu.VMEM((held, rows, hidden), bf),
            pltpu.VMEM((held, rows, 2 * hidden), bf),
            pltpu.VMEM((blocks // NY, NY * count, lanes), bf),
            pltpu.VMEM((2, quarter, columns), bf),
        ]
        + [pltpu.VMEM((n, count, width), bf) for n in levels + [NZ + 1]]
        + [pltpu.VMEM((n, count, wide), bf) for n in levels + [NZ + 1]]
        + [
            dma((sum(Gather.sends(p) for p in plans),)),
            dma((sum(p.blocks for p in plans),)),
            dma(()),
            dma((sends,)),
            dma((recvs,)),
            dma((sends,)),
            dma((recvs,)),
            dma((held * NX * NC + blocks // NY,)),
            dma((held * NX * NC,)),
        ],
        compiler_params=pltpu.CompilerParams(
            collective_id=collective_id, has_side_effects=True, vmem_limit_bytes=67043328
        ),
        name="experts",
    )(payload, cots, *parts)


MODEL_WIDTH = 1536
QUERY_HEADS = 24
KEY_VALUE_HEADS = 8
HEAD_SIZE = 64
EXPERT_HIDDEN = 512
EXPERT_COUNT = 32
TOP = 8
CAP = 40


norm_eps = 1e-06
attn_scale = 0.015625
rope_base = 10000.0
masked_logits = -1e30


def rope_tables(positions):
    half = HEAD_SIZE // 2
    frequency = jnp.power(
        jnp.float32(rope_base), -2.0 * jnp.arange(half, dtype=jnp.float32) / HEAD_SIZE
    )
    angle = positions.astype(jnp.float32)[:, None] * frequency[None, :]
    return (jnp.cos(angle)[:, None, :], jnp.sin(angle)[:, None, :])


def rotate_pairs(value_tensor, cosine_table, sine_table):
    half = value_tensor.shape[-1] // 2
    first = value_tensor[..., :half]
    second = value_tensor[..., half:]
    return jnp.concatenate(
        [first * cosine_table - second * sine_table, second * cosine_table + first * sine_table],
        axis=-1,
    )


def rms_forward(wide, gain):
    inverse = lax.rsqrt(jnp.mean(wide * wide, axis=-1, keepdims=True) + norm_eps)
    unit = wide * inverse
    return (unit, inverse, (unit * gain.astype(jnp.float32)).astype(jnp.bfloat16))


def rms_backward(grad, unit, inverse, gain):
    scaled = grad * gain.astype(jnp.float32)
    back = inverse * (scaled - unit * jnp.mean(scaled * unit, axis=-1, keepdims=True))
    return (back, jnp.sum(grad * unit, axis=0))


def piece_scores(query_rows, key_section, positions):
    token_count = key_section.shape[0]
    key_tensor = key_section.reshape(token_count, KEY_VALUE_HEADS, HEAD_SIZE)
    scores = (
        jnp.einsum("tkgd,nkd->kgtn", query_rows, key_tensor, preferred_element_type=jnp.float32)
        * attn_scale
    )
    visible = jnp.arange(token_count, dtype=jnp.int32)[None, :] <= positions[:, None]
    return (jnp.where(visible, scores, masked_logits), visible, key_tensor)


def local(
    hidden,
    routes,
    attn_norm,
    ffn_norm,
    w_q,
    key_weight,
    value_weight,
    w_o,
    router,
    expert_in,
    expert_out,
    cotangent,
):
    token_rows = hidden.shape[1]
    query_group = QUERY_HEADS // KEY_VALUE_HEADS
    ctx_size = lax.axis_size(CTX)
    sequence_length = token_rows * ctx_size
    positions = lax.axis_index(CTX) * token_rows + jnp.arange(token_rows, dtype=jnp.int32)
    cosine_table, sine_table = rope_tables(positions)
    contract_rows = (((0,), (0,)), ((), ()))
    contract_cols = (((1,), (1,)), ((), ()))
    layer = (
        lax.all_gather(attn_norm, (CTX, FSDP), axis=0, tiled=True),
        lax.all_gather(ffn_norm, (CTX, FSDP), axis=0, tiled=True),
        lax.all_gather(w_q, (CTX, FSDP), axis=0, tiled=True),
        lax.all_gather(key_weight, (CTX, FSDP), axis=0, tiled=True),
        lax.all_gather(value_weight, (CTX, FSDP), axis=0, tiled=True),
        lax.all_gather(w_o, (CTX, FSDP), axis=0, tiled=True),
        lax.all_gather(router, (CTX, FSDP), axis=0, tiled=True),
    )
    attn_gain, ffn_gain, query_w, key_weight_matrix, value_w, output_w, router_w = layer
    experts = (
        lax.all_gather(expert_in, FSDP, axis=1, tiled=True),
        lax.all_gather(expert_out, FSDP, axis=1, tiled=True),
    )
    weight_in, weight_out = experts
    wide = hidden[0].astype(jnp.float32)
    attn_unit, inverse_one, attention_input = rms_forward(wide, attn_gain)
    query_linear = jnp.dot(attention_input, query_w, preferred_element_type=jnp.float32).reshape(
        token_rows, QUERY_HEADS, HEAD_SIZE
    )
    query_rows = (
        rotate_pairs(query_linear, cosine_table, sine_table)
        .astype(jnp.bfloat16)
        .reshape(token_rows, KEY_VALUE_HEADS, query_group, HEAD_SIZE)
    )
    key_linear = jnp.dot(
        attention_input, key_weight_matrix, preferred_element_type=jnp.float32
    ).reshape(token_rows, KEY_VALUE_HEADS, HEAD_SIZE)
    key_matrix_rows = (
        rotate_pairs(key_linear, cosine_table, sine_table)
        .astype(jnp.bfloat16)
        .reshape(token_rows, KEY_VALUE_HEADS * HEAD_SIZE)
    )
    value_rows = jnp.dot(attention_input, value_w, preferred_element_type=jnp.float32).astype(
        jnp.bfloat16
    )
    init_state = (
        jnp.full((KEY_VALUE_HEADS, query_group, token_rows), masked_logits, jnp.float32),
        jnp.zeros((KEY_VALUE_HEADS, query_group, token_rows), jnp.float32),
        jnp.zeros((KEY_VALUE_HEADS, query_group, token_rows, HEAD_SIZE), jnp.float32),
    )
    key_section = lax.all_gather(key_matrix_rows, CTX, axis=0, tiled=True)
    value_section = lax.all_gather(value_rows, CTX, axis=0, tiled=True)

    def compute(current):
        best, total, weighted = current
        scores, visible, key_tensor = piece_scores(query_rows, key_section, positions)
        value_tensor = value_section.reshape(value_section.shape[0], KEY_VALUE_HEADS, HEAD_SIZE)
        new_best = jnp.maximum(best, jnp.max(scores, axis=-1))
        weights = jnp.where(visible, jnp.exp(scores - new_best[..., None]), 0.0)
        total = jnp.sum(weights, axis=-1)
        weighted = jnp.einsum(
            "kgtn,nkd->kgtd",
            weights.astype(jnp.bfloat16),
            value_tensor,
            preferred_element_type=jnp.float32,
        )
        return (new_best, total, weighted)

    best, total, weighted = lax.cond(
        jnp.int32(0) <= positions[-1], compute, lambda current: current, init_state
    )
    log_sum_rows = best + jnp.log(total)
    attention_output = (
        jnp.transpose(weighted / total[..., None], (2, 0, 1, 3))
        .reshape(token_rows, QUERY_HEADS * HEAD_SIZE)
        .astype(jnp.bfloat16)
    )
    mixed = wide + jnp.dot(attention_output, output_w, preferred_element_type=jnp.float32)
    ffn_unit, inverse_two, ffn_in = rms_forward(mixed, ffn_gain)
    logits = jnp.dot(ffn_in, router_w, preferred_element_type=jnp.float32)
    route = routes[0]
    indicator = (route[:, :, None] == jnp.arange(EXPERT_COUNT, dtype=jnp.int32)).astype(jnp.float32)
    chosen = jnp.sum(indicator * logits[:, None, :], axis=-1)
    gates = jax.nn.softmax(chosen, axis=-1)
    flat_route = route.reshape(-1)
    counter = (flat_route[:, None] == jnp.arange(EXPERT_COUNT, dtype=jnp.int32)).astype(jnp.int32)
    slot = jnp.sum(counter * (jnp.cumsum(counter, axis=0) - 1), axis=1)
    target = flat_route * CAP + slot
    owner = (
        jnp.full((EXPERT_COUNT * CAP,), token_rows * TOP, jnp.int32)
        .at[target]
        .set(jnp.arange(token_rows * TOP, dtype=jnp.int32))
    )
    ffn_pad = jnp.concatenate([ffn_in, jnp.zeros((1, MODEL_WIDTH), jnp.bfloat16)], axis=0)
    local_experts = weight_in.shape[0]
    outgoing = ffn_pad[owner // TOP].reshape(ctx_size, local_experts, CAP, MODEL_WIDTH)
    received = lax.all_to_all(outgoing, CTX, split_axis=0, concat_axis=2, tiled=True)[0]
    act = jnp.einsum("erd,edf->erf", received, weight_in, preferred_element_type=jnp.float32)
    gate_part = act[..., :EXPERT_HIDDEN]
    up_part = act[..., EXPERT_HIDDEN:]
    sigma = jax.nn.sigmoid(gate_part)
    inner = (gate_part * sigma * up_part).astype(jnp.bfloat16)
    produced = jnp.einsum(
        "erf,edf->erd", inner, weight_out, preferred_element_type=jnp.float32
    ).astype(jnp.bfloat16)
    returned = lax.all_to_all(
        produced[None], CTX, split_axis=2, concat_axis=0, tiled=True
    ).reshape(EXPERT_COUNT * CAP, MODEL_WIDTH)
    picked = returned[target].reshape(token_rows, TOP, MODEL_WIDTH)
    layer_out = (mixed + jnp.sum(gates[..., None] * picked, axis=1)).astype(jnp.bfloat16)
    cot = cotangent[0]
    layer = (
        lax.all_gather(attn_norm, (CTX, FSDP), axis=0, tiled=True),
        lax.all_gather(ffn_norm, (CTX, FSDP), axis=0, tiled=True),
        lax.all_gather(w_q, (CTX, FSDP), axis=0, tiled=True),
        lax.all_gather(key_weight, (CTX, FSDP), axis=0, tiled=True),
        lax.all_gather(value_weight, (CTX, FSDP), axis=0, tiled=True),
        lax.all_gather(w_o, (CTX, FSDP), axis=0, tiled=True),
        lax.all_gather(router, (CTX, FSDP), axis=0, tiled=True),
    )
    attn_gain, ffn_gain, query_w, key_weight_matrix, value_w, output_w, router_w = layer
    experts = (
        lax.all_gather(expert_in, FSDP, axis=1, tiled=True),
        lax.all_gather(expert_out, FSDP, axis=1, tiled=True),
    )
    weight_in, weight_out = experts
    grad_gate = jnp.sum(cot[:, None, :] * picked, axis=-1)
    slot_grads = (
        (gates[..., None] * cot[:, None, :])
        .astype(jnp.bfloat16)
        .reshape(token_rows * TOP, MODEL_WIDTH)
    )
    slot_pad = jnp.concatenate([slot_grads, jnp.zeros((1, MODEL_WIDTH), jnp.bfloat16)], axis=0)
    grad_outgoing = slot_pad[owner].reshape(ctx_size, local_experts, CAP, MODEL_WIDTH)
    grad_received = lax.all_to_all(grad_outgoing, CTX, split_axis=0, concat_axis=2, tiled=True)[0]
    grad_w_out = jnp.einsum(
        "erd,erf->edf", grad_received, inner, preferred_element_type=jnp.float32
    )
    grad_inner = jnp.einsum(
        "erd,edf->erf", grad_received, weight_out, preferred_element_type=jnp.float32
    )
    grad_act = jnp.concatenate(
        [
            grad_inner * up_part * sigma * (1.0 + gate_part * (1.0 - sigma)),
            grad_inner * gate_part * sigma,
        ],
        axis=-1,
    ).astype(jnp.bfloat16)
    grad_w_in = jnp.einsum("erd,erf->edf", received, grad_act, preferred_element_type=jnp.float32)
    grad_rows = jnp.einsum(
        "erf,edf->erd", grad_act, weight_in, preferred_element_type=jnp.float32
    ).astype(jnp.bfloat16)
    grad_back = lax.all_to_all(
        grad_rows[None], CTX, split_axis=2, concat_axis=0, tiled=True
    ).reshape(EXPERT_COUNT * CAP, MODEL_WIDTH)
    grad_expert_in, grad_expert_out = (
        lax.psum_scatter(
            grad_w_in.astype(jnp.bfloat16), FSDP, scatter_dimension=1, tiled=True
        ).astype(jnp.float32),
        lax.psum_scatter(
            grad_w_out.astype(jnp.bfloat16), FSDP, scatter_dimension=1, tiled=True
        ).astype(jnp.float32),
    )
    grad_chosen = gates * (grad_gate - jnp.sum(gates * grad_gate, axis=-1, keepdims=True))
    grad_logits = jnp.sum(indicator * grad_chosen[..., None], axis=1).astype(jnp.bfloat16)
    grad_router_part = lax.dot_general(
        ffn_in, grad_logits, contract_rows, preferred_element_type=jnp.float32
    )
    grad_ffn_in = lax.dot_general(
        grad_logits, router_w, contract_cols, preferred_element_type=jnp.float32
    )
    grad_ffn_in = grad_ffn_in + jnp.sum(
        grad_back[target].reshape(token_rows, TOP, MODEL_WIDTH), axis=1, dtype=jnp.float32
    )
    back_two, grad_ffn_gain = rms_backward(grad_ffn_in, ffn_unit, inverse_two, ffn_gain)
    grad_mixed = cot + back_two
    grad_attn = grad_mixed.astype(jnp.bfloat16)
    grad_wo_part = lax.dot_general(
        attention_output, grad_attn, contract_rows, preferred_element_type=jnp.float32
    )
    attention_output_gradient = lax.dot_general(
        grad_attn, output_w, contract_cols, preferred_element_type=jnp.float32
    ).astype(jnp.bfloat16)
    head_gradient = attention_output_gradient.reshape(
        token_rows, KEY_VALUE_HEADS, query_group, HEAD_SIZE
    )
    delta_rows = jnp.sum(
        head_gradient.astype(jnp.float32)
        * attention_output.reshape(token_rows, KEY_VALUE_HEADS, query_group, HEAD_SIZE).astype(
            jnp.float32
        ),
        axis=-1,
    )
    delta_rows = jnp.transpose(delta_rows, (1, 2, 0))
    init_back = (
        jnp.zeros((token_rows, KEY_VALUE_HEADS, query_group, HEAD_SIZE), jnp.float32),
        jnp.zeros((sequence_length, 2 * KEY_VALUE_HEADS * HEAD_SIZE), jnp.float32),
    )
    attend_key_section = lax.all_gather(key_matrix_rows, CTX, axis=0, tiled=True)
    attend_value_section = lax.all_gather(value_rows, CTX, axis=0, tiled=True)

    def compute(current):
        token_count = attend_key_section.shape[0]
        scores, visible, key_tensor = piece_scores(query_rows, attend_key_section, positions)
        value_tensor = attend_value_section.reshape(token_count, KEY_VALUE_HEADS, HEAD_SIZE)
        weights_full = jnp.where(visible, jnp.exp(scores - log_sum_rows[..., None]), 0.0)
        grad_probs = jnp.einsum(
            "tkgd,nkd->kgtn", head_gradient, value_tensor, preferred_element_type=jnp.float32
        )
        grad_scores = (weights_full * (grad_probs - delta_rows[..., None])).astype(jnp.bfloat16)
        grad_query = attn_scale * jnp.einsum(
            "kgtn,nkd->tkgd", grad_scores, key_tensor, preferred_element_type=jnp.float32
        )
        key_portion = attn_scale * jnp.einsum(
            "kgtn,tkgd->nkd", grad_scores, query_rows, preferred_element_type=jnp.float32
        )
        value_portion = jnp.einsum(
            "kgtn,tkgd->nkd",
            weights_full.astype(jnp.bfloat16),
            head_gradient,
            preferred_element_type=jnp.float32,
        )
        update = jnp.concatenate(
            [
                key_portion.reshape(token_count, KEY_VALUE_HEADS * HEAD_SIZE),
                value_portion.reshape(token_count, KEY_VALUE_HEADS * HEAD_SIZE),
            ],
            axis=1,
        )
        return (grad_query, update)

    grad_query, grad_keys_full = lax.cond(
        jnp.int32(0) <= positions[-1], compute, lambda current: current, init_back
    )
    local_gradients = lax.psum_scatter(
        grad_keys_full.astype(jnp.bfloat16), CTX, scatter_dimension=0, tiled=True
    ).astype(jnp.float32)
    query_back = (
        rotate_pairs(
            grad_query.reshape(token_rows, QUERY_HEADS, HEAD_SIZE), cosine_table, -sine_table
        )
        .astype(jnp.bfloat16)
        .reshape(token_rows, QUERY_HEADS * HEAD_SIZE)
    )
    key_backward_rows = (
        rotate_pairs(
            local_gradients[:, : KEY_VALUE_HEADS * HEAD_SIZE].reshape(
                token_rows, KEY_VALUE_HEADS, HEAD_SIZE
            ),
            cosine_table,
            -sine_table,
        )
        .astype(jnp.bfloat16)
        .reshape(token_rows, KEY_VALUE_HEADS * HEAD_SIZE)
    )
    value_backward_rows = local_gradients[:, KEY_VALUE_HEADS * HEAD_SIZE :].astype(jnp.bfloat16)
    grad_wq_part = lax.dot_general(
        attention_input, query_back, contract_rows, preferred_element_type=jnp.float32
    )
    grad_wk_part = lax.dot_general(
        attention_input, key_backward_rows, contract_rows, preferred_element_type=jnp.float32
    )
    grad_wv_part = lax.dot_general(
        attention_input, value_backward_rows, contract_rows, preferred_element_type=jnp.float32
    )
    grad_attn_in = lax.dot_general(
        query_back, query_w, contract_cols, preferred_element_type=jnp.float32
    )
    grad_attn_in = grad_attn_in + lax.dot_general(
        key_backward_rows, key_weight_matrix, contract_cols, preferred_element_type=jnp.float32
    )
    grad_attn_in = grad_attn_in + lax.dot_general(
        value_backward_rows, value_w, contract_cols, preferred_element_type=jnp.float32
    )
    back_one, grad_attn_gain = rms_backward(grad_attn_in, attn_unit, inverse_one, attn_gain)
    grad_input = grad_mixed + back_one
    partial_sums = (
        lax.psum_scatter(
            grad_attn_gain.astype(jnp.bfloat16), CTX, scatter_dimension=0, tiled=True
        ).astype(jnp.float32),
        lax.psum_scatter(
            grad_ffn_gain.astype(jnp.bfloat16), CTX, scatter_dimension=0, tiled=True
        ).astype(jnp.float32),
        lax.psum_scatter(
            grad_wq_part.astype(jnp.bfloat16), CTX, scatter_dimension=0, tiled=True
        ).astype(jnp.float32),
        lax.psum_scatter(
            grad_wk_part.astype(jnp.bfloat16), CTX, scatter_dimension=0, tiled=True
        ).astype(jnp.float32),
        lax.psum_scatter(
            grad_wv_part.astype(jnp.bfloat16), CTX, scatter_dimension=0, tiled=True
        ).astype(jnp.float32),
        lax.psum_scatter(
            grad_wo_part.astype(jnp.bfloat16), CTX, scatter_dimension=0, tiled=True
        ).astype(jnp.float32),
        lax.psum_scatter(
            grad_router_part.astype(jnp.bfloat16), CTX, scatter_dimension=0, tiled=True
        ).astype(jnp.float32),
    )
    summed = (
        lax.psum_scatter(
            partial_sums[0].astype(jnp.bfloat16), FSDP, scatter_dimension=0, tiled=True
        ).astype(jnp.float32),
        lax.psum_scatter(
            partial_sums[1].astype(jnp.bfloat16), FSDP, scatter_dimension=0, tiled=True
        ).astype(jnp.float32),
        lax.psum_scatter(
            partial_sums[2].astype(jnp.bfloat16), FSDP, scatter_dimension=0, tiled=True
        ).astype(jnp.float32),
        lax.psum_scatter(
            partial_sums[3].astype(jnp.bfloat16), FSDP, scatter_dimension=0, tiled=True
        ).astype(jnp.float32),
        lax.psum_scatter(
            partial_sums[4].astype(jnp.bfloat16), FSDP, scatter_dimension=0, tiled=True
        ).astype(jnp.float32),
        lax.psum_scatter(
            partial_sums[5].astype(jnp.bfloat16), FSDP, scatter_dimension=0, tiled=True
        ).astype(jnp.float32),
        lax.psum_scatter(
            partial_sums[6].astype(jnp.bfloat16), FSDP, scatter_dimension=0, tiled=True
        ).astype(jnp.float32),
    )
    return (
        layer_out[None],
        grad_input[None],
        summed[0],
        summed[1],
        summed[2],
        summed[3],
        summed[4],
        summed[5],
        summed[6],
        grad_expert_in,
        grad_expert_out,
    )


def swap(a, flip):
    return lax.ppermute(a, FSDP, [(i, i ^ flip) for i in range(NX * NC)])


def fast(
    hidden,
    routes,
    attn_norm,
    ffn_norm,
    w_q,
    key_weight,
    value_weight,
    w_o,
    router,
    expert_in,
    expert_out,
    cotangent,
):
    tokens = hidden.shape[1]
    group = QUERY_HEADS // KEY_VALUE_HEADS
    ctx_size = NZ * NY
    ctx = lax.axis_index(CTX)
    fsdp = lax.axis_index(FSDP)
    core = fsdp % NC
    rows = w_q.shape[0]
    quarter = expert_in.shape[1]
    kv_width = KEY_VALUE_HEADS * HEAD_SIZE
    q_width = QUERY_HEADS * HEAD_SIZE
    held = expert_in.shape[0] // NC
    bf = jnp.bfloat16
    f32 = jnp.float32
    positions = ctx * tokens + jnp.arange(tokens, dtype=jnp.int32)
    cosine_table, sine_table = rope_tables(positions)
    contract_rows = (((0,), (0,)), ((), ()))
    contract_cols = (((1,), (1,)), ((), ()))
    wide = hidden[0].astype(f32)
    cot = cotangent[0]

    pack_one = jnp.concatenate([w_q, key_weight, value_weight], axis=1)
    pack_two = jnp.concatenate(
        [w_o, router, attn_norm[:, None], ffn_norm[:, None], jnp.zeros((rows, 94), bf)], axis=1
    )
    route = routes[0]
    indicator = (route[:, :, None] == jnp.arange(EXPERT_COUNT, dtype=jnp.int32)).astype(f32)
    cot_pack = jnp.concatenate(
        [
            cot.astype(bf),
            jnp.sum(indicator, axis=1).astype(bf),
            jnp.zeros((tokens, 128 - EXPERT_COUNT), bf),
        ],
        axis=1,
    )
    experts = jnp.concatenate([expert_in, expert_out], axis=2)
    experts = experts.reshape(NC, held, quarter, experts.shape[2])
    mine = lax.dynamic_index_in_dim(experts, core, 0, False)
    other = lax.dynamic_index_in_dim(experts, 1 - core, 0, False)
    one, two, cots = gather(
        [pack_one, pack_two, cot_pack],
        [
            Plan(0, (Z, Y, X, C,), (Z, Y, X, C,)),
            Plan(1, (Z, X, Y, C,), (Z, Y, X, C,)),
            Plan(2, (Z, Y, C,), (C, Z, Y,), rows=(0, tokens // 2)),
            Plan(2, (Y, Z, C,), (C, Z, Y,), rows=(tokens // 2, tokens // 2)),
        ],
        0,
        "gather_weights",
    )
    one, mine, other = lax.optimization_barrier((one, mine, other))
    parts = [mine, swap(other, 1), swap(mine, 2), swap(other, 3)]
    one = one.reshape(MODEL_WIDTH, -1)
    two = two.reshape(MODEL_WIDTH, -1)
    output_w = two[:, :MODEL_WIDTH]
    small = two[:, MODEL_WIDTH:]
    router_w = small[:, :EXPERT_COUNT]
    gains = lax.dot_general(
        jnp.eye(128, dtype=bf), small, contract_cols, preferred_element_type=f32
    )
    attn_gain, ffn_gain = gains[EXPERT_COUNT], gains[EXPERT_COUNT + 1]

    attn_unit, inverse_one, attention_input = rms_forward(wide, attn_gain)
    linear = jnp.dot(attention_input, one, preferred_element_type=f32)
    query_rows = (
        rotate_pairs(linear[:, :q_width].reshape(tokens, QUERY_HEADS, HEAD_SIZE), cosine_table, sine_table)
        .astype(bf)
        .reshape(tokens, KEY_VALUE_HEADS, group, HEAD_SIZE)
    )
    key_rows = (
        rotate_pairs(
            linear[:, q_width : q_width + kv_width].reshape(tokens, KEY_VALUE_HEADS, HEAD_SIZE),
            cosine_table,
            sine_table,
        )
        .astype(bf)
        .reshape(tokens, kv_width)
    )
    value_rows = linear[:, q_width + kv_width :].astype(bf)
    (kv,) = gather(
        [jnp.concatenate([key_rows, value_rows], axis=1)],
        [Plan(0, (Z, Y,), (Z, Y,))],
        1,
        "gather_keys",
    )
    kv = kv.reshape(ctx_size * tokens, 2 * kv_width)
    key_section, value_section = kv[:, :kv_width], kv[:, kv_width:]
    value_tensor = value_section.reshape(ctx_size * tokens, KEY_VALUE_HEADS, HEAD_SIZE)
    scores, visible, key_tensor = piece_scores(query_rows, key_section, positions)
    best = jnp.max(scores, axis=-1)
    weights = jnp.where(visible, jnp.exp(scores - best[..., None]), 0.0)
    total = jnp.sum(weights, axis=-1)
    weighted = jnp.einsum(
        "kgtn,nkd->kgtd", weights.astype(bf), value_tensor, preferred_element_type=f32
    )
    log_sum_rows = best + jnp.log(total)
    attention_output = (
        jnp.transpose(weighted / total[..., None], (2, 0, 1, 3)).reshape(tokens, q_width).astype(bf)
    )
    mixed = wide + jnp.dot(attention_output, output_w, preferred_element_type=f32)
    ffn_unit, inverse_two, ffn_in = rms_forward(mixed, ffn_gain)
    logits = jnp.dot(ffn_in, router_w, preferred_element_type=f32)
    chosen = jnp.sum(indicator * logits[:, None, :], axis=-1)
    gates = jax.nn.softmax(chosen, axis=-1)
    gate_map = jnp.sum(indicator * gates[..., None], axis=1)
    payload = jnp.concatenate(
        [ffn_in, gate_map.astype(bf), jnp.zeros((tokens, 128 - EXPERT_COUNT), bf)], axis=1
    )
    gin, moe_out, *pieces = moe(payload, cots, parts, CAP, 2)
    own_sum = pieces[0].astype(f32) + swap(pieces[2], 2).astype(f32)
    core_sum = swap(pieces[1], 1).astype(f32) + swap(pieces[3], 3).astype(f32)
    grad_experts = jnp.where(
        core == 0,
        jnp.concatenate([own_sum, core_sum]),
        jnp.concatenate([core_sum, own_sum]),
    )
    grad_expert_in = grad_experts[:, :, : 2 * EXPERT_HIDDEN]
    grad_expert_out = grad_experts[:, :, 2 * EXPERT_HIDDEN :]
    layer_out = (mixed + moe_out).astype(bf)
    grad_gate_map = gin[:, MODEL_WIDTH : MODEL_WIDTH + EXPERT_COUNT] + gin[
        :, MODEL_WIDTH + EXPERT_COUNT : MODEL_WIDTH + 2 * EXPERT_COUNT
    ]
    grad_gate = jnp.sum(indicator * grad_gate_map[:, None, :], axis=-1)
    grad_chosen = gates * (grad_gate - jnp.sum(gates * grad_gate, axis=-1, keepdims=True))
    grad_logits = jnp.sum(indicator * grad_chosen[..., None], axis=1).astype(bf)
    grad_router_part = lax.dot_general(
        ffn_in, grad_logits, contract_rows, preferred_element_type=f32
    )
    grad_ffn_in = gin[:, :MODEL_WIDTH] + lax.dot_general(
        grad_logits, router_w, contract_cols, preferred_element_type=f32
    )
    back_two, _ = rms_backward(grad_ffn_in, ffn_unit, inverse_two, ffn_gain)
    grad_mixed = cot + back_two
    grad_attn = grad_mixed.astype(bf)
    grad_wo_part = lax.dot_general(
        attention_output, grad_attn, contract_rows, preferred_element_type=f32
    )
    attention_output_gradient = lax.dot_general(
        grad_attn, output_w, contract_cols, preferred_element_type=f32
    ).astype(bf)
    head_gradient = attention_output_gradient.reshape(tokens, KEY_VALUE_HEADS, group, HEAD_SIZE)
    delta_rows = jnp.sum(
        head_gradient.astype(f32)
        * attention_output.reshape(tokens, KEY_VALUE_HEADS, group, HEAD_SIZE).astype(f32),
        axis=-1,
    )
    delta_rows = jnp.transpose(delta_rows, (1, 2, 0))
    weights_full = jnp.where(visible, jnp.exp(scores - log_sum_rows[..., None]), 0.0)
    grad_probs = jnp.einsum(
        "tkgd,nkd->kgtn", head_gradient, value_tensor, preferred_element_type=f32
    )
    grad_scores = (weights_full * (grad_probs - delta_rows[..., None])).astype(bf)
    grad_query = attn_scale * jnp.einsum(
        "kgtn,nkd->tkgd", grad_scores, key_tensor, preferred_element_type=f32
    )
    key_portion = attn_scale * jnp.einsum(
        "kgtn,tkgd->nkd", grad_scores, query_rows, preferred_element_type=f32
    )
    value_portion = jnp.einsum(
        "kgtn,tkgd->nkd", weights_full.astype(bf), head_gradient, preferred_element_type=f32
    )
    update = jnp.concatenate(
        [
            key_portion.astype(bf).reshape(ctx_size, tokens, kv_width),
            value_portion.astype(bf).reshape(ctx_size, tokens, kv_width),
        ],
        axis=2,
    )
    (local_gradients,) = reduce_scatter(
        [update], [Plan(0, (Y,), (Z, Y,))], [f32], 4, "return_keys"
    )
    query_back = (
        rotate_pairs(
            grad_query.reshape(tokens, QUERY_HEADS, HEAD_SIZE), cosine_table, -sine_table
        )
        .astype(bf)
        .reshape(tokens, q_width)
    )
    key_back = (
        rotate_pairs(
            local_gradients[:, :kv_width].reshape(tokens, KEY_VALUE_HEADS, HEAD_SIZE),
            cosine_table,
            -sine_table,
        )
        .astype(bf)
        .reshape(tokens, kv_width)
    )
    back = jnp.concatenate([query_back, key_back, local_gradients[:, kv_width:].astype(bf)], axis=1)
    grad_one = lax.dot_general(attention_input, back, contract_rows, preferred_element_type=f32)
    grad_attn_in = lax.dot_general(back, one, contract_cols, preferred_element_type=f32)
    back_one, _ = rms_backward(grad_attn_in, attn_unit, inverse_one, attn_gain)
    grad_input = grad_mixed + back_one
    attn_gain_grad = jnp.sum(grad_attn_in * attn_unit, axis=0)
    ffn_gain_grad = jnp.sum(grad_ffn_in * ffn_unit, axis=0)
    grad_two = jnp.concatenate(
        [
            grad_wo_part,
            grad_router_part,
            attn_gain_grad[:, None],
            ffn_gain_grad[:, None],
            jnp.zeros((MODEL_WIDTH, 94), f32),
        ],
        axis=1,
    )
    sum_one, sum_two = reduce_scatter(
        [
            grad_one.astype(bf).reshape(-1, rows, grad_one.shape[1]),
            grad_two.astype(bf).reshape(-1, rows, grad_two.shape[1]),
        ],
        [Plan(0, (C, X, Y,), (Z, Y, X, C,)), Plan(1, (C, Y, X,), (Z, Y, X, C,))],
        [f32, f32],
        5,
        "return_weights",
    )
    at = MODEL_WIDTH + EXPERT_COUNT
    return (
        layer_out[None],
        grad_input[None],
        sum_two[:, at],
        sum_two[:, at + 1],
        sum_one[:, :q_width],
        sum_one[:, q_width : q_width + kv_width],
        sum_one[:, q_width + kv_width :],
        sum_two[:, :MODEL_WIDTH],
        sum_two[:, MODEL_WIDTH:at],
        grad_expert_in,
        grad_expert_out,
    )


def solution(mesh):
    placed = (
        P(FSDP, CTX, None),
        P(FSDP, CTX, None),
        P((CTX, FSDP)),
        P((CTX, FSDP)),
        P((CTX, FSDP), None),
        P((CTX, FSDP), None),
        P((CTX, FSDP), None),
        P((CTX, FSDP), None),
        P((CTX, FSDP), None),
        P(CTX, FSDP, None),
        P(CTX, FSDP, None),
        P(FSDP, CTX, None),
    )
    small = mesh.shape[CTX] == NZ * NY and mesh.shape[FSDP] == NX * NC
    return jax.shard_map(
        fast if small else local,
        mesh=mesh,
        in_specs=placed,
        out_specs=(
            P(FSDP, CTX, None),
            P(FSDP, CTX, None),
            P((CTX, FSDP)),
            P((CTX, FSDP)),
            P((CTX, FSDP), None),
            P((CTX, FSDP), None),
            P((CTX, FSDP), None),
            P((CTX, FSDP), None),
            P((CTX, FSDP), None),
            P(CTX, FSDP, None),
            P(CTX, FSDP, None),
        ),
        check_vma=False,
    )
```

```python
import functools
import itertools

import jax
import jax.numpy as jnp
from jax import lax
from jax.experimental import pallas as pl
from jax.experimental.pallas import tpu as pltpu
from jax.sharding import PartitionSpec as P


NY = 2
NZ = 4
NX = 2
NC = 2
DEV = pl.DeviceIdType.MESH
CTX, FSDP = "ctx", "fsdp"
Z, Y, X, C = 0, 1, 2, 3
SIZES = {Z: NZ, Y: NY, X: NX, C: NC}
UP, DOWN = 4, 5


class Plan:
    def __init__(self, ref, order, index, rows=None):
        self.ref, self.order, self.index, self.rows = ref, order, index, rows
        self.blocks = 1
        for d in index:
            self.blocks *= SIZES[d]


class Place:
    def __init__(self):
        ctx = lax.axis_index(CTX)
        fsdp = lax.axis_index(FSDP)
        self.at = {Z: ctx // NY, Y: ctx % NY, X: fsdp // NC, C: fsdp % NC}
        z = self.at[Z]
        low = z < NZ // 2
        base = jnp.where(low, z, NZ - 1 - z)
        near = [base, 1 - base, jnp.int32(2), jnp.int32(3)]
        self.order = [z] + [jnp.where(low, k, NZ - 1 - k) for k in near[1:]]

    def device(self, dim, value):
        spot = dict(self.at)
        spot[dim] = value
        return (spot[Z] * NY + spot[Y], spot[X] * NC + spot[C])

    def across(self, dim):
        return self.device(dim, 1 - self.at[dim])

    def along(self, step):
        return self.device(Z, self.at[Z] + step)

    def coords(self, z_from, flips):
        spot = {d: (1 - self.at[d] if d in flips else self.at[d]) for d in (Y, X, C)}
        spot[Z] = z_from
        return spot


def flat_index(spot, dims):
    index = 0
    for d in dims:
        index = index * SIZES[d] + spot[d]
    return index


def subsets(dims):
    return [c for n in range(len(dims) + 1) for c in itertools.combinations(dims, n)]


def greet(place, dims):
    barrier = pltpu.get_barrier_semaphore()
    z = place.at[Z]
    count = jnp.int32(0)
    for d in dims:
        if d == Z:
            @pl.when(z > 0)
            def _():
                pl.semaphore_signal(barrier, inc=1, device_id=place.along(-1), device_id_type=DEV)

            @pl.when(z < NZ - 1)
            def _():
                pl.semaphore_signal(barrier, inc=1, device_id=place.along(1), device_id_type=DEV)

            count = count + jnp.where(z > 0, 1, 0) + jnp.where(z < NZ - 1, 1, 0)
        else:
            pl.semaphore_signal(barrier, inc=1, device_id=place.across(d), device_id_type=DEV)
            count = count + 1
    pl.semaphore_wait(barrier, count)


def gather_events(order):
    pairs = [d for d in order if d != Z]
    events = [(k, f) for k in range(NZ) for f in subsets(pairs)]
    return sorted(events, key=lambda e: (e[0] + len(e[1]), len(e[1])))


def gather_sends(order, k, flips):
    z_at = order.index(Z)
    last = max([order.index(d) for d in flips] + ([z_at] if k > 0 else []) + [-1])
    out = []
    for position, d in enumerate(order):
        if position > last:
            out.extend([UP, DOWN] if d == Z else [d])
    if k > 0 and last == z_at:
        out.extend([UP, DOWN])
    return out


def gather_kernel(plans, n_in, *refs):
    ins, outs = refs[:n_in], refs[n_in : 2 * n_in]
    send_sem, recv_sem, own_sem = refs[2 * n_in :]
    place = Place()
    z = place.at[Z]
    greet(place, sorted({d for p in plans for d in p.order}))
    pending = []
    slot = 0
    queue = []
    for n, plan in enumerate(plans):
        for rank, event in enumerate(gather_events(plan.order)):
            queue.append((rank / len(gather_events(plan.order)), n, event))
    queue.sort(key=lambda q: (q[0], q[1]))
    bases = [sum(p.blocks for p in plans[:n]) for n in range(len(plans))]
    for _, n, (k, flips) in queue:
        plan = plans[n]
        src = ins[plan.ref]
        out = outs[plan.ref]
        rows = plan.rows
        z_from = place.order[k]
        spot = place.coords(z_from, flips)
        index = flat_index(spot, plan.index)
        target = out.at[index] if rows is None else out.at[index, pl.ds(rows[0], rows[1])]
        sem = recv_sem.at[bases[n] + index]
        own = k == 0 and not flips
        source = (src if rows is None else src.at[pl.ds(rows[0], rows[1])]) if own else target
        if not own:
            pltpu.make_async_remote_copy(
                src_ref=target, dst_ref=target, send_sem=own_sem.at[0], recv_sem=sem,
                device_id=place.across(C), device_id_type=DEV,
            ).wait_recv()
        for way in gather_sends(plan.order, k, flips):
            if way in (UP, DOWN):
                step = 1 if way == UP else -1
                go = z < NZ - 1 if way == UP else z > 0
                if k > 0:
                    go = jnp.logical_and(go, z_from < z if way == UP else z_from > z)
                dest = place.device(Z, jnp.clip(z + step, 0, NZ - 1))
            else:
                go, dest = None, place.across(way)
            copy = pltpu.make_async_remote_copy(
                src_ref=source, dst_ref=target, send_sem=send_sem.at[slot], recv_sem=sem,
                device_id=dest, device_id_type=DEV,
            )
            slot += 1
            if go is None:
                copy.start()
            else:
                pl.when(go)(copy.start)
            pending.append((go, copy.wait_send))
        if own:
            copy = pltpu.make_async_copy(source, target, own_sem.at[1 + n])
            copy.start()
            pending.append((None, copy.wait))
    for go, wait in pending:
        if go is None:
            wait()
        else:
            pl.when(go)(wait)


def gather(arrays, plans, collective_id):
    n = len(arrays)
    sends = sum(len(gather_sends(p.order, k, f)) for p in plans for k, f in gather_events(p.order))
    blocks = {p.ref: p.blocks for p in plans}
    return pl.pallas_call(
        functools.partial(gather_kernel, plans, n),
        out_shape=[jax.ShapeDtypeStruct((blocks[i],) + a.shape, a.dtype) for i, a in enumerate(arrays)],
        in_specs=[pl.BlockSpec(memory_space=pltpu.VMEM)] * n,
        out_specs=[pl.BlockSpec(memory_space=pl.ANY)] * n,
        scratch_shapes=[
            pltpu.SemaphoreType.DMA((sends,)),
            pltpu.SemaphoreType.DMA((sum(p.blocks for p in plans),)),
            pltpu.SemaphoreType.DMA((1 + len(plans),)),
        ],
        compiler_params=pltpu.CompilerParams(collective_id=collective_id, has_side_effects=True),
    )(*arrays)


def add_into(acc, other):
    acc[...] = (acc[...].astype(jnp.float32) + other[...].astype(jnp.float32)).astype(acc.dtype)


def reduce_kernel(plans, n_in, *refs):
    ins, outs = refs[:n_in], refs[n_in : 2 * n_in]
    rest = list(refs[2 * n_in :])
    send_sem, recv_sem, own_sem = rest[:3]
    buffers = rest[3:]
    place = Place()
    z = place.at[Z]
    greet(place, sorted({d for p in plans for d in p.order} | {Z}))
    pending = []
    slots = [0, 0]

    def push(source, target, sem, dest):
        copy = pltpu.make_async_remote_copy(
            src_ref=source, dst_ref=target, send_sem=send_sem.at[slots[0]], recv_sem=sem,
            device_id=dest, device_id_type=DEV,
        )
        slots[0] += 1
        copy.start()
        pending.append(copy)

    def arrived(target, sem):
        pltpu.make_async_remote_copy(
            src_ref=target, dst_ref=target, send_sem=own_sem.at[0], recv_sem=sem,
            device_id=place.across(C), device_id_type=DEV,
        ).wait_recv()

    work = []
    far = list(reversed(range(NZ)))
    own_slot = 1
    state = []
    base = 0
    for n, plan in enumerate(plans):
        dims = plan.order
        acc = buffers[0]
        levels = buffers[1 : 1 + len(dims)]
        chain = buffers[1 + len(dims)]
        buffers = buffers[2 + len(dims) :]
        kept = [subsets(dims[p + 1 :]) for p in range(len(dims))]
        counts = [NZ * len(f) for f in kept]
        level_base = [base + sum(counts[:p]) for p in range(len(dims))]
        chain_base = base + sum(counts)
        base = chain_base + 2 * NZ
        state.append((acc, levels, chain, kept, level_base, chain_base))
        own_copies = {}
        src = ins[plan.ref]
        for k in far:
            for f in kept[0]:
                gone = flat_index(place.coords(place.order[k], (dims[0],) + f), plan.index)
                spot = place.order[k] * len(kept[0]) + kept[0].index(f)
                work.append((0, n, k, f, gone, spot))
                mine = flat_index(place.coords(place.order[k], f), plan.index)
                copy = pltpu.make_async_copy(src.at[mine], acc.at[spot], own_sem.at[own_slot])
                own_slot += 1
                own_copies[(k, f)] = copy
        state[-1] += (own_copies,)
    for _, n, k, f, gone, spot in sorted(work, key=lambda w: (-w[2],)):
        plan = plans[n]
        acc, levels, chain, kept, level_base, chain_base, own_copies = state[n]
        push(ins[plan.ref].at[gone], levels[0].at[spot], recv_sem.at[level_base[0] + spot], place.across(plan.order[0]))
        own_copies[(k, f)].start()

    def level_step(n, p, k):
        plan = plans[n]
        dims = plan.order
        acc, levels, _, kept, level_base, _, own_copies = state[n]
        for f in sorted(kept[p], key=lambda f: -len(f)):
            spot = place.order[k] * len(kept[p]) + kept[p].index(f)
            at = place.order[k] * len(kept[0]) + kept[0].index(f)
            if p == 0:
                own_copies[(k, f)].wait()
            arrived(levels[p].at[spot], recv_sem.at[level_base[p] + spot])
            add_into(acc.at[at], levels[p].at[spot])
            later = p + 1
            if later < len(dims) and dims[later] in f:
                left = tuple(d for d in f if d != dims[later])
                there = place.order[k] * len(kept[later]) + kept[later].index(left)
                push(
                    acc.at[at], levels[later].at[there],
                    recv_sem.at[level_base[later] + there], place.across(dims[later]),
                )

    def chain_step(n, k):
        acc, _, chain, kept, _, chain_base, _ = state[n]
        dest = place.order[k]
        up = dest > z
        lane = jnp.where(up, 0, 1)
        at = dest * len(kept[0])
        spot = lane * NZ + dest

        @pl.when(jnp.where(up, z > 0, z < NZ - 1))
        def _():
            arrived(chain.at[spot], recv_sem.at[chain_base + spot])
            add_into(acc.at[at], chain.at[spot])

        push(acc.at[at], chain.at[spot], recv_sem.at[chain_base + spot], place.along(jnp.where(up, 1, -1)))

    most = max(len(p.order) for p in plans)
    for step in range(NZ + most):
        for n, plan in enumerate(plans):
            for p in range(len(plan.order)):
                if 0 <= step - p < NZ:
                    level_step(n, p, far[step - p])
            p = len(plan.order)
            if 0 <= step - p < NZ - 1:
                chain_step(n, far[step - p])
    for n, plan in enumerate(plans):
        acc, levels, chain, kept, level_base, chain_base, own_copies = state[n]
        at = z * len(kept[0])

        @pl.when(z > 0)
        def _():
            spot = z
            arrived(chain.at[spot], recv_sem.at[chain_base + spot])
            add_into(acc.at[at], chain.at[spot])

        @pl.when(z < NZ - 1)
        def _():
            spot = NZ + z
            arrived(chain.at[spot], recv_sem.at[chain_base + spot])
            add_into(acc.at[at], chain.at[spot])

        outs[plan.ref][...] = acc[at].astype(outs[plan.ref].dtype)
    for copy in pending:
        copy.wait_send()


def reduce_scatter(arrays, plans, out_dtypes, collective_id):
    n = len(arrays)
    scratch = []
    sends = recvs = owns = 0
    for p in plans:
        a = arrays[p.ref]
        block = a.shape[1:]
        kept = [len(subsets(p.order[q + 1 :])) for q in range(len(p.order))]
        scratch.append(pltpu.VMEM((NZ * kept[0],) + block, a.dtype))
        for q in kept:
            scratch.append(pltpu.VMEM((NZ * q,) + block, a.dtype))
        scratch.append(pltpu.VMEM((2 * NZ,) + block, a.dtype))
        sends += NZ * sum(kept) + NZ - 1
        recvs += NZ * sum(kept) + 2 * NZ
        owns += NZ * kept[0]
    return pl.pallas_call(
        functools.partial(reduce_kernel, plans, n),
        out_shape=[jax.ShapeDtypeStruct(a.shape[1:], d) for a, d in zip(arrays, out_dtypes)],
        in_specs=[pl.BlockSpec(memory_space=pl.ANY)] * n,
        out_specs=[pl.BlockSpec(memory_space=pltpu.VMEM)] * n,
        scratch_shapes=[
            pltpu.SemaphoreType.DMA((sends,)),
            pltpu.SemaphoreType.DMA((recvs,)),
            pltpu.SemaphoreType.DMA((1 + owns,)),
        ]
        + scratch,
        compiler_params=pltpu.CompilerParams(
            collective_id=collective_id, has_side_effects=True, vmem_limit_bytes=60 * 1024 * 1024
        ),
    )(*arrays)


class Gather:
    def __init__(self, place, plan, src, out, send_sem, recv_sem, spare_sem, slot, base):
        self.place, self.plan, self.src, self.out = place, plan, src, out
        self.send_sem, self.recv_sem, self.spare_sem = send_sem, recv_sem, spare_sem
        self.slot, self.base = slot, base
        self.pending = []

    @staticmethod
    def sends(plan):
        return sum(len(gather_sends(plan.order, k, f)) for k, f in gather_events(plan.order))

    def step(self, k, flips):
        place, plan = self.place, self.plan
        z = place.at[Z]
        z_from = place.order[k]
        index = flat_index(place.coords(z_from, flips), plan.index)
        rows = plan.rows
        target = self.out.at[index] if rows is None else self.out.at[index, pl.ds(rows[0], rows[1])]
        sem = self.recv_sem.at[self.base + index]
        own = k == 0 and not flips
        source = target
        if own:
            source = self.src if rows is None else self.src.at[pl.ds(rows[0], rows[1])]
        else:
            pltpu.make_async_remote_copy(
                src_ref=target, dst_ref=target, send_sem=self.spare_sem, recv_sem=sem,
                device_id=place.across(C), device_id_type=DEV,
            ).wait_recv()
        for way in gather_sends(plan.order, k, flips):
            if way in (UP, DOWN):
                step = 1 if way == UP else -1
                go = z < NZ - 1 if way == UP else z > 0
                if k > 0:
                    go = jnp.logical_and(go, z_from < z if way == UP else z_from > z)
                dest = place.device(Z, jnp.clip(z + step, 0, NZ - 1))
            else:
                go, dest = None, place.across(way)
            copy = pltpu.make_async_remote_copy(
                src_ref=source, dst_ref=target, send_sem=self.send_sem.at[self.slot], recv_sem=sem,
                device_id=dest, device_id_type=DEV,
            )
            self.slot += 1
            if go is None:
                copy.start()
            else:
                pl.when(go)(copy.start)
            self.pending.append((go, copy.wait_send))

    def finish(self):
        for go, wait in self.pending:
            if go is None:
                wait()
            else:
                pl.when(go)(wait)


class Reduce:
    def __init__(self, place, plan, held, levels, chain, send_sem, recv_sem, spare_sem):
        self.place, self.plan, self.held, self.levels, self.chain = place, plan, held, levels, chain
        self.send_sem, self.recv_sem, self.spare_sem = send_sem, recv_sem, spare_sem
        dims = plan.order
        self.kept = [subsets(dims[p + 1 :]) for p in range(len(dims))]
        self.base = [NZ * sum(len(f) for f in self.kept[:p]) for p in range(len(dims) + 1)]
        self.slot = 0
        self.pending = []

    @staticmethod
    def counts(plan):
        kept = [NZ * len(subsets(plan.order[p + 1 :])) for p in range(len(plan.order))]
        return kept, sum(kept) + NZ - 1, sum(kept) + NZ + 1

    def push(self, source, target, sem, dest):
        copy = pltpu.make_async_remote_copy(
            src_ref=source, dst_ref=target, send_sem=self.send_sem.at[self.slot], recv_sem=sem,
            device_id=dest, device_id_type=DEV,
        )
        self.slot += 1
        copy.start()
        self.pending.append(copy)

    def arrived(self, target, sem):
        pltpu.make_async_remote_copy(
            src_ref=target, dst_ref=target, send_sem=self.spare_sem, recv_sem=sem,
            device_id=self.place.across(C), device_id_type=DEV,
        ).wait_recv()

    def block(self, k, flips):
        return flat_index(self.place.coords(self.place.order[k], flips), self.plan.index)

    def first(self, k):
        dim = self.plan.order[0]
        for n, f in enumerate(self.kept[0]):
            spot = self.place.order[k] * len(self.kept[0]) + n
            self.push(
                self.held.at[self.block(k, (dim,) + f)], self.levels[0].at[spot],
                self.recv_sem.at[spot], self.place.across(dim),
            )

    def level(self, p, k):
        dims = self.plan.order
        z_to = self.place.order[k]
        for f in sorted(self.kept[p], key=lambda f: -len(f)):
            spot = z_to * len(self.kept[p]) + self.kept[p].index(f)
            mine = self.held.at[self.block(k, f)]
            self.arrived(self.levels[p].at[spot], self.recv_sem.at[self.base[p] + spot])
            add_into(mine, self.levels[p].at[spot])
            later = p + 1
            if later < len(dims) and dims[later] in f:
                left = tuple(d for d in f if d != dims[later])
                there = z_to * len(self.kept[later]) + self.kept[later].index(left)
                self.push(
                    mine, self.levels[later].at[there],
                    self.recv_sem.at[self.base[later] + there], self.place.across(dims[later]),
                )

    def along(self, k):
        z = self.place.at[Z]
        dest = self.place.order[k]
        up = dest > z
        spot = dest + jnp.where(up, 1, 0)
        mine = self.held.at[self.block(k, ())]
        sem = self.recv_sem.at[self.base[-1] + spot]

        @pl.when(jnp.where(up, z > 0, z < NZ - 1))
        def _():
            self.arrived(self.chain.at[spot], sem)
            add_into(mine, self.chain.at[spot])

        self.push(mine, self.chain.at[spot], sem, self.place.along(jnp.where(up, 1, -1)))

    def last(self, out):
        z = self.place.at[Z]
        mine = self.held.at[self.block(0, ())]
        for go, spot in ((z > 0, z + 1), (z < NZ - 1, z)):

            @pl.when(go)
            def _():
                self.arrived(self.chain.at[spot], self.recv_sem.at[self.base[-1] + spot])
                add_into(mine, self.chain.at[spot])

        out[...] = mine[...].astype(out.dtype)

    def steps(self):
        depth = len(self.plan.order)
        far = list(reversed(range(NZ)))
        out = []
        for t in range(NZ + depth):
            for p in range(depth):
                if 0 <= t - p < NZ:
                    out.append(functools.partial(self.level, p, far[t - p]))
            if 0 <= t - depth < NZ - 1:
                out.append(functools.partial(self.along, far[t - depth]))
        return out

    def finish(self):
        for copy in self.pending:
            copy.wait_send()


def tile_up(n, m):
    return (n + m - 1) // m * m


def columns_of(width, chunk=512):
    return [(i, min(chunk, width - i)) for i in range(0, width, chunk)]


def moe_kernel(plans, back, width, hidden, cap, *refs):
    payload, cots, w_own, w_core, w_x, w_both = refs[:6]
    gin_out, moe_out = refs[6:8]
    grads = refs[8:12]
    (
        seen, cot_seen, weights, taken, cot_taken, rows_buf, scaled, grad_act, pick, stage,
        lvl_a0, lvl_a1, chain_a, lvl_b0, lvl_b1, chain_b,
        send_sem, recv_sem, spare_sem, send_a, recv_a, send_b, recv_b, load_sem, store_sem,
    ) = refs[12:]
    bf, f32 = jnp.bfloat16, jnp.float32
    place = Place()
    count = payload.shape[0]
    pair = 2 * cap
    wide = width + 128
    quarter = width // (NX * NC)
    half = NZ * pair
    lanes = pick.shape[2]
    held = weights.shape[0]
    fsdp = place.at[X] * NC + place.at[C]
    first = (((place.at[Z] * NY + place.at[Y]) * NC) + place.at[C]) * held

    loads = []
    for j, ref in enumerate((w_own, w_core, w_x, w_both)):
        rows = pl.ds(pl.multiple_of((fsdp ^ j) * quarter, quarter), quarter)
        for e in range(held):
            loads.append(pltpu.make_async_copy(ref.at[e], weights.at[e, rows], load_sem.at[len(loads)]))
    base_of = lambda h, k: (jnp.where(h == 0, place.at[C], 1 - place.at[C]) * NZ + place.order[k]) * NY
    cot_loads = {}
    for k in range(NZ):
        for h in range(2):
            at = pl.ds(base_of(h, k), NY)
            cot_loads[(h, k)] = pltpu.make_async_copy(cots.at[at], cot_seen.at[at], load_sem.at[len(loads) + len(cot_loads)])

    greet(place, (Z, Y, C))
    ways = []
    send_at = 0
    for n, plan in enumerate(plans):
        ways.append(Gather(place, plan, payload, seen, send_sem, recv_sem, spare_sem, send_at, n * plan.blocks))
        send_at += Gather.sends(plan)
    for way in ways:
        way.step(0, ())
    for key in cot_loads:
        cot_loads[key].start()
    for copy in loads:
        copy.start()
    seen[flat_index(place.at, plans[0].index)] = payload[...]

    row_id = lax.broadcasted_iota(jnp.int32, (NY * count, NY * count), 0)
    col_id = lax.broadcasted_iota(jnp.int32, (NY * count, NY * count), 1)
    earlier = jnp.logical_and(col_id < row_id, col_id // count == row_id // count).astype(bf)
    lane_id = lax.broadcasted_iota(jnp.int32, (1, 128), 1)
    here = [(lane_id == first + e).astype(f32) for e in range(held)]
    pick_lane = lax.broadcasted_iota(jnp.int32, (NY * count, lanes), 1).astype(f32)
    y_shift = (lax.broadcasted_iota(jnp.int32, (NY * count, 1), 0) // count * cap).astype(f32)

    def dispatch(source, target, h, k, cols):
        at = pl.ds(base_of(h, k), NY)
        r = (h * NZ + k) * pair
        for c0, cn in cols:
            block = source[at, :, c0 : c0 + cn].reshape(NY * count, cn)
            got = lax.dot_general(
                pick[h * NZ + k], block, (((0,), (0,)), ((), ())), preferred_element_type=f32
            ).astype(bf)
            for e in range(held):
                target[e, r : r + pair, c0 : c0 + cn] = got[e * pair : (e + 1) * pair]

    def cot_chunk(h, k):
        cot_loads[(h, k)].wait()
        at = pl.ds(base_of(h, k), NY)
        chosen = cot_seen[at, :, width:wide].reshape(NY * count, 128)
        before = jnp.dot(earlier, chosen, preferred_element_type=f32)
        picked = None
        for e in range(held):
            is_here = jnp.sum(chosen.astype(f32) * here[e], axis=1, keepdims=True)
            slot = jnp.sum(before * here[e], axis=1, keepdims=True) + y_shift + e * pair
            target = jnp.where(is_here > 0.5, slot, -1.0)
            hit = pick_lane == target
            picked = hit if picked is None else jnp.logical_or(picked, hit)
        pick[h * NZ + k] = picked.astype(f32).astype(bf)
        dispatch(cot_seen, cot_taken, h, k, columns_of(width))

    def hidden_chunk(h, e, n, tile):
        rows = pl.ds(h * half, half)
        tokens_in = taken[e, rows, :width]
        gate = jnp.sum(taken[e, rows, width:wide].astype(f32) * here[e], axis=1, keepdims=True)
        col = n * tile
        g = jnp.dot(tokens_in, weights[e, :, col : col + tile], preferred_element_type=f32)
        u = jnp.dot(tokens_in, weights[e, :, hidden + col : hidden + col + tile], preferred_element_type=f32)
        raw = jnp.dot(
            cot_taken[e, rows, :], weights[e, :, 2 * hidden + col : 2 * hidden + col + tile], preferred_element_type=f32
        )
        s = jax.nn.sigmoid(g)
        gs = g * s
        inner = gs * u
        scaled[e, rows, col : col + tile] = (inner * gate).astype(bf)
        grad_inner = raw * gate
        grad_act[e, rows, col : col + tile] = (grad_inner * u * s * (1.0 + g * (1.0 - s))).astype(bf)
        grad_act[e, rows, hidden + col : hidden + col + tile] = (grad_inner * gs).astype(bf)
        return jnp.sum(raw * inner, axis=1, keepdims=True)

    def hidden_part(h, e):
        tile = min(256, hidden)
        gate_grad = sum(hidden_chunk(h, e, n, tile) for n in range(hidden // tile))
        high = gate_grad.astype(bf).astype(f32)
        there = pl.ds(h * half, half)
        apart = (lane_id == EXPERT_COUNT + first + e).astype(f32)
        rows_buf[e, there, width:wide] = (high * here[e] + (gate_grad - high) * apart).astype(bf)

    def project(h, e, left, weight_cols):
        rows = pl.ds(h * half, half)
        lo, n = weight_cols
        for c0, cn in columns_of(width):
            rows_buf[e, rows, c0 : c0 + cn] = lax.dot_general(
                left[e, rows, :], weights[e, c0 : c0 + cn, lo : lo + n], (((1,), (1,)), ((), ())), preferred_element_type=f32
            ).astype(bf)

    def combine(target, h, k, cols):
        at = pl.ds(base_of(h, k), NY)
        r = (h * NZ + k) * pair
        for c0, cn in cols:
            parts = [rows_buf[e, r : r + pair, c0 : c0 + cn] for e in range(held)]
            if lanes > held * pair:
                parts.append(jnp.zeros((lanes - held * pair, cn), bf))
            got = jnp.dot(pick[h * NZ + k], jnp.concatenate(parts, axis=0), preferred_element_type=f32)
            target[at, :, c0 : c0 + cn] = got.astype(bf).reshape(NY, count, cn)

    stores = []

    def weight_grad(e, j):
        rows = pl.ds(pl.multiple_of((fsdp ^ j) * quarter, 128), quarter)
        slot = len(stores) % 2
        if len(stores) >= 2:
            stores[-2].wait()
        for c0, cn in columns_of(2 * hidden):
            stage[slot, :, c0 : c0 + cn] = lax.dot_general(
                taken[e, :, rows], grad_act[e, :, c0 : c0 + cn], (((0,), (0,)), ((), ())), preferred_element_type=f32
            ).astype(bf)
        stage[slot, :, 2 * hidden :] = lax.dot_general(
            cot_taken[e, :, rows], scaled[e], (((0,), (0,)), ((), ())), preferred_element_type=f32
        ).astype(bf)
        copy = pltpu.make_async_copy(stage.at[slot], grads[j].at[e], store_sem.at[len(stores)])
        copy.start()
        stores.append(copy)

    work = [functools.partial(cot_chunk, h, k) for h in range(NC) for k in range(NZ)]
    all_cols = columns_of(width) + [(width, 128)]
    ready = {(h, k): 0 for h in range(NC) for k in range(NZ)}
    ready[(0, 0)] = 1
    for k, flips in gather_events(plans[0].order)[1:]:
        for way in ways:
            way.step(k, flips)
        key = (1 if C in flips else 0, k)
        ready[key] += 1
        if ready[key] == NY:
            work.append(functools.partial(dispatch, seen, taken, *key, all_cols))
        for _ in range(min(len(work), 1 if k < NZ - 1 else 2)):
            work.pop(0)()
    for chunk in work:
        chunk()
    for copy in loads:
        copy.wait()
    for h in range(NC):
        for e in range(held):
            hidden_part(h, e)
    for way in ways:
        way.finish()

    far = list(reversed(range(NZ)))
    spare = spare_sem
    out_way = Reduce(place, back, seen.at[:, :, pl.ds(0, width)], (lvl_a0, lvl_a1), chain_a, send_a, recv_a, spare)
    in_way = Reduce(place, back, cot_seen, (lvl_b0, lvl_b1), chain_b, send_b, recv_b, spare)
    out_steps, in_steps = out_way.steps(), in_way.steps()

    def out_step():
        if out_steps:
            out_steps.pop(0)()

    for h in reversed(range(NC)):
        for e in range(held):
            project(h, e, scaled, (2 * hidden, hidden))
        for k in far:
            combine(seen, h, k, columns_of(width))
            if h == 1:
                out_way.first(k)
    for h in reversed(range(NC)):
        for e in range(held):
            project(h, e, grad_act, (0, 2 * hidden))
            out_step()
        for k in far:
            combine(cot_seen, h, k, all_cols)
            if h == 1:
                in_way.first(k)
            out_step()
    grad_work = [functools.partial(weight_grad, e, j) for j in reversed(range(NX * NC)) for e in range(held)]
    while out_steps or in_steps or grad_work:
        if grad_work:
            grad_work.pop(0)()
        out_step()
        if in_steps:
            in_steps.pop(0)()
        if in_steps:
            in_steps.pop(0)()
    out_way.last(moe_out)
    in_way.last(gin_out)
    for copy in stores[-2:]:
        copy.wait()
    out_way.finish()
    in_way.finish()


def moe(payload, cots, parts, cap, collective_id):
    count, wide = payload.shape
    width = wide - 128
    held, quarter, columns = parts[0].shape
    hidden = columns // 3
    cut = count * 3 // 4
    plans = [
        Plan(0, (Z, Y, C), (C, Z, Y), rows=(0, cut)),
        Plan(0, (Y, Z, C), (C, Z, Y), rows=(cut, count - cut)),
    ]
    back = Plan(0, (C, Y), (C, Z, Y))
    levels, sends, recvs = Reduce.counts(back)
    blocks = NC * NZ * NY
    pair = NY * cap
    rows = blocks // NY * pair
    lanes = tile_up(held * pair, 128)
    bf, f32 = jnp.bfloat16, jnp.float32
    whole = pl.BlockSpec(memory_space=pltpu.VMEM)
    apart = pl.BlockSpec(memory_space=pl.ANY)
    dma = pltpu.SemaphoreType.DMA
    return pl.pallas_call(
        functools.partial(moe_kernel, plans, back, width, hidden, cap),
        out_shape=[
            jax.ShapeDtypeStruct((count, wide), f32),
            jax.ShapeDtypeStruct((count, width), f32),
        ]
        + [jax.ShapeDtypeStruct((held, quarter, columns), bf)] * (NX * NC),
        in_specs=[whole] + [apart] * 5,
        out_specs=[whole] * 2 + [apart] * (NX * NC),
        scratch_shapes=[
            pltpu.VMEM((blocks, count, wide), bf),
            pltpu.VMEM((blocks, count, wide), bf),
            pltpu.VMEM((held, NX * NC * quarter, columns), bf),
            pltpu.VMEM((held, rows, wide), bf),
            pltpu.VMEM((held, rows, width), bf),
            pltpu.VMEM((held, rows, wide), bf),
            pltpu.VMEM((held, rows, hidden), bf),
            pltpu.VMEM((held, rows, 2 * hidden), bf),
            pltpu.VMEM((blocks // NY, NY * count, lanes), bf),
            pltpu.VMEM((2, quarter, columns), bf),
        ]
        + [pltpu.VMEM((n, count, width), bf) for n in levels + [NZ + 1]]
        + [pltpu.VMEM((n, count, wide), bf) for n in levels + [NZ + 1]]
        + [
            dma((sum(Gather.sends(p) for p in plans),)),
            dma((sum(p.blocks for p in plans),)),
            dma(()),
            dma((sends,)),
            dma((recvs,)),
            dma((sends,)),
            dma((recvs,)),
            dma((held * NX * NC + blocks // NY,)),
            dma((held * NX * NC,)),
        ],
        compiler_params=pltpu.CompilerParams(
            collective_id=collective_id, has_side_effects=True, vmem_limit_bytes=67043328
        ),
        name="experts",
    )(payload, cots, *parts)


MODEL_WIDTH = 1536
QUERY_HEADS = 24
KEY_VALUE_HEADS = 8
HEAD_SIZE = 64
EXPERT_HIDDEN = 512
EXPERT_COUNT = 32
TOP = 8
CAP = 40


norm_eps = 1e-06
attn_scale = 0.015625
rope_base = 10000.0
masked_logits = -1e30


def rope_tables(positions):
    half = HEAD_SIZE // 2
    frequency = jnp.power(
        jnp.float32(rope_base), -2.0 * jnp.arange(half, dtype=jnp.float32) / HEAD_SIZE
    )
    angle = positions.astype(jnp.float32)[:, None] * frequency[None, :]
    return (jnp.cos(angle)[:, None, :], jnp.sin(angle)[:, None, :])


def rotate_pairs(value_tensor, cosine_table, sine_table):
    half = value_tensor.shape[-1] // 2
    first = value_tensor[..., :half]
    second = value_tensor[..., half:]
    return jnp.concatenate(
        [first * cosine_table - second * sine_table, second * cosine_table + first * sine_table],
        axis=-1,
    )


def rms_forward(wide, gain):
    inverse = lax.rsqrt(jnp.mean(wide * wide, axis=-1, keepdims=True) + norm_eps)
    unit = wide * inverse
    return (unit, inverse, (unit * gain.astype(jnp.float32)).astype(jnp.bfloat16))


def rms_backward(grad, unit, inverse, gain):
    scaled = grad * gain.astype(jnp.float32)
    back = inverse * (scaled - unit * jnp.mean(scaled * unit, axis=-1, keepdims=True))
    return (back, jnp.sum(grad * unit, axis=0))


def piece_scores(query_rows, key_section, positions):
    token_count = key_section.shape[0]
    key_tensor = key_section.reshape(token_count, KEY_VALUE_HEADS, HEAD_SIZE)
    scores = (
        jnp.einsum("tkgd,nkd->kgtn", query_rows, key_tensor, preferred_element_type=jnp.float32)
        * attn_scale
    )
    visible = jnp.arange(token_count, dtype=jnp.int32)[None, :] <= positions[:, None]
    return (jnp.where(visible, scores, masked_logits), visible, key_tensor)


def local(
    hidden,
    routes,
    attn_norm,
    ffn_norm,
    w_q,
    key_weight,
    value_weight,
    w_o,
    router,
    expert_in,
    expert_out,
    cotangent,
):
    token_rows = hidden.shape[1]
    query_group = QUERY_HEADS // KEY_VALUE_HEADS
    ctx_size = lax.axis_size(CTX)
    sequence_length = token_rows * ctx_size
    positions = lax.axis_index(CTX) * token_rows + jnp.arange(token_rows, dtype=jnp.int32)
    cosine_table, sine_table = rope_tables(positions)
    contract_rows = (((0,), (0,)), ((), ()))
    contract_cols = (((1,), (1,)), ((), ()))
    layer = (
        lax.all_gather(attn_norm, (CTX, FSDP), axis=0, tiled=True),
        lax.all_gather(ffn_norm, (CTX, FSDP), axis=0, tiled=True),
        lax.all_gather(w_q, (CTX, FSDP), axis=0, tiled=True),
        lax.all_gather(key_weight, (CTX, FSDP), axis=0, tiled=True),
        lax.all_gather(value_weight, (CTX, FSDP), axis=0, tiled=True),
        lax.all_gather(w_o, (CTX, FSDP), axis=0, tiled=True),
        lax.all_gather(router, (CTX, FSDP), axis=0, tiled=True),
    )
    attn_gain, ffn_gain, query_w, key_weight_matrix, value_w, output_w, router_w = layer
    experts = (
        lax.all_gather(expert_in, FSDP, axis=1, tiled=True),
        lax.all_gather(expert_out, FSDP, axis=1, tiled=True),
    )
    weight_in, weight_out = experts
    wide = hidden[0].astype(jnp.float32)
    attn_unit, inverse_one, attention_input = rms_forward(wide, attn_gain)
    query_linear = jnp.dot(attention_input, query_w, preferred_element_type=jnp.float32).reshape(
        token_rows, QUERY_HEADS, HEAD_SIZE
    )
    query_rows = (
        rotate_pairs(query_linear, cosine_table, sine_table)
        .astype(jnp.bfloat16)
        .reshape(token_rows, KEY_VALUE_HEADS, query_group, HEAD_SIZE)
    )
    key_linear = jnp.dot(
        attention_input, key_weight_matrix, preferred_element_type=jnp.float32
    ).reshape(token_rows, KEY_VALUE_HEADS, HEAD_SIZE)
    key_matrix_rows = (
        rotate_pairs(key_linear, cosine_table, sine_table)
        .astype(jnp.bfloat16)
        .reshape(token_rows, KEY_VALUE_HEADS * HEAD_SIZE)
    )
    value_rows = jnp.dot(attention_input, value_w, preferred_element_type=jnp.float32).astype(
        jnp.bfloat16
    )
    init_state = (
        jnp.full((KEY_VALUE_HEADS, query_group, token_rows), masked_logits, jnp.float32),
        jnp.zeros((KEY_VALUE_HEADS, query_group, token_rows), jnp.float32),
        jnp.zeros((KEY_VALUE_HEADS, query_group, token_rows, HEAD_SIZE), jnp.float32),
    )
    key_section = lax.all_gather(key_matrix_rows, CTX, axis=0, tiled=True)
    value_section = lax.all_gather(value_rows, CTX, axis=0, tiled=True)

    def compute(current):
        best, total, weighted = current
        scores, visible, _ = piece_scores(query_rows, key_section, positions)
        value_tensor = value_section.reshape(value_section.shape[0], KEY_VALUE_HEADS, HEAD_SIZE)
        new_best = jnp.maximum(best, jnp.max(scores, axis=-1))
        weights = jnp.where(visible, jnp.exp(scores - new_best[..., None]), 0.0)
        total = jnp.sum(weights, axis=-1)
        weighted = jnp.einsum(
            "kgtn,nkd->kgtd",
            weights.astype(jnp.bfloat16),
            value_tensor,
            preferred_element_type=jnp.float32,
        )
        return (new_best, total, weighted)

    best, total, weighted = lax.cond(
        jnp.int32(0) <= positions[-1], compute, lambda current: current, init_state
    )
    log_sum_rows = best + jnp.log(total)
    attention_output = (
        jnp.transpose(weighted / total[..., None], (2, 0, 1, 3))
        .reshape(token_rows, QUERY_HEADS * HEAD_SIZE)
        .astype(jnp.bfloat16)
    )
    mixed = wide + jnp.dot(attention_output, output_w, preferred_element_type=jnp.float32)
    ffn_unit, inverse_two, ffn_in = rms_forward(mixed, ffn_gain)
    logits = jnp.dot(ffn_in, router_w, preferred_element_type=jnp.float32)
    route = routes[0]
    indicator = (route[:, :, None] == jnp.arange(EXPERT_COUNT, dtype=jnp.int32)).astype(jnp.float32)
    chosen = jnp.sum(indicator * logits[:, None, :], axis=-1)
    gates = jax.nn.softmax(chosen, axis=-1)
    flat_route = route.reshape(-1)
    counter = (flat_route[:, None] == jnp.arange(EXPERT_COUNT, dtype=jnp.int32)).astype(jnp.int32)
    slot = jnp.sum(counter * (jnp.cumsum(counter, axis=0) - 1), axis=1)
    target = flat_route * CAP + slot
    owner = (
        jnp.full((EXPERT_COUNT * CAP,), token_rows * TOP, jnp.int32)
        .at[target]
        .set(jnp.arange(token_rows * TOP, dtype=jnp.int32))
    )
    ffn_pad = jnp.concatenate([ffn_in, jnp.zeros((1, MODEL_WIDTH), jnp.bfloat16)], axis=0)
    local_experts = weight_in.shape[0]
    outgoing = ffn_pad[owner // TOP].reshape(ctx_size, local_experts, CAP, MODEL_WIDTH)
    received = lax.all_to_all(outgoing, CTX, split_axis=0, concat_axis=2, tiled=True)[0]
    act = jnp.einsum("erd,edf->erf", received, weight_in, preferred_element_type=jnp.float32)
    gate_part = act[..., :EXPERT_HIDDEN]
    up_part = act[..., EXPERT_HIDDEN:]
    sigma = jax.nn.sigmoid(gate_part)
    inner = (gate_part * sigma * up_part).astype(jnp.bfloat16)
    produced = jnp.einsum(
        "erf,edf->erd", inner, weight_out, preferred_element_type=jnp.float32
    ).astype(jnp.bfloat16)
    returned = lax.all_to_all(
        produced[None], CTX, split_axis=2, concat_axis=0, tiled=True
    ).reshape(EXPERT_COUNT * CAP, MODEL_WIDTH)
    picked = returned[target].reshape(token_rows, TOP, MODEL_WIDTH)
    layer_out = (mixed + jnp.sum(gates[..., None] * picked, axis=1)).astype(jnp.bfloat16)
    cot = cotangent[0]
    layer = (
        lax.all_gather(attn_norm, (CTX, FSDP), axis=0, tiled=True),
        lax.all_gather(ffn_norm, (CTX, FSDP), axis=0, tiled=True),
        lax.all_gather(w_q, (CTX, FSDP), axis=0, tiled=True),
        lax.all_gather(key_weight, (CTX, FSDP), axis=0, tiled=True),
        lax.all_gather(value_weight, (CTX, FSDP), axis=0, tiled=True),
        lax.all_gather(w_o, (CTX, FSDP), axis=0, tiled=True),
        lax.all_gather(router, (CTX, FSDP), axis=0, tiled=True),
    )
    attn_gain, ffn_gain, query_w, key_weight_matrix, value_w, output_w, router_w = layer
    experts = (
        lax.all_gather(expert_in, FSDP, axis=1, tiled=True),
        lax.all_gather(expert_out, FSDP, axis=1, tiled=True),
    )
    weight_in, weight_out = experts
    grad_gate = jnp.sum(cot[:, None, :] * picked, axis=-1)
    slot_grads = (
        (gates[..., None] * cot[:, None, :])
        .astype(jnp.bfloat16)
        .reshape(token_rows * TOP, MODEL_WIDTH)
    )
    slot_pad = jnp.concatenate([slot_grads, jnp.zeros((1, MODEL_WIDTH), jnp.bfloat16)], axis=0)
    grad_outgoing = slot_pad[owner].reshape(ctx_size, local_experts, CAP, MODEL_WIDTH)
    grad_received = lax.all_to_all(grad_outgoing, CTX, split_axis=0, concat_axis=2, tiled=True)[0]
    grad_w_out = jnp.einsum(
        "erd,erf->edf", grad_received, inner, preferred_element_type=jnp.float32
    )
    grad_inner = jnp.einsum(
        "erd,edf->erf", grad_received, weight_out, preferred_element_type=jnp.float32
    )
    grad_act = jnp.concatenate(
        [
            grad_inner * up_part * sigma * (1.0 + gate_part * (1.0 - sigma)),
            grad_inner * gate_part * sigma,
        ],
        axis=-1,
    ).astype(jnp.bfloat16)
    grad_w_in = jnp.einsum("erd,erf->edf", received, grad_act, preferred_element_type=jnp.float32)
    grad_rows = jnp.einsum(
        "erf,edf->erd", grad_act, weight_in, preferred_element_type=jnp.float32
    ).astype(jnp.bfloat16)
    grad_back = lax.all_to_all(
        grad_rows[None], CTX, split_axis=2, concat_axis=0, tiled=True
    ).reshape(EXPERT_COUNT * CAP, MODEL_WIDTH)
    grad_expert_in, grad_expert_out = (
        lax.psum_scatter(
            grad_w_in.astype(jnp.bfloat16), FSDP, scatter_dimension=1, tiled=True
        ).astype(jnp.float32),
        lax.psum_scatter(
            grad_w_out.astype(jnp.bfloat16), FSDP, scatter_dimension=1, tiled=True
        ).astype(jnp.float32),
    )
    grad_chosen = gates * (grad_gate - jnp.sum(gates * grad_gate, axis=-1, keepdims=True))
    grad_logits = jnp.sum(indicator * grad_chosen[..., None], axis=1).astype(jnp.bfloat16)
    grad_router_part = lax.dot_general(
        ffn_in, grad_logits, contract_rows, preferred_element_type=jnp.float32
    )
    grad_ffn_in = lax.dot_general(
        grad_logits, router_w, contract_cols, preferred_element_type=jnp.float32
    )
    grad_ffn_in = grad_ffn_in + jnp.sum(
        grad_back[target].reshape(token_rows, TOP, MODEL_WIDTH), axis=1, dtype=jnp.float32
    )
    back_two, grad_ffn_gain = rms_backward(grad_ffn_in, ffn_unit, inverse_two, ffn_gain)
    grad_mixed = cot + back_two
    grad_attn = grad_mixed.astype(jnp.bfloat16)
    grad_wo_part = lax.dot_general(
        attention_output, grad_attn, contract_rows, preferred_element_type=jnp.float32
    )
    attention_output_gradient = lax.dot_general(
        grad_attn, output_w, contract_cols, preferred_element_type=jnp.float32
    ).astype(jnp.bfloat16)
    head_gradient = attention_output_gradient.reshape(
        token_rows, KEY_VALUE_HEADS, query_group, HEAD_SIZE
    )
    delta_rows = jnp.sum(
        head_gradient.astype(jnp.float32)
        * attention_output.reshape(token_rows, KEY_VALUE_HEADS, query_group, HEAD_SIZE).astype(
            jnp.float32
        ),
        axis=-1,
    )
    delta_rows = jnp.transpose(delta_rows, (1, 2, 0))
    init_back = (
        jnp.zeros((token_rows, KEY_VALUE_HEADS, query_group, HEAD_SIZE), jnp.float32),
        jnp.zeros((sequence_length, 2 * KEY_VALUE_HEADS * HEAD_SIZE), jnp.float32),
    )
    attend_key_section = lax.all_gather(key_matrix_rows, CTX, axis=0, tiled=True)
    attend_value_section = lax.all_gather(value_rows, CTX, axis=0, tiled=True)

    def compute(current):
        token_count = attend_key_section.shape[0]
        scores, visible, key_tensor = piece_scores(query_rows, attend_key_section, positions)
        value_tensor = attend_value_section.reshape(token_count, KEY_VALUE_HEADS, HEAD_SIZE)
        weights_full = jnp.where(visible, jnp.exp(scores - log_sum_rows[..., None]), 0.0)
        grad_probs = jnp.einsum(
            "tkgd,nkd->kgtn", head_gradient, value_tensor, preferred_element_type=jnp.float32
        )
        grad_scores = (weights_full * (grad_probs - delta_rows[..., None])).astype(jnp.bfloat16)
        grad_query = attn_scale * jnp.einsum(
            "kgtn,nkd->tkgd", grad_scores, key_tensor, preferred_element_type=jnp.float32
        )
        key_portion = attn_scale * jnp.einsum(
            "kgtn,tkgd->nkd", grad_scores, query_rows, preferred_element_type=jnp.float32
        )
        value_portion = jnp.einsum(
            "kgtn,tkgd->nkd",
            weights_full.astype(jnp.bfloat16),
            head_gradient,
            preferred_element_type=jnp.float32,
        )
        update = jnp.concatenate(
            [
                key_portion.reshape(token_count, KEY_VALUE_HEADS * HEAD_SIZE),
                value_portion.reshape(token_count, KEY_VALUE_HEADS * HEAD_SIZE),
            ],
            axis=1,
        )
        return (grad_query, update)

    grad_query, grad_keys_full = lax.cond(
        jnp.int32(0) <= positions[-1], compute, lambda current: current, init_back
    )
    local_gradients = lax.psum_scatter(
        grad_keys_full.astype(jnp.bfloat16), CTX, scatter_dimension=0, tiled=True
    ).astype(jnp.float32)
    query_back = (
        rotate_pairs(
            grad_query.reshape(token_rows, QUERY_HEADS, HEAD_SIZE), cosine_table, -sine_table
        )
        .astype(jnp.bfloat16)
        .reshape(token_rows, QUERY_HEADS * HEAD_SIZE)
    )
    key_backward_rows = (
        rotate_pairs(
            local_gradients[:, : KEY_VALUE_HEADS * HEAD_SIZE].reshape(
                token_rows, KEY_VALUE_HEADS, HEAD_SIZE
            ),
            cosine_table,
            -sine_table,
        )
        .astype(jnp.bfloat16)
        .reshape(token_rows, KEY_VALUE_HEADS * HEAD_SIZE)
    )
    value_backward_rows = local_gradients[:, KEY_VALUE_HEADS * HEAD_SIZE :].astype(jnp.bfloat16)
    grad_wq_part = lax.dot_general(
        attention_input, query_back, contract_rows, preferred_element_type=jnp.float32
    )
    grad_wk_part = lax.dot_general(
        attention_input, key_backward_rows, contract_rows, preferred_element_type=jnp.float32
    )
    grad_wv_part = lax.dot_general(
        attention_input, value_backward_rows, contract_rows, preferred_element_type=jnp.float32
    )
    grad_attn_in = lax.dot_general(
        query_back, query_w, contract_cols, preferred_element_type=jnp.float32
    )
    grad_attn_in = grad_attn_in + lax.dot_general(
        key_backward_rows, key_weight_matrix, contract_cols, preferred_element_type=jnp.float32
    )
    grad_attn_in = grad_attn_in + lax.dot_general(
        value_backward_rows, value_w, contract_cols, preferred_element_type=jnp.float32
    )
    back_one, grad_attn_gain = rms_backward(grad_attn_in, attn_unit, inverse_one, attn_gain)
    grad_input = grad_mixed + back_one
    partial_sums = (
        lax.psum_scatter(
            grad_attn_gain.astype(jnp.bfloat16), CTX, scatter_dimension=0, tiled=True
        ).astype(jnp.float32),
        lax.psum_scatter(
            grad_ffn_gain.astype(jnp.bfloat16), CTX, scatter_dimension=0, tiled=True
        ).astype(jnp.float32),
        lax.psum_scatter(
            grad_wq_part.astype(jnp.bfloat16), CTX, scatter_dimension=0, tiled=True
        ).astype(jnp.float32),
        lax.psum_scatter(
            grad_wk_part.astype(jnp.bfloat16), CTX, scatter_dimension=0, tiled=True
        ).astype(jnp.float32),
        lax.psum_scatter(
            grad_wv_part.astype(jnp.bfloat16), CTX, scatter_dimension=0, tiled=True
        ).astype(jnp.float32),
        lax.psum_scatter(
            grad_wo_part.astype(jnp.bfloat16), CTX, scatter_dimension=0, tiled=True
        ).astype(jnp.float32),
        lax.psum_scatter(
            grad_router_part.astype(jnp.bfloat16), CTX, scatter_dimension=0, tiled=True
        ).astype(jnp.float32),
    )
    summed = (
        lax.psum_scatter(
            partial_sums[0].astype(jnp.bfloat16), FSDP, scatter_dimension=0, tiled=True
        ).astype(jnp.float32),
        lax.psum_scatter(
            partial_sums[1].astype(jnp.bfloat16), FSDP, scatter_dimension=0, tiled=True
        ).astype(jnp.float32),
        lax.psum_scatter(
            partial_sums[2].astype(jnp.bfloat16), FSDP, scatter_dimension=0, tiled=True
        ).astype(jnp.float32),
        lax.psum_scatter(
            partial_sums[3].astype(jnp.bfloat16), FSDP, scatter_dimension=0, tiled=True
        ).astype(jnp.float32),
        lax.psum_scatter(
            partial_sums[4].astype(jnp.bfloat16), FSDP, scatter_dimension=0, tiled=True
        ).astype(jnp.float32),
        lax.psum_scatter(
            partial_sums[5].astype(jnp.bfloat16), FSDP, scatter_dimension=0, tiled=True
        ).astype(jnp.float32),
        lax.psum_scatter(
            partial_sums[6].astype(jnp.bfloat16), FSDP, scatter_dimension=0, tiled=True
        ).astype(jnp.float32),
    )
    return (
        layer_out[None],
        grad_input[None],
        summed[0],
        summed[1],
        summed[2],
        summed[3],
        summed[4],
        summed[5],
        summed[6],
        grad_expert_in,
        grad_expert_out,
    )


def swap(a, flip):
    return lax.ppermute(a, FSDP, [(i, i ^ flip) for i in range(NX * NC)])


def fast_body(
    hidden,
    routes,
    attn_norm,
    ffn_norm,
    w_q,
    key_weight,
    value_weight,
    w_o,
    router,
    expert_in,
    expert_out,
    cotangent,
):
    tokens = hidden.shape[1]
    group = QUERY_HEADS // KEY_VALUE_HEADS
    ctx_size = NZ * NY
    ctx = lax.axis_index(CTX)
    fsdp = lax.axis_index(FSDP)
    core = fsdp % NC
    rows = w_q.shape[0]
    quarter = expert_in.shape[1]
    kv_width = KEY_VALUE_HEADS * HEAD_SIZE
    q_width = QUERY_HEADS * HEAD_SIZE
    held = expert_in.shape[0] // NC
    bf = jnp.bfloat16
    f32 = jnp.float32
    positions = ctx * tokens + jnp.arange(tokens, dtype=jnp.int32)
    cosine_table, sine_table = rope_tables(positions)
    contract_rows = (((0,), (0,)), ((), ()))
    contract_cols = (((1,), (1,)), ((), ()))
    wide = hidden[0].astype(f32)
    cot = cotangent[0]

    pack_one = jnp.concatenate([w_q, key_weight, value_weight], axis=1)
    pack_two = jnp.concatenate(
        [w_o, router, attn_norm[:, None], ffn_norm[:, None], jnp.zeros((rows, 94), bf)], axis=1
    )
    route = routes[0]
    indicator = (route[:, :, None] == jnp.arange(EXPERT_COUNT, dtype=jnp.int32)).astype(f32)
    cot_pack = jnp.concatenate(
        [
            cot.astype(bf),
            jnp.sum(indicator, axis=1).astype(bf),
            jnp.zeros((tokens, 128 - EXPERT_COUNT), bf),
        ],
        axis=1,
    )
    experts = jnp.concatenate([expert_in, expert_out], axis=2)
    experts = experts.reshape(NC, held, quarter, experts.shape[2])
    mine = lax.dynamic_index_in_dim(experts, core, 0, False)
    other = lax.dynamic_index_in_dim(experts, 1 - core, 0, False)
    parts = [mine, swap(other, 1), swap(mine, 2), swap(other, 3)]
    one, two, cots = gather(
        [pack_one, pack_two, cot_pack],
        [
            Plan(0, (X, Z, Y, C), (Z, Y, X, C), rows=(0, 2 * rows // 3)),
            Plan(0, (X, Y, Z, C), (Z, Y, X, C), rows=(2 * rows // 3, rows // 3)),
            Plan(1, (Z, Y, X, C), (Z, Y, X, C)),
            Plan(2, (Z, Y, C), (C, Z, Y)),
        ],
        0,
    )
    one = one.reshape(MODEL_WIDTH, -1)
    two = two.reshape(MODEL_WIDTH, -1)
    output_w = two[:, :MODEL_WIDTH]
    small = two[:, MODEL_WIDTH:]
    router_w = small[:, :EXPERT_COUNT]
    gains = lax.dot_general(
        jnp.eye(128, dtype=bf), small, contract_cols, preferred_element_type=f32
    )
    attn_gain, ffn_gain = gains[EXPERT_COUNT], gains[EXPERT_COUNT + 1]

    attn_unit, inverse_one, attention_input = rms_forward(wide, attn_gain)
    linear = jnp.dot(attention_input, one, preferred_element_type=f32)
    query_rows = (
        rotate_pairs(linear[:, :q_width].reshape(tokens, QUERY_HEADS, HEAD_SIZE), cosine_table, sine_table)
        .astype(bf)
        .reshape(tokens, KEY_VALUE_HEADS, group, HEAD_SIZE)
    )
    key_rows = (
        rotate_pairs(
            linear[:, q_width : q_width + kv_width].reshape(tokens, KEY_VALUE_HEADS, HEAD_SIZE),
            cosine_table,
            sine_table,
        )
        .astype(bf)
        .reshape(tokens, kv_width)
    )
    value_rows = linear[:, q_width + kv_width :].astype(bf)
    (kv,) = gather(
        [jnp.concatenate([key_rows, value_rows], axis=1)], [Plan(0, (Z, Y,), (Z, Y,))], 1
    )
    kv = kv.reshape(ctx_size * tokens, 2 * kv_width)
    key_section, value_section = kv[:, :kv_width], kv[:, kv_width:]
    value_tensor = value_section.reshape(ctx_size * tokens, KEY_VALUE_HEADS, HEAD_SIZE)
    scores, visible, key_tensor = piece_scores(query_rows, key_section, positions)
    best = jnp.max(scores, axis=-1)
    weights = jnp.where(visible, jnp.exp(scores - best[..., None]), 0.0)
    total = jnp.sum(weights, axis=-1)
    weighted = jnp.einsum(
        "kgtn,nkd->kgtd", weights.astype(bf), value_tensor, preferred_element_type=f32
    )
    log_sum_rows = best + jnp.log(total)
    attention_output = (
        jnp.transpose(weighted / total[..., None], (2, 0, 1, 3)).reshape(tokens, q_width).astype(bf)
    )
    mixed = wide + jnp.dot(attention_output, output_w, preferred_element_type=f32)
    ffn_unit, inverse_two, ffn_in = rms_forward(mixed, ffn_gain)
    logits = jnp.dot(ffn_in, router_w, preferred_element_type=f32)
    chosen = jnp.sum(indicator * logits[:, None, :], axis=-1)
    gates = jax.nn.softmax(chosen, axis=-1)
    gate_map = jnp.sum(indicator * gates[..., None], axis=1)
    payload = jnp.concatenate(
        [ffn_in, gate_map.astype(bf), jnp.zeros((tokens, 128 - EXPERT_COUNT), bf)], axis=1
    )
    gin, moe_out, *pieces = moe(payload, cots, parts, CAP, 2)
    across = [swap(pieces[j], j) for j in range(1, NX * NC)]
    own_sum = pieces[0].astype(f32) + across[1].astype(f32)
    core_sum = across[0].astype(f32) + across[2].astype(f32)
    grad_experts = jnp.where(
        core == 0,
        jnp.concatenate([own_sum, core_sum]),
        jnp.concatenate([core_sum, own_sum]),
    )
    grad_expert_in = grad_experts[:, :, : 2 * EXPERT_HIDDEN]
    grad_expert_out = grad_experts[:, :, 2 * EXPERT_HIDDEN :]
    layer_out = (mixed + moe_out).astype(bf)
    grad_gate_map = gin[:, MODEL_WIDTH : MODEL_WIDTH + EXPERT_COUNT] + gin[
        :, MODEL_WIDTH + EXPERT_COUNT : MODEL_WIDTH + 2 * EXPERT_COUNT
    ]
    grad_gate = jnp.sum(indicator * grad_gate_map[:, None, :], axis=-1)
    grad_chosen = gates * (grad_gate - jnp.sum(gates * grad_gate, axis=-1, keepdims=True))
    grad_logits = jnp.sum(indicator * grad_chosen[..., None], axis=1).astype(bf)
    grad_router_part = lax.dot_general(
        ffn_in, grad_logits, contract_rows, preferred_element_type=f32
    )
    grad_ffn_in = gin[:, :MODEL_WIDTH] + lax.dot_general(
        grad_logits, router_w, contract_cols, preferred_element_type=f32
    )
    back_two, _ = rms_backward(grad_ffn_in, ffn_unit, inverse_two, ffn_gain)
    grad_mixed = cot + back_two
    grad_attn = grad_mixed.astype(bf)
    grad_wo_part = lax.dot_general(
        attention_output, grad_attn, contract_rows, preferred_element_type=f32
    )
    attention_output_gradient = lax.dot_general(
        grad_attn, output_w, contract_cols, preferred_element_type=f32
    ).astype(bf)
    head_gradient = attention_output_gradient.reshape(tokens, KEY_VALUE_HEADS, group, HEAD_SIZE)
    delta_rows = jnp.sum(
        head_gradient.astype(f32)
        * attention_output.reshape(tokens, KEY_VALUE_HEADS, group, HEAD_SIZE).astype(f32),
        axis=-1,
    )
    delta_rows = jnp.transpose(delta_rows, (1, 2, 0))
    weights_full = jnp.where(visible, jnp.exp(scores - log_sum_rows[..., None]), 0.0)
    grad_probs = jnp.einsum(
        "tkgd,nkd->kgtn", head_gradient, value_tensor, preferred_element_type=f32
    )
    grad_scores = (weights_full * (grad_probs - delta_rows[..., None])).astype(bf)
    grad_query = attn_scale * jnp.einsum(
        "kgtn,nkd->tkgd", grad_scores, key_tensor, preferred_element_type=f32
    )
    key_portion = attn_scale * jnp.einsum(
        "kgtn,tkgd->nkd", grad_scores, query_rows, preferred_element_type=f32
    )
    value_portion = jnp.einsum(
        "kgtn,tkgd->nkd", weights_full.astype(bf), head_gradient, preferred_element_type=f32
    )
    update = jnp.concatenate(
        [
            key_portion.astype(bf).reshape(ctx_size, tokens, kv_width),
            value_portion.astype(bf).reshape(ctx_size, tokens, kv_width),
        ],
        axis=2,
    )
    (local_gradients,) = reduce_scatter([update], [Plan(0, (Y,), (Z, Y,))], [f32], 4)
    query_back = (
        rotate_pairs(
            grad_query.reshape(tokens, QUERY_HEADS, HEAD_SIZE), cosine_table, -sine_table
        )
        .astype(bf)
        .reshape(tokens, q_width)
    )
    key_back = (
        rotate_pairs(
            local_gradients[:, :kv_width].reshape(tokens, KEY_VALUE_HEADS, HEAD_SIZE),
            cosine_table,
            -sine_table,
        )
        .astype(bf)
        .reshape(tokens, kv_width)
    )
    back = jnp.concatenate([query_back, key_back, local_gradients[:, kv_width:].astype(bf)], axis=1)
    grad_one = lax.dot_general(attention_input, back, contract_rows, preferred_element_type=f32)
    grad_attn_in = lax.dot_general(back, one, contract_cols, preferred_element_type=f32)
    back_one, _ = rms_backward(grad_attn_in, attn_unit, inverse_one, attn_gain)
    grad_input = grad_mixed + back_one
    attn_gain_grad = jnp.sum(grad_attn_in * attn_unit, axis=0)
    ffn_gain_grad = jnp.sum(grad_ffn_in * ffn_unit, axis=0)
    grad_two = jnp.concatenate(
        [
            grad_wo_part,
            grad_router_part,
            attn_gain_grad[:, None],
            ffn_gain_grad[:, None],
            jnp.zeros((MODEL_WIDTH, 94), f32),
        ],
        axis=1,
    )
    sum_one, sum_two = reduce_scatter(
        [
            grad_one.astype(bf).reshape(-1, rows, grad_one.shape[1]),
            grad_two.astype(bf).reshape(-1, rows, grad_two.shape[1]),
        ],
        [Plan(0, (C, X, Y,), (Z, Y, X, C,)), Plan(1, (C, Y, X,), (Z, Y, X, C,))],
        [f32, f32],
        5,
    )
    at = MODEL_WIDTH + EXPERT_COUNT
    return (
        layer_out[None],
        grad_input[None],
        sum_two[:, at],
        sum_two[:, at + 1],
        sum_one[:, :q_width],
        sum_one[:, q_width : q_width + kv_width],
        sum_one[:, q_width + kv_width :],
        sum_two[:, :MODEL_WIDTH],
        sum_two[:, MODEL_WIDTH:at],
        grad_expert_in,
        grad_expert_out,
    )


def fast(*args):
    return fast_body(*args)


def solution(mesh):
    placed = (
        P(FSDP, CTX, None),
        P(FSDP, CTX, None),
        P((CTX, FSDP)),
        P((CTX, FSDP)),
        P((CTX, FSDP), None),
        P((CTX, FSDP), None),
        P((CTX, FSDP), None),
        P((CTX, FSDP), None),
        P((CTX, FSDP), None),
        P(CTX, FSDP, None),
        P(CTX, FSDP, None),
        P(FSDP, CTX, None),
    )
    small = mesh.shape[CTX] == NZ * NY and mesh.shape[FSDP] == NX * NC
    return jax.shard_map(
        fast if small else local,
        mesh=mesh,
        in_specs=placed,
        out_specs=(
            P(FSDP, CTX, None),
            P(FSDP, CTX, None),
            P((CTX, FSDP)),
            P((CTX, FSDP)),
            P((CTX, FSDP), None),
            P((CTX, FSDP), None),
            P((CTX, FSDP), None),
            P((CTX, FSDP), None),
            P((CTX, FSDP), None),
            P(CTX, FSDP, None),
            P(CTX, FSDP, None),
        ),
        check_vma=False,
    )
```

```python
import functools
import itertools

import jax
import jax.numpy as jnp
from jax import lax
from jax.experimental import pallas as pl
from jax.experimental.pallas import tpu as pltpu
from jax.sharding import PartitionSpec as P


NY = 2
NZ = 4
NX = 2
NC = 2
DEV = pl.DeviceIdType.MESH
CTX, FSDP = "ctx", "fsdp"
Z, Y, X, C = 0, 1, 2, 3
SIZES = {Z: NZ, Y: NY, X: NX, C: NC}
UP, DOWN = 4, 5


class Plan:
    def __init__(self, ref, order, index, rows=None, view=None):
        self.ref, self.order, self.index, self.rows, self.view = ref, order, index, rows, view
        self.blocks = 1
        for d in index:
            self.blocks *= SIZES[d]


class Place:
    def __init__(self):
        ctx = lax.axis_index(CTX)
        fsdp = lax.axis_index(FSDP)
        self.at = {Z: ctx // NY, Y: ctx % NY, X: fsdp // NC, C: fsdp % NC}
        z = self.at[Z]
        low = z < NZ // 2
        base = jnp.where(low, z, NZ - 1 - z)
        near = [base, 1 - base, jnp.int32(2), jnp.int32(3)]
        self.order = [z] + [jnp.where(low, k, NZ - 1 - k) for k in near[1:]]

    def device(self, dim, value):
        spot = dict(self.at)
        spot[dim] = value
        return (spot[Z] * NY + spot[Y], spot[X] * NC + spot[C])

    def across(self, dim):
        return self.device(dim, 1 - self.at[dim])

    def along(self, step):
        return self.device(Z, self.at[Z] + step)

    def coords(self, z_from, flips):
        spot = {d: (1 - self.at[d] if d in flips else self.at[d]) for d in (Y, X, C)}
        spot[Z] = z_from
        return spot


def flat_index(spot, dims):
    index = 0
    for d in dims:
        index = index * SIZES[d] + spot[d]
    return index


def subsets(dims):
    return [c for n in range(len(dims) + 1) for c in itertools.combinations(dims, n)]


def greet(place, dims):
    barrier = pltpu.get_barrier_semaphore()
    z = place.at[Z]
    count = jnp.int32(0)
    for d in dims:
        if d == Z:
            @pl.when(z > 0)
            def _():
                pl.semaphore_signal(barrier, inc=1, device_id=place.along(-1), device_id_type=DEV)

            @pl.when(z < NZ - 1)
            def _():
                pl.semaphore_signal(barrier, inc=1, device_id=place.along(1), device_id_type=DEV)

            count = count + jnp.where(z > 0, 1, 0) + jnp.where(z < NZ - 1, 1, 0)
        else:
            pl.semaphore_signal(barrier, inc=1, device_id=place.across(d), device_id_type=DEV)
            count = count + 1
    pl.semaphore_wait(barrier, count)


def gather_events(order):
    pairs = [d for d in order if d != Z]
    events = [(k, f) for k in range(NZ) for f in subsets(pairs)]
    return sorted(events, key=lambda e: (e[0] + len(e[1]), len(e[1])))


def gather_sends(order, k, flips):
    z_at = order.index(Z)
    last = max([order.index(d) for d in flips] + ([z_at] if k > 0 else []) + [-1])
    out = []
    for position, d in enumerate(order):
        if position > last:
            out.extend([UP, DOWN] if d == Z else [d])
    if k > 0 and last == z_at:
        out.extend([UP, DOWN])
    return out


def gather_kernel(plans, n_in, *refs):
    ins, outs = refs[:n_in], refs[n_in : 2 * n_in]
    send_sem, recv_sem, own_sem = refs[2 * n_in :]
    place = Place()
    z = place.at[Z]
    greet(place, sorted({d for p in plans for d in p.order}))
    pending = []
    slot = 0
    queue = []
    for n, plan in enumerate(plans):
        for rank, event in enumerate(gather_events(plan.order)):
            queue.append((rank / len(gather_events(plan.order)), n, event))
    queue.sort(key=lambda q: (q[0], q[1]))
    bases = [sum(p.blocks for p in plans[:n]) for n in range(len(plans))]
    for _, n, (k, flips) in queue:
        plan = plans[n]
        src = ins[plan.ref]
        out = outs[plan.ref]
        rows = plan.rows
        z_from = place.order[k]
        spot = place.coords(z_from, flips)
        index = flat_index(spot, plan.index)
        own = k == 0 and not flips
        if plan.view is not None:
            target = plan.view(out, spot, rows)
            source = src.at[:, pl.ds(rows[0], rows[1])] if own else target
        else:
            target = out.at[index] if rows is None else out.at[index, pl.ds(rows[0], rows[1])]
            source = (src if rows is None else src.at[pl.ds(rows[0], rows[1])]) if own else target
        sem = recv_sem.at[bases[n] + index]
        if not own:
            pltpu.make_async_remote_copy(
                src_ref=target, dst_ref=target, send_sem=own_sem.at[0], recv_sem=sem,
                device_id=place.across(C), device_id_type=DEV,
            ).wait_recv()
        for way in gather_sends(plan.order, k, flips):
            if way in (UP, DOWN):
                step = 1 if way == UP else -1
                go = z < NZ - 1 if way == UP else z > 0
                if k > 0:
                    go = jnp.logical_and(go, z_from < z if way == UP else z_from > z)
                dest = place.device(Z, jnp.clip(z + step, 0, NZ - 1))
            else:
                go, dest = None, place.across(way)
            copy = pltpu.make_async_remote_copy(
                src_ref=source, dst_ref=target, send_sem=send_sem.at[slot], recv_sem=sem,
                device_id=dest, device_id_type=DEV,
            )
            slot += 1
            if go is None:
                copy.start()
            else:
                pl.when(go)(copy.start)
            pending.append((go, copy.wait_send))
        if own:
            copy = pltpu.make_async_copy(source, target, own_sem.at[1 + n])
            copy.start()
            pending.append((None, copy.wait))
    for go, wait in pending:
        if go is None:
            wait()
        else:
            pl.when(go)(wait)


def gather(arrays, plans, collective_id, shapes=None):
    n = len(arrays)
    sends = sum(len(gather_sends(p.order, k, f)) for p in plans for k, f in gather_events(p.order))
    blocks = {p.ref: p.blocks for p in plans}
    return pl.pallas_call(
        functools.partial(gather_kernel, plans, n),
        out_shape=[
            jax.ShapeDtypeStruct((shapes or {}).get(i, (blocks[i],) + a.shape), a.dtype)
            for i, a in enumerate(arrays)
        ],
        in_specs=[pl.BlockSpec(memory_space=pltpu.VMEM)] * n,
        out_specs=[pl.BlockSpec(memory_space=pl.ANY)] * n,
        scratch_shapes=[
            pltpu.SemaphoreType.DMA((sends,)),
            pltpu.SemaphoreType.DMA((sum(p.blocks for p in plans),)),
            pltpu.SemaphoreType.DMA((1 + len(plans),)),
        ],
        compiler_params=pltpu.CompilerParams(collective_id=collective_id, has_side_effects=True),
    )(*arrays)


def add_into(acc, other):
    acc[...] = (acc[...].astype(jnp.float32) + other[...].astype(jnp.float32)).astype(acc.dtype)


def reduce_kernel(plans, n_in, *refs):
    ins, outs = refs[:n_in], refs[n_in : 2 * n_in]
    rest = list(refs[2 * n_in :])
    send_sem, recv_sem, own_sem = rest[:3]
    buffers = rest[3:]
    place = Place()
    z = place.at[Z]
    greet(place, sorted({d for p in plans for d in p.order} | {Z}))
    pending = []
    slots = [0, 0]

    def push(source, target, sem, dest):
        copy = pltpu.make_async_remote_copy(
            src_ref=source, dst_ref=target, send_sem=send_sem.at[slots[0]], recv_sem=sem,
            device_id=dest, device_id_type=DEV,
        )
        slots[0] += 1
        copy.start()
        pending.append(copy)

    def arrived(target, sem):
        pltpu.make_async_remote_copy(
            src_ref=target, dst_ref=target, send_sem=own_sem.at[0], recv_sem=sem,
            device_id=place.across(C), device_id_type=DEV,
        ).wait_recv()

    work = []
    far = list(reversed(range(NZ)))
    own_slot = 1
    state = []
    base = 0
    for n, plan in enumerate(plans):
        dims = plan.order
        acc = buffers[0]
        levels = buffers[1 : 1 + len(dims)]
        chain = buffers[1 + len(dims)]
        buffers = buffers[2 + len(dims) :]
        kept = [subsets(dims[p + 1 :]) for p in range(len(dims))]
        counts = [NZ * len(f) for f in kept]
        level_base = [base + sum(counts[:p]) for p in range(len(dims))]
        chain_base = base + sum(counts)
        base = chain_base + 2 * NZ
        state.append((acc, levels, chain, kept, level_base, chain_base))
        own_copies = {}
        src = ins[plan.ref]
        for k in far:
            for f in kept[0]:
                gone = flat_index(place.coords(place.order[k], (dims[0],) + f), plan.index)
                spot = place.order[k] * len(kept[0]) + kept[0].index(f)
                work.append((0, n, k, f, gone, spot))
                mine = flat_index(place.coords(place.order[k], f), plan.index)
                copy = pltpu.make_async_copy(src.at[mine], acc.at[spot], own_sem.at[own_slot])
                own_slot += 1
                own_copies[(k, f)] = copy
        state[-1] += (own_copies,)
    for _, n, k, f, gone, spot in sorted(work, key=lambda w: (-w[2],)):
        plan = plans[n]
        acc, levels, chain, kept, level_base, chain_base, own_copies = state[n]
        push(ins[plan.ref].at[gone], levels[0].at[spot], recv_sem.at[level_base[0] + spot], place.across(plan.order[0]))
        own_copies[(k, f)].start()

    def level_step(n, p, k):
        plan = plans[n]
        dims = plan.order
        acc, levels, _, kept, level_base, _, own_copies = state[n]
        for f in sorted(kept[p], key=lambda f: -len(f)):
            spot = place.order[k] * len(kept[p]) + kept[p].index(f)
            at = place.order[k] * len(kept[0]) + kept[0].index(f)
            if p == 0:
                own_copies[(k, f)].wait()
            arrived(levels[p].at[spot], recv_sem.at[level_base[p] + spot])
            add_into(acc.at[at], levels[p].at[spot])
            later = p + 1
            if later < len(dims) and dims[later] in f:
                left = tuple(d for d in f if d != dims[later])
                there = place.order[k] * len(kept[later]) + kept[later].index(left)
                push(
                    acc.at[at], levels[later].at[there],
                    recv_sem.at[level_base[later] + there], place.across(dims[later]),
                )

    def chain_step(n, k):
        acc, _, chain, kept, _, chain_base, _ = state[n]
        dest = place.order[k]
        up = dest > z
        lane = jnp.where(up, 0, 1)
        at = dest * len(kept[0])
        spot = lane * NZ + dest

        @pl.when(jnp.where(up, z > 0, z < NZ - 1))
        def _():
            arrived(chain.at[spot], recv_sem.at[chain_base + spot])
            add_into(acc.at[at], chain.at[spot])

        push(acc.at[at], chain.at[spot], recv_sem.at[chain_base + spot], place.along(jnp.where(up, 1, -1)))

    most = max(len(p.order) for p in plans)
    for step in range(NZ + most):
        for n, plan in enumerate(plans):
            for p in range(len(plan.order)):
                if 0 <= step - p < NZ:
                    level_step(n, p, far[step - p])
            p = len(plan.order)
            if 0 <= step - p < NZ - 1:
                chain_step(n, far[step - p])
    for n, plan in enumerate(plans):
        acc, levels, chain, kept, level_base, chain_base, own_copies = state[n]
        at = z * len(kept[0])

        @pl.when(z > 0)
        def _():
            spot = z
            arrived(chain.at[spot], recv_sem.at[chain_base + spot])
            add_into(acc.at[at], chain.at[spot])

        @pl.when(z < NZ - 1)
        def _():
            spot = NZ + z
            arrived(chain.at[spot], recv_sem.at[chain_base + spot])
            add_into(acc.at[at], chain.at[spot])

        outs[plan.ref][...] = acc[at].astype(outs[plan.ref].dtype)
    for copy in pending:
        copy.wait_send()


def reduce_scatter(arrays, plans, out_dtypes, collective_id):
    n = len(arrays)
    scratch = []
    sends = recvs = owns = 0
    for p in plans:
        a = arrays[p.ref]
        block = a.shape[1:]
        kept = [len(subsets(p.order[q + 1 :])) for q in range(len(p.order))]
        scratch.append(pltpu.VMEM((NZ * kept[0],) + block, a.dtype))
        for q in kept:
            scratch.append(pltpu.VMEM((NZ * q,) + block, a.dtype))
        scratch.append(pltpu.VMEM((2 * NZ,) + block, a.dtype))
        sends += NZ * sum(kept) + NZ - 1
        recvs += NZ * sum(kept) + 2 * NZ
        owns += NZ * kept[0]
    return pl.pallas_call(
        functools.partial(reduce_kernel, plans, n),
        out_shape=[jax.ShapeDtypeStruct(a.shape[1:], d) for a, d in zip(arrays, out_dtypes)],
        in_specs=[pl.BlockSpec(memory_space=pl.ANY)] * n,
        out_specs=[pl.BlockSpec(memory_space=pltpu.VMEM)] * n,
        scratch_shapes=[
            pltpu.SemaphoreType.DMA((sends,)),
            pltpu.SemaphoreType.DMA((recvs,)),
            pltpu.SemaphoreType.DMA((1 + owns,)),
        ]
        + scratch,
        compiler_params=pltpu.CompilerParams(
            collective_id=collective_id, has_side_effects=True, vmem_limit_bytes=60 * 1024 * 1024
        ),
    )(*arrays)


class Gather:
    def __init__(self, place, plan, src, out, send_sem, recv_sem, spare_sem, slot, base):
        self.place, self.plan, self.src, self.out = place, plan, src, out
        self.send_sem, self.recv_sem, self.spare_sem = send_sem, recv_sem, spare_sem
        self.slot, self.base = slot, base
        self.pending = []

    @staticmethod
    def sends(plan):
        return sum(len(gather_sends(plan.order, k, f)) for k, f in gather_events(plan.order))

    def step(self, k, flips):
        place, plan = self.place, self.plan
        z = place.at[Z]
        z_from = place.order[k]
        index = flat_index(place.coords(z_from, flips), plan.index)
        rows = plan.rows
        target = self.out.at[index] if rows is None else self.out.at[index, pl.ds(rows[0], rows[1])]
        sem = self.recv_sem.at[self.base + index]
        own = k == 0 and not flips
        source = target
        if own:
            source = self.src if rows is None else self.src.at[pl.ds(rows[0], rows[1])]
        else:
            pltpu.make_async_remote_copy(
                src_ref=target, dst_ref=target, send_sem=self.spare_sem, recv_sem=sem,
                device_id=place.across(C), device_id_type=DEV,
            ).wait_recv()
        for way in gather_sends(plan.order, k, flips):
            if way in (UP, DOWN):
                step = 1 if way == UP else -1
                go = z < NZ - 1 if way == UP else z > 0
                if k > 0:
                    go = jnp.logical_and(go, z_from < z if way == UP else z_from > z)
                dest = place.device(Z, jnp.clip(z + step, 0, NZ - 1))
            else:
                go, dest = None, place.across(way)
            copy = pltpu.make_async_remote_copy(
                src_ref=source, dst_ref=target, send_sem=self.send_sem.at[self.slot], recv_sem=sem,
                device_id=dest, device_id_type=DEV,
            )
            self.slot += 1
            if go is None:
                copy.start()
            else:
                pl.when(go)(copy.start)
            self.pending.append((go, copy.wait_send))

    def finish(self):
        for go, wait in self.pending:
            if go is None:
                wait()
            else:
                pl.when(go)(wait)


class Reduce:
    def __init__(self, place, plan, held, levels, chain, send_sem, recv_sem, spare_sem):
        self.place, self.plan, self.held, self.levels, self.chain = place, plan, held, levels, chain
        self.send_sem, self.recv_sem, self.spare_sem = send_sem, recv_sem, spare_sem
        dims = plan.order
        self.kept = [subsets(dims[p + 1 :]) for p in range(len(dims))]
        self.base = [NZ * sum(len(f) for f in self.kept[:p]) for p in range(len(dims) + 1)]
        self.slot = 0
        self.pending = []

    @staticmethod
    def counts(plan):
        kept = [NZ * len(subsets(plan.order[p + 1 :])) for p in range(len(plan.order))]
        return kept, sum(kept) + NZ - 1, sum(kept) + NZ + 1

    def push(self, source, target, sem, dest):
        copy = pltpu.make_async_remote_copy(
            src_ref=source, dst_ref=target, send_sem=self.send_sem.at[self.slot], recv_sem=sem,
            device_id=dest, device_id_type=DEV,
        )
        self.slot += 1
        copy.start()
        self.pending.append(copy)

    def arrived(self, target, sem):
        pltpu.make_async_remote_copy(
            src_ref=target, dst_ref=target, send_sem=self.spare_sem, recv_sem=sem,
            device_id=self.place.across(C), device_id_type=DEV,
        ).wait_recv()

    def block(self, k, flips):
        return flat_index(self.place.coords(self.place.order[k], flips), self.plan.index)

    def first(self, k):
        dim = self.plan.order[0]
        for n, f in enumerate(self.kept[0]):
            spot = self.place.order[k] * len(self.kept[0]) + n
            self.push(
                self.held.at[self.block(k, (dim,) + f)], self.levels[0].at[spot],
                self.recv_sem.at[spot], self.place.across(dim),
            )

    def level(self, p, k):
        dims = self.plan.order
        z_to = self.place.order[k]
        for f in sorted(self.kept[p], key=lambda f: -len(f)):
            spot = z_to * len(self.kept[p]) + self.kept[p].index(f)
            mine = self.held.at[self.block(k, f)]
            self.arrived(self.levels[p].at[spot], self.recv_sem.at[self.base[p] + spot])
            add_into(mine, self.levels[p].at[spot])
            later = p + 1
            if later < len(dims) and dims[later] in f:
                left = tuple(d for d in f if d != dims[later])
                there = z_to * len(self.kept[later]) + self.kept[later].index(left)
                self.push(
                    mine, self.levels[later].at[there],
                    self.recv_sem.at[self.base[later] + there], self.place.across(dims[later]),
                )

    def along(self, k):
        z = self.place.at[Z]
        dest = self.place.order[k]
        up = dest > z
        spot = dest + jnp.where(up, 1, 0)
        mine = self.held.at[self.block(k, ())]
        sem = self.recv_sem.at[self.base[-1] + spot]

        @pl.when(jnp.where(up, z > 0, z < NZ - 1))
        def _():
            self.arrived(self.chain.at[spot], sem)
            add_into(mine, self.chain.at[spot])

        self.push(mine, self.chain.at[spot], sem, self.place.along(jnp.where(up, 1, -1)))

    def last(self, out):
        z = self.place.at[Z]
        mine = self.held.at[self.block(0, ())]
        for go, spot in ((z > 0, z + 1), (z < NZ - 1, z)):

            @pl.when(go)
            def _():
                self.arrived(self.chain.at[spot], self.recv_sem.at[self.base[-1] + spot])
                add_into(mine, self.chain.at[spot])

        out[...] = mine[...].astype(out.dtype)

    def at_time(self, t):
        depth = len(self.plan.order)
        far = list(reversed(range(NZ)))
        out = [functools.partial(self.level, p, far[t - p]) for p in range(depth) if 0 <= t - p < NZ]
        if 0 <= t - depth < NZ - 1:
            out.append(functools.partial(self.along, far[t - depth]))
        return out

    def steps(self):
        return [step for t in range(NZ + len(self.plan.order)) for step in self.at_time(t)]

    def finish(self):
        for copy in self.pending:
            copy.wait_send()


def tile_up(n, m):
    return (n + m - 1) // m * m


def columns_of(width, chunk=512):
    return [(i, min(chunk, width - i)) for i in range(0, width, chunk)]


def moe_kernel(plans, back, width, hidden, cap, *refs):
    payload, cots, w_own, w_core, w_x, w_both = refs[:6]
    gin_out, moe_out = refs[6:8]
    grads = refs[8:12]
    (
        seen, cot_seen, weights, taken, cot_taken, rows_buf, scaled, grad_act, pick, stage,
        lvl_a0, lvl_a1, chain_a, lvl_b0, lvl_b1, chain_b,
        send_sem, recv_sem, spare_sem, send_a, recv_a, send_b, recv_b, load_sem, store_sem,
    ) = refs[12:]
    bf, f32 = jnp.bfloat16, jnp.float32
    place = Place()
    count = payload.shape[0]
    pair = 2 * cap
    wide = width + 128
    quarter = width // (NX * NC)
    half = NZ * pair
    lanes = pick.shape[2]
    held = weights.shape[0]
    fsdp = place.at[X] * NC + place.at[C]
    first = (((place.at[Z] * NY + place.at[Y]) * NC) + place.at[C]) * held

    loads = []
    for j, ref in enumerate((w_own, w_core, w_x, w_both)):
        rows = pl.ds(pl.multiple_of((fsdp ^ j) * quarter, quarter), quarter)
        for e in range(held):
            loads.append(pltpu.make_async_copy(ref.at[e], weights.at[e, rows], load_sem.at[len(loads)]))
    base_of = lambda h, k: (jnp.where(h == 0, place.at[C], 1 - place.at[C]) * NZ + place.order[k]) * NY
    cot_loads = {}
    for k in range(NZ):
        for h in range(2):
            at = pl.ds(base_of(h, k), NY)
            cot_loads[(h, k)] = pltpu.make_async_copy(cots.at[at], cot_seen.at[at], load_sem.at[len(loads) + len(cot_loads)])

    greet(place, (Z, Y, C))
    ways = []
    send_at = 0
    for n, plan in enumerate(plans):
        ways.append(Gather(place, plan, payload, seen, send_sem, recv_sem, spare_sem, send_at, n * plan.blocks))
        send_at += Gather.sends(plan)
    for way in ways:
        way.step(0, ())
    for key in cot_loads:
        cot_loads[key].start()
    for copy in loads:
        copy.start()
    seen[flat_index(place.at, plans[0].index)] = payload[...]

    row_id = lax.broadcasted_iota(jnp.int32, (NY * count, NY * count), 0)
    col_id = lax.broadcasted_iota(jnp.int32, (NY * count, NY * count), 1)
    earlier = jnp.logical_and(col_id < row_id, col_id // count == row_id // count).astype(bf)
    lane_id = lax.broadcasted_iota(jnp.int32, (1, 128), 1)
    here = [(lane_id == first + e).astype(f32) for e in range(held)]
    pick_lane = lax.broadcasted_iota(jnp.int32, (NY * count, lanes), 1).astype(f32)
    y_shift = (lax.broadcasted_iota(jnp.int32, (NY * count, 1), 0) // count * cap).astype(f32)

    def dispatch(source, target, h, k, cols):
        at = pl.ds(base_of(h, k), NY)
        r = (h * NZ + k) * pair
        for c0, cn in cols:
            block = source[at, :, c0 : c0 + cn].reshape(NY * count, cn)
            got = lax.dot_general(
                pick[h * NZ + k], block, (((0,), (0,)), ((), ())), preferred_element_type=f32
            ).astype(bf)
            for e in range(held):
                target[e, r : r + pair, c0 : c0 + cn] = got[e * pair : (e + 1) * pair]

    def cot_chunk(h, k):
        cot_loads[(h, k)].wait()
        at = pl.ds(base_of(h, k), NY)
        chosen = cot_seen[at, :, width:wide].reshape(NY * count, 128)
        before = jnp.dot(earlier, chosen, preferred_element_type=f32)
        picked = None
        for e in range(held):
            is_here = jnp.sum(chosen.astype(f32) * here[e], axis=1, keepdims=True)
            slot = jnp.sum(before * here[e], axis=1, keepdims=True) + y_shift + e * pair
            target = jnp.where(is_here > 0.5, slot, -1.0)
            hit = pick_lane == target
            picked = hit if picked is None else jnp.logical_or(picked, hit)
        pick[h * NZ + k] = picked.astype(f32).astype(bf)
        dispatch(cot_seen, cot_taken, h, k, columns_of(width))

    def hidden_chunk(h, e, n, tile):
        rows = pl.ds(h * half, half)
        tokens_in = taken[e, rows, :width]
        gate = jnp.sum(taken[e, rows, width:wide].astype(f32) * here[e], axis=1, keepdims=True)
        col = n * tile
        g = jnp.dot(tokens_in, weights[e, :, col : col + tile], preferred_element_type=f32)
        u = jnp.dot(tokens_in, weights[e, :, hidden + col : hidden + col + tile], preferred_element_type=f32)
        raw = jnp.dot(
            cot_taken[e, rows, :], weights[e, :, 2 * hidden + col : 2 * hidden + col + tile], preferred_element_type=f32
        )
        s = jax.nn.sigmoid(g)
        gs = g * s
        inner = gs * u
        scaled[e, rows, col : col + tile] = (inner * gate).astype(bf)
        grad_inner = raw * gate
        grad_act[e, rows, col : col + tile] = (grad_inner * u * s * (1.0 + g * (1.0 - s))).astype(bf)
        grad_act[e, rows, hidden + col : hidden + col + tile] = (grad_inner * gs).astype(bf)
        return jnp.sum(raw * inner, axis=1, keepdims=True)

    def hidden_part(h, e):
        tile = min(256, hidden)
        gate_grad = sum(hidden_chunk(h, e, n, tile) for n in range(hidden // tile))
        high = gate_grad.astype(bf).astype(f32)
        there = pl.ds(h * half, half)
        apart = (lane_id == EXPERT_COUNT + first + e).astype(f32)
        rows_buf[e, there, width:wide] = (high * here[e] + (gate_grad - high) * apart).astype(bf)

    def project(h, e, left, weight_cols):
        rows = pl.ds(h * half, half)
        lo, n = weight_cols
        for c0, cn in columns_of(width):
            rows_buf[e, rows, c0 : c0 + cn] = lax.dot_general(
                left[e, rows, :], weights[e, c0 : c0 + cn, lo : lo + n], (((1,), (1,)), ((), ())), preferred_element_type=f32
            ).astype(bf)

    def combine(target, h, k, cols):
        at = pl.ds(base_of(h, k), NY)
        r = (h * NZ + k) * pair
        for c0, cn in cols:
            parts = [rows_buf[e, r : r + pair, c0 : c0 + cn] for e in range(held)]
            if lanes > held * pair:
                parts.append(jnp.zeros((lanes - held * pair, cn), bf))
            got = jnp.dot(pick[h * NZ + k], jnp.concatenate(parts, axis=0), preferred_element_type=f32)
            target[at, :, c0 : c0 + cn] = got.astype(bf).reshape(NY, count, cn)

    stores = []

    def weight_grad(e, j):
        rows = pl.ds(pl.multiple_of((fsdp ^ j) * quarter, 128), quarter)
        slot = len(stores) % 2
        if len(stores) >= 2:
            stores[-2].wait()
        for c0, cn in columns_of(2 * hidden):
            stage[slot, :, c0 : c0 + cn] = lax.dot_general(
                taken[e, :, rows], grad_act[e, :, c0 : c0 + cn], (((0,), (0,)), ((), ())), preferred_element_type=f32
            ).astype(bf)
        stage[slot, :, 2 * hidden :] = lax.dot_general(
            cot_taken[e, :, rows], scaled[e], (((0,), (0,)), ((), ())), preferred_element_type=f32
        ).astype(bf)
        copy = pltpu.make_async_copy(stage.at[slot], grads[j].at[e], store_sem.at[len(stores)])
        copy.start()
        stores.append(copy)

    work = [functools.partial(cot_chunk, h, k) for h in range(NC) for k in range(NZ)]
    all_cols = columns_of(width) + [(width, 128)]
    ready = {(h, k): 0 for h in range(NC) for k in range(NZ)}
    ready[(0, 0)] = 1
    for k, flips in gather_events(plans[0].order)[1:]:
        for way in ways:
            way.step(k, flips)
        key = (1 if C in flips else 0, k)
        ready[key] += 1
        if ready[key] == NY:
            work.append(functools.partial(dispatch, seen, taken, *key, all_cols))
        for _ in range(min(len(work), 1 if k < NZ - 1 else 2)):
            work.pop(0)()
    for chunk in work:
        chunk()
    for copy in loads:
        copy.wait()
    for h in range(NC):
        for e in range(held):
            hidden_part(h, e)
    for way in ways:
        way.finish()

    far = list(reversed(range(NZ)))
    spare = spare_sem
    out_way = Reduce(place, back, seen.at[:, :, pl.ds(0, width)], (lvl_a0, lvl_a1), chain_a, send_a, recv_a, spare)
    in_way = Reduce(place, back, cot_seen, (lvl_b0, lvl_b1), chain_b, send_b, recv_b, spare)
    out_steps, in_steps = out_way.steps(), in_way.steps()

    def out_step():
        if out_steps:
            out_steps.pop(0)()

    for h in reversed(range(NC)):
        for e in range(held):
            project(h, e, scaled, (2 * hidden, hidden))
        for k in far:
            combine(seen, h, k, columns_of(width))
            if h == 1:
                out_way.first(k)
    for h in reversed(range(NC)):
        for e in range(held):
            project(h, e, grad_act, (0, 2 * hidden))
            out_step()
        for k in far:
            combine(cot_seen, h, k, all_cols)
            if h == 1:
                in_way.first(k)
            out_step()
    grad_work = [functools.partial(weight_grad, e, j) for j in reversed(range(NX * NC)) for e in range(held)]
    while out_steps or in_steps or grad_work:
        if grad_work:
            grad_work.pop(0)()
        out_step()
        if in_steps:
            in_steps.pop(0)()
        if in_steps:
            in_steps.pop(0)()
    out_way.last(moe_out)
    in_way.last(gin_out)
    for copy in stores[-2:]:
        copy.wait()
    out_way.finish()
    in_way.finish()


def moe(payload, cots, parts, cap, collective_id):
    count, wide = payload.shape
    width = wide - 128
    held, quarter, columns = parts[0].shape
    hidden = columns // 3
    cut = count * 3 // 4
    plans = [
        Plan(0, (Z, Y, C), (C, Z, Y), rows=(0, cut)),
        Plan(0, (Y, Z, C), (C, Z, Y), rows=(cut, count - cut)),
    ]
    back = Plan(0, (C, Y), (C, Z, Y))
    levels, sends, recvs = Reduce.counts(back)
    blocks = NC * NZ * NY
    pair = NY * cap
    rows = blocks // NY * pair
    lanes = tile_up(held * pair, 128)
    bf, f32 = jnp.bfloat16, jnp.float32
    whole = pl.BlockSpec(memory_space=pltpu.VMEM)
    apart = pl.BlockSpec(memory_space=pl.ANY)
    dma = pltpu.SemaphoreType.DMA
    return pl.pallas_call(
        functools.partial(moe_kernel, plans, back, width, hidden, cap),
        out_shape=[
            jax.ShapeDtypeStruct((count, wide), f32),
            jax.ShapeDtypeStruct((count, width), f32),
        ]
        + [jax.ShapeDtypeStruct((held, quarter, columns), bf)] * (NX * NC),
        in_specs=[whole] + [apart] * 5,
        out_specs=[whole] * 2 + [apart] * (NX * NC),
        scratch_shapes=[
            pltpu.VMEM((blocks, count, wide), bf),
            pltpu.VMEM((blocks, count, wide), bf),
            pltpu.VMEM((held, NX * NC * quarter, columns), bf),
            pltpu.VMEM((held, rows, wide), bf),
            pltpu.VMEM((held, rows, width), bf),
            pltpu.VMEM((held, rows, wide), bf),
            pltpu.VMEM((held, rows, hidden), bf),
            pltpu.VMEM((held, rows, 2 * hidden), bf),
            pltpu.VMEM((blocks // NY, NY * count, lanes), bf),
            pltpu.VMEM((2, quarter, columns), bf),
        ]
        + [pltpu.VMEM((n, count, width), bf) for n in levels + [NZ + 1]]
        + [pltpu.VMEM((n, count, wide), bf) for n in levels + [NZ + 1]]
        + [
            dma((sum(Gather.sends(p) for p in plans),)),
            dma((sum(p.blocks for p in plans),)),
            dma(()),
            dma((sends,)),
            dma((recvs,)),
            dma((sends,)),
            dma((recvs,)),
            dma((held * NX * NC + blocks // NY,)),
            dma((held * NX * NC,)),
        ],
        compiler_params=pltpu.CompilerParams(
            collective_id=collective_id, has_side_effects=True, vmem_limit_bytes=67043328
        ),
        name="experts",
    )(payload, cots, *parts)


def weight_view(out, spot, rows):
    return out.at[spot[Z] * NY + spot[Y], :, spot[C], pl.ds(rows[0], rows[1])]


def weights_kernel(plans, *refs):
    left_one, right_one, left_two, right_two, left_small, right_small = refs[:6]
    outs = refs[6:8]
    held_one, held_two = refs[8:10]
    buffers = refs[10:18]
    send_one, recv_one, send_two, recv_two, spare = refs[18:]
    place = Place()
    greet(place, (Z, Y, X, C))
    ways = [
        Reduce(place, plans[0], held_one, buffers[0:3], buffers[3], send_one, recv_one, spare),
        Reduce(place, plans[1], held_two, buffers[4:7], buffers[7], send_two, recv_two, spare),
    ]
    group = NY * NX * NC
    rows = group * held_one.shape[1]

    def products(left, right, held, k, shift):
        at = pl.ds(pl.multiple_of(place.order[k] * rows, 128), rows)
        block = left[:, at]
        for c0, cn in columns_of(right.shape[1]):
            got = lax.dot_general(
                block, right[:, c0 : c0 + cn], (((0,), (0,)), ((), ())), preferred_element_type=jnp.float32
            )
            held[pl.ds(place.order[k] * group, group), :, shift + c0 : shift + c0 + cn] = got.astype(
                held.dtype
            ).reshape(group, rows // group, cn)

    far = list(reversed(range(NZ)))
    for t in range(NZ):
        k = far[t]
        products(left_one, right_one, held_one, k, 0)
        ways[0].first(k)
        products(left_two, right_two, held_two, k, 0)
        products(left_small, right_small, held_two, k, right_two.shape[1])
        ways[1].first(k)
        if t > 0:
            for way in ways:
                for step in way.at_time(t - 1):
                    step()
    for t in range(NZ - 1, NZ + 3):
        for way in ways:
            for step in way.at_time(t):
                step()
    for way, out in zip(ways, outs):
        way.last(out)
    for way in ways:
        way.finish()


def return_weights(lefts, rights, collective_id):
    width = lefts[0].shape[1]
    rows = width // (NZ * NY * NX * NC)
    widths = [rights[0].shape[1], rights[1].shape[1] + rights[2].shape[1]]
    plans = [Plan(0, (C, X, Y), (Z, Y, X, C)), Plan(1, (C, Y, X), (Z, Y, X, C))]
    bf = jnp.bfloat16
    levels, sends, recvs = Reduce.counts(plans[0])
    dma = pltpu.SemaphoreType.DMA
    operands = [a for pair in zip(lefts, rights) for a in pair]
    return pl.pallas_call(
        functools.partial(weights_kernel, plans),
        out_shape=[jax.ShapeDtypeStruct((rows, w), jnp.float32) for w in widths],
        in_specs=[pl.BlockSpec(memory_space=pltpu.VMEM)] * 6,
        out_specs=[pl.BlockSpec(memory_space=pltpu.VMEM)] * 2,
        scratch_shapes=[pltpu.VMEM((plans[0].blocks, rows, w), bf) for w in widths]
        + [pltpu.VMEM((n, rows, w), bf) for w in widths for n in levels + [NZ + 1]]
        + [dma((sends,)), dma((recvs,)), dma((sends,)), dma((recvs,)), dma(())],
        compiler_params=pltpu.CompilerParams(
            collective_id=collective_id, has_side_effects=True, vmem_limit_bytes=60 * 1024 * 1024
        ),
        name="return_weights",
    )(*operands)


MODEL_WIDTH = 1536
QUERY_HEADS = 24
KEY_VALUE_HEADS = 8
HEAD_SIZE = 64
EXPERT_HIDDEN = 512
EXPERT_COUNT = 32
TOP = 8
CAP = 40


norm_eps = 1e-06
attn_scale = 0.015625
rope_base = 10000.0
masked_logits = -1e30


def rope_tables(positions):
    half = HEAD_SIZE // 2
    frequency = jnp.power(
        jnp.float32(rope_base), -2.0 * jnp.arange(half, dtype=jnp.float32) / HEAD_SIZE
    )
    angle = positions.astype(jnp.float32)[:, None] * frequency[None, :]
    return (jnp.cos(angle)[:, None, :], jnp.sin(angle)[:, None, :])


def rotate_pairs(value_tensor, cosine_table, sine_table):
    half = value_tensor.shape[-1] // 2
    first = value_tensor[..., :half]
    second = value_tensor[..., half:]
    return jnp.concatenate(
        [first * cosine_table - second * sine_table, second * cosine_table + first * sine_table],
        axis=-1,
    )


def rms_forward(wide, gain):
    inverse = lax.rsqrt(jnp.mean(wide * wide, axis=-1, keepdims=True) + norm_eps)
    unit = wide * inverse
    return (unit, inverse, (unit * gain.astype(jnp.float32)).astype(jnp.bfloat16))


def rms_backward(grad, unit, inverse, gain):
    scaled = grad * gain.astype(jnp.float32)
    back = inverse * (scaled - unit * jnp.mean(scaled * unit, axis=-1, keepdims=True))
    return (back, jnp.sum(grad * unit, axis=0))


def piece_scores(query_rows, key_section, positions):
    token_count = key_section.shape[0]
    key_tensor = key_section.reshape(token_count, KEY_VALUE_HEADS, HEAD_SIZE)
    scores = (
        jnp.einsum("tkgd,nkd->kgtn", query_rows, key_tensor, preferred_element_type=jnp.float32)
        * attn_scale
    )
    visible = jnp.arange(token_count, dtype=jnp.int32)[None, :] <= positions[:, None]
    return (jnp.where(visible, scores, masked_logits), visible, key_tensor)


def local(
    hidden,
    routes,
    attn_norm,
    ffn_norm,
    w_q,
    key_weight,
    value_weight,
    w_o,
    router,
    expert_in,
    expert_out,
    cotangent,
):
    token_rows = hidden.shape[1]
    query_group = QUERY_HEADS // KEY_VALUE_HEADS
    ctx_size = lax.axis_size(CTX)
    sequence_length = token_rows * ctx_size
    positions = lax.axis_index(CTX) * token_rows + jnp.arange(token_rows, dtype=jnp.int32)
    cosine_table, sine_table = rope_tables(positions)
    contract_rows = (((0,), (0,)), ((), ()))
    contract_cols = (((1,), (1,)), ((), ()))
    layer = (
        lax.all_gather(attn_norm, (CTX, FSDP), axis=0, tiled=True),
        lax.all_gather(ffn_norm, (CTX, FSDP), axis=0, tiled=True),
        lax.all_gather(w_q, (CTX, FSDP), axis=0, tiled=True),
        lax.all_gather(key_weight, (CTX, FSDP), axis=0, tiled=True),
        lax.all_gather(value_weight, (CTX, FSDP), axis=0, tiled=True),
        lax.all_gather(w_o, (CTX, FSDP), axis=0, tiled=True),
        lax.all_gather(router, (CTX, FSDP), axis=0, tiled=True),
    )
    attn_gain, ffn_gain, query_w, key_weight_matrix, value_w, output_w, router_w = layer
    experts = (
        lax.all_gather(expert_in, FSDP, axis=1, tiled=True),
        lax.all_gather(expert_out, FSDP, axis=1, tiled=True),
    )
    weight_in, weight_out = experts
    wide = hidden[0].astype(jnp.float32)
    attn_unit, inverse_one, attention_input = rms_forward(wide, attn_gain)
    query_linear = jnp.dot(attention_input, query_w, preferred_element_type=jnp.float32).reshape(
        token_rows, QUERY_HEADS, HEAD_SIZE
    )
    query_rows = (
        rotate_pairs(query_linear, cosine_table, sine_table)
        .astype(jnp.bfloat16)
        .reshape(token_rows, KEY_VALUE_HEADS, query_group, HEAD_SIZE)
    )
    key_linear = jnp.dot(
        attention_input, key_weight_matrix, preferred_element_type=jnp.float32
    ).reshape(token_rows, KEY_VALUE_HEADS, HEAD_SIZE)
    key_matrix_rows = (
        rotate_pairs(key_linear, cosine_table, sine_table)
        .astype(jnp.bfloat16)
        .reshape(token_rows, KEY_VALUE_HEADS * HEAD_SIZE)
    )
    value_rows = jnp.dot(attention_input, value_w, preferred_element_type=jnp.float32).astype(
        jnp.bfloat16
    )
    init_state = (
        jnp.full((KEY_VALUE_HEADS, query_group, token_rows), masked_logits, jnp.float32),
        jnp.zeros((KEY_VALUE_HEADS, query_group, token_rows), jnp.float32),
        jnp.zeros((KEY_VALUE_HEADS, query_group, token_rows, HEAD_SIZE), jnp.float32),
    )
    key_section = lax.all_gather(key_matrix_rows, CTX, axis=0, tiled=True)
    value_section = lax.all_gather(value_rows, CTX, axis=0, tiled=True)

    def compute(current):
        best, total, weighted = current
        scores, visible, _ = piece_scores(query_rows, key_section, positions)
        value_tensor = value_section.reshape(value_section.shape[0], KEY_VALUE_HEADS, HEAD_SIZE)
        new_best = jnp.maximum(best, jnp.max(scores, axis=-1))
        weights = jnp.where(visible, jnp.exp(scores - new_best[..., None]), 0.0)
        total = jnp.sum(weights, axis=-1)
        weighted = jnp.einsum(
            "kgtn,nkd->kgtd",
            weights.astype(jnp.bfloat16),
            value_tensor,
            preferred_element_type=jnp.float32,
        )
        return (new_best, total, weighted)

    best, total, weighted = lax.cond(
        jnp.int32(0) <= positions[-1], compute, lambda current: current, init_state
    )
    log_sum_rows = best + jnp.log(total)
    attention_output = (
        jnp.transpose(weighted / total[..., None], (2, 0, 1, 3))
        .reshape(token_rows, QUERY_HEADS * HEAD_SIZE)
        .astype(jnp.bfloat16)
    )
    mixed = wide + jnp.dot(attention_output, output_w, preferred_element_type=jnp.float32)
    ffn_unit, inverse_two, ffn_in = rms_forward(mixed, ffn_gain)
    logits = jnp.dot(ffn_in, router_w, preferred_element_type=jnp.float32)
    route = routes[0]
    indicator = (route[:, :, None] == jnp.arange(EXPERT_COUNT, dtype=jnp.int32)).astype(jnp.float32)
    chosen = jnp.sum(indicator * logits[:, None, :], axis=-1)
    gates = jax.nn.softmax(chosen, axis=-1)
    flat_route = route.reshape(-1)
    counter = (flat_route[:, None] == jnp.arange(EXPERT_COUNT, dtype=jnp.int32)).astype(jnp.int32)
    slot = jnp.sum(counter * (jnp.cumsum(counter, axis=0) - 1), axis=1)
    target = flat_route * CAP + slot
    owner = (
        jnp.full((EXPERT_COUNT * CAP,), token_rows * TOP, jnp.int32)
        .at[target]
        .set(jnp.arange(token_rows * TOP, dtype=jnp.int32))
    )
    ffn_pad = jnp.concatenate([ffn_in, jnp.zeros((1, MODEL_WIDTH), jnp.bfloat16)], axis=0)
    local_experts = weight_in.shape[0]
    outgoing = ffn_pad[owner // TOP].reshape(ctx_size, local_experts, CAP, MODEL_WIDTH)
    received = lax.all_to_all(outgoing, CTX, split_axis=0, concat_axis=2, tiled=True)[0]
    act = jnp.einsum("erd,edf->erf", received, weight_in, preferred_element_type=jnp.float32)
    gate_part = act[..., :EXPERT_HIDDEN]
    up_part = act[..., EXPERT_HIDDEN:]
    sigma = jax.nn.sigmoid(gate_part)
    inner = (gate_part * sigma * up_part).astype(jnp.bfloat16)
    produced = jnp.einsum(
        "erf,edf->erd", inner, weight_out, preferred_element_type=jnp.float32
    ).astype(jnp.bfloat16)
    returned = lax.all_to_all(
        produced[None], CTX, split_axis=2, concat_axis=0, tiled=True
    ).reshape(EXPERT_COUNT * CAP, MODEL_WIDTH)
    picked = returned[target].reshape(token_rows, TOP, MODEL_WIDTH)
    layer_out = (mixed + jnp.sum(gates[..., None] * picked, axis=1)).astype(jnp.bfloat16)
    cot = cotangent[0]
    layer = (
        lax.all_gather(attn_norm, (CTX, FSDP), axis=0, tiled=True),
        lax.all_gather(ffn_norm, (CTX, FSDP), axis=0, tiled=True),
        lax.all_gather(w_q, (CTX, FSDP), axis=0, tiled=True),
        lax.all_gather(key_weight, (CTX, FSDP), axis=0, tiled=True),
        lax.all_gather(value_weight, (CTX, FSDP), axis=0, tiled=True),
        lax.all_gather(w_o, (CTX, FSDP), axis=0, tiled=True),
        lax.all_gather(router, (CTX, FSDP), axis=0, tiled=True),
    )
    attn_gain, ffn_gain, query_w, key_weight_matrix, value_w, output_w, router_w = layer
    experts = (
        lax.all_gather(expert_in, FSDP, axis=1, tiled=True),
        lax.all_gather(expert_out, FSDP, axis=1, tiled=True),
    )
    weight_in, weight_out = experts
    grad_gate = jnp.sum(cot[:, None, :] * picked, axis=-1)
    slot_grads = (
        (gates[..., None] * cot[:, None, :])
        .astype(jnp.bfloat16)
        .reshape(token_rows * TOP, MODEL_WIDTH)
    )
    slot_pad = jnp.concatenate([slot_grads, jnp.zeros((1, MODEL_WIDTH), jnp.bfloat16)], axis=0)
    grad_outgoing = slot_pad[owner].reshape(ctx_size, local_experts, CAP, MODEL_WIDTH)
    grad_received = lax.all_to_all(grad_outgoing, CTX, split_axis=0, concat_axis=2, tiled=True)[0]
    grad_w_out = jnp.einsum(
        "erd,erf->edf", grad_received, inner, preferred_element_type=jnp.float32
    )
    grad_inner = jnp.einsum(
        "erd,edf->erf", grad_received, weight_out, preferred_element_type=jnp.float32
    )
    grad_act = jnp.concatenate(
        [
            grad_inner * up_part * sigma * (1.0 + gate_part * (1.0 - sigma)),
            grad_inner * gate_part * sigma,
        ],
        axis=-1,
    ).astype(jnp.bfloat16)
    grad_w_in = jnp.einsum("erd,erf->edf", received, grad_act, preferred_element_type=jnp.float32)
    grad_rows = jnp.einsum(
        "erf,edf->erd", grad_act, weight_in, preferred_element_type=jnp.float32
    ).astype(jnp.bfloat16)
    grad_back = lax.all_to_all(
        grad_rows[None], CTX, split_axis=2, concat_axis=0, tiled=True
    ).reshape(EXPERT_COUNT * CAP, MODEL_WIDTH)
    grad_expert_in, grad_expert_out = (
        lax.psum_scatter(
            grad_w_in.astype(jnp.bfloat16), FSDP, scatter_dimension=1, tiled=True
        ).astype(jnp.float32),
        lax.psum_scatter(
            grad_w_out.astype(jnp.bfloat16), FSDP, scatter_dimension=1, tiled=True
        ).astype(jnp.float32),
    )
    grad_chosen = gates * (grad_gate - jnp.sum(gates * grad_gate, axis=-1, keepdims=True))
    grad_logits = jnp.sum(indicator * grad_chosen[..., None], axis=1).astype(jnp.bfloat16)
    grad_router_part = lax.dot_general(
        ffn_in, grad_logits, contract_rows, preferred_element_type=jnp.float32
    )
    grad_ffn_in = lax.dot_general(
        grad_logits, router_w, contract_cols, preferred_element_type=jnp.float32
    )
    grad_ffn_in = grad_ffn_in + jnp.sum(
        grad_back[target].reshape(token_rows, TOP, MODEL_WIDTH), axis=1, dtype=jnp.float32
    )
    back_two, grad_ffn_gain = rms_backward(grad_ffn_in, ffn_unit, inverse_two, ffn_gain)
    grad_mixed = cot + back_two
    grad_attn = grad_mixed.astype(jnp.bfloat16)
    grad_wo_part = lax.dot_general(
        attention_output, grad_attn, contract_rows, preferred_element_type=jnp.float32
    )
    attention_output_gradient = lax.dot_general(
        grad_attn, output_w, contract_cols, preferred_element_type=jnp.float32
    ).astype(jnp.bfloat16)
    head_gradient = attention_output_gradient.reshape(
        token_rows, KEY_VALUE_HEADS, query_group, HEAD_SIZE
    )
    delta_rows = jnp.sum(
        head_gradient.astype(jnp.float32)
        * attention_output.reshape(token_rows, KEY_VALUE_HEADS, query_group, HEAD_SIZE).astype(
            jnp.float32
        ),
        axis=-1,
    )
    delta_rows = jnp.transpose(delta_rows, (1, 2, 0))
    init_back = (
        jnp.zeros((token_rows, KEY_VALUE_HEADS, query_group, HEAD_SIZE), jnp.float32),
        jnp.zeros((sequence_length, 2 * KEY_VALUE_HEADS * HEAD_SIZE), jnp.float32),
    )
    attend_key_section = lax.all_gather(key_matrix_rows, CTX, axis=0, tiled=True)
    attend_value_section = lax.all_gather(value_rows, CTX, axis=0, tiled=True)

    def compute(current):
        token_count = attend_key_section.shape[0]
        scores, visible, key_tensor = piece_scores(query_rows, attend_key_section, positions)
        value_tensor = attend_value_section.reshape(token_count, KEY_VALUE_HEADS, HEAD_SIZE)
        weights_full = jnp.where(visible, jnp.exp(scores - log_sum_rows[..., None]), 0.0)
        grad_probs = jnp.einsum(
            "tkgd,nkd->kgtn", head_gradient, value_tensor, preferred_element_type=jnp.float32
        )
        grad_scores = (weights_full * (grad_probs - delta_rows[..., None])).astype(jnp.bfloat16)
        grad_query = attn_scale * jnp.einsum(
            "kgtn,nkd->tkgd", grad_scores, key_tensor, preferred_element_type=jnp.float32
        )
        key_portion = attn_scale * jnp.einsum(
            "kgtn,tkgd->nkd", grad_scores, query_rows, preferred_element_type=jnp.float32
        )
        value_portion = jnp.einsum(
            "kgtn,tkgd->nkd",
            weights_full.astype(jnp.bfloat16),
            head_gradient,
            preferred_element_type=jnp.float32,
        )
        update = jnp.concatenate(
            [
                key_portion.reshape(token_count, KEY_VALUE_HEADS * HEAD_SIZE),
                value_portion.reshape(token_count, KEY_VALUE_HEADS * HEAD_SIZE),
            ],
            axis=1,
        )
        return (grad_query, update)

    grad_query, grad_keys_full = lax.cond(
        jnp.int32(0) <= positions[-1], compute, lambda current: current, init_back
    )
    local_gradients = lax.psum_scatter(
        grad_keys_full.astype(jnp.bfloat16), CTX, scatter_dimension=0, tiled=True
    ).astype(jnp.float32)
    query_back = (
        rotate_pairs(
            grad_query.reshape(token_rows, QUERY_HEADS, HEAD_SIZE), cosine_table, -sine_table
        )
        .astype(jnp.bfloat16)
        .reshape(token_rows, QUERY_HEADS * HEAD_SIZE)
    )
    key_backward_rows = (
        rotate_pairs(
            local_gradients[:, : KEY_VALUE_HEADS * HEAD_SIZE].reshape(
                token_rows, KEY_VALUE_HEADS, HEAD_SIZE
            ),
            cosine_table,
            -sine_table,
        )
        .astype(jnp.bfloat16)
        .reshape(token_rows, KEY_VALUE_HEADS * HEAD_SIZE)
    )
    value_backward_rows = local_gradients[:, KEY_VALUE_HEADS * HEAD_SIZE :].astype(jnp.bfloat16)
    grad_wq_part = lax.dot_general(
        attention_input, query_back, contract_rows, preferred_element_type=jnp.float32
    )
    grad_wk_part = lax.dot_general(
        attention_input, key_backward_rows, contract_rows, preferred_element_type=jnp.float32
    )
    grad_wv_part = lax.dot_general(
        attention_input, value_backward_rows, contract_rows, preferred_element_type=jnp.float32
    )
    grad_attn_in = lax.dot_general(
        query_back, query_w, contract_cols, preferred_element_type=jnp.float32
    )
    grad_attn_in = grad_attn_in + lax.dot_general(
        key_backward_rows, key_weight_matrix, contract_cols, preferred_element_type=jnp.float32
    )
    grad_attn_in = grad_attn_in + lax.dot_general(
        value_backward_rows, value_w, contract_cols, preferred_element_type=jnp.float32
    )
    back_one, grad_attn_gain = rms_backward(grad_attn_in, attn_unit, inverse_one, attn_gain)
    grad_input = grad_mixed + back_one
    partial_sums = (
        lax.psum_scatter(
            grad_attn_gain.astype(jnp.bfloat16), CTX, scatter_dimension=0, tiled=True
        ).astype(jnp.float32),
        lax.psum_scatter(
            grad_ffn_gain.astype(jnp.bfloat16), CTX, scatter_dimension=0, tiled=True
        ).astype(jnp.float32),
        lax.psum_scatter(
            grad_wq_part.astype(jnp.bfloat16), CTX, scatter_dimension=0, tiled=True
        ).astype(jnp.float32),
        lax.psum_scatter(
            grad_wk_part.astype(jnp.bfloat16), CTX, scatter_dimension=0, tiled=True
        ).astype(jnp.float32),
        lax.psum_scatter(
            grad_wv_part.astype(jnp.bfloat16), CTX, scatter_dimension=0, tiled=True
        ).astype(jnp.float32),
        lax.psum_scatter(
            grad_wo_part.astype(jnp.bfloat16), CTX, scatter_dimension=0, tiled=True
        ).astype(jnp.float32),
        lax.psum_scatter(
            grad_router_part.astype(jnp.bfloat16), CTX, scatter_dimension=0, tiled=True
        ).astype(jnp.float32),
    )
    summed = (
        lax.psum_scatter(
            partial_sums[0].astype(jnp.bfloat16), FSDP, scatter_dimension=0, tiled=True
        ).astype(jnp.float32),
        lax.psum_scatter(
            partial_sums[1].astype(jnp.bfloat16), FSDP, scatter_dimension=0, tiled=True
        ).astype(jnp.float32),
        lax.psum_scatter(
            partial_sums[2].astype(jnp.bfloat16), FSDP, scatter_dimension=0, tiled=True
        ).astype(jnp.float32),
        lax.psum_scatter(
            partial_sums[3].astype(jnp.bfloat16), FSDP, scatter_dimension=0, tiled=True
        ).astype(jnp.float32),
        lax.psum_scatter(
            partial_sums[4].astype(jnp.bfloat16), FSDP, scatter_dimension=0, tiled=True
        ).astype(jnp.float32),
        lax.psum_scatter(
            partial_sums[5].astype(jnp.bfloat16), FSDP, scatter_dimension=0, tiled=True
        ).astype(jnp.float32),
        lax.psum_scatter(
            partial_sums[6].astype(jnp.bfloat16), FSDP, scatter_dimension=0, tiled=True
        ).astype(jnp.float32),
    )
    return (
        layer_out[None],
        grad_input[None],
        summed[0],
        summed[1],
        summed[2],
        summed[3],
        summed[4],
        summed[5],
        summed[6],
        grad_expert_in,
        grad_expert_out,
    )


def swap(a, flip):
    return lax.ppermute(a, FSDP, [(i, i ^ flip) for i in range(NX * NC)])


def fast_body(
    hidden,
    routes,
    attn_norm,
    ffn_norm,
    w_q,
    key_weight,
    value_weight,
    w_o,
    router,
    expert_in,
    expert_out,
    cotangent,
):
    tokens = hidden.shape[1]
    group = QUERY_HEADS // KEY_VALUE_HEADS
    ctx_size = NZ * NY
    ctx = lax.axis_index(CTX)
    fsdp = lax.axis_index(FSDP)
    core = fsdp % NC
    rows = w_q.shape[0]
    quarter = expert_in.shape[1]
    kv_width = KEY_VALUE_HEADS * HEAD_SIZE
    q_width = QUERY_HEADS * HEAD_SIZE
    held = expert_in.shape[0] // NC
    bf = jnp.bfloat16
    f32 = jnp.float32
    positions = ctx * tokens + jnp.arange(tokens, dtype=jnp.int32)
    cosine_table, sine_table = rope_tables(positions)
    contract_cols = (((1,), (1,)), ((), ()))
    wide = hidden[0].astype(f32)
    cot = cotangent[0]

    pack_one = jnp.concatenate([w_q, key_weight, value_weight], axis=1)
    pack_two = jnp.concatenate(
        [w_o, router, attn_norm[:, None], ffn_norm[:, None], jnp.zeros((rows, 94), bf)], axis=1
    )
    route = routes[0]
    indicator = (route[:, :, None] == jnp.arange(EXPERT_COUNT, dtype=jnp.int32)).astype(f32)
    cot_pack = jnp.concatenate(
        [
            cot.astype(bf),
            jnp.sum(indicator, axis=1).astype(bf),
            jnp.zeros((tokens, 128 - EXPERT_COUNT), bf),
        ],
        axis=1,
    )
    experts = jnp.concatenate([expert_in, expert_out], axis=2)
    experts = experts.reshape(NC, held, quarter, experts.shape[2])
    mine = lax.dynamic_index_in_dim(experts, core, 0, False)
    other = lax.dynamic_index_in_dim(experts, 1 - core, 0, False)
    far_one, far_two = swap(pack_one, 2), swap(pack_two, 2)
    far_one, far_two, mine, other = lax.optimization_barrier((far_one, far_two, mine, other))
    parts = [mine, swap(other, 1), swap(mine, 2), swap(other, 3)]
    both = lambda near, far: jnp.where(
        fsdp < NC, jnp.stack([near, far]), jnp.stack([far, near])
    )
    part = rows // 3
    groups = ctx_size, NX, NC, rows
    one, two, cots = gather(
        [both(pack_one, far_one), both(pack_two, far_two), cot_pack],
        [
            Plan(0, (Z, Y, C), (Z, Y, C), rows=(0, 2 * part), view=weight_view),
            Plan(0, (Y, Z, C), (Z, Y, C), rows=(2 * part, part), view=weight_view),
            Plan(1, (Z, Y, C), (Z, Y, C), rows=(0, rows), view=weight_view),
            Plan(2, (Z, Y, C), (C, Z, Y)),
        ],
        0,
        {0: groups + pack_one.shape[1:], 1: groups + pack_two.shape[1:]},
    )
    one = one.reshape(MODEL_WIDTH, -1)
    two = two.reshape(MODEL_WIDTH, -1)
    output_w = two[:, :MODEL_WIDTH]
    small = two[:, MODEL_WIDTH:]
    router_w = small[:, :EXPERT_COUNT]
    gains = lax.dot_general(
        jnp.eye(128, dtype=bf), small, contract_cols, preferred_element_type=f32
    )
    attn_gain, ffn_gain = gains[EXPERT_COUNT], gains[EXPERT_COUNT + 1]

    attn_unit, inverse_one, attention_input = rms_forward(wide, attn_gain)
    linear = jnp.dot(attention_input, one, preferred_element_type=f32)
    query_rows = (
        rotate_pairs(linear[:, :q_width].reshape(tokens, QUERY_HEADS, HEAD_SIZE), cosine_table, sine_table)
        .astype(bf)
        .reshape(tokens, KEY_VALUE_HEADS, group, HEAD_SIZE)
    )
    key_rows = (
        rotate_pairs(
            linear[:, q_width : q_width + kv_width].reshape(tokens, KEY_VALUE_HEADS, HEAD_SIZE),
            cosine_table,
            sine_table,
        )
        .astype(bf)
        .reshape(tokens, kv_width)
    )
    value_rows = linear[:, q_width + kv_width :].astype(bf)
    (kv,) = gather(
        [jnp.concatenate([key_rows, value_rows], axis=1)], [Plan(0, (Z, Y,), (Z, Y,))], 1
    )
    kv = kv.reshape(ctx_size * tokens, 2 * kv_width)
    key_section, value_section = kv[:, :kv_width], kv[:, kv_width:]
    value_tensor = value_section.reshape(ctx_size * tokens, KEY_VALUE_HEADS, HEAD_SIZE)
    scores, visible, key_tensor = piece_scores(query_rows, key_section, positions)
    best = jnp.max(scores, axis=-1)
    weights = jnp.where(visible, jnp.exp(scores - best[..., None]), 0.0)
    total = jnp.sum(weights, axis=-1)
    weighted = jnp.einsum(
        "kgtn,nkd->kgtd", weights.astype(bf), value_tensor, preferred_element_type=f32
    )
    log_sum_rows = best + jnp.log(total)
    attention_output = (
        jnp.transpose(weighted / total[..., None], (2, 0, 1, 3)).reshape(tokens, q_width).astype(bf)
    )
    mixed = wide + jnp.dot(attention_output, output_w, preferred_element_type=f32)
    ffn_unit, inverse_two, ffn_in = rms_forward(mixed, ffn_gain)
    logits = jnp.dot(ffn_in, router_w, preferred_element_type=f32)
    chosen = jnp.sum(indicator * logits[:, None, :], axis=-1)
    gates = jax.nn.softmax(chosen, axis=-1)
    gate_map = jnp.sum(indicator * gates[..., None], axis=1)
    payload = jnp.concatenate(
        [ffn_in, gate_map.astype(bf), jnp.zeros((tokens, 128 - EXPERT_COUNT), bf)], axis=1
    )
    gin, moe_out, *pieces = moe(payload, cots, parts, CAP, 2)
    across = [swap(pieces[j], j) for j in range(1, NX * NC)]
    own_sum = pieces[0].astype(f32) + across[1].astype(f32)
    core_sum = across[0].astype(f32) + across[2].astype(f32)
    grad_experts = jnp.where(
        core == 0,
        jnp.concatenate([own_sum, core_sum]),
        jnp.concatenate([core_sum, own_sum]),
    )
    grad_expert_in = grad_experts[:, :, : 2 * EXPERT_HIDDEN]
    grad_expert_out = grad_experts[:, :, 2 * EXPERT_HIDDEN :]
    layer_out = (mixed + moe_out).astype(bf)
    grad_gate_map = gin[:, MODEL_WIDTH : MODEL_WIDTH + EXPERT_COUNT] + gin[
        :, MODEL_WIDTH + EXPERT_COUNT : MODEL_WIDTH + 2 * EXPERT_COUNT
    ]
    grad_gate = jnp.sum(indicator * grad_gate_map[:, None, :], axis=-1)
    grad_chosen = gates * (grad_gate - jnp.sum(gates * grad_gate, axis=-1, keepdims=True))
    grad_logits = jnp.sum(indicator * grad_chosen[..., None], axis=1).astype(bf)
    grad_ffn_in = gin[:, :MODEL_WIDTH] + lax.dot_general(
        grad_logits, router_w, contract_cols, preferred_element_type=f32
    )
    back_two, _ = rms_backward(grad_ffn_in, ffn_unit, inverse_two, ffn_gain)
    grad_mixed = cot + back_two
    grad_attn = grad_mixed.astype(bf)
    attention_output_gradient = lax.dot_general(
        grad_attn, output_w, contract_cols, preferred_element_type=f32
    ).astype(bf)
    head_gradient = attention_output_gradient.reshape(tokens, KEY_VALUE_HEADS, group, HEAD_SIZE)
    delta_rows = jnp.sum(
        head_gradient.astype(f32)
        * attention_output.reshape(tokens, KEY_VALUE_HEADS, group, HEAD_SIZE).astype(f32),
        axis=-1,
    )
    delta_rows = jnp.transpose(delta_rows, (1, 2, 0))
    weights_full = jnp.where(visible, jnp.exp(scores - log_sum_rows[..., None]), 0.0)
    grad_probs = jnp.einsum(
        "tkgd,nkd->kgtn", head_gradient, value_tensor, preferred_element_type=f32
    )
    grad_scores = (weights_full * (grad_probs - delta_rows[..., None])).astype(bf)
    grad_query = attn_scale * jnp.einsum(
        "kgtn,nkd->tkgd", grad_scores, key_tensor, preferred_element_type=f32
    )
    key_portion = attn_scale * jnp.einsum(
        "kgtn,tkgd->nkd", grad_scores, query_rows, preferred_element_type=f32
    )
    value_portion = jnp.einsum(
        "kgtn,tkgd->nkd", weights_full.astype(bf), head_gradient, preferred_element_type=f32
    )
    update = jnp.concatenate(
        [
            key_portion.astype(bf).reshape(ctx_size, tokens, kv_width),
            value_portion.astype(bf).reshape(ctx_size, tokens, kv_width),
        ],
        axis=2,
    )
    (local_gradients,) = reduce_scatter([update], [Plan(0, (Y,), (Z, Y,))], [f32], 4)
    query_back = (
        rotate_pairs(
            grad_query.reshape(tokens, QUERY_HEADS, HEAD_SIZE), cosine_table, -sine_table
        )
        .astype(bf)
        .reshape(tokens, q_width)
    )
    key_back = (
        rotate_pairs(
            local_gradients[:, :kv_width].reshape(tokens, KEY_VALUE_HEADS, HEAD_SIZE),
            cosine_table,
            -sine_table,
        )
        .astype(bf)
        .reshape(tokens, kv_width)
    )
    back = jnp.concatenate([query_back, key_back, local_gradients[:, kv_width:].astype(bf)], axis=1)
    grad_attn_in = lax.dot_general(back, one, contract_cols, preferred_element_type=f32)
    back_one, _ = rms_backward(grad_attn_in, attn_unit, inverse_one, attn_gain)
    grad_input = grad_mixed + back_one
    halves = []
    for factor in (grad_attn_in * attn_unit, grad_ffn_in * ffn_unit):
        high = factor.astype(bf)
        halves += [high, (factor - high.astype(f32)).astype(bf)]
    column = lambda n: jnp.broadcast_to((jnp.arange(128) == n).astype(bf), (tokens, 128))
    sum_one, sum_two = return_weights(
        [attention_input, attention_output, jnp.concatenate([ffn_in] + halves)],
        [
            back,
            grad_attn,
            jnp.concatenate(
                [
                    jnp.concatenate([grad_logits, jnp.zeros((tokens, 128 - EXPERT_COUNT), bf)], axis=1),
                    column(EXPERT_COUNT),
                    column(EXPERT_COUNT),
                    column(EXPERT_COUNT + 1),
                    column(EXPERT_COUNT + 1),
                ]
            ),
        ],
        5,
    )
    at = MODEL_WIDTH + EXPERT_COUNT
    return (
        layer_out[None],
        grad_input[None],
        sum_two[:, at],
        sum_two[:, at + 1],
        sum_one[:, :q_width],
        sum_one[:, q_width : q_width + kv_width],
        sum_one[:, q_width + kv_width :],
        sum_two[:, :MODEL_WIDTH],
        sum_two[:, MODEL_WIDTH:at],
        grad_expert_in,
        grad_expert_out,
    )


def fast(*args):
    return fast_body(*args)


def solution(mesh):
    placed = (
        P(FSDP, CTX, None),
        P(FSDP, CTX, None),
        P((CTX, FSDP)),
        P((CTX, FSDP)),
        P((CTX, FSDP), None),
        P((CTX, FSDP), None),
        P((CTX, FSDP), None),
        P((CTX, FSDP), None),
        P((CTX, FSDP), None),
        P(CTX, FSDP, None),
        P(CTX, FSDP, None),
        P(FSDP, CTX, None),
    )
    small = mesh.shape[CTX] == NZ * NY and mesh.shape[FSDP] == NX * NC
    return jax.shard_map(
        fast if small else local,
        mesh=mesh,
        in_specs=placed,
        out_specs=(
            P(FSDP, CTX, None),
            P(FSDP, CTX, None),
            P((CTX, FSDP)),
            P((CTX, FSDP)),
            P((CTX, FSDP), None),
            P((CTX, FSDP), None),
            P((CTX, FSDP), None),
            P((CTX, FSDP), None),
            P((CTX, FSDP), None),
            P(CTX, FSDP, None),
            P(CTX, FSDP, None),
        ),
        check_vma=False,
    )
```

```python
import functools
import itertools

import jax
import jax.numpy as jnp
from jax import lax
from jax.experimental import pallas as pl
from jax.experimental.pallas import tpu as pltpu
from jax.sharding import PartitionSpec as P


NY = 2
NZ = 4
NX = 2
NC = 2
DEV = pl.DeviceIdType.MESH
CTX, FSDP = "ctx", "fsdp"
Z, Y, X, C = 0, 1, 2, 3
SIZES = {Z: NZ, Y: NY, X: NX, C: NC}
UP, DOWN = 4, 5


class Plan:
    def __init__(self, ref, order, index, rows=None, view=None):
        self.ref, self.order, self.index, self.rows, self.view = ref, order, index, rows, view
        self.blocks = 1
        for d in index:
            self.blocks *= SIZES[d]


class Place:
    def __init__(self):
        ctx = lax.axis_index(CTX)
        fsdp = lax.axis_index(FSDP)
        self.at = {Z: ctx // NY, Y: ctx % NY, X: fsdp // NC, C: fsdp % NC}
        z = self.at[Z]
        low = z < NZ // 2
        base = jnp.where(low, z, NZ - 1 - z)
        near = [base, 1 - base, jnp.int32(2), jnp.int32(3)]
        self.order = [z] + [jnp.where(low, k, NZ - 1 - k) for k in near[1:]]

    def device(self, dim, value):
        spot = dict(self.at)
        spot[dim] = value
        return (spot[Z] * NY + spot[Y], spot[X] * NC + spot[C])

    def across(self, dim):
        return self.device(dim, 1 - self.at[dim])

    def along(self, step):
        return self.device(Z, self.at[Z] + step)

    def coords(self, z_from, flips):
        spot = {d: (1 - self.at[d] if d in flips else self.at[d]) for d in (Y, X, C)}
        spot[Z] = z_from
        return spot


def flat_index(spot, dims):
    index = 0
    for d in dims:
        index = index * SIZES[d] + spot[d]
    return index


def subsets(dims):
    return [c for n in range(len(dims) + 1) for c in itertools.combinations(dims, n)]


def greet(place, dims):
    barrier = pltpu.get_barrier_semaphore()
    z = place.at[Z]
    count = jnp.int32(0)
    for d in dims:
        if d == Z:
            @pl.when(z > 0)
            def _():
                pl.semaphore_signal(barrier, inc=1, device_id=place.along(-1), device_id_type=DEV)

            @pl.when(z < NZ - 1)
            def _():
                pl.semaphore_signal(barrier, inc=1, device_id=place.along(1), device_id_type=DEV)

            count = count + jnp.where(z > 0, 1, 0) + jnp.where(z < NZ - 1, 1, 0)
        else:
            pl.semaphore_signal(barrier, inc=1, device_id=place.across(d), device_id_type=DEV)
            count = count + 1
    pl.semaphore_wait(barrier, count)


def gather_events(order):
    pairs = [d for d in order if d != Z]
    events = [(k, f) for k in range(NZ) for f in subsets(pairs)]
    return sorted(events, key=lambda e: (e[0] + len(e[1]), len(e[1])))


def gather_sends(order, k, flips):
    z_at = order.index(Z)
    last = max([order.index(d) for d in flips] + ([z_at] if k > 0 else []) + [-1])
    out = []
    for position, d in enumerate(order):
        if position > last:
            out.extend([UP, DOWN] if d == Z else [d])
    if k > 0 and last == z_at:
        out.extend([UP, DOWN])
    return out


def gather_kernel(plans, n_in, *refs):
    ins, outs = refs[:n_in], refs[n_in : 2 * n_in]
    send_sem, recv_sem, own_sem = refs[2 * n_in :]
    place = Place()
    z = place.at[Z]
    greet(place, sorted({d for p in plans for d in p.order}))
    pending = []
    slot = 0
    queue = []
    for n, plan in enumerate(plans):
        for rank, event in enumerate(gather_events(plan.order)):
            queue.append((rank / len(gather_events(plan.order)), n, event))
    queue.sort(key=lambda q: (q[0], q[1]))
    bases = [sum(p.blocks for p in plans[:n]) for n in range(len(plans))]
    for _, n, (k, flips) in queue:
        plan = plans[n]
        src = ins[plan.ref]
        out = outs[plan.ref]
        rows = plan.rows
        z_from = place.order[k]
        spot = place.coords(z_from, flips)
        index = flat_index(spot, plan.index)
        own = k == 0 and not flips
        if plan.view is not None:
            target = plan.view(out, spot, rows)
            source = src.at[:, pl.ds(rows[0], rows[1])] if own else target
        else:
            target = out.at[index] if rows is None else out.at[index, pl.ds(rows[0], rows[1])]
            source = (src if rows is None else src.at[pl.ds(rows[0], rows[1])]) if own else target
        sem = recv_sem.at[bases[n] + index]
        if not own:
            pltpu.make_async_remote_copy(
                src_ref=target, dst_ref=target, send_sem=own_sem.at[0], recv_sem=sem,
                device_id=place.across(C), device_id_type=DEV,
            ).wait_recv()
        for way in gather_sends(plan.order, k, flips):
            if way in (UP, DOWN):
                step = 1 if way == UP else -1
                go = z < NZ - 1 if way == UP else z > 0
                if k > 0:
                    go = jnp.logical_and(go, z_from < z if way == UP else z_from > z)
                dest = place.device(Z, jnp.clip(z + step, 0, NZ - 1))
            else:
                go, dest = None, place.across(way)
            copy = pltpu.make_async_remote_copy(
                src_ref=source, dst_ref=target, send_sem=send_sem.at[slot], recv_sem=sem,
                device_id=dest, device_id_type=DEV,
            )
            slot += 1
            if go is None:
                copy.start()
            else:
                pl.when(go)(copy.start)
            pending.append((go, copy.wait_send))
        if own:
            copy = pltpu.make_async_copy(source, target, own_sem.at[1 + n])
            copy.start()
            pending.append((None, copy.wait))
    for go, wait in pending:
        if go is None:
            wait()
        else:
            pl.when(go)(wait)


def gather(arrays, plans, collective_id, shapes=None):
    n = len(arrays)
    sends = sum(len(gather_sends(p.order, k, f)) for p in plans for k, f in gather_events(p.order))
    blocks = {p.ref: p.blocks for p in plans}
    return pl.pallas_call(
        functools.partial(gather_kernel, plans, n),
        out_shape=[
            jax.ShapeDtypeStruct((shapes or {}).get(i, (blocks[i],) + a.shape), a.dtype)
            for i, a in enumerate(arrays)
        ],
        in_specs=[pl.BlockSpec(memory_space=pltpu.VMEM)] * n,
        out_specs=[pl.BlockSpec(memory_space=pl.ANY)] * n,
        scratch_shapes=[
            pltpu.SemaphoreType.DMA((sends,)),
            pltpu.SemaphoreType.DMA((sum(p.blocks for p in plans),)),
            pltpu.SemaphoreType.DMA((1 + len(plans),)),
        ],
        compiler_params=pltpu.CompilerParams(collective_id=collective_id, has_side_effects=True),
    )(*arrays)


def add_into(acc, other):
    acc[...] = (acc[...].astype(jnp.float32) + other[...].astype(jnp.float32)).astype(acc.dtype)


def reduce_kernel(plans, n_in, *refs):
    ins, outs = refs[:n_in], refs[n_in : 2 * n_in]
    rest = list(refs[2 * n_in :])
    send_sem, recv_sem, own_sem = rest[:3]
    buffers = rest[3:]
    place = Place()
    z = place.at[Z]
    greet(place, sorted({d for p in plans for d in p.order} | {Z}))
    pending = []
    slots = [0, 0]

    def push(source, target, sem, dest):
        copy = pltpu.make_async_remote_copy(
            src_ref=source, dst_ref=target, send_sem=send_sem.at[slots[0]], recv_sem=sem,
            device_id=dest, device_id_type=DEV,
        )
        slots[0] += 1
        copy.start()
        pending.append(copy)

    def arrived(target, sem):
        pltpu.make_async_remote_copy(
            src_ref=target, dst_ref=target, send_sem=own_sem.at[0], recv_sem=sem,
            device_id=place.across(C), device_id_type=DEV,
        ).wait_recv()

    work = []
    far = list(reversed(range(NZ)))
    own_slot = 1
    state = []
    base = 0
    for n, plan in enumerate(plans):
        dims = plan.order
        acc = buffers[0]
        levels = buffers[1 : 1 + len(dims)]
        chain = buffers[1 + len(dims)]
        buffers = buffers[2 + len(dims) :]
        kept = [subsets(dims[p + 1 :]) for p in range(len(dims))]
        counts = [NZ * len(f) for f in kept]
        level_base = [base + sum(counts[:p]) for p in range(len(dims))]
        chain_base = base + sum(counts)
        base = chain_base + 2 * NZ
        state.append((acc, levels, chain, kept, level_base, chain_base))
        own_copies = {}
        src = ins[plan.ref]
        for k in far:
            for f in kept[0]:
                gone = flat_index(place.coords(place.order[k], (dims[0],) + f), plan.index)
                spot = place.order[k] * len(kept[0]) + kept[0].index(f)
                work.append((0, n, k, f, gone, spot))
                mine = flat_index(place.coords(place.order[k], f), plan.index)
                copy = pltpu.make_async_copy(src.at[mine], acc.at[spot], own_sem.at[own_slot])
                own_slot += 1
                own_copies[(k, f)] = copy
        state[-1] += (own_copies,)
    for _, n, k, f, gone, spot in sorted(work, key=lambda w: (-w[2],)):
        plan = plans[n]
        acc, levels, chain, kept, level_base, chain_base, own_copies = state[n]
        push(ins[plan.ref].at[gone], levels[0].at[spot], recv_sem.at[level_base[0] + spot], place.across(plan.order[0]))
        own_copies[(k, f)].start()

    def level_step(n, p, k):
        plan = plans[n]
        dims = plan.order
        acc, levels, _, kept, level_base, _, own_copies = state[n]
        for f in sorted(kept[p], key=lambda f: -len(f)):
            spot = place.order[k] * len(kept[p]) + kept[p].index(f)
            at = place.order[k] * len(kept[0]) + kept[0].index(f)
            if p == 0:
                own_copies[(k, f)].wait()
            arrived(levels[p].at[spot], recv_sem.at[level_base[p] + spot])
            add_into(acc.at[at], levels[p].at[spot])
            later = p + 1
            if later < len(dims) and dims[later] in f:
                left = tuple(d for d in f if d != dims[later])
                there = place.order[k] * len(kept[later]) + kept[later].index(left)
                push(
                    acc.at[at], levels[later].at[there],
                    recv_sem.at[level_base[later] + there], place.across(dims[later]),
                )

    def chain_step(n, k):
        acc, _, chain, kept, _, chain_base, _ = state[n]
        dest = place.order[k]
        up = dest > z
        lane = jnp.where(up, 0, 1)
        at = dest * len(kept[0])
        spot = lane * NZ + dest

        @pl.when(jnp.where(up, z > 0, z < NZ - 1))
        def _():
            arrived(chain.at[spot], recv_sem.at[chain_base + spot])
            add_into(acc.at[at], chain.at[spot])

        push(acc.at[at], chain.at[spot], recv_sem.at[chain_base + spot], place.along(jnp.where(up, 1, -1)))

    most = max(len(p.order) for p in plans)
    for step in range(NZ + most):
        for n, plan in enumerate(plans):
            for p in range(len(plan.order)):
                if 0 <= step - p < NZ:
                    level_step(n, p, far[step - p])
            p = len(plan.order)
            if 0 <= step - p < NZ - 1:
                chain_step(n, far[step - p])
    for n, plan in enumerate(plans):
        acc, levels, chain, kept, level_base, chain_base, own_copies = state[n]
        at = z * len(kept[0])

        @pl.when(z > 0)
        def _():
            spot = z
            arrived(chain.at[spot], recv_sem.at[chain_base + spot])
            add_into(acc.at[at], chain.at[spot])

        @pl.when(z < NZ - 1)
        def _():
            spot = NZ + z
            arrived(chain.at[spot], recv_sem.at[chain_base + spot])
            add_into(acc.at[at], chain.at[spot])

        outs[plan.ref][...] = acc[at].astype(outs[plan.ref].dtype)
    for copy in pending:
        copy.wait_send()


def reduce_scatter(arrays, plans, out_dtypes, collective_id):
    n = len(arrays)
    scratch = []
    sends = recvs = owns = 0
    for p in plans:
        a = arrays[p.ref]
        block = a.shape[1:]
        kept = [len(subsets(p.order[q + 1 :])) for q in range(len(p.order))]
        scratch.append(pltpu.VMEM((NZ * kept[0],) + block, a.dtype))
        for q in kept:
            scratch.append(pltpu.VMEM((NZ * q,) + block, a.dtype))
        scratch.append(pltpu.VMEM((2 * NZ,) + block, a.dtype))
        sends += NZ * sum(kept) + NZ - 1
        recvs += NZ * sum(kept) + 2 * NZ
        owns += NZ * kept[0]
    return pl.pallas_call(
        functools.partial(reduce_kernel, plans, n),
        out_shape=[jax.ShapeDtypeStruct(a.shape[1:], d) for a, d in zip(arrays, out_dtypes)],
        in_specs=[pl.BlockSpec(memory_space=pl.ANY)] * n,
        out_specs=[pl.BlockSpec(memory_space=pltpu.VMEM)] * n,
        scratch_shapes=[
            pltpu.SemaphoreType.DMA((sends,)),
            pltpu.SemaphoreType.DMA((recvs,)),
            pltpu.SemaphoreType.DMA((1 + owns,)),
        ]
        + scratch,
        compiler_params=pltpu.CompilerParams(
            collective_id=collective_id, has_side_effects=True, vmem_limit_bytes=60 * 1024 * 1024
        ),
    )(*arrays)


class Gather:
    def __init__(self, place, plan, src, out, send_sem, recv_sem, spare_sem, slot, base):
        self.place, self.plan, self.src, self.out = place, plan, src, out
        self.send_sem, self.recv_sem, self.spare_sem = send_sem, recv_sem, spare_sem
        self.slot, self.base = slot, base
        self.pending = []

    @staticmethod
    def sends(plan):
        return sum(len(gather_sends(plan.order, k, f)) for k, f in gather_events(plan.order))

    def step(self, k, flips):
        place, plan = self.place, self.plan
        z = place.at[Z]
        z_from = place.order[k]
        index = flat_index(place.coords(z_from, flips), plan.index)
        rows = plan.rows
        target = self.out.at[index] if rows is None else self.out.at[index, pl.ds(rows[0], rows[1])]
        sem = self.recv_sem.at[self.base + index]
        own = k == 0 and not flips
        source = target
        if own:
            source = self.src if rows is None else self.src.at[pl.ds(rows[0], rows[1])]
        else:
            pltpu.make_async_remote_copy(
                src_ref=target, dst_ref=target, send_sem=self.spare_sem, recv_sem=sem,
                device_id=place.across(C), device_id_type=DEV,
            ).wait_recv()
        for way in gather_sends(plan.order, k, flips):
            if way in (UP, DOWN):
                step = 1 if way == UP else -1
                go = z < NZ - 1 if way == UP else z > 0
                if k > 0:
                    go = jnp.logical_and(go, z_from < z if way == UP else z_from > z)
                dest = place.device(Z, jnp.clip(z + step, 0, NZ - 1))
            else:
                go, dest = None, place.across(way)
            copy = pltpu.make_async_remote_copy(
                src_ref=source, dst_ref=target, send_sem=self.send_sem.at[self.slot], recv_sem=sem,
                device_id=dest, device_id_type=DEV,
            )
            self.slot += 1
            if go is None:
                copy.start()
            else:
                pl.when(go)(copy.start)
            self.pending.append((go, copy.wait_send))

    def finish(self):
        for go, wait in self.pending:
            if go is None:
                wait()
            else:
                pl.when(go)(wait)


class Reduce:
    def __init__(self, place, plan, held, levels, chain, send_sem, recv_sem, spare_sem):
        self.place, self.plan, self.held, self.levels, self.chain = place, plan, held, levels, chain
        self.send_sem, self.recv_sem, self.spare_sem = send_sem, recv_sem, spare_sem
        dims = plan.order
        self.kept = [subsets(dims[p + 1 :]) for p in range(len(dims))]
        self.base = [NZ * sum(len(f) for f in self.kept[:p]) for p in range(len(dims) + 1)]
        self.slot = 0
        self.pending = []

    @staticmethod
    def counts(plan):
        kept = [NZ * len(subsets(plan.order[p + 1 :])) for p in range(len(plan.order))]
        return kept, sum(kept) + NZ - 1, sum(kept) + NZ + 1

    def push(self, source, target, sem, dest):
        copy = pltpu.make_async_remote_copy(
            src_ref=source, dst_ref=target, send_sem=self.send_sem.at[self.slot], recv_sem=sem,
            device_id=dest, device_id_type=DEV,
        )
        self.slot += 1
        copy.start()
        self.pending.append(copy)

    def arrived(self, target, sem):
        pltpu.make_async_remote_copy(
            src_ref=target, dst_ref=target, send_sem=self.spare_sem, recv_sem=sem,
            device_id=self.place.across(C), device_id_type=DEV,
        ).wait_recv()

    def block(self, k, flips):
        return flat_index(self.place.coords(self.place.order[k], flips), self.plan.index)

    def first(self, k):
        dim = self.plan.order[0]
        for n, f in enumerate(self.kept[0]):
            spot = self.place.order[k] * len(self.kept[0]) + n
            self.push(
                self.held.at[self.block(k, (dim,) + f)], self.levels[0].at[spot],
                self.recv_sem.at[spot], self.place.across(dim),
            )

    def level(self, p, k):
        dims = self.plan.order
        z_to = self.place.order[k]
        for f in sorted(self.kept[p], key=lambda f: -len(f)):
            spot = z_to * len(self.kept[p]) + self.kept[p].index(f)
            mine = self.held.at[self.block(k, f)]
            self.arrived(self.levels[p].at[spot], self.recv_sem.at[self.base[p] + spot])
            add_into(mine, self.levels[p].at[spot])
            later = p + 1
            if later < len(dims) and dims[later] in f:
                left = tuple(d for d in f if d != dims[later])
                there = z_to * len(self.kept[later]) + self.kept[later].index(left)
                self.push(
                    mine, self.levels[later].at[there],
                    self.recv_sem.at[self.base[later] + there], self.place.across(dims[later]),
                )

    def along(self, k):
        z = self.place.at[Z]
        dest = self.place.order[k]
        up = dest > z
        spot = dest + jnp.where(up, 1, 0)
        mine = self.held.at[self.block(k, ())]
        sem = self.recv_sem.at[self.base[-1] + spot]

        @pl.when(jnp.where(up, z > 0, z < NZ - 1))
        def _():
            self.arrived(self.chain.at[spot], sem)
            add_into(mine, self.chain.at[spot])

        self.push(mine, self.chain.at[spot], sem, self.place.along(jnp.where(up, 1, -1)))

    def last(self, out, base=None):
        z = self.place.at[Z]
        mine = self.held.at[self.block(0, ())]
        for go, spot in ((z > 0, z + 1), (z < NZ - 1, z)):

            @pl.when(go)
            def _():
                self.arrived(self.chain.at[spot], self.recv_sem.at[self.base[-1] + spot])
                add_into(mine, self.chain.at[spot])

        total = mine[...].astype(jnp.float32)
        if base is not None:
            total = base[...] + total
        out[...] = total.astype(out.dtype)

    def at_time(self, t):
        depth = len(self.plan.order)
        far = list(reversed(range(NZ)))
        out = [functools.partial(self.level, p, far[t - p]) for p in range(depth) if 0 <= t - p < NZ]
        if 0 <= t - depth < NZ - 1:
            out.append(functools.partial(self.along, far[t - depth]))
        return out

    def steps(self):
        return [step for t in range(NZ + len(self.plan.order)) for step in self.at_time(t)]

    def finish(self):
        for copy in self.pending:
            copy.wait_send()


def tile_up(n, m):
    return (n + m - 1) // m * m


def columns_of(width, chunk=512):
    return [(i, min(chunk, width - i)) for i in range(0, width, chunk)]


def moe_kernel(plans, back, width, hidden, cap, *refs):
    payload, cots, w_own, w_core, w_x, w_both = refs[:6]
    gin_out, part_out = refs[6:8]
    grads = refs[8:12]
    (
        seen, cot_seen, weights, taken, cot_taken, rows_buf, scaled, grad_act, pick, stage,
        lvl_b0, lvl_b1, chain_b,
        send_sem, recv_sem, spare_sem, send_b, recv_b, load_sem, store_sem, part_sem,
    ) = refs[12:]
    bf, f32 = jnp.bfloat16, jnp.float32
    place = Place()
    count = payload.shape[0]
    pair = 2 * cap
    wide = width + 128
    quarter = width // (NX * NC)
    half = NZ * pair
    lanes = pick.shape[2]
    held = weights.shape[0]
    fsdp = place.at[X] * NC + place.at[C]
    first = (((place.at[Z] * NY + place.at[Y]) * NC) + place.at[C]) * held

    loads = []
    for j, ref in enumerate((w_own, w_core, w_x, w_both)):
        rows = pl.ds(pl.multiple_of((fsdp ^ j) * quarter, quarter), quarter)
        for e in range(held):
            loads.append(pltpu.make_async_copy(ref.at[e], weights.at[e, rows], load_sem.at[len(loads)]))
    base_of = lambda h, k: (jnp.where(h == 0, place.at[C], 1 - place.at[C]) * NZ + place.order[k]) * NY
    cot_loads = {}
    for k in range(NZ):
        for h in range(2):
            at = pl.ds(base_of(h, k), NY)
            cot_loads[(h, k)] = pltpu.make_async_copy(cots.at[at], cot_seen.at[at], load_sem.at[len(loads) + len(cot_loads)])

    greet(place, (Z, Y, C))
    ways = []
    send_at = 0
    for n, plan in enumerate(plans):
        ways.append(Gather(place, plan, payload, seen, send_sem, recv_sem, spare_sem, send_at, n * plan.blocks))
        send_at += Gather.sends(plan)
    for way in ways:
        way.step(0, ())
    for key in cot_loads:
        cot_loads[key].start()
    for copy in loads:
        copy.start()
    seen[flat_index(place.at, plans[0].index)] = payload[...]

    row_id = lax.broadcasted_iota(jnp.int32, (NY * count, NY * count), 0)
    col_id = lax.broadcasted_iota(jnp.int32, (NY * count, NY * count), 1)
    earlier = jnp.logical_and(col_id < row_id, col_id // count == row_id // count).astype(bf)
    lane_id = lax.broadcasted_iota(jnp.int32, (1, 128), 1)
    here = [(lane_id == first + e).astype(f32) for e in range(held)]
    pick_lane = lax.broadcasted_iota(jnp.int32, (NY * count, lanes), 1).astype(f32)
    y_shift = (lax.broadcasted_iota(jnp.int32, (NY * count, 1), 0) // count * cap).astype(f32)

    def dispatch(source, target, h, k, cols):
        at = pl.ds(base_of(h, k), NY)
        r = (h * NZ + k) * pair
        for c0, cn in cols:
            block = source[at, :, c0 : c0 + cn].reshape(NY * count, cn)
            got = lax.dot_general(
                pick[h * NZ + k], block, (((0,), (0,)), ((), ())), preferred_element_type=f32
            ).astype(bf)
            for e in range(held):
                target[e, r : r + pair, c0 : c0 + cn] = got[e * pair : (e + 1) * pair]

    def cot_chunk(h, k):
        cot_loads[(h, k)].wait()
        at = pl.ds(base_of(h, k), NY)
        chosen = cot_seen[at, :, width:wide].reshape(NY * count, 128)
        before = jnp.dot(earlier, chosen, preferred_element_type=f32)
        picked = None
        for e in range(held):
            is_here = jnp.sum(chosen.astype(f32) * here[e], axis=1, keepdims=True)
            slot = jnp.sum(before * here[e], axis=1, keepdims=True) + y_shift + e * pair
            target = jnp.where(is_here > 0.5, slot, -1.0)
            hit = pick_lane == target
            picked = hit if picked is None else jnp.logical_or(picked, hit)
        pick[h * NZ + k] = picked.astype(f32).astype(bf)
        dispatch(cot_seen, cot_taken, h, k, columns_of(width))

    def hidden_chunk(h, e, n, tile):
        rows = pl.ds(h * half, half)
        tokens_in = taken[e, rows, :width]
        gate = jnp.sum(taken[e, rows, width:wide].astype(f32) * here[e], axis=1, keepdims=True)
        col = n * tile
        g = jnp.dot(tokens_in, weights[e, :, col : col + tile], preferred_element_type=f32)
        u = jnp.dot(tokens_in, weights[e, :, hidden + col : hidden + col + tile], preferred_element_type=f32)
        raw = jnp.dot(
            cot_taken[e, rows, :], weights[e, :, 2 * hidden + col : 2 * hidden + col + tile], preferred_element_type=f32
        )
        s = jax.nn.sigmoid(g)
        gs = g * s
        inner = gs * u
        scaled[e, rows, col : col + tile] = (inner * gate).astype(bf)
        grad_inner = raw * gate
        grad_act[e, rows, col : col + tile] = (grad_inner * u * s * (1.0 + g * (1.0 - s))).astype(bf)
        grad_act[e, rows, hidden + col : hidden + col + tile] = (grad_inner * gs).astype(bf)
        return jnp.sum(raw * inner, axis=1, keepdims=True)

    def hidden_part(h, e):
        tile = min(256, hidden)
        gate_grad = sum(hidden_chunk(h, e, n, tile) for n in range(hidden // tile))
        high = gate_grad.astype(bf).astype(f32)
        there = pl.ds(h * half, half)
        apart = (lane_id == EXPERT_COUNT + first + e).astype(f32)
        rows_buf[e, there, width:wide] = (high * here[e] + (gate_grad - high) * apart).astype(bf)

    def project(h, e, left, weight_cols):
        rows = pl.ds(h * half, half)
        lo, n = weight_cols
        for c0, cn in columns_of(width):
            rows_buf[e, rows, c0 : c0 + cn] = lax.dot_general(
                left[e, rows, :], weights[e, c0 : c0 + cn, lo : lo + n], (((1,), (1,)), ((), ())), preferred_element_type=f32
            ).astype(bf)

    def combine(target, h, k, cols):
        at = pl.ds(base_of(h, k), NY)
        r = (h * NZ + k) * pair
        for c0, cn in cols:
            parts = [rows_buf[e, r : r + pair, c0 : c0 + cn] for e in range(held)]
            if lanes > held * pair:
                parts.append(jnp.zeros((lanes - held * pair, cn), bf))
            got = jnp.dot(pick[h * NZ + k], jnp.concatenate(parts, axis=0), preferred_element_type=f32)
            target[at, :, c0 : c0 + cn] = got.astype(bf).reshape(NY, count, cn)

    stores = []

    def weight_grad(e, j):
        rows = pl.ds(pl.multiple_of((fsdp ^ j) * quarter, 128), quarter)
        slot = len(stores) % 2
        if len(stores) >= 2:
            stores[-2].wait()
        for c0, cn in columns_of(2 * hidden):
            stage[slot, :, c0 : c0 + cn] = lax.dot_general(
                taken[e, :, rows], grad_act[e, :, c0 : c0 + cn], (((0,), (0,)), ((), ())), preferred_element_type=f32
            ).astype(bf)
        stage[slot, :, 2 * hidden :] = lax.dot_general(
            cot_taken[e, :, rows], scaled[e], (((0,), (0,)), ((), ())), preferred_element_type=f32
        ).astype(bf)
        copy = pltpu.make_async_copy(stage.at[slot], grads[j].at[e], store_sem.at[len(stores)])
        copy.start()
        stores.append(copy)

    work = [functools.partial(cot_chunk, h, k) for h in range(NC) for k in range(NZ)]
    all_cols = columns_of(width) + [(width, 128)]
    ready = {(h, k): 0 for h in range(NC) for k in range(NZ)}
    ready[(0, 0)] = 1
    for k, flips in gather_events(plans[0].order)[1:]:
        for way in ways:
            way.step(k, flips)
        key = (1 if C in flips else 0, k)
        ready[key] += 1
        if ready[key] == NY:
            work.append(functools.partial(dispatch, seen, taken, *key, all_cols))
        for _ in range(min(len(work), 1 if k < NZ - 1 else 2)):
            work.pop(0)()
    for chunk in work:
        chunk()
    for copy in loads:
        copy.wait()
    for h in range(NC):
        for e in range(held):
            hidden_part(h, e)
    for way in ways:
        way.finish()

    far = list(reversed(range(NZ)))
    spare = spare_sem
    in_way = Reduce(place, back, cot_seen, (lvl_b0, lvl_b1), chain_b, send_b, recv_b, spare)
    in_steps = in_way.steps()
    for h in reversed(range(NC)):
        for e in range(held):
            project(h, e, grad_act, (0, 2 * hidden))
        for k in far:
            combine(cot_seen, h, k, all_cols)
            if h == 1:
                in_way.first(k)
    part_copies = []
    work = []

    def out_part(h, k):
        combine(seen, h, k, columns_of(width))
        at = pl.ds(base_of(h, k), NY)
        copy = pltpu.make_async_copy(seen.at[at, :, pl.ds(0, width)], part_out.at[at], part_sem.at[len(part_copies)])
        copy.start()
        part_copies.append(copy)

    for h in range(NC):
        for e in range(held):
            work.append(functools.partial(project, h, e, scaled, (2 * hidden, hidden)))
        for k in range(NZ):
            work.append(functools.partial(out_part, h, k))
    work += [functools.partial(weight_grad, e, j) for j in reversed(range(NX * NC)) for e in range(held)]
    while in_steps or work:
        if in_steps:
            in_steps.pop(0)()
        for _ in range(2):
            if work:
                work.pop(0)()
    in_way.last(gin_out)
    for copy in stores[-2:] + part_copies:
        copy.wait()
    in_way.finish()


def moe(payload, cots, parts, cap, collective_id):
    count, wide = payload.shape
    width = wide - 128
    held, quarter, columns = parts[0].shape
    hidden = columns // 3
    cut = count * 3 // 4
    plans = [
        Plan(0, (Z, Y, C), (C, Z, Y), rows=(0, cut)),
        Plan(0, (Y, Z, C), (C, Z, Y), rows=(cut, count - cut)),
    ]
    back = Plan(0, (C, Y), (C, Z, Y))
    levels, sends, recvs = Reduce.counts(back)
    blocks = NC * NZ * NY
    pair = NY * cap
    rows = blocks // NY * pair
    lanes = tile_up(held * pair, 128)
    bf, f32 = jnp.bfloat16, jnp.float32
    whole = pl.BlockSpec(memory_space=pltpu.VMEM)
    apart = pl.BlockSpec(memory_space=pl.ANY)
    dma = pltpu.SemaphoreType.DMA
    return pl.pallas_call(
        functools.partial(moe_kernel, plans, back, width, hidden, cap),
        out_shape=[
            jax.ShapeDtypeStruct((count, wide), f32),
            jax.ShapeDtypeStruct((blocks, count, width), bf),
        ]
        + [jax.ShapeDtypeStruct((held, quarter, columns), bf)] * (NX * NC),
        in_specs=[whole] + [apart] * 5,
        out_specs=[whole] + [apart] * (1 + NX * NC),
        scratch_shapes=[
            pltpu.VMEM((blocks, count, wide), bf),
            pltpu.VMEM((blocks, count, wide), bf),
            pltpu.VMEM((held, NX * NC * quarter, columns), bf),
            pltpu.VMEM((held, rows, wide), bf),
            pltpu.VMEM((held, rows, width), bf),
            pltpu.VMEM((held, rows, wide), bf),
            pltpu.VMEM((held, rows, hidden), bf),
            pltpu.VMEM((held, rows, 2 * hidden), bf),
            pltpu.VMEM((blocks // NY, NY * count, lanes), bf),
            pltpu.VMEM((2, quarter, columns), bf),
        ]
        + [pltpu.VMEM((n, count, wide), bf) for n in levels + [NZ + 1]]
        + [
            dma((sum(Gather.sends(p) for p in plans),)),
            dma((sum(p.blocks for p in plans),)),
            dma(()),
            dma((sends,)),
            dma((recvs,)),
            dma((held * NX * NC + blocks // NY,)),
            dma((held * NX * NC,)),
            dma((blocks // NY,)),
        ],
        compiler_params=pltpu.CompilerParams(
            collective_id=collective_id, has_side_effects=True, vmem_limit_bytes=67043328
        ),
        name="experts",
    )(payload, cots, *parts)


def weight_view(out, spot, rows):
    return out.at[spot[Z] * NY + spot[Y], :, spot[C], pl.ds(rows[0], rows[1])]


def weights_kernel(plans, *refs):
    left_one, right_one, left_two, right_two, left_small, right_small, part, mixed = refs[:8]
    outs = refs[8:11]
    held_one, held_two, held_out = refs[11:14]
    buffers = refs[14:25]
    send_one, recv_one, send_two, recv_two, send_out, recv_out, spare, load_sem = refs[25:]
    place = Place()
    loads = []
    far = list(reversed(range(NZ)))
    for k in far:
        for h in (1 - place.at[C], place.at[C]):
            at = pl.ds((h * NZ + place.order[k]) * NY, NY)
            loads.append(pltpu.make_async_copy(part.at[at], held_out.at[at], load_sem.at[len(loads)]))
    for copy in loads:
        copy.start()
    greet(place, (Z, Y, X, C))
    ways = [
        Reduce(place, plans[0], held_one, buffers[0:3], buffers[3], send_one, recv_one, spare),
        Reduce(place, plans[1], held_two, buffers[4:7], buffers[7], send_two, recv_two, spare),
        Reduce(place, plans[2], held_out, buffers[8:10], buffers[10], send_out, recv_out, spare),
    ]
    group = NY * NX * NC
    rows = group * held_one.shape[1]

    def products(left, right, held, k, shift):
        at = pl.ds(pl.multiple_of(place.order[k] * rows, 128), rows)
        block = left[:, at]
        for c0, cn in columns_of(right.shape[1]):
            got = lax.dot_general(
                block, right[:, c0 : c0 + cn], (((0,), (0,)), ((), ())), preferred_element_type=jnp.float32
            )
            held[pl.ds(place.order[k] * group, group), :, shift + c0 : shift + c0 + cn] = got.astype(
                held.dtype
            ).reshape(group, rows // group, cn)

    for t in range(NZ):
        k = far[t]
        products(left_one, right_one, held_one, k, 0)
        ways[0].first(k)
        products(left_two, right_two, held_two, k, 0)
        products(left_small, right_small, held_two, k, right_two.shape[1])
        ways[1].first(k)
        for copy in loads[2 * t : 2 * t + 2]:
            copy.wait()
        ways[2].first(k)
        if t > 0:
            for way in ways:
                for step in way.at_time(t - 1):
                    step()
    for t in range(NZ - 1, NZ + 3):
        for way in ways:
            for step in way.at_time(t):
                step()
    for way, out in zip(ways, outs):
        way.last(out, mixed if way is ways[2] else None)
    for way in ways:
        way.finish()


def return_weights(lefts, rights, part, mixed, collective_id):
    width = lefts[0].shape[1]
    rows = width // (NZ * NY * NX * NC)
    widths = [rights[0].shape[1], rights[1].shape[1] + rights[2].shape[1]]
    plans = [
        Plan(0, (C, X, Y), (Z, Y, X, C)),
        Plan(1, (C, X, Y), (Z, Y, X, C)),
        Plan(2, (C, Y), (C, Z, Y)),
    ]
    bf = jnp.bfloat16
    levels, sends, recvs = Reduce.counts(plans[0])
    out_levels, out_sends, out_recvs = Reduce.counts(plans[2])
    dma = pltpu.SemaphoreType.DMA
    operands = [a for pair in zip(lefts, rights) for a in pair] + [part, mixed]
    vmem = pl.BlockSpec(memory_space=pltpu.VMEM)
    return pl.pallas_call(
        functools.partial(weights_kernel, plans),
        out_shape=[jax.ShapeDtypeStruct((rows, w), jnp.float32) for w in widths]
        + [jax.ShapeDtypeStruct(mixed.shape, bf)],
        in_specs=[vmem] * 6 + [pl.BlockSpec(memory_space=pl.ANY), vmem],
        out_specs=[vmem] * 3,
        scratch_shapes=[pltpu.VMEM((plans[0].blocks, rows, w), bf) for w in widths]
        + [pltpu.VMEM(part.shape, bf)]
        + [pltpu.VMEM((n, rows, w), bf) for w in widths for n in levels + [NZ + 1]]
        + [pltpu.VMEM((n,) + part.shape[1:], bf) for n in out_levels + [NZ + 1]]
        + [dma((n,)) for n in (sends, recvs, sends, recvs, out_sends, out_recvs)]
        + [dma(()), dma((NC * NZ,))],
        compiler_params=pltpu.CompilerParams(
            collective_id=collective_id, has_side_effects=True, vmem_limit_bytes=60 * 1024 * 1024
        ),
        name="return_weights",
    )(*operands)


def add_kernel(core_ref, own, core_part, x_part, both_part, in_out, out_out):
    core = core_ref[0]
    split = in_out.shape[3]
    for at, left, right in ((core, own, x_part), (1 - core, core_part, both_part)):
        total = left[0].astype(jnp.float32) + right[0].astype(jnp.float32)
        in_out[at, 0] = total[:, :split]
        out_out[at, 0] = total[:, split:]


def add_experts(pieces, core, split):
    held, quarter, columns = pieces[0].shape
    step = quarter // 2
    spec = pl.BlockSpec((1, step, columns), lambda e, r, c: (e, r, 0))
    outs = (split, columns - split)
    return pl.pallas_call(
        add_kernel,
        grid_spec=pltpu.PrefetchScalarGridSpec(
            num_scalar_prefetch=1,
            grid=(held, 2),
            in_specs=[spec] * 4,
            out_specs=[pl.BlockSpec((NC, 1, step, w), lambda e, r, c: (0, e, r, 0)) for w in outs],
        ),
        out_shape=[jax.ShapeDtypeStruct((NC, held, quarter, w), jnp.float32) for w in outs],
        name="add_experts",
    )(core[None], *pieces)


MODEL_WIDTH = 1536
QUERY_HEADS = 24
KEY_VALUE_HEADS = 8
HEAD_SIZE = 64
EXPERT_HIDDEN = 512
EXPERT_COUNT = 32
TOP = 8
CAP = 40


norm_eps = 1e-06
attn_scale = 0.015625
rope_base = 10000.0
masked_logits = -1e30


def rope_tables(positions):
    half = HEAD_SIZE // 2
    frequency = jnp.power(
        jnp.float32(rope_base), -2.0 * jnp.arange(half, dtype=jnp.float32) / HEAD_SIZE
    )
    angle = positions.astype(jnp.float32)[:, None] * frequency[None, :]
    return (jnp.cos(angle)[:, None, :], jnp.sin(angle)[:, None, :])


def rotate_pairs(value_tensor, cosine_table, sine_table):
    half = value_tensor.shape[-1] // 2
    first = value_tensor[..., :half]
    second = value_tensor[..., half:]
    return jnp.concatenate(
        [first * cosine_table - second * sine_table, second * cosine_table + first * sine_table],
        axis=-1,
    )


def rms_forward(wide, gain):
    inverse = lax.rsqrt(jnp.mean(wide * wide, axis=-1, keepdims=True) + norm_eps)
    unit = wide * inverse
    return (unit, inverse, (unit * gain.astype(jnp.float32)).astype(jnp.bfloat16))


def rms_backward(grad, unit, inverse, gain):
    scaled = grad * gain.astype(jnp.float32)
    back = inverse * (scaled - unit * jnp.mean(scaled * unit, axis=-1, keepdims=True))
    return (back, jnp.sum(grad * unit, axis=0))


def piece_scores(query_rows, key_section, positions):
    token_count = key_section.shape[0]
    key_tensor = key_section.reshape(token_count, KEY_VALUE_HEADS, HEAD_SIZE)
    scores = (
        jnp.einsum("tkgd,nkd->kgtn", query_rows, key_tensor, preferred_element_type=jnp.float32)
        * attn_scale
    )
    visible = jnp.arange(token_count, dtype=jnp.int32)[None, :] <= positions[:, None]
    return (jnp.where(visible, scores, masked_logits), visible, key_tensor)


def local(
    hidden,
    routes,
    attn_norm,
    ffn_norm,
    w_q,
    key_weight,
    value_weight,
    w_o,
    router,
    expert_in,
    expert_out,
    cotangent,
):
    token_rows = hidden.shape[1]
    query_group = QUERY_HEADS // KEY_VALUE_HEADS
    ctx_size = lax.axis_size(CTX)
    sequence_length = token_rows * ctx_size
    positions = lax.axis_index(CTX) * token_rows + jnp.arange(token_rows, dtype=jnp.int32)
    cosine_table, sine_table = rope_tables(positions)
    contract_rows = (((0,), (0,)), ((), ()))
    contract_cols = (((1,), (1,)), ((), ()))
    layer = (
        lax.all_gather(attn_norm, (CTX, FSDP), axis=0, tiled=True),
        lax.all_gather(ffn_norm, (CTX, FSDP), axis=0, tiled=True),
        lax.all_gather(w_q, (CTX, FSDP), axis=0, tiled=True),
        lax.all_gather(key_weight, (CTX, FSDP), axis=0, tiled=True),
        lax.all_gather(value_weight, (CTX, FSDP), axis=0, tiled=True),
        lax.all_gather(w_o, (CTX, FSDP), axis=0, tiled=True),
        lax.all_gather(router, (CTX, FSDP), axis=0, tiled=True),
    )
    attn_gain, ffn_gain, query_w, key_weight_matrix, value_w, output_w, router_w = layer
    experts = (
        lax.all_gather(expert_in, FSDP, axis=1, tiled=True),
        lax.all_gather(expert_out, FSDP, axis=1, tiled=True),
    )
    weight_in, weight_out = experts
    wide = hidden[0].astype(jnp.float32)
    attn_unit, inverse_one, attention_input = rms_forward(wide, attn_gain)
    query_linear = jnp.dot(attention_input, query_w, preferred_element_type=jnp.float32).reshape(
        token_rows, QUERY_HEADS, HEAD_SIZE
    )
    query_rows = (
        rotate_pairs(query_linear, cosine_table, sine_table)
        .astype(jnp.bfloat16)
        .reshape(token_rows, KEY_VALUE_HEADS, query_group, HEAD_SIZE)
    )
    key_linear = jnp.dot(
        attention_input, key_weight_matrix, preferred_element_type=jnp.float32
    ).reshape(token_rows, KEY_VALUE_HEADS, HEAD_SIZE)
    key_matrix_rows = (
        rotate_pairs(key_linear, cosine_table, sine_table)
        .astype(jnp.bfloat16)
        .reshape(token_rows, KEY_VALUE_HEADS * HEAD_SIZE)
    )
    value_rows = jnp.dot(attention_input, value_w, preferred_element_type=jnp.float32).astype(
        jnp.bfloat16
    )
    init_state = (
        jnp.full((KEY_VALUE_HEADS, query_group, token_rows), masked_logits, jnp.float32),
        jnp.zeros((KEY_VALUE_HEADS, query_group, token_rows), jnp.float32),
        jnp.zeros((KEY_VALUE_HEADS, query_group, token_rows, HEAD_SIZE), jnp.float32),
    )
    key_section = lax.all_gather(key_matrix_rows, CTX, axis=0, tiled=True)
    value_section = lax.all_gather(value_rows, CTX, axis=0, tiled=True)

    def compute(current):
        best, total, weighted = current
        scores, visible, _ = piece_scores(query_rows, key_section, positions)
        value_tensor = value_section.reshape(value_section.shape[0], KEY_VALUE_HEADS, HEAD_SIZE)
        new_best = jnp.maximum(best, jnp.max(scores, axis=-1))
        weights = jnp.where(visible, jnp.exp(scores - new_best[..., None]), 0.0)
        total = jnp.sum(weights, axis=-1)
        weighted = jnp.einsum(
            "kgtn,nkd->kgtd",
            weights.astype(jnp.bfloat16),
            value_tensor,
            preferred_element_type=jnp.float32,
        )
        return (new_best, total, weighted)

    best, total, weighted = lax.cond(
        jnp.int32(0) <= positions[-1], compute, lambda current: current, init_state
    )
    log_sum_rows = best + jnp.log(total)
    attention_output = (
        jnp.transpose(weighted / total[..., None], (2, 0, 1, 3))
        .reshape(token_rows, QUERY_HEADS * HEAD_SIZE)
        .astype(jnp.bfloat16)
    )
    mixed = wide + jnp.dot(attention_output, output_w, preferred_element_type=jnp.float32)
    ffn_unit, inverse_two, ffn_in = rms_forward(mixed, ffn_gain)
    logits = jnp.dot(ffn_in, router_w, preferred_element_type=jnp.float32)
    route = routes[0]
    indicator = (route[:, :, None] == jnp.arange(EXPERT_COUNT, dtype=jnp.int32)).astype(jnp.float32)
    chosen = jnp.sum(indicator * logits[:, None, :], axis=-1)
    gates = jax.nn.softmax(chosen, axis=-1)
    flat_route = route.reshape(-1)
    counter = (flat_route[:, None] == jnp.arange(EXPERT_COUNT, dtype=jnp.int32)).astype(jnp.int32)
    slot = jnp.sum(counter * (jnp.cumsum(counter, axis=0) - 1), axis=1)
    target = flat_route * CAP + slot
    owner = (
        jnp.full((EXPERT_COUNT * CAP,), token_rows * TOP, jnp.int32)
        .at[target]
        .set(jnp.arange(token_rows * TOP, dtype=jnp.int32))
    )
    ffn_pad = jnp.concatenate([ffn_in, jnp.zeros((1, MODEL_WIDTH), jnp.bfloat16)], axis=0)
    local_experts = weight_in.shape[0]
    outgoing = ffn_pad[owner // TOP].reshape(ctx_size, local_experts, CAP, MODEL_WIDTH)
    received = lax.all_to_all(outgoing, CTX, split_axis=0, concat_axis=2, tiled=True)[0]
    act = jnp.einsum("erd,edf->erf", received, weight_in, preferred_element_type=jnp.float32)
    gate_part = act[..., :EXPERT_HIDDEN]
    up_part = act[..., EXPERT_HIDDEN:]
    sigma = jax.nn.sigmoid(gate_part)
    inner = (gate_part * sigma * up_part).astype(jnp.bfloat16)
    produced = jnp.einsum(
        "erf,edf->erd", inner, weight_out, preferred_element_type=jnp.float32
    ).astype(jnp.bfloat16)
    returned = lax.all_to_all(
        produced[None], CTX, split_axis=2, concat_axis=0, tiled=True
    ).reshape(EXPERT_COUNT * CAP, MODEL_WIDTH)
    picked = returned[target].reshape(token_rows, TOP, MODEL_WIDTH)
    layer_out = (mixed + jnp.sum(gates[..., None] * picked, axis=1)).astype(jnp.bfloat16)
    cot = cotangent[0]
    layer = (
        lax.all_gather(attn_norm, (CTX, FSDP), axis=0, tiled=True),
        lax.all_gather(ffn_norm, (CTX, FSDP), axis=0, tiled=True),
        lax.all_gather(w_q, (CTX, FSDP), axis=0, tiled=True),
        lax.all_gather(key_weight, (CTX, FSDP), axis=0, tiled=True),
        lax.all_gather(value_weight, (CTX, FSDP), axis=0, tiled=True),
        lax.all_gather(w_o, (CTX, FSDP), axis=0, tiled=True),
        lax.all_gather(router, (CTX, FSDP), axis=0, tiled=True),
    )
    attn_gain, ffn_gain, query_w, key_weight_matrix, value_w, output_w, router_w = layer
    experts = (
        lax.all_gather(expert_in, FSDP, axis=1, tiled=True),
        lax.all_gather(expert_out, FSDP, axis=1, tiled=True),
    )
    weight_in, weight_out = experts
    grad_gate = jnp.sum(cot[:, None, :] * picked, axis=-1)
    slot_grads = (
        (gates[..., None] * cot[:, None, :])
        .astype(jnp.bfloat16)
        .reshape(token_rows * TOP, MODEL_WIDTH)
    )
    slot_pad = jnp.concatenate([slot_grads, jnp.zeros((1, MODEL_WIDTH), jnp.bfloat16)], axis=0)
    grad_outgoing = slot_pad[owner].reshape(ctx_size, local_experts, CAP, MODEL_WIDTH)
    grad_received = lax.all_to_all(grad_outgoing, CTX, split_axis=0, concat_axis=2, tiled=True)[0]
    grad_w_out = jnp.einsum(
        "erd,erf->edf", grad_received, inner, preferred_element_type=jnp.float32
    )
    grad_inner = jnp.einsum(
        "erd,edf->erf", grad_received, weight_out, preferred_element_type=jnp.float32
    )
    grad_act = jnp.concatenate(
        [
            grad_inner * up_part * sigma * (1.0 + gate_part * (1.0 - sigma)),
            grad_inner * gate_part * sigma,
        ],
        axis=-1,
    ).astype(jnp.bfloat16)
    grad_w_in = jnp.einsum("erd,erf->edf", received, grad_act, preferred_element_type=jnp.float32)
    grad_rows = jnp.einsum(
        "erf,edf->erd", grad_act, weight_in, preferred_element_type=jnp.float32
    ).astype(jnp.bfloat16)
    grad_back = lax.all_to_all(
        grad_rows[None], CTX, split_axis=2, concat_axis=0, tiled=True
    ).reshape(EXPERT_COUNT * CAP, MODEL_WIDTH)
    grad_expert_in, grad_expert_out = (
        lax.psum_scatter(
            grad_w_in.astype(jnp.bfloat16), FSDP, scatter_dimension=1, tiled=True
        ).astype(jnp.float32),
        lax.psum_scatter(
            grad_w_out.astype(jnp.bfloat16), FSDP, scatter_dimension=1, tiled=True
        ).astype(jnp.float32),
    )
    grad_chosen = gates * (grad_gate - jnp.sum(gates * grad_gate, axis=-1, keepdims=True))
    grad_logits = jnp.sum(indicator * grad_chosen[..., None], axis=1).astype(jnp.bfloat16)
    grad_router_part = lax.dot_general(
        ffn_in, grad_logits, contract_rows, preferred_element_type=jnp.float32
    )
    grad_ffn_in = lax.dot_general(
        grad_logits, router_w, contract_cols, preferred_element_type=jnp.float32
    )
    grad_ffn_in = grad_ffn_in + jnp.sum(
        grad_back[target].reshape(token_rows, TOP, MODEL_WIDTH), axis=1, dtype=jnp.float32
    )
    back_two, grad_ffn_gain = rms_backward(grad_ffn_in, ffn_unit, inverse_two, ffn_gain)
    grad_mixed = cot + back_two
    grad_attn = grad_mixed.astype(jnp.bfloat16)
    grad_wo_part = lax.dot_general(
        attention_output, grad_attn, contract_rows, preferred_element_type=jnp.float32
    )
    attention_output_gradient = lax.dot_general(
        grad_attn, output_w, contract_cols, preferred_element_type=jnp.float32
    ).astype(jnp.bfloat16)
    head_gradient = attention_output_gradient.reshape(
        token_rows, KEY_VALUE_HEADS, query_group, HEAD_SIZE
    )
    delta_rows = jnp.sum(
        head_gradient.astype(jnp.float32)
        * attention_output.reshape(token_rows, KEY_VALUE_HEADS, query_group, HEAD_SIZE).astype(
            jnp.float32
        ),
        axis=-1,
    )
    delta_rows = jnp.transpose(delta_rows, (1, 2, 0))
    init_back = (
        jnp.zeros((token_rows, KEY_VALUE_HEADS, query_group, HEAD_SIZE), jnp.float32),
        jnp.zeros((sequence_length, 2 * KEY_VALUE_HEADS * HEAD_SIZE), jnp.float32),
    )
    attend_key_section = lax.all_gather(key_matrix_rows, CTX, axis=0, tiled=True)
    attend_value_section = lax.all_gather(value_rows, CTX, axis=0, tiled=True)

    def compute(current):
        token_count = attend_key_section.shape[0]
        scores, visible, key_tensor = piece_scores(query_rows, attend_key_section, positions)
        value_tensor = attend_value_section.reshape(token_count, KEY_VALUE_HEADS, HEAD_SIZE)
        weights_full = jnp.where(visible, jnp.exp(scores - log_sum_rows[..., None]), 0.0)
        grad_probs = jnp.einsum(
            "tkgd,nkd->kgtn", head_gradient, value_tensor, preferred_element_type=jnp.float32
        )
        grad_scores = (weights_full * (grad_probs - delta_rows[..., None])).astype(jnp.bfloat16)
        grad_query = attn_scale * jnp.einsum(
            "kgtn,nkd->tkgd", grad_scores, key_tensor, preferred_element_type=jnp.float32
        )
        key_portion = attn_scale * jnp.einsum(
            "kgtn,tkgd->nkd", grad_scores, query_rows, preferred_element_type=jnp.float32
        )
        value_portion = jnp.einsum(
            "kgtn,tkgd->nkd",
            weights_full.astype(jnp.bfloat16),
            head_gradient,
            preferred_element_type=jnp.float32,
        )
        update = jnp.concatenate(
            [
                key_portion.reshape(token_count, KEY_VALUE_HEADS * HEAD_SIZE),
                value_portion.reshape(token_count, KEY_VALUE_HEADS * HEAD_SIZE),
            ],
            axis=1,
        )
        return (grad_query, update)

    grad_query, grad_keys_full = lax.cond(
        jnp.int32(0) <= positions[-1], compute, lambda current: current, init_back
    )
    local_gradients = lax.psum_scatter(
        grad_keys_full.astype(jnp.bfloat16), CTX, scatter_dimension=0, tiled=True
    ).astype(jnp.float32)
    query_back = (
        rotate_pairs(
            grad_query.reshape(token_rows, QUERY_HEADS, HEAD_SIZE), cosine_table, -sine_table
        )
        .astype(jnp.bfloat16)
        .reshape(token_rows, QUERY_HEADS * HEAD_SIZE)
    )
    key_backward_rows = (
        rotate_pairs(
            local_gradients[:, : KEY_VALUE_HEADS * HEAD_SIZE].reshape(
                token_rows, KEY_VALUE_HEADS, HEAD_SIZE
            ),
            cosine_table,
            -sine_table,
        )
        .astype(jnp.bfloat16)
        .reshape(token_rows, KEY_VALUE_HEADS * HEAD_SIZE)
    )
    value_backward_rows = local_gradients[:, KEY_VALUE_HEADS * HEAD_SIZE :].astype(jnp.bfloat16)
    grad_wq_part = lax.dot_general(
        attention_input, query_back, contract_rows, preferred_element_type=jnp.float32
    )
    grad_wk_part = lax.dot_general(
        attention_input, key_backward_rows, contract_rows, preferred_element_type=jnp.float32
    )
    grad_wv_part = lax.dot_general(
        attention_input, value_backward_rows, contract_rows, preferred_element_type=jnp.float32
    )
    grad_attn_in = lax.dot_general(
        query_back, query_w, contract_cols, preferred_element_type=jnp.float32
    )
    grad_attn_in = grad_attn_in + lax.dot_general(
        key_backward_rows, key_weight_matrix, contract_cols, preferred_element_type=jnp.float32
    )
    grad_attn_in = grad_attn_in + lax.dot_general(
        value_backward_rows, value_w, contract_cols, preferred_element_type=jnp.float32
    )
    back_one, grad_attn_gain = rms_backward(grad_attn_in, attn_unit, inverse_one, attn_gain)
    grad_input = grad_mixed + back_one
    partial_sums = (
        lax.psum_scatter(
            grad_attn_gain.astype(jnp.bfloat16), CTX, scatter_dimension=0, tiled=True
        ).astype(jnp.float32),
        lax.psum_scatter(
            grad_ffn_gain.astype(jnp.bfloat16), CTX, scatter_dimension=0, tiled=True
        ).astype(jnp.float32),
        lax.psum_scatter(
            grad_wq_part.astype(jnp.bfloat16), CTX, scatter_dimension=0, tiled=True
        ).astype(jnp.float32),
        lax.psum_scatter(
            grad_wk_part.astype(jnp.bfloat16), CTX, scatter_dimension=0, tiled=True
        ).astype(jnp.float32),
        lax.psum_scatter(
            grad_wv_part.astype(jnp.bfloat16), CTX, scatter_dimension=0, tiled=True
        ).astype(jnp.float32),
        lax.psum_scatter(
            grad_wo_part.astype(jnp.bfloat16), CTX, scatter_dimension=0, tiled=True
        ).astype(jnp.float32),
        lax.psum_scatter(
            grad_router_part.astype(jnp.bfloat16), CTX, scatter_dimension=0, tiled=True
        ).astype(jnp.float32),
    )
    summed = (
        lax.psum_scatter(
            partial_sums[0].astype(jnp.bfloat16), FSDP, scatter_dimension=0, tiled=True
        ).astype(jnp.float32),
        lax.psum_scatter(
            partial_sums[1].astype(jnp.bfloat16), FSDP, scatter_dimension=0, tiled=True
        ).astype(jnp.float32),
        lax.psum_scatter(
            partial_sums[2].astype(jnp.bfloat16), FSDP, scatter_dimension=0, tiled=True
        ).astype(jnp.float32),
        lax.psum_scatter(
            partial_sums[3].astype(jnp.bfloat16), FSDP, scatter_dimension=0, tiled=True
        ).astype(jnp.float32),
        lax.psum_scatter(
            partial_sums[4].astype(jnp.bfloat16), FSDP, scatter_dimension=0, tiled=True
        ).astype(jnp.float32),
        lax.psum_scatter(
            partial_sums[5].astype(jnp.bfloat16), FSDP, scatter_dimension=0, tiled=True
        ).astype(jnp.float32),
        lax.psum_scatter(
            partial_sums[6].astype(jnp.bfloat16), FSDP, scatter_dimension=0, tiled=True
        ).astype(jnp.float32),
    )
    return (
        layer_out[None],
        grad_input[None],
        summed[0],
        summed[1],
        summed[2],
        summed[3],
        summed[4],
        summed[5],
        summed[6],
        grad_expert_in,
        grad_expert_out,
    )


def swap(a, flip):
    return lax.ppermute(a, FSDP, [(i, i ^ flip) for i in range(NX * NC)])


def fast_body(
    hidden,
    routes,
    attn_norm,
    ffn_norm,
    w_q,
    key_weight,
    value_weight,
    w_o,
    router,
    expert_in,
    expert_out,
    cotangent,
):
    tokens = hidden.shape[1]
    group = QUERY_HEADS // KEY_VALUE_HEADS
    ctx_size = NZ * NY
    ctx = lax.axis_index(CTX)
    fsdp = lax.axis_index(FSDP)
    core = fsdp % NC
    rows = w_q.shape[0]
    quarter = expert_in.shape[1]
    kv_width = KEY_VALUE_HEADS * HEAD_SIZE
    q_width = QUERY_HEADS * HEAD_SIZE
    held = expert_in.shape[0] // NC
    bf = jnp.bfloat16
    f32 = jnp.float32
    positions = ctx * tokens + jnp.arange(tokens, dtype=jnp.int32)
    cosine_table, sine_table = rope_tables(positions)
    contract_cols = (((1,), (1,)), ((), ()))
    wide = hidden[0].astype(f32)
    cot = cotangent[0]

    pack_one = jnp.concatenate([w_q, key_weight, value_weight], axis=1)
    pack_two = jnp.concatenate(
        [w_o, router, attn_norm[:, None], ffn_norm[:, None], jnp.zeros((rows, 94), bf)], axis=1
    )
    route = routes[0]
    indicator = (route[:, :, None] == jnp.arange(EXPERT_COUNT, dtype=jnp.int32)).astype(f32)
    cot_pack = jnp.concatenate(
        [
            cot.astype(bf),
            jnp.sum(indicator, axis=1).astype(bf),
            jnp.zeros((tokens, 128 - EXPERT_COUNT), bf),
        ],
        axis=1,
    )
    experts = jnp.concatenate([expert_in, expert_out], axis=2)
    experts = experts.reshape(NC, held, quarter, experts.shape[2])
    mine = lax.dynamic_index_in_dim(experts, core, 0, False)
    other = lax.dynamic_index_in_dim(experts, 1 - core, 0, False)
    far_one, far_two = swap(pack_one, 2), swap(pack_two, 2)
    far_one, far_two, mine, other = lax.optimization_barrier((far_one, far_two, mine, other))
    parts = [mine, swap(other, 1), swap(mine, 2), swap(other, 3)]
    both = lambda near, far: jnp.where(
        fsdp < NC, jnp.stack([near, far]), jnp.stack([far, near])
    )
    part = rows // 3
    groups = ctx_size, NX, NC, rows
    one, two, cots = gather(
        [both(pack_one, far_one), both(pack_two, far_two), cot_pack],
        [
            Plan(0, (Z, Y, C), (Z, Y, C), rows=(0, 2 * part), view=weight_view),
            Plan(0, (Y, Z, C), (Z, Y, C), rows=(2 * part, part), view=weight_view),
            Plan(1, (Z, Y, C), (Z, Y, C), rows=(0, rows), view=weight_view),
            Plan(2, (Z, Y, C), (C, Z, Y)),
        ],
        0,
        {0: groups + pack_one.shape[1:], 1: groups + pack_two.shape[1:]},
    )
    one = one.reshape(MODEL_WIDTH, -1)
    two = two.reshape(MODEL_WIDTH, -1)
    output_w = two[:, :MODEL_WIDTH]
    small = two[:, MODEL_WIDTH:]
    router_w = small[:, :EXPERT_COUNT]
    gains = lax.dot_general(
        jnp.eye(128, dtype=bf), small, contract_cols, preferred_element_type=f32
    )
    attn_gain, ffn_gain = gains[EXPERT_COUNT], gains[EXPERT_COUNT + 1]

    attn_unit, inverse_one, attention_input = rms_forward(wide, attn_gain)
    linear = jnp.dot(attention_input, one, preferred_element_type=f32)
    query_rows = (
        rotate_pairs(linear[:, :q_width].reshape(tokens, QUERY_HEADS, HEAD_SIZE), cosine_table, sine_table)
        .astype(bf)
        .reshape(tokens, KEY_VALUE_HEADS, group, HEAD_SIZE)
    )
    key_rows = (
        rotate_pairs(
            linear[:, q_width : q_width + kv_width].reshape(tokens, KEY_VALUE_HEADS, HEAD_SIZE),
            cosine_table,
            sine_table,
        )
        .astype(bf)
        .reshape(tokens, kv_width)
    )
    value_rows = linear[:, q_width + kv_width :].astype(bf)
    (kv,) = gather(
        [jnp.concatenate([key_rows, value_rows], axis=1)], [Plan(0, (Z, Y,), (Z, Y,))], 1
    )
    kv = kv.reshape(ctx_size * tokens, 2 * kv_width)
    key_section, value_section = kv[:, :kv_width], kv[:, kv_width:]
    value_tensor = value_section.reshape(ctx_size * tokens, KEY_VALUE_HEADS, HEAD_SIZE)
    scores, visible, key_tensor = piece_scores(query_rows, key_section, positions)
    best = jnp.max(scores, axis=-1)
    weights = jnp.where(visible, jnp.exp(scores - best[..., None]), 0.0)
    total = jnp.sum(weights, axis=-1)
    weighted = jnp.einsum(
        "kgtn,nkd->kgtd", weights.astype(bf), value_tensor, preferred_element_type=f32
    )
    log_sum_rows = best + jnp.log(total)
    attention_output = (
        jnp.transpose(weighted / total[..., None], (2, 0, 1, 3)).reshape(tokens, q_width).astype(bf)
    )
    mixed = wide + jnp.dot(attention_output, output_w, preferred_element_type=f32)
    ffn_unit, inverse_two, ffn_in = rms_forward(mixed, ffn_gain)
    logits = jnp.dot(ffn_in, router_w, preferred_element_type=f32)
    chosen = jnp.sum(indicator * logits[:, None, :], axis=-1)
    gates = jax.nn.softmax(chosen, axis=-1)
    gate_map = jnp.sum(indicator * gates[..., None], axis=1)
    payload = jnp.concatenate(
        [ffn_in, gate_map.astype(bf), jnp.zeros((tokens, 128 - EXPERT_COUNT), bf)], axis=1
    )
    gin, moe_part, *pieces = moe(payload, cots, parts, CAP, 2)
    across = [swap(pieces[j], j) for j in range(1, NX * NC)]
    grad_gate_map = gin[:, MODEL_WIDTH : MODEL_WIDTH + EXPERT_COUNT] + gin[
        :, MODEL_WIDTH + EXPERT_COUNT : MODEL_WIDTH + 2 * EXPERT_COUNT
    ]
    grad_gate = jnp.sum(indicator * grad_gate_map[:, None, :], axis=-1)
    grad_chosen = gates * (grad_gate - jnp.sum(gates * grad_gate, axis=-1, keepdims=True))
    grad_logits = jnp.sum(indicator * grad_chosen[..., None], axis=1).astype(bf)
    grad_ffn_in = gin[:, :MODEL_WIDTH] + lax.dot_general(
        grad_logits, router_w, contract_cols, preferred_element_type=f32
    )
    back_two, _ = rms_backward(grad_ffn_in, ffn_unit, inverse_two, ffn_gain)
    grad_mixed = cot + back_two
    grad_attn = grad_mixed.astype(bf)
    attention_output_gradient = lax.dot_general(
        grad_attn, output_w, contract_cols, preferred_element_type=f32
    ).astype(bf)
    head_gradient = attention_output_gradient.reshape(tokens, KEY_VALUE_HEADS, group, HEAD_SIZE)
    delta_rows = jnp.sum(
        head_gradient.astype(f32)
        * attention_output.reshape(tokens, KEY_VALUE_HEADS, group, HEAD_SIZE).astype(f32),
        axis=-1,
    )
    delta_rows = jnp.transpose(delta_rows, (1, 2, 0))
    weights_full = jnp.where(visible, jnp.exp(scores - log_sum_rows[..., None]), 0.0)
    grad_probs = jnp.einsum(
        "tkgd,nkd->kgtn", head_gradient, value_tensor, preferred_element_type=f32
    )
    grad_scores = (weights_full * (grad_probs - delta_rows[..., None])).astype(bf)
    grad_query = attn_scale * jnp.einsum(
        "kgtn,nkd->tkgd", grad_scores, key_tensor, preferred_element_type=f32
    )
    key_portion = attn_scale * jnp.einsum(
        "kgtn,tkgd->nkd", grad_scores, query_rows, preferred_element_type=f32
    )
    value_portion = jnp.einsum(
        "kgtn,tkgd->nkd", weights_full.astype(bf), head_gradient, preferred_element_type=f32
    )
    update = jnp.concatenate(
        [
            key_portion.astype(bf).reshape(ctx_size, tokens, kv_width),
            value_portion.astype(bf).reshape(ctx_size, tokens, kv_width),
        ],
        axis=2,
    )
    (local_gradients,) = reduce_scatter([update], [Plan(0, (Y,), (Z, Y,))], [f32], 4)
    query_back = (
        rotate_pairs(
            grad_query.reshape(tokens, QUERY_HEADS, HEAD_SIZE), cosine_table, -sine_table
        )
        .astype(bf)
        .reshape(tokens, q_width)
    )
    key_back = (
        rotate_pairs(
            local_gradients[:, :kv_width].reshape(tokens, KEY_VALUE_HEADS, HEAD_SIZE),
            cosine_table,
            -sine_table,
        )
        .astype(bf)
        .reshape(tokens, kv_width)
    )
    back = jnp.concatenate([query_back, key_back, local_gradients[:, kv_width:].astype(bf)], axis=1)
    grad_attn_in = lax.dot_general(back, one, contract_cols, preferred_element_type=f32)
    back_one, _ = rms_backward(grad_attn_in, attn_unit, inverse_one, attn_gain)
    grad_input = grad_mixed + back_one
    halves = []
    for factor in (grad_attn_in * attn_unit, grad_ffn_in * ffn_unit):
        high = factor.astype(bf)
        halves += [high, (factor - high.astype(f32)).astype(bf)]
    column = lambda n: jnp.broadcast_to((jnp.arange(128) == n).astype(bf), (tokens, 128))
    sum_one, sum_two, layer_out = return_weights(
        [attention_input, attention_output, jnp.concatenate([ffn_in] + halves)],
        [
            back,
            grad_attn,
            jnp.concatenate(
                [
                    jnp.concatenate([grad_logits, jnp.zeros((tokens, 128 - EXPERT_COUNT), bf)], axis=1),
                    column(EXPERT_COUNT),
                    column(EXPERT_COUNT),
                    column(EXPERT_COUNT + 1),
                    column(EXPERT_COUNT + 1),
                ]
            ),
        ],
        moe_part,
        mixed,
        5,
    )
    grad_expert_in, grad_expert_out = (
        g.reshape(NC * held, quarter, -1)
        for g in add_experts([pieces[0]] + across, core, 2 * EXPERT_HIDDEN)
    )
    at = MODEL_WIDTH + EXPERT_COUNT
    return (
        layer_out[None],
        grad_input[None],
        sum_two[:, at],
        sum_two[:, at + 1],
        sum_one[:, :q_width],
        sum_one[:, q_width : q_width + kv_width],
        sum_one[:, q_width + kv_width :],
        sum_two[:, :MODEL_WIDTH],
        sum_two[:, MODEL_WIDTH:at],
        grad_expert_in,
        grad_expert_out,
    )


def fast(*args):
    return fast_body(*args)


def solution(mesh):
    placed = (
        P(FSDP, CTX, None),
        P(FSDP, CTX, None),
        P((CTX, FSDP)),
        P((CTX, FSDP)),
        P((CTX, FSDP), None),
        P((CTX, FSDP), None),
        P((CTX, FSDP), None),
        P((CTX, FSDP), None),
        P((CTX, FSDP), None),
        P(CTX, FSDP, None),
        P(CTX, FSDP, None),
        P(FSDP, CTX, None),
    )
    small = mesh.shape[CTX] == NZ * NY and mesh.shape[FSDP] == NX * NC
    return jax.shard_map(
        fast if small else local,
        mesh=mesh,
        in_specs=placed,
        out_specs=(
            P(FSDP, CTX, None),
            P(FSDP, CTX, None),
            P((CTX, FSDP)),
            P((CTX, FSDP)),
            P((CTX, FSDP), None),
            P((CTX, FSDP), None),
            P((CTX, FSDP), None),
            P((CTX, FSDP), None),
            P((CTX, FSDP), None),
            P(CTX, FSDP, None),
            P(CTX, FSDP, None),
        ),
        check_vma=False,
    )
```

```python
import functools
import itertools

import jax
import jax.numpy as jnp
from jax import lax
from jax.experimental import pallas as pl
from jax.experimental.pallas import tpu as pltpu
from jax.sharding import PartitionSpec as P


NY = 2
NZ = 4
NX = 2
NC = 2
DEV = pl.DeviceIdType.MESH
CTX, FSDP = "ctx", "fsdp"
Z, Y, X, C = 0, 1, 2, 3
SIZES = {Z: NZ, Y: NY, X: NX, C: NC}
UP, DOWN = 4, 5


class Plan:
    def __init__(self, ref, order, index, rows=None, view=None):
        self.ref, self.order, self.index, self.rows, self.view = ref, order, index, rows, view
        self.blocks = 1
        for d in index:
            self.blocks *= SIZES[d]


class Place:
    def __init__(self):
        ctx = lax.axis_index(CTX)
        fsdp = lax.axis_index(FSDP)
        self.at = {Z: ctx // NY, Y: ctx % NY, X: fsdp // NC, C: fsdp % NC}
        z = self.at[Z]
        low = z < NZ // 2
        base = jnp.where(low, z, NZ - 1 - z)
        near = [base, 1 - base, jnp.int32(2), jnp.int32(3)]
        self.order = [z] + [jnp.where(low, k, NZ - 1 - k) for k in near[1:]]

    def device(self, dim, value):
        spot = dict(self.at)
        spot[dim] = value
        return (spot[Z] * NY + spot[Y], spot[X] * NC + spot[C])

    def across(self, dim):
        return self.device(dim, 1 - self.at[dim])

    def along(self, step):
        return self.device(Z, self.at[Z] + step)

    def coords(self, z_from, flips):
        spot = {d: (1 - self.at[d] if d in flips else self.at[d]) for d in (Y, X, C)}
        spot[Z] = z_from
        return spot


def flat_index(spot, dims):
    index = 0
    for d in dims:
        index = index * SIZES[d] + spot[d]
    return index


def subsets(dims):
    return [c for n in range(len(dims) + 1) for c in itertools.combinations(dims, n)]


def greet(place, dims):
    barrier = pltpu.get_barrier_semaphore()
    z = place.at[Z]
    count = jnp.int32(0)
    for d in dims:
        if d == Z:
            @pl.when(z > 0)
            def _():
                pl.semaphore_signal(barrier, inc=1, device_id=place.along(-1), device_id_type=DEV)

            @pl.when(z < NZ - 1)
            def _():
                pl.semaphore_signal(barrier, inc=1, device_id=place.along(1), device_id_type=DEV)

            count = count + jnp.where(z > 0, 1, 0) + jnp.where(z < NZ - 1, 1, 0)
        else:
            pl.semaphore_signal(barrier, inc=1, device_id=place.across(d), device_id_type=DEV)
            count = count + 1
    pl.semaphore_wait(barrier, count)


def gather_events(order):
    pairs = [d for d in order if d != Z]
    events = [(k, f) for k in range(NZ) for f in subsets(pairs)]
    return sorted(events, key=lambda e: (e[0] + len(e[1]), len(e[1])))


def gather_sends(order, k, flips):
    z_at = order.index(Z)
    last = max([order.index(d) for d in flips] + ([z_at] if k > 0 else []) + [-1])
    out = []
    for position, d in enumerate(order):
        if position > last:
            out.extend([UP, DOWN] if d == Z else [d])
    if k > 0 and last == z_at:
        out.extend([UP, DOWN])
    return out


def gather_kernel(plans, n_in, *refs):
    ins, outs = refs[:n_in], refs[n_in : 2 * n_in]
    send_sem, recv_sem, own_sem = refs[2 * n_in :]
    place = Place()
    z = place.at[Z]
    greet(place, sorted({d for p in plans for d in p.order}))
    pending = []
    slot = 0
    queue = []
    for n, plan in enumerate(plans):
        for rank, event in enumerate(gather_events(plan.order)):
            queue.append((rank / len(gather_events(plan.order)), n, event))
    queue.sort(key=lambda q: (q[0], q[1]))
    bases = [sum(p.blocks for p in plans[:n]) for n in range(len(plans))]
    for _, n, (k, flips) in queue:
        plan = plans[n]
        src = ins[plan.ref]
        out = outs[plan.ref]
        rows = plan.rows
        z_from = place.order[k]
        spot = place.coords(z_from, flips)
        index = flat_index(spot, plan.index)
        own = k == 0 and not flips
        if plan.view is not None:
            target = plan.view(out, spot, rows)
            source = src.at[:, pl.ds(rows[0], rows[1])] if own else target
        else:
            target = out.at[index] if rows is None else out.at[index, pl.ds(rows[0], rows[1])]
            source = (src if rows is None else src.at[pl.ds(rows[0], rows[1])]) if own else target
        sem = recv_sem.at[bases[n] + index]
        if not own:
            pltpu.make_async_remote_copy(
                src_ref=target, dst_ref=target, send_sem=own_sem.at[0], recv_sem=sem,
                device_id=place.across(C), device_id_type=DEV,
            ).wait_recv()
        for way in gather_sends(plan.order, k, flips):
            if way in (UP, DOWN):
                step = 1 if way == UP else -1
                go = z < NZ - 1 if way == UP else z > 0
                if k > 0:
                    go = jnp.logical_and(go, z_from < z if way == UP else z_from > z)
                dest = place.device(Z, jnp.clip(z + step, 0, NZ - 1))
            else:
                go, dest = None, place.across(way)
            copy = pltpu.make_async_remote_copy(
                src_ref=source, dst_ref=target, send_sem=send_sem.at[slot], recv_sem=sem,
                device_id=dest, device_id_type=DEV,
            )
            slot += 1
            if go is None:
                copy.start()
            else:
                pl.when(go)(copy.start)
            pending.append((go, copy.wait_send))
        if own:
            copy = pltpu.make_async_copy(source, target, own_sem.at[1 + n])
            copy.start()
            pending.append((None, copy.wait))
    for go, wait in pending:
        if go is None:
            wait()
        else:
            pl.when(go)(wait)


def gather(arrays, plans, collective_id, shapes=None):
    n = len(arrays)
    sends = sum(len(gather_sends(p.order, k, f)) for p in plans for k, f in gather_events(p.order))
    blocks = {p.ref: p.blocks for p in plans}
    return pl.pallas_call(
        functools.partial(gather_kernel, plans, n),
        out_shape=[
            jax.ShapeDtypeStruct((shapes or {}).get(i, (blocks[i],) + a.shape), a.dtype)
            for i, a in enumerate(arrays)
        ],
        in_specs=[pl.BlockSpec(memory_space=pltpu.VMEM)] * n,
        out_specs=[pl.BlockSpec(memory_space=pl.ANY)] * n,
        scratch_shapes=[
            pltpu.SemaphoreType.DMA((sends,)),
            pltpu.SemaphoreType.DMA((sum(p.blocks for p in plans),)),
            pltpu.SemaphoreType.DMA((1 + len(plans),)),
        ],
        compiler_params=pltpu.CompilerParams(collective_id=collective_id, has_side_effects=True),
    )(*arrays)


def add_into(acc, other):
    acc[...] = (acc[...].astype(jnp.float32) + other[...].astype(jnp.float32)).astype(acc.dtype)


class Gather:
    def __init__(self, place, plan, src, out, send_sem, recv_sem, spare_sem, slot, base):
        self.place, self.plan, self.src, self.out = place, plan, src, out
        self.send_sem, self.recv_sem, self.spare_sem = send_sem, recv_sem, spare_sem
        self.slot, self.base = slot, base
        self.pending = []

    @staticmethod
    def sends(plan):
        return sum(len(gather_sends(plan.order, k, f)) for k, f in gather_events(plan.order))

    def goes(self, way, k):
        z, z_from = self.place.at[Z], self.place.order[k]
        if way == UP:
            return z < NZ - 1 if k == 0 else jnp.logical_and(z < NZ - 1, z_from < z)
        return z > 0 if k == 0 else jnp.logical_and(z > 0, z_from > z)

    def part(self, ref):
        rows = self.plan.rows
        return ref if rows is None else ref.at[pl.ds(rows[0], rows[1])]

    def step(self, k, flips):
        place, plan = self.place, self.plan
        index = flat_index(place.coords(place.order[k], flips), plan.index)
        target = self.part(self.out.at[index])
        sem = self.recv_sem.at[self.base + index]
        source = target
        if k == 0 and not flips:
            source = self.part(self.src)
        else:
            pltpu.make_async_remote_copy(
                src_ref=target, dst_ref=target, send_sem=self.spare_sem, recv_sem=sem,
                device_id=place.across(C), device_id_type=DEV,
            ).wait_recv()
        for way in gather_sends(plan.order, k, flips):
            if way in (UP, DOWN):
                dest = place.device(Z, jnp.clip(place.at[Z] + (1 if way == UP else -1), 0, NZ - 1))
            else:
                dest = place.across(way)
            copy = pltpu.make_async_remote_copy(
                src_ref=source, dst_ref=target, send_sem=self.send_sem.at[self.slot], recv_sem=sem,
                device_id=dest, device_id_type=DEV,
            )
            if way in (UP, DOWN):
                pl.when(self.goes(way, k))(copy.start)
            else:
                copy.start()
            self.pending.append((way, k, self.slot))
            self.slot += 1

    def finish(self):
        for way, k, slot in self.pending:
            block = self.part(self.src)
            copy = pltpu.make_async_remote_copy(
                src_ref=block, dst_ref=block, send_sem=self.send_sem.at[slot], recv_sem=self.spare_sem,
                device_id=self.place.across(C), device_id_type=DEV,
            )
            if way in (UP, DOWN):
                pl.when(self.goes(way, k))(copy.wait_send)
            else:
                copy.wait_send()


class Reduce:
    def __init__(self, place, plan, held, levels, chain, send_sem, recv_sem, spare_sem):
        self.place, self.plan, self.held, self.levels, self.chain = place, plan, held, levels, chain
        self.send_sem, self.recv_sem, self.spare_sem = send_sem, recv_sem, spare_sem
        dims = plan.order
        self.kept = [subsets(dims[p + 1 :]) for p in range(len(dims))]
        self.base = [NZ * sum(len(f) for f in self.kept[:p]) for p in range(len(dims) + 1)]
        self.slot = 0

    @staticmethod
    def counts(plan):
        kept = [NZ * len(subsets(plan.order[p + 1 :])) for p in range(len(plan.order))]
        return kept, sum(kept) + NZ - 1, sum(kept) + NZ + 1

    def push(self, source, target, sem, dest):
        copy = pltpu.make_async_remote_copy(
            src_ref=source, dst_ref=target, send_sem=self.send_sem.at[self.slot], recv_sem=sem,
            device_id=dest, device_id_type=DEV,
        )
        self.slot += 1
        copy.start()

    def arrived(self, target, sem):
        pltpu.make_async_remote_copy(
            src_ref=target, dst_ref=target, send_sem=self.spare_sem, recv_sem=sem,
            device_id=self.place.across(C), device_id_type=DEV,
        ).wait_recv()

    def block(self, k, flips):
        return flat_index(self.place.coords(self.place.order[k], flips), self.plan.index)

    def first(self, k):
        dim = self.plan.order[0]
        for n, f in enumerate(self.kept[0]):
            spot = self.place.order[k] * len(self.kept[0]) + n
            self.push(
                self.held.at[self.block(k, (dim,) + f)], self.levels[0].at[spot],
                self.recv_sem.at[spot], self.place.across(dim),
            )

    def level(self, p, k):
        dims = self.plan.order
        z_to = self.place.order[k]
        for f in sorted(self.kept[p], key=lambda f: -len(f)):
            spot = z_to * len(self.kept[p]) + self.kept[p].index(f)
            mine = self.held.at[self.block(k, f)]
            self.arrived(self.levels[p].at[spot], self.recv_sem.at[self.base[p] + spot])
            add_into(mine, self.levels[p].at[spot])
            later = p + 1
            if later < len(dims) and dims[later] in f:
                left = tuple(d for d in f if d != dims[later])
                there = z_to * len(self.kept[later]) + self.kept[later].index(left)
                self.push(
                    mine, self.levels[later].at[there],
                    self.recv_sem.at[self.base[later] + there], self.place.across(dims[later]),
                )

    def along(self, k):
        z = self.place.at[Z]
        dest = self.place.order[k]
        up = dest > z
        spot = dest + jnp.where(up, 1, 0)
        mine = self.held.at[self.block(k, ())]
        sem = self.recv_sem.at[self.base[-1] + spot]

        @pl.when(jnp.where(up, z > 0, z < NZ - 1))
        def _():
            self.arrived(self.chain.at[spot], sem)
            add_into(mine, self.chain.at[spot])

        self.push(mine, self.chain.at[spot], sem, self.place.along(jnp.where(up, 1, -1)))

    def last(self, out, base=None):
        z = self.place.at[Z]
        mine = self.held.at[self.block(0, ())]
        for go, spot in ((z > 0, z + 1), (z < NZ - 1, z)):

            @pl.when(go)
            def _():
                self.arrived(self.chain.at[spot], self.recv_sem.at[self.base[-1] + spot])
                add_into(mine, self.chain.at[spot])

        total = mine[...].astype(jnp.float32)
        if base is not None:
            total = base[...] + total
        out[...] = total.astype(out.dtype)

    def at_time(self, t):
        depth = len(self.plan.order)
        far = list(reversed(range(NZ)))
        out = [functools.partial(self.level, p, far[t - p]) for p in range(depth) if 0 <= t - p < NZ]
        if 0 <= t - depth < NZ - 1:
            out.append(functools.partial(self.along, far[t - depth]))
        return out

    def steps(self):
        return [step for t in range(NZ + len(self.plan.order)) for step in self.at_time(t)]

    def finish(self):
        block = self.levels[0].at[0]
        for slot in range(self.slot):
            pltpu.make_async_remote_copy(
                src_ref=block, dst_ref=block, send_sem=self.send_sem.at[slot], recv_sem=self.spare_sem,
                device_id=self.place.across(C), device_id_type=DEV,
            ).wait_send()


def tile_up(n, m):
    return (n + m - 1) // m * m


def columns_of(width, chunk=512):
    return [(i, min(chunk, width - i)) for i in range(0, width, chunk)]


def moe_kernel(plans, back, width, hidden, cap, *refs):
    payload, cots, w_own, w_core, w_x, w_both = refs[:6]
    gin_out, part_out = refs[6:8]
    grads = refs[8:12]
    (
        seen, cot_seen, weights, taken, cot_taken, rows_buf, scaled, grad_act, pick, stage,
        lvl_b0, lvl_b1, chain_b,
        send_sem, recv_sem, spare_sem, send_b, recv_b, load_sem, store_sem, part_sem,
    ) = refs[12:]
    bf, f32 = jnp.bfloat16, jnp.float32
    place = Place()
    count = payload.shape[0]
    pair = 2 * cap
    wide = width + 128
    quarter = width // (NX * NC)
    half = NZ * pair
    lanes = pick.shape[2]
    held = weights.shape[0]
    fsdp = place.at[X] * NC + place.at[C]
    first = (((place.at[Z] * NY + place.at[Y]) * NC) + place.at[C]) * held

    loads = []
    for j, ref in enumerate((w_own, w_core, w_x, w_both)):
        rows = pl.ds(pl.multiple_of((fsdp ^ j) * quarter, quarter), quarter)
        for e in range(held):
            loads.append(pltpu.make_async_copy(ref.at[e], weights.at[e, rows], load_sem.at[len(loads)]))
    base_of = lambda h, k: (jnp.where(h == 0, place.at[C], 1 - place.at[C]) * NZ + place.order[k]) * NY
    cot_loads = {}
    for k in range(NZ):
        for h in range(2):
            at = pl.ds(base_of(h, k), NY)
            cot_loads[(h, k)] = pltpu.make_async_copy(cots.at[at], cot_seen.at[at], load_sem.at[len(loads) + len(cot_loads)])

    greet(place, (Z, Y, C))
    ways = []
    send_at = 0
    for n, plan in enumerate(plans):
        ways.append(Gather(place, plan, payload, seen, send_sem, recv_sem, spare_sem, send_at, n * plan.blocks))
        send_at += Gather.sends(plan)
    for way in ways:
        way.step(0, ())
    for key in cot_loads:
        cot_loads[key].start()
    for copy in loads:
        copy.start()
    seen[flat_index(place.at, plans[0].index)] = payload[...]

    row_id = lax.broadcasted_iota(jnp.int32, (NY * count, NY * count), 0)
    col_id = lax.broadcasted_iota(jnp.int32, (NY * count, NY * count), 1)
    earlier = jnp.logical_and(col_id < row_id, col_id // count == row_id // count).astype(bf)
    lane_id = lax.broadcasted_iota(jnp.int32, (1, 128), 1)
    here = [(lane_id == first + e).astype(f32) for e in range(held)]
    pick_lane = lax.broadcasted_iota(jnp.int32, (NY * count, lanes), 1).astype(f32)
    y_shift = (lax.broadcasted_iota(jnp.int32, (NY * count, 1), 0) // count * cap).astype(f32)

    def dispatch(source, target, h, k, cols):
        at = pl.ds(base_of(h, k), NY)
        r = (h * NZ + k) * pair
        for c0, cn in cols:
            block = source[at, :, c0 : c0 + cn].reshape(NY * count, cn)
            got = lax.dot_general(
                pick[h * NZ + k], block, (((0,), (0,)), ((), ())), preferred_element_type=f32
            ).astype(bf)
            for e in range(held):
                target[e, r : r + pair, c0 : c0 + cn] = got[e * pair : (e + 1) * pair]

    def cot_chunk(h, k):
        cot_loads[(h, k)].wait()
        at = pl.ds(base_of(h, k), NY)
        chosen = cot_seen[at, :, width:wide].reshape(NY * count, 128)
        before = jnp.dot(earlier, chosen, preferred_element_type=f32)
        picked = None
        for e in range(held):
            is_here = jnp.sum(chosen.astype(f32) * here[e], axis=1, keepdims=True)
            slot = jnp.sum(before * here[e], axis=1, keepdims=True) + y_shift + e * pair
            target = jnp.where(is_here > 0.5, slot, -1.0)
            hit = pick_lane == target
            picked = hit if picked is None else jnp.logical_or(picked, hit)
        pick[h * NZ + k] = picked.astype(f32).astype(bf)
        dispatch(cot_seen, cot_taken, h, k, columns_of(width))

    def hidden_chunk(h, e, n, tile):
        rows = pl.ds(h * half, half)
        tokens_in = taken[e, rows, :width]
        gate = jnp.sum(taken[e, rows, width:wide].astype(f32) * here[e], axis=1, keepdims=True)
        col = n * tile
        g = jnp.dot(tokens_in, weights[e, :, col : col + tile], preferred_element_type=f32)
        u = jnp.dot(tokens_in, weights[e, :, hidden + col : hidden + col + tile], preferred_element_type=f32)
        raw = jnp.dot(
            cot_taken[e, rows, :], weights[e, :, 2 * hidden + col : 2 * hidden + col + tile], preferred_element_type=f32
        )
        s = jax.nn.sigmoid(g)
        gs = g * s
        inner = gs * u
        scaled[e, rows, col : col + tile] = (inner * gate).astype(bf)
        grad_inner = raw * gate
        grad_act[e, rows, col : col + tile] = (grad_inner * u * s * (1.0 + g * (1.0 - s))).astype(bf)
        grad_act[e, rows, hidden + col : hidden + col + tile] = (grad_inner * gs).astype(bf)
        return jnp.sum(raw * inner, axis=1, keepdims=True)

    def hidden_part(h, e):
        tile = min(256, hidden)
        gate_grad = sum(hidden_chunk(h, e, n, tile) for n in range(hidden // tile))
        high = gate_grad.astype(bf).astype(f32)
        there = pl.ds(h * half, half)
        apart = (lane_id == EXPERT_COUNT + first + e).astype(f32)
        rows_buf[e, there, width:wide] = (high * here[e] + (gate_grad - high) * apart).astype(bf)

    def project(h, e, left, weight_cols):
        rows = pl.ds(h * half, half)
        lo, n = weight_cols
        for c0, cn in columns_of(width):
            rows_buf[e, rows, c0 : c0 + cn] = lax.dot_general(
                left[e, rows, :], weights[e, c0 : c0 + cn, lo : lo + n], (((1,), (1,)), ((), ())), preferred_element_type=f32
            ).astype(bf)

    def combine(target, h, k, cols):
        at = pl.ds(base_of(h, k), NY)
        r = (h * NZ + k) * pair
        for c0, cn in cols:
            parts = [rows_buf[e, r : r + pair, c0 : c0 + cn] for e in range(held)]
            if lanes > held * pair:
                parts.append(jnp.zeros((lanes - held * pair, cn), bf))
            got = jnp.dot(pick[h * NZ + k], jnp.concatenate(parts, axis=0), preferred_element_type=f32)
            target[at, :, c0 : c0 + cn] = got.astype(bf).reshape(NY, count, cn)

    stores = []

    def weight_grad(e, j):
        rows = pl.ds(pl.multiple_of((fsdp ^ j) * quarter, 128), quarter)
        slot = len(stores) % 2
        if len(stores) >= 2:
            stores[-2].wait()
        for c0, cn in columns_of(2 * hidden):
            stage[slot, :, c0 : c0 + cn] = lax.dot_general(
                taken[e, :, rows], grad_act[e, :, c0 : c0 + cn], (((0,), (0,)), ((), ())), preferred_element_type=f32
            ).astype(bf)
        stage[slot, :, 2 * hidden :] = lax.dot_general(
            cot_taken[e, :, rows], scaled[e], (((0,), (0,)), ((), ())), preferred_element_type=f32
        ).astype(bf)
        copy = pltpu.make_async_copy(stage.at[slot], grads[j].at[e], store_sem.at[len(stores)])
        copy.start()
        stores.append(copy)

    work = [functools.partial(cot_chunk, h, k) for h in range(NC) for k in range(NZ)]
    all_cols = columns_of(width) + [(width, 128)]
    ready = {(h, k): 0 for h in range(NC) for k in range(NZ)}
    ready[(0, 0)] = 1
    for k, flips in gather_events(plans[0].order)[1:]:
        for way in ways:
            way.step(k, flips)
        key = (1 if C in flips else 0, k)
        ready[key] += 1
        if ready[key] == NY:
            work.append(functools.partial(dispatch, seen, taken, *key, all_cols))
        for _ in range(min(len(work), 1 if k < NZ - 1 else 2)):
            work.pop(0)()
    for chunk in work:
        chunk()
    for copy in loads:
        copy.wait()
    for h in range(NC):
        for e in range(held):
            hidden_part(h, e)
    for way in ways:
        way.finish()

    far = list(reversed(range(NZ)))
    spare = spare_sem
    in_way = Reduce(place, back, cot_seen, (lvl_b0, lvl_b1), chain_b, send_b, recv_b, spare)
    in_steps = in_way.steps()
    for h in reversed(range(NC)):
        for e in range(held):
            project(h, e, grad_act, (0, 2 * hidden))
        for k in far:
            combine(cot_seen, h, k, all_cols)
            if h == 1:
                in_way.first(k)
    part_copies = []
    work = []

    def out_part(h, k):
        combine(seen, h, k, columns_of(width))
        at = pl.ds(base_of(h, k), NY)
        copy = pltpu.make_async_copy(seen.at[at, :, pl.ds(0, width)], part_out.at[at], part_sem.at[len(part_copies)])
        copy.start()
        part_copies.append(copy)

    for h in range(NC):
        for e in range(held):
            work.append(functools.partial(project, h, e, scaled, (2 * hidden, hidden)))
        for k in range(NZ):
            work.append(functools.partial(out_part, h, k))
    work += [functools.partial(weight_grad, e, j) for j in reversed(range(NX * NC)) for e in range(held)]
    while in_steps or work:
        if in_steps:
            in_steps.pop(0)()
        for _ in range(2):
            if work:
                work.pop(0)()
    in_way.last(gin_out)
    for copy in stores[-2:] + part_copies:
        copy.wait()
    in_way.finish()


def moe(payload, cots, parts, cap, collective_id):
    count, wide = payload.shape
    width = wide - 128
    held, quarter, columns = parts[0].shape
    hidden = columns // 3
    cut = count * 3 // 4
    plans = [
        Plan(0, (Z, Y, C), (C, Z, Y), rows=(0, cut)),
        Plan(0, (Y, Z, C), (C, Z, Y), rows=(cut, count - cut)),
    ]
    back = Plan(0, (C, Y), (C, Z, Y))
    levels, sends, recvs = Reduce.counts(back)
    blocks = NC * NZ * NY
    pair = NY * cap
    rows = blocks // NY * pair
    lanes = tile_up(held * pair, 128)
    bf, f32 = jnp.bfloat16, jnp.float32
    whole = pl.BlockSpec(memory_space=pltpu.VMEM)
    apart = pl.BlockSpec(memory_space=pl.ANY)
    dma = pltpu.SemaphoreType.DMA
    return pl.pallas_call(
        functools.partial(moe_kernel, plans, back, width, hidden, cap),
        out_shape=[
            jax.ShapeDtypeStruct((count, wide), f32),
            jax.ShapeDtypeStruct((blocks, count, width), bf),
        ]
        + [jax.ShapeDtypeStruct((held, quarter, columns), bf)] * (NX * NC),
        in_specs=[whole] + [apart] * 5,
        out_specs=[whole] + [apart] * (1 + NX * NC),
        scratch_shapes=[
            pltpu.VMEM((blocks, count, wide), bf),
            pltpu.VMEM((blocks, count, wide), bf),
            pltpu.VMEM((held, NX * NC * quarter, columns), bf),
            pltpu.VMEM((held, rows, wide), bf),
            pltpu.VMEM((held, rows, width), bf),
            pltpu.VMEM((held, rows, wide), bf),
            pltpu.VMEM((held, rows, hidden), bf),
            pltpu.VMEM((held, rows, 2 * hidden), bf),
            pltpu.VMEM((blocks // NY, NY * count, lanes), bf),
            pltpu.VMEM((2, quarter, columns), bf),
        ]
        + [pltpu.VMEM((n, count, wide), bf) for n in levels + [NZ + 1]]
        + [
            dma((sum(Gather.sends(p) for p in plans),)),
            dma((sum(p.blocks for p in plans),)),
            dma(()),
            dma((sends,)),
            dma((recvs,)),
            dma((held * NX * NC + blocks // NY,)),
            dma((held * NX * NC,)),
            dma((blocks // NY,)),
        ],
        compiler_params=pltpu.CompilerParams(
            collective_id=collective_id, has_side_effects=True, vmem_limit_bytes=67043328
        ),
        name="experts",
    )(payload, cots, *parts)


def weight_view(out, spot, rows):
    return out.at[spot[Z] * NY + spot[Y], :, spot[C], pl.ds(rows[0], rows[1])]


def weights_kernel(plans, *refs):
    left_one, right_one, left_two, right_two, left_small, right_small = refs[:6]
    outs = refs[6:8]
    held_one, held_two = refs[8:10]
    buffers = refs[10:18]
    send_one, recv_one, send_two, recv_two, spare = refs[18:]
    place = Place()
    far = list(reversed(range(NZ)))
    greet(place, (Z, Y, X, C))
    ways = [
        Reduce(place, plans[0], held_one, buffers[0:3], buffers[3], send_one, recv_one, spare),
        Reduce(place, plans[1], held_two, buffers[4:7], buffers[7], send_two, recv_two, spare),
    ]
    group = NY * NX * NC
    rows = group * held_one.shape[1]

    def products(left, right, held, k, shift):
        at = pl.ds(pl.multiple_of(place.order[k] * rows, 128), rows)
        block = left[:, at]
        for c0, cn in columns_of(right.shape[1]):
            got = lax.dot_general(
                block, right[:, c0 : c0 + cn], (((0,), (0,)), ((), ())), preferred_element_type=jnp.float32
            )
            held[pl.ds(place.order[k] * group, group), :, shift + c0 : shift + c0 + cn] = got.astype(
                held.dtype
            ).reshape(group, rows // group, cn)

    for t in range(NZ):
        k = far[t]
        products(left_one, right_one, held_one, k, 0)
        ways[0].first(k)
        products(left_two, right_two, held_two, k, 0)
        products(left_small, right_small, held_two, k, right_two.shape[1])
        ways[1].first(k)
        if t > 0:
            for way in ways:
                for step in way.at_time(t - 1):
                    step()
    for t in range(NZ - 1, NZ + 3):
        for way in ways:
            for step in way.at_time(t):
                step()
    for way, out in zip(ways, outs):
        way.last(out)
    for way in ways:
        way.finish()


def return_weights(lefts, rights, collective_id):
    width = lefts[0].shape[1]
    rows = width // (NZ * NY * NX * NC)
    widths = [rights[0].shape[1], rights[1].shape[1] + rights[2].shape[1]]
    plans = [Plan(0, (C, Y, X), (Z, Y, X, C)), Plan(1, (C, X, Y), (Z, Y, X, C))]
    bf = jnp.bfloat16
    levels, sends, recvs = Reduce.counts(plans[0])
    dma = pltpu.SemaphoreType.DMA
    vmem = pl.BlockSpec(memory_space=pltpu.VMEM)
    return pl.pallas_call(
        functools.partial(weights_kernel, plans),
        out_shape=[jax.ShapeDtypeStruct((rows, w), jnp.float32) for w in widths],
        in_specs=[vmem] * 6,
        out_specs=[vmem] * 2,
        scratch_shapes=[pltpu.VMEM((plans[0].blocks, rows, w), bf) for w in widths]
        + [pltpu.VMEM((n, rows, w), bf) for w in widths for n in levels + [NZ + 1]]
        + [dma((n,)) for n in (sends, recvs, sends, recvs)]
        + [dma(())],
        compiler_params=pltpu.CompilerParams(
            collective_id=collective_id, has_side_effects=True, vmem_limit_bytes=60 * 1024 * 1024
        ),
        name="return_weights",
    )(*[a for pair in zip(lefts, rights) for a in pair])


def place_heads(source, target):
    count = source.shape[0]
    group = QUERY_HEADS // KEY_VALUE_HEADS
    lane = lax.broadcasted_iota(jnp.int32, (1, 2 * HEAD_SIZE), 1)
    for h in range(QUERY_HEADS):
        m, g = h // group, h % group
        block = source[:, h // 2 * 128 : h // 2 * 128 + 128].astype(jnp.float32)
        if h % 2 != m % 2:
            block = pltpu.roll(block, HEAD_SIZE, 1)
        block = jnp.where(lane // HEAD_SIZE == m % 2, block, 0.0)
        target[m, g * count : (g + 1) * count] = block.astype(target.dtype)


def collect_heads(source, target):
    count = target.shape[0]
    group = QUERY_HEADS // KEY_VALUE_HEADS
    lane = lax.broadcasted_iota(jnp.int32, (1, 2 * HEAD_SIZE), 1)
    for pair in range(QUERY_HEADS // 2):
        sides = []
        for h in (2 * pair, 2 * pair + 1):
            m, g = h // group, h % group
            block = source[m, g * count : (g + 1) * count]
            sides.append(block if h % 2 == m % 2 else pltpu.roll(block, HEAD_SIZE, 1))
        target[:, pair * 128 : pair * 128 + 128] = jnp.where(lane < HEAD_SIZE, *sides).astype(target.dtype)


class Scores:
    def __init__(self, place, queries, keys):
        self.queries, self.keys = queries, keys
        group = QUERY_HEADS // KEY_VALUE_HEADS
        count = keys.shape[1]
        self.total = keys.shape[0] * count
        row = lax.broadcasted_iota(jnp.int32, (group * count, 1), 0) % count
        self.position = row + (place.at[Z] * NY + place.at[Y]) * count
        self.column = lax.broadcasted_iota(jnp.int32, (1, self.total), 1)

    def pair(self, m, shift):
        at = pl.ds(pl.multiple_of(shift + m // 2 * 128, 128), 128)
        return self.keys[:, :, at].reshape(self.total, 128)

    def of(self, m, keys):
        found = lax.dot_general(
            self.queries[m], keys, (((1,), (1,)), ((), ())), preferred_element_type=jnp.float32
        )
        return jnp.where(self.column <= self.position, found * attn_scale, masked_logits)


def attend_kernel(plans, own_kv, queries, own_cots, out, log_sums, kv_out, cots, seen, placed, raw, *sems):
    send_kv, recv_kv, send_cot, recv_cot, spare, own_sem = sems
    place = Place()
    bf, f32 = jnp.bfloat16, jnp.float32
    greet(place, (Z, Y, C))
    kv_way = Gather(place, plans[0], own_kv, seen, send_kv, recv_kv, spare, 0, 0)
    cot_ways, at = [], 0
    for n, plan in enumerate(plans[1:]):
        cot_ways.append(Gather(place, plan, own_cots, cots, send_cot, recv_cot, spare, at, n * plan.blocks))
        at += Gather.sends(plan)
    kv_way.step(0, ())
    for way in cot_ways:
        way.step(0, ())
    mine = pltpu.make_async_copy(own_cots, cots.at[flat_index(place.at, plans[1].index)], own_sem.at[0])
    mine.start()
    seen[flat_index(place.at, plans[0].index)] = own_kv[...]
    place_heads(queries, placed)
    log_sums[...] = jnp.zeros(log_sums.shape, f32)
    early = [e for e in gather_events(plans[1].order)[1:]]
    kv_events = gather_events(plans[0].order)[1:]
    for k, flips in kv_events:
        kv_way.step(k, flips)
        if len(early) > 8:
            event = early.pop(0)
            for way in cot_ways:
                way.step(*event)
    keep = pltpu.make_async_copy(seen, kv_out, own_sem.at[1])
    keep.start()
    scores = Scores(place, placed, seen)
    lane = lax.broadcasted_iota(jnp.int32, (1, 128), 1)
    width = KEY_VALUE_HEADS * HEAD_SIZE

    def head(m, carry):
        for i in range(KEY_VALUE_HEADS):
            if early:
                event = early.pop(0)

                @pl.when(m == i)
                def _():
                    for way in cot_ways:
                        way.step(*event)

        s = scores.of(m, scores.pair(m, 0))
        best = jnp.max(s, axis=1, keepdims=True)
        weights = jnp.exp(s - best)
        total = jnp.sum(weights, axis=1, keepdims=True)
        mixed = jnp.dot(weights.astype(bf), scores.pair(m, width), preferred_element_type=f32)
        raw[m] = mixed / total
        log_sums[...] = jnp.where(lane == m, best + jnp.log(total), log_sums[...])
        return carry

    lax.fori_loop(0, KEY_VALUE_HEADS, head, 0)
    collect_heads(raw, out)
    keep.wait()
    mine.wait()
    kv_way.finish()
    for way in cot_ways:
        way.finish()


def attend(own_kv, queries, own_cots, collective_id):
    count, kv_width = own_kv.shape
    cut = count * 3 // 4
    plans = [
        Plan(0, (Z, Y), (Z, Y)),
        Plan(1, (Z, Y, C), (C, Z, Y), rows=(0, cut)),
        Plan(1, (Y, Z, C), (C, Z, Y), rows=(cut, count - cut)),
    ]
    bf, f32 = jnp.bfloat16, jnp.float32
    group = QUERY_HEADS // KEY_VALUE_HEADS
    vmem = pl.BlockSpec(memory_space=pltpu.VMEM)
    apart = pl.BlockSpec(memory_space=pl.ANY)
    dma = pltpu.SemaphoreType.DMA
    kv_shape = (plans[0].blocks, count, kv_width)
    heads = (KEY_VALUE_HEADS, group * count, 2 * HEAD_SIZE)
    return pl.pallas_call(
        functools.partial(attend_kernel, plans),
        out_shape=[
            jax.ShapeDtypeStruct(queries.shape, bf),
            jax.ShapeDtypeStruct((group * count, 128), f32),
            jax.ShapeDtypeStruct(kv_shape, bf),
            jax.ShapeDtypeStruct((plans[1].blocks,) + own_cots.shape, bf),
        ],
        in_specs=[vmem] * 3,
        out_specs=[vmem, vmem, apart, apart],
        scratch_shapes=[pltpu.VMEM(kv_shape, bf), pltpu.VMEM(heads, bf), pltpu.VMEM(heads, f32)]
        + [
            dma((Gather.sends(plans[0]),)),
            dma((plans[0].blocks,)),
            dma((Gather.sends(plans[1]) + Gather.sends(plans[2]),)),
            dma((plans[1].blocks + plans[2].blocks,)),
            dma(()),
            dma((2,)),
        ],
        compiler_params=pltpu.CompilerParams(
            collective_id=collective_id, has_side_effects=True, vmem_limit_bytes=56 * 1024 * 1024
        ),
        name="attend",
    )(own_kv, queries, own_cots)


def attend_back_kernel(plans, *refs):
    queries, grads, outputs, log_sums, keys, part, mixed = refs[:7]
    query_grad, kv_grad, layer_out = refs[7:10]
    placed, grads_placed, raw, deltas, held, held_out = refs[10:16]
    level, chain, out_level, out_level_two, out_chain = refs[16:21]
    send_kv, recv_kv, send_out, recv_out, spare, load_sem = refs[21:]
    place = Place()
    bf, f32 = jnp.bfloat16, jnp.float32
    far = list(reversed(range(NZ)))
    loads = []
    for k in far:
        for h in (1 - place.at[C], place.at[C]):
            at = pl.ds((h * NZ + place.order[k]) * NY, NY)
            loads.append(pltpu.make_async_copy(part.at[at], held_out.at[at], load_sem.at[len(loads)]))
    for copy in loads:
        copy.start()
    greet(place, (Z, Y, C))
    kv_way = Reduce(place, plans[0], held, (level,), chain, send_kv, recv_kv, spare)
    out_way = Reduce(place, plans[1], held_out, (out_level, out_level_two), out_chain, send_out, recv_out, spare)
    for copy in loads:
        copy.wait()
    for k in far:
        out_way.first(k)
    place_heads(queries, placed)
    place_heads(grads, grads_placed)
    count = queries.shape[0]
    group = QUERY_HEADS // KEY_VALUE_HEADS
    lane = lax.broadcasted_iota(jnp.int32, (1, 128), 1)
    for g in range(group):
        found = jnp.zeros((count, 128), f32)
        for m in range(KEY_VALUE_HEADS):
            h = m * group + g
            at = slice(h // 2 * 128, h // 2 * 128 + 128)
            both = grads[:, at].astype(f32) * outputs[:, at].astype(f32)
            delta = jnp.sum(jnp.where(lane // HEAD_SIZE == h % 2, both, 0.0), axis=1, keepdims=True)
            found = jnp.where(lane == m, delta, found)
        deltas[g * count : (g + 1) * count] = found
    scores = Scores(place, placed, keys)
    width = KEY_VALUE_HEADS * HEAD_SIZE
    blocks = keys.shape[0]
    steps = out_way.steps()
    turns = KEY_VALUE_HEADS // 2

    def pair(p, carry):
        for i in range(turns):
            now = [steps.pop(0) for _ in range(min(len(steps), 2))]

            @pl.when(p == i)
            def _():
                for step in now:
                    step()

        key_sum = value_sum = None
        for side in range(2):
            m = 2 * p + side
            k_pair, v_pair = scores.pair(m, 0), scores.pair(m, width)
            of_head = lambda ref: jnp.sum(jnp.where(lane == m, ref[...], 0.0), axis=1, keepdims=True)
            weights = jnp.exp(scores.of(m, k_pair) - of_head(log_sums))
            grad = grads_placed[m]
            grad_probs = lax.dot_general(grad, v_pair, (((1,), (1,)), ((), ())), preferred_element_type=f32)
            grad_scores = (weights * (grad_probs - of_head(deltas))).astype(bf)
            raw[m] = attn_scale * jnp.dot(grad_scores, k_pair, preferred_element_type=f32)
            over_rows = (((0,), (0,)), ((), ()))
            key_part = lax.dot_general(grad_scores, placed[m], over_rows, preferred_element_type=f32)
            value_part = lax.dot_general(weights.astype(bf), grad, over_rows, preferred_element_type=f32)
            key_sum = key_part if key_sum is None else key_sum + key_part
            value_sum = value_part if value_sum is None else value_sum + value_part
        at = pl.multiple_of(p * 128, 128)
        held[:, :, pl.ds(at, 128)] = (attn_scale * key_sum).astype(bf).reshape(blocks, count, 128)
        at = pl.multiple_of(width + p * 128, 128)
        held[:, :, pl.ds(at, 128)] = value_sum.astype(bf).reshape(blocks, count, 128)
        return carry

    lax.fori_loop(0, turns, pair, 0)
    for k in far:
        kv_way.first(k)
    collect_heads(raw, query_grad)
    kv_steps = kv_way.steps()
    while steps or kv_steps:
        for way in (kv_steps, kv_steps, steps):
            if way:
                way.pop(0)()
    kv_way.last(kv_grad)
    out_way.last(layer_out, mixed)
    kv_way.finish()
    out_way.finish()


def attend_back(queries, grads, outputs, log_sums, keys, part, mixed, collective_id):
    count, kv_width = keys.shape[1:]
    plans = [Plan(0, (Y,), (Z, Y)), Plan(1, (C, Y), (C, Z, Y))]
    bf, f32 = jnp.bfloat16, jnp.float32
    group = QUERY_HEADS // KEY_VALUE_HEADS
    vmem = pl.BlockSpec(memory_space=pltpu.VMEM)
    dma = pltpu.SemaphoreType.DMA
    heads = (KEY_VALUE_HEADS, group * count, 2 * HEAD_SIZE)
    levels, sends, recvs = Reduce.counts(plans[0])
    out_levels, out_sends, out_recvs = Reduce.counts(plans[1])
    return pl.pallas_call(
        functools.partial(attend_back_kernel, plans),
        out_shape=[
            jax.ShapeDtypeStruct(queries.shape, f32),
            jax.ShapeDtypeStruct((count, kv_width), f32),
            jax.ShapeDtypeStruct(mixed.shape, bf),
        ],
        in_specs=[vmem] * 5 + [pl.BlockSpec(memory_space=pl.ANY), vmem],
        out_specs=[vmem] * 3,
        scratch_shapes=[
            pltpu.VMEM(heads, bf),
            pltpu.VMEM(heads, bf),
            pltpu.VMEM(heads, f32),
            pltpu.VMEM((group * count, 128), f32),
            pltpu.VMEM(keys.shape, bf),
            pltpu.VMEM(part.shape, bf),
        ]
        + [pltpu.VMEM((n,) + keys.shape[1:], bf) for n in levels + [NZ + 1]]
        + [pltpu.VMEM((n,) + part.shape[1:], bf) for n in out_levels + [NZ + 1]]
        + [dma((n,)) for n in (sends, recvs, out_sends, out_recvs)]
        + [dma(()), dma((NC * NZ,))],
        compiler_params=pltpu.CompilerParams(
            collective_id=collective_id, has_side_effects=True, vmem_limit_bytes=60 * 1024 * 1024
        ),
        name="attend_back",
    )(queries, grads, outputs, log_sums, keys, part, mixed)


def last_kernel(core_ref, own, core_part, x_part, both_part, one, two, *outs):
    core = core_ref[0]
    in_out, out_out = outs[:2]
    split = in_out.shape[3]
    for at, left, right in ((core, own, x_part), (1 - core, core_part, both_part)):
        total = left[0].astype(jnp.float32) + right[0].astype(jnp.float32)
        in_out[at, 0] = total[:, :split]
        out_out[at, 0] = total[:, split:]

    @pl.when(jnp.logical_and(pl.program_id(0) == 0, pl.program_id(1) == 0))
    def _():
        wq, wk, wv, wo, router, first_gain, second_gain = outs[2:]
        q, k = wq.shape[1], wk.shape[1]
        wq[...] = one[:, :q]
        wk[...] = one[:, q : q + k]
        wv[...] = one[:, q + k :]
        width = wo.shape[1]
        wo[...] = two[:, :width]
        small = two[:, width:]
        router[...] = small[:, : router.shape[1]]
        turned = small.T
        at = router.shape[1]
        first_gain[...] = turned[at : at + 1]
        second_gain[...] = turned[at + 1 : at + 2]


def last_outputs(pieces, core, split, one, two, widths):
    held, quarter, columns = pieces[0].shape
    step = quarter // 2
    rows = one.shape[0]
    spec = pl.BlockSpec((1, step, columns), lambda e, r, c: (e, r, 0))
    fixed = lambda a, b: pl.BlockSpec((a, b), lambda e, r, c: (0, 0))
    outs = (split, columns - split)
    shapes = [(rows, w) for w in widths] + [(1, rows)] * 2
    return pl.pallas_call(
        last_kernel,
        grid_spec=pltpu.PrefetchScalarGridSpec(
            num_scalar_prefetch=1,
            grid=(held, 2),
            in_specs=[spec] * 4 + [fixed(*one.shape), fixed(*two.shape)],
            out_specs=[pl.BlockSpec((NC, 1, step, w), lambda e, r, c: (0, e, r, 0)) for w in outs]
            + [fixed(*s) for s in shapes],
        ),
        out_shape=[jax.ShapeDtypeStruct((NC, held, quarter, w), jnp.float32) for w in outs]
        + [jax.ShapeDtypeStruct(s, jnp.float32) for s in shapes],
        name="last_outputs",
    )(core[None], *pieces, one, two)


MODEL_WIDTH = 1536
QUERY_HEADS = 24
KEY_VALUE_HEADS = 8
HEAD_SIZE = 64
EXPERT_HIDDEN = 512
EXPERT_COUNT = 32
TOP = 8
CAP = 40


norm_eps = 1e-06
attn_scale = 0.015625
rope_base = 10000.0
masked_logits = -1e30


def rope_tables(positions):
    half = HEAD_SIZE // 2
    frequency = jnp.power(
        jnp.float32(rope_base), -2.0 * jnp.arange(half, dtype=jnp.float32) / HEAD_SIZE
    )
    angle = positions.astype(jnp.float32)[:, None] * frequency[None, :]
    return (jnp.cos(angle)[:, None, :], jnp.sin(angle)[:, None, :])


def rotate_pairs(value_tensor, cosine_table, sine_table):
    half = value_tensor.shape[-1] // 2
    first = value_tensor[..., :half]
    second = value_tensor[..., half:]
    return jnp.concatenate(
        [first * cosine_table - second * sine_table, second * cosine_table + first * sine_table],
        axis=-1,
    )


def rms_forward(wide, gain):
    inverse = lax.rsqrt(jnp.mean(wide * wide, axis=-1, keepdims=True) + norm_eps)
    unit = wide * inverse
    return (unit, inverse, (unit * gain.astype(jnp.float32)).astype(jnp.bfloat16))


def rms_backward(grad, unit, inverse, gain):
    scaled = grad * gain.astype(jnp.float32)
    back = inverse * (scaled - unit * jnp.mean(scaled * unit, axis=-1, keepdims=True))
    return (back, jnp.sum(grad * unit, axis=0))


def piece_scores(query_rows, key_section, positions):
    token_count = key_section.shape[0]
    key_tensor = key_section.reshape(token_count, KEY_VALUE_HEADS, HEAD_SIZE)
    scores = (
        jnp.einsum("tkgd,nkd->kgtn", query_rows, key_tensor, preferred_element_type=jnp.float32)
        * attn_scale
    )
    visible = jnp.arange(token_count, dtype=jnp.int32)[None, :] <= positions[:, None]
    return (jnp.where(visible, scores, masked_logits), visible, key_tensor)


def local(
    hidden,
    routes,
    attn_norm,
    ffn_norm,
    w_q,
    key_weight,
    value_weight,
    w_o,
    router,
    expert_in,
    expert_out,
    cotangent,
):
    token_rows = hidden.shape[1]
    query_group = QUERY_HEADS // KEY_VALUE_HEADS
    ctx_size = lax.axis_size(CTX)
    sequence_length = token_rows * ctx_size
    positions = lax.axis_index(CTX) * token_rows + jnp.arange(token_rows, dtype=jnp.int32)
    cosine_table, sine_table = rope_tables(positions)
    contract_rows = (((0,), (0,)), ((), ()))
    contract_cols = (((1,), (1,)), ((), ()))
    layer = (
        lax.all_gather(attn_norm, (CTX, FSDP), axis=0, tiled=True),
        lax.all_gather(ffn_norm, (CTX, FSDP), axis=0, tiled=True),
        lax.all_gather(w_q, (CTX, FSDP), axis=0, tiled=True),
        lax.all_gather(key_weight, (CTX, FSDP), axis=0, tiled=True),
        lax.all_gather(value_weight, (CTX, FSDP), axis=0, tiled=True),
        lax.all_gather(w_o, (CTX, FSDP), axis=0, tiled=True),
        lax.all_gather(router, (CTX, FSDP), axis=0, tiled=True),
    )
    attn_gain, ffn_gain, query_w, key_weight_matrix, value_w, output_w, router_w = layer
    experts = (
        lax.all_gather(expert_in, FSDP, axis=1, tiled=True),
        lax.all_gather(expert_out, FSDP, axis=1, tiled=True),
    )
    weight_in, weight_out = experts
    wide = hidden[0].astype(jnp.float32)
    attn_unit, inverse_one, attention_input = rms_forward(wide, attn_gain)
    query_linear = jnp.dot(attention_input, query_w, preferred_element_type=jnp.float32).reshape(
        token_rows, QUERY_HEADS, HEAD_SIZE
    )
    query_rows = (
        rotate_pairs(query_linear, cosine_table, sine_table)
        .astype(jnp.bfloat16)
        .reshape(token_rows, KEY_VALUE_HEADS, query_group, HEAD_SIZE)
    )
    key_linear = jnp.dot(
        attention_input, key_weight_matrix, preferred_element_type=jnp.float32
    ).reshape(token_rows, KEY_VALUE_HEADS, HEAD_SIZE)
    key_matrix_rows = (
        rotate_pairs(key_linear, cosine_table, sine_table)
        .astype(jnp.bfloat16)
        .reshape(token_rows, KEY_VALUE_HEADS * HEAD_SIZE)
    )
    value_rows = jnp.dot(attention_input, value_w, preferred_element_type=jnp.float32).astype(
        jnp.bfloat16
    )
    init_state = (
        jnp.full((KEY_VALUE_HEADS, query_group, token_rows), masked_logits, jnp.float32),
        jnp.zeros((KEY_VALUE_HEADS, query_group, token_rows), jnp.float32),
        jnp.zeros((KEY_VALUE_HEADS, query_group, token_rows, HEAD_SIZE), jnp.float32),
    )
    key_section = lax.all_gather(key_matrix_rows, CTX, axis=0, tiled=True)
    value_section = lax.all_gather(value_rows, CTX, axis=0, tiled=True)

    def compute(current):
        best, total, weighted = current
        scores, visible, _ = piece_scores(query_rows, key_section, positions)
        value_tensor = value_section.reshape(value_section.shape[0], KEY_VALUE_HEADS, HEAD_SIZE)
        new_best = jnp.maximum(best, jnp.max(scores, axis=-1))
        weights = jnp.where(visible, jnp.exp(scores - new_best[..., None]), 0.0)
        total = jnp.sum(weights, axis=-1)
        weighted = jnp.einsum(
            "kgtn,nkd->kgtd",
            weights.astype(jnp.bfloat16),
            value_tensor,
            preferred_element_type=jnp.float32,
        )
        return (new_best, total, weighted)

    best, total, weighted = lax.cond(
        jnp.int32(0) <= positions[-1], compute, lambda current: current, init_state
    )
    log_sum_rows = best + jnp.log(total)
    attention_output = (
        jnp.transpose(weighted / total[..., None], (2, 0, 1, 3))
        .reshape(token_rows, QUERY_HEADS * HEAD_SIZE)
        .astype(jnp.bfloat16)
    )
    mixed = wide + jnp.dot(attention_output, output_w, preferred_element_type=jnp.float32)
    ffn_unit, inverse_two, ffn_in = rms_forward(mixed, ffn_gain)
    logits = jnp.dot(ffn_in, router_w, preferred_element_type=jnp.float32)
    route = routes[0]
    indicator = (route[:, :, None] == jnp.arange(EXPERT_COUNT, dtype=jnp.int32)).astype(jnp.float32)
    chosen = jnp.sum(indicator * logits[:, None, :], axis=-1)
    gates = jax.nn.softmax(chosen, axis=-1)
    flat_route = route.reshape(-1)
    counter = (flat_route[:, None] == jnp.arange(EXPERT_COUNT, dtype=jnp.int32)).astype(jnp.int32)
    slot = jnp.sum(counter * (jnp.cumsum(counter, axis=0) - 1), axis=1)
    target = flat_route * CAP + slot
    owner = (
        jnp.full((EXPERT_COUNT * CAP,), token_rows * TOP, jnp.int32)
        .at[target]
        .set(jnp.arange(token_rows * TOP, dtype=jnp.int32))
    )
    ffn_pad = jnp.concatenate([ffn_in, jnp.zeros((1, MODEL_WIDTH), jnp.bfloat16)], axis=0)
    local_experts = weight_in.shape[0]
    outgoing = ffn_pad[owner // TOP].reshape(ctx_size, local_experts, CAP, MODEL_WIDTH)
    received = lax.all_to_all(outgoing, CTX, split_axis=0, concat_axis=2, tiled=True)[0]
    act = jnp.einsum("erd,edf->erf", received, weight_in, preferred_element_type=jnp.float32)
    gate_part = act[..., :EXPERT_HIDDEN]
    up_part = act[..., EXPERT_HIDDEN:]
    sigma = jax.nn.sigmoid(gate_part)
    inner = (gate_part * sigma * up_part).astype(jnp.bfloat16)
    produced = jnp.einsum(
        "erf,edf->erd", inner, weight_out, preferred_element_type=jnp.float32
    ).astype(jnp.bfloat16)
    returned = lax.all_to_all(
        produced[None], CTX, split_axis=2, concat_axis=0, tiled=True
    ).reshape(EXPERT_COUNT * CAP, MODEL_WIDTH)
    picked = returned[target].reshape(token_rows, TOP, MODEL_WIDTH)
    layer_out = (mixed + jnp.sum(gates[..., None] * picked, axis=1)).astype(jnp.bfloat16)
    cot = cotangent[0]
    layer = (
        lax.all_gather(attn_norm, (CTX, FSDP), axis=0, tiled=True),
        lax.all_gather(ffn_norm, (CTX, FSDP), axis=0, tiled=True),
        lax.all_gather(w_q, (CTX, FSDP), axis=0, tiled=True),
        lax.all_gather(key_weight, (CTX, FSDP), axis=0, tiled=True),
        lax.all_gather(value_weight, (CTX, FSDP), axis=0, tiled=True),
        lax.all_gather(w_o, (CTX, FSDP), axis=0, tiled=True),
        lax.all_gather(router, (CTX, FSDP), axis=0, tiled=True),
    )
    attn_gain, ffn_gain, query_w, key_weight_matrix, value_w, output_w, router_w = layer
    experts = (
        lax.all_gather(expert_in, FSDP, axis=1, tiled=True),
        lax.all_gather(expert_out, FSDP, axis=1, tiled=True),
    )
    weight_in, weight_out = experts
    grad_gate = jnp.sum(cot[:, None, :] * picked, axis=-1)
    slot_grads = (
        (gates[..., None] * cot[:, None, :])
        .astype(jnp.bfloat16)
        .reshape(token_rows * TOP, MODEL_WIDTH)
    )
    slot_pad = jnp.concatenate([slot_grads, jnp.zeros((1, MODEL_WIDTH), jnp.bfloat16)], axis=0)
    grad_outgoing = slot_pad[owner].reshape(ctx_size, local_experts, CAP, MODEL_WIDTH)
    grad_received = lax.all_to_all(grad_outgoing, CTX, split_axis=0, concat_axis=2, tiled=True)[0]
    grad_w_out = jnp.einsum(
        "erd,erf->edf", grad_received, inner, preferred_element_type=jnp.float32
    )
    grad_inner = jnp.einsum(
        "erd,edf->erf", grad_received, weight_out, preferred_element_type=jnp.float32
    )
    grad_act = jnp.concatenate(
        [
            grad_inner * up_part * sigma * (1.0 + gate_part * (1.0 - sigma)),
            grad_inner * gate_part * sigma,
        ],
        axis=-1,
    ).astype(jnp.bfloat16)
    grad_w_in = jnp.einsum("erd,erf->edf", received, grad_act, preferred_element_type=jnp.float32)
    grad_rows = jnp.einsum(
        "erf,edf->erd", grad_act, weight_in, preferred_element_type=jnp.float32
    ).astype(jnp.bfloat16)
    grad_back = lax.all_to_all(
        grad_rows[None], CTX, split_axis=2, concat_axis=0, tiled=True
    ).reshape(EXPERT_COUNT * CAP, MODEL_WIDTH)
    grad_expert_in, grad_expert_out = (
        lax.psum_scatter(
            grad_w_in.astype(jnp.bfloat16), FSDP, scatter_dimension=1, tiled=True
        ).astype(jnp.float32),
        lax.psum_scatter(
            grad_w_out.astype(jnp.bfloat16), FSDP, scatter_dimension=1, tiled=True
        ).astype(jnp.float32),
    )
    grad_chosen = gates * (grad_gate - jnp.sum(gates * grad_gate, axis=-1, keepdims=True))
    grad_logits = jnp.sum(indicator * grad_chosen[..., None], axis=1).astype(jnp.bfloat16)
    grad_router_part = lax.dot_general(
        ffn_in, grad_logits, contract_rows, preferred_element_type=jnp.float32
    )
    grad_ffn_in = lax.dot_general(
        grad_logits, router_w, contract_cols, preferred_element_type=jnp.float32
    )
    grad_ffn_in = grad_ffn_in + jnp.sum(
        grad_back[target].reshape(token_rows, TOP, MODEL_WIDTH), axis=1, dtype=jnp.float32
    )
    back_two, grad_ffn_gain = rms_backward(grad_ffn_in, ffn_unit, inverse_two, ffn_gain)
    grad_mixed = cot + back_two
    grad_attn = grad_mixed.astype(jnp.bfloat16)
    grad_wo_part = lax.dot_general(
        attention_output, grad_attn, contract_rows, preferred_element_type=jnp.float32
    )
    attention_output_gradient = lax.dot_general(
        grad_attn, output_w, contract_cols, preferred_element_type=jnp.float32
    ).astype(jnp.bfloat16)
    head_gradient = attention_output_gradient.reshape(
        token_rows, KEY_VALUE_HEADS, query_group, HEAD_SIZE
    )
    delta_rows = jnp.sum(
        head_gradient.astype(jnp.float32)
        * attention_output.reshape(token_rows, KEY_VALUE_HEADS, query_group, HEAD_SIZE).astype(
            jnp.float32
        ),
        axis=-1,
    )
    delta_rows = jnp.transpose(delta_rows, (1, 2, 0))
    init_back = (
        jnp.zeros((token_rows, KEY_VALUE_HEADS, query_group, HEAD_SIZE), jnp.float32),
        jnp.zeros((sequence_length, 2 * KEY_VALUE_HEADS * HEAD_SIZE), jnp.float32),
    )
    attend_key_section = lax.all_gather(key_matrix_rows, CTX, axis=0, tiled=True)
    attend_value_section = lax.all_gather(value_rows, CTX, axis=0, tiled=True)

    def compute(current):
        token_count = attend_key_section.shape[0]
        scores, visible, key_tensor = piece_scores(query_rows, attend_key_section, positions)
        value_tensor = attend_value_section.reshape(token_count, KEY_VALUE_HEADS, HEAD_SIZE)
        weights_full = jnp.where(visible, jnp.exp(scores - log_sum_rows[..., None]), 0.0)
        grad_probs = jnp.einsum(
            "tkgd,nkd->kgtn", head_gradient, value_tensor, preferred_element_type=jnp.float32
        )
        grad_scores = (weights_full * (grad_probs - delta_rows[..., None])).astype(jnp.bfloat16)
        grad_query = attn_scale * jnp.einsum(
            "kgtn,nkd->tkgd", grad_scores, key_tensor, preferred_element_type=jnp.float32
        )
        key_portion = attn_scale * jnp.einsum(
            "kgtn,tkgd->nkd", grad_scores, query_rows, preferred_element_type=jnp.float32
        )
        value_portion = jnp.einsum(
            "kgtn,tkgd->nkd",
            weights_full.astype(jnp.bfloat16),
            head_gradient,
            preferred_element_type=jnp.float32,
        )
        update = jnp.concatenate(
            [
                key_portion.reshape(token_count, KEY_VALUE_HEADS * HEAD_SIZE),
                value_portion.reshape(token_count, KEY_VALUE_HEADS * HEAD_SIZE),
            ],
            axis=1,
        )
        return (grad_query, update)

    grad_query, grad_keys_full = lax.cond(
        jnp.int32(0) <= positions[-1], compute, lambda current: current, init_back
    )
    local_gradients = lax.psum_scatter(
        grad_keys_full.astype(jnp.bfloat16), CTX, scatter_dimension=0, tiled=True
    ).astype(jnp.float32)
    query_back = (
        rotate_pairs(
            grad_query.reshape(token_rows, QUERY_HEADS, HEAD_SIZE), cosine_table, -sine_table
        )
        .astype(jnp.bfloat16)
        .reshape(token_rows, QUERY_HEADS * HEAD_SIZE)
    )
    key_backward_rows = (
        rotate_pairs(
            local_gradients[:, : KEY_VALUE_HEADS * HEAD_SIZE].reshape(
                token_rows, KEY_VALUE_HEADS, HEAD_SIZE
            ),
            cosine_table,
            -sine_table,
        )
        .astype(jnp.bfloat16)
        .reshape(token_rows, KEY_VALUE_HEADS * HEAD_SIZE)
    )
    value_backward_rows = local_gradients[:, KEY_VALUE_HEADS * HEAD_SIZE :].astype(jnp.bfloat16)
    grad_wq_part = lax.dot_general(
        attention_input, query_back, contract_rows, preferred_element_type=jnp.float32
    )
    grad_wk_part = lax.dot_general(
        attention_input, key_backward_rows, contract_rows, preferred_element_type=jnp.float32
    )
    grad_wv_part = lax.dot_general(
        attention_input, value_backward_rows, contract_rows, preferred_element_type=jnp.float32
    )
    grad_attn_in = lax.dot_general(
        query_back, query_w, contract_cols, preferred_element_type=jnp.float32
    )
    grad_attn_in = grad_attn_in + lax.dot_general(
        key_backward_rows, key_weight_matrix, contract_cols, preferred_element_type=jnp.float32
    )
    grad_attn_in = grad_attn_in + lax.dot_general(
        value_backward_rows, value_w, contract_cols, preferred_element_type=jnp.float32
    )
    back_one, grad_attn_gain = rms_backward(grad_attn_in, attn_unit, inverse_one, attn_gain)
    grad_input = grad_mixed + back_one
    partial_sums = (
        lax.psum_scatter(
            grad_attn_gain.astype(jnp.bfloat16), CTX, scatter_dimension=0, tiled=True
        ).astype(jnp.float32),
        lax.psum_scatter(
            grad_ffn_gain.astype(jnp.bfloat16), CTX, scatter_dimension=0, tiled=True
        ).astype(jnp.float32),
        lax.psum_scatter(
            grad_wq_part.astype(jnp.bfloat16), CTX, scatter_dimension=0, tiled=True
        ).astype(jnp.float32),
        lax.psum_scatter(
            grad_wk_part.astype(jnp.bfloat16), CTX, scatter_dimension=0, tiled=True
        ).astype(jnp.float32),
        lax.psum_scatter(
            grad_wv_part.astype(jnp.bfloat16), CTX, scatter_dimension=0, tiled=True
        ).astype(jnp.float32),
        lax.psum_scatter(
            grad_wo_part.astype(jnp.bfloat16), CTX, scatter_dimension=0, tiled=True
        ).astype(jnp.float32),
        lax.psum_scatter(
            grad_router_part.astype(jnp.bfloat16), CTX, scatter_dimension=0, tiled=True
        ).astype(jnp.float32),
    )
    summed = (
        lax.psum_scatter(
            partial_sums[0].astype(jnp.bfloat16), FSDP, scatter_dimension=0, tiled=True
        ).astype(jnp.float32),
        lax.psum_scatter(
            partial_sums[1].astype(jnp.bfloat16), FSDP, scatter_dimension=0, tiled=True
        ).astype(jnp.float32),
        lax.psum_scatter(
            partial_sums[2].astype(jnp.bfloat16), FSDP, scatter_dimension=0, tiled=True
        ).astype(jnp.float32),
        lax.psum_scatter(
            partial_sums[3].astype(jnp.bfloat16), FSDP, scatter_dimension=0, tiled=True
        ).astype(jnp.float32),
        lax.psum_scatter(
            partial_sums[4].astype(jnp.bfloat16), FSDP, scatter_dimension=0, tiled=True
        ).astype(jnp.float32),
        lax.psum_scatter(
            partial_sums[5].astype(jnp.bfloat16), FSDP, scatter_dimension=0, tiled=True
        ).astype(jnp.float32),
        lax.psum_scatter(
            partial_sums[6].astype(jnp.bfloat16), FSDP, scatter_dimension=0, tiled=True
        ).astype(jnp.float32),
    )
    return (
        layer_out[None],
        grad_input[None],
        summed[0],
        summed[1],
        summed[2],
        summed[3],
        summed[4],
        summed[5],
        summed[6],
        grad_expert_in,
        grad_expert_out,
    )


def swap(a, flip):
    return lax.ppermute(a, FSDP, [(i, i ^ flip) for i in range(NX * NC)])


def fast_body(
    hidden,
    routes,
    attn_norm,
    ffn_norm,
    w_q,
    key_weight,
    value_weight,
    w_o,
    router,
    expert_in,
    expert_out,
    cotangent,
):
    tokens = hidden.shape[1]
    ctx_size = NZ * NY
    ctx = lax.axis_index(CTX)
    fsdp = lax.axis_index(FSDP)
    core = fsdp % NC
    rows = w_q.shape[0]
    quarter = expert_in.shape[1]
    kv_width = KEY_VALUE_HEADS * HEAD_SIZE
    q_width = QUERY_HEADS * HEAD_SIZE
    held = expert_in.shape[0] // NC
    bf = jnp.bfloat16
    f32 = jnp.float32
    positions = ctx * tokens + jnp.arange(tokens, dtype=jnp.int32)
    cosine_table, sine_table = rope_tables(positions)
    contract_cols = (((1,), (1,)), ((), ()))
    wide = hidden[0].astype(f32)
    cot = cotangent[0]

    pack_one = jnp.concatenate([w_q, key_weight, value_weight], axis=1)
    pack_two = jnp.concatenate(
        [w_o, router, attn_norm[:, None], ffn_norm[:, None], jnp.zeros((rows, 94), bf)], axis=1
    )
    route = routes[0]
    indicator = (route[:, :, None] == jnp.arange(EXPERT_COUNT, dtype=jnp.int32)).astype(f32)
    cot_pack = jnp.concatenate(
        [
            cot.astype(bf),
            jnp.sum(indicator, axis=1).astype(bf),
            jnp.zeros((tokens, 128 - EXPERT_COUNT), bf),
        ],
        axis=1,
    )
    experts = jnp.concatenate([expert_in, expert_out], axis=2)
    experts = experts.reshape(NC, held, quarter, experts.shape[2])
    mine = lax.dynamic_index_in_dim(experts, core, 0, False)
    other = lax.dynamic_index_in_dim(experts, 1 - core, 0, False)
    far_one, far_two = swap(pack_one, 2), swap(pack_two, 2)
    far_one, far_two, mine, other = lax.optimization_barrier((far_one, far_two, mine, other))
    parts = [mine, swap(other, 1), swap(mine, 2), swap(other, 3)]
    both = lambda near, far: jnp.where(
        fsdp < NC, jnp.stack([near, far]), jnp.stack([far, near])
    )
    part = rows // 3
    groups = ctx_size, NX, NC, rows
    one, two = gather(
        [both(pack_one, far_one), both(pack_two, far_two)],
        [
            Plan(0, (Z, Y, C), (Z, Y, C), rows=(0, 2 * part), view=weight_view),
            Plan(0, (Y, Z, C), (Z, Y, C), rows=(2 * part, part), view=weight_view),
            Plan(1, (Z, Y, C), (Z, Y, C), rows=(0, rows), view=weight_view),
        ],
        0,
        {0: groups + pack_one.shape[1:], 1: groups + pack_two.shape[1:]},
    )
    one = one.reshape(MODEL_WIDTH, -1)
    two = two.reshape(MODEL_WIDTH, -1)
    output_w = two[:, :MODEL_WIDTH]
    small = two[:, MODEL_WIDTH:]
    router_w = small[:, :EXPERT_COUNT]
    gains = lax.dot_general(
        jnp.eye(128, dtype=bf), small, contract_cols, preferred_element_type=f32
    )
    attn_gain, ffn_gain = gains[EXPERT_COUNT], gains[EXPERT_COUNT + 1]

    attn_unit, inverse_one, attention_input = rms_forward(wide, attn_gain)
    linear = jnp.dot(attention_input, one, preferred_element_type=f32)
    query_rows = (
        rotate_pairs(linear[:, :q_width].reshape(tokens, QUERY_HEADS, HEAD_SIZE), cosine_table, sine_table)
        .astype(bf)
        .reshape(tokens, q_width)
    )
    key_rows = (
        rotate_pairs(
            linear[:, q_width : q_width + kv_width].reshape(tokens, KEY_VALUE_HEADS, HEAD_SIZE),
            cosine_table,
            sine_table,
        )
        .astype(bf)
        .reshape(tokens, kv_width)
    )
    value_rows = linear[:, q_width + kv_width :].astype(bf)
    attention_output, log_sums, kv, cots = attend(
        jnp.concatenate([key_rows, value_rows], axis=1), query_rows, cot_pack, 1
    )
    mixed = wide + jnp.dot(attention_output, output_w, preferred_element_type=f32)
    ffn_unit, inverse_two, ffn_in = rms_forward(mixed, ffn_gain)
    logits = jnp.dot(ffn_in, router_w, preferred_element_type=f32)
    chosen = jnp.sum(indicator * logits[:, None, :], axis=-1)
    gates = jax.nn.softmax(chosen, axis=-1)
    gate_map = jnp.sum(indicator * gates[..., None], axis=1)
    payload = jnp.concatenate(
        [ffn_in, gate_map.astype(bf), jnp.zeros((tokens, 128 - EXPERT_COUNT), bf)], axis=1
    )
    gin, moe_part, *pieces = moe(payload, cots, parts, CAP, 2)
    across = [swap(pieces[j], j) for j in range(1, NX * NC)]
    grad_gate_map = gin[:, MODEL_WIDTH : MODEL_WIDTH + EXPERT_COUNT] + gin[
        :, MODEL_WIDTH + EXPERT_COUNT : MODEL_WIDTH + 2 * EXPERT_COUNT
    ]
    grad_gate = jnp.sum(indicator * grad_gate_map[:, None, :], axis=-1)
    grad_chosen = gates * (grad_gate - jnp.sum(gates * grad_gate, axis=-1, keepdims=True))
    grad_logits = jnp.sum(indicator * grad_chosen[..., None], axis=1).astype(bf)
    grad_ffn_in = gin[:, :MODEL_WIDTH] + lax.dot_general(
        grad_logits, router_w, contract_cols, preferred_element_type=f32
    )
    back_two, _ = rms_backward(grad_ffn_in, ffn_unit, inverse_two, ffn_gain)
    grad_mixed = cot + back_two
    grad_attn = grad_mixed.astype(bf)
    attention_output_gradient = lax.dot_general(
        grad_attn, output_w, contract_cols, preferred_element_type=f32
    ).astype(bf)
    grad_query, local_gradients, layer_out = attend_back(
        query_rows, attention_output_gradient, attention_output, log_sums, kv, moe_part, mixed, 4
    )
    query_back = (
        rotate_pairs(
            grad_query.reshape(tokens, QUERY_HEADS, HEAD_SIZE), cosine_table, -sine_table
        )
        .astype(bf)
        .reshape(tokens, q_width)
    )
    key_back = (
        rotate_pairs(
            local_gradients[:, :kv_width].reshape(tokens, KEY_VALUE_HEADS, HEAD_SIZE),
            cosine_table,
            -sine_table,
        )
        .astype(bf)
        .reshape(tokens, kv_width)
    )
    back = jnp.concatenate([query_back, key_back, local_gradients[:, kv_width:].astype(bf)], axis=1)
    grad_attn_in = lax.dot_general(back, one, contract_cols, preferred_element_type=f32)
    back_one, _ = rms_backward(grad_attn_in, attn_unit, inverse_one, attn_gain)
    grad_input = grad_mixed + back_one
    halves = []
    for factor in (grad_attn_in * attn_unit, grad_ffn_in * ffn_unit):
        high = factor.astype(bf)
        halves += [high, (factor - high.astype(f32)).astype(bf)]
    column = lambda n: jnp.broadcast_to((jnp.arange(128) == n).astype(bf), (tokens, 128))
    sum_one, sum_two = return_weights(
        [attention_input, attention_output, jnp.concatenate([ffn_in] + halves)],
        [
            back,
            grad_attn,
            jnp.concatenate(
                [
                    jnp.concatenate([grad_logits, jnp.zeros((tokens, 128 - EXPERT_COUNT), bf)], axis=1),
                    column(EXPERT_COUNT),
                    column(EXPERT_COUNT),
                    column(EXPERT_COUNT + 1),
                    column(EXPERT_COUNT + 1),
                ]
            ),
        ],
        5,
    )
    grad_expert_in, grad_expert_out, *rest, first_gain, second_gain = last_outputs(
        [pieces[0]] + across,
        core,
        2 * EXPERT_HIDDEN,
        sum_one,
        sum_two,
        (q_width, kv_width, kv_width, MODEL_WIDTH, EXPERT_COUNT),
    )
    return (
        layer_out[None],
        grad_input[None],
        first_gain.reshape(rows),
        second_gain.reshape(rows),
        *rest,
        grad_expert_in.reshape(NC * held, quarter, -1),
        grad_expert_out.reshape(NC * held, quarter, -1),
    )


def fast(*args):
    return fast_body(*args)


def solution(mesh):
    placed = (
        P(FSDP, CTX, None),
        P(FSDP, CTX, None),
        P((CTX, FSDP)),
        P((CTX, FSDP)),
        P((CTX, FSDP), None),
        P((CTX, FSDP), None),
        P((CTX, FSDP), None),
        P((CTX, FSDP), None),
        P((CTX, FSDP), None),
        P(CTX, FSDP, None),
        P(CTX, FSDP, None),
        P(FSDP, CTX, None),
    )
    small = mesh.shape[CTX] == NZ * NY and mesh.shape[FSDP] == NX * NC
    return jax.shard_map(
        fast if small else local,
        mesh=mesh,
        in_specs=placed,
        out_specs=(
            P(FSDP, CTX, None),
            P(FSDP, CTX, None),
            P((CTX, FSDP)),
            P((CTX, FSDP)),
            P((CTX, FSDP), None),
            P((CTX, FSDP), None),
            P((CTX, FSDP), None),
            P((CTX, FSDP), None),
            P((CTX, FSDP), None),
            P(CTX, FSDP, None),
            P(CTX, FSDP, None),
        ),
        check_vma=False,
    )
```

```python
import functools
import itertools

import jax
import jax.numpy as jnp
from jax import lax
from jax.experimental import pallas as pl
from jax.experimental.pallas import tpu as pltpu
from jax.sharding import PartitionSpec as P


NY = 2
NZ = 4
NX = 2
NC = 2
DEV = pl.DeviceIdType.MESH
CTX, FSDP = "ctx", "fsdp"
Z, Y, X, C = 0, 1, 2, 3
SIZES = {Z: NZ, Y: NY, X: NX, C: NC}
UP, DOWN = 4, 5


class Plan:
    def __init__(self, ref, order, index, rows=None, view=None):
        self.ref, self.order, self.index, self.rows, self.view = ref, order, index, rows, view
        self.blocks = 1
        for d in index:
            self.blocks *= SIZES[d]


class Place:
    def __init__(self):
        ctx = lax.axis_index(CTX)
        fsdp = lax.axis_index(FSDP)
        self.at = {Z: ctx // NY, Y: ctx % NY, X: fsdp // NC, C: fsdp % NC}
        z = self.at[Z]
        low = z < NZ // 2
        base = jnp.where(low, z, NZ - 1 - z)
        near = [base, 1 - base, jnp.int32(2), jnp.int32(3)]
        self.order = [z] + [jnp.where(low, k, NZ - 1 - k) for k in near[1:]]

    def device(self, dim, value):
        spot = dict(self.at)
        spot[dim] = value
        return (spot[Z] * NY + spot[Y], spot[X] * NC + spot[C])

    def across(self, dim):
        return self.device(dim, 1 - self.at[dim])

    def along(self, step):
        return self.device(Z, self.at[Z] + step)

    def coords(self, z_from, flips):
        spot = {d: (1 - self.at[d] if d in flips else self.at[d]) for d in (Y, X, C)}
        spot[Z] = z_from
        return spot


def flat_index(spot, dims):
    index = 0
    for d in dims:
        index = index * SIZES[d] + spot[d]
    return index


def subsets(dims):
    return [c for n in range(len(dims) + 1) for c in itertools.combinations(dims, n)]


def greet(place, dims):
    barrier = pltpu.get_barrier_semaphore()
    z = place.at[Z]
    count = jnp.int32(0)
    for d in dims:
        if d == Z:
            @pl.when(z > 0)
            def _():
                pl.semaphore_signal(barrier, inc=1, device_id=place.along(-1), device_id_type=DEV)

            @pl.when(z < NZ - 1)
            def _():
                pl.semaphore_signal(barrier, inc=1, device_id=place.along(1), device_id_type=DEV)

            count = count + jnp.where(z > 0, 1, 0) + jnp.where(z < NZ - 1, 1, 0)
        else:
            pl.semaphore_signal(barrier, inc=1, device_id=place.across(d), device_id_type=DEV)
            count = count + 1
    pl.semaphore_wait(barrier, count)


def gather_events(order):
    pairs = [d for d in order if d != Z]
    events = [(k, f) for k in range(NZ) for f in subsets(pairs)]
    return sorted(events, key=lambda e: (e[0] + len(e[1]), len(e[1])))


def gather_sends(order, k, flips):
    z_at = order.index(Z)
    last = max([order.index(d) for d in flips] + ([z_at] if k > 0 else []) + [-1])
    out = []
    for position, d in enumerate(order):
        if position > last:
            out.extend([UP, DOWN] if d == Z else [d])
    if k > 0 and last == z_at:
        out.extend([UP, DOWN])
    return out


def gather_kernel(plans, n_in, *refs):
    ins, outs = refs[:n_in], refs[n_in : 2 * n_in]
    send_sem, recv_sem, own_sem = refs[2 * n_in :]
    place = Place()
    z = place.at[Z]
    greet(place, sorted({d for p in plans for d in p.order}))
    pending = []
    slot = 0
    queue = []
    for n, plan in enumerate(plans):
        for rank, event in enumerate(gather_events(plan.order)):
            queue.append((rank / len(gather_events(plan.order)), n, event))
    queue.sort(key=lambda q: (q[0], q[1]))
    bases = [sum(p.blocks for p in plans[:n]) for n in range(len(plans))]
    for _, n, (k, flips) in queue:
        plan = plans[n]
        src = ins[plan.ref]
        out = outs[plan.ref]
        rows = plan.rows
        z_from = place.order[k]
        spot = place.coords(z_from, flips)
        index = flat_index(spot, plan.index)
        own = k == 0 and not flips
        if plan.view is not None:
            target = plan.view(out, spot, rows)
            source = src.at[:, pl.ds(rows[0], rows[1])] if own else target
        else:
            target = out.at[index] if rows is None else out.at[index, pl.ds(rows[0], rows[1])]
            source = (src if rows is None else src.at[pl.ds(rows[0], rows[1])]) if own else target
        sem = recv_sem.at[bases[n] + index]
        if not own:
            pltpu.make_async_remote_copy(
                src_ref=target, dst_ref=target, send_sem=own_sem.at[0], recv_sem=sem,
                device_id=place.across(C), device_id_type=DEV,
            ).wait_recv()
        for way in gather_sends(plan.order, k, flips):
            if way in (UP, DOWN):
                step = 1 if way == UP else -1
                go = z < NZ - 1 if way == UP else z > 0
                if k > 0:
                    go = jnp.logical_and(go, z_from < z if way == UP else z_from > z)
                dest = place.device(Z, jnp.clip(z + step, 0, NZ - 1))
            else:
                go, dest = None, place.across(way)
            copy = pltpu.make_async_remote_copy(
                src_ref=source, dst_ref=target, send_sem=send_sem.at[slot], recv_sem=sem,
                device_id=dest, device_id_type=DEV,
            )
            slot += 1
            if go is None:
                copy.start()
            else:
                pl.when(go)(copy.start)
            pending.append((go, copy.wait_send))
        if own:
            copy = pltpu.make_async_copy(source, target, own_sem.at[1 + n])
            copy.start()
            pending.append((None, copy.wait))
    for go, wait in pending:
        if go is None:
            wait()
        else:
            pl.when(go)(wait)


def gather(arrays, plans, collective_id, shapes=None):
    n = len(arrays)
    sends = sum(len(gather_sends(p.order, k, f)) for p in plans for k, f in gather_events(p.order))
    blocks = {p.ref: p.blocks for p in plans}
    return pl.pallas_call(
        functools.partial(gather_kernel, plans, n),
        out_shape=[
            jax.ShapeDtypeStruct((shapes or {}).get(i, (blocks[i],) + a.shape), a.dtype)
            for i, a in enumerate(arrays)
        ],
        in_specs=[pl.BlockSpec(memory_space=pltpu.VMEM)] * n,
        out_specs=[pl.BlockSpec(memory_space=pl.ANY)] * n,
        scratch_shapes=[
            pltpu.SemaphoreType.DMA((sends,)),
            pltpu.SemaphoreType.DMA((sum(p.blocks for p in plans),)),
            pltpu.SemaphoreType.DMA((1 + len(plans),)),
        ],
        compiler_params=pltpu.CompilerParams(collective_id=collective_id, has_side_effects=True),
    )(*arrays)


def add_into(acc, other):
    acc[...] = (acc[...].astype(jnp.float32) + other[...].astype(jnp.float32)).astype(acc.dtype)


class Gather:
    def __init__(self, place, plan, src, out, send_sem, recv_sem, spare_sem, slot, base):
        self.place, self.plan, self.src, self.out = place, plan, src, out
        self.send_sem, self.recv_sem, self.spare_sem = send_sem, recv_sem, spare_sem
        self.slot, self.base = slot, base
        self.pending = []

    @staticmethod
    def sends(plan):
        return sum(len(gather_sends(plan.order, k, f)) for k, f in gather_events(plan.order))

    def goes(self, way, k):
        z, z_from = self.place.at[Z], self.place.order[k]
        if way == UP:
            return z < NZ - 1 if k == 0 else jnp.logical_and(z < NZ - 1, z_from < z)
        return z > 0 if k == 0 else jnp.logical_and(z > 0, z_from > z)

    def part(self, ref):
        rows = self.plan.rows
        return ref if rows is None else ref.at[pl.ds(rows[0], rows[1])]

    def step(self, k, flips):
        place, plan = self.place, self.plan
        index = flat_index(place.coords(place.order[k], flips), plan.index)
        target = self.part(self.out.at[index])
        sem = self.recv_sem.at[self.base + index]
        source = target
        if k == 0 and not flips:
            source = self.part(self.src)
        else:
            pltpu.make_async_remote_copy(
                src_ref=target, dst_ref=target, send_sem=self.spare_sem, recv_sem=sem,
                device_id=place.across(C), device_id_type=DEV,
            ).wait_recv()
        for way in gather_sends(plan.order, k, flips):
            if way in (UP, DOWN):
                dest = place.device(Z, jnp.clip(place.at[Z] + (1 if way == UP else -1), 0, NZ - 1))
            else:
                dest = place.across(way)
            copy = pltpu.make_async_remote_copy(
                src_ref=source, dst_ref=target, send_sem=self.send_sem.at[self.slot], recv_sem=sem,
                device_id=dest, device_id_type=DEV,
            )
            if way in (UP, DOWN):
                pl.when(self.goes(way, k))(copy.start)
            else:
                copy.start()
            self.pending.append((way, k, self.slot))
            self.slot += 1

    def finish(self):
        for way, k, slot in self.pending:
            block = self.part(self.src)
            copy = pltpu.make_async_remote_copy(
                src_ref=block, dst_ref=block, send_sem=self.send_sem.at[slot], recv_sem=self.spare_sem,
                device_id=self.place.across(C), device_id_type=DEV,
            )
            if way in (UP, DOWN):
                pl.when(self.goes(way, k))(copy.wait_send)
            else:
                copy.wait_send()


class Reduce:
    def __init__(self, place, plan, held, levels, chain, send_sem, recv_sem, spare_sem):
        self.place, self.plan, self.held, self.levels, self.chain = place, plan, held, levels, chain
        self.send_sem, self.recv_sem, self.spare_sem = send_sem, recv_sem, spare_sem
        dims = plan.order
        self.kept = [subsets(dims[p + 1 :]) for p in range(len(dims))]
        self.base = [NZ * sum(len(f) for f in self.kept[:p]) for p in range(len(dims) + 1)]
        self.slot = 0

    @staticmethod
    def counts(plan):
        kept = [NZ * len(subsets(plan.order[p + 1 :])) for p in range(len(plan.order))]
        return kept, sum(kept) + NZ - 1, sum(kept) + NZ + 1

    def push(self, source, target, sem, dest):
        copy = pltpu.make_async_remote_copy(
            src_ref=source, dst_ref=target, send_sem=self.send_sem.at[self.slot], recv_sem=sem,
            device_id=dest, device_id_type=DEV,
        )
        self.slot += 1
        copy.start()

    def arrived(self, target, sem):
        pltpu.make_async_remote_copy(
            src_ref=target, dst_ref=target, send_sem=self.spare_sem, recv_sem=sem,
            device_id=self.place.across(C), device_id_type=DEV,
        ).wait_recv()

    def block(self, k, flips):
        return flat_index(self.place.coords(self.place.order[k], flips), self.plan.index)

    def first(self, k):
        dim = self.plan.order[0]
        for n, f in enumerate(self.kept[0]):
            spot = self.place.order[k] * len(self.kept[0]) + n
            self.push(
                self.held.at[self.block(k, (dim,) + f)], self.levels[0].at[spot],
                self.recv_sem.at[spot], self.place.across(dim),
            )

    def level(self, p, k):
        dims = self.plan.order
        z_to = self.place.order[k]
        for f in sorted(self.kept[p], key=lambda f: -len(f)):
            spot = z_to * len(self.kept[p]) + self.kept[p].index(f)
            mine = self.held.at[self.block(k, f)]
            self.arrived(self.levels[p].at[spot], self.recv_sem.at[self.base[p] + spot])
            add_into(mine, self.levels[p].at[spot])
            later = p + 1
            if later < len(dims) and dims[later] in f:
                left = tuple(d for d in f if d != dims[later])
                there = z_to * len(self.kept[later]) + self.kept[later].index(left)
                self.push(
                    mine, self.levels[later].at[there],
                    self.recv_sem.at[self.base[later] + there], self.place.across(dims[later]),
                )

    def along(self, k):
        z = self.place.at[Z]
        dest = self.place.order[k]
        up = dest > z
        spot = dest + jnp.where(up, 1, 0)
        mine = self.held.at[self.block(k, ())]
        sem = self.recv_sem.at[self.base[-1] + spot]

        @pl.when(jnp.where(up, z > 0, z < NZ - 1))
        def _():
            self.arrived(self.chain.at[spot], sem)
            add_into(mine, self.chain.at[spot])

        self.push(mine, self.chain.at[spot], sem, self.place.along(jnp.where(up, 1, -1)))

    def last(self, out, base=None):
        z = self.place.at[Z]
        mine = self.held.at[self.block(0, ())]
        for go, spot in ((z > 0, z + 1), (z < NZ - 1, z)):

            @pl.when(go)
            def _():
                self.arrived(self.chain.at[spot], self.recv_sem.at[self.base[-1] + spot])
                add_into(mine, self.chain.at[spot])

        total = mine[...].astype(jnp.float32)
        if base is not None:
            total = base[...] + total
        out[...] = total.astype(out.dtype)

    def at_time(self, t):
        depth = len(self.plan.order)
        far = list(reversed(range(NZ)))
        out = [functools.partial(self.level, p, far[t - p]) for p in range(depth) if 0 <= t - p < NZ]
        if 0 <= t - depth < NZ - 1:
            out.append(functools.partial(self.along, far[t - depth]))
        return out

    def steps(self):
        return [step for t in range(NZ + len(self.plan.order)) for step in self.at_time(t)]

    def finish(self):
        block = self.levels[0].at[0]
        for slot in range(self.slot):
            pltpu.make_async_remote_copy(
                src_ref=block, dst_ref=block, send_sem=self.send_sem.at[slot], recv_sem=self.spare_sem,
                device_id=self.place.across(C), device_id_type=DEV,
            ).wait_send()


def tile_up(n, m):
    return (n + m - 1) // m * m


def columns_of(width, chunk=512):
    return [(i, min(chunk, width - i)) for i in range(0, width, chunk)]


def moe_kernel(plans, back, width, hidden, cap, *refs):
    payload, cots, w_own, w_core, w_x, w_both = refs[:6]
    gin_out, part_out = refs[6:8]
    grads = refs[8:12]
    (
        seen, cot_seen, weights, taken, cot_taken, rows_buf, scaled, grad_act, pick, stage,
        lvl_b0, lvl_b1, chain_b,
        send_sem, recv_sem, spare_sem, send_b, recv_b, load_sem, store_sem, part_sem,
    ) = refs[12:]
    bf, f32 = jnp.bfloat16, jnp.float32
    place = Place()
    count = payload.shape[0]
    pair = 2 * cap
    wide = width + 128
    quarter = width // (NX * NC)
    half = NZ * pair
    lanes = pick.shape[2]
    held = weights.shape[0]
    fsdp = place.at[X] * NC + place.at[C]
    first = (((place.at[Z] * NY + place.at[Y]) * NC) + place.at[C]) * held

    loads = []
    for j, ref in enumerate((w_own, w_core, w_x, w_both)):
        rows = pl.ds(pl.multiple_of((fsdp ^ j) * quarter, quarter), quarter)
        for e in range(held):
            loads.append(pltpu.make_async_copy(ref.at[e], weights.at[e, rows], load_sem.at[len(loads)]))
    base_of = lambda h, k: (jnp.where(h == 0, place.at[C], 1 - place.at[C]) * NZ + place.order[k]) * NY
    cot_loads = {}
    for k in range(NZ):
        for h in range(2):
            at = pl.ds(base_of(h, k), NY)
            cot_loads[(h, k)] = pltpu.make_async_copy(cots.at[at], cot_seen.at[at], load_sem.at[len(loads) + len(cot_loads)])

    greet(place, (Z, Y, C))
    ways = []
    send_at = 0
    for n, plan in enumerate(plans):
        ways.append(Gather(place, plan, payload, seen, send_sem, recv_sem, spare_sem, send_at, n * plan.blocks))
        send_at += Gather.sends(plan)
    for way in ways:
        way.step(0, ())
    for key in cot_loads:
        cot_loads[key].start()
    for copy in loads:
        copy.start()
    seen[flat_index(place.at, plans[0].index)] = payload[...]

    row_id = lax.broadcasted_iota(jnp.int32, (NY * count, NY * count), 0)
    col_id = lax.broadcasted_iota(jnp.int32, (NY * count, NY * count), 1)
    earlier = jnp.logical_and(col_id < row_id, col_id // count == row_id // count).astype(bf)
    lane_id = lax.broadcasted_iota(jnp.int32, (1, 128), 1)
    here = [(lane_id == first + e).astype(f32) for e in range(held)]
    pick_lane = lax.broadcasted_iota(jnp.int32, (NY * count, lanes), 1).astype(f32)
    y_shift = (lax.broadcasted_iota(jnp.int32, (NY * count, 1), 0) // count * cap).astype(f32)

    def dispatch(source, target, h, k, cols):
        at = pl.ds(base_of(h, k), NY)
        r = (h * NZ + k) * pair
        for c0, cn in cols:
            block = source[at, :, c0 : c0 + cn].reshape(NY * count, cn)
            got = lax.dot_general(
                pick[h * NZ + k], block, (((0,), (0,)), ((), ())), preferred_element_type=f32
            ).astype(bf)
            for e in range(held):
                target[e, r : r + pair, c0 : c0 + cn] = got[e * pair : (e + 1) * pair]

    def cot_chunk(h, k):
        cot_loads[(h, k)].wait()
        at = pl.ds(base_of(h, k), NY)
        chosen = cot_seen[at, :, width:wide].reshape(NY * count, 128)
        before = jnp.dot(earlier, chosen, preferred_element_type=f32)
        picked = None
        for e in range(held):
            is_here = jnp.sum(chosen.astype(f32) * here[e], axis=1, keepdims=True)
            slot = jnp.sum(before * here[e], axis=1, keepdims=True) + y_shift + e * pair
            target = jnp.where(is_here > 0.5, slot, -1.0)
            hit = pick_lane == target
            picked = hit if picked is None else jnp.logical_or(picked, hit)
        pick[h * NZ + k] = picked.astype(f32).astype(bf)
        dispatch(cot_seen, cot_taken, h, k, columns_of(width))

    def hidden_chunk(h, e, n, tile):
        rows = pl.ds(h * half, half)
        tokens_in = taken[e, rows, :width]
        gate = jnp.sum(taken[e, rows, width:wide].astype(f32) * here[e], axis=1, keepdims=True)
        col = n * tile
        g = jnp.dot(tokens_in, weights[e, :, col : col + tile], preferred_element_type=f32)
        u = jnp.dot(tokens_in, weights[e, :, hidden + col : hidden + col + tile], preferred_element_type=f32)
        raw = jnp.dot(
            cot_taken[e, rows, :], weights[e, :, 2 * hidden + col : 2 * hidden + col + tile], preferred_element_type=f32
        )
        s = jax.nn.sigmoid(g)
        gs = g * s
        inner = gs * u
        scaled[e, rows, col : col + tile] = (inner * gate).astype(bf)
        grad_inner = raw * gate
        grad_act[e, rows, col : col + tile] = (grad_inner * u * s * (1.0 + g * (1.0 - s))).astype(bf)
        grad_act[e, rows, hidden + col : hidden + col + tile] = (grad_inner * gs).astype(bf)
        return jnp.sum(raw * inner, axis=1, keepdims=True)

    def hidden_part(h, e):
        tile = min(256, hidden)
        gate_grad = sum(hidden_chunk(h, e, n, tile) for n in range(hidden // tile))
        high = gate_grad.astype(bf).astype(f32)
        there = pl.ds(h * half, half)
        apart = (lane_id == EXPERT_COUNT + first + e).astype(f32)
        rows_buf[e, there, width:wide] = (high * here[e] + (gate_grad - high) * apart).astype(bf)

    def project(h, e, left, weight_cols):
        rows = pl.ds(h * half, half)
        lo, n = weight_cols
        for c0, cn in columns_of(width):
            rows_buf[e, rows, c0 : c0 + cn] = lax.dot_general(
                left[e, rows, :], weights[e, c0 : c0 + cn, lo : lo + n], (((1,), (1,)), ((), ())), preferred_element_type=f32
            ).astype(bf)

    def combine(target, h, k, cols):
        at = pl.ds(base_of(h, k), NY)
        r = (h * NZ + k) * pair
        for c0, cn in cols:
            parts = [rows_buf[e, r : r + pair, c0 : c0 + cn] for e in range(held)]
            if lanes > held * pair:
                parts.append(jnp.zeros((lanes - held * pair, cn), bf))
            got = jnp.dot(pick[h * NZ + k], jnp.concatenate(parts, axis=0), preferred_element_type=f32)
            target[at, :, c0 : c0 + cn] = got.astype(bf).reshape(NY, count, cn)

    stores = []

    def weight_grad(e, j):
        rows = pl.ds(pl.multiple_of((fsdp ^ j) * quarter, 128), quarter)
        slot = len(stores) % 2
        if len(stores) >= 2:
            stores[-2].wait()
        for c0, cn in columns_of(2 * hidden):
            stage[slot, :, c0 : c0 + cn] = lax.dot_general(
                taken[e, :, rows], grad_act[e, :, c0 : c0 + cn], (((0,), (0,)), ((), ())), preferred_element_type=f32
            ).astype(bf)
        stage[slot, :, 2 * hidden :] = lax.dot_general(
            cot_taken[e, :, rows], scaled[e], (((0,), (0,)), ((), ())), preferred_element_type=f32
        ).astype(bf)
        copy = pltpu.make_async_copy(stage.at[slot], grads[j].at[e], store_sem.at[len(stores)])
        copy.start()
        stores.append(copy)

    work = [functools.partial(cot_chunk, h, k) for h in range(NC) for k in range(NZ)]
    all_cols = columns_of(width) + [(width, 128)]
    ready = {(h, k): 0 for h in range(NC) for k in range(NZ)}
    ready[(0, 0)] = 1
    for k, flips in gather_events(plans[0].order)[1:]:
        for way in ways:
            way.step(k, flips)
        key = (1 if C in flips else 0, k)
        ready[key] += 1
        if ready[key] == NY:
            work.append(functools.partial(dispatch, seen, taken, *key, all_cols))
        for _ in range(min(len(work), 1 if k < NZ - 1 else 2)):
            work.pop(0)()
    for chunk in work:
        chunk()
    for copy in loads:
        copy.wait()
    for h in range(NC):
        for e in range(held):
            hidden_part(h, e)
    for way in ways:
        way.finish()

    far = list(reversed(range(NZ)))
    spare = spare_sem
    in_way = Reduce(place, back, cot_seen, (lvl_b0, lvl_b1), chain_b, send_b, recv_b, spare)
    in_steps = in_way.steps()
    for h in reversed(range(NC)):
        for e in range(held):
            project(h, e, grad_act, (0, 2 * hidden))
        for k in far:
            combine(cot_seen, h, k, all_cols)
            if h == 1:
                in_way.first(k)
    part_copies = []
    work = []

    def out_part(h, k):
        combine(seen, h, k, columns_of(width))
        at = pl.ds(base_of(h, k), NY)
        copy = pltpu.make_async_copy(seen.at[at, :, pl.ds(0, width)], part_out.at[at], part_sem.at[len(part_copies)])
        copy.start()
        part_copies.append(copy)

    for h in range(NC):
        for e in range(held):
            work.append(functools.partial(project, h, e, scaled, (2 * hidden, hidden)))
        for k in range(NZ):
            work.append(functools.partial(out_part, h, k))
    work += [functools.partial(weight_grad, e, j) for j in reversed(range(NX * NC)) for e in range(held)]
    while in_steps or work:
        if in_steps:
            in_steps.pop(0)()
        for _ in range(2):
            if work:
                work.pop(0)()
    in_way.last(gin_out)
    for copy in stores[-2:] + part_copies:
        copy.wait()
    in_way.finish()


def moe(payload, cots, parts, cap, collective_id):
    count, wide = payload.shape
    width = wide - 128
    held, quarter, columns = parts[0].shape
    hidden = columns // 3
    cut = count * 3 // 4
    plans = [
        Plan(0, (Z, Y, C), (C, Z, Y), rows=(0, cut)),
        Plan(0, (Y, Z, C), (C, Z, Y), rows=(cut, count - cut)),
    ]
    back = Plan(0, (C, Y), (C, Z, Y))
    levels, sends, recvs = Reduce.counts(back)
    blocks = NC * NZ * NY
    pair = NY * cap
    rows = blocks // NY * pair
    lanes = tile_up(held * pair, 128)
    bf, f32 = jnp.bfloat16, jnp.float32
    whole = pl.BlockSpec(memory_space=pltpu.VMEM)
    apart = pl.BlockSpec(memory_space=pl.ANY)
    dma = pltpu.SemaphoreType.DMA
    return pl.pallas_call(
        functools.partial(moe_kernel, plans, back, width, hidden, cap),
        out_shape=[
            jax.ShapeDtypeStruct((count, wide), f32),
            jax.ShapeDtypeStruct((blocks, count, width), bf),
        ]
        + [jax.ShapeDtypeStruct((held, quarter, columns), bf)] * (NX * NC),
        in_specs=[whole] + [apart] * 5,
        out_specs=[whole] + [apart] * (1 + NX * NC),
        scratch_shapes=[
            pltpu.VMEM((blocks, count, wide), bf),
            pltpu.VMEM((blocks, count, wide), bf),
            pltpu.VMEM((held, NX * NC * quarter, columns), bf),
            pltpu.VMEM((held, rows, wide), bf),
            pltpu.VMEM((held, rows, width), bf),
            pltpu.VMEM((held, rows, wide), bf),
            pltpu.VMEM((held, rows, hidden), bf),
            pltpu.VMEM((held, rows, 2 * hidden), bf),
            pltpu.VMEM((blocks // NY, NY * count, lanes), bf),
            pltpu.VMEM((2, quarter, columns), bf),
        ]
        + [pltpu.VMEM((n, count, wide), bf) for n in levels + [NZ + 1]]
        + [
            dma((sum(Gather.sends(p) for p in plans),)),
            dma((sum(p.blocks for p in plans),)),
            dma(()),
            dma((sends,)),
            dma((recvs,)),
            dma((held * NX * NC + blocks // NY,)),
            dma((held * NX * NC,)),
            dma((blocks // NY,)),
        ],
        compiler_params=pltpu.CompilerParams(
            collective_id=collective_id, has_side_effects=True, vmem_limit_bytes=67043328
        ),
        name="experts",
    )(payload, cots, *parts)


def weights_kernel(plans, *refs):
    left_one, right_one, left_two, right_two, left_small, right_small = refs[:6]
    outs = refs[6:8]
    held_one, held_two = refs[8:10]
    buffers = refs[10:18]
    send_one, recv_one, send_two, recv_two, spare = refs[18:]
    place = Place()
    far = list(reversed(range(NZ)))
    greet(place, (Z, Y, X, C))
    ways = [
        Reduce(place, plans[0], held_one, buffers[0:3], buffers[3], send_one, recv_one, spare),
        Reduce(place, plans[1], held_two, buffers[4:7], buffers[7], send_two, recv_two, spare),
    ]
    group = NY * NX * NC
    rows = group * held_one.shape[1]

    def products(left, right, held, k, shift):
        at = pl.ds(pl.multiple_of(place.order[k] * rows, 128), rows)
        block = left[:, at]
        for c0, cn in columns_of(right.shape[1]):
            got = lax.dot_general(
                block, right[:, c0 : c0 + cn], (((0,), (0,)), ((), ())), preferred_element_type=jnp.float32
            )
            held[pl.ds(place.order[k] * group, group), :, shift + c0 : shift + c0 + cn] = got.astype(
                held.dtype
            ).reshape(group, rows // group, cn)

    for t in range(NZ):
        k = far[t]
        products(left_one, right_one, held_one, k, 0)
        ways[0].first(k)
        products(left_two, right_two, held_two, k, 0)
        products(left_small, right_small, held_two, k, right_two.shape[1])
        ways[1].first(k)
        if t > 0:
            for way in ways:
                for step in way.at_time(t - 1):
                    step()
    for t in range(NZ - 1, NZ + 3):
        for way in ways:
            for step in way.at_time(t):
                step()
    for way, out in zip(ways, outs):
        way.last(out)
    for way in ways:
        way.finish()


def return_weights(lefts, rights, collective_id):
    width = lefts[0].shape[1]
    rows = width // (NZ * NY * NX * NC)
    widths = [rights[0].shape[1], rights[1].shape[1] + rights[2].shape[1]]
    plans = [Plan(0, (C, Y, X), (Z, Y, X, C)), Plan(1, (C, X, Y), (Z, Y, X, C))]
    bf = jnp.bfloat16
    levels, sends, recvs = Reduce.counts(plans[0])
    dma = pltpu.SemaphoreType.DMA
    vmem = pl.BlockSpec(memory_space=pltpu.VMEM)
    return pl.pallas_call(
        functools.partial(weights_kernel, plans),
        out_shape=[jax.ShapeDtypeStruct((rows, w), jnp.float32) for w in widths],
        in_specs=[vmem] * 6,
        out_specs=[vmem] * 2,
        scratch_shapes=[pltpu.VMEM((plans[0].blocks, rows, w), bf) for w in widths]
        + [pltpu.VMEM((n, rows, w), bf) for w in widths for n in levels + [NZ + 1]]
        + [dma((n,)) for n in (sends, recvs, sends, recvs)]
        + [dma(())],
        compiler_params=pltpu.CompilerParams(
            collective_id=collective_id, has_side_effects=True, vmem_limit_bytes=60 * 1024 * 1024
        ),
        name="return_weights",
    )(*[a for pair in zip(lefts, rights) for a in pair])


def turn(block, cosine, sine):
    lane = lax.broadcasted_iota(jnp.int32, (1, 128), 1)
    half = HEAD_SIZE // 2
    other = jnp.where(lane % HEAD_SIZE < half, pltpu.roll(block, 128 - half, 1), pltpu.roll(block, half, 1))
    return block * cosine + other * sine


def place_heads(read, target, count):
    group = QUERY_HEADS // KEY_VALUE_HEADS
    lane = lax.broadcasted_iota(jnp.int32, (1, 2 * HEAD_SIZE), 1)
    for pair in range(QUERY_HEADS // 2):
        both = read(pair)
        for h in (2 * pair, 2 * pair + 1):
            m, g = h // group, h % group
            block = both if h % 2 == m % 2 else pltpu.roll(both, HEAD_SIZE, 1)
            block = jnp.where(lane // HEAD_SIZE == m % 2, block, 0.0)
            target[m, g * count : (g + 1) * count] = block.astype(target.dtype)


def collect_heads(source, target, count, finish):
    group = QUERY_HEADS // KEY_VALUE_HEADS
    lane = lax.broadcasted_iota(jnp.int32, (1, 2 * HEAD_SIZE), 1)
    for pair in range(QUERY_HEADS // 2):
        sides = []
        for h in (2 * pair, 2 * pair + 1):
            m, g = h // group, h % group
            block = source[m, g * count : (g + 1) * count]
            sides.append(block if h % 2 == m % 2 else pltpu.roll(block, HEAD_SIZE, 1))
        both = finish(jnp.where(lane < HEAD_SIZE, *sides))
        target[:, pair * 128 : pair * 128 + 128] = both.astype(target.dtype)


class Scores:
    def __init__(self, place, queries, keys):
        self.queries, self.keys = queries, keys
        group = QUERY_HEADS // KEY_VALUE_HEADS
        count = keys.shape[1]
        self.total = keys.shape[0] * count
        row = lax.broadcasted_iota(jnp.int32, (group * count, 1), 0) % count
        self.position = row + (place.at[Z] * NY + place.at[Y]) * count
        self.column = lax.broadcasted_iota(jnp.int32, (1, self.total), 1)

    def pair(self, m, shift):
        at = pl.ds(pl.multiple_of(shift + m // 2 * 128, 128), 128)
        return self.keys[:, :, at].reshape(self.total, 128)

    def of(self, m, keys):
        found = lax.dot_general(
            self.queries[m], keys, (((1,), (1,)), ((), ())), preferred_element_type=jnp.float32
        )
        return jnp.where(self.column <= self.position, found * attn_scale, masked_logits)


def attend_kernel(
    plans, linear, own_cots, cosine, sine, out, log_sums, kv_out, cots, placed, seen, own_kv, raw, *sems
):
    send_kv, recv_kv, send_cot, recv_cot, spare, own_sem = sems
    place = Place()
    bf, f32 = jnp.bfloat16, jnp.float32
    count = linear.shape[0]
    width = KEY_VALUE_HEADS * HEAD_SIZE
    q_width = QUERY_HEADS * HEAD_SIZE
    for c0 in range(0, width, 128):
        block = linear[:, q_width + c0 : q_width + c0 + 128]
        own_kv[:, c0 : c0 + 128] = turn(block, cosine[...], sine[...]).astype(bf)
    own_kv[:, width:] = linear[:, q_width + width :].astype(bf)
    greet(place, (Z, Y, C))
    kv_way = Gather(place, plans[0], own_kv, seen, send_kv, recv_kv, spare, 0, 0)
    cot_ways, at = [], 0
    for n, plan in enumerate(plans[1:]):
        cot_ways.append(Gather(place, plan, own_cots, cots, send_cot, recv_cot, spare, at, n * plan.blocks))
        at += Gather.sends(plan)
    kv_way.step(0, ())
    for way in cot_ways:
        way.step(0, ())
    mine = pltpu.make_async_copy(own_cots, cots.at[flat_index(place.at, plans[1].index)], own_sem.at[0])
    mine.start()
    seen[flat_index(place.at, plans[0].index)] = own_kv[...]
    place_heads(lambda pair: turn(linear[:, pair * 128 : pair * 128 + 128], cosine[...], sine[...]), placed, count)
    log_sums[...] = jnp.zeros(log_sums.shape, f32)
    early = [e for e in gather_events(plans[1].order)[1:]]
    kv_events = gather_events(plans[0].order)[1:]
    for k, flips in kv_events:
        kv_way.step(k, flips)
        if len(early) > 8:
            event = early.pop(0)
            for way in cot_ways:
                way.step(*event)
    keep = pltpu.make_async_copy(seen, kv_out, own_sem.at[1])
    keep.start()
    scores = Scores(place, placed, seen)
    lane = lax.broadcasted_iota(jnp.int32, (1, 128), 1)

    def head(m, carry):
        for i in range(KEY_VALUE_HEADS):
            if early:
                event = early.pop(0)

                @pl.when(m == i)
                def _():
                    for way in cot_ways:
                        way.step(*event)

        s = scores.of(m, scores.pair(m, 0))
        best = jnp.max(s, axis=1, keepdims=True)
        weights = jnp.exp(s - best)
        total = jnp.sum(weights, axis=1, keepdims=True)
        mixed = jnp.dot(weights.astype(bf), scores.pair(m, width), preferred_element_type=f32)
        raw[m] = mixed / total
        log_sums[...] = jnp.where(lane == m, best + jnp.log(total), log_sums[...])
        return carry

    lax.fori_loop(0, KEY_VALUE_HEADS, head, 0)
    collect_heads(raw, out, count, lambda block: block)
    keep.wait()
    mine.wait()
    kv_way.finish()
    for way in cot_ways:
        way.finish()


def attend(linear, own_cots, cosine, sine, collective_id):
    count = linear.shape[0]
    kv_width = 2 * KEY_VALUE_HEADS * HEAD_SIZE
    cut = count * 3 // 4
    plans = [
        Plan(0, (Z, Y), (Z, Y)),
        Plan(1, (Z, Y, C), (C, Z, Y), rows=(0, cut)),
        Plan(1, (Y, Z, C), (C, Z, Y), rows=(cut, count - cut)),
    ]
    bf, f32 = jnp.bfloat16, jnp.float32
    group = QUERY_HEADS // KEY_VALUE_HEADS
    vmem = pl.BlockSpec(memory_space=pltpu.VMEM)
    apart = pl.BlockSpec(memory_space=pl.ANY)
    dma = pltpu.SemaphoreType.DMA
    kv_shape = (plans[0].blocks, count, kv_width)
    heads = (KEY_VALUE_HEADS, group * count, 2 * HEAD_SIZE)
    return pl.pallas_call(
        functools.partial(attend_kernel, plans),
        out_shape=[
            jax.ShapeDtypeStruct((count, QUERY_HEADS * HEAD_SIZE), bf),
            jax.ShapeDtypeStruct((group * count, 128), f32),
            jax.ShapeDtypeStruct(kv_shape, bf),
            jax.ShapeDtypeStruct((plans[1].blocks,) + own_cots.shape, bf),
            jax.ShapeDtypeStruct(heads, bf),
        ],
        in_specs=[vmem] * 4,
        out_specs=[vmem, vmem, apart, apart, vmem],
        scratch_shapes=[pltpu.VMEM(kv_shape, bf), pltpu.VMEM((count, kv_width), bf), pltpu.VMEM(heads, f32)]
        + [
            dma((Gather.sends(plans[0]),)),
            dma((plans[0].blocks,)),
            dma((Gather.sends(plans[1]) + Gather.sends(plans[2]),)),
            dma((plans[1].blocks + plans[2].blocks,)),
            dma(()),
            dma((2,)),
        ],
        compiler_params=pltpu.CompilerParams(
            collective_id=collective_id, has_side_effects=True, vmem_limit_bytes=56 * 1024 * 1024
        ),
        name="attend",
    )(linear, own_cots, cosine, sine)


def attend_back_kernel(plans, *refs):
    placed, grads, outputs, log_sums, keys, part, mixed, cosine, sine = refs[:9]
    back, layer_out = refs[9:11]
    kv_grad, grads_placed, raw, deltas, held, held_out = refs[11:17]
    level, chain, out_level, out_level_two, out_chain = refs[17:22]
    send_kv, recv_kv, send_out, recv_out, spare, load_sem = refs[22:]
    place = Place()
    bf, f32 = jnp.bfloat16, jnp.float32
    far = list(reversed(range(NZ)))
    loads = []
    for k in far:
        for h in (1 - place.at[C], place.at[C]):
            at = pl.ds((h * NZ + place.order[k]) * NY, NY)
            loads.append(pltpu.make_async_copy(part.at[at], held_out.at[at], load_sem.at[len(loads)]))
    for copy in loads:
        copy.start()
    greet(place, (Z, Y, C))
    kv_way = Reduce(place, plans[0], held, (level,), chain, send_kv, recv_kv, spare)
    out_way = Reduce(place, plans[1], held_out, (out_level, out_level_two), out_chain, send_out, recv_out, spare)
    for copy in loads:
        copy.wait()
    for k in far:
        out_way.first(k)
    count = grads.shape[0]
    place_heads(lambda pair: grads[:, pair * 128 : pair * 128 + 128].astype(f32), grads_placed, count)
    group = QUERY_HEADS // KEY_VALUE_HEADS
    lane = lax.broadcasted_iota(jnp.int32, (1, 128), 1)
    for g in range(group):
        found = jnp.zeros((count, 128), f32)
        for m in range(KEY_VALUE_HEADS):
            h = m * group + g
            at = slice(h // 2 * 128, h // 2 * 128 + 128)
            both = grads[:, at].astype(f32) * outputs[:, at].astype(f32)
            delta = jnp.sum(jnp.where(lane // HEAD_SIZE == h % 2, both, 0.0), axis=1, keepdims=True)
            found = jnp.where(lane == m, delta, found)
        deltas[g * count : (g + 1) * count] = found
    scores = Scores(place, placed, keys)
    width = KEY_VALUE_HEADS * HEAD_SIZE
    blocks = keys.shape[0]
    turns = KEY_VALUE_HEADS // 2
    early = [[(out_way.level, 0, 3)], [(out_way.level, 0, 2)], [(out_way.level, 1, 3)], [(out_way.level, 1, 2), (out_way.along, 3)]]

    def pair(p, carry):
        for i in range(turns):

            @pl.when(p == i)
            def _():
                for step, *at in early[i]:
                    step(*at)

        key_sum = value_sum = None
        for side in range(2):
            m = 2 * p + side
            k_pair, v_pair = scores.pair(m, 0), scores.pair(m, width)
            of_head = lambda ref: jnp.sum(jnp.where(lane == m, ref[...], 0.0), axis=1, keepdims=True)
            weights = jnp.exp(scores.of(m, k_pair) - of_head(log_sums))
            grad = grads_placed[m]
            grad_probs = lax.dot_general(grad, v_pair, (((1,), (1,)), ((), ())), preferred_element_type=f32)
            grad_scores = (weights * (grad_probs - of_head(deltas))).astype(bf)
            raw[m] = attn_scale * jnp.dot(grad_scores, k_pair, preferred_element_type=f32)
            over_rows = (((0,), (0,)), ((), ()))
            key_part = lax.dot_general(grad_scores, placed[m], over_rows, preferred_element_type=f32)
            value_part = lax.dot_general(weights.astype(bf), grad, over_rows, preferred_element_type=f32)
            key_sum = key_part if key_sum is None else key_sum + key_part
            value_sum = value_part if value_sum is None else value_sum + value_part
        at = pl.multiple_of(p * 128, 128)
        held[:, :, pl.ds(at, 128)] = (attn_scale * key_sum).astype(bf).reshape(blocks, count, 128)
        at = pl.multiple_of(width + p * 128, 128)
        held[:, :, pl.ds(at, 128)] = value_sum.astype(bf).reshape(blocks, count, 128)
        return carry

    lax.fori_loop(0, turns, pair, 0)
    for k in far:
        kv_way.first(k)
    out_way.level(0, 1)
    out_way.level(0, 0)
    collect_heads(raw, back, count, lambda block: turn(block, cosine[...], -sine[...]))
    kv_way.level(0, 3)
    kv_way.level(0, 2)
    kv_way.along(3)
    kv_way.level(0, 1)
    kv_way.along(2)
    out_way.along(2)
    kv_way.level(0, 0)
    kv_way.along(1)
    kv_way.last(kv_grad)
    q_width = QUERY_HEADS * HEAD_SIZE
    for c0 in range(0, width, 128):
        block = turn(kv_grad[:, c0 : c0 + 128], cosine[...], -sine[...])
        back[:, q_width + c0 : q_width + c0 + 128] = block.astype(bf)
    back[:, q_width + width :] = kv_grad[:, width:].astype(bf)
    out_way.level(1, 1)
    out_way.along(1)
    out_way.level(1, 0)
    out_way.last(layer_out, mixed)
    kv_way.finish()
    out_way.finish()


def attend_back(placed, grads, outputs, log_sums, keys, part, mixed, cosine, sine, collective_id):
    count, kv_width = keys.shape[1:]
    plans = [Plan(0, (Y,), (Z, Y)), Plan(1, (C, Y), (C, Z, Y))]
    bf, f32 = jnp.bfloat16, jnp.float32
    group = QUERY_HEADS // KEY_VALUE_HEADS
    vmem = pl.BlockSpec(memory_space=pltpu.VMEM)
    dma = pltpu.SemaphoreType.DMA
    heads = (KEY_VALUE_HEADS, group * count, 2 * HEAD_SIZE)
    levels, sends, recvs = Reduce.counts(plans[0])
    out_levels, out_sends, out_recvs = Reduce.counts(plans[1])
    return pl.pallas_call(
        functools.partial(attend_back_kernel, plans),
        out_shape=[
            jax.ShapeDtypeStruct((count, grads.shape[1] + kv_width), bf),
            jax.ShapeDtypeStruct(mixed.shape, bf),
        ],
        in_specs=[vmem] * 5 + [pl.BlockSpec(memory_space=pl.ANY)] + [vmem] * 3,
        out_specs=[vmem] * 2,
        scratch_shapes=[
            pltpu.VMEM((count, kv_width), f32),
            pltpu.VMEM(heads, bf),
            pltpu.VMEM(heads, f32),
            pltpu.VMEM((group * count, 128), f32),
            pltpu.VMEM(keys.shape, bf),
            pltpu.VMEM(part.shape, bf),
        ]
        + [pltpu.VMEM((n,) + keys.shape[1:], bf) for n in levels + [NZ + 1]]
        + [pltpu.VMEM((n,) + part.shape[1:], bf) for n in out_levels + [NZ + 1]]
        + [dma((n,)) for n in (sends, recvs, out_sends, out_recvs)]
        + [dma(()), dma((NC * NZ,))],
        compiler_params=pltpu.CompilerParams(
            collective_id=collective_id, has_side_effects=True, vmem_limit_bytes=60 * 1024 * 1024
        ),
        name="attend_back",
    )(placed, grads, outputs, log_sums, keys, part, mixed, cosine, sine)


def last_kernel(core_ref, own, core_part, x_part, both_part, one, two, *outs):
    core = core_ref[0]
    in_out, out_out = outs[:2]
    split = in_out.shape[3]
    for at, left, right in ((core, own, x_part), (1 - core, core_part, both_part)):
        total = left[0].astype(jnp.float32) + right[0].astype(jnp.float32)
        in_out[at, 0] = total[:, :split]
        out_out[at, 0] = total[:, split:]

    @pl.when(jnp.logical_and(pl.program_id(0) == 0, pl.program_id(1) == 0))
    def _():
        wq, wk, wv, wo, router, first_gain, second_gain = outs[2:]
        q, k = wq.shape[1], wk.shape[1]
        wq[...] = one[:, :q]
        wk[...] = one[:, q : q + k]
        wv[...] = one[:, q + k :]
        width = wo.shape[1]
        wo[...] = two[:, :width]
        small = two[:, width:]
        router[...] = small[:, : router.shape[1]]
        turned = small.T
        at = router.shape[1]
        first_gain[...] = turned[at : at + 1]
        second_gain[...] = turned[at + 1 : at + 2]


def last_outputs(pieces, core, split, one, two, widths):
    held, quarter, columns = pieces[0].shape
    step = quarter // 2
    rows = one.shape[0]
    spec = pl.BlockSpec((1, step, columns), lambda e, r, c: (e, r, 0))
    fixed = lambda a, b: pl.BlockSpec((a, b), lambda e, r, c: (0, 0))
    outs = (split, columns - split)
    shapes = [(rows, w) for w in widths] + [(1, rows)] * 2
    return pl.pallas_call(
        last_kernel,
        grid_spec=pltpu.PrefetchScalarGridSpec(
            num_scalar_prefetch=1,
            grid=(held, 2),
            in_specs=[spec] * 4 + [fixed(*one.shape), fixed(*two.shape)],
            out_specs=[pl.BlockSpec((NC, 1, step, w), lambda e, r, c: (0, e, r, 0)) for w in outs]
            + [fixed(*s) for s in shapes],
        ),
        out_shape=[jax.ShapeDtypeStruct((NC, held, quarter, w), jnp.float32) for w in outs]
        + [jax.ShapeDtypeStruct(s, jnp.float32) for s in shapes],
        name="last_outputs",
    )(core[None], *pieces, one, two)


MODEL_WIDTH = 1536
QUERY_HEADS = 24
KEY_VALUE_HEADS = 8
HEAD_SIZE = 64
EXPERT_HIDDEN = 512
EXPERT_COUNT = 32
TOP = 8
CAP = 40


norm_eps = 1e-06
attn_scale = 0.015625
rope_base = 10000.0
masked_logits = -1e30


def rope_tables(positions):
    half = HEAD_SIZE // 2
    frequency = jnp.power(
        jnp.float32(rope_base), -2.0 * jnp.arange(half, dtype=jnp.float32) / HEAD_SIZE
    )
    angle = positions.astype(jnp.float32)[:, None] * frequency[None, :]
    return (jnp.cos(angle)[:, None, :], jnp.sin(angle)[:, None, :])


def rotate_pairs(value_tensor, cosine_table, sine_table):
    half = value_tensor.shape[-1] // 2
    first = value_tensor[..., :half]
    second = value_tensor[..., half:]
    return jnp.concatenate(
        [first * cosine_table - second * sine_table, second * cosine_table + first * sine_table],
        axis=-1,
    )


def rms_forward(wide, gain):
    inverse = lax.rsqrt(jnp.mean(wide * wide, axis=-1, keepdims=True) + norm_eps)
    unit = wide * inverse
    return (unit, inverse, (unit * gain.astype(jnp.float32)).astype(jnp.bfloat16))


def rms_backward(grad, unit, inverse, gain):
    scaled = grad * gain.astype(jnp.float32)
    back = inverse * (scaled - unit * jnp.mean(scaled * unit, axis=-1, keepdims=True))
    return (back, jnp.sum(grad * unit, axis=0))


def piece_scores(query_rows, key_section, positions):
    token_count = key_section.shape[0]
    key_tensor = key_section.reshape(token_count, KEY_VALUE_HEADS, HEAD_SIZE)
    scores = (
        jnp.einsum("tkgd,nkd->kgtn", query_rows, key_tensor, preferred_element_type=jnp.float32)
        * attn_scale
    )
    visible = jnp.arange(token_count, dtype=jnp.int32)[None, :] <= positions[:, None]
    return (jnp.where(visible, scores, masked_logits), visible, key_tensor)


def local(
    hidden,
    routes,
    attn_norm,
    ffn_norm,
    w_q,
    key_weight,
    value_weight,
    w_o,
    router,
    expert_in,
    expert_out,
    cotangent,
):
    token_rows = hidden.shape[1]
    query_group = QUERY_HEADS // KEY_VALUE_HEADS
    ctx_size = lax.axis_size(CTX)
    sequence_length = token_rows * ctx_size
    positions = lax.axis_index(CTX) * token_rows + jnp.arange(token_rows, dtype=jnp.int32)
    cosine_table, sine_table = rope_tables(positions)
    contract_rows = (((0,), (0,)), ((), ()))
    contract_cols = (((1,), (1,)), ((), ()))
    layer = (
        lax.all_gather(attn_norm, (CTX, FSDP), axis=0, tiled=True),
        lax.all_gather(ffn_norm, (CTX, FSDP), axis=0, tiled=True),
        lax.all_gather(w_q, (CTX, FSDP), axis=0, tiled=True),
        lax.all_gather(key_weight, (CTX, FSDP), axis=0, tiled=True),
        lax.all_gather(value_weight, (CTX, FSDP), axis=0, tiled=True),
        lax.all_gather(w_o, (CTX, FSDP), axis=0, tiled=True),
        lax.all_gather(router, (CTX, FSDP), axis=0, tiled=True),
    )
    attn_gain, ffn_gain, query_w, key_weight_matrix, value_w, output_w, router_w = layer
    experts = (
        lax.all_gather(expert_in, FSDP, axis=1, tiled=True),
        lax.all_gather(expert_out, FSDP, axis=1, tiled=True),
    )
    weight_in, weight_out = experts
    wide = hidden[0].astype(jnp.float32)
    attn_unit, inverse_one, attention_input = rms_forward(wide, attn_gain)
    query_linear = jnp.dot(attention_input, query_w, preferred_element_type=jnp.float32).reshape(
        token_rows, QUERY_HEADS, HEAD_SIZE
    )
    query_rows = (
        rotate_pairs(query_linear, cosine_table, sine_table)
        .astype(jnp.bfloat16)
        .reshape(token_rows, KEY_VALUE_HEADS, query_group, HEAD_SIZE)
    )
    key_linear = jnp.dot(
        attention_input, key_weight_matrix, preferred_element_type=jnp.float32
    ).reshape(token_rows, KEY_VALUE_HEADS, HEAD_SIZE)
    key_matrix_rows = (
        rotate_pairs(key_linear, cosine_table, sine_table)
        .astype(jnp.bfloat16)
        .reshape(token_rows, KEY_VALUE_HEADS * HEAD_SIZE)
    )
    value_rows = jnp.dot(attention_input, value_w, preferred_element_type=jnp.float32).astype(
        jnp.bfloat16
    )
    init_state = (
        jnp.full((KEY_VALUE_HEADS, query_group, token_rows), masked_logits, jnp.float32),
        jnp.zeros((KEY_VALUE_HEADS, query_group, token_rows), jnp.float32),
        jnp.zeros((KEY_VALUE_HEADS, query_group, token_rows, HEAD_SIZE), jnp.float32),
    )
    key_section = lax.all_gather(key_matrix_rows, CTX, axis=0, tiled=True)
    value_section = lax.all_gather(value_rows, CTX, axis=0, tiled=True)

    def compute(current):
        best, total, weighted = current
        scores, visible, _ = piece_scores(query_rows, key_section, positions)
        value_tensor = value_section.reshape(value_section.shape[0], KEY_VALUE_HEADS, HEAD_SIZE)
        new_best = jnp.maximum(best, jnp.max(scores, axis=-1))
        weights = jnp.where(visible, jnp.exp(scores - new_best[..., None]), 0.0)
        total = jnp.sum(weights, axis=-1)
        weighted = jnp.einsum(
            "kgtn,nkd->kgtd",
            weights.astype(jnp.bfloat16),
            value_tensor,
            preferred_element_type=jnp.float32,
        )
        return (new_best, total, weighted)

    best, total, weighted = lax.cond(
        jnp.int32(0) <= positions[-1], compute, lambda current: current, init_state
    )
    log_sum_rows = best + jnp.log(total)
    attention_output = (
        jnp.transpose(weighted / total[..., None], (2, 0, 1, 3))
        .reshape(token_rows, QUERY_HEADS * HEAD_SIZE)
        .astype(jnp.bfloat16)
    )
    mixed = wide + jnp.dot(attention_output, output_w, preferred_element_type=jnp.float32)
    ffn_unit, inverse_two, ffn_in = rms_forward(mixed, ffn_gain)
    logits = jnp.dot(ffn_in, router_w, preferred_element_type=jnp.float32)
    route = routes[0]
    indicator = (route[:, :, None] == jnp.arange(EXPERT_COUNT, dtype=jnp.int32)).astype(jnp.float32)
    chosen = jnp.sum(indicator * logits[:, None, :], axis=-1)
    gates = jax.nn.softmax(chosen, axis=-1)
    flat_route = route.reshape(-1)
    counter = (flat_route[:, None] == jnp.arange(EXPERT_COUNT, dtype=jnp.int32)).astype(jnp.int32)
    slot = jnp.sum(counter * (jnp.cumsum(counter, axis=0) - 1), axis=1)
    target = flat_route * CAP + slot
    owner = (
        jnp.full((EXPERT_COUNT * CAP,), token_rows * TOP, jnp.int32)
        .at[target]
        .set(jnp.arange(token_rows * TOP, dtype=jnp.int32))
    )
    ffn_pad = jnp.concatenate([ffn_in, jnp.zeros((1, MODEL_WIDTH), jnp.bfloat16)], axis=0)
    local_experts = weight_in.shape[0]
    outgoing = ffn_pad[owner // TOP].reshape(ctx_size, local_experts, CAP, MODEL_WIDTH)
    received = lax.all_to_all(outgoing, CTX, split_axis=0, concat_axis=2, tiled=True)[0]
    act = jnp.einsum("erd,edf->erf", received, weight_in, preferred_element_type=jnp.float32)
    gate_part = act[..., :EXPERT_HIDDEN]
    up_part = act[..., EXPERT_HIDDEN:]
    sigma = jax.nn.sigmoid(gate_part)
    inner = (gate_part * sigma * up_part).astype(jnp.bfloat16)
    produced = jnp.einsum(
        "erf,edf->erd", inner, weight_out, preferred_element_type=jnp.float32
    ).astype(jnp.bfloat16)
    returned = lax.all_to_all(
        produced[None], CTX, split_axis=2, concat_axis=0, tiled=True
    ).reshape(EXPERT_COUNT * CAP, MODEL_WIDTH)
    picked = returned[target].reshape(token_rows, TOP, MODEL_WIDTH)
    layer_out = (mixed + jnp.sum(gates[..., None] * picked, axis=1)).astype(jnp.bfloat16)
    cot = cotangent[0]
    layer = (
        lax.all_gather(attn_norm, (CTX, FSDP), axis=0, tiled=True),
        lax.all_gather(ffn_norm, (CTX, FSDP), axis=0, tiled=True),
        lax.all_gather(w_q, (CTX, FSDP), axis=0, tiled=True),
        lax.all_gather(key_weight, (CTX, FSDP), axis=0, tiled=True),
        lax.all_gather(value_weight, (CTX, FSDP), axis=0, tiled=True),
        lax.all_gather(w_o, (CTX, FSDP), axis=0, tiled=True),
        lax.all_gather(router, (CTX, FSDP), axis=0, tiled=True),
    )
    attn_gain, ffn_gain, query_w, key_weight_matrix, value_w, output_w, router_w = layer
    experts = (
        lax.all_gather(expert_in, FSDP, axis=1, tiled=True),
        lax.all_gather(expert_out, FSDP, axis=1, tiled=True),
    )
    weight_in, weight_out = experts
    grad_gate = jnp.sum(cot[:, None, :] * picked, axis=-1)
    slot_grads = (
        (gates[..., None] * cot[:, None, :])
        .astype(jnp.bfloat16)
        .reshape(token_rows * TOP, MODEL_WIDTH)
    )
    slot_pad = jnp.concatenate([slot_grads, jnp.zeros((1, MODEL_WIDTH), jnp.bfloat16)], axis=0)
    grad_outgoing = slot_pad[owner].reshape(ctx_size, local_experts, CAP, MODEL_WIDTH)
    grad_received = lax.all_to_all(grad_outgoing, CTX, split_axis=0, concat_axis=2, tiled=True)[0]
    grad_w_out = jnp.einsum(
        "erd,erf->edf", grad_received, inner, preferred_element_type=jnp.float32
    )
    grad_inner = jnp.einsum(
        "erd,edf->erf", grad_received, weight_out, preferred_element_type=jnp.float32
    )
    grad_act = jnp.concatenate(
        [
            grad_inner * up_part * sigma * (1.0 + gate_part * (1.0 - sigma)),
            grad_inner * gate_part * sigma,
        ],
        axis=-1,
    ).astype(jnp.bfloat16)
    grad_w_in = jnp.einsum("erd,erf->edf", received, grad_act, preferred_element_type=jnp.float32)
    grad_rows = jnp.einsum(
        "erf,edf->erd", grad_act, weight_in, preferred_element_type=jnp.float32
    ).astype(jnp.bfloat16)
    grad_back = lax.all_to_all(
        grad_rows[None], CTX, split_axis=2, concat_axis=0, tiled=True
    ).reshape(EXPERT_COUNT * CAP, MODEL_WIDTH)
    grad_expert_in, grad_expert_out = (
        lax.psum_scatter(
            grad_w_in.astype(jnp.bfloat16), FSDP, scatter_dimension=1, tiled=True
        ).astype(jnp.float32),
        lax.psum_scatter(
            grad_w_out.astype(jnp.bfloat16), FSDP, scatter_dimension=1, tiled=True
        ).astype(jnp.float32),
    )
    grad_chosen = gates * (grad_gate - jnp.sum(gates * grad_gate, axis=-1, keepdims=True))
    grad_logits = jnp.sum(indicator * grad_chosen[..., None], axis=1).astype(jnp.bfloat16)
    grad_router_part = lax.dot_general(
        ffn_in, grad_logits, contract_rows, preferred_element_type=jnp.float32
    )
    grad_ffn_in = lax.dot_general(
        grad_logits, router_w, contract_cols, preferred_element_type=jnp.float32
    )
    grad_ffn_in = grad_ffn_in + jnp.sum(
        grad_back[target].reshape(token_rows, TOP, MODEL_WIDTH), axis=1, dtype=jnp.float32
    )
    back_two, grad_ffn_gain = rms_backward(grad_ffn_in, ffn_unit, inverse_two, ffn_gain)
    grad_mixed = cot + back_two
    grad_attn = grad_mixed.astype(jnp.bfloat16)
    grad_wo_part = lax.dot_general(
        attention_output, grad_attn, contract_rows, preferred_element_type=jnp.float32
    )
    attention_output_gradient = lax.dot_general(
        grad_attn, output_w, contract_cols, preferred_element_type=jnp.float32
    ).astype(jnp.bfloat16)
    head_gradient = attention_output_gradient.reshape(
        token_rows, KEY_VALUE_HEADS, query_group, HEAD_SIZE
    )
    delta_rows = jnp.sum(
        head_gradient.astype(jnp.float32)
        * attention_output.reshape(token_rows, KEY_VALUE_HEADS, query_group, HEAD_SIZE).astype(
            jnp.float32
        ),
        axis=-1,
    )
    delta_rows = jnp.transpose(delta_rows, (1, 2, 0))
    init_back = (
        jnp.zeros((token_rows, KEY_VALUE_HEADS, query_group, HEAD_SIZE), jnp.float32),
        jnp.zeros((sequence_length, 2 * KEY_VALUE_HEADS * HEAD_SIZE), jnp.float32),
    )
    attend_key_section = lax.all_gather(key_matrix_rows, CTX, axis=0, tiled=True)
    attend_value_section = lax.all_gather(value_rows, CTX, axis=0, tiled=True)

    def compute(current):
        token_count = attend_key_section.shape[0]
        scores, visible, key_tensor = piece_scores(query_rows, attend_key_section, positions)
        value_tensor = attend_value_section.reshape(token_count, KEY_VALUE_HEADS, HEAD_SIZE)
        weights_full = jnp.where(visible, jnp.exp(scores - log_sum_rows[..., None]), 0.0)
        grad_probs = jnp.einsum(
            "tkgd,nkd->kgtn", head_gradient, value_tensor, preferred_element_type=jnp.float32
        )
        grad_scores = (weights_full * (grad_probs - delta_rows[..., None])).astype(jnp.bfloat16)
        grad_query = attn_scale * jnp.einsum(
            "kgtn,nkd->tkgd", grad_scores, key_tensor, preferred_element_type=jnp.float32
        )
        key_portion = attn_scale * jnp.einsum(
            "kgtn,tkgd->nkd", grad_scores, query_rows, preferred_element_type=jnp.float32
        )
        value_portion = jnp.einsum(
            "kgtn,tkgd->nkd",
            weights_full.astype(jnp.bfloat16),
            head_gradient,
            preferred_element_type=jnp.float32,
        )
        update = jnp.concatenate(
            [
                key_portion.reshape(token_count, KEY_VALUE_HEADS * HEAD_SIZE),
                value_portion.reshape(token_count, KEY_VALUE_HEADS * HEAD_SIZE),
            ],
            axis=1,
        )
        return (grad_query, update)

    grad_query, grad_keys_full = lax.cond(
        jnp.int32(0) <= positions[-1], compute, lambda current: current, init_back
    )
    local_gradients = lax.psum_scatter(
        grad_keys_full.astype(jnp.bfloat16), CTX, scatter_dimension=0, tiled=True
    ).astype(jnp.float32)
    query_back = (
        rotate_pairs(
            grad_query.reshape(token_rows, QUERY_HEADS, HEAD_SIZE), cosine_table, -sine_table
        )
        .astype(jnp.bfloat16)
        .reshape(token_rows, QUERY_HEADS * HEAD_SIZE)
    )
    key_backward_rows = (
        rotate_pairs(
            local_gradients[:, : KEY_VALUE_HEADS * HEAD_SIZE].reshape(
                token_rows, KEY_VALUE_HEADS, HEAD_SIZE
            ),
            cosine_table,
            -sine_table,
        )
        .astype(jnp.bfloat16)
        .reshape(token_rows, KEY_VALUE_HEADS * HEAD_SIZE)
    )
    value_backward_rows = local_gradients[:, KEY_VALUE_HEADS * HEAD_SIZE :].astype(jnp.bfloat16)
    grad_wq_part = lax.dot_general(
        attention_input, query_back, contract_rows, preferred_element_type=jnp.float32
    )
    grad_wk_part = lax.dot_general(
        attention_input, key_backward_rows, contract_rows, preferred_element_type=jnp.float32
    )
    grad_wv_part = lax.dot_general(
        attention_input, value_backward_rows, contract_rows, preferred_element_type=jnp.float32
    )
    grad_attn_in = lax.dot_general(
        query_back, query_w, contract_cols, preferred_element_type=jnp.float32
    )
    grad_attn_in = grad_attn_in + lax.dot_general(
        key_backward_rows, key_weight_matrix, contract_cols, preferred_element_type=jnp.float32
    )
    grad_attn_in = grad_attn_in + lax.dot_general(
        value_backward_rows, value_w, contract_cols, preferred_element_type=jnp.float32
    )
    back_one, grad_attn_gain = rms_backward(grad_attn_in, attn_unit, inverse_one, attn_gain)
    grad_input = grad_mixed + back_one
    partial_sums = (
        lax.psum_scatter(
            grad_attn_gain.astype(jnp.bfloat16), CTX, scatter_dimension=0, tiled=True
        ).astype(jnp.float32),
        lax.psum_scatter(
            grad_ffn_gain.astype(jnp.bfloat16), CTX, scatter_dimension=0, tiled=True
        ).astype(jnp.float32),
        lax.psum_scatter(
            grad_wq_part.astype(jnp.bfloat16), CTX, scatter_dimension=0, tiled=True
        ).astype(jnp.float32),
        lax.psum_scatter(
            grad_wk_part.astype(jnp.bfloat16), CTX, scatter_dimension=0, tiled=True
        ).astype(jnp.float32),
        lax.psum_scatter(
            grad_wv_part.astype(jnp.bfloat16), CTX, scatter_dimension=0, tiled=True
        ).astype(jnp.float32),
        lax.psum_scatter(
            grad_wo_part.astype(jnp.bfloat16), CTX, scatter_dimension=0, tiled=True
        ).astype(jnp.float32),
        lax.psum_scatter(
            grad_router_part.astype(jnp.bfloat16), CTX, scatter_dimension=0, tiled=True
        ).astype(jnp.float32),
    )
    summed = (
        lax.psum_scatter(
            partial_sums[0].astype(jnp.bfloat16), FSDP, scatter_dimension=0, tiled=True
        ).astype(jnp.float32),
        lax.psum_scatter(
            partial_sums[1].astype(jnp.bfloat16), FSDP, scatter_dimension=0, tiled=True
        ).astype(jnp.float32),
        lax.psum_scatter(
            partial_sums[2].astype(jnp.bfloat16), FSDP, scatter_dimension=0, tiled=True
        ).astype(jnp.float32),
        lax.psum_scatter(
            partial_sums[3].astype(jnp.bfloat16), FSDP, scatter_dimension=0, tiled=True
        ).astype(jnp.float32),
        lax.psum_scatter(
            partial_sums[4].astype(jnp.bfloat16), FSDP, scatter_dimension=0, tiled=True
        ).astype(jnp.float32),
        lax.psum_scatter(
            partial_sums[5].astype(jnp.bfloat16), FSDP, scatter_dimension=0, tiled=True
        ).astype(jnp.float32),
        lax.psum_scatter(
            partial_sums[6].astype(jnp.bfloat16), FSDP, scatter_dimension=0, tiled=True
        ).astype(jnp.float32),
    )
    return (
        layer_out[None],
        grad_input[None],
        summed[0],
        summed[1],
        summed[2],
        summed[3],
        summed[4],
        summed[5],
        summed[6],
        grad_expert_in,
        grad_expert_out,
    )


def swap(a, flip):
    return lax.ppermute(a, FSDP, [(i, i ^ flip) for i in range(NX * NC)])


def fast_body(
    hidden,
    routes,
    attn_norm,
    ffn_norm,
    w_q,
    key_weight,
    value_weight,
    w_o,
    router,
    expert_in,
    expert_out,
    cotangent,
):
    tokens = hidden.shape[1]
    ctx = lax.axis_index(CTX)
    fsdp = lax.axis_index(FSDP)
    core = fsdp % NC
    rows = w_q.shape[0]
    quarter = expert_in.shape[1]
    kv_width = KEY_VALUE_HEADS * HEAD_SIZE
    q_width = QUERY_HEADS * HEAD_SIZE
    held = expert_in.shape[0] // NC
    bf = jnp.bfloat16
    f32 = jnp.float32
    positions = ctx * tokens + jnp.arange(tokens, dtype=jnp.int32)
    cosine_table, sine_table = (table[:, 0] for table in rope_tables(positions))
    cosine = jnp.concatenate([cosine_table] * 4, axis=1)
    sine = jnp.concatenate([-sine_table, sine_table] * 2, axis=1)
    contract_cols = (((1,), (1,)), ((), ()))
    wide = hidden[0].astype(f32)
    cot = cotangent[0]

    pack_one = jnp.concatenate([w_q, key_weight, value_weight], axis=1)
    pack_two = jnp.concatenate(
        [w_o, router, attn_norm[:, None], ffn_norm[:, None], jnp.zeros((rows, 94), bf)], axis=1
    )
    route = routes[0]
    indicator = (route[:, :, None] == jnp.arange(EXPERT_COUNT, dtype=jnp.int32)).astype(f32)
    cot_pack = jnp.concatenate(
        [
            cot.astype(bf),
            jnp.sum(indicator, axis=1).astype(bf),
            jnp.zeros((tokens, 128 - EXPERT_COUNT), bf),
        ],
        axis=1,
    )
    experts = jnp.concatenate([expert_in, expert_out], axis=2)
    experts = experts.reshape(NC, held, quarter, experts.shape[2])
    mine = lax.dynamic_index_in_dim(experts, core, 0, False)
    other = lax.dynamic_index_in_dim(experts, 1 - core, 0, False)
    part = rows // 3
    whole = (Z, Y, X, C)
    one, two = gather(
        [pack_one, pack_two],
        [
            Plan(0, (X, Z, Y, C), whole, rows=(0, 2 * part)),
            Plan(0, (X, Y, Z, C), whole, rows=(2 * part, part)),
            Plan(1, (Z, Y, X, C), whole),
        ],
        0,
    )
    one, mine, other = lax.optimization_barrier((one, mine, other))
    parts = [mine, swap(other, 1), swap(mine, 2), swap(other, 3)]
    one = one.reshape(MODEL_WIDTH, -1)
    two = two.reshape(MODEL_WIDTH, -1)
    output_w = two[:, :MODEL_WIDTH]
    small = two[:, MODEL_WIDTH:]
    router_w = small[:, :EXPERT_COUNT]
    gains = lax.dot_general(
        jnp.eye(128, dtype=bf), small, contract_cols, preferred_element_type=f32
    )
    attn_gain, ffn_gain = gains[EXPERT_COUNT], gains[EXPERT_COUNT + 1]

    attn_unit, inverse_one, attention_input = rms_forward(wide, attn_gain)
    linear = jnp.dot(attention_input, one, preferred_element_type=f32)
    attention_output, log_sums, kv, cots, queries = attend(linear, cot_pack, cosine, sine, 1)
    mixed = wide + jnp.dot(attention_output, output_w, preferred_element_type=f32)
    ffn_unit, inverse_two, ffn_in = rms_forward(mixed, ffn_gain)
    logits = jnp.dot(ffn_in, router_w, preferred_element_type=f32)
    chosen = jnp.sum(indicator * logits[:, None, :], axis=-1)
    gates = jax.nn.softmax(chosen, axis=-1)
    gate_map = jnp.sum(indicator * gates[..., None], axis=1)
    payload = jnp.concatenate(
        [ffn_in, gate_map.astype(bf), jnp.zeros((tokens, 128 - EXPERT_COUNT), bf)], axis=1
    )
    gin, moe_part, *pieces = moe(payload, cots, parts, CAP, 2)
    across = [swap(pieces[j], j) for j in range(1, NX * NC)]
    grad_gate_map = gin[:, MODEL_WIDTH : MODEL_WIDTH + EXPERT_COUNT] + gin[
        :, MODEL_WIDTH + EXPERT_COUNT : MODEL_WIDTH + 2 * EXPERT_COUNT
    ]
    grad_gate = jnp.sum(indicator * grad_gate_map[:, None, :], axis=-1)
    grad_chosen = gates * (grad_gate - jnp.sum(gates * grad_gate, axis=-1, keepdims=True))
    grad_logits = jnp.sum(indicator * grad_chosen[..., None], axis=1).astype(bf)
    grad_ffn_in = gin[:, :MODEL_WIDTH] + lax.dot_general(
        grad_logits, router_w, contract_cols, preferred_element_type=f32
    )
    back_two, _ = rms_backward(grad_ffn_in, ffn_unit, inverse_two, ffn_gain)
    grad_mixed = cot + back_two
    grad_attn = grad_mixed.astype(bf)
    attention_output_gradient = lax.dot_general(
        grad_attn, output_w, contract_cols, preferred_element_type=f32
    ).astype(bf)
    back, layer_out = attend_back(
        queries, attention_output_gradient, attention_output, log_sums, kv, moe_part, mixed, cosine, sine, 4
    )
    grad_attn_in = lax.dot_general(back, one, contract_cols, preferred_element_type=f32)
    back_one, _ = rms_backward(grad_attn_in, attn_unit, inverse_one, attn_gain)
    grad_input = grad_mixed + back_one
    halves = []
    for factor in (grad_attn_in * attn_unit, grad_ffn_in * ffn_unit):
        high = factor.astype(bf)
        halves += [high, (factor - high.astype(f32)).astype(bf)]
    column = lambda n: jnp.broadcast_to((jnp.arange(128) == n).astype(bf), (tokens, 128))
    sum_one, sum_two = return_weights(
        [attention_input, attention_output, jnp.concatenate([ffn_in] + halves)],
        [
            back,
            grad_attn,
            jnp.concatenate(
                [
                    jnp.concatenate([grad_logits, jnp.zeros((tokens, 128 - EXPERT_COUNT), bf)], axis=1),
                    column(EXPERT_COUNT),
                    column(EXPERT_COUNT),
                    column(EXPERT_COUNT + 1),
                    column(EXPERT_COUNT + 1),
                ]
            ),
        ],
        5,
    )
    grad_expert_in, grad_expert_out, *rest, first_gain, second_gain = last_outputs(
        [pieces[0]] + across,
        core,
        2 * EXPERT_HIDDEN,
        sum_one,
        sum_two,
        (q_width, kv_width, kv_width, MODEL_WIDTH, EXPERT_COUNT),
    )
    return (
        layer_out[None],
        grad_input[None],
        first_gain.reshape(rows),
        second_gain.reshape(rows),
        *rest,
        grad_expert_in.reshape(NC * held, quarter, -1),
        grad_expert_out.reshape(NC * held, quarter, -1),
    )


def fast(*args):
    return fast_body(*args)


def solution(mesh):
    placed = (
        P(FSDP, CTX, None),
        P(FSDP, CTX, None),
        P((CTX, FSDP)),
        P((CTX, FSDP)),
        P((CTX, FSDP), None),
        P((CTX, FSDP), None),
        P((CTX, FSDP), None),
        P((CTX, FSDP), None),
        P((CTX, FSDP), None),
        P(CTX, FSDP, None),
        P(CTX, FSDP, None),
        P(FSDP, CTX, None),
    )
    small = mesh.shape[CTX] == NZ * NY and mesh.shape[FSDP] == NX * NC
    return jax.shard_map(
        fast if small else local,
        mesh=mesh,
        in_specs=placed,
        out_specs=(
            P(FSDP, CTX, None),
            P(FSDP, CTX, None),
            P((CTX, FSDP)),
            P((CTX, FSDP)),
            P((CTX, FSDP), None),
            P((CTX, FSDP), None),
            P((CTX, FSDP), None),
            P((CTX, FSDP), None),
            P((CTX, FSDP), None),
            P(CTX, FSDP, None),
            P(CTX, FSDP, None),
        ),
        check_vma=False,
    )
```

```python
import functools
import itertools

import jax
import jax.numpy as jnp
from jax import lax
from jax.experimental import pallas as pl
from jax.experimental.pallas import tpu as pltpu
from jax.sharding import PartitionSpec as P


NY = 2
NZ = 4
NX = 2
NC = 2
DEV = pl.DeviceIdType.MESH
CTX, FSDP = "ctx", "fsdp"
Z, Y, X, C = 0, 1, 2, 3
SIZES = {Z: NZ, Y: NY, X: NX, C: NC}
UP, DOWN = 4, 5


class Plan:
    def __init__(self, ref, order, index, rows=None, view=None):
        self.ref, self.order, self.index, self.rows, self.view = ref, order, index, rows, view
        self.blocks = 1
        for d in index:
            self.blocks *= SIZES[d]


class Place:
    def __init__(self):
        ctx = lax.axis_index(CTX)
        fsdp = lax.axis_index(FSDP)
        self.at = {Z: ctx // NY, Y: ctx % NY, X: fsdp // NC, C: fsdp % NC}
        z = self.at[Z]
        low = z < NZ // 2
        base = jnp.where(low, z, NZ - 1 - z)
        near = [base, 1 - base, jnp.int32(2), jnp.int32(3)]
        self.order = [z] + [jnp.where(low, k, NZ - 1 - k) for k in near[1:]]

    def device(self, dim, value):
        spot = dict(self.at)
        spot[dim] = value
        return (spot[Z] * NY + spot[Y], spot[X] * NC + spot[C])

    def across(self, dim):
        return self.device(dim, 1 - self.at[dim])

    def along(self, step):
        return self.device(Z, self.at[Z] + step)

    def coords(self, z_from, flips):
        spot = {d: (1 - self.at[d] if d in flips else self.at[d]) for d in (Y, X, C)}
        spot[Z] = z_from
        return spot


def flat_index(spot, dims):
    index = 0
    for d in dims:
        index = index * SIZES[d] + spot[d]
    return index


def subsets(dims):
    return [c for n in range(len(dims) + 1) for c in itertools.combinations(dims, n)]


def greet(place, dims):
    barrier = pltpu.get_barrier_semaphore()
    z = place.at[Z]
    count = jnp.int32(0)
    for d in dims:
        if d == Z:
            @pl.when(z > 0)
            def _():
                pl.semaphore_signal(barrier, inc=1, device_id=place.along(-1), device_id_type=DEV)

            @pl.when(z < NZ - 1)
            def _():
                pl.semaphore_signal(barrier, inc=1, device_id=place.along(1), device_id_type=DEV)

            count = count + jnp.where(z > 0, 1, 0) + jnp.where(z < NZ - 1, 1, 0)
        else:
            pl.semaphore_signal(barrier, inc=1, device_id=place.across(d), device_id_type=DEV)
            count = count + 1
    pl.semaphore_wait(barrier, count)


def gather_events(order):
    pairs = [d for d in order if d != Z]
    events = [(k, f) for k in range(NZ) for f in subsets(pairs)]
    return sorted(events, key=lambda e: (e[0] + len(e[1]), len(e[1])))


def gather_sends(order, k, flips):
    z_at = order.index(Z)
    last = max([order.index(d) for d in flips] + ([z_at] if k > 0 else []) + [-1])
    out = []
    for position, d in enumerate(order):
        if position > last:
            out.extend([UP, DOWN] if d == Z else [d])
    if k > 0 and last == z_at:
        out.extend([UP, DOWN])
    return out


def gather_kernel(plans, n_in, *refs):
    ins, (first_w, second_w), outs = refs[:n_in], refs[n_in : n_in + 2], refs[n_in + 2 : 2 * n_in + 2]
    mine, other, send_sem, recv_sem, own_sem, stage, load_sem, store_sem = refs[2 * n_in + 2 :]
    place = Place()
    held = mine.shape[0]
    split = first_w.shape[2]
    loads = []
    for side in range(2):
        base = (place.at[C] if side == 0 else 1 - place.at[C]) * held
        for e in range(held):
            to = stage.at[side * held + e]
            for w, at in ((first_w, pl.ds(0, split)), (second_w, pl.ds(split, second_w.shape[2]))):
                loads.append(pltpu.make_async_copy(w.at[base + e], to.at[:, at], load_sem.at[len(loads)]))
    for copy in loads:
        copy.start()
    stores = [
        pltpu.make_async_copy(stage.at[pl.ds(n * held, held)], out, store_sem.at[n]) for n, out in enumerate((mine, other))
    ]
    z = place.at[Z]
    greet(place, sorted({d for p in plans for d in p.order}))
    pending = []
    slot = 0
    queue = []
    for n, plan in enumerate(plans):
        for rank, event in enumerate(gather_events(plan.order)):
            queue.append((rank / len(gather_events(plan.order)), n, event))
    queue.sort(key=lambda q: (q[0], q[1]))
    bases = [sum(p.blocks for p in plans[:n]) for n in range(len(plans))]
    for turn_at, (_, n, (k, flips)) in enumerate(queue):
        if turn_at == len(queue) // 3:
            for copy in loads:
                copy.wait()
            for copy in stores:
                copy.start()
        plan = plans[n]
        src = ins[plan.ref]
        out = outs[plan.ref]
        rows = plan.rows
        z_from = place.order[k]
        spot = place.coords(z_from, flips)
        index = flat_index(spot, plan.index)
        own = k == 0 and not flips
        if plan.view is not None:
            target = plan.view(out, spot, rows)
            source = src.at[:, pl.ds(rows[0], rows[1])] if own else target
        else:
            target = out.at[index] if rows is None else out.at[index, pl.ds(rows[0], rows[1])]
            source = (src if rows is None else src.at[pl.ds(rows[0], rows[1])]) if own else target
        sem = recv_sem.at[bases[n] + index]
        if not own:
            pltpu.make_async_remote_copy(
                src_ref=target, dst_ref=target, send_sem=own_sem.at[0], recv_sem=sem,
                device_id=place.across(C), device_id_type=DEV,
            ).wait_recv()
        for way in gather_sends(plan.order, k, flips):
            if way in (UP, DOWN):
                step = 1 if way == UP else -1
                go = z < NZ - 1 if way == UP else z > 0
                if k > 0:
                    go = jnp.logical_and(go, z_from < z if way == UP else z_from > z)
                dest = place.device(Z, jnp.clip(z + step, 0, NZ - 1))
            else:
                go, dest = None, place.across(way)
            copy = pltpu.make_async_remote_copy(
                src_ref=source, dst_ref=target, send_sem=send_sem.at[slot], recv_sem=sem,
                device_id=dest, device_id_type=DEV,
            )
            slot += 1
            if go is None:
                copy.start()
            else:
                pl.when(go)(copy.start)
            pending.append((go, copy.wait_send))
        if own:
            copy = pltpu.make_async_copy(source, target, own_sem.at[1 + n])
            copy.start()
            pending.append((None, copy.wait))
    for copy in stores:
        copy.wait()
    for go, wait in pending:
        if go is None:
            wait()
        else:
            pl.when(go)(wait)


def gather_weights(arrays, experts, plans, collective_id):
    n = len(arrays)
    sends = sum(len(gather_sends(p.order, k, f)) for p in plans for k, f in gather_events(p.order))
    blocks = {p.ref: p.blocks for p in plans}
    held = experts[0].shape[0] // NC
    pack = (held, experts[0].shape[1], experts[0].shape[2] + experts[1].shape[2])
    apart = pl.BlockSpec(memory_space=pl.ANY)
    dma = pltpu.SemaphoreType.DMA
    return pl.pallas_call(
        functools.partial(gather_kernel, plans, n),
        out_shape=[jax.ShapeDtypeStruct((blocks[i],) + a.shape, a.dtype) for i, a in enumerate(arrays)]
        + [jax.ShapeDtypeStruct(pack, experts[0].dtype)] * 2,
        in_specs=[pl.BlockSpec(memory_space=pltpu.VMEM)] * n + [apart] * 2,
        out_specs=[apart] * (n + 2),
        scratch_shapes=[
            dma((sends,)),
            dma((sum(p.blocks for p in plans),)),
            dma((1 + len(plans),)),
            pltpu.VMEM((NC * held,) + pack[1:], experts[0].dtype),
            dma((2 * NC * held,)),
            dma((2,)),
        ],
        compiler_params=pltpu.CompilerParams(collective_id=collective_id, has_side_effects=True),
        name="gather_weights",
    )(*arrays, *experts)


def add_into(acc, other):
    acc[...] = (acc[...].astype(jnp.float32) + other[...].astype(jnp.float32)).astype(acc.dtype)


class Gather:
    def __init__(self, place, plan, src, out, send_sem, recv_sem, spare_sem, slot, base):
        self.place, self.plan, self.src, self.out = place, plan, src, out
        self.send_sem, self.recv_sem, self.spare_sem = send_sem, recv_sem, spare_sem
        self.slot, self.base = slot, base
        self.pending = []

    @staticmethod
    def sends(plan):
        return sum(len(gather_sends(plan.order, k, f)) for k, f in gather_events(plan.order))

    def goes(self, way, k):
        z, z_from = self.place.at[Z], self.place.order[k]
        if way == UP:
            return z < NZ - 1 if k == 0 else jnp.logical_and(z < NZ - 1, z_from < z)
        return z > 0 if k == 0 else jnp.logical_and(z > 0, z_from > z)

    def part(self, ref):
        rows = self.plan.rows
        return ref if rows is None else ref.at[pl.ds(rows[0], rows[1])]

    def step(self, k, flips):
        place, plan = self.place, self.plan
        index = flat_index(place.coords(place.order[k], flips), plan.index)
        target = self.part(self.out.at[index])
        sem = self.recv_sem.at[self.base + index]
        source = target
        if k == 0 and not flips:
            source = self.part(self.src)
        else:
            pltpu.make_async_remote_copy(
                src_ref=target, dst_ref=target, send_sem=self.spare_sem, recv_sem=sem,
                device_id=place.across(C), device_id_type=DEV,
            ).wait_recv()
        for way in gather_sends(plan.order, k, flips):
            if way in (UP, DOWN):
                dest = place.device(Z, jnp.clip(place.at[Z] + (1 if way == UP else -1), 0, NZ - 1))
            else:
                dest = place.across(way)
            copy = pltpu.make_async_remote_copy(
                src_ref=source, dst_ref=target, send_sem=self.send_sem.at[self.slot], recv_sem=sem,
                device_id=dest, device_id_type=DEV,
            )
            if way in (UP, DOWN):
                pl.when(self.goes(way, k))(copy.start)
            else:
                copy.start()
            self.pending.append((way, k, self.slot))
            self.slot += 1

    def finish(self):
        for way, k, slot in self.pending:
            block = self.part(self.src)
            copy = pltpu.make_async_remote_copy(
                src_ref=block, dst_ref=block, send_sem=self.send_sem.at[slot], recv_sem=self.spare_sem,
                device_id=self.place.across(C), device_id_type=DEV,
            )
            if way in (UP, DOWN):
                pl.when(self.goes(way, k))(copy.wait_send)
            else:
                copy.wait_send()


class Reduce:
    def __init__(self, place, plan, held, levels, chain, send_sem, recv_sem, spare_sem):
        self.place, self.plan, self.held, self.levels, self.chain = place, plan, held, levels, chain
        self.send_sem, self.recv_sem, self.spare_sem = send_sem, recv_sem, spare_sem
        dims = plan.order
        self.kept = [subsets(dims[p + 1 :]) for p in range(len(dims))]
        self.base = [NZ * sum(len(f) for f in self.kept[:p]) for p in range(len(dims) + 1)]
        self.slot = 0

    @staticmethod
    def counts(plan):
        kept = [NZ * len(subsets(plan.order[p + 1 :])) for p in range(len(plan.order))]
        return kept, sum(kept) + NZ - 1, sum(kept) + NZ + 1

    def push(self, source, target, sem, dest):
        copy = pltpu.make_async_remote_copy(
            src_ref=source, dst_ref=target, send_sem=self.send_sem.at[self.slot], recv_sem=sem,
            device_id=dest, device_id_type=DEV,
        )
        self.slot += 1
        copy.start()

    def arrived(self, target, sem):
        pltpu.make_async_remote_copy(
            src_ref=target, dst_ref=target, send_sem=self.spare_sem, recv_sem=sem,
            device_id=self.place.across(C), device_id_type=DEV,
        ).wait_recv()

    def block(self, k, flips):
        return flat_index(self.place.coords(self.place.order[k], flips), self.plan.index)

    def first(self, k):
        dim = self.plan.order[0]
        for n, f in enumerate(self.kept[0]):
            spot = self.place.order[k] * len(self.kept[0]) + n
            self.push(
                self.held.at[self.block(k, (dim,) + f)], self.levels[0].at[spot],
                self.recv_sem.at[spot], self.place.across(dim),
            )

    def level(self, p, k):
        dims = self.plan.order
        z_to = self.place.order[k]
        for f in sorted(self.kept[p], key=lambda f: -len(f)):
            spot = z_to * len(self.kept[p]) + self.kept[p].index(f)
            mine = self.held.at[self.block(k, f)]
            self.arrived(self.levels[p].at[spot], self.recv_sem.at[self.base[p] + spot])
            add_into(mine, self.levels[p].at[spot])
            later = p + 1
            if later < len(dims) and dims[later] in f:
                left = tuple(d for d in f if d != dims[later])
                there = z_to * len(self.kept[later]) + self.kept[later].index(left)
                self.push(
                    mine, self.levels[later].at[there],
                    self.recv_sem.at[self.base[later] + there], self.place.across(dims[later]),
                )

    def along(self, k):
        z = self.place.at[Z]
        dest = self.place.order[k]
        up = dest > z
        spot = dest + jnp.where(up, 1, 0)
        mine = self.held.at[self.block(k, ())]
        sem = self.recv_sem.at[self.base[-1] + spot]

        @pl.when(jnp.where(up, z > 0, z < NZ - 1))
        def _():
            self.arrived(self.chain.at[spot], sem)
            add_into(mine, self.chain.at[spot])

        self.push(mine, self.chain.at[spot], sem, self.place.along(jnp.where(up, 1, -1)))

    def last(self, out, base=None):
        z = self.place.at[Z]
        mine = self.held.at[self.block(0, ())]
        for go, spot in ((z > 0, z + 1), (z < NZ - 1, z)):

            @pl.when(go)
            def _():
                self.arrived(self.chain.at[spot], self.recv_sem.at[self.base[-1] + spot])
                add_into(mine, self.chain.at[spot])

        total = mine[...].astype(jnp.float32)
        if base is not None:
            total = base[...] + total
        out[...] = total.astype(out.dtype)

    def at_time(self, t):
        depth = len(self.plan.order)
        far = list(reversed(range(NZ)))
        out = [functools.partial(self.level, p, far[t - p]) for p in range(depth) if 0 <= t - p < NZ]
        if 0 <= t - depth < NZ - 1:
            out.append(functools.partial(self.along, far[t - depth]))
        return out

    def steps(self):
        return [step for t in range(NZ + len(self.plan.order)) for step in self.at_time(t)]

    def finish(self):
        block = self.levels[0].at[0]
        for slot in range(self.slot):
            pltpu.make_async_remote_copy(
                src_ref=block, dst_ref=block, send_sem=self.send_sem.at[slot], recv_sem=self.spare_sem,
                device_id=self.place.across(C), device_id_type=DEV,
            ).wait_send()


def tile_up(n, m):
    return (n + m - 1) // m * m


def columns_of(width, chunk=512):
    return [(i, min(chunk, width - i)) for i in range(0, width, chunk)]


def moe_kernel(plans, back, width, hidden, cap, *refs):
    payload, cots, w_own, w_core, w_x, w_both = refs[:6]
    gin_out, part_out = refs[6:8]
    grads = refs[8:12]
    (
        seen, cot_seen, weights, taken, cot_taken, rows_buf, scaled, grad_act, pick, stage,
        lvl_b0, lvl_b1, chain_b,
        send_sem, recv_sem, spare_sem, send_b, recv_b, load_sem, store_sem, part_sem,
    ) = refs[12:]
    bf, f32 = jnp.bfloat16, jnp.float32
    place = Place()
    count = payload.shape[0]
    pair = 2 * cap
    wide = width + 128
    quarter = width // (NX * NC)
    half = NZ * pair
    lanes = pick.shape[2]
    held = weights.shape[0]
    fsdp = place.at[X] * NC + place.at[C]
    first = (((place.at[Z] * NY + place.at[Y]) * NC) + place.at[C]) * held

    loads = []
    for j, ref in enumerate((w_own, w_core, w_x, w_both)):
        rows = pl.ds(pl.multiple_of((fsdp ^ j) * quarter, quarter), quarter)
        for e in range(held):
            loads.append(pltpu.make_async_copy(ref.at[e], weights.at[e, rows], load_sem.at[len(loads)]))
    base_of = lambda h, k: (jnp.where(h == 0, place.at[C], 1 - place.at[C]) * NZ + place.order[k]) * NY
    cot_loads = {}
    for k in range(NZ):
        for h in range(2):
            at = pl.ds(base_of(h, k), NY)
            cot_loads[(h, k)] = pltpu.make_async_copy(cots.at[at], cot_seen.at[at], load_sem.at[len(loads) + len(cot_loads)])

    greet(place, (Z, Y, C))
    ways = []
    send_at = 0
    for n, plan in enumerate(plans):
        ways.append(Gather(place, plan, payload, seen, send_sem, recv_sem, spare_sem, send_at, n * plan.blocks))
        send_at += Gather.sends(plan)
    for way in ways:
        way.step(0, ())
    for key in cot_loads:
        cot_loads[key].start()
    for copy in loads:
        copy.start()
    seen[flat_index(place.at, plans[0].index)] = payload[...]

    row_id = lax.broadcasted_iota(jnp.int32, (NY * count, NY * count), 0)
    col_id = lax.broadcasted_iota(jnp.int32, (NY * count, NY * count), 1)
    earlier = jnp.logical_and(col_id < row_id, col_id // count == row_id // count).astype(bf)
    lane_id = lax.broadcasted_iota(jnp.int32, (1, 128), 1)
    here = [(lane_id == first + e).astype(f32) for e in range(held)]
    pick_lane = lax.broadcasted_iota(jnp.int32, (NY * count, lanes), 1).astype(f32)
    y_shift = (lax.broadcasted_iota(jnp.int32, (NY * count, 1), 0) // count * cap).astype(f32)

    row_of = lambda h, k: (k * NC + h) * pair

    def dispatch(source, target, h, k, cols):
        at = pl.ds(base_of(h, k), NY)
        r = row_of(h, k)
        for c0, cn in cols:
            block = source[at, :, c0 : c0 + cn].reshape(NY * count, cn)
            got = lax.dot_general(
                pick[h * NZ + k], block, (((0,), (0,)), ((), ())), preferred_element_type=f32
            ).astype(bf)
            for e in range(held):
                target[e, r : r + pair, c0 : c0 + cn] = got[e * pair : (e + 1) * pair]

    def cot_chunk(h, k):
        cot_loads[(h, k)].wait()
        at = pl.ds(base_of(h, k), NY)
        chosen = cot_seen[at, :, width:wide].reshape(NY * count, 128)
        before = jnp.dot(earlier, chosen, preferred_element_type=f32)
        picked = None
        for e in range(held):
            is_here = jnp.sum(chosen.astype(f32) * here[e], axis=1, keepdims=True)
            slot = jnp.sum(before * here[e], axis=1, keepdims=True) + y_shift + e * pair
            target = jnp.where(is_here > 0.5, slot, -1.0)
            hit = pick_lane == target
            picked = hit if picked is None else jnp.logical_or(picked, hit)
        pick[h * NZ + k] = picked.astype(f32).astype(bf)
        dispatch(cot_seen, cot_taken, h, k, columns_of(width))

    def hidden_chunk(h, e, n, tile):
        rows = pl.ds(h * half, half)
        tokens_in = taken[e, rows, :width]
        gate = jnp.sum(taken[e, rows, width:wide].astype(f32) * here[e], axis=1, keepdims=True)
        col = n * tile
        g = jnp.dot(tokens_in, weights[e, :, col : col + tile], preferred_element_type=f32)
        u = jnp.dot(tokens_in, weights[e, :, hidden + col : hidden + col + tile], preferred_element_type=f32)
        raw = jnp.dot(
            cot_taken[e, rows, :], weights[e, :, 2 * hidden + col : 2 * hidden + col + tile], preferred_element_type=f32
        )
        s = jax.nn.sigmoid(g)
        gs = g * s
        inner = gs * u
        scaled[e, rows, col : col + tile] = (inner * gate).astype(bf)
        grad_inner = raw * gate
        grad_act[e, rows, col : col + tile] = (grad_inner * u * s * (1.0 + g * (1.0 - s))).astype(bf)
        grad_act[e, rows, hidden + col : hidden + col + tile] = (grad_inner * gs).astype(bf)
        return jnp.sum(raw * inner, axis=1, keepdims=True)

    tile = min(256, hidden)
    found = {}

    def hidden_step(h, e, n):
        got = hidden_chunk(h, e, n, tile)
        found[(h, e)] = got if n == 0 else found[(h, e)] + got
        if n == hidden // tile - 1:
            gate_grad = found.pop((h, e))
            high = gate_grad.astype(bf).astype(f32)
            there = pl.ds(h * half, half)
            apart = (lane_id == EXPERT_COUNT + first + e).astype(f32)
            rows_buf[e, there, width:wide] = (high * here[e] + (gate_grad - high) * apart).astype(bf)

    def hidden_steps(h):
        return [functools.partial(hidden_step, h, e, n) for e in range(held) for n in range(hidden // tile)]

    def project(h, e, left, weight_cols):
        rows = pl.ds(h * half, half)
        lo, n = weight_cols
        for c0, cn in columns_of(width):
            rows_buf[e, rows, c0 : c0 + cn] = lax.dot_general(
                left[e, rows, :], weights[e, c0 : c0 + cn, lo : lo + n], (((1,), (1,)), ((), ())), preferred_element_type=f32
            ).astype(bf)

    def combine(target, h, k, cols):
        at = pl.ds(base_of(h, k), NY)
        r = row_of(h, k)
        for c0, cn in cols:
            parts = [rows_buf[e, r : r + pair, c0 : c0 + cn] for e in range(held)]
            if lanes > held * pair:
                parts.append(jnp.zeros((lanes - held * pair, cn), bf))
            got = jnp.dot(pick[h * NZ + k], jnp.concatenate(parts, axis=0), preferred_element_type=f32)
            target[at, :, c0 : c0 + cn] = got.astype(bf).reshape(NY, count, cn)

    stores = []

    def weight_grad(e, j):
        rows = pl.ds(pl.multiple_of((fsdp ^ j) * quarter, 128), quarter)
        slot = len(stores) % 2
        if len(stores) >= 2:
            stores[-2].wait()
        for c0, cn in columns_of(2 * hidden):
            stage[slot, :, c0 : c0 + cn] = lax.dot_general(
                taken[e, :, rows], grad_act[e, :, c0 : c0 + cn], (((0,), (0,)), ((), ())), preferred_element_type=f32
            ).astype(bf)
        stage[slot, :, 2 * hidden :] = lax.dot_general(
            cot_taken[e, :, rows], scaled[e], (((0,), (0,)), ((), ())), preferred_element_type=f32
        ).astype(bf)
        copy = pltpu.make_async_copy(stage.at[slot], grads[j].at[e], store_sem.at[len(stores)])
        copy.start()
        stores.append(copy)

    work = [functools.partial(cot_chunk, h, k) for h in range(NC) for k in range(NZ)]
    all_cols = columns_of(width) + [(width, 128)]
    ready = {(h, k): 0 for h in range(NC) for k in range(NZ)}
    ready[(0, 0)] = 1
    near_begun = False

    def wait_weights():
        for copy in loads:
            copy.wait()

    for k, flips in gather_events(plans[0].order)[1:]:
        for way in ways:
            way.step(k, flips)
        key = (1 if C in flips else 0, k)
        ready[key] += 1
        if ready[key] == NY:
            work.append(functools.partial(dispatch, seen, taken, *key, all_cols))
            if all(ready[(g, n)] == NY for g in range(NC) for n in range(NZ // 2)) and not near_begun:
                near_begun = True
                work += [wait_weights] + hidden_steps(0)
        for _ in range(min(len(work), 1 if k < NZ - 1 else 2)):
            work.pop(0)()
    for chunk in work:
        chunk()
    for chunk in hidden_steps(1):
        chunk()

    far = list(reversed(range(NZ)))
    spare = spare_sem
    in_way = Reduce(place, back, cot_seen, (lvl_b0, lvl_b1), chain_b, send_b, recv_b, spare)
    in_steps = in_way.steps()
    for e in range(held):
        project(1, e, grad_act, (0, 2 * hidden))
    for k in far[: NZ // 2]:
        combine(cot_seen, 1, k, all_cols)
        in_way.first(k)
    for k in far[: NZ // 2]:
        combine(cot_seen, 0, k, all_cols)
    in_steps.pop(0)()
    for e in range(held):
        project(0, e, grad_act, (0, 2 * hidden))
    in_steps.pop(0)()
    for k in far[NZ // 2 :]:
        combine(cot_seen, 1, k, all_cols)
        in_way.first(k)
    in_steps.pop(0)()
    for k in far[NZ // 2 :]:
        combine(cot_seen, 0, k, all_cols)
    for way in ways:
        way.finish()
    part_copies = []
    work = []

    def out_part(h, k):
        combine(seen, h, k, columns_of(width))
        at = pl.ds(base_of(h, k), NY)
        copy = pltpu.make_async_copy(seen.at[at, :, pl.ds(0, width)], part_out.at[at], part_sem.at[len(part_copies)])
        copy.start()
        part_copies.append(copy)

    for n in range(2):
        for e in range(held):
            work.append(functools.partial(project, n, e, scaled, (2 * hidden, hidden)))
        for k in range(n * NZ // 2, (n + 1) * NZ // 2):
            for h in range(NC):
                work.append(functools.partial(out_part, h, k))
    work += [functools.partial(weight_grad, e, j) for j in reversed(range(NX * NC)) for e in range(held)]
    while in_steps or work:
        if in_steps:
            in_steps.pop(0)()
        for _ in range(2):
            if work:
                work.pop(0)()
    in_way.last(gin_out)
    for copy in stores[-2:] + part_copies:
        copy.wait()
    in_way.finish()


def moe(payload, cots, parts, cap, collective_id):
    count, wide = payload.shape
    width = wide - 128
    held, quarter, columns = parts[0].shape
    hidden = columns // 3
    cut = count * 3 // 4
    plans = [
        Plan(0, (Z, Y, C), (C, Z, Y), rows=(0, cut)),
        Plan(0, (Y, Z, C), (C, Z, Y), rows=(cut, count - cut)),
    ]
    back = Plan(0, (C, Y), (C, Z, Y))
    levels, sends, recvs = Reduce.counts(back)
    blocks = NC * NZ * NY
    pair = NY * cap
    rows = blocks // NY * pair
    lanes = tile_up(held * pair, 128)
    bf, f32 = jnp.bfloat16, jnp.float32
    whole = pl.BlockSpec(memory_space=pltpu.VMEM)
    apart = pl.BlockSpec(memory_space=pl.ANY)
    dma = pltpu.SemaphoreType.DMA
    return pl.pallas_call(
        functools.partial(moe_kernel, plans, back, width, hidden, cap),
        out_shape=[
            jax.ShapeDtypeStruct((count, wide), f32),
            jax.ShapeDtypeStruct((blocks, count, width), bf),
        ]
        + [jax.ShapeDtypeStruct((held, quarter, columns), bf)] * (NX * NC),
        in_specs=[whole] + [apart] * 5,
        out_specs=[whole] + [apart] * (1 + NX * NC),
        scratch_shapes=[
            pltpu.VMEM((blocks, count, wide), bf),
            pltpu.VMEM((blocks, count, wide), bf),
            pltpu.VMEM((held, NX * NC * quarter, columns), bf),
            pltpu.VMEM((held, rows, wide), bf),
            pltpu.VMEM((held, rows, width), bf),
            pltpu.VMEM((held, rows, wide), bf),
            pltpu.VMEM((held, rows, hidden), bf),
            pltpu.VMEM((held, rows, 2 * hidden), bf),
            pltpu.VMEM((blocks // NY, NY * count, lanes), bf),
            pltpu.VMEM((2, quarter, columns), bf),
        ]
        + [pltpu.VMEM((n, count, wide), bf) for n in levels + [NZ + 1]]
        + [
            dma((sum(Gather.sends(p) for p in plans),)),
            dma((sum(p.blocks for p in plans),)),
            dma(()),
            dma((sends,)),
            dma((recvs,)),
            dma((held * NX * NC + blocks // NY,)),
            dma((held * NX * NC,)),
            dma((blocks // NY,)),
        ],
        compiler_params=pltpu.CompilerParams(
            collective_id=collective_id, has_side_effects=True, vmem_limit_bytes=67043328
        ),
        name="experts",
    )(payload, cots, *parts)


def weights_kernel(plans, *refs):
    left_one, right_one, left_two, right_two, left_small, right_small = refs[:6]
    outs = refs[6:8]
    held_one, held_two = refs[8:10]
    buffers = refs[10:18]
    send_one, recv_one, send_two, recv_two, spare = refs[18:]
    place = Place()
    far = list(reversed(range(NZ)))
    greet(place, (Z, Y, X, C))
    ways = [
        Reduce(place, plans[0], held_one, buffers[0:3], buffers[3], send_one, recv_one, spare),
        Reduce(place, plans[1], held_two, buffers[4:7], buffers[7], send_two, recv_two, spare),
    ]
    group = NY * NX * NC
    rows = group * held_one.shape[1]

    def products(left, right, held, k, shift):
        at = pl.ds(pl.multiple_of(place.order[k] * rows, 128), rows)
        block = left[:, at]
        for c0, cn in columns_of(right.shape[1]):
            got = lax.dot_general(
                block, right[:, c0 : c0 + cn], (((0,), (0,)), ((), ())), preferred_element_type=jnp.float32
            )
            held[pl.ds(place.order[k] * group, group), :, shift + c0 : shift + c0 + cn] = got.astype(
                held.dtype
            ).reshape(group, rows // group, cn)

    for t in range(NZ):
        k = far[t]
        products(left_one, right_one, held_one, k, 0)
        ways[0].first(k)
        products(left_two, right_two, held_two, k, 0)
        products(left_small, right_small, held_two, k, right_two.shape[1])
        ways[1].first(k)
        if t > 0:
            for way in ways:
                for step in way.at_time(t - 1):
                    step()
    for t in range(NZ - 1, NZ + 3):
        for way in ways:
            for step in way.at_time(t):
                step()
    for way, out in zip(ways, outs):
        way.last(out)
    for way in ways:
        way.finish()


def return_weights(lefts, rights, collective_id):
    width = lefts[0].shape[1]
    rows = width // (NZ * NY * NX * NC)
    widths = [rights[0].shape[1], rights[1].shape[1] + rights[2].shape[1]]
    plans = [Plan(0, (C, Y, X), (Z, Y, X, C)), Plan(1, (C, X, Y), (Z, Y, X, C))]
    bf = jnp.bfloat16
    levels, sends, recvs = Reduce.counts(plans[0])
    dma = pltpu.SemaphoreType.DMA
    vmem = pl.BlockSpec(memory_space=pltpu.VMEM)
    return pl.pallas_call(
        functools.partial(weights_kernel, plans),
        out_shape=[jax.ShapeDtypeStruct((rows, w), jnp.float32) for w in widths],
        in_specs=[vmem] * 6,
        out_specs=[vmem] * 2,
        scratch_shapes=[pltpu.VMEM((plans[0].blocks, rows, w), bf) for w in widths]
        + [pltpu.VMEM((n, rows, w), bf) for w in widths for n in levels + [NZ + 1]]
        + [dma((n,)) for n in (sends, recvs, sends, recvs)]
        + [dma(())],
        compiler_params=pltpu.CompilerParams(
            collective_id=collective_id, has_side_effects=True, vmem_limit_bytes=60 * 1024 * 1024
        ),
        name="return_weights",
    )(*[a for pair in zip(lefts, rights) for a in pair])


def turn(block, cosine, sine):
    lane = lax.broadcasted_iota(jnp.int32, (1, 128), 1)
    half = HEAD_SIZE // 2
    other = jnp.where(lane % HEAD_SIZE < half, pltpu.roll(block, 128 - half, 1), pltpu.roll(block, half, 1))
    return block * cosine + other * sine


def place_heads(read, target, count):
    group = QUERY_HEADS // KEY_VALUE_HEADS
    lane = lax.broadcasted_iota(jnp.int32, (1, 2 * HEAD_SIZE), 1)
    for pair in range(QUERY_HEADS // 2):
        both = read(pair)
        for h in (2 * pair, 2 * pair + 1):
            m, g = h // group, h % group
            block = both if h % 2 == m % 2 else pltpu.roll(both, HEAD_SIZE, 1)
            block = jnp.where(lane // HEAD_SIZE == m % 2, block, 0.0)
            target[m, g * count : (g + 1) * count] = block.astype(target.dtype)


def collect_heads(source, target, count, finish):
    group = QUERY_HEADS // KEY_VALUE_HEADS
    lane = lax.broadcasted_iota(jnp.int32, (1, 2 * HEAD_SIZE), 1)
    for pair in range(QUERY_HEADS // 2):
        sides = []
        for h in (2 * pair, 2 * pair + 1):
            m, g = h // group, h % group
            block = source[m, g * count : (g + 1) * count]
            sides.append(block if h % 2 == m % 2 else pltpu.roll(block, HEAD_SIZE, 1))
        both = finish(jnp.where(lane < HEAD_SIZE, *sides))
        target[:, pair * 128 : pair * 128 + 128] = both.astype(target.dtype)


class Scores:
    def __init__(self, place, queries, keys):
        self.queries, self.keys = queries, keys
        group = QUERY_HEADS // KEY_VALUE_HEADS
        count = keys.shape[1]
        self.total = keys.shape[0] * count
        row = lax.broadcasted_iota(jnp.int32, (group * count, 1), 0) % count
        self.position = row + (place.at[Z] * NY + place.at[Y]) * count
        self.column = lax.broadcasted_iota(jnp.int32, (1, self.total), 1)

    def pair(self, m, shift):
        at = pl.ds(pl.multiple_of(shift + m // 2 * 128, 128), 128)
        return self.keys[:, :, at].reshape(self.total, 128)

    def of(self, m, keys):
        found = lax.dot_general(
            self.queries[m], keys, (((1,), (1,)), ((), ())), preferred_element_type=jnp.float32
        )
        return jnp.where(self.column <= self.position, found * attn_scale, masked_logits)


def attend_kernel(
    plans, linear, cot, routes, cosine, sine, out, log_sums, kv_out, cots, placed, seen, own_kv, own_cots, raw, *sems
):
    send_kv, recv_kv, send_cot, recv_cot, spare, own_sem = sems
    place = Place()
    bf, f32 = jnp.bfloat16, jnp.float32
    count = linear.shape[0]
    width = KEY_VALUE_HEADS * HEAD_SIZE
    q_width = QUERY_HEADS * HEAD_SIZE
    for c0 in range(0, width, 128):
        block = linear[:, q_width + c0 : q_width + c0 + 128]
        own_kv[:, c0 : c0 + 128] = turn(block, cosine[...], sine[...]).astype(bf)
    own_kv[:, width:] = linear[:, q_width + width :].astype(bf)
    model = cot.shape[1]
    own_cots[:, :model] = cot[...].astype(bf)
    expert = lax.broadcasted_iota(jnp.int32, (1, 128), 1)
    routed = routes[:, 0:1] == expert
    for n in range(1, routes.shape[1]):
        routed = jnp.logical_or(routed, routes[:, n : n + 1] == expert)
    own_cots[:, model:] = routed.astype(f32).astype(bf)
    greet(place, (Z, Y, C))
    kv_way = Gather(place, plans[0], own_kv, seen, send_kv, recv_kv, spare, 0, 0)
    cot_ways, at = [], 0
    for n, plan in enumerate(plans[1:]):
        cot_ways.append(Gather(place, plan, own_cots, cots, send_cot, recv_cot, spare, at, n * plan.blocks))
        at += Gather.sends(plan)
    kv_way.step(0, ())
    for way in cot_ways:
        way.step(0, ())
    mine = pltpu.make_async_copy(own_cots, cots.at[flat_index(place.at, plans[1].index)], own_sem.at[0])
    mine.start()
    seen[flat_index(place.at, plans[0].index)] = own_kv[...]
    place_heads(lambda pair: turn(linear[:, pair * 128 : pair * 128 + 128], cosine[...], sine[...]), placed, count)
    log_sums[...] = jnp.zeros(log_sums.shape, f32)
    early = [e for e in gather_events(plans[1].order)[1:]]
    kv_events = gather_events(plans[0].order)[1:]
    for k, flips in kv_events:
        kv_way.step(k, flips)
        if len(early) > 8:
            event = early.pop(0)
            for way in cot_ways:
                way.step(*event)
    keep = pltpu.make_async_copy(seen, kv_out, own_sem.at[1])
    keep.start()
    scores = Scores(place, placed, seen)
    lane = lax.broadcasted_iota(jnp.int32, (1, 128), 1)

    def head(m, carry):
        for i in range(KEY_VALUE_HEADS):
            if early:
                event = early.pop(0)

                @pl.when(m == i)
                def _():
                    for way in cot_ways:
                        way.step(*event)

        s = scores.of(m, scores.pair(m, 0))
        best = jnp.max(s, axis=1, keepdims=True)
        weights = jnp.exp(s - best)
        total = jnp.sum(weights, axis=1, keepdims=True)
        mixed = jnp.dot(weights.astype(bf), scores.pair(m, width), preferred_element_type=f32)
        raw[m] = mixed / total
        log_sums[...] = jnp.where(lane == m, best + jnp.log(total), log_sums[...])
        return carry

    lax.fori_loop(0, KEY_VALUE_HEADS, head, 0)
    collect_heads(raw, out, count, lambda block: block)
    keep.wait()
    mine.wait()
    kv_way.finish()
    for way in cot_ways:
        way.finish()


def attend(linear, cot, routes, cosine, sine, collective_id):
    count = linear.shape[0]
    kv_width = 2 * KEY_VALUE_HEADS * HEAD_SIZE
    cut = count * 3 // 4
    plans = [
        Plan(0, (Z, Y), (Z, Y)),
        Plan(1, (Z, Y, C), (C, Z, Y), rows=(0, cut)),
        Plan(1, (Y, Z, C), (C, Z, Y), rows=(cut, count - cut)),
    ]
    bf, f32 = jnp.bfloat16, jnp.float32
    group = QUERY_HEADS // KEY_VALUE_HEADS
    vmem = pl.BlockSpec(memory_space=pltpu.VMEM)
    apart = pl.BlockSpec(memory_space=pl.ANY)
    dma = pltpu.SemaphoreType.DMA
    kv_shape = (plans[0].blocks, count, kv_width)
    cot_shape = (count, cot.shape[1] + 128)
    heads = (KEY_VALUE_HEADS, group * count, 2 * HEAD_SIZE)
    return pl.pallas_call(
        functools.partial(attend_kernel, plans),
        out_shape=[
            jax.ShapeDtypeStruct((count, QUERY_HEADS * HEAD_SIZE), bf),
            jax.ShapeDtypeStruct((group * count, 128), f32),
            jax.ShapeDtypeStruct(kv_shape, bf),
            jax.ShapeDtypeStruct((plans[1].blocks,) + cot_shape, bf),
            jax.ShapeDtypeStruct(heads, bf),
        ],
        in_specs=[vmem] * 5,
        out_specs=[vmem, vmem, apart, apart, vmem],
        scratch_shapes=[
            pltpu.VMEM(kv_shape, bf),
            pltpu.VMEM((count, kv_width), bf),
            pltpu.VMEM(cot_shape, bf),
            pltpu.VMEM(heads, f32),
        ]
        + [
            dma((Gather.sends(plans[0]),)),
            dma((plans[0].blocks,)),
            dma((Gather.sends(plans[1]) + Gather.sends(plans[2]),)),
            dma((plans[1].blocks + plans[2].blocks,)),
            dma(()),
            dma((2,)),
        ],
        compiler_params=pltpu.CompilerParams(
            collective_id=collective_id, has_side_effects=True, vmem_limit_bytes=56 * 1024 * 1024
        ),
        name="attend",
    )(linear, cot, routes, cosine, sine)


def attend_back_kernel(plans, *refs):
    placed, grads, outputs, log_sums, keys, part, mixed, cosine, sine = refs[:9]
    back, layer_out = refs[9:11]
    kv_grad, grads_placed, raw, deltas, held, held_out = refs[11:17]
    level, chain, out_level, out_level_two, out_chain = refs[17:22]
    send_kv, recv_kv, send_out, recv_out, spare, load_sem = refs[22:]
    place = Place()
    bf, f32 = jnp.bfloat16, jnp.float32
    far = list(reversed(range(NZ)))
    loads = []
    for k in far:
        for h in (1 - place.at[C], place.at[C]):
            at = pl.ds((h * NZ + place.order[k]) * NY, NY)
            loads.append(pltpu.make_async_copy(part.at[at], held_out.at[at], load_sem.at[len(loads)]))
    for copy in loads:
        copy.start()
    greet(place, (Z, Y, C))
    kv_way = Reduce(place, plans[0], held, (level,), chain, send_kv, recv_kv, spare)
    out_way = Reduce(place, plans[1], held_out, (out_level, out_level_two), out_chain, send_out, recv_out, spare)
    for copy in loads:
        copy.wait()
    for k in far:
        out_way.first(k)
    count = grads.shape[0]
    place_heads(lambda pair: grads[:, pair * 128 : pair * 128 + 128].astype(f32), grads_placed, count)
    group = QUERY_HEADS // KEY_VALUE_HEADS
    lane = lax.broadcasted_iota(jnp.int32, (1, 128), 1)
    for g in range(group):
        found = jnp.zeros((count, 128), f32)
        for m in range(KEY_VALUE_HEADS):
            h = m * group + g
            at = slice(h // 2 * 128, h // 2 * 128 + 128)
            both = grads[:, at].astype(f32) * outputs[:, at].astype(f32)
            delta = jnp.sum(jnp.where(lane // HEAD_SIZE == h % 2, both, 0.0), axis=1, keepdims=True)
            found = jnp.where(lane == m, delta, found)
        deltas[g * count : (g + 1) * count] = found
    scores = Scores(place, placed, keys)
    width = KEY_VALUE_HEADS * HEAD_SIZE
    blocks = keys.shape[0]
    turns = KEY_VALUE_HEADS // 2
    early = [[(out_way.level, 0, 3)], [(out_way.level, 0, 2)], [(out_way.level, 1, 3)], [(out_way.level, 1, 2), (out_way.along, 3)]]

    def pair(p, carry):
        for i in range(turns):

            @pl.when(p == i)
            def _():
                for step, *at in early[i]:
                    step(*at)

        key_sum = value_sum = None
        for side in range(2):
            m = 2 * p + side
            k_pair, v_pair = scores.pair(m, 0), scores.pair(m, width)
            of_head = lambda ref: jnp.sum(jnp.where(lane == m, ref[...], 0.0), axis=1, keepdims=True)
            weights = jnp.exp(scores.of(m, k_pair) - of_head(log_sums))
            grad = grads_placed[m]
            grad_probs = lax.dot_general(grad, v_pair, (((1,), (1,)), ((), ())), preferred_element_type=f32)
            grad_scores = (weights * (grad_probs - of_head(deltas))).astype(bf)
            raw[m] = attn_scale * jnp.dot(grad_scores, k_pair, preferred_element_type=f32)
            over_rows = (((0,), (0,)), ((), ()))
            key_part = lax.dot_general(grad_scores, placed[m], over_rows, preferred_element_type=f32)
            value_part = lax.dot_general(weights.astype(bf), grad, over_rows, preferred_element_type=f32)
            key_sum = key_part if key_sum is None else key_sum + key_part
            value_sum = value_part if value_sum is None else value_sum + value_part
        at = pl.multiple_of(p * 128, 128)
        held[:, :, pl.ds(at, 128)] = (attn_scale * key_sum).astype(bf).reshape(blocks, count, 128)
        at = pl.multiple_of(width + p * 128, 128)
        held[:, :, pl.ds(at, 128)] = value_sum.astype(bf).reshape(blocks, count, 128)
        return carry

    lax.fori_loop(0, turns, pair, 0)
    for k in far:
        kv_way.first(k)
    out_way.level(0, 1)
    out_way.level(0, 0)
    collect_heads(raw, back, count, lambda block: turn(block, cosine[...], -sine[...]))
    kv_way.level(0, 3)
    kv_way.level(0, 2)
    kv_way.along(3)
    kv_way.level(0, 1)
    kv_way.along(2)
    out_way.along(2)
    kv_way.level(0, 0)
    kv_way.along(1)
    kv_way.last(kv_grad)
    q_width = QUERY_HEADS * HEAD_SIZE
    for c0 in range(0, width, 128):
        block = turn(kv_grad[:, c0 : c0 + 128], cosine[...], -sine[...])
        back[:, q_width + c0 : q_width + c0 + 128] = block.astype(bf)
    back[:, q_width + width :] = kv_grad[:, width:].astype(bf)
    out_way.level(1, 1)
    out_way.along(1)
    out_way.level(1, 0)
    out_way.last(layer_out, mixed)
    kv_way.finish()
    out_way.finish()


def attend_back(placed, grads, outputs, log_sums, keys, part, mixed, cosine, sine, collective_id):
    count, kv_width = keys.shape[1:]
    plans = [Plan(0, (Y,), (Z, Y)), Plan(1, (C, Y), (C, Z, Y))]
    bf, f32 = jnp.bfloat16, jnp.float32
    group = QUERY_HEADS // KEY_VALUE_HEADS
    vmem = pl.BlockSpec(memory_space=pltpu.VMEM)
    dma = pltpu.SemaphoreType.DMA
    heads = (KEY_VALUE_HEADS, group * count, 2 * HEAD_SIZE)
    levels, sends, recvs = Reduce.counts(plans[0])
    out_levels, out_sends, out_recvs = Reduce.counts(plans[1])
    return pl.pallas_call(
        functools.partial(attend_back_kernel, plans),
        out_shape=[
            jax.ShapeDtypeStruct((count, grads.shape[1] + kv_width), bf),
            jax.ShapeDtypeStruct(mixed.shape, bf),
        ],
        in_specs=[vmem] * 5 + [pl.BlockSpec(memory_space=pl.ANY)] + [vmem] * 3,
        out_specs=[vmem] * 2,
        scratch_shapes=[
            pltpu.VMEM((count, kv_width), f32),
            pltpu.VMEM(heads, bf),
            pltpu.VMEM(heads, f32),
            pltpu.VMEM((group * count, 128), f32),
            pltpu.VMEM(keys.shape, bf),
            pltpu.VMEM(part.shape, bf),
        ]
        + [pltpu.VMEM((n,) + keys.shape[1:], bf) for n in levels + [NZ + 1]]
        + [pltpu.VMEM((n,) + part.shape[1:], bf) for n in out_levels + [NZ + 1]]
        + [dma((n,)) for n in (sends, recvs, out_sends, out_recvs)]
        + [dma(()), dma((NC * NZ,))],
        compiler_params=pltpu.CompilerParams(
            collective_id=collective_id, has_side_effects=True, vmem_limit_bytes=60 * 1024 * 1024
        ),
        name="attend_back",
    )(placed, grads, outputs, log_sums, keys, part, mixed, cosine, sine)


def last_kernel(core_ref, own, core_part, x_part, both_part, one, two, *outs):
    core = core_ref[0]
    in_out, out_out = outs[:2]
    split = in_out.shape[3]
    for at, left, right in ((core, own, x_part), (1 - core, core_part, both_part)):
        total = left[0].astype(jnp.float32) + right[0].astype(jnp.float32)
        in_out[at, 0] = total[:, :split]
        out_out[at, 0] = total[:, split:]

    @pl.when(jnp.logical_and(pl.program_id(0) == 0, pl.program_id(1) == 0))
    def _():
        wq, wk, wv, wo, router, first_gain, second_gain = outs[2:]
        q, k = wq.shape[1], wk.shape[1]
        wq[...] = one[:, :q]
        wk[...] = one[:, q : q + k]
        wv[...] = one[:, q + k :]
        width = wo.shape[1]
        wo[...] = two[:, :width]
        small = two[:, width:]
        router[...] = small[:, : router.shape[1]]
        turned = small.T
        at = router.shape[1]
        first_gain[...] = turned[at : at + 1]
        second_gain[...] = turned[at + 1 : at + 2]


def last_outputs(pieces, core, split, one, two, widths):
    held, quarter, columns = pieces[0].shape
    step = quarter // 2
    rows = one.shape[0]
    spec = pl.BlockSpec((1, step, columns), lambda e, r, c: (e, r, 0))
    fixed = lambda a, b: pl.BlockSpec((a, b), lambda e, r, c: (0, 0))
    outs = (split, columns - split)
    shapes = [(rows, w) for w in widths] + [(1, rows)] * 2
    return pl.pallas_call(
        last_kernel,
        grid_spec=pltpu.PrefetchScalarGridSpec(
            num_scalar_prefetch=1,
            grid=(held, 2),
            in_specs=[spec] * 4 + [fixed(*one.shape), fixed(*two.shape)],
            out_specs=[pl.BlockSpec((NC, 1, step, w), lambda e, r, c: (0, e, r, 0)) for w in outs]
            + [fixed(*s) for s in shapes],
        ),
        out_shape=[jax.ShapeDtypeStruct((NC, held, quarter, w), jnp.float32) for w in outs]
        + [jax.ShapeDtypeStruct(s, jnp.float32) for s in shapes],
        name="last_outputs",
    )(core[None], *pieces, one, two)


MODEL_WIDTH = 1536
QUERY_HEADS = 24
KEY_VALUE_HEADS = 8
HEAD_SIZE = 64
EXPERT_HIDDEN = 512
EXPERT_COUNT = 32
TOP = 8
CAP = 40


norm_eps = 1e-06
attn_scale = 0.015625
rope_base = 10000.0
masked_logits = -1e30


def rope_tables(positions):
    half = HEAD_SIZE // 2
    frequency = jnp.power(
        jnp.float32(rope_base), -2.0 * jnp.arange(half, dtype=jnp.float32) / HEAD_SIZE
    )
    angle = positions.astype(jnp.float32)[:, None] * frequency[None, :]
    return (jnp.cos(angle)[:, None, :], jnp.sin(angle)[:, None, :])


def rotate_pairs(value_tensor, cosine_table, sine_table):
    half = value_tensor.shape[-1] // 2
    first = value_tensor[..., :half]
    second = value_tensor[..., half:]
    return jnp.concatenate(
        [first * cosine_table - second * sine_table, second * cosine_table + first * sine_table],
        axis=-1,
    )


def rms_forward(wide, gain):
    inverse = lax.rsqrt(jnp.mean(wide * wide, axis=-1, keepdims=True) + norm_eps)
    unit = wide * inverse
    return (unit, inverse, (unit * gain.astype(jnp.float32)).astype(jnp.bfloat16))


def rms_backward(grad, unit, inverse, gain):
    scaled = grad * gain.astype(jnp.float32)
    back = inverse * (scaled - unit * jnp.mean(scaled * unit, axis=-1, keepdims=True))
    return (back, jnp.sum(grad * unit, axis=0))


def piece_scores(query_rows, key_section, positions):
    token_count = key_section.shape[0]
    key_tensor = key_section.reshape(token_count, KEY_VALUE_HEADS, HEAD_SIZE)
    scores = (
        jnp.einsum("tkgd,nkd->kgtn", query_rows, key_tensor, preferred_element_type=jnp.float32)
        * attn_scale
    )
    visible = jnp.arange(token_count, dtype=jnp.int32)[None, :] <= positions[:, None]
    return (jnp.where(visible, scores, masked_logits), visible, key_tensor)


def local(
    hidden,
    routes,
    attn_norm,
    ffn_norm,
    w_q,
    key_weight,
    value_weight,
    w_o,
    router,
    expert_in,
    expert_out,
    cotangent,
):
    token_rows = hidden.shape[1]
    query_group = QUERY_HEADS // KEY_VALUE_HEADS
    ctx_size = lax.axis_size(CTX)
    sequence_length = token_rows * ctx_size
    positions = lax.axis_index(CTX) * token_rows + jnp.arange(token_rows, dtype=jnp.int32)
    cosine_table, sine_table = rope_tables(positions)
    contract_rows = (((0,), (0,)), ((), ()))
    contract_cols = (((1,), (1,)), ((), ()))
    layer = (
        lax.all_gather(attn_norm, (CTX, FSDP), axis=0, tiled=True),
        lax.all_gather(ffn_norm, (CTX, FSDP), axis=0, tiled=True),
        lax.all_gather(w_q, (CTX, FSDP), axis=0, tiled=True),
        lax.all_gather(key_weight, (CTX, FSDP), axis=0, tiled=True),
        lax.all_gather(value_weight, (CTX, FSDP), axis=0, tiled=True),
        lax.all_gather(w_o, (CTX, FSDP), axis=0, tiled=True),
        lax.all_gather(router, (CTX, FSDP), axis=0, tiled=True),
    )
    attn_gain, ffn_gain, query_w, key_weight_matrix, value_w, output_w, router_w = layer
    experts = (
        lax.all_gather(expert_in, FSDP, axis=1, tiled=True),
        lax.all_gather(expert_out, FSDP, axis=1, tiled=True),
    )
    weight_in, weight_out = experts
    wide = hidden[0].astype(jnp.float32)
    attn_unit, inverse_one, attention_input = rms_forward(wide, attn_gain)
    query_linear = jnp.dot(attention_input, query_w, preferred_element_type=jnp.float32).reshape(
        token_rows, QUERY_HEADS, HEAD_SIZE
    )
    query_rows = (
        rotate_pairs(query_linear, cosine_table, sine_table)
        .astype(jnp.bfloat16)
        .reshape(token_rows, KEY_VALUE_HEADS, query_group, HEAD_SIZE)
    )
    key_linear = jnp.dot(
        attention_input, key_weight_matrix, preferred_element_type=jnp.float32
    ).reshape(token_rows, KEY_VALUE_HEADS, HEAD_SIZE)
    key_matrix_rows = (
        rotate_pairs(key_linear, cosine_table, sine_table)
        .astype(jnp.bfloat16)
        .reshape(token_rows, KEY_VALUE_HEADS * HEAD_SIZE)
    )
    value_rows = jnp.dot(attention_input, value_w, preferred_element_type=jnp.float32).astype(
        jnp.bfloat16
    )
    init_state = (
        jnp.full((KEY_VALUE_HEADS, query_group, token_rows), masked_logits, jnp.float32),
        jnp.zeros((KEY_VALUE_HEADS, query_group, token_rows), jnp.float32),
        jnp.zeros((KEY_VALUE_HEADS, query_group, token_rows, HEAD_SIZE), jnp.float32),
    )
    key_section = lax.all_gather(key_matrix_rows, CTX, axis=0, tiled=True)
    value_section = lax.all_gather(value_rows, CTX, axis=0, tiled=True)

    def compute(current):
        best, total, weighted = current
        scores, visible, _ = piece_scores(query_rows, key_section, positions)
        value_tensor = value_section.reshape(value_section.shape[0], KEY_VALUE_HEADS, HEAD_SIZE)
        new_best = jnp.maximum(best, jnp.max(scores, axis=-1))
        weights = jnp.where(visible, jnp.exp(scores - new_best[..., None]), 0.0)
        total = jnp.sum(weights, axis=-1)
        weighted = jnp.einsum(
            "kgtn,nkd->kgtd",
            weights.astype(jnp.bfloat16),
            value_tensor,
            preferred_element_type=jnp.float32,
        )
        return (new_best, total, weighted)

    best, total, weighted = lax.cond(
        jnp.int32(0) <= positions[-1], compute, lambda current: current, init_state
    )
    log_sum_rows = best + jnp.log(total)
    attention_output = (
        jnp.transpose(weighted / total[..., None], (2, 0, 1, 3))
        .reshape(token_rows, QUERY_HEADS * HEAD_SIZE)
        .astype(jnp.bfloat16)
    )
    mixed = wide + jnp.dot(attention_output, output_w, preferred_element_type=jnp.float32)
    ffn_unit, inverse_two, ffn_in = rms_forward(mixed, ffn_gain)
    logits = jnp.dot(ffn_in, router_w, preferred_element_type=jnp.float32)
    route = routes[0]
    indicator = (route[:, :, None] == jnp.arange(EXPERT_COUNT, dtype=jnp.int32)).astype(jnp.float32)
    chosen = jnp.sum(indicator * logits[:, None, :], axis=-1)
    gates = jax.nn.softmax(chosen, axis=-1)
    flat_route = route.reshape(-1)
    counter = (flat_route[:, None] == jnp.arange(EXPERT_COUNT, dtype=jnp.int32)).astype(jnp.int32)
    slot = jnp.sum(counter * (jnp.cumsum(counter, axis=0) - 1), axis=1)
    target = flat_route * CAP + slot
    owner = (
        jnp.full((EXPERT_COUNT * CAP,), token_rows * TOP, jnp.int32)
        .at[target]
        .set(jnp.arange(token_rows * TOP, dtype=jnp.int32))
    )
    ffn_pad = jnp.concatenate([ffn_in, jnp.zeros((1, MODEL_WIDTH), jnp.bfloat16)], axis=0)
    local_experts = weight_in.shape[0]
    outgoing = ffn_pad[owner // TOP].reshape(ctx_size, local_experts, CAP, MODEL_WIDTH)
    received = lax.all_to_all(outgoing, CTX, split_axis=0, concat_axis=2, tiled=True)[0]
    act = jnp.einsum("erd,edf->erf", received, weight_in, preferred_element_type=jnp.float32)
    gate_part = act[..., :EXPERT_HIDDEN]
    up_part = act[..., EXPERT_HIDDEN:]
    sigma = jax.nn.sigmoid(gate_part)
    inner = (gate_part * sigma * up_part).astype(jnp.bfloat16)
    produced = jnp.einsum(
        "erf,edf->erd", inner, weight_out, preferred_element_type=jnp.float32
    ).astype(jnp.bfloat16)
    returned = lax.all_to_all(
        produced[None], CTX, split_axis=2, concat_axis=0, tiled=True
    ).reshape(EXPERT_COUNT * CAP, MODEL_WIDTH)
    picked = returned[target].reshape(token_rows, TOP, MODEL_WIDTH)
    layer_out = (mixed + jnp.sum(gates[..., None] * picked, axis=1)).astype(jnp.bfloat16)
    cot = cotangent[0]
    layer = (
        lax.all_gather(attn_norm, (CTX, FSDP), axis=0, tiled=True),
        lax.all_gather(ffn_norm, (CTX, FSDP), axis=0, tiled=True),
        lax.all_gather(w_q, (CTX, FSDP), axis=0, tiled=True),
        lax.all_gather(key_weight, (CTX, FSDP), axis=0, tiled=True),
        lax.all_gather(value_weight, (CTX, FSDP), axis=0, tiled=True),
        lax.all_gather(w_o, (CTX, FSDP), axis=0, tiled=True),
        lax.all_gather(router, (CTX, FSDP), axis=0, tiled=True),
    )
    attn_gain, ffn_gain, query_w, key_weight_matrix, value_w, output_w, router_w = layer
    experts = (
        lax.all_gather(expert_in, FSDP, axis=1, tiled=True),
        lax.all_gather(expert_out, FSDP, axis=1, tiled=True),
    )
    weight_in, weight_out = experts
    grad_gate = jnp.sum(cot[:, None, :] * picked, axis=-1)
    slot_grads = (
        (gates[..., None] * cot[:, None, :])
        .astype(jnp.bfloat16)
        .reshape(token_rows * TOP, MODEL_WIDTH)
    )
    slot_pad = jnp.concatenate([slot_grads, jnp.zeros((1, MODEL_WIDTH), jnp.bfloat16)], axis=0)
    grad_outgoing = slot_pad[owner].reshape(ctx_size, local_experts, CAP, MODEL_WIDTH)
    grad_received = lax.all_to_all(grad_outgoing, CTX, split_axis=0, concat_axis=2, tiled=True)[0]
    grad_w_out = jnp.einsum(
        "erd,erf->edf", grad_received, inner, preferred_element_type=jnp.float32
    )
    grad_inner = jnp.einsum(
        "erd,edf->erf", grad_received, weight_out, preferred_element_type=jnp.float32
    )
    grad_act = jnp.concatenate(
        [
            grad_inner * up_part * sigma * (1.0 + gate_part * (1.0 - sigma)),
            grad_inner * gate_part * sigma,
        ],
        axis=-1,
    ).astype(jnp.bfloat16)
    grad_w_in = jnp.einsum("erd,erf->edf", received, grad_act, preferred_element_type=jnp.float32)
    grad_rows = jnp.einsum(
        "erf,edf->erd", grad_act, weight_in, preferred_element_type=jnp.float32
    ).astype(jnp.bfloat16)
    grad_back = lax.all_to_all(
        grad_rows[None], CTX, split_axis=2, concat_axis=0, tiled=True
    ).reshape(EXPERT_COUNT * CAP, MODEL_WIDTH)
    grad_expert_in, grad_expert_out = (
        lax.psum_scatter(
            grad_w_in.astype(jnp.bfloat16), FSDP, scatter_dimension=1, tiled=True
        ).astype(jnp.float32),
        lax.psum_scatter(
            grad_w_out.astype(jnp.bfloat16), FSDP, scatter_dimension=1, tiled=True
        ).astype(jnp.float32),
    )
    grad_chosen = gates * (grad_gate - jnp.sum(gates * grad_gate, axis=-1, keepdims=True))
    grad_logits = jnp.sum(indicator * grad_chosen[..., None], axis=1).astype(jnp.bfloat16)
    grad_router_part = lax.dot_general(
        ffn_in, grad_logits, contract_rows, preferred_element_type=jnp.float32
    )
    grad_ffn_in = lax.dot_general(
        grad_logits, router_w, contract_cols, preferred_element_type=jnp.float32
    )
    grad_ffn_in = grad_ffn_in + jnp.sum(
        grad_back[target].reshape(token_rows, TOP, MODEL_WIDTH), axis=1, dtype=jnp.float32
    )
    back_two, grad_ffn_gain = rms_backward(grad_ffn_in, ffn_unit, inverse_two, ffn_gain)
    grad_mixed = cot + back_two
    grad_attn = grad_mixed.astype(jnp.bfloat16)
    grad_wo_part = lax.dot_general(
        attention_output, grad_attn, contract_rows, preferred_element_type=jnp.float32
    )
    attention_output_gradient = lax.dot_general(
        grad_attn, output_w, contract_cols, preferred_element_type=jnp.float32
    ).astype(jnp.bfloat16)
    head_gradient = attention_output_gradient.reshape(
        token_rows, KEY_VALUE_HEADS, query_group, HEAD_SIZE
    )
    delta_rows = jnp.sum(
        head_gradient.astype(jnp.float32)
        * attention_output.reshape(token_rows, KEY_VALUE_HEADS, query_group, HEAD_SIZE).astype(
            jnp.float32
        ),
        axis=-1,
    )
    delta_rows = jnp.transpose(delta_rows, (1, 2, 0))
    init_back = (
        jnp.zeros((token_rows, KEY_VALUE_HEADS, query_group, HEAD_SIZE), jnp.float32),
        jnp.zeros((sequence_length, 2 * KEY_VALUE_HEADS * HEAD_SIZE), jnp.float32),
    )
    attend_key_section = lax.all_gather(key_matrix_rows, CTX, axis=0, tiled=True)
    attend_value_section = lax.all_gather(value_rows, CTX, axis=0, tiled=True)

    def compute(current):
        token_count = attend_key_section.shape[0]
        scores, visible, key_tensor = piece_scores(query_rows, attend_key_section, positions)
        value_tensor = attend_value_section.reshape(token_count, KEY_VALUE_HEADS, HEAD_SIZE)
        weights_full = jnp.where(visible, jnp.exp(scores - log_sum_rows[..., None]), 0.0)
        grad_probs = jnp.einsum(
            "tkgd,nkd->kgtn", head_gradient, value_tensor, preferred_element_type=jnp.float32
        )
        grad_scores = (weights_full * (grad_probs - delta_rows[..., None])).astype(jnp.bfloat16)
        grad_query = attn_scale * jnp.einsum(
            "kgtn,nkd->tkgd", grad_scores, key_tensor, preferred_element_type=jnp.float32
        )
        key_portion = attn_scale * jnp.einsum(
            "kgtn,tkgd->nkd", grad_scores, query_rows, preferred_element_type=jnp.float32
        )
        value_portion = jnp.einsum(
            "kgtn,tkgd->nkd",
            weights_full.astype(jnp.bfloat16),
            head_gradient,
            preferred_element_type=jnp.float32,
        )
        update = jnp.concatenate(
            [
                key_portion.reshape(token_count, KEY_VALUE_HEADS * HEAD_SIZE),
                value_portion.reshape(token_count, KEY_VALUE_HEADS * HEAD_SIZE),
            ],
            axis=1,
        )
        return (grad_query, update)

    grad_query, grad_keys_full = lax.cond(
        jnp.int32(0) <= positions[-1], compute, lambda current: current, init_back
    )
    local_gradients = lax.psum_scatter(
        grad_keys_full.astype(jnp.bfloat16), CTX, scatter_dimension=0, tiled=True
    ).astype(jnp.float32)
    query_back = (
        rotate_pairs(
            grad_query.reshape(token_rows, QUERY_HEADS, HEAD_SIZE), cosine_table, -sine_table
        )
        .astype(jnp.bfloat16)
        .reshape(token_rows, QUERY_HEADS * HEAD_SIZE)
    )
    key_backward_rows = (
        rotate_pairs(
            local_gradients[:, : KEY_VALUE_HEADS * HEAD_SIZE].reshape(
                token_rows, KEY_VALUE_HEADS, HEAD_SIZE
            ),
            cosine_table,
            -sine_table,
        )
        .astype(jnp.bfloat16)
        .reshape(token_rows, KEY_VALUE_HEADS * HEAD_SIZE)
    )
    value_backward_rows = local_gradients[:, KEY_VALUE_HEADS * HEAD_SIZE :].astype(jnp.bfloat16)
    grad_wq_part = lax.dot_general(
        attention_input, query_back, contract_rows, preferred_element_type=jnp.float32
    )
    grad_wk_part = lax.dot_general(
        attention_input, key_backward_rows, contract_rows, preferred_element_type=jnp.float32
    )
    grad_wv_part = lax.dot_general(
        attention_input, value_backward_rows, contract_rows, preferred_element_type=jnp.float32
    )
    grad_attn_in = lax.dot_general(
        query_back, query_w, contract_cols, preferred_element_type=jnp.float32
    )
    grad_attn_in = grad_attn_in + lax.dot_general(
        key_backward_rows, key_weight_matrix, contract_cols, preferred_element_type=jnp.float32
    )
    grad_attn_in = grad_attn_in + lax.dot_general(
        value_backward_rows, value_w, contract_cols, preferred_element_type=jnp.float32
    )
    back_one, grad_attn_gain = rms_backward(grad_attn_in, attn_unit, inverse_one, attn_gain)
    grad_input = grad_mixed + back_one
    partial_sums = (
        lax.psum_scatter(
            grad_attn_gain.astype(jnp.bfloat16), CTX, scatter_dimension=0, tiled=True
        ).astype(jnp.float32),
        lax.psum_scatter(
            grad_ffn_gain.astype(jnp.bfloat16), CTX, scatter_dimension=0, tiled=True
        ).astype(jnp.float32),
        lax.psum_scatter(
            grad_wq_part.astype(jnp.bfloat16), CTX, scatter_dimension=0, tiled=True
        ).astype(jnp.float32),
        lax.psum_scatter(
            grad_wk_part.astype(jnp.bfloat16), CTX, scatter_dimension=0, tiled=True
        ).astype(jnp.float32),
        lax.psum_scatter(
            grad_wv_part.astype(jnp.bfloat16), CTX, scatter_dimension=0, tiled=True
        ).astype(jnp.float32),
        lax.psum_scatter(
            grad_wo_part.astype(jnp.bfloat16), CTX, scatter_dimension=0, tiled=True
        ).astype(jnp.float32),
        lax.psum_scatter(
            grad_router_part.astype(jnp.bfloat16), CTX, scatter_dimension=0, tiled=True
        ).astype(jnp.float32),
    )
    summed = (
        lax.psum_scatter(
            partial_sums[0].astype(jnp.bfloat16), FSDP, scatter_dimension=0, tiled=True
        ).astype(jnp.float32),
        lax.psum_scatter(
            partial_sums[1].astype(jnp.bfloat16), FSDP, scatter_dimension=0, tiled=True
        ).astype(jnp.float32),
        lax.psum_scatter(
            partial_sums[2].astype(jnp.bfloat16), FSDP, scatter_dimension=0, tiled=True
        ).astype(jnp.float32),
        lax.psum_scatter(
            partial_sums[3].astype(jnp.bfloat16), FSDP, scatter_dimension=0, tiled=True
        ).astype(jnp.float32),
        lax.psum_scatter(
            partial_sums[4].astype(jnp.bfloat16), FSDP, scatter_dimension=0, tiled=True
        ).astype(jnp.float32),
        lax.psum_scatter(
            partial_sums[5].astype(jnp.bfloat16), FSDP, scatter_dimension=0, tiled=True
        ).astype(jnp.float32),
        lax.psum_scatter(
            partial_sums[6].astype(jnp.bfloat16), FSDP, scatter_dimension=0, tiled=True
        ).astype(jnp.float32),
    )
    return (
        layer_out[None],
        grad_input[None],
        summed[0],
        summed[1],
        summed[2],
        summed[3],
        summed[4],
        summed[5],
        summed[6],
        grad_expert_in,
        grad_expert_out,
    )


def swap(a, flip):
    return lax.ppermute(a, FSDP, [(i, i ^ flip) for i in range(NX * NC)])


def fast_body(
    hidden,
    routes,
    attn_norm,
    ffn_norm,
    w_q,
    key_weight,
    value_weight,
    w_o,
    router,
    expert_in,
    expert_out,
    cotangent,
):
    tokens = hidden.shape[1]
    ctx = lax.axis_index(CTX)
    fsdp = lax.axis_index(FSDP)
    core = fsdp % NC
    rows = w_q.shape[0]
    quarter = expert_in.shape[1]
    kv_width = KEY_VALUE_HEADS * HEAD_SIZE
    q_width = QUERY_HEADS * HEAD_SIZE
    held = expert_in.shape[0] // NC
    bf = jnp.bfloat16
    f32 = jnp.float32
    positions = ctx * tokens + jnp.arange(tokens, dtype=jnp.int32)
    cosine_table, sine_table = (table[:, 0] for table in rope_tables(positions))
    cosine = jnp.concatenate([cosine_table] * 4, axis=1)
    sine = jnp.concatenate([-sine_table, sine_table] * 2, axis=1)
    contract_cols = (((1,), (1,)), ((), ()))
    wide = hidden[0].astype(f32)
    cot = cotangent[0]

    pack_one = jnp.concatenate([w_q, key_weight, value_weight], axis=1)
    pack_two = jnp.concatenate(
        [w_o, router, attn_norm[:, None], ffn_norm[:, None], jnp.zeros((rows, 94), bf)], axis=1
    )
    route = routes[0]
    indicator = (route[:, :, None] == jnp.arange(EXPERT_COUNT, dtype=jnp.int32)).astype(f32)
    part = rows // 3
    whole = (Z, Y, X, C)
    one, two, mine, other = gather_weights(
        [pack_one, pack_two],
        [expert_in, expert_out],
        [
            Plan(0, (X, Z, Y, C), whole, rows=(0, 2 * part)),
            Plan(0, (X, Y, Z, C), whole, rows=(2 * part, part)),
            Plan(1, (Z, Y, X, C), whole),
        ],
        0,
    )
    parts = [mine, swap(other, 1), swap(mine, 2), swap(other, 3)]
    one = one.reshape(MODEL_WIDTH, -1)
    two = two.reshape(MODEL_WIDTH, -1)
    output_w = two[:, :MODEL_WIDTH]
    small = two[:, MODEL_WIDTH:]
    router_w = small[:, :EXPERT_COUNT]
    gains = lax.dot_general(
        jnp.eye(128, dtype=bf), small, contract_cols, preferred_element_type=f32
    )
    attn_gain, ffn_gain = gains[EXPERT_COUNT], gains[EXPERT_COUNT + 1]

    attn_unit, inverse_one, attention_input = rms_forward(wide, attn_gain)
    linear = jnp.dot(attention_input, one, preferred_element_type=f32)
    attention_output, log_sums, kv, cots, queries = attend(linear, cot, route, cosine, sine, 1)
    mixed = wide + jnp.dot(attention_output, output_w, preferred_element_type=f32)
    ffn_unit, inverse_two, ffn_in = rms_forward(mixed, ffn_gain)
    logits = jnp.dot(ffn_in, router_w, preferred_element_type=f32)
    chosen = jnp.sum(indicator * logits[:, None, :], axis=-1)
    gates = jax.nn.softmax(chosen, axis=-1)
    gate_map = jnp.sum(indicator * gates[..., None], axis=1)
    payload = jnp.concatenate(
        [ffn_in, gate_map.astype(bf), jnp.zeros((tokens, 128 - EXPERT_COUNT), bf)], axis=1
    )
    gin, moe_part, *pieces = moe(payload, cots, parts, CAP, 2)
    across = [swap(pieces[j], j) for j in range(1, NX * NC)]
    grad_gate_map = gin[:, MODEL_WIDTH : MODEL_WIDTH + EXPERT_COUNT] + gin[
        :, MODEL_WIDTH + EXPERT_COUNT : MODEL_WIDTH + 2 * EXPERT_COUNT
    ]
    grad_gate = jnp.sum(indicator * grad_gate_map[:, None, :], axis=-1)
    grad_chosen = gates * (grad_gate - jnp.sum(gates * grad_gate, axis=-1, keepdims=True))
    grad_logits = jnp.sum(indicator * grad_chosen[..., None], axis=1).astype(bf)
    grad_ffn_in = gin[:, :MODEL_WIDTH] + lax.dot_general(
        grad_logits, router_w, contract_cols, preferred_element_type=f32
    )
    back_two, _ = rms_backward(grad_ffn_in, ffn_unit, inverse_two, ffn_gain)
    grad_mixed = cot + back_two
    grad_attn = grad_mixed.astype(bf)
    attention_output_gradient = lax.dot_general(
        grad_attn, output_w, contract_cols, preferred_element_type=f32
    ).astype(bf)
    back, layer_out = attend_back(
        queries, attention_output_gradient, attention_output, log_sums, kv, moe_part, mixed, cosine, sine, 4
    )
    grad_attn_in = lax.dot_general(back, one, contract_cols, preferred_element_type=f32)
    back_one, _ = rms_backward(grad_attn_in, attn_unit, inverse_one, attn_gain)
    grad_input = grad_mixed + back_one
    halves = []
    for factor in (grad_attn_in * attn_unit, grad_ffn_in * ffn_unit):
        high = factor.astype(bf)
        halves += [high, (factor - high.astype(f32)).astype(bf)]
    column = lambda n: jnp.broadcast_to((jnp.arange(128) == n).astype(bf), (tokens, 128))
    sum_one, sum_two = return_weights(
        [attention_input, attention_output, jnp.concatenate([ffn_in] + halves)],
        [
            back,
            grad_attn,
            jnp.concatenate(
                [
                    jnp.concatenate([grad_logits, jnp.zeros((tokens, 128 - EXPERT_COUNT), bf)], axis=1),
                    column(EXPERT_COUNT),
                    column(EXPERT_COUNT),
                    column(EXPERT_COUNT + 1),
                    column(EXPERT_COUNT + 1),
                ]
            ),
        ],
        5,
    )
    grad_expert_in, grad_expert_out, *rest, first_gain, second_gain = last_outputs(
        [pieces[0]] + across,
        core,
        2 * EXPERT_HIDDEN,
        sum_one,
        sum_two,
        (q_width, kv_width, kv_width, MODEL_WIDTH, EXPERT_COUNT),
    )
    return (
        layer_out[None],
        grad_input[None],
        first_gain.reshape(rows),
        second_gain.reshape(rows),
        *rest,
        grad_expert_in.reshape(NC * held, quarter, -1),
        grad_expert_out.reshape(NC * held, quarter, -1),
    )


def fast(*args):
    return fast_body(*args)


def solution(mesh):
    placed = (
        P(FSDP, CTX, None),
        P(FSDP, CTX, None),
        P((CTX, FSDP)),
        P((CTX, FSDP)),
        P((CTX, FSDP), None),
        P((CTX, FSDP), None),
        P((CTX, FSDP), None),
        P((CTX, FSDP), None),
        P((CTX, FSDP), None),
        P(CTX, FSDP, None),
        P(CTX, FSDP, None),
        P(FSDP, CTX, None),
    )
    small = mesh.shape[CTX] == NZ * NY and mesh.shape[FSDP] == NX * NC
    return jax.shard_map(
        fast if small else local,
        mesh=mesh,
        in_specs=placed,
        out_specs=(
            P(FSDP, CTX, None),
            P(FSDP, CTX, None),
            P((CTX, FSDP)),
            P((CTX, FSDP)),
            P((CTX, FSDP), None),
            P((CTX, FSDP), None),
            P((CTX, FSDP), None),
            P((CTX, FSDP), None),
            P((CTX, FSDP), None),
            P(CTX, FSDP, None),
            P(CTX, FSDP, None),
        ),
        check_vma=False,
    )
```

```python
import functools
import itertools

import jax
import jax.numpy as jnp
from jax import lax
from jax.experimental import pallas as pl
from jax.experimental.pallas import tpu as pltpu
from jax.sharding import PartitionSpec as P


NY = 2
NZ = 4
NX = 2
NC = 2
DEV = pl.DeviceIdType.MESH
CTX, FSDP = "ctx", "fsdp"
Z, Y, X, C = 0, 1, 2, 3
SIZES = {Z: NZ, Y: NY, X: NX, C: NC}
UP, DOWN = 4, 5


class Plan:
    def __init__(self, ref, order, index, rows=None, view=None):
        self.ref, self.order, self.index, self.rows, self.view = ref, order, index, rows, view
        self.blocks = 1
        for d in index:
            self.blocks *= SIZES[d]


class Place:
    def __init__(self):
        ctx = lax.axis_index(CTX)
        fsdp = lax.axis_index(FSDP)
        self.at = {Z: ctx // NY, Y: ctx % NY, X: fsdp // NC, C: fsdp % NC}
        z = self.at[Z]
        low = z < NZ // 2
        base = jnp.where(low, z, NZ - 1 - z)
        near = [base, 1 - base, jnp.int32(2), jnp.int32(3)]
        self.order = [z] + [jnp.where(low, k, NZ - 1 - k) for k in near[1:]]

    def device(self, dim, value):
        spot = dict(self.at)
        spot[dim] = value
        return (spot[Z] * NY + spot[Y], spot[X] * NC + spot[C])

    def across(self, dim):
        return self.device(dim, 1 - self.at[dim])

    def along(self, step):
        return self.device(Z, self.at[Z] + step)

    def coords(self, z_from, flips):
        spot = {d: (1 - self.at[d] if d in flips else self.at[d]) for d in (Y, X, C)}
        spot[Z] = z_from
        return spot


def flat_index(spot, dims):
    index = 0
    for d in dims:
        index = index * SIZES[d] + spot[d]
    return index


def subsets(dims):
    return [c for n in range(len(dims) + 1) for c in itertools.combinations(dims, n)]


def greet(place, dims, more=()):
    barrier = pltpu.get_barrier_semaphore()
    z = place.at[Z]
    count = jnp.int32(0)
    for d in dims:
        if d == Z:
            @pl.when(z > 0)
            def _():
                pl.semaphore_signal(barrier, inc=1, device_id=place.along(-1), device_id_type=DEV)

            @pl.when(z < NZ - 1)
            def _():
                pl.semaphore_signal(barrier, inc=1, device_id=place.along(1), device_id_type=DEV)

            count = count + jnp.where(z > 0, 1, 0) + jnp.where(z < NZ - 1, 1, 0)
        else:
            pl.semaphore_signal(barrier, inc=1, device_id=place.across(d), device_id_type=DEV)
            count = count + 1
    for device in more:
        pl.semaphore_signal(barrier, inc=1, device_id=device, device_id_type=DEV)
        count = count + 1
    pl.semaphore_wait(barrier, count)


def gather_events(order):
    pairs = [d for d in order if d != Z]
    events = [(k, f) for k in range(NZ) for f in subsets(pairs)]
    return sorted(events, key=lambda e: (e[0] + len(e[1]), len(e[1])))


def gather_sends(order, k, flips):
    z_at = order.index(Z)
    last = max([order.index(d) for d in flips] + ([z_at] if k > 0 else []) + [-1])
    out = []
    for position, d in enumerate(order):
        if position > last:
            out.extend([UP, DOWN] if d == Z else [d])
    if k > 0 and last == z_at:
        out.extend([UP, DOWN])
    return out


def gather_kernel(plans, *refs):
    w_q, w_k, w_v, w_o, router, first_gain, second_gain, first_w, second_w = refs[:9]
    outs, (mine, *others) = refs[9:11], refs[11:14]
    send_sem, recv_sem, own_sem, stage, load_sem, store_sem, pack_one, pack_two = refs[14:]
    ins = pack_one, pack_two
    place = Place()
    held = mine.shape[0]
    split = first_w.shape[2]
    loads = []
    for side in range(2):
        base = (place.at[C] if side == 0 else 1 - place.at[C]) * held
        for e in range(held):
            to = stage.at[side * held + e]
            for w, at in ((first_w, pl.ds(0, split)), (second_w, pl.ds(split, second_w.shape[2]))):
                loads.append(pltpu.make_async_copy(w.at[base + e], to.at[:, at], load_sem.at[len(loads)]))
    for copy in loads:
        copy.start()
    stores = [pltpu.make_async_copy(stage.at[pl.ds(0, held)], mine, store_sem.at[0])] + [
        pltpu.make_async_copy(stage.at[pl.ds(held + e, 1)], out, store_sem.at[1 + e]) for e, out in enumerate(others)
    ]
    at = 0
    for w in (w_q, w_k, w_v):
        pack_one[:, at : at + w.shape[1]] = w[...]
        at += w.shape[1]
    model = w_o.shape[1]
    rows = w_o.shape[0]
    pack_two[:, :model] = w_o[...]
    same = lax.broadcasted_iota(jnp.int32, (rows, rows), 0) == lax.broadcasted_iota(jnp.int32, (rows, rows), 1)
    upright = lambda gain: jnp.sum(jnp.where(same, gain[...].astype(jnp.float32), 0.0), axis=1, keepdims=True)
    lane = lax.broadcasted_iota(jnp.int32, (1, 128), 1)
    count = router.shape[1]
    small = jnp.where(lane == count, upright(first_gain), jnp.where(lane == count + 1, upright(second_gain), 0.0))
    pack_two[:, model:] = small.astype(pack_two.dtype)
    pack_two[:, model : model + count] = router[...]
    z = place.at[Z]
    greet(place, sorted({d for p in plans for d in p.order}))
    pending = []
    slot = 0
    queue = []
    for n, plan in enumerate(plans):
        for rank, event in enumerate(gather_events(plan.order)):
            queue.append((rank / len(gather_events(plan.order)), n, event))
    queue.sort(key=lambda q: (q[0], q[1]))
    bases = [sum(p.blocks for p in plans[:n]) for n in range(len(plans))]
    for turn_at, (_, n, (k, flips)) in enumerate(queue):
        if turn_at == len(queue) // 3:
            for copy in loads:
                copy.wait()
            for copy in stores:
                copy.start()
        plan = plans[n]
        src = ins[plan.ref]
        out = outs[plan.ref]
        rows = plan.rows
        z_from = place.order[k]
        spot = place.coords(z_from, flips)
        index = flat_index(spot, plan.index)
        own = k == 0 and not flips
        if plan.view is not None:
            target = plan.view(out, spot, rows)
            source = src.at[:, pl.ds(rows[0], rows[1])] if own else target
        else:
            target = out.at[index] if rows is None else out.at[index, pl.ds(rows[0], rows[1])]
            source = (src if rows is None else src.at[pl.ds(rows[0], rows[1])]) if own else target
        sem = recv_sem.at[bases[n] + index]
        if not own:
            pltpu.make_async_remote_copy(
                src_ref=target, dst_ref=target, send_sem=own_sem.at[0], recv_sem=sem,
                device_id=place.across(C), device_id_type=DEV,
            ).wait_recv()
        for way in gather_sends(plan.order, k, flips):
            if way in (UP, DOWN):
                step = 1 if way == UP else -1
                go = z < NZ - 1 if way == UP else z > 0
                if k > 0:
                    go = jnp.logical_and(go, z_from < z if way == UP else z_from > z)
                dest = place.device(Z, jnp.clip(z + step, 0, NZ - 1))
            else:
                go, dest = None, place.across(way)
            copy = pltpu.make_async_remote_copy(
                src_ref=source, dst_ref=target, send_sem=send_sem.at[slot], recv_sem=sem,
                device_id=dest, device_id_type=DEV,
            )
            slot += 1
            if go is None:
                copy.start()
            else:
                pl.when(go)(copy.start)
            pending.append((go, copy.wait_send))
        if own:
            copy = pltpu.make_async_copy(source, target, own_sem.at[1 + n])
            copy.start()
            pending.append((None, copy.wait))
    for copy in stores:
        copy.wait()
    for go, wait in pending:
        if go is None:
            wait()
        else:
            pl.when(go)(wait)


def gather_weights(weights, experts, plans, collective_id):
    sends = sum(len(gather_sends(p.order, k, f)) for p in plans for k, f in gather_events(p.order))
    rows = weights[0].shape[0]
    bf = weights[0].dtype
    widths = [sum(w.shape[1] for w in weights[:3]), weights[3].shape[1] + 128]
    held = experts[0].shape[0] // NC
    pack = (experts[0].shape[1], experts[0].shape[2] + experts[1].shape[2])
    apart = pl.BlockSpec(memory_space=pl.ANY)
    dma = pltpu.SemaphoreType.DMA
    return pl.pallas_call(
        functools.partial(gather_kernel, plans),
        out_shape=[jax.ShapeDtypeStruct((plans[0].blocks, rows, w), bf) for w in widths]
        + [jax.ShapeDtypeStruct((n,) + pack, bf) for n in [held] + [1] * held],
        in_specs=[pl.BlockSpec(memory_space=pltpu.VMEM)] * len(weights) + [apart] * 2,
        out_specs=[apart] * (3 + held),
        scratch_shapes=[
            dma((sends,)),
            dma((sum(p.blocks for p in plans),)),
            dma((1 + len(plans),)),
            pltpu.VMEM((NC * held,) + pack, bf),
            dma((2 * NC * held,)),
            dma((1 + held,)),
        ]
        + [pltpu.VMEM((rows, w), bf) for w in widths],
        compiler_params=pltpu.CompilerParams(collective_id=collective_id, has_side_effects=True),
        name="gather_weights",
    )(*weights, *experts)


def add_into(acc, other):
    acc[...] = (acc[...].astype(jnp.float32) + other[...].astype(jnp.float32)).astype(acc.dtype)


class Gather:
    def __init__(self, place, plan, src, out, send_sem, recv_sem, spare_sem, slot, base):
        self.place, self.plan, self.src, self.out = place, plan, src, out
        self.send_sem, self.recv_sem, self.spare_sem = send_sem, recv_sem, spare_sem
        self.slot, self.base = slot, base
        self.pending = []

    @staticmethod
    def sends(plan):
        return sum(len(gather_sends(plan.order, k, f)) for k, f in gather_events(plan.order))

    def goes(self, way, k):
        z, z_from = self.place.at[Z], self.place.order[k]
        if way == UP:
            return z < NZ - 1 if k == 0 else jnp.logical_and(z < NZ - 1, z_from < z)
        return z > 0 if k == 0 else jnp.logical_and(z > 0, z_from > z)

    def part(self, ref):
        rows = self.plan.rows
        return ref if rows is None else ref.at[pl.ds(rows[0], rows[1])]

    def step(self, k, flips):
        place, plan = self.place, self.plan
        index = flat_index(place.coords(place.order[k], flips), plan.index)
        target = self.part(self.out.at[index])
        sem = self.recv_sem.at[self.base + index]
        source = target
        if k == 0 and not flips:
            source = self.part(self.src)
        else:
            pltpu.make_async_remote_copy(
                src_ref=target, dst_ref=target, send_sem=self.spare_sem, recv_sem=sem,
                device_id=place.across(C), device_id_type=DEV,
            ).wait_recv()
        for way in gather_sends(plan.order, k, flips):
            if way in (UP, DOWN):
                dest = place.device(Z, jnp.clip(place.at[Z] + (1 if way == UP else -1), 0, NZ - 1))
            else:
                dest = place.across(way)
            copy = pltpu.make_async_remote_copy(
                src_ref=source, dst_ref=target, send_sem=self.send_sem.at[self.slot], recv_sem=sem,
                device_id=dest, device_id_type=DEV,
            )
            if way in (UP, DOWN):
                pl.when(self.goes(way, k))(copy.start)
            else:
                copy.start()
            self.pending.append((way, k, self.slot))
            self.slot += 1

    def finish(self):
        for way, k, slot in self.pending:
            block = self.part(self.src)
            copy = pltpu.make_async_remote_copy(
                src_ref=block, dst_ref=block, send_sem=self.send_sem.at[slot], recv_sem=self.spare_sem,
                device_id=self.place.across(C), device_id_type=DEV,
            )
            if way in (UP, DOWN):
                pl.when(self.goes(way, k))(copy.wait_send)
            else:
                copy.wait_send()


class Reduce:
    def __init__(self, place, plan, held, levels, chain, send_sem, recv_sem, spare_sem):
        self.place, self.plan, self.held, self.levels, self.chain = place, plan, held, levels, chain
        self.send_sem, self.recv_sem, self.spare_sem = send_sem, recv_sem, spare_sem
        dims = plan.order
        self.kept = [subsets(dims[p + 1 :]) for p in range(len(dims))]
        self.base = [NZ * sum(len(f) for f in self.kept[:p]) for p in range(len(dims) + 1)]
        self.slot = 0

    @staticmethod
    def counts(plan):
        kept = [NZ * len(subsets(plan.order[p + 1 :])) for p in range(len(plan.order))]
        return kept, sum(kept) + NZ - 1, sum(kept) + NZ + 1

    def push(self, source, target, sem, dest):
        copy = pltpu.make_async_remote_copy(
            src_ref=source, dst_ref=target, send_sem=self.send_sem.at[self.slot], recv_sem=sem,
            device_id=dest, device_id_type=DEV,
        )
        self.slot += 1
        copy.start()

    def arrived(self, target, sem):
        pltpu.make_async_remote_copy(
            src_ref=target, dst_ref=target, send_sem=self.spare_sem, recv_sem=sem,
            device_id=self.place.across(C), device_id_type=DEV,
        ).wait_recv()

    def block(self, k, flips):
        return flat_index(self.place.coords(self.place.order[k], flips), self.plan.index)

    def first(self, k):
        dim = self.plan.order[0]
        for n, f in enumerate(self.kept[0]):
            spot = self.place.order[k] * len(self.kept[0]) + n
            self.push(
                self.held.at[self.block(k, (dim,) + f)], self.levels[0].at[spot],
                self.recv_sem.at[spot], self.place.across(dim),
            )

    def level(self, p, k):
        dims = self.plan.order
        z_to = self.place.order[k]
        for f in sorted(self.kept[p], key=lambda f: -len(f)):
            spot = z_to * len(self.kept[p]) + self.kept[p].index(f)
            mine = self.held.at[self.block(k, f)]
            self.arrived(self.levels[p].at[spot], self.recv_sem.at[self.base[p] + spot])
            add_into(mine, self.levels[p].at[spot])
            later = p + 1
            if later < len(dims) and dims[later] in f:
                left = tuple(d for d in f if d != dims[later])
                there = z_to * len(self.kept[later]) + self.kept[later].index(left)
                self.push(
                    mine, self.levels[later].at[there],
                    self.recv_sem.at[self.base[later] + there], self.place.across(dims[later]),
                )

    def along(self, k):
        z = self.place.at[Z]
        dest = self.place.order[k]
        up = dest > z
        spot = dest + jnp.where(up, 1, 0)
        mine = self.held.at[self.block(k, ())]
        sem = self.recv_sem.at[self.base[-1] + spot]

        @pl.when(jnp.where(up, z > 0, z < NZ - 1))
        def _():
            self.arrived(self.chain.at[spot], sem)
            add_into(mine, self.chain.at[spot])

        self.push(mine, self.chain.at[spot], sem, self.place.along(jnp.where(up, 1, -1)))

    def last(self, out, base=None):
        z = self.place.at[Z]
        mine = self.held.at[self.block(0, ())]
        for go, spot in ((z > 0, z + 1), (z < NZ - 1, z)):

            @pl.when(go)
            def _():
                self.arrived(self.chain.at[spot], self.recv_sem.at[self.base[-1] + spot])
                add_into(mine, self.chain.at[spot])

        total = mine[...].astype(jnp.float32)
        if base is not None:
            total = base[...] + total
        out[...] = total.astype(out.dtype)

    def at_time(self, t):
        depth = len(self.plan.order)
        far = list(reversed(range(NZ)))
        out = [functools.partial(self.level, p, far[t - p]) for p in range(depth) if 0 <= t - p < NZ]
        if 0 <= t - depth < NZ - 1:
            out.append(functools.partial(self.along, far[t - depth]))
        return out

    def steps(self):
        return [step for t in range(NZ + len(self.plan.order)) for step in self.at_time(t)]

    def finish(self):
        block = self.levels[0].at[0]
        for slot in range(self.slot):
            pltpu.make_async_remote_copy(
                src_ref=block, dst_ref=block, send_sem=self.send_sem.at[slot], recv_sem=self.spare_sem,
                device_id=self.place.across(C), device_id_type=DEV,
            ).wait_send()


def tile_up(n, m):
    return (n + m - 1) // m * m


def columns_of(width, chunk=512):
    return [(i, min(chunk, width - i)) for i in range(0, width, chunk)]


def moe_kernel(plans, back, width, hidden, cap, *refs):
    payload, cots, w_own, w_x, w_core, w_core_last, w_both, w_send = refs[:8]
    gin_out, part_out = refs[8:10]
    grads = refs[10:14]
    (
        seen, cot_seen, weights, taken, cot_taken, rows_buf, scaled, grad_act, pick, stage,
        lvl_b0, lvl_b1, chain_b,
        send_sem, recv_sem, spare_sem, send_b, recv_b, load_sem, store_sem, part_sem, piece_sem,
    ) = refs[14:]
    bf, f32 = jnp.bfloat16, jnp.float32
    place = Place()
    count = payload.shape[0]
    pair = 2 * cap
    wide = width + 128
    quarter = width // (NX * NC)
    half = NZ * pair
    lanes = pick.shape[2]
    held = weights.shape[0]
    fsdp = place.at[X] * NC + place.at[C]
    first = (((place.at[Z] * NY + place.at[Y]) * NC) + place.at[C]) * held

    loads = []
    rows_of = lambda owner: pl.ds(pl.multiple_of(owner * quarter, quarter), quarter)
    sources = [(w_own, e, e, 0) for e in range(held)] + [(w_x, e, e, 2) for e in range(held)]
    sources += [(w_core, 0, 0, 1), (w_core_last, 0, held - 1, 1), (w_both, 0, 0, 3)]
    for ref, at, e, j in sources:
        loads.append(pltpu.make_async_copy(ref.at[at], weights.at[e, rows_of(fsdp ^ j)], load_sem.at[len(loads)]))
    there = (place.at[Z] * NY + place.at[Y], (1 - place.at[X]) * NC + 1 - place.at[C])
    piece = pltpu.make_async_remote_copy(
        src_ref=w_send.at[0], dst_ref=weights.at[held - 1, rows_of(fsdp)],
        send_sem=piece_sem.at[0], recv_sem=piece_sem.at[1], device_id=there, device_id_type=DEV,
    )
    base_of = lambda h, k: (jnp.where(h == 0, place.at[C], 1 - place.at[C]) * NZ + place.order[k]) * NY
    cot_loads = {}
    for k in range(NZ):
        for h in range(2):
            at = pl.ds(base_of(h, k), NY)
            cot_loads[(h, k)] = pltpu.make_async_copy(cots.at[at], cot_seen.at[at], load_sem.at[len(loads) + len(cot_loads)])

    greet(place, (Z, Y, C), (there,))
    piece.start()
    ways = []
    send_at = 0
    for n, plan in enumerate(plans):
        ways.append(Gather(place, plan, payload, seen, send_sem, recv_sem, spare_sem, send_at, n * plan.blocks))
        send_at += Gather.sends(plan)
    for way in ways:
        way.step(0, ())
    for key in cot_loads:
        cot_loads[key].start()
    for copy in loads:
        copy.start()
    seen[flat_index(place.at, plans[0].index)] = payload[...]

    row_id = lax.broadcasted_iota(jnp.int32, (NY * count, NY * count), 0)
    col_id = lax.broadcasted_iota(jnp.int32, (NY * count, NY * count), 1)
    earlier = jnp.logical_and(col_id < row_id, col_id // count == row_id // count).astype(bf)
    lane_id = lax.broadcasted_iota(jnp.int32, (1, 128), 1)
    here = [(lane_id == first + e).astype(f32) for e in range(held)]
    pick_lane = lax.broadcasted_iota(jnp.int32, (NY * count, lanes), 1).astype(f32)
    y_shift = (lax.broadcasted_iota(jnp.int32, (NY * count, 1), 0) // count * cap).astype(f32)

    row_of = lambda h, k: (k * NC + h) * pair

    def dispatch(source, target, h, k, cols):
        at = pl.ds(base_of(h, k), NY)
        r = row_of(h, k)
        for c0, cn in cols:
            block = source[at, :, c0 : c0 + cn].reshape(NY * count, cn)
            got = lax.dot_general(
                pick[h * NZ + k], block, (((0,), (0,)), ((), ())), preferred_element_type=f32
            ).astype(bf)
            for e in range(held):
                target[e, r : r + pair, c0 : c0 + cn] = got[e * pair : (e + 1) * pair]

    def cot_chunk(h, k):
        cot_loads[(h, k)].wait()
        at = pl.ds(base_of(h, k), NY)
        chosen = cot_seen[at, :, width:wide].reshape(NY * count, 128)
        before = jnp.dot(earlier, chosen, preferred_element_type=f32)
        picked = None
        for e in range(held):
            is_here = jnp.sum(chosen.astype(f32) * here[e], axis=1, keepdims=True)
            slot = jnp.sum(before * here[e], axis=1, keepdims=True) + y_shift + e * pair
            target = jnp.where(is_here > 0.5, slot, -1.0)
            hit = pick_lane == target
            picked = hit if picked is None else jnp.logical_or(picked, hit)
        pick[h * NZ + k] = picked.astype(f32).astype(bf)
        dispatch(cot_seen, cot_taken, h, k, columns_of(width))

    def hidden_chunk(h, e, n, tile):
        rows = pl.ds(h * half, half)
        tokens_in = taken[e, rows, :width]
        gate = jnp.sum(taken[e, rows, width:wide].astype(f32) * here[e], axis=1, keepdims=True)
        col = n * tile
        g = jnp.dot(tokens_in, weights[e, :, col : col + tile], preferred_element_type=f32)
        u = jnp.dot(tokens_in, weights[e, :, hidden + col : hidden + col + tile], preferred_element_type=f32)
        raw = jnp.dot(
            cot_taken[e, rows, :], weights[e, :, 2 * hidden + col : 2 * hidden + col + tile], preferred_element_type=f32
        )
        s = jax.nn.sigmoid(g)
        gs = g * s
        inner = gs * u
        scaled[e, rows, col : col + tile] = (inner * gate).astype(bf)
        grad_inner = raw * gate
        grad_act[e, rows, col : col + tile] = (grad_inner * u * s * (1.0 + g * (1.0 - s))).astype(bf)
        grad_act[e, rows, hidden + col : hidden + col + tile] = (grad_inner * gs).astype(bf)
        return jnp.sum(raw * inner, axis=1, keepdims=True)

    tile = min(256, hidden)
    found = {}

    def hidden_step(h, e, n):
        got = hidden_chunk(h, e, n, tile)
        found[(h, e)] = got if n == 0 else found[(h, e)] + got
        if n == hidden // tile - 1:
            gate_grad = found.pop((h, e))
            high = gate_grad.astype(bf).astype(f32)
            there = pl.ds(h * half, half)
            apart = (lane_id == EXPERT_COUNT + first + e).astype(f32)
            rows_buf[e, there, width:wide] = (high * here[e] + (gate_grad - high) * apart).astype(bf)

    def hidden_steps(h):
        return [functools.partial(hidden_step, h, e, n) for e in range(held) for n in range(hidden // tile)]

    def project(h, e, left, weight_cols):
        rows = pl.ds(h * half, half)
        lo, n = weight_cols
        for c0, cn in columns_of(width):
            rows_buf[e, rows, c0 : c0 + cn] = lax.dot_general(
                left[e, rows, :], weights[e, c0 : c0 + cn, lo : lo + n], (((1,), (1,)), ((), ())), preferred_element_type=f32
            ).astype(bf)

    def combine(target, h, k, cols):
        at = pl.ds(base_of(h, k), NY)
        r = row_of(h, k)
        for c0, cn in cols:
            parts = [rows_buf[e, r : r + pair, c0 : c0 + cn] for e in range(held)]
            if lanes > held * pair:
                parts.append(jnp.zeros((lanes - held * pair, cn), bf))
            got = jnp.dot(pick[h * NZ + k], jnp.concatenate(parts, axis=0), preferred_element_type=f32)
            target[at, :, c0 : c0 + cn] = got.astype(bf).reshape(NY, count, cn)

    stores = []

    def weight_grad(e, j):
        rows = pl.ds(pl.multiple_of((fsdp ^ j) * quarter, 128), quarter)
        slot = len(stores) % 2
        if len(stores) >= 2:
            stores[-2].wait()
        for c0, cn in columns_of(2 * hidden):
            stage[slot, :, c0 : c0 + cn] = lax.dot_general(
                taken[e, :, rows], grad_act[e, :, c0 : c0 + cn], (((0,), (0,)), ((), ())), preferred_element_type=f32
            ).astype(bf)
        stage[slot, :, 2 * hidden :] = lax.dot_general(
            cot_taken[e, :, rows], scaled[e], (((0,), (0,)), ((), ())), preferred_element_type=f32
        ).astype(bf)
        copy = pltpu.make_async_copy(stage.at[slot], grads[j].at[e], store_sem.at[len(stores)])
        copy.start()
        stores.append(copy)

    work = [functools.partial(cot_chunk, h, k) for h in range(NC) for k in range(NZ)]
    all_cols = columns_of(width) + [(width, 128)]
    ready = {(h, k): 0 for h in range(NC) for k in range(NZ)}
    ready[(0, 0)] = 1
    near_begun = False

    def wait_weights():
        for copy in loads:
            copy.wait()
        arrived = weights.at[held - 1, rows_of(fsdp ^ 3)]
        pltpu.make_async_remote_copy(
            src_ref=arrived, dst_ref=arrived, send_sem=piece_sem.at[0], recv_sem=piece_sem.at[1],
            device_id=there, device_id_type=DEV,
        ).wait_recv()

    for k, flips in gather_events(plans[0].order)[1:]:
        for way in ways:
            way.step(k, flips)
        key = (1 if C in flips else 0, k)
        ready[key] += 1
        if ready[key] == NY:
            work.append(functools.partial(dispatch, seen, taken, *key, all_cols))
            if all(ready[(g, n)] == NY for g in range(NC) for n in range(NZ // 2)) and not near_begun:
                near_begun = True
                work += [wait_weights] + hidden_steps(0)
        for _ in range(min(len(work), 1 if k < NZ - 1 else 2)):
            work.pop(0)()
    for chunk in work:
        chunk()
    for chunk in hidden_steps(1):
        chunk()

    far = list(reversed(range(NZ)))
    spare = spare_sem
    in_way = Reduce(place, back, cot_seen, (lvl_b0, lvl_b1), chain_b, send_b, recv_b, spare)
    in_steps = in_way.steps()
    for e in range(held):
        project(1, e, grad_act, (0, 2 * hidden))
    for k in far[: NZ // 2]:
        combine(cot_seen, 1, k, all_cols)
        in_way.first(k)
    for k in far[: NZ // 2]:
        combine(cot_seen, 0, k, all_cols)
    in_steps.pop(0)()
    for e in range(held):
        project(0, e, grad_act, (0, 2 * hidden))
    in_steps.pop(0)()
    for k in far[NZ // 2 :]:
        combine(cot_seen, 1, k, all_cols)
        in_way.first(k)
    in_steps.pop(0)()
    for k in far[NZ // 2 :]:
        combine(cot_seen, 0, k, all_cols)
    for way in ways:
        way.finish()
    part_copies = []
    work = []

    def out_part(h, k):
        combine(seen, h, k, columns_of(width))
        at = pl.ds(base_of(h, k), NY)
        copy = pltpu.make_async_copy(seen.at[at, :, pl.ds(0, width)], part_out.at[at], part_sem.at[len(part_copies)])
        copy.start()
        part_copies.append(copy)

    for n in range(2):
        for e in range(held):
            work.append(functools.partial(project, n, e, scaled, (2 * hidden, hidden)))
        for k in range(n * NZ // 2, (n + 1) * NZ // 2):
            for h in range(NC):
                work.append(functools.partial(out_part, h, k))
    work += [functools.partial(weight_grad, e, j) for j in reversed(range(NX * NC)) for e in range(held)]
    while in_steps or work:
        if in_steps:
            in_steps.pop(0)()
        for _ in range(2):
            if work:
                work.pop(0)()
    in_way.last(gin_out)
    piece.wait_send()
    for copy in stores[-2:] + part_copies:
        copy.wait()
    in_way.finish()


def moe(payload, cots, parts, cap, collective_id):
    count, wide = payload.shape
    width = wide - 128
    held, quarter, columns = parts[0].shape
    hidden = columns // 3
    cut = count * 3 // 4
    plans = [
        Plan(0, (Z, Y, C), (C, Z, Y), rows=(0, cut)),
        Plan(0, (Y, Z, C), (C, Z, Y), rows=(cut, count - cut)),
    ]
    back = Plan(0, (C, Y), (C, Z, Y))
    levels, sends, recvs = Reduce.counts(back)
    blocks = NC * NZ * NY
    pair = NY * cap
    rows = blocks // NY * pair
    lanes = tile_up(held * pair, 128)
    bf, f32 = jnp.bfloat16, jnp.float32
    whole = pl.BlockSpec(memory_space=pltpu.VMEM)
    apart = pl.BlockSpec(memory_space=pl.ANY)
    dma = pltpu.SemaphoreType.DMA
    return pl.pallas_call(
        functools.partial(moe_kernel, plans, back, width, hidden, cap),
        out_shape=[
            jax.ShapeDtypeStruct((count, wide), f32),
            jax.ShapeDtypeStruct((blocks, count, width), bf),
        ]
        + [jax.ShapeDtypeStruct((held, quarter, columns), bf)] * (NX * NC),
        in_specs=[whole] + [apart] * 7,
        out_specs=[whole] + [apart] * (1 + NX * NC),
        scratch_shapes=[
            pltpu.VMEM((blocks, count, wide), bf),
            pltpu.VMEM((blocks, count, wide), bf),
            pltpu.VMEM((held, NX * NC * quarter, columns), bf),
            pltpu.VMEM((held, rows, wide), bf),
            pltpu.VMEM((held, rows, width), bf),
            pltpu.VMEM((held, rows, wide), bf),
            pltpu.VMEM((held, rows, hidden), bf),
            pltpu.VMEM((held, rows, 2 * hidden), bf),
            pltpu.VMEM((blocks // NY, NY * count, lanes), bf),
            pltpu.VMEM((2, quarter, columns), bf),
        ]
        + [pltpu.VMEM((n, count, wide), bf) for n in levels + [NZ + 1]]
        + [
            dma((sum(Gather.sends(p) for p in plans),)),
            dma((sum(p.blocks for p in plans),)),
            dma(()),
            dma((sends,)),
            dma((recvs,)),
            dma((held * NX * NC + blocks // NY,)),
            dma((held * NX * NC,)),
            dma((blocks // NY,)),
            dma((2,)),
        ],
        compiler_params=pltpu.CompilerParams(
            collective_id=collective_id, has_side_effects=True, vmem_limit_bytes=67043328
        ),
        name="experts",
    )(payload, cots, *parts)


def weights_kernel(plans, gain_at, *refs):
    left_one, right_one, left_two, right_two, left_small, right_small = refs[:6]
    matrix_in, unit, inverse, gain, grad_mixed = refs[6:11]
    outs, grad_input = refs[11:14], refs[14]
    held = refs[15:18]
    buffers = refs[18:30]
    matrix, grad_in, halves = refs[30:33]
    sems, (spare, matrix_sem) = refs[33:39], refs[39:]
    bf, f32 = jnp.bfloat16, jnp.float32
    place = Place()
    far = list(reversed(range(NZ)))
    fetch = pltpu.make_async_copy(matrix_in, matrix, matrix_sem)
    fetch.start()
    greet(place, (Z, Y, X, C))
    *ways, small_way = [
        Reduce(place, plan, held[n], buffers[4 * n : 4 * n + 3], buffers[4 * n + 3], sems[2 * n], sems[2 * n + 1], spare)
        for n, plan in enumerate(plans)
    ]
    group = NY * NX * NC
    rows = group * held[0].shape[1]

    def products(pairs, target, k):
        at = pl.ds(pl.multiple_of(place.order[k] * rows, 128), rows)
        for c0, cn in columns_of(target.shape[2]):
            got = sum(
                lax.dot_general(
                    left[:, at], right[:, c0 : c0 + cn], (((0,), (0,)), ((), ())), preferred_element_type=f32
                )
                for left, right in pairs
            )
            target[pl.ds(place.order[k] * group, group), :, c0 : c0 + cn] = got.astype(target.dtype).reshape(
                group, rows // group, cn
            )

    def round_of(some, t):
        for way in some:
            for step in way.at_time(t):
                step()

    for t in range(NZ):
        products([(left_one, right_one)], held[0], far[t])
        ways[0].first(far[t])
        products([(left_two, right_two)], held[1], far[t])
        ways[1].first(far[t])
        if t > 0:
            round_of(ways, t - 1)
    fetch.wait()
    for c0, cn in columns_of(grad_in.shape[1]):
        grad_in[:, c0 : c0 + cn] = lax.dot_general(
            right_one[...], matrix[c0 : c0 + cn], (((1,), (1,)), ((), ())), preferred_element_type=f32
        )
    count = grad_in.shape[0]
    factor = grad_in[...] * unit[...]
    high = factor.astype(bf)
    halves[:count] = high
    halves[count:] = (factor - high.astype(f32)).astype(bf)
    scaled = grad_in[...] * gain[...]
    mean = jnp.mean(scaled * unit[...], axis=1, keepdims=True)
    grad_input[...] = grad_mixed[...] + inverse[...] * (scaled - unit[...] * mean)
    column = (lax.broadcasted_iota(jnp.int32, (2 * count, 128), 1) == gain_at).astype(f32).astype(bf)
    for k in far:
        products([(left_small, right_small), (halves, column)], held[2], k)
        small_way.first(k)
    late = [(0, 1, 2), (3, 4), (5,), (6,)]
    for n, t in enumerate(range(NZ - 1, NZ + 3)):
        round_of(ways, t)
        for t_small in late[n]:
            round_of([small_way], t_small)
    for way, out in zip(ways + [small_way], outs):
        way.last(out)
    for way in ways + [small_way]:
        way.finish()


def return_weights(lefts, rights, matrix, unit, inverse, gain, grad_mixed, gain_at, collective_id):
    width = lefts[0].shape[1]
    rows = width // (NZ * NY * NX * NC)
    widths = [r.shape[1] for r in rights]
    whole = (Z, Y, X, C)
    plans = [Plan(0, (C, Y, X), whole), Plan(1, (C, X, Y), whole), Plan(2, (C, Y, X), whole)]
    bf, f32 = jnp.bfloat16, jnp.float32
    levels, sends, recvs = Reduce.counts(plans[0])
    dma = pltpu.SemaphoreType.DMA
    vmem = pl.BlockSpec(memory_space=pltpu.VMEM)
    count = unit.shape[0]
    return pl.pallas_call(
        functools.partial(weights_kernel, plans, gain_at),
        out_shape=[jax.ShapeDtypeStruct((rows, w), f32) for w in widths] + [jax.ShapeDtypeStruct(unit.shape, f32)],
        in_specs=[vmem] * 6 + [pl.BlockSpec(memory_space=pl.ANY)] + [vmem] * 4,
        out_specs=[vmem] * 4,
        scratch_shapes=[pltpu.VMEM((plans[0].blocks, rows, w), bf) for w in widths]
        + [pltpu.VMEM((n, rows, w), bf) for w in widths for n in levels + [NZ + 1]]
        + [pltpu.VMEM(matrix.shape, bf), pltpu.VMEM(unit.shape, f32), pltpu.VMEM((2 * count, width), bf)]
        + [dma((n,)) for _ in plans for n in (sends, recvs)]
        + [dma(()), dma(())],
        compiler_params=pltpu.CompilerParams(
            collective_id=collective_id, has_side_effects=True, vmem_limit_bytes=64 * 1024 * 1024
        ),
        name="return_weights",
    )(*[a for pair in zip(lefts, rights) for a in pair], matrix, unit, inverse, gain, grad_mixed)


def turn(block, cosine, sine):
    lane = lax.broadcasted_iota(jnp.int32, (1, 128), 1)
    half = HEAD_SIZE // 2
    other = jnp.where(lane % HEAD_SIZE < half, pltpu.roll(block, 128 - half, 1), pltpu.roll(block, half, 1))
    return block * cosine + other * sine


def place_heads(read, target, count):
    group = QUERY_HEADS // KEY_VALUE_HEADS
    lane = lax.broadcasted_iota(jnp.int32, (1, 2 * HEAD_SIZE), 1)
    for pair in range(QUERY_HEADS // 2):
        both = read(pair)
        for h in (2 * pair, 2 * pair + 1):
            m, g = h // group, h % group
            block = both if h % 2 == m % 2 else pltpu.roll(both, HEAD_SIZE, 1)
            block = jnp.where(lane // HEAD_SIZE == m % 2, block, 0.0)
            target[m, g * count : (g + 1) * count] = block.astype(target.dtype)


def collect_heads(source, target, count, finish):
    group = QUERY_HEADS // KEY_VALUE_HEADS
    lane = lax.broadcasted_iota(jnp.int32, (1, 2 * HEAD_SIZE), 1)
    for pair in range(QUERY_HEADS // 2):
        sides = []
        for h in (2 * pair, 2 * pair + 1):
            m, g = h // group, h % group
            block = source[m, g * count : (g + 1) * count]
            sides.append(block if h % 2 == m % 2 else pltpu.roll(block, HEAD_SIZE, 1))
        both = finish(jnp.where(lane < HEAD_SIZE, *sides))
        target[:, pair * 128 : pair * 128 + 128] = both.astype(target.dtype)


class Scores:
    def __init__(self, place, queries, keys):
        self.queries, self.keys = queries, keys
        group = QUERY_HEADS // KEY_VALUE_HEADS
        count = keys.shape[1]
        self.total = keys.shape[0] * count
        row = lax.broadcasted_iota(jnp.int32, (group * count, 1), 0) % count
        self.position = row + (place.at[Z] * NY + place.at[Y]) * count
        self.column = lax.broadcasted_iota(jnp.int32, (1, self.total), 1)

    def pair(self, m, shift):
        at = pl.ds(pl.multiple_of(shift + m // 2 * 128, 128), 128)
        return self.keys[:, :, at].reshape(self.total, 128)

    def of(self, m, keys):
        found = lax.dot_general(
            self.queries[m], keys, (((1,), (1,)), ((), ())), preferred_element_type=jnp.float32
        )
        return jnp.where(self.column <= self.position, found * attn_scale, masked_logits)


def attend_kernel(
    plans, linear, cot, routes, cosine, sine, out, log_sums, kv_out, cots, placed, seen, own_kv, own_cots, raw, *sems
):
    send_kv, recv_kv, send_cot, recv_cot, spare, own_sem = sems
    place = Place()
    bf, f32 = jnp.bfloat16, jnp.float32
    count = linear.shape[0]
    width = KEY_VALUE_HEADS * HEAD_SIZE
    q_width = QUERY_HEADS * HEAD_SIZE
    for c0 in range(0, width, 128):
        block = linear[:, q_width + c0 : q_width + c0 + 128]
        own_kv[:, c0 : c0 + 128] = turn(block, cosine[...], sine[...]).astype(bf)
    own_kv[:, width:] = linear[:, q_width + width :].astype(bf)
    model = cot.shape[1]
    own_cots[:, :model] = cot[...].astype(bf)
    expert = lax.broadcasted_iota(jnp.int32, (1, 128), 1)
    routed = routes[:, 0:1] == expert
    for n in range(1, routes.shape[1]):
        routed = jnp.logical_or(routed, routes[:, n : n + 1] == expert)
    own_cots[:, model:] = routed.astype(f32).astype(bf)
    greet(place, (Z, Y, C))
    kv_way = Gather(place, plans[0], own_kv, seen, send_kv, recv_kv, spare, 0, 0)
    cot_ways, at = [], 0
    for n, plan in enumerate(plans[1:]):
        cot_ways.append(Gather(place, plan, own_cots, cots, send_cot, recv_cot, spare, at, n * plan.blocks))
        at += Gather.sends(plan)
    kv_way.step(0, ())
    for way in cot_ways:
        way.step(0, ())
    mine = pltpu.make_async_copy(own_cots, cots.at[flat_index(place.at, plans[1].index)], own_sem.at[0])
    mine.start()
    seen[flat_index(place.at, plans[0].index)] = own_kv[...]
    place_heads(lambda pair: turn(linear[:, pair * 128 : pair * 128 + 128], cosine[...], sine[...]), placed, count)
    log_sums[...] = jnp.zeros(log_sums.shape, f32)
    early = [e for e in gather_events(plans[1].order)[1:]]
    kv_events = gather_events(plans[0].order)[1:]
    for k, flips in kv_events:
        kv_way.step(k, flips)
        if len(early) > 8:
            event = early.pop(0)
            for way in cot_ways:
                way.step(*event)
    keep = pltpu.make_async_copy(seen, kv_out, own_sem.at[1])
    keep.start()
    scores = Scores(place, placed, seen)
    lane = lax.broadcasted_iota(jnp.int32, (1, 128), 1)

    def head(m, carry):
        for i in range(KEY_VALUE_HEADS):
            if early:
                event = early.pop(0)

                @pl.when(m == i)
                def _():
                    for way in cot_ways:
                        way.step(*event)

        s = scores.of(m, scores.pair(m, 0))
        best = jnp.max(s, axis=1, keepdims=True)
        weights = jnp.exp(s - best)
        total = jnp.sum(weights, axis=1, keepdims=True)
        mixed = jnp.dot(weights.astype(bf), scores.pair(m, width), preferred_element_type=f32)
        raw[m] = mixed / total
        log_sums[...] = jnp.where(lane == m, best + jnp.log(total), log_sums[...])
        return carry

    lax.fori_loop(0, KEY_VALUE_HEADS, head, 0)
    collect_heads(raw, out, count, lambda block: block)
    keep.wait()
    mine.wait()
    kv_way.finish()
    for way in cot_ways:
        way.finish()


def attend(linear, cot, routes, cosine, sine, collective_id):
    count = linear.shape[0]
    kv_width = 2 * KEY_VALUE_HEADS * HEAD_SIZE
    cut = count * 3 // 4
    plans = [
        Plan(0, (Z, Y), (Z, Y)),
        Plan(1, (Z, Y, C), (C, Z, Y), rows=(0, cut)),
        Plan(1, (Y, Z, C), (C, Z, Y), rows=(cut, count - cut)),
    ]
    bf, f32 = jnp.bfloat16, jnp.float32
    group = QUERY_HEADS // KEY_VALUE_HEADS
    vmem = pl.BlockSpec(memory_space=pltpu.VMEM)
    apart = pl.BlockSpec(memory_space=pl.ANY)
    dma = pltpu.SemaphoreType.DMA
    kv_shape = (plans[0].blocks, count, kv_width)
    cot_shape = (count, cot.shape[1] + 128)
    heads = (KEY_VALUE_HEADS, group * count, 2 * HEAD_SIZE)
    return pl.pallas_call(
        functools.partial(attend_kernel, plans),
        out_shape=[
            jax.ShapeDtypeStruct((count, QUERY_HEADS * HEAD_SIZE), bf),
            jax.ShapeDtypeStruct((group * count, 128), f32),
            jax.ShapeDtypeStruct(kv_shape, bf),
            jax.ShapeDtypeStruct((plans[1].blocks,) + cot_shape, bf),
            jax.ShapeDtypeStruct(heads, bf),
        ],
        in_specs=[vmem] * 5,
        out_specs=[vmem, vmem, apart, apart, vmem],
        scratch_shapes=[
            pltpu.VMEM(kv_shape, bf),
            pltpu.VMEM((count, kv_width), bf),
            pltpu.VMEM(cot_shape, bf),
            pltpu.VMEM(heads, f32),
        ]
        + [
            dma((Gather.sends(plans[0]),)),
            dma((plans[0].blocks,)),
            dma((Gather.sends(plans[1]) + Gather.sends(plans[2]),)),
            dma((plans[1].blocks + plans[2].blocks,)),
            dma(()),
            dma((2,)),
        ],
        compiler_params=pltpu.CompilerParams(
            collective_id=collective_id, has_side_effects=True, vmem_limit_bytes=56 * 1024 * 1024
        ),
        name="attend",
    )(linear, cot, routes, cosine, sine)


def attend_back_kernel(plans, *refs):
    placed, grad_attn, outputs, log_sums, keys, part, w_o, mixed, cosine, sine = refs[:10]
    back, layer_out = refs[10:12]
    kv_grad, grads_placed, raw, deltas, held, held_out, grads, matrix = refs[12:20]
    level, chain, out_level, out_level_two, out_chain = refs[20:25]
    send_kv, recv_kv, send_out, recv_out, spare, load_sem, matrix_sem = refs[25:]
    place = Place()
    bf, f32 = jnp.bfloat16, jnp.float32
    far = list(reversed(range(NZ)))
    loads = []
    for k in far:
        for h in (1 - place.at[C], place.at[C]):
            at = pl.ds((h * NZ + place.order[k]) * NY, NY)
            loads.append(pltpu.make_async_copy(part.at[at], held_out.at[at], load_sem.at[len(loads)]))
    for copy in loads:
        copy.start()
    fetch = pltpu.make_async_copy(w_o.at[:, pl.ds(0, matrix.shape[1])], matrix, matrix_sem)
    fetch.start()
    greet(place, (Z, Y, C))
    kv_way = Reduce(place, plans[0], held, (level,), chain, send_kv, recv_kv, spare)
    out_way = Reduce(place, plans[1], held_out, (out_level, out_level_two), out_chain, send_out, recv_out, spare)
    for copy in loads:
        copy.wait()
    for k in far:
        out_way.first(k)
    count = grads.shape[0]
    fetch.wait()
    for c0, cn in columns_of(grads.shape[1]):
        grads[:, c0 : c0 + cn] = lax.dot_general(
            grad_attn[...], matrix[c0 : c0 + cn], (((1,), (1,)), ((), ())), preferred_element_type=f32
        ).astype(bf)
    place_heads(lambda pair: grads[:, pair * 128 : pair * 128 + 128].astype(f32), grads_placed, count)
    group = QUERY_HEADS // KEY_VALUE_HEADS
    lane = lax.broadcasted_iota(jnp.int32, (1, 128), 1)
    for g in range(group):
        found = jnp.zeros((count, 128), f32)
        for m in range(KEY_VALUE_HEADS):
            h = m * group + g
            at = slice(h // 2 * 128, h // 2 * 128 + 128)
            both = grads[:, at].astype(f32) * outputs[:, at].astype(f32)
            delta = jnp.sum(jnp.where(lane // HEAD_SIZE == h % 2, both, 0.0), axis=1, keepdims=True)
            found = jnp.where(lane == m, delta, found)
        deltas[g * count : (g + 1) * count] = found
    scores = Scores(place, placed, keys)
    width = KEY_VALUE_HEADS * HEAD_SIZE
    blocks = keys.shape[0]
    turns = KEY_VALUE_HEADS // 2
    early = [[(out_way.level, 0, 3)], [(out_way.level, 0, 2)], [(out_way.level, 1, 3)], [(out_way.level, 1, 2), (out_way.along, 3)]]

    def pair(p, carry):
        for i in range(turns):

            @pl.when(p == i)
            def _():
                for step, *at in early[i]:
                    step(*at)

        key_sum = value_sum = None
        for side in range(2):
            m = 2 * p + side
            k_pair, v_pair = scores.pair(m, 0), scores.pair(m, width)
            of_head = lambda ref: jnp.sum(jnp.where(lane == m, ref[...], 0.0), axis=1, keepdims=True)
            weights = jnp.exp(scores.of(m, k_pair) - of_head(log_sums))
            grad = grads_placed[m]
            grad_probs = lax.dot_general(grad, v_pair, (((1,), (1,)), ((), ())), preferred_element_type=f32)
            grad_scores = (weights * (grad_probs - of_head(deltas))).astype(bf)
            raw[m] = attn_scale * jnp.dot(grad_scores, k_pair, preferred_element_type=f32)
            over_rows = (((0,), (0,)), ((), ()))
            key_part = lax.dot_general(grad_scores, placed[m], over_rows, preferred_element_type=f32)
            value_part = lax.dot_general(weights.astype(bf), grad, over_rows, preferred_element_type=f32)
            key_sum = key_part if key_sum is None else key_sum + key_part
            value_sum = value_part if value_sum is None else value_sum + value_part
        at = pl.multiple_of(p * 128, 128)
        held[:, :, pl.ds(at, 128)] = (attn_scale * key_sum).astype(bf).reshape(blocks, count, 128)
        at = pl.multiple_of(width + p * 128, 128)
        held[:, :, pl.ds(at, 128)] = value_sum.astype(bf).reshape(blocks, count, 128)
        return carry

    lax.fori_loop(0, turns, pair, 0)
    for k in far:
        kv_way.first(k)
    out_way.level(0, 1)
    out_way.level(0, 0)
    collect_heads(raw, back, count, lambda block: turn(block, cosine[...], -sine[...]))
    kv_way.level(0, 3)
    kv_way.level(0, 2)
    kv_way.along(3)
    kv_way.level(0, 1)
    kv_way.along(2)
    out_way.along(2)
    kv_way.level(0, 0)
    kv_way.along(1)
    kv_way.last(kv_grad)
    q_width = QUERY_HEADS * HEAD_SIZE
    for c0 in range(0, width, 128):
        block = turn(kv_grad[:, c0 : c0 + 128], cosine[...], -sine[...])
        back[:, q_width + c0 : q_width + c0 + 128] = block.astype(bf)
    back[:, q_width + width :] = kv_grad[:, width:].astype(bf)
    out_way.level(1, 1)
    out_way.along(1)
    out_way.level(1, 0)
    out_way.last(layer_out, mixed)
    kv_way.finish()
    out_way.finish()


def attend_back(placed, grad_attn, outputs, log_sums, keys, part, w_o, mixed, cosine, sine, collective_id):
    count, kv_width = keys.shape[1:]
    plans = [Plan(0, (Y,), (Z, Y)), Plan(1, (C, Y), (C, Z, Y))]
    bf, f32 = jnp.bfloat16, jnp.float32
    group = QUERY_HEADS // KEY_VALUE_HEADS
    vmem = pl.BlockSpec(memory_space=pltpu.VMEM)
    dma = pltpu.SemaphoreType.DMA
    heads = (KEY_VALUE_HEADS, group * count, 2 * HEAD_SIZE)
    levels, sends, recvs = Reduce.counts(plans[0])
    out_levels, out_sends, out_recvs = Reduce.counts(plans[1])
    return pl.pallas_call(
        functools.partial(attend_back_kernel, plans),
        out_shape=[
            jax.ShapeDtypeStruct((count, outputs.shape[1] + kv_width), bf),
            jax.ShapeDtypeStruct(mixed.shape, bf),
        ],
        in_specs=[vmem] * 5 + [pl.BlockSpec(memory_space=pl.ANY)] * 2 + [vmem] * 3,
        out_specs=[vmem] * 2,
        scratch_shapes=[
            pltpu.VMEM((count, kv_width), f32),
            pltpu.VMEM(heads, bf),
            pltpu.VMEM(heads, f32),
            pltpu.VMEM((group * count, 128), f32),
            pltpu.VMEM(keys.shape, bf),
            pltpu.VMEM(part.shape, bf),
            pltpu.VMEM(outputs.shape, bf),
            pltpu.VMEM((w_o.shape[0], grad_attn.shape[1]), bf),
        ]
        + [pltpu.VMEM((n,) + keys.shape[1:], bf) for n in levels + [NZ + 1]]
        + [pltpu.VMEM((n,) + part.shape[1:], bf) for n in out_levels + [NZ + 1]]
        + [dma((n,)) for n in (sends, recvs, out_sends, out_recvs)]
        + [dma(()), dma((NC * NZ,)), dma(())],
        compiler_params=pltpu.CompilerParams(
            collective_id=collective_id, has_side_effects=True, vmem_limit_bytes=60 * 1024 * 1024
        ),
        name="attend_back",
    )(placed, grad_attn, outputs, log_sums, keys, part, w_o, mixed, cosine, sine)


def last_kernel(core_ref, own, core_part, x_part, both_part, one, two, small, *outs):
    core = core_ref[0]
    in_out, out_out = outs[:2]
    split = in_out.shape[3]
    for at, left, right in ((core, own, x_part), (1 - core, core_part, both_part)):
        total = left[0].astype(jnp.float32) + right[0].astype(jnp.float32)
        in_out[at, 0] = total[:, :split]
        out_out[at, 0] = total[:, split:]

    @pl.when(jnp.logical_and(pl.program_id(0) == 0, pl.program_id(1) == 0))
    def _():
        wq, wk, wv, wo, router, first_gain, second_gain = outs[2:]
        q, k = wq.shape[1], wk.shape[1]
        wq[...] = one[:, :q]
        wk[...] = one[:, q : q + k]
        wv[...] = one[:, q + k :]
        wo[...] = two[...]
        router[...] = small[:, : router.shape[1]]
        turned = small[...].T
        at = router.shape[1]
        first_gain[...] = turned[at : at + 1]
        second_gain[...] = turned[at + 1 : at + 2]


def last_outputs(pieces, core, split, sums, widths):
    held, quarter, columns = pieces[0].shape
    step = quarter // 2
    rows = sums[0].shape[0]
    spec = pl.BlockSpec((1, step, columns), lambda e, r, c: (e, r, 0))
    fixed = lambda a, b: pl.BlockSpec((a, b), lambda e, r, c: (0, 0))
    outs = (split, columns - split)
    shapes = [(rows, w) for w in widths] + [(1, rows)] * 2
    return pl.pallas_call(
        last_kernel,
        grid_spec=pltpu.PrefetchScalarGridSpec(
            num_scalar_prefetch=1,
            grid=(held, 2),
            in_specs=[spec] * 4 + [fixed(*a.shape) for a in sums],
            out_specs=[pl.BlockSpec((NC, 1, step, w), lambda e, r, c: (0, e, r, 0)) for w in outs]
            + [fixed(*s) for s in shapes],
        ),
        out_shape=[jax.ShapeDtypeStruct((NC, held, quarter, w), jnp.float32) for w in outs]
        + [jax.ShapeDtypeStruct(s, jnp.float32) for s in shapes],
        name="last_outputs",
    )(core[None], *pieces, *sums)


MODEL_WIDTH = 1536
QUERY_HEADS = 24
KEY_VALUE_HEADS = 8
HEAD_SIZE = 64
EXPERT_HIDDEN = 512
EXPERT_COUNT = 32
TOP = 8
CAP = 40


norm_eps = 1e-06
attn_scale = 0.015625
rope_base = 10000.0
masked_logits = -1e30


def rope_tables(positions):
    half = HEAD_SIZE // 2
    frequency = jnp.power(
        jnp.float32(rope_base), -2.0 * jnp.arange(half, dtype=jnp.float32) / HEAD_SIZE
    )
    angle = positions.astype(jnp.float32)[:, None] * frequency[None, :]
    return (jnp.cos(angle)[:, None, :], jnp.sin(angle)[:, None, :])


def rotate_pairs(value_tensor, cosine_table, sine_table):
    half = value_tensor.shape[-1] // 2
    first = value_tensor[..., :half]
    second = value_tensor[..., half:]
    return jnp.concatenate(
        [first * cosine_table - second * sine_table, second * cosine_table + first * sine_table],
        axis=-1,
    )


def rms_forward(wide, gain):
    inverse = lax.rsqrt(jnp.mean(wide * wide, axis=-1, keepdims=True) + norm_eps)
    unit = wide * inverse
    return (unit, inverse, (unit * gain.astype(jnp.float32)).astype(jnp.bfloat16))


def rms_backward(grad, unit, inverse, gain):
    scaled = grad * gain.astype(jnp.float32)
    back = inverse * (scaled - unit * jnp.mean(scaled * unit, axis=-1, keepdims=True))
    return (back, jnp.sum(grad * unit, axis=0))


def piece_scores(query_rows, key_section, positions):
    token_count = key_section.shape[0]
    key_tensor = key_section.reshape(token_count, KEY_VALUE_HEADS, HEAD_SIZE)
    scores = (
        jnp.einsum("tkgd,nkd->kgtn", query_rows, key_tensor, preferred_element_type=jnp.float32)
        * attn_scale
    )
    visible = jnp.arange(token_count, dtype=jnp.int32)[None, :] <= positions[:, None]
    return (jnp.where(visible, scores, masked_logits), visible, key_tensor)


def local(
    hidden,
    routes,
    attn_norm,
    ffn_norm,
    w_q,
    key_weight,
    value_weight,
    w_o,
    router,
    expert_in,
    expert_out,
    cotangent,
):
    token_rows = hidden.shape[1]
    query_group = QUERY_HEADS // KEY_VALUE_HEADS
    ctx_size = lax.axis_size(CTX)
    sequence_length = token_rows * ctx_size
    positions = lax.axis_index(CTX) * token_rows + jnp.arange(token_rows, dtype=jnp.int32)
    cosine_table, sine_table = rope_tables(positions)
    contract_rows = (((0,), (0,)), ((), ()))
    contract_cols = (((1,), (1,)), ((), ()))
    layer = (
        lax.all_gather(attn_norm, (CTX, FSDP), axis=0, tiled=True),
        lax.all_gather(ffn_norm, (CTX, FSDP), axis=0, tiled=True),
        lax.all_gather(w_q, (CTX, FSDP), axis=0, tiled=True),
        lax.all_gather(key_weight, (CTX, FSDP), axis=0, tiled=True),
        lax.all_gather(value_weight, (CTX, FSDP), axis=0, tiled=True),
        lax.all_gather(w_o, (CTX, FSDP), axis=0, tiled=True),
        lax.all_gather(router, (CTX, FSDP), axis=0, tiled=True),
    )
    attn_gain, ffn_gain, query_w, key_weight_matrix, value_w, output_w, router_w = layer
    experts = (
        lax.all_gather(expert_in, FSDP, axis=1, tiled=True),
        lax.all_gather(expert_out, FSDP, axis=1, tiled=True),
    )
    weight_in, weight_out = experts
    wide = hidden[0].astype(jnp.float32)
    attn_unit, inverse_one, attention_input = rms_forward(wide, attn_gain)
    query_linear = jnp.dot(attention_input, query_w, preferred_element_type=jnp.float32).reshape(
        token_rows, QUERY_HEADS, HEAD_SIZE
    )
    query_rows = (
        rotate_pairs(query_linear, cosine_table, sine_table)
        .astype(jnp.bfloat16)
        .reshape(token_rows, KEY_VALUE_HEADS, query_group, HEAD_SIZE)
    )
    key_linear = jnp.dot(
        attention_input, key_weight_matrix, preferred_element_type=jnp.float32
    ).reshape(token_rows, KEY_VALUE_HEADS, HEAD_SIZE)
    key_matrix_rows = (
        rotate_pairs(key_linear, cosine_table, sine_table)
        .astype(jnp.bfloat16)
        .reshape(token_rows, KEY_VALUE_HEADS * HEAD_SIZE)
    )
    value_rows = jnp.dot(attention_input, value_w, preferred_element_type=jnp.float32).astype(
        jnp.bfloat16
    )
    init_state = (
        jnp.full((KEY_VALUE_HEADS, query_group, token_rows), masked_logits, jnp.float32),
        jnp.zeros((KEY_VALUE_HEADS, query_group, token_rows), jnp.float32),
        jnp.zeros((KEY_VALUE_HEADS, query_group, token_rows, HEAD_SIZE), jnp.float32),
    )
    key_section = lax.all_gather(key_matrix_rows, CTX, axis=0, tiled=True)
    value_section = lax.all_gather(value_rows, CTX, axis=0, tiled=True)

    def compute(current):
        best, total, weighted = current
        scores, visible, _ = piece_scores(query_rows, key_section, positions)
        value_tensor = value_section.reshape(value_section.shape[0], KEY_VALUE_HEADS, HEAD_SIZE)
        new_best = jnp.maximum(best, jnp.max(scores, axis=-1))
        weights = jnp.where(visible, jnp.exp(scores - new_best[..., None]), 0.0)
        total = jnp.sum(weights, axis=-1)
        weighted = jnp.einsum(
            "kgtn,nkd->kgtd",
            weights.astype(jnp.bfloat16),
            value_tensor,
            preferred_element_type=jnp.float32,
        )
        return (new_best, total, weighted)

    best, total, weighted = lax.cond(
        jnp.int32(0) <= positions[-1], compute, lambda current: current, init_state
    )
    log_sum_rows = best + jnp.log(total)
    attention_output = (
        jnp.transpose(weighted / total[..., None], (2, 0, 1, 3))
        .reshape(token_rows, QUERY_HEADS * HEAD_SIZE)
        .astype(jnp.bfloat16)
    )
    mixed = wide + jnp.dot(attention_output, output_w, preferred_element_type=jnp.float32)
    ffn_unit, inverse_two, ffn_in = rms_forward(mixed, ffn_gain)
    logits = jnp.dot(ffn_in, router_w, preferred_element_type=jnp.float32)
    route = routes[0]
    indicator = (route[:, :, None] == jnp.arange(EXPERT_COUNT, dtype=jnp.int32)).astype(jnp.float32)
    chosen = jnp.sum(indicator * logits[:, None, :], axis=-1)
    gates = jax.nn.softmax(chosen, axis=-1)
    flat_route = route.reshape(-1)
    counter = (flat_route[:, None] == jnp.arange(EXPERT_COUNT, dtype=jnp.int32)).astype(jnp.int32)
    slot = jnp.sum(counter * (jnp.cumsum(counter, axis=0) - 1), axis=1)
    target = flat_route * CAP + slot
    owner = (
        jnp.full((EXPERT_COUNT * CAP,), token_rows * TOP, jnp.int32)
        .at[target]
        .set(jnp.arange(token_rows * TOP, dtype=jnp.int32))
    )
    ffn_pad = jnp.concatenate([ffn_in, jnp.zeros((1, MODEL_WIDTH), jnp.bfloat16)], axis=0)
    local_experts = weight_in.shape[0]
    outgoing = ffn_pad[owner // TOP].reshape(ctx_size, local_experts, CAP, MODEL_WIDTH)
    received = lax.all_to_all(outgoing, CTX, split_axis=0, concat_axis=2, tiled=True)[0]
    act = jnp.einsum("erd,edf->erf", received, weight_in, preferred_element_type=jnp.float32)
    gate_part = act[..., :EXPERT_HIDDEN]
    up_part = act[..., EXPERT_HIDDEN:]
    sigma = jax.nn.sigmoid(gate_part)
    inner = (gate_part * sigma * up_part).astype(jnp.bfloat16)
    produced = jnp.einsum(
        "erf,edf->erd", inner, weight_out, preferred_element_type=jnp.float32
    ).astype(jnp.bfloat16)
    returned = lax.all_to_all(
        produced[None], CTX, split_axis=2, concat_axis=0, tiled=True
    ).reshape(EXPERT_COUNT * CAP, MODEL_WIDTH)
    picked = returned[target].reshape(token_rows, TOP, MODEL_WIDTH)
    layer_out = (mixed + jnp.sum(gates[..., None] * picked, axis=1)).astype(jnp.bfloat16)
    cot = cotangent[0]
    layer = (
        lax.all_gather(attn_norm, (CTX, FSDP), axis=0, tiled=True),
        lax.all_gather(ffn_norm, (CTX, FSDP), axis=0, tiled=True),
        lax.all_gather(w_q, (CTX, FSDP), axis=0, tiled=True),
        lax.all_gather(key_weight, (CTX, FSDP), axis=0, tiled=True),
        lax.all_gather(value_weight, (CTX, FSDP), axis=0, tiled=True),
        lax.all_gather(w_o, (CTX, FSDP), axis=0, tiled=True),
        lax.all_gather(router, (CTX, FSDP), axis=0, tiled=True),
    )
    attn_gain, ffn_gain, query_w, key_weight_matrix, value_w, output_w, router_w = layer
    experts = (
        lax.all_gather(expert_in, FSDP, axis=1, tiled=True),
        lax.all_gather(expert_out, FSDP, axis=1, tiled=True),
    )
    weight_in, weight_out = experts
    grad_gate = jnp.sum(cot[:, None, :] * picked, axis=-1)
    slot_grads = (
        (gates[..., None] * cot[:, None, :])
        .astype(jnp.bfloat16)
        .reshape(token_rows * TOP, MODEL_WIDTH)
    )
    slot_pad = jnp.concatenate([slot_grads, jnp.zeros((1, MODEL_WIDTH), jnp.bfloat16)], axis=0)
    grad_outgoing = slot_pad[owner].reshape(ctx_size, local_experts, CAP, MODEL_WIDTH)
    grad_received = lax.all_to_all(grad_outgoing, CTX, split_axis=0, concat_axis=2, tiled=True)[0]
    grad_w_out = jnp.einsum(
        "erd,erf->edf", grad_received, inner, preferred_element_type=jnp.float32
    )
    grad_inner = jnp.einsum(
        "erd,edf->erf", grad_received, weight_out, preferred_element_type=jnp.float32
    )
    grad_act = jnp.concatenate(
        [
            grad_inner * up_part * sigma * (1.0 + gate_part * (1.0 - sigma)),
            grad_inner * gate_part * sigma,
        ],
        axis=-1,
    ).astype(jnp.bfloat16)
    grad_w_in = jnp.einsum("erd,erf->edf", received, grad_act, preferred_element_type=jnp.float32)
    grad_rows = jnp.einsum(
        "erf,edf->erd", grad_act, weight_in, preferred_element_type=jnp.float32
    ).astype(jnp.bfloat16)
    grad_back = lax.all_to_all(
        grad_rows[None], CTX, split_axis=2, concat_axis=0, tiled=True
    ).reshape(EXPERT_COUNT * CAP, MODEL_WIDTH)
    grad_expert_in, grad_expert_out = (
        lax.psum_scatter(
            grad_w_in.astype(jnp.bfloat16), FSDP, scatter_dimension=1, tiled=True
        ).astype(jnp.float32),
        lax.psum_scatter(
            grad_w_out.astype(jnp.bfloat16), FSDP, scatter_dimension=1, tiled=True
        ).astype(jnp.float32),
    )
    grad_chosen = gates * (grad_gate - jnp.sum(gates * grad_gate, axis=-1, keepdims=True))
    grad_logits = jnp.sum(indicator * grad_chosen[..., None], axis=1).astype(jnp.bfloat16)
    grad_router_part = lax.dot_general(
        ffn_in, grad_logits, contract_rows, preferred_element_type=jnp.float32
    )
    grad_ffn_in = lax.dot_general(
        grad_logits, router_w, contract_cols, preferred_element_type=jnp.float32
    )
    grad_ffn_in = grad_ffn_in + jnp.sum(
        grad_back[target].reshape(token_rows, TOP, MODEL_WIDTH), axis=1, dtype=jnp.float32
    )
    back_two, grad_ffn_gain = rms_backward(grad_ffn_in, ffn_unit, inverse_two, ffn_gain)
    grad_mixed = cot + back_two
    grad_attn = grad_mixed.astype(jnp.bfloat16)
    grad_wo_part = lax.dot_general(
        attention_output, grad_attn, contract_rows, preferred_element_type=jnp.float32
    )
    attention_output_gradient = lax.dot_general(
        grad_attn, output_w, contract_cols, preferred_element_type=jnp.float32
    ).astype(jnp.bfloat16)
    head_gradient = attention_output_gradient.reshape(
        token_rows, KEY_VALUE_HEADS, query_group, HEAD_SIZE
    )
    delta_rows = jnp.sum(
        head_gradient.astype(jnp.float32)
        * attention_output.reshape(token_rows, KEY_VALUE_HEADS, query_group, HEAD_SIZE).astype(
            jnp.float32
        ),
        axis=-1,
    )
    delta_rows = jnp.transpose(delta_rows, (1, 2, 0))
    init_back = (
        jnp.zeros((token_rows, KEY_VALUE_HEADS, query_group, HEAD_SIZE), jnp.float32),
        jnp.zeros((sequence_length, 2 * KEY_VALUE_HEADS * HEAD_SIZE), jnp.float32),
    )
    attend_key_section = lax.all_gather(key_matrix_rows, CTX, axis=0, tiled=True)
    attend_value_section = lax.all_gather(value_rows, CTX, axis=0, tiled=True)

    def compute(current):
        token_count = attend_key_section.shape[0]
        scores, visible, key_tensor = piece_scores(query_rows, attend_key_section, positions)
        value_tensor = attend_value_section.reshape(token_count, KEY_VALUE_HEADS, HEAD_SIZE)
        weights_full = jnp.where(visible, jnp.exp(scores - log_sum_rows[..., None]), 0.0)
        grad_probs = jnp.einsum(
            "tkgd,nkd->kgtn", head_gradient, value_tensor, preferred_element_type=jnp.float32
        )
        grad_scores = (weights_full * (grad_probs - delta_rows[..., None])).astype(jnp.bfloat16)
        grad_query = attn_scale * jnp.einsum(
            "kgtn,nkd->tkgd", grad_scores, key_tensor, preferred_element_type=jnp.float32
        )
        key_portion = attn_scale * jnp.einsum(
            "kgtn,tkgd->nkd", grad_scores, query_rows, preferred_element_type=jnp.float32
        )
        value_portion = jnp.einsum(
            "kgtn,tkgd->nkd",
            weights_full.astype(jnp.bfloat16),
            head_gradient,
            preferred_element_type=jnp.float32,
        )
        update = jnp.concatenate(
            [
                key_portion.reshape(token_count, KEY_VALUE_HEADS * HEAD_SIZE),
                value_portion.reshape(token_count, KEY_VALUE_HEADS * HEAD_SIZE),
            ],
            axis=1,
        )
        return (grad_query, update)

    grad_query, grad_keys_full = lax.cond(
        jnp.int32(0) <= positions[-1], compute, lambda current: current, init_back
    )
    local_gradients = lax.psum_scatter(
        grad_keys_full.astype(jnp.bfloat16), CTX, scatter_dimension=0, tiled=True
    ).astype(jnp.float32)
    query_back = (
        rotate_pairs(
            grad_query.reshape(token_rows, QUERY_HEADS, HEAD_SIZE), cosine_table, -sine_table
        )
        .astype(jnp.bfloat16)
        .reshape(token_rows, QUERY_HEADS * HEAD_SIZE)
    )
    key_backward_rows = (
        rotate_pairs(
            local_gradients[:, : KEY_VALUE_HEADS * HEAD_SIZE].reshape(
                token_rows, KEY_VALUE_HEADS, HEAD_SIZE
            ),
            cosine_table,
            -sine_table,
        )
        .astype(jnp.bfloat16)
        .reshape(token_rows, KEY_VALUE_HEADS * HEAD_SIZE)
    )
    value_backward_rows = local_gradients[:, KEY_VALUE_HEADS * HEAD_SIZE :].astype(jnp.bfloat16)
    grad_wq_part = lax.dot_general(
        attention_input, query_back, contract_rows, preferred_element_type=jnp.float32
    )
    grad_wk_part = lax.dot_general(
        attention_input, key_backward_rows, contract_rows, preferred_element_type=jnp.float32
    )
    grad_wv_part = lax.dot_general(
        attention_input, value_backward_rows, contract_rows, preferred_element_type=jnp.float32
    )
    grad_attn_in = lax.dot_general(
        query_back, query_w, contract_cols, preferred_element_type=jnp.float32
    )
    grad_attn_in = grad_attn_in + lax.dot_general(
        key_backward_rows, key_weight_matrix, contract_cols, preferred_element_type=jnp.float32
    )
    grad_attn_in = grad_attn_in + lax.dot_general(
        value_backward_rows, value_w, contract_cols, preferred_element_type=jnp.float32
    )
    back_one, grad_attn_gain = rms_backward(grad_attn_in, attn_unit, inverse_one, attn_gain)
    grad_input = grad_mixed + back_one
    partial_sums = (
        lax.psum_scatter(
            grad_attn_gain.astype(jnp.bfloat16), CTX, scatter_dimension=0, tiled=True
        ).astype(jnp.float32),
        lax.psum_scatter(
            grad_ffn_gain.astype(jnp.bfloat16), CTX, scatter_dimension=0, tiled=True
        ).astype(jnp.float32),
        lax.psum_scatter(
            grad_wq_part.astype(jnp.bfloat16), CTX, scatter_dimension=0, tiled=True
        ).astype(jnp.float32),
        lax.psum_scatter(
            grad_wk_part.astype(jnp.bfloat16), CTX, scatter_dimension=0, tiled=True
        ).astype(jnp.float32),
        lax.psum_scatter(
            grad_wv_part.astype(jnp.bfloat16), CTX, scatter_dimension=0, tiled=True
        ).astype(jnp.float32),
        lax.psum_scatter(
            grad_wo_part.astype(jnp.bfloat16), CTX, scatter_dimension=0, tiled=True
        ).astype(jnp.float32),
        lax.psum_scatter(
            grad_router_part.astype(jnp.bfloat16), CTX, scatter_dimension=0, tiled=True
        ).astype(jnp.float32),
    )
    summed = (
        lax.psum_scatter(
            partial_sums[0].astype(jnp.bfloat16), FSDP, scatter_dimension=0, tiled=True
        ).astype(jnp.float32),
        lax.psum_scatter(
            partial_sums[1].astype(jnp.bfloat16), FSDP, scatter_dimension=0, tiled=True
        ).astype(jnp.float32),
        lax.psum_scatter(
            partial_sums[2].astype(jnp.bfloat16), FSDP, scatter_dimension=0, tiled=True
        ).astype(jnp.float32),
        lax.psum_scatter(
            partial_sums[3].astype(jnp.bfloat16), FSDP, scatter_dimension=0, tiled=True
        ).astype(jnp.float32),
        lax.psum_scatter(
            partial_sums[4].astype(jnp.bfloat16), FSDP, scatter_dimension=0, tiled=True
        ).astype(jnp.float32),
        lax.psum_scatter(
            partial_sums[5].astype(jnp.bfloat16), FSDP, scatter_dimension=0, tiled=True
        ).astype(jnp.float32),
        lax.psum_scatter(
            partial_sums[6].astype(jnp.bfloat16), FSDP, scatter_dimension=0, tiled=True
        ).astype(jnp.float32),
    )
    return (
        layer_out[None],
        grad_input[None],
        summed[0],
        summed[1],
        summed[2],
        summed[3],
        summed[4],
        summed[5],
        summed[6],
        grad_expert_in,
        grad_expert_out,
    )


def swap(a, flip):
    return lax.ppermute(a, FSDP, [(i, i ^ flip) for i in range(NX * NC)])


def fast_body(
    hidden,
    routes,
    attn_norm,
    ffn_norm,
    w_q,
    key_weight,
    value_weight,
    w_o,
    router,
    expert_in,
    expert_out,
    cotangent,
):
    tokens = hidden.shape[1]
    ctx = lax.axis_index(CTX)
    fsdp = lax.axis_index(FSDP)
    core = fsdp % NC
    rows = w_q.shape[0]
    quarter = expert_in.shape[1]
    kv_width = KEY_VALUE_HEADS * HEAD_SIZE
    q_width = QUERY_HEADS * HEAD_SIZE
    held = expert_in.shape[0] // NC
    bf = jnp.bfloat16
    f32 = jnp.float32
    positions = ctx * tokens + jnp.arange(tokens, dtype=jnp.int32)
    cosine_table, sine_table = (table[:, 0] for table in rope_tables(positions))
    cosine = jnp.concatenate([cosine_table] * 4, axis=1)
    sine = jnp.concatenate([-sine_table, sine_table] * 2, axis=1)
    contract_cols = (((1,), (1,)), ((), ()))
    wide = hidden[0].astype(f32)
    cot = cotangent[0]

    route = routes[0]
    indicator = (route[:, :, None] == jnp.arange(EXPERT_COUNT, dtype=jnp.int32)).astype(f32)
    part = rows // 3
    whole = (Z, Y, X, C)
    one, two, mine, *others = gather_weights(
        [w_q, key_weight, value_weight, w_o, router, attn_norm[None], ffn_norm[None]],
        [expert_in, expert_out],
        [
            Plan(0, (X, Z, Y, C), whole, rows=(0, 2 * part)),
            Plan(0, (X, Y, Z, C), whole, rows=(2 * part, part)),
            Plan(1, (Z, Y, X, C), whole),
        ],
        0,
    )
    parts = [mine, swap(mine, 2)] + [swap(other, 1) for other in others] + [swap(others[0], 3)]
    one = one.reshape(MODEL_WIDTH, -1)
    two = two.reshape(MODEL_WIDTH, -1)
    output_w = two[:, :MODEL_WIDTH]
    small = two[:, MODEL_WIDTH:]
    router_w = small[:, :EXPERT_COUNT]
    gains = lax.dot_general(
        jnp.eye(128, dtype=bf), small, contract_cols, preferred_element_type=f32
    )
    attn_gain, ffn_gain = gains[EXPERT_COUNT], gains[EXPERT_COUNT + 1]

    attn_unit, inverse_one, attention_input = rms_forward(wide, attn_gain)
    linear = jnp.dot(attention_input, one, preferred_element_type=f32)
    attention_output, log_sums, kv, cots, queries = attend(linear, cot, route, cosine, sine, 1)
    mixed = wide + jnp.dot(attention_output, output_w, preferred_element_type=f32)
    ffn_unit, inverse_two, ffn_in = rms_forward(mixed, ffn_gain)
    logits = jnp.dot(ffn_in, router_w, preferred_element_type=f32)
    chosen = jnp.sum(indicator * logits[:, None, :], axis=-1)
    gates = jax.nn.softmax(chosen, axis=-1)
    gate_map = jnp.sum(indicator * gates[..., None], axis=1)
    payload = jnp.concatenate(
        [ffn_in, gate_map.astype(bf), jnp.zeros((tokens, 128 - EXPERT_COUNT), bf)], axis=1
    )
    gin, moe_part, *pieces = moe(payload, cots, parts + others[-1:], CAP, 2)
    across = [swap(pieces[j], j) for j in range(1, NX * NC)]
    grad_gate_map = gin[:, MODEL_WIDTH : MODEL_WIDTH + EXPERT_COUNT] + gin[
        :, MODEL_WIDTH + EXPERT_COUNT : MODEL_WIDTH + 2 * EXPERT_COUNT
    ]
    grad_logits = (
        gate_map * (grad_gate_map - jnp.sum(gate_map * grad_gate_map, axis=-1, keepdims=True))
    ).astype(bf)
    grad_ffn_in = gin[:, :MODEL_WIDTH] + lax.dot_general(
        grad_logits, router_w, contract_cols, preferred_element_type=f32
    )
    back_two, _ = rms_backward(grad_ffn_in, ffn_unit, inverse_two, ffn_gain)
    grad_mixed = cot + back_two
    grad_attn = grad_mixed.astype(bf)
    back, layer_out = attend_back(
        queries, grad_attn, attention_output, log_sums, kv, moe_part, two, mixed, cosine, sine, 4
    )
    factor = grad_ffn_in * ffn_unit
    high = factor.astype(bf)
    low = (factor - high.astype(f32)).astype(bf)
    column = jnp.broadcast_to((jnp.arange(128) == EXPERT_COUNT + 1).astype(bf), (tokens, 128))
    logits_wide = jnp.concatenate([grad_logits, jnp.zeros((tokens, 128 - EXPERT_COUNT), bf)], axis=1)
    *sums, grad_input = return_weights(
        [attention_input, attention_output, jnp.concatenate([ffn_in, high, low])],
        [back, grad_attn, jnp.concatenate([logits_wide, column, column])],
        one,
        attn_unit,
        inverse_one,
        attn_gain.astype(f32)[None],
        grad_mixed,
        EXPERT_COUNT,
        5,
    )
    grad_expert_in, grad_expert_out, *rest, first_gain, second_gain = last_outputs(
        [pieces[0]] + across,
        core,
        2 * EXPERT_HIDDEN,
        sums,
        (q_width, kv_width, kv_width, MODEL_WIDTH, EXPERT_COUNT),
    )
    return (
        layer_out[None],
        grad_input[None],
        first_gain.reshape(rows),
        second_gain.reshape(rows),
        *rest,
        grad_expert_in.reshape(NC * held, quarter, -1),
        grad_expert_out.reshape(NC * held, quarter, -1),
    )


def fast(*args):
    return fast_body(*args)


def solution(mesh):
    placed = (
        P(FSDP, CTX, None),
        P(FSDP, CTX, None),
        P((CTX, FSDP)),
        P((CTX, FSDP)),
        P((CTX, FSDP), None),
        P((CTX, FSDP), None),
        P((CTX, FSDP), None),
        P((CTX, FSDP), None),
        P((CTX, FSDP), None),
        P(CTX, FSDP, None),
        P(CTX, FSDP, None),
        P(FSDP, CTX, None),
    )
    small = mesh.shape[CTX] == NZ * NY and mesh.shape[FSDP] == NX * NC
    return jax.shard_map(
        fast if small else local,
        mesh=mesh,
        in_specs=placed,
        out_specs=(
            P(FSDP, CTX, None),
            P(FSDP, CTX, None),
            P((CTX, FSDP)),
            P((CTX, FSDP)),
            P((CTX, FSDP), None),
            P((CTX, FSDP), None),
            P((CTX, FSDP), None),
            P((CTX, FSDP), None),
            P((CTX, FSDP), None),
            P(CTX, FSDP, None),
            P(CTX, FSDP, None),
        ),
        check_vma=False,
    )
```

```python
import functools
import itertools

import jax
import jax.numpy as jnp
from jax import lax
from jax.experimental import pallas as pl
from jax.experimental.pallas import tpu as pltpu
from jax.sharding import PartitionSpec as P


NY = 2
NZ = 4
NX = 2
NC = 2
DEV = pl.DeviceIdType.MESH
CTX, FSDP = "ctx", "fsdp"
Z, Y, X, C = 0, 1, 2, 3
SIZES = {Z: NZ, Y: NY, X: NX, C: NC}
UP, DOWN = 4, 5


class Plan:
    def __init__(self, ref, order, index, rows=None, view=None):
        self.ref, self.order, self.index, self.rows, self.view = ref, order, index, rows, view
        self.blocks = 1
        for d in index:
            self.blocks *= SIZES[d]


class Place:
    def __init__(self):
        ctx = lax.axis_index(CTX)
        fsdp = lax.axis_index(FSDP)
        self.at = {Z: ctx // NY, Y: ctx % NY, X: fsdp // NC, C: fsdp % NC}
        z = self.at[Z]
        low = z < NZ // 2
        base = jnp.where(low, z, NZ - 1 - z)
        near = [base, 1 - base, jnp.int32(2), jnp.int32(3)]
        self.order = [z] + [jnp.where(low, k, NZ - 1 - k) for k in near[1:]]

    def device(self, dim, value):
        spot = dict(self.at)
        spot[dim] = value
        return (spot[Z] * NY + spot[Y], spot[X] * NC + spot[C])

    def across(self, dim):
        return self.device(dim, 1 - self.at[dim])

    def along(self, step):
        return self.device(Z, self.at[Z] + step)

    def coords(self, z_from, flips):
        spot = {d: (1 - self.at[d] if d in flips else self.at[d]) for d in (Y, X, C)}
        spot[Z] = z_from
        return spot


def flat_index(spot, dims):
    index = 0
    for d in dims:
        index = index * SIZES[d] + spot[d]
    return index


def subsets(dims):
    return [c for n in range(len(dims) + 1) for c in itertools.combinations(dims, n)]


def greet(place, dims, more=()):
    barrier = pltpu.get_barrier_semaphore()
    z = place.at[Z]
    count = jnp.int32(0)
    for d in dims:
        if d == Z:
            @pl.when(z > 0)
            def _():
                pl.semaphore_signal(barrier, inc=1, device_id=place.along(-1), device_id_type=DEV)

            @pl.when(z < NZ - 1)
            def _():
                pl.semaphore_signal(barrier, inc=1, device_id=place.along(1), device_id_type=DEV)

            count = count + jnp.where(z > 0, 1, 0) + jnp.where(z < NZ - 1, 1, 0)
        else:
            pl.semaphore_signal(barrier, inc=1, device_id=place.across(d), device_id_type=DEV)
            count = count + 1
    for device in more:
        pl.semaphore_signal(barrier, inc=1, device_id=device, device_id_type=DEV)
        count = count + 1
    pl.semaphore_wait(barrier, count)


def gather_events(order):
    pairs = [d for d in order if d != Z]
    events = [(k, f) for k in range(NZ) for f in subsets(pairs)]
    return sorted(events, key=lambda e: (e[0] + len(e[1]), len(e[1])))


def gather_sends(order, k, flips):
    z_at = order.index(Z)
    last = max([order.index(d) for d in flips] + ([z_at] if k > 0 else []) + [-1])
    out = []
    for position, d in enumerate(order):
        if position > last:
            out.extend([UP, DOWN] if d == Z else [d])
    if k > 0 and last == z_at:
        out.extend([UP, DOWN])
    return out


def gather_kernel(plans, *refs):
    w_q, w_k, w_v, w_o, router, first_gain, second_gain, first_w, second_w = refs[:9]
    outs, (mine, *others) = refs[9:11], refs[11:14]
    send_sem, recv_sem, own_sem, stage, load_sem, store_sem, pack_one, pack_two = refs[14:]
    ins = pack_one, pack_two
    place = Place()
    held = mine.shape[0]
    split = first_w.shape[2]
    loads = []
    for side in range(2):
        base = (place.at[C] if side == 0 else 1 - place.at[C]) * held
        for e in range(held):
            to = stage.at[side * held + e]
            for w, at in ((first_w, pl.ds(0, split)), (second_w, pl.ds(split, second_w.shape[2]))):
                loads.append(pltpu.make_async_copy(w.at[base + e], to.at[:, at], load_sem.at[len(loads)]))
    for copy in loads:
        copy.start()
    stores = [pltpu.make_async_copy(stage.at[pl.ds(0, held)], mine, store_sem.at[0])] + [
        pltpu.make_async_copy(stage.at[pl.ds(held + e, 1)], out, store_sem.at[1 + e]) for e, out in enumerate(others)
    ]
    at = 0
    for w in (w_q, w_k, w_v):
        pack_one[:, at : at + w.shape[1]] = w[...]
        at += w.shape[1]
    model = w_o.shape[1]
    rows = w_o.shape[0]
    pack_two[:, :model] = w_o[...]
    same = lax.broadcasted_iota(jnp.int32, (rows, rows), 0) == lax.broadcasted_iota(jnp.int32, (rows, rows), 1)
    upright = lambda gain: jnp.sum(jnp.where(same, gain[...].astype(jnp.float32), 0.0), axis=1, keepdims=True)
    lane = lax.broadcasted_iota(jnp.int32, (1, 128), 1)
    count = router.shape[1]
    small = jnp.where(lane == count, upright(first_gain), jnp.where(lane == count + 1, upright(second_gain), 0.0))
    pack_two[:, model:] = small.astype(pack_two.dtype)
    pack_two[:, model : model + count] = router[...]
    z = place.at[Z]
    greet(place, sorted({d for p in plans for d in p.order}))
    pending = []
    slot = 0
    queue = []
    for n, plan in enumerate(plans):
        for rank, event in enumerate(gather_events(plan.order)):
            queue.append((rank / len(gather_events(plan.order)), n, event))
    queue.sort(key=lambda q: (q[0], q[1]))
    bases = [sum(p.blocks for p in plans[:n]) for n in range(len(plans))]
    for turn_at, (_, n, (k, flips)) in enumerate(queue):
        if turn_at == len(queue) // 3:
            for copy in loads:
                copy.wait()
            for copy in stores:
                copy.start()
        plan = plans[n]
        src = ins[plan.ref]
        out = outs[plan.ref]
        rows = plan.rows
        z_from = place.order[k]
        spot = place.coords(z_from, flips)
        index = flat_index(spot, plan.index)
        own = k == 0 and not flips
        if plan.view is not None:
            target = plan.view(out, spot, rows)
            source = src.at[:, pl.ds(rows[0], rows[1])] if own else target
        else:
            target = out.at[index] if rows is None else out.at[index, pl.ds(rows[0], rows[1])]
            source = (src if rows is None else src.at[pl.ds(rows[0], rows[1])]) if own else target
        sem = recv_sem.at[bases[n] + index]
        if not own:
            pltpu.make_async_remote_copy(
                src_ref=target, dst_ref=target, send_sem=own_sem.at[0], recv_sem=sem,
                device_id=place.across(C), device_id_type=DEV,
            ).wait_recv()
        for way in gather_sends(plan.order, k, flips):
            if way in (UP, DOWN):
                step = 1 if way == UP else -1
                go = z < NZ - 1 if way == UP else z > 0
                if k > 0:
                    go = jnp.logical_and(go, z_from < z if way == UP else z_from > z)
                dest = place.device(Z, jnp.clip(z + step, 0, NZ - 1))
            else:
                go, dest = None, place.across(way)
            copy = pltpu.make_async_remote_copy(
                src_ref=source, dst_ref=target, send_sem=send_sem.at[slot], recv_sem=sem,
                device_id=dest, device_id_type=DEV,
            )
            slot += 1
            if go is None:
                copy.start()
            else:
                pl.when(go)(copy.start)
            pending.append((go, copy.wait_send))
        if own:
            copy = pltpu.make_async_copy(source, target, own_sem.at[1 + n])
            copy.start()
            pending.append((None, copy.wait))
    for copy in stores:
        copy.wait()
    for go, wait in pending:
        if go is None:
            wait()
        else:
            pl.when(go)(wait)


def gather_weights(weights, experts, plans, collective_id):
    sends = sum(len(gather_sends(p.order, k, f)) for p in plans for k, f in gather_events(p.order))
    rows = weights[0].shape[0]
    bf = weights[0].dtype
    widths = [sum(w.shape[1] for w in weights[:3]), weights[3].shape[1] + 128]
    held = experts[0].shape[0] // NC
    pack = (experts[0].shape[1], experts[0].shape[2] + experts[1].shape[2])
    apart = pl.BlockSpec(memory_space=pl.ANY)
    dma = pltpu.SemaphoreType.DMA
    return pl.pallas_call(
        functools.partial(gather_kernel, plans),
        out_shape=[jax.ShapeDtypeStruct((plans[0].blocks, rows, w), bf) for w in widths]
        + [jax.ShapeDtypeStruct((n,) + pack, bf) for n in [held] + [1] * held],
        in_specs=[pl.BlockSpec(memory_space=pltpu.VMEM)] * len(weights) + [apart] * 2,
        out_specs=[apart] * (3 + held),
        scratch_shapes=[
            dma((sends,)),
            dma((sum(p.blocks for p in plans),)),
            dma((1 + len(plans),)),
            pltpu.VMEM((NC * held,) + pack, bf),
            dma((2 * NC * held,)),
            dma((1 + held,)),
        ]
        + [pltpu.VMEM((rows, w), bf) for w in widths],
        compiler_params=pltpu.CompilerParams(collective_id=collective_id, has_side_effects=True),
        name="gather_weights",
    )(*weights, *experts)


def add_into(acc, other):
    acc[...] = (acc[...].astype(jnp.float32) + other[...].astype(jnp.float32)).astype(acc.dtype)


class Gather:
    def __init__(self, place, plan, src, out, send_sem, recv_sem, spare_sem, slot, base):
        self.place, self.plan, self.src, self.out = place, plan, src, out
        self.send_sem, self.recv_sem, self.spare_sem = send_sem, recv_sem, spare_sem
        self.slot, self.base = slot, base
        self.pending = []

    @staticmethod
    def sends(plan):
        return sum(len(gather_sends(plan.order, k, f)) for k, f in gather_events(plan.order))

    def goes(self, way, k):
        z, z_from = self.place.at[Z], self.place.order[k]
        if way == UP:
            return z < NZ - 1 if k == 0 else jnp.logical_and(z < NZ - 1, z_from < z)
        return z > 0 if k == 0 else jnp.logical_and(z > 0, z_from > z)

    def part(self, ref):
        rows = self.plan.rows
        return ref if rows is None else ref.at[pl.ds(rows[0], rows[1])]

    def step(self, k, flips):
        place, plan = self.place, self.plan
        index = flat_index(place.coords(place.order[k], flips), plan.index)
        target = self.part(self.out.at[index])
        sem = self.recv_sem.at[self.base + index]
        source = target
        if k == 0 and not flips:
            source = self.part(self.src)
        else:
            pltpu.make_async_remote_copy(
                src_ref=target, dst_ref=target, send_sem=self.spare_sem, recv_sem=sem,
                device_id=place.across(C), device_id_type=DEV,
            ).wait_recv()
        for way in gather_sends(plan.order, k, flips):
            if way in (UP, DOWN):
                dest = place.device(Z, jnp.clip(place.at[Z] + (1 if way == UP else -1), 0, NZ - 1))
            else:
                dest = place.across(way)
            copy = pltpu.make_async_remote_copy(
                src_ref=source, dst_ref=target, send_sem=self.send_sem.at[self.slot], recv_sem=sem,
                device_id=dest, device_id_type=DEV,
            )
            if way in (UP, DOWN):
                pl.when(self.goes(way, k))(copy.start)
            else:
                copy.start()
            self.pending.append((way, k, self.slot))
            self.slot += 1

    def finish(self):
        for way, k, slot in self.pending:
            block = self.part(self.src)
            copy = pltpu.make_async_remote_copy(
                src_ref=block, dst_ref=block, send_sem=self.send_sem.at[slot], recv_sem=self.spare_sem,
                device_id=self.place.across(C), device_id_type=DEV,
            )
            if way in (UP, DOWN):
                pl.when(self.goes(way, k))(copy.wait_send)
            else:
                copy.wait_send()


class Reduce:
    def __init__(self, place, plan, held, levels, chain, send_sem, recv_sem, spare_sem):
        self.place, self.plan, self.held, self.levels, self.chain = place, plan, held, levels, chain
        self.send_sem, self.recv_sem, self.spare_sem = send_sem, recv_sem, spare_sem
        self.order, self.chain_at, self.kept, counts = Reduce.shape(plan)
        self.base = [sum(counts[:p]) for p in range(len(counts))]
        self.slot = 0

    @staticmethod
    def shape(plan):
        order = plan.order if Z in plan.order else plan.order + (Z,)
        at = order.index(Z)
        kept = [subsets(tuple(d for d in order[p + 1 :] if d != Z)) for p in range(len(order))]
        times = [NZ if p < at else NZ + 1 if p == at else 1 for p in range(len(order))]
        return order, at, kept, [n * len(f) for n, f in zip(times, kept)]

    @staticmethod
    def counts(plan):
        _, at, kept, counts = Reduce.shape(plan)
        buffers = counts[:at] + counts[at + 1 :] + [counts[at]]
        return buffers, sum(counts) - 2 * len(kept[at]), sum(counts)

    def level_of(self, p):
        return self.levels[p if p < self.chain_at else p - 1]

    def push(self, source, target, sem, dest):
        copy = pltpu.make_async_remote_copy(
            src_ref=source, dst_ref=target, send_sem=self.send_sem.at[self.slot], recv_sem=sem,
            device_id=dest, device_id_type=DEV,
        )
        self.slot += 1
        copy.start()

    def arrived(self, target, sem):
        pltpu.make_async_remote_copy(
            src_ref=target, dst_ref=target, send_sem=self.spare_sem, recv_sem=sem,
            device_id=self.place.across(C), device_id_type=DEV,
        ).wait_recv()

    def block(self, k, flips):
        return self.held.at[flat_index(self.place.coords(self.place.order[k], flips), self.plan.index)]

    def spot(self, p, k, flips):
        at = self.kept[p].index(flips)
        return at if p > self.chain_at else self.place.order[k] * len(self.kept[p]) + at

    def send(self, p, k, flips):
        dim = self.order[p]
        spot = self.spot(p, k, tuple(d for d in flips if d != dim))
        self.push(
            self.block(k, flips), self.level_of(p).at[spot],
            self.recv_sem.at[self.base[p] + spot], self.place.across(dim),
        )

    def first(self, k):
        for f in self.kept[0]:
            self.send(0, k, (self.order[0],) + f)

    def forward(self, p, k, flips):
        later = p + 1
        if later < len(self.order) and self.order[later] in flips:
            self.send(later, k, flips)

    def level(self, p, k):
        for f in sorted(self.kept[p], key=lambda f: -len(f)):
            spot = self.spot(p, k, f)
            self.arrived(self.level_of(p).at[spot], self.recv_sem.at[self.base[p] + spot])
            add_into(self.block(k, f), self.level_of(p).at[spot])
            self.forward(p, k, f)

    def link(self, spot, n):
        at = spot * len(self.kept[self.chain_at]) + n
        return self.chain.at[at], self.recv_sem.at[self.base[self.chain_at] + at]

    def along(self, k):
        z = self.place.at[Z]
        dest = self.place.order[k]
        up = dest > z
        for n, f in enumerate(self.kept[self.chain_at]):
            mine = self.block(k, f)
            target, sem = self.link(dest + jnp.where(up, 1, 0), n)

            @pl.when(jnp.where(up, z > 0, z < NZ - 1))
            def _():
                self.arrived(target, sem)
                add_into(mine, target)

            self.push(mine, target, sem, self.place.along(jnp.where(up, 1, -1)))

    def settle(self):
        z = self.place.at[Z]
        kept = self.kept[self.chain_at]
        for f in sorted(kept, key=lambda f: -len(f)):
            mine = self.block(0, f)
            for go, spot in ((z > 0, z + 1), (z < NZ - 1, z)):
                target, sem = self.link(spot, kept.index(f))

                @pl.when(go)
                def _():
                    self.arrived(target, sem)
                    add_into(mine, target)

            self.forward(self.chain_at, 0, f)

    def last(self, out, base=None):
        if self.chain_at == len(self.order) - 1:
            self.settle()
        total = self.block(0, ())[...].astype(jnp.float32)
        if base is not None:
            total = base[...] + total
        out[...] = total.astype(out.dtype)

    def at_time(self, t):
        far = list(reversed(range(NZ)))
        at = self.chain_at
        out = [functools.partial(self.level, p, far[t - p]) for p in range(at) if 0 <= t - p < NZ]
        if 0 <= t - at < NZ - 1:
            out.append(functools.partial(self.along, far[t - at]))
        if t - at == NZ - 1 and at < len(self.order) - 1:
            out.append(self.settle)
        out += [functools.partial(self.level, p, 0) for p in range(at + 1, len(self.order)) if t == NZ - 1 + p]
        return out

    def steps(self):
        return [step for t in range(NZ + len(self.order)) for step in self.at_time(t)]

    def finish(self):
        block = self.level_of(0).at[0]
        for slot in range(self.slot):
            pltpu.make_async_remote_copy(
                src_ref=block, dst_ref=block, send_sem=self.send_sem.at[slot], recv_sem=self.spare_sem,
                device_id=self.place.across(C), device_id_type=DEV,
            ).wait_send()


def tile_up(n, m):
    return (n + m - 1) // m * m


def columns_of(width, chunk=512):
    return [(i, min(chunk, width - i)) for i in range(0, width, chunk)]


def moe_kernel(plans, back, width, hidden, cap, *refs):
    payload, cots, w_own, w_x, w_core, w_core_last, w_both, w_send = refs[:8]
    gin_out, part_out = refs[8:10]
    grads = refs[10:14]
    (
        seen, cot_seen, weights, taken, cot_taken, rows_buf, scaled, grad_act, pick, stage,
        lvl_b0, lvl_b1, chain_b,
        send_sem, recv_sem, spare_sem, send_b, recv_b, load_sem, store_sem, part_sem, piece_sem,
    ) = refs[14:]
    bf, f32 = jnp.bfloat16, jnp.float32
    place = Place()
    count = payload.shape[0]
    pair = 2 * cap
    wide = width + 128
    quarter = width // (NX * NC)
    half = NZ * pair
    lanes = pick.shape[2]
    held = weights.shape[0]
    fsdp = place.at[X] * NC + place.at[C]
    first = (((place.at[Z] * NY + place.at[Y]) * NC) + place.at[C]) * held

    loads = []
    rows_of = lambda owner: pl.ds(pl.multiple_of(owner * quarter, quarter), quarter)
    sources = [(w_own, e, e, 0) for e in range(held)] + [(w_x, e, e, 2) for e in range(held)]
    sources += [(w_core, 0, 0, 1), (w_core_last, 0, held - 1, 1), (w_both, 0, 0, 3)]
    for ref, at, e, j in sources:
        loads.append(pltpu.make_async_copy(ref.at[at], weights.at[e, rows_of(fsdp ^ j)], load_sem.at[len(loads)]))
    there = (place.at[Z] * NY + place.at[Y], (1 - place.at[X]) * NC + 1 - place.at[C])
    piece = pltpu.make_async_remote_copy(
        src_ref=w_send.at[0], dst_ref=weights.at[held - 1, rows_of(fsdp)],
        send_sem=piece_sem.at[0], recv_sem=piece_sem.at[1], device_id=there, device_id_type=DEV,
    )
    base_of = lambda h, k: (jnp.where(h == 0, place.at[C], 1 - place.at[C]) * NZ + place.order[k]) * NY
    cot_loads = {}
    for k in range(NZ):
        for h in range(2):
            at = pl.ds(base_of(h, k), NY)
            cot_loads[(h, k)] = pltpu.make_async_copy(cots.at[at], cot_seen.at[at], load_sem.at[len(loads) + len(cot_loads)])

    greet(place, (Z, Y, C), (there,))
    piece.start()
    ways = []
    send_at = 0
    for n, plan in enumerate(plans):
        ways.append(Gather(place, plan, payload, seen, send_sem, recv_sem, spare_sem, send_at, n * plan.blocks))
        send_at += Gather.sends(plan)
    for way in ways:
        way.step(0, ())
    for key in cot_loads:
        cot_loads[key].start()
    for copy in loads:
        copy.start()
    seen[flat_index(place.at, plans[0].index)] = payload[...]

    row_id = lax.broadcasted_iota(jnp.int32, (NY * count, NY * count), 0)
    col_id = lax.broadcasted_iota(jnp.int32, (NY * count, NY * count), 1)
    earlier = jnp.logical_and(col_id < row_id, col_id // count == row_id // count).astype(bf)
    lane_id = lax.broadcasted_iota(jnp.int32, (1, 128), 1)
    here = [(lane_id == first + e).astype(f32) for e in range(held)]
    pick_lane = lax.broadcasted_iota(jnp.int32, (NY * count, lanes), 1).astype(f32)
    y_shift = (lax.broadcasted_iota(jnp.int32, (NY * count, 1), 0) // count * cap).astype(f32)

    row_of = lambda h, k: (k * NC + h) * pair

    def dispatch(source, target, h, k, cols):
        at = pl.ds(base_of(h, k), NY)
        r = row_of(h, k)
        for c0, cn in cols:
            block = source[at, :, c0 : c0 + cn].reshape(NY * count, cn)
            got = lax.dot_general(
                pick[h * NZ + k], block, (((0,), (0,)), ((), ())), preferred_element_type=f32
            ).astype(bf)
            for e in range(held):
                target[e, r : r + pair, c0 : c0 + cn] = got[e * pair : (e + 1) * pair]

    def cot_chunk(h, k):
        cot_loads[(h, k)].wait()
        at = pl.ds(base_of(h, k), NY)
        chosen = cot_seen[at, :, width:wide].reshape(NY * count, 128)
        before = jnp.dot(earlier, chosen, preferred_element_type=f32)
        picked = None
        for e in range(held):
            is_here = jnp.sum(chosen.astype(f32) * here[e], axis=1, keepdims=True)
            slot = jnp.sum(before * here[e], axis=1, keepdims=True) + y_shift + e * pair
            target = jnp.where(is_here > 0.5, slot, -1.0)
            hit = pick_lane == target
            picked = hit if picked is None else jnp.logical_or(picked, hit)
        pick[h * NZ + k] = picked.astype(f32).astype(bf)
        dispatch(cot_seen, cot_taken, h, k, columns_of(width))

    def hidden_chunk(h, e, n, tile):
        rows = pl.ds(h * half, half)
        tokens_in = taken[e, rows, :width]
        gate = jnp.sum(taken[e, rows, width:wide].astype(f32) * here[e], axis=1, keepdims=True)
        col = n * tile
        g = jnp.dot(tokens_in, weights[e, :, col : col + tile], preferred_element_type=f32)
        u = jnp.dot(tokens_in, weights[e, :, hidden + col : hidden + col + tile], preferred_element_type=f32)
        raw = jnp.dot(
            cot_taken[e, rows, :], weights[e, :, 2 * hidden + col : 2 * hidden + col + tile], preferred_element_type=f32
        )
        s = jax.nn.sigmoid(g)
        gs = g * s
        inner = gs * u
        scaled[e, rows, col : col + tile] = (inner * gate).astype(bf)
        grad_inner = raw * gate
        grad_act[e, rows, col : col + tile] = (grad_inner * u * s * (1.0 + g * (1.0 - s))).astype(bf)
        grad_act[e, rows, hidden + col : hidden + col + tile] = (grad_inner * gs).astype(bf)
        return jnp.sum(raw * inner, axis=1, keepdims=True)

    tile = min(256, hidden)
    found = {}

    def hidden_step(h, e, n):
        got = hidden_chunk(h, e, n, tile)
        found[(h, e)] = got if n == 0 else found[(h, e)] + got
        if n == hidden // tile - 1:
            gate_grad = found.pop((h, e))
            high = gate_grad.astype(bf).astype(f32)
            there = pl.ds(h * half, half)
            apart = (lane_id == EXPERT_COUNT + first + e).astype(f32)
            rows_buf[e, there, width:wide] = (high * here[e] + (gate_grad - high) * apart).astype(bf)

    def hidden_steps(h):
        return [functools.partial(hidden_step, h, e, n) for e in range(held) for n in range(hidden // tile)]

    def project(h, e, left, weight_cols):
        rows = pl.ds(h * half, half)
        lo, n = weight_cols
        for c0, cn in columns_of(width):
            rows_buf[e, rows, c0 : c0 + cn] = lax.dot_general(
                left[e, rows, :], weights[e, c0 : c0 + cn, lo : lo + n], (((1,), (1,)), ((), ())), preferred_element_type=f32
            ).astype(bf)

    def combine(target, h, k, cols):
        at = pl.ds(base_of(h, k), NY)
        r = row_of(h, k)
        for c0, cn in cols:
            parts = [rows_buf[e, r : r + pair, c0 : c0 + cn] for e in range(held)]
            if lanes > held * pair:
                parts.append(jnp.zeros((lanes - held * pair, cn), bf))
            got = jnp.dot(pick[h * NZ + k], jnp.concatenate(parts, axis=0), preferred_element_type=f32)
            target[at, :, c0 : c0 + cn] = got.astype(bf).reshape(NY, count, cn)

    stores = []

    def weight_grad(e, j):
        rows = pl.ds(pl.multiple_of((fsdp ^ j) * quarter, 128), quarter)
        slot = len(stores) % 2
        if len(stores) >= 2:
            stores[-2].wait()
        for c0, cn in columns_of(2 * hidden):
            stage[slot, :, c0 : c0 + cn] = lax.dot_general(
                taken[e, :, rows], grad_act[e, :, c0 : c0 + cn], (((0,), (0,)), ((), ())), preferred_element_type=f32
            ).astype(bf)
        stage[slot, :, 2 * hidden :] = lax.dot_general(
            cot_taken[e, :, rows], scaled[e], (((0,), (0,)), ((), ())), preferred_element_type=f32
        ).astype(bf)
        copy = pltpu.make_async_copy(stage.at[slot], grads[j].at[e], store_sem.at[len(stores)])
        copy.start()
        stores.append(copy)

    work = [functools.partial(cot_chunk, h, k) for h in range(NC) for k in range(NZ)]
    all_cols = columns_of(width) + [(width, 128)]
    ready = {(h, k): 0 for h in range(NC) for k in range(NZ)}
    ready[(0, 0)] = 1
    near_begun = False

    def wait_weights():
        for copy in loads:
            copy.wait()
        arrived = weights.at[held - 1, rows_of(fsdp ^ 3)]
        pltpu.make_async_remote_copy(
            src_ref=arrived, dst_ref=arrived, send_sem=piece_sem.at[0], recv_sem=piece_sem.at[1],
            device_id=there, device_id_type=DEV,
        ).wait_recv()

    for k, flips in gather_events(plans[0].order)[1:]:
        for way in ways:
            way.step(k, flips)
        key = (1 if C in flips else 0, k)
        ready[key] += 1
        if ready[key] == NY:
            work.append(functools.partial(dispatch, seen, taken, *key, all_cols))
            if all(ready[(g, n)] == NY for g in range(NC) for n in range(NZ // 2)) and not near_begun:
                near_begun = True
                work += [wait_weights] + hidden_steps(0)
        for _ in range(min(len(work), 1 if k < NZ - 1 else 2)):
            work.pop(0)()
    for chunk in work:
        chunk()
    for chunk in hidden_steps(1):
        chunk()

    far = list(reversed(range(NZ)))
    spare = spare_sem
    in_way = Reduce(place, back, cot_seen, (lvl_b0, lvl_b1), chain_b, send_b, recv_b, spare)
    in_steps = in_way.steps()
    for e in range(held):
        project(1, e, grad_act, (0, 2 * hidden))
    for k in far[: NZ // 2]:
        combine(cot_seen, 1, k, all_cols)
        in_way.first(k)
    for k in far[: NZ // 2]:
        combine(cot_seen, 0, k, all_cols)
    in_steps.pop(0)()
    for e in range(held):
        project(0, e, grad_act, (0, 2 * hidden))
    in_steps.pop(0)()
    for k in far[NZ // 2 :]:
        combine(cot_seen, 1, k, all_cols)
        in_way.first(k)
    in_steps.pop(0)()
    for k in far[NZ // 2 :]:
        combine(cot_seen, 0, k, all_cols)
    for way in ways:
        way.finish()
    part_copies = []
    work = []

    def out_part(h, k):
        combine(seen, h, k, columns_of(width))
        at = pl.ds(base_of(h, k), NY)
        copy = pltpu.make_async_copy(seen.at[at, :, pl.ds(0, width)], part_out.at[at], part_sem.at[len(part_copies)])
        copy.start()
        part_copies.append(copy)

    for n in range(2):
        for e in range(held):
            work.append(functools.partial(project, n, e, scaled, (2 * hidden, hidden)))
        for k in range(n * NZ // 2, (n + 1) * NZ // 2):
            for h in range(NC):
                work.append(functools.partial(out_part, h, k))
    work += [functools.partial(weight_grad, e, j) for j in reversed(range(NX * NC)) for e in range(held)]
    while in_steps or work:
        if in_steps:
            in_steps.pop(0)()
        for _ in range(2):
            if work:
                work.pop(0)()
    in_way.last(gin_out)
    piece.wait_send()
    for copy in stores[-2:] + part_copies:
        copy.wait()
    in_way.finish()


def moe(payload, cots, parts, cap, collective_id):
    count, wide = payload.shape
    width = wide - 128
    held, quarter, columns = parts[0].shape
    hidden = columns // 3
    cut = count * 3 // 4
    plans = [
        Plan(0, (Z, Y, C), (C, Z, Y), rows=(0, cut)),
        Plan(0, (Y, Z, C), (C, Z, Y), rows=(cut, count - cut)),
    ]
    back = Plan(0, (C, Y), (C, Z, Y))
    levels, sends, recvs = Reduce.counts(back)
    blocks = NC * NZ * NY
    pair = NY * cap
    rows = blocks // NY * pair
    lanes = tile_up(held * pair, 128)
    bf, f32 = jnp.bfloat16, jnp.float32
    whole = pl.BlockSpec(memory_space=pltpu.VMEM)
    apart = pl.BlockSpec(memory_space=pl.ANY)
    dma = pltpu.SemaphoreType.DMA
    return pl.pallas_call(
        functools.partial(moe_kernel, plans, back, width, hidden, cap),
        out_shape=[
            jax.ShapeDtypeStruct((count, wide), f32),
            jax.ShapeDtypeStruct((blocks, count, width), bf),
        ]
        + [jax.ShapeDtypeStruct((held, quarter, columns), bf)] * (NX * NC),
        in_specs=[whole] + [apart] * 7,
        out_specs=[whole] + [apart] * (1 + NX * NC),
        scratch_shapes=[
            pltpu.VMEM((blocks, count, wide), bf),
            pltpu.VMEM((blocks, count, wide), bf),
            pltpu.VMEM((held, NX * NC * quarter, columns), bf),
            pltpu.VMEM((held, rows, wide), bf),
            pltpu.VMEM((held, rows, width), bf),
            pltpu.VMEM((held, rows, wide), bf),
            pltpu.VMEM((held, rows, hidden), bf),
            pltpu.VMEM((held, rows, 2 * hidden), bf),
            pltpu.VMEM((blocks // NY, NY * count, lanes), bf),
            pltpu.VMEM((2, quarter, columns), bf),
        ]
        + [pltpu.VMEM((n, count, wide), bf) for n in levels]
        + [
            dma((sum(Gather.sends(p) for p in plans),)),
            dma((sum(p.blocks for p in plans),)),
            dma(()),
            dma((sends,)),
            dma((recvs,)),
            dma((held * NX * NC + blocks // NY,)),
            dma((held * NX * NC,)),
            dma((blocks // NY,)),
            dma((2,)),
        ],
        compiler_params=pltpu.CompilerParams(
            collective_id=collective_id, has_side_effects=True, vmem_limit_bytes=67043328
        ),
        name="experts",
    )(payload, cots, *parts)


def weights_kernel(plans, gain_at, *refs):
    left_one, right_one, left_two, right_two, left_small, right_small = refs[:6]
    matrix_in, unit, inverse, gain, grad_mixed = refs[6:11]
    n_ways = len(plans)
    outs, grad_input = refs[11:14], refs[14]
    held = refs[15 : 15 + n_ways]
    buffers, refs = refs[15 + n_ways : 15 + 5 * n_ways], refs[15 + 5 * n_ways :]
    matrix, grad_in, halves = refs[:3]
    sems, (spare, matrix_sem) = refs[3 : 3 + 2 * n_ways], refs[3 + 2 * n_ways :]
    bf, f32 = jnp.bfloat16, jnp.float32
    place = Place()
    far = list(reversed(range(NZ)))
    fetch = pltpu.make_async_copy(matrix_in, matrix, matrix_sem)
    fetch.start()
    greet(place, (Z, Y, X, C))
    *ways, small_way = [
        Reduce(place, plan, held[n], buffers[4 * n : 4 * n + 3], buffers[4 * n + 3], sems[2 * n], sems[2 * n + 1], spare)
        for n, plan in enumerate(plans)
    ]
    group = NY * NX * NC
    rows = group * held[0].shape[1]

    def products(pairs, target, k, shift=0):
        at = pl.ds(pl.multiple_of(place.order[k] * rows, 128), rows)
        for c0, cn in columns_of(target.shape[2]):
            got = sum(
                lax.dot_general(
                    left[:, at], right[:, shift + c0 : shift + c0 + cn], (((0,), (0,)), ((), ())),
                    preferred_element_type=f32,
                )
                for left, right in pairs
            )
            target[pl.ds(place.order[k] * group, group), :, c0 : c0 + cn] = got.astype(target.dtype).reshape(
                group, rows // group, cn
            )

    def round_of(some, t):
        for way in some:
            for step in way.at_time(t):
                step()

    for t in range(NZ):
        for n, way in enumerate(ways):
            width = held[n].shape[2]
            products([(left_one, right_one) if n < 2 else (left_two, right_two)], held[n], far[t], n % 2 * width)
            way.first(far[t])
        if t > 0:
            round_of(ways, t - 1)
    fetch.wait()
    for c0, cn in columns_of(grad_in.shape[1]):
        grad_in[:, c0 : c0 + cn] = lax.dot_general(
            right_one[...], matrix[c0 : c0 + cn], (((1,), (1,)), ((), ())), preferred_element_type=f32
        )
    count = grad_in.shape[0]
    factor = grad_in[...] * unit[...]
    high = factor.astype(bf)
    halves[:count] = high
    halves[count:] = (factor - high.astype(f32)).astype(bf)
    scaled = grad_in[...] * gain[...]
    mean = jnp.mean(scaled * unit[...], axis=1, keepdims=True)
    grad_input[...] = grad_mixed[...] + inverse[...] * (scaled - unit[...] * mean)
    column = (lax.broadcasted_iota(jnp.int32, (2 * count, 128), 1) == gain_at).astype(f32).astype(bf)
    for k in far:
        products([(left_small, right_small), (halves, column)], held[-1], k)
        small_way.first(k)
    late = [(0, 1, 2), (3, 4), (5,), (6,)]
    for n, t in enumerate(range(NZ - 1, NZ + 3)):
        round_of(ways, t)
        for t_small in late[n]:
            round_of([small_way], t_small)
    for n, way in enumerate(ways):
        width = held[n].shape[2]
        way.last(outs[n // 2].at[:, pl.ds(n % 2 * width, width)])
    small_way.last(outs[2])
    for way in ways + [small_way]:
        way.finish()


def return_weights(lefts, rights, matrix, unit, inverse, gain, grad_mixed, gain_at, collective_id):
    width = lefts[0].shape[1]
    rows = width // (NZ * NY * NX * NC)
    widths = [r.shape[1] for r in rights]
    whole = (Z, Y, X, C)
    orders = ((C, Y, Z, X), (C, X, Z, Y), (C, Y, X, Z), (C, X, Y, Z), (C, Y, X, Z))
    plans = [Plan(0, order, whole) for order in orders]
    parts = [widths[0] // 2] * 2 + [widths[1] // 2] * 2 + [widths[2]]
    bf, f32 = jnp.bfloat16, jnp.float32
    dma = pltpu.SemaphoreType.DMA
    vmem = pl.BlockSpec(memory_space=pltpu.VMEM)
    count = unit.shape[0]
    return pl.pallas_call(
        functools.partial(weights_kernel, plans, gain_at),
        out_shape=[jax.ShapeDtypeStruct((rows, w), f32) for w in widths] + [jax.ShapeDtypeStruct(unit.shape, f32)],
        in_specs=[vmem] * 6 + [pl.BlockSpec(memory_space=pl.ANY)] + [vmem] * 4,
        out_specs=[vmem] * 4,
        scratch_shapes=[pltpu.VMEM((plans[0].blocks, rows, w), bf) for w in parts]
        + [pltpu.VMEM((n, rows, w), bf) for p, w in zip(plans, parts) for n in Reduce.counts(p)[0]]
        + [pltpu.VMEM(matrix.shape, bf), pltpu.VMEM(unit.shape, f32), pltpu.VMEM((2 * count, width), bf)]
        + [dma((n,)) for p in plans for n in Reduce.counts(p)[1:]]
        + [dma(()), dma(())],
        compiler_params=pltpu.CompilerParams(
            collective_id=collective_id, has_side_effects=True, vmem_limit_bytes=64 * 1024 * 1024
        ),
        name="return_weights",
    )(*[a for pair in zip(lefts, rights) for a in pair], matrix, unit, inverse, gain, grad_mixed)


def turn(block, cosine, sine):
    lane = lax.broadcasted_iota(jnp.int32, (1, 128), 1)
    half = HEAD_SIZE // 2
    other = jnp.where(lane % HEAD_SIZE < half, pltpu.roll(block, 128 - half, 1), pltpu.roll(block, half, 1))
    return block * cosine + other * sine


def place_heads(read, target, count):
    group = QUERY_HEADS // KEY_VALUE_HEADS
    lane = lax.broadcasted_iota(jnp.int32, (1, 2 * HEAD_SIZE), 1)
    for pair in range(QUERY_HEADS // 2):
        both = read(pair)
        for h in (2 * pair, 2 * pair + 1):
            m, g = h // group, h % group
            block = both if h % 2 == m % 2 else pltpu.roll(both, HEAD_SIZE, 1)
            block = jnp.where(lane // HEAD_SIZE == m % 2, block, 0.0)
            target[m, g * count : (g + 1) * count] = block.astype(target.dtype)


def collect_heads(source, target, count, finish):
    group = QUERY_HEADS // KEY_VALUE_HEADS
    lane = lax.broadcasted_iota(jnp.int32, (1, 2 * HEAD_SIZE), 1)
    for pair in range(QUERY_HEADS // 2):
        sides = []
        for h in (2 * pair, 2 * pair + 1):
            m, g = h // group, h % group
            block = source[m, g * count : (g + 1) * count]
            sides.append(block if h % 2 == m % 2 else pltpu.roll(block, HEAD_SIZE, 1))
        both = finish(jnp.where(lane < HEAD_SIZE, *sides))
        target[:, pair * 128 : pair * 128 + 128] = both.astype(target.dtype)


class Scores:
    def __init__(self, place, queries, keys):
        self.queries, self.keys = queries, keys
        group = QUERY_HEADS // KEY_VALUE_HEADS
        count = keys.shape[1]
        self.total = keys.shape[0] * count
        row = lax.broadcasted_iota(jnp.int32, (group * count, 1), 0) % count
        self.position = row + (place.at[Z] * NY + place.at[Y]) * count
        self.column = lax.broadcasted_iota(jnp.int32, (1, self.total), 1)

    def pair(self, m, shift):
        at = pl.ds(pl.multiple_of(shift + m // 2 * 128, 128), 128)
        return self.keys[:, :, at].reshape(self.total, 128)

    def of(self, m, keys):
        found = lax.dot_general(
            self.queries[m], keys, (((1,), (1,)), ((), ())), preferred_element_type=jnp.float32
        )
        return jnp.where(self.column <= self.position, found * attn_scale, masked_logits)


def attend_kernel(
    plans, linear, cot, routes, cosine, sine, out, log_sums, kv_out, cots, placed, seen, own_kv, own_cots, raw, *sems
):
    send_kv, recv_kv, send_cot, recv_cot, spare, own_sem = sems
    place = Place()
    bf, f32 = jnp.bfloat16, jnp.float32
    count = linear.shape[0]
    width = KEY_VALUE_HEADS * HEAD_SIZE
    q_width = QUERY_HEADS * HEAD_SIZE
    for c0 in range(0, width, 128):
        block = linear[:, q_width + c0 : q_width + c0 + 128]
        own_kv[:, c0 : c0 + 128] = turn(block, cosine[...], sine[...]).astype(bf)
    own_kv[:, width:] = linear[:, q_width + width :].astype(bf)
    model = cot.shape[1]
    own_cots[:, :model] = cot[...].astype(bf)
    expert = lax.broadcasted_iota(jnp.int32, (1, 128), 1)
    routed = routes[:, 0:1] == expert
    for n in range(1, routes.shape[1]):
        routed = jnp.logical_or(routed, routes[:, n : n + 1] == expert)
    own_cots[:, model:] = routed.astype(f32).astype(bf)
    greet(place, (Z, Y, C))
    kv_way = Gather(place, plans[0], own_kv, seen, send_kv, recv_kv, spare, 0, 0)
    cot_ways, at = [], 0
    for n, plan in enumerate(plans[1:]):
        cot_ways.append(Gather(place, plan, own_cots, cots, send_cot, recv_cot, spare, at, n * plan.blocks))
        at += Gather.sends(plan)
    kv_way.step(0, ())
    for way in cot_ways:
        way.step(0, ())
    mine = pltpu.make_async_copy(own_cots, cots.at[flat_index(place.at, plans[1].index)], own_sem.at[0])
    mine.start()
    seen[flat_index(place.at, plans[0].index)] = own_kv[...]
    place_heads(lambda pair: turn(linear[:, pair * 128 : pair * 128 + 128], cosine[...], sine[...]), placed, count)
    log_sums[...] = jnp.zeros(log_sums.shape, f32)
    early = [e for e in gather_events(plans[1].order)[1:]]
    kv_events = gather_events(plans[0].order)[1:]
    for k, flips in kv_events:
        kv_way.step(k, flips)
        if len(early) > 8:
            event = early.pop(0)
            for way in cot_ways:
                way.step(*event)
    keep = pltpu.make_async_copy(seen, kv_out, own_sem.at[1])
    keep.start()
    scores = Scores(place, placed, seen)
    lane = lax.broadcasted_iota(jnp.int32, (1, 128), 1)

    def head(m, carry):
        for i in range(KEY_VALUE_HEADS):
            if early:
                event = early.pop(0)

                @pl.when(m == i)
                def _():
                    for way in cot_ways:
                        way.step(*event)

        s = scores.of(m, scores.pair(m, 0))
        best = jnp.max(s, axis=1, keepdims=True)
        weights = jnp.exp(s - best)
        total = jnp.sum(weights, axis=1, keepdims=True)
        mixed = jnp.dot(weights.astype(bf), scores.pair(m, width), preferred_element_type=f32)
        raw[m] = mixed / total
        log_sums[...] = jnp.where(lane == m, best + jnp.log(total), log_sums[...])
        return carry

    lax.fori_loop(0, KEY_VALUE_HEADS, head, 0)
    collect_heads(raw, out, count, lambda block: block)
    keep.wait()
    mine.wait()
    kv_way.finish()
    for way in cot_ways:
        way.finish()


def attend(linear, cot, routes, cosine, sine, collective_id):
    count = linear.shape[0]
    kv_width = 2 * KEY_VALUE_HEADS * HEAD_SIZE
    cut = count * 3 // 4
    plans = [
        Plan(0, (Z, Y), (Z, Y)),
        Plan(1, (Z, Y, C), (C, Z, Y), rows=(0, cut)),
        Plan(1, (Y, Z, C), (C, Z, Y), rows=(cut, count - cut)),
    ]
    bf, f32 = jnp.bfloat16, jnp.float32
    group = QUERY_HEADS // KEY_VALUE_HEADS
    vmem = pl.BlockSpec(memory_space=pltpu.VMEM)
    apart = pl.BlockSpec(memory_space=pl.ANY)
    dma = pltpu.SemaphoreType.DMA
    kv_shape = (plans[0].blocks, count, kv_width)
    cot_shape = (count, cot.shape[1] + 128)
    heads = (KEY_VALUE_HEADS, group * count, 2 * HEAD_SIZE)
    return pl.pallas_call(
        functools.partial(attend_kernel, plans),
        out_shape=[
            jax.ShapeDtypeStruct((count, QUERY_HEADS * HEAD_SIZE), bf),
            jax.ShapeDtypeStruct((group * count, 128), f32),
            jax.ShapeDtypeStruct(kv_shape, bf),
            jax.ShapeDtypeStruct((plans[1].blocks,) + cot_shape, bf),
            jax.ShapeDtypeStruct(heads, bf),
        ],
        in_specs=[vmem] * 5,
        out_specs=[vmem, vmem, apart, apart, vmem],
        scratch_shapes=[
            pltpu.VMEM(kv_shape, bf),
            pltpu.VMEM((count, kv_width), bf),
            pltpu.VMEM(cot_shape, bf),
            pltpu.VMEM(heads, f32),
        ]
        + [
            dma((Gather.sends(plans[0]),)),
            dma((plans[0].blocks,)),
            dma((Gather.sends(plans[1]) + Gather.sends(plans[2]),)),
            dma((plans[1].blocks + plans[2].blocks,)),
            dma(()),
            dma((2,)),
        ],
        compiler_params=pltpu.CompilerParams(
            collective_id=collective_id, has_side_effects=True, vmem_limit_bytes=56 * 1024 * 1024
        ),
        name="attend",
    )(linear, cot, routes, cosine, sine)


def attend_back_kernel(plans, *refs):
    placed, grad_attn, outputs, log_sums, keys, part, w_o, mixed, cosine, sine = refs[:10]
    back, layer_out = refs[10:12]
    kv_grad, grads_placed, raw, deltas, held, held_out, grads, matrix = refs[12:20]
    level, chain, out_level, out_level_two, out_chain = refs[20:25]
    send_kv, recv_kv, send_out, recv_out, spare, load_sem, matrix_sem = refs[25:]
    place = Place()
    bf, f32 = jnp.bfloat16, jnp.float32
    far = list(reversed(range(NZ)))
    loads = []
    for k in far:
        for h in (1 - place.at[C], place.at[C]):
            at = pl.ds((h * NZ + place.order[k]) * NY, NY)
            loads.append(pltpu.make_async_copy(part.at[at], held_out.at[at], load_sem.at[len(loads)]))
    for copy in loads:
        copy.start()
    fetch = pltpu.make_async_copy(w_o.at[:, pl.ds(0, matrix.shape[1])], matrix, matrix_sem)
    fetch.start()
    greet(place, (Z, Y, C))
    kv_way = Reduce(place, plans[0], held, (level,), chain, send_kv, recv_kv, spare)
    out_way = Reduce(place, plans[1], held_out, (out_level, out_level_two), out_chain, send_out, recv_out, spare)
    for copy in loads:
        copy.wait()
    for k in far:
        out_way.first(k)
    count = grads.shape[0]
    fetch.wait()
    for c0, cn in columns_of(grads.shape[1]):
        grads[:, c0 : c0 + cn] = lax.dot_general(
            grad_attn[...], matrix[c0 : c0 + cn], (((1,), (1,)), ((), ())), preferred_element_type=f32
        ).astype(bf)
    place_heads(lambda pair: grads[:, pair * 128 : pair * 128 + 128].astype(f32), grads_placed, count)
    group = QUERY_HEADS // KEY_VALUE_HEADS
    lane = lax.broadcasted_iota(jnp.int32, (1, 128), 1)
    for g in range(group):
        found = jnp.zeros((count, 128), f32)
        for m in range(KEY_VALUE_HEADS):
            h = m * group + g
            at = slice(h // 2 * 128, h // 2 * 128 + 128)
            both = grads[:, at].astype(f32) * outputs[:, at].astype(f32)
            delta = jnp.sum(jnp.where(lane // HEAD_SIZE == h % 2, both, 0.0), axis=1, keepdims=True)
            found = jnp.where(lane == m, delta, found)
        deltas[g * count : (g + 1) * count] = found
    scores = Scores(place, placed, keys)
    width = KEY_VALUE_HEADS * HEAD_SIZE
    blocks = keys.shape[0]
    turns = KEY_VALUE_HEADS // 2
    early = [[(out_way.level, 0, 3)], [(out_way.level, 0, 2)], [(out_way.level, 1, 3)], [(out_way.level, 1, 2), (out_way.along, 3)]]

    def pair(p, carry):
        for i in range(turns):

            @pl.when(p == i)
            def _():
                for step, *at in early[i]:
                    step(*at)

        key_sum = value_sum = None
        for side in range(2):
            m = 2 * p + side
            k_pair, v_pair = scores.pair(m, 0), scores.pair(m, width)
            of_head = lambda ref: jnp.sum(jnp.where(lane == m, ref[...], 0.0), axis=1, keepdims=True)
            weights = jnp.exp(scores.of(m, k_pair) - of_head(log_sums))
            grad = grads_placed[m]
            grad_probs = lax.dot_general(grad, v_pair, (((1,), (1,)), ((), ())), preferred_element_type=f32)
            grad_scores = (weights * (grad_probs - of_head(deltas))).astype(bf)
            raw[m] = attn_scale * jnp.dot(grad_scores, k_pair, preferred_element_type=f32)
            over_rows = (((0,), (0,)), ((), ()))
            key_part = lax.dot_general(grad_scores, placed[m], over_rows, preferred_element_type=f32)
            value_part = lax.dot_general(weights.astype(bf), grad, over_rows, preferred_element_type=f32)
            key_sum = key_part if key_sum is None else key_sum + key_part
            value_sum = value_part if value_sum is None else value_sum + value_part
        at = pl.multiple_of(p * 128, 128)
        held[:, :, pl.ds(at, 128)] = (attn_scale * key_sum).astype(bf).reshape(blocks, count, 128)
        at = pl.multiple_of(width + p * 128, 128)
        held[:, :, pl.ds(at, 128)] = value_sum.astype(bf).reshape(blocks, count, 128)
        return carry

    lax.fori_loop(0, turns, pair, 0)
    for k in far:
        kv_way.first(k)
    out_way.level(0, 1)
    out_way.level(0, 0)
    collect_heads(raw, back, count, lambda block: turn(block, cosine[...], -sine[...]))
    kv_way.level(0, 3)
    kv_way.level(0, 2)
    kv_way.along(3)
    kv_way.level(0, 1)
    kv_way.along(2)
    out_way.along(2)
    kv_way.level(0, 0)
    kv_way.along(1)
    kv_way.last(kv_grad)
    q_width = QUERY_HEADS * HEAD_SIZE
    for c0 in range(0, width, 128):
        block = turn(kv_grad[:, c0 : c0 + 128], cosine[...], -sine[...])
        back[:, q_width + c0 : q_width + c0 + 128] = block.astype(bf)
    back[:, q_width + width :] = kv_grad[:, width:].astype(bf)
    out_way.level(1, 1)
    out_way.along(1)
    out_way.level(1, 0)
    out_way.last(layer_out, mixed)
    kv_way.finish()
    out_way.finish()


def attend_back(placed, grad_attn, outputs, log_sums, keys, part, w_o, mixed, cosine, sine, collective_id):
    count, kv_width = keys.shape[1:]
    plans = [Plan(0, (Y,), (Z, Y)), Plan(1, (C, Y), (C, Z, Y))]
    bf, f32 = jnp.bfloat16, jnp.float32
    group = QUERY_HEADS // KEY_VALUE_HEADS
    vmem = pl.BlockSpec(memory_space=pltpu.VMEM)
    dma = pltpu.SemaphoreType.DMA
    heads = (KEY_VALUE_HEADS, group * count, 2 * HEAD_SIZE)
    levels, sends, recvs = Reduce.counts(plans[0])
    out_levels, out_sends, out_recvs = Reduce.counts(plans[1])
    return pl.pallas_call(
        functools.partial(attend_back_kernel, plans),
        out_shape=[
            jax.ShapeDtypeStruct((count, outputs.shape[1] + kv_width), bf),
            jax.ShapeDtypeStruct(mixed.shape, bf),
        ],
        in_specs=[vmem] * 5 + [pl.BlockSpec(memory_space=pl.ANY)] * 2 + [vmem] * 3,
        out_specs=[vmem] * 2,
        scratch_shapes=[
            pltpu.VMEM((count, kv_width), f32),
            pltpu.VMEM(heads, bf),
            pltpu.VMEM(heads, f32),
            pltpu.VMEM((group * count, 128), f32),
            pltpu.VMEM(keys.shape, bf),
            pltpu.VMEM(part.shape, bf),
            pltpu.VMEM(outputs.shape, bf),
            pltpu.VMEM((w_o.shape[0], grad_attn.shape[1]), bf),
        ]
        + [pltpu.VMEM((n,) + keys.shape[1:], bf) for n in levels]
        + [pltpu.VMEM((n,) + part.shape[1:], bf) for n in out_levels]
        + [dma((n,)) for n in (sends, recvs, out_sends, out_recvs)]
        + [dma(()), dma((NC * NZ,)), dma(())],
        compiler_params=pltpu.CompilerParams(
            collective_id=collective_id, has_side_effects=True, vmem_limit_bytes=60 * 1024 * 1024
        ),
        name="attend_back",
    )(placed, grad_attn, outputs, log_sums, keys, part, w_o, mixed, cosine, sine)


def last_kernel(core_ref, own, core_part, x_part, both_part, one, two, small, *outs):
    core = core_ref[0]
    in_out, out_out = outs[:2]
    split = in_out.shape[3]
    for at, left, right in ((core, own, x_part), (1 - core, core_part, both_part)):
        total = left[0].astype(jnp.float32) + right[0].astype(jnp.float32)
        in_out[at, 0] = total[:, :split]
        out_out[at, 0] = total[:, split:]

    @pl.when(jnp.logical_and(pl.program_id(0) == 0, pl.program_id(1) == 0))
    def _():
        wq, wk, wv, wo, router, first_gain, second_gain = outs[2:]
        q, k = wq.shape[1], wk.shape[1]
        wq[...] = one[:, :q]
        wk[...] = one[:, q : q + k]
        wv[...] = one[:, q + k :]
        wo[...] = two[...]
        router[...] = small[:, : router.shape[1]]
        turned = small[...].T
        at = router.shape[1]
        first_gain[...] = turned[at : at + 1]
        second_gain[...] = turned[at + 1 : at + 2]


def last_outputs(pieces, core, split, sums, widths):
    held, quarter, columns = pieces[0].shape
    step = quarter // 2
    rows = sums[0].shape[0]
    spec = pl.BlockSpec((1, step, columns), lambda e, r, c: (e, r, 0))
    fixed = lambda a, b: pl.BlockSpec((a, b), lambda e, r, c: (0, 0))
    outs = (split, columns - split)
    shapes = [(rows, w) for w in widths] + [(1, rows)] * 2
    return pl.pallas_call(
        last_kernel,
        grid_spec=pltpu.PrefetchScalarGridSpec(
            num_scalar_prefetch=1,
            grid=(held, 2),
            in_specs=[spec] * 4 + [fixed(*a.shape) for a in sums],
            out_specs=[pl.BlockSpec((NC, 1, step, w), lambda e, r, c: (0, e, r, 0)) for w in outs]
            + [fixed(*s) for s in shapes],
        ),
        out_shape=[jax.ShapeDtypeStruct((NC, held, quarter, w), jnp.float32) for w in outs]
        + [jax.ShapeDtypeStruct(s, jnp.float32) for s in shapes],
        name="last_outputs",
    )(core[None], *pieces, *sums)


MODEL_WIDTH = 1536
QUERY_HEADS = 24
KEY_VALUE_HEADS = 8
HEAD_SIZE = 64
EXPERT_HIDDEN = 512
EXPERT_COUNT = 32
TOP = 8
CAP = 40


norm_eps = 1e-06
attn_scale = 0.015625
rope_base = 10000.0
masked_logits = -1e30


def rope_tables(positions):
    half = HEAD_SIZE // 2
    frequency = jnp.power(
        jnp.float32(rope_base), -2.0 * jnp.arange(half, dtype=jnp.float32) / HEAD_SIZE
    )
    angle = positions.astype(jnp.float32)[:, None] * frequency[None, :]
    return (jnp.cos(angle)[:, None, :], jnp.sin(angle)[:, None, :])


def rotate_pairs(value_tensor, cosine_table, sine_table):
    half = value_tensor.shape[-1] // 2
    first = value_tensor[..., :half]
    second = value_tensor[..., half:]
    return jnp.concatenate(
        [first * cosine_table - second * sine_table, second * cosine_table + first * sine_table],
        axis=-1,
    )


def rms_forward(wide, gain):
    inverse = lax.rsqrt(jnp.mean(wide * wide, axis=-1, keepdims=True) + norm_eps)
    unit = wide * inverse
    return (unit, inverse, (unit * gain.astype(jnp.float32)).astype(jnp.bfloat16))


def rms_backward(grad, unit, inverse, gain):
    scaled = grad * gain.astype(jnp.float32)
    back = inverse * (scaled - unit * jnp.mean(scaled * unit, axis=-1, keepdims=True))
    return (back, jnp.sum(grad * unit, axis=0))


def piece_scores(query_rows, key_section, positions):
    token_count = key_section.shape[0]
    key_tensor = key_section.reshape(token_count, KEY_VALUE_HEADS, HEAD_SIZE)
    scores = (
        jnp.einsum("tkgd,nkd->kgtn", query_rows, key_tensor, preferred_element_type=jnp.float32)
        * attn_scale
    )
    visible = jnp.arange(token_count, dtype=jnp.int32)[None, :] <= positions[:, None]
    return (jnp.where(visible, scores, masked_logits), visible, key_tensor)


def local(
    hidden,
    routes,
    attn_norm,
    ffn_norm,
    w_q,
    key_weight,
    value_weight,
    w_o,
    router,
    expert_in,
    expert_out,
    cotangent,
):
    token_rows = hidden.shape[1]
    query_group = QUERY_HEADS // KEY_VALUE_HEADS
    ctx_size = lax.axis_size(CTX)
    sequence_length = token_rows * ctx_size
    positions = lax.axis_index(CTX) * token_rows + jnp.arange(token_rows, dtype=jnp.int32)
    cosine_table, sine_table = rope_tables(positions)
    contract_rows = (((0,), (0,)), ((), ()))
    contract_cols = (((1,), (1,)), ((), ()))
    layer = (
        lax.all_gather(attn_norm, (CTX, FSDP), axis=0, tiled=True),
        lax.all_gather(ffn_norm, (CTX, FSDP), axis=0, tiled=True),
        lax.all_gather(w_q, (CTX, FSDP), axis=0, tiled=True),
        lax.all_gather(key_weight, (CTX, FSDP), axis=0, tiled=True),
        lax.all_gather(value_weight, (CTX, FSDP), axis=0, tiled=True),
        lax.all_gather(w_o, (CTX, FSDP), axis=0, tiled=True),
        lax.all_gather(router, (CTX, FSDP), axis=0, tiled=True),
    )
    attn_gain, ffn_gain, query_w, key_weight_matrix, value_w, output_w, router_w = layer
    experts = (
        lax.all_gather(expert_in, FSDP, axis=1, tiled=True),
        lax.all_gather(expert_out, FSDP, axis=1, tiled=True),
    )
    weight_in, weight_out = experts
    wide = hidden[0].astype(jnp.float32)
    attn_unit, inverse_one, attention_input = rms_forward(wide, attn_gain)
    query_linear = jnp.dot(attention_input, query_w, preferred_element_type=jnp.float32).reshape(
        token_rows, QUERY_HEADS, HEAD_SIZE
    )
    query_rows = (
        rotate_pairs(query_linear, cosine_table, sine_table)
        .astype(jnp.bfloat16)
        .reshape(token_rows, KEY_VALUE_HEADS, query_group, HEAD_SIZE)
    )
    key_linear = jnp.dot(
        attention_input, key_weight_matrix, preferred_element_type=jnp.float32
    ).reshape(token_rows, KEY_VALUE_HEADS, HEAD_SIZE)
    key_matrix_rows = (
        rotate_pairs(key_linear, cosine_table, sine_table)
        .astype(jnp.bfloat16)
        .reshape(token_rows, KEY_VALUE_HEADS * HEAD_SIZE)
    )
    value_rows = jnp.dot(attention_input, value_w, preferred_element_type=jnp.float32).astype(
        jnp.bfloat16
    )
    init_state = (
        jnp.full((KEY_VALUE_HEADS, query_group, token_rows), masked_logits, jnp.float32),
        jnp.zeros((KEY_VALUE_HEADS, query_group, token_rows), jnp.float32),
        jnp.zeros((KEY_VALUE_HEADS, query_group, token_rows, HEAD_SIZE), jnp.float32),
    )
    key_section = lax.all_gather(key_matrix_rows, CTX, axis=0, tiled=True)
    value_section = lax.all_gather(value_rows, CTX, axis=0, tiled=True)

    def compute(current):
        best, total, weighted = current
        scores, visible, _ = piece_scores(query_rows, key_section, positions)
        value_tensor = value_section.reshape(value_section.shape[0], KEY_VALUE_HEADS, HEAD_SIZE)
        new_best = jnp.maximum(best, jnp.max(scores, axis=-1))
        weights = jnp.where(visible, jnp.exp(scores - new_best[..., None]), 0.0)
        total = jnp.sum(weights, axis=-1)
        weighted = jnp.einsum(
            "kgtn,nkd->kgtd",
            weights.astype(jnp.bfloat16),
            value_tensor,
            preferred_element_type=jnp.float32,
        )
        return (new_best, total, weighted)

    best, total, weighted = lax.cond(
        jnp.int32(0) <= positions[-1], compute, lambda current: current, init_state
    )
    log_sum_rows = best + jnp.log(total)
    attention_output = (
        jnp.transpose(weighted / total[..., None], (2, 0, 1, 3))
        .reshape(token_rows, QUERY_HEADS * HEAD_SIZE)
        .astype(jnp.bfloat16)
    )
    mixed = wide + jnp.dot(attention_output, output_w, preferred_element_type=jnp.float32)
    ffn_unit, inverse_two, ffn_in = rms_forward(mixed, ffn_gain)
    logits = jnp.dot(ffn_in, router_w, preferred_element_type=jnp.float32)
    route = routes[0]
    indicator = (route[:, :, None] == jnp.arange(EXPERT_COUNT, dtype=jnp.int32)).astype(jnp.float32)
    chosen = jnp.sum(indicator * logits[:, None, :], axis=-1)
    gates = jax.nn.softmax(chosen, axis=-1)
    flat_route = route.reshape(-1)
    counter = (flat_route[:, None] == jnp.arange(EXPERT_COUNT, dtype=jnp.int32)).astype(jnp.int32)
    slot = jnp.sum(counter * (jnp.cumsum(counter, axis=0) - 1), axis=1)
    target = flat_route * CAP + slot
    owner = (
        jnp.full((EXPERT_COUNT * CAP,), token_rows * TOP, jnp.int32)
        .at[target]
        .set(jnp.arange(token_rows * TOP, dtype=jnp.int32))
    )
    ffn_pad = jnp.concatenate([ffn_in, jnp.zeros((1, MODEL_WIDTH), jnp.bfloat16)], axis=0)
    local_experts = weight_in.shape[0]
    outgoing = ffn_pad[owner // TOP].reshape(ctx_size, local_experts, CAP, MODEL_WIDTH)
    received = lax.all_to_all(outgoing, CTX, split_axis=0, concat_axis=2, tiled=True)[0]
    act = jnp.einsum("erd,edf->erf", received, weight_in, preferred_element_type=jnp.float32)
    gate_part = act[..., :EXPERT_HIDDEN]
    up_part = act[..., EXPERT_HIDDEN:]
    sigma = jax.nn.sigmoid(gate_part)
    inner = (gate_part * sigma * up_part).astype(jnp.bfloat16)
    produced = jnp.einsum(
        "erf,edf->erd", inner, weight_out, preferred_element_type=jnp.float32
    ).astype(jnp.bfloat16)
    returned = lax.all_to_all(
        produced[None], CTX, split_axis=2, concat_axis=0, tiled=True
    ).reshape(EXPERT_COUNT * CAP, MODEL_WIDTH)
    picked = returned[target].reshape(token_rows, TOP, MODEL_WIDTH)
    layer_out = (mixed + jnp.sum(gates[..., None] * picked, axis=1)).astype(jnp.bfloat16)
    cot = cotangent[0]
    layer = (
        lax.all_gather(attn_norm, (CTX, FSDP), axis=0, tiled=True),
        lax.all_gather(ffn_norm, (CTX, FSDP), axis=0, tiled=True),
        lax.all_gather(w_q, (CTX, FSDP), axis=0, tiled=True),
        lax.all_gather(key_weight, (CTX, FSDP), axis=0, tiled=True),
        lax.all_gather(value_weight, (CTX, FSDP), axis=0, tiled=True),
        lax.all_gather(w_o, (CTX, FSDP), axis=0, tiled=True),
        lax.all_gather(router, (CTX, FSDP), axis=0, tiled=True),
    )
    attn_gain, ffn_gain, query_w, key_weight_matrix, value_w, output_w, router_w = layer
    experts = (
        lax.all_gather(expert_in, FSDP, axis=1, tiled=True),
        lax.all_gather(expert_out, FSDP, axis=1, tiled=True),
    )
    weight_in, weight_out = experts
    grad_gate = jnp.sum(cot[:, None, :] * picked, axis=-1)
    slot_grads = (
        (gates[..., None] * cot[:, None, :])
        .astype(jnp.bfloat16)
        .reshape(token_rows * TOP, MODEL_WIDTH)
    )
    slot_pad = jnp.concatenate([slot_grads, jnp.zeros((1, MODEL_WIDTH), jnp.bfloat16)], axis=0)
    grad_outgoing = slot_pad[owner].reshape(ctx_size, local_experts, CAP, MODEL_WIDTH)
    grad_received = lax.all_to_all(grad_outgoing, CTX, split_axis=0, concat_axis=2, tiled=True)[0]
    grad_w_out = jnp.einsum(
        "erd,erf->edf", grad_received, inner, preferred_element_type=jnp.float32
    )
    grad_inner = jnp.einsum(
        "erd,edf->erf", grad_received, weight_out, preferred_element_type=jnp.float32
    )
    grad_act = jnp.concatenate(
        [
            grad_inner * up_part * sigma * (1.0 + gate_part * (1.0 - sigma)),
            grad_inner * gate_part * sigma,
        ],
        axis=-1,
    ).astype(jnp.bfloat16)
    grad_w_in = jnp.einsum("erd,erf->edf", received, grad_act, preferred_element_type=jnp.float32)
    grad_rows = jnp.einsum(
        "erf,edf->erd", grad_act, weight_in, preferred_element_type=jnp.float32
    ).astype(jnp.bfloat16)
    grad_back = lax.all_to_all(
        grad_rows[None], CTX, split_axis=2, concat_axis=0, tiled=True
    ).reshape(EXPERT_COUNT * CAP, MODEL_WIDTH)
    grad_expert_in, grad_expert_out = (
        lax.psum_scatter(
            grad_w_in.astype(jnp.bfloat16), FSDP, scatter_dimension=1, tiled=True
        ).astype(jnp.float32),
        lax.psum_scatter(
            grad_w_out.astype(jnp.bfloat16), FSDP, scatter_dimension=1, tiled=True
        ).astype(jnp.float32),
    )
    grad_chosen = gates * (grad_gate - jnp.sum(gates * grad_gate, axis=-1, keepdims=True))
    grad_logits = jnp.sum(indicator * grad_chosen[..., None], axis=1).astype(jnp.bfloat16)
    grad_router_part = lax.dot_general(
        ffn_in, grad_logits, contract_rows, preferred_element_type=jnp.float32
    )
    grad_ffn_in = lax.dot_general(
        grad_logits, router_w, contract_cols, preferred_element_type=jnp.float32
    )
    grad_ffn_in = grad_ffn_in + jnp.sum(
        grad_back[target].reshape(token_rows, TOP, MODEL_WIDTH), axis=1, dtype=jnp.float32
    )
    back_two, grad_ffn_gain = rms_backward(grad_ffn_in, ffn_unit, inverse_two, ffn_gain)
    grad_mixed = cot + back_two
    grad_attn = grad_mixed.astype(jnp.bfloat16)
    grad_wo_part = lax.dot_general(
        attention_output, grad_attn, contract_rows, preferred_element_type=jnp.float32
    )
    attention_output_gradient = lax.dot_general(
        grad_attn, output_w, contract_cols, preferred_element_type=jnp.float32
    ).astype(jnp.bfloat16)
    head_gradient = attention_output_gradient.reshape(
        token_rows, KEY_VALUE_HEADS, query_group, HEAD_SIZE
    )
    delta_rows = jnp.sum(
        head_gradient.astype(jnp.float32)
        * attention_output.reshape(token_rows, KEY_VALUE_HEADS, query_group, HEAD_SIZE).astype(
            jnp.float32
        ),
        axis=-1,
    )
    delta_rows = jnp.transpose(delta_rows, (1, 2, 0))
    init_back = (
        jnp.zeros((token_rows, KEY_VALUE_HEADS, query_group, HEAD_SIZE), jnp.float32),
        jnp.zeros((sequence_length, 2 * KEY_VALUE_HEADS * HEAD_SIZE), jnp.float32),
    )
    attend_key_section = lax.all_gather(key_matrix_rows, CTX, axis=0, tiled=True)
    attend_value_section = lax.all_gather(value_rows, CTX, axis=0, tiled=True)

    def compute(current):
        token_count = attend_key_section.shape[0]
        scores, visible, key_tensor = piece_scores(query_rows, attend_key_section, positions)
        value_tensor = attend_value_section.reshape(token_count, KEY_VALUE_HEADS, HEAD_SIZE)
        weights_full = jnp.where(visible, jnp.exp(scores - log_sum_rows[..., None]), 0.0)
        grad_probs = jnp.einsum(
            "tkgd,nkd->kgtn", head_gradient, value_tensor, preferred_element_type=jnp.float32
        )
        grad_scores = (weights_full * (grad_probs - delta_rows[..., None])).astype(jnp.bfloat16)
        grad_query = attn_scale * jnp.einsum(
            "kgtn,nkd->tkgd", grad_scores, key_tensor, preferred_element_type=jnp.float32
        )
        key_portion = attn_scale * jnp.einsum(
            "kgtn,tkgd->nkd", grad_scores, query_rows, preferred_element_type=jnp.float32
        )
        value_portion = jnp.einsum(
            "kgtn,tkgd->nkd",
            weights_full.astype(jnp.bfloat16),
            head_gradient,
            preferred_element_type=jnp.float32,
        )
        update = jnp.concatenate(
            [
                key_portion.reshape(token_count, KEY_VALUE_HEADS * HEAD_SIZE),
                value_portion.reshape(token_count, KEY_VALUE_HEADS * HEAD_SIZE),
            ],
            axis=1,
        )
        return (grad_query, update)

    grad_query, grad_keys_full = lax.cond(
        jnp.int32(0) <= positions[-1], compute, lambda current: current, init_back
    )
    local_gradients = lax.psum_scatter(
        grad_keys_full.astype(jnp.bfloat16), CTX, scatter_dimension=0, tiled=True
    ).astype(jnp.float32)
    query_back = (
        rotate_pairs(
            grad_query.reshape(token_rows, QUERY_HEADS, HEAD_SIZE), cosine_table, -sine_table
        )
        .astype(jnp.bfloat16)
        .reshape(token_rows, QUERY_HEADS * HEAD_SIZE)
    )
    key_backward_rows = (
        rotate_pairs(
            local_gradients[:, : KEY_VALUE_HEADS * HEAD_SIZE].reshape(
                token_rows, KEY_VALUE_HEADS, HEAD_SIZE
            ),
            cosine_table,
            -sine_table,
        )
        .astype(jnp.bfloat16)
        .reshape(token_rows, KEY_VALUE_HEADS * HEAD_SIZE)
    )
    value_backward_rows = local_gradients[:, KEY_VALUE_HEADS * HEAD_SIZE :].astype(jnp.bfloat16)
    grad_wq_part = lax.dot_general(
        attention_input, query_back, contract_rows, preferred_element_type=jnp.float32
    )
    grad_wk_part = lax.dot_general(
        attention_input, key_backward_rows, contract_rows, preferred_element_type=jnp.float32
    )
    grad_wv_part = lax.dot_general(
        attention_input, value_backward_rows, contract_rows, preferred_element_type=jnp.float32
    )
    grad_attn_in = lax.dot_general(
        query_back, query_w, contract_cols, preferred_element_type=jnp.float32
    )
    grad_attn_in = grad_attn_in + lax.dot_general(
        key_backward_rows, key_weight_matrix, contract_cols, preferred_element_type=jnp.float32
    )
    grad_attn_in = grad_attn_in + lax.dot_general(
        value_backward_rows, value_w, contract_cols, preferred_element_type=jnp.float32
    )
    back_one, grad_attn_gain = rms_backward(grad_attn_in, attn_unit, inverse_one, attn_gain)
    grad_input = grad_mixed + back_one
    partial_sums = (
        lax.psum_scatter(
            grad_attn_gain.astype(jnp.bfloat16), CTX, scatter_dimension=0, tiled=True
        ).astype(jnp.float32),
        lax.psum_scatter(
            grad_ffn_gain.astype(jnp.bfloat16), CTX, scatter_dimension=0, tiled=True
        ).astype(jnp.float32),
        lax.psum_scatter(
            grad_wq_part.astype(jnp.bfloat16), CTX, scatter_dimension=0, tiled=True
        ).astype(jnp.float32),
        lax.psum_scatter(
            grad_wk_part.astype(jnp.bfloat16), CTX, scatter_dimension=0, tiled=True
        ).astype(jnp.float32),
        lax.psum_scatter(
            grad_wv_part.astype(jnp.bfloat16), CTX, scatter_dimension=0, tiled=True
        ).astype(jnp.float32),
        lax.psum_scatter(
            grad_wo_part.astype(jnp.bfloat16), CTX, scatter_dimension=0, tiled=True
        ).astype(jnp.float32),
        lax.psum_scatter(
            grad_router_part.astype(jnp.bfloat16), CTX, scatter_dimension=0, tiled=True
        ).astype(jnp.float32),
    )
    summed = (
        lax.psum_scatter(
            partial_sums[0].astype(jnp.bfloat16), FSDP, scatter_dimension=0, tiled=True
        ).astype(jnp.float32),
        lax.psum_scatter(
            partial_sums[1].astype(jnp.bfloat16), FSDP, scatter_dimension=0, tiled=True
        ).astype(jnp.float32),
        lax.psum_scatter(
            partial_sums[2].astype(jnp.bfloat16), FSDP, scatter_dimension=0, tiled=True
        ).astype(jnp.float32),
        lax.psum_scatter(
            partial_sums[3].astype(jnp.bfloat16), FSDP, scatter_dimension=0, tiled=True
        ).astype(jnp.float32),
        lax.psum_scatter(
            partial_sums[4].astype(jnp.bfloat16), FSDP, scatter_dimension=0, tiled=True
        ).astype(jnp.float32),
        lax.psum_scatter(
            partial_sums[5].astype(jnp.bfloat16), FSDP, scatter_dimension=0, tiled=True
        ).astype(jnp.float32),
        lax.psum_scatter(
            partial_sums[6].astype(jnp.bfloat16), FSDP, scatter_dimension=0, tiled=True
        ).astype(jnp.float32),
    )
    return (
        layer_out[None],
        grad_input[None],
        summed[0],
        summed[1],
        summed[2],
        summed[3],
        summed[4],
        summed[5],
        summed[6],
        grad_expert_in,
        grad_expert_out,
    )


def swap(a, flip):
    return lax.ppermute(a, FSDP, [(i, i ^ flip) for i in range(NX * NC)])


def fast_body(
    hidden,
    routes,
    attn_norm,
    ffn_norm,
    w_q,
    key_weight,
    value_weight,
    w_o,
    router,
    expert_in,
    expert_out,
    cotangent,
):
    tokens = hidden.shape[1]
    ctx = lax.axis_index(CTX)
    fsdp = lax.axis_index(FSDP)
    core = fsdp % NC
    rows = w_q.shape[0]
    quarter = expert_in.shape[1]
    kv_width = KEY_VALUE_HEADS * HEAD_SIZE
    q_width = QUERY_HEADS * HEAD_SIZE
    held = expert_in.shape[0] // NC
    bf = jnp.bfloat16
    f32 = jnp.float32
    positions = ctx * tokens + jnp.arange(tokens, dtype=jnp.int32)
    cosine_table, sine_table = (table[:, 0] for table in rope_tables(positions))
    cosine = jnp.concatenate([cosine_table] * 4, axis=1)
    sine = jnp.concatenate([-sine_table, sine_table] * 2, axis=1)
    contract_cols = (((1,), (1,)), ((), ()))
    wide = hidden[0].astype(f32)
    cot = cotangent[0]

    route = routes[0]
    indicator = (route[:, :, None] == jnp.arange(EXPERT_COUNT, dtype=jnp.int32)).astype(f32)
    part = rows // 3
    whole = (Z, Y, X, C)
    one, two, mine, *others = gather_weights(
        [w_q, key_weight, value_weight, w_o, router, attn_norm[None], ffn_norm[None]],
        [expert_in, expert_out],
        [
            Plan(0, (X, Z, Y, C), whole, rows=(2 * part, part)),
            Plan(1, (X, Z, Y, C), whole, rows=(part, part)),
            Plan(1, (X, Y, Z, C), whole, rows=(2 * part, part)),
            Plan(0, (Z, Y, X, C), whole, rows=(0, 2 * part)),
            Plan(1, (Z, Y, X, C), whole, rows=(0, part)),
        ],
        0,
    )
    parts = [mine, swap(mine, 2)] + [swap(other, 1) for other in others] + [swap(others[0], 3)]
    one = one.reshape(MODEL_WIDTH, -1)
    two = two.reshape(MODEL_WIDTH, -1)
    output_w = two[:, :MODEL_WIDTH]
    small = two[:, MODEL_WIDTH:]
    router_w = small[:, :EXPERT_COUNT]
    gains = lax.dot_general(
        jnp.eye(128, dtype=bf), small, contract_cols, preferred_element_type=f32
    )
    attn_gain, ffn_gain = gains[EXPERT_COUNT], gains[EXPERT_COUNT + 1]

    attn_unit, inverse_one, attention_input = rms_forward(wide, attn_gain)
    linear = jnp.dot(attention_input, one, preferred_element_type=f32)
    attention_output, log_sums, kv, cots, queries = attend(linear, cot, route, cosine, sine, 1)
    mixed = wide + jnp.dot(attention_output, output_w, preferred_element_type=f32)
    ffn_unit, inverse_two, ffn_in = rms_forward(mixed, ffn_gain)
    logits = jnp.dot(ffn_in, router_w, preferred_element_type=f32)
    chosen = jnp.sum(indicator * logits[:, None, :], axis=-1)
    gates = jax.nn.softmax(chosen, axis=-1)
    gate_map = jnp.sum(indicator * gates[..., None], axis=1)
    payload = jnp.concatenate(
        [ffn_in, gate_map.astype(bf), jnp.zeros((tokens, 128 - EXPERT_COUNT), bf)], axis=1
    )
    gin, moe_part, *pieces = moe(payload, cots, parts + others[-1:], CAP, 2)
    across = [swap(pieces[j], j) for j in range(1, NX * NC)]
    grad_gate_map = gin[:, MODEL_WIDTH : MODEL_WIDTH + EXPERT_COUNT] + gin[
        :, MODEL_WIDTH + EXPERT_COUNT : MODEL_WIDTH + 2 * EXPERT_COUNT
    ]
    grad_logits = (
        gate_map * (grad_gate_map - jnp.sum(gate_map * grad_gate_map, axis=-1, keepdims=True))
    ).astype(bf)
    grad_ffn_in = gin[:, :MODEL_WIDTH] + lax.dot_general(
        grad_logits, router_w, contract_cols, preferred_element_type=f32
    )
    back_two, _ = rms_backward(grad_ffn_in, ffn_unit, inverse_two, ffn_gain)
    grad_mixed = cot + back_two
    grad_attn = grad_mixed.astype(bf)
    back, layer_out = attend_back(
        queries, grad_attn, attention_output, log_sums, kv, moe_part, two, mixed, cosine, sine, 4
    )
    factor = grad_ffn_in * ffn_unit
    high = factor.astype(bf)
    low = (factor - high.astype(f32)).astype(bf)
    column = jnp.broadcast_to((jnp.arange(128) == EXPERT_COUNT + 1).astype(bf), (tokens, 128))
    logits_wide = jnp.concatenate([grad_logits, jnp.zeros((tokens, 128 - EXPERT_COUNT), bf)], axis=1)
    *sums, grad_input = return_weights(
        [attention_input, attention_output, jnp.concatenate([ffn_in, high, low])],
        [back, grad_attn, jnp.concatenate([logits_wide, column, column])],
        one,
        attn_unit,
        inverse_one,
        attn_gain.astype(f32)[None],
        grad_mixed,
        EXPERT_COUNT,
        5,
    )
    grad_expert_in, grad_expert_out, *rest, first_gain, second_gain = last_outputs(
        [pieces[0]] + across,
        core,
        2 * EXPERT_HIDDEN,
        sums,
        (q_width, kv_width, kv_width, MODEL_WIDTH, EXPERT_COUNT),
    )
    return (
        layer_out[None],
        grad_input[None],
        first_gain.reshape(rows),
        second_gain.reshape(rows),
        *rest,
        grad_expert_in.reshape(NC * held, quarter, -1),
        grad_expert_out.reshape(NC * held, quarter, -1),
    )


def fast(*args):
    return fast_body(*args)


def solution(mesh):
    placed = (
        P(FSDP, CTX, None),
        P(FSDP, CTX, None),
        P((CTX, FSDP)),
        P((CTX, FSDP)),
        P((CTX, FSDP), None),
        P((CTX, FSDP), None),
        P((CTX, FSDP), None),
        P((CTX, FSDP), None),
        P((CTX, FSDP), None),
        P(CTX, FSDP, None),
        P(CTX, FSDP, None),
        P(FSDP, CTX, None),
    )
    small = mesh.shape[CTX] == NZ * NY and mesh.shape[FSDP] == NX * NC
    return jax.shard_map(
        fast if small else local,
        mesh=mesh,
        in_specs=placed,
        out_specs=(
            P(FSDP, CTX, None),
            P(FSDP, CTX, None),
            P((CTX, FSDP)),
            P((CTX, FSDP)),
            P((CTX, FSDP), None),
            P((CTX, FSDP), None),
            P((CTX, FSDP), None),
            P((CTX, FSDP), None),
            P((CTX, FSDP), None),
            P(CTX, FSDP, None),
            P(CTX, FSDP, None),
        ),
        check_vma=False,
    )
```

```python
import functools
import itertools

import jax
import jax.numpy as jnp
from jax import lax
from jax.experimental import pallas as pl
from jax.experimental.pallas import tpu as pltpu
from jax.sharding import PartitionSpec as P


NY = 2
NZ = 4
NX = 2
NC = 2
DEV = pl.DeviceIdType.MESH
CTX, FSDP = "ctx", "fsdp"
Z, Y, X, C = 0, 1, 2, 3
SIZES = {Z: NZ, Y: NY, X: NX, C: NC}
UP, DOWN = 4, 5


class Plan:
    def __init__(self, ref, order, index, rows=None, view=None):
        self.ref, self.order, self.index, self.rows, self.view = ref, order, index, rows, view
        self.blocks = 1
        for d in index:
            self.blocks *= SIZES[d]


class Place:
    def __init__(self):
        ctx = lax.axis_index(CTX)
        fsdp = lax.axis_index(FSDP)
        self.at = {Z: ctx // NY, Y: ctx % NY, X: fsdp // NC, C: fsdp % NC}
        z = self.at[Z]
        low = z < NZ // 2
        base = jnp.where(low, z, NZ - 1 - z)
        near = [base, 1 - base, jnp.int32(2), jnp.int32(3)]
        self.order = [z] + [jnp.where(low, k, NZ - 1 - k) for k in near[1:]]

    def device(self, dim, value):
        spot = dict(self.at)
        spot[dim] = value
        return (spot[Z] * NY + spot[Y], spot[X] * NC + spot[C])

    def across(self, dim):
        return self.device(dim, 1 - self.at[dim])

    def along(self, step):
        return self.device(Z, self.at[Z] + step)

    def coords(self, z_from, flips):
        spot = {d: (1 - self.at[d] if d in flips else self.at[d]) for d in (Y, X, C)}
        spot[Z] = z_from
        return spot


def flat_index(spot, dims):
    index = 0
    for d in dims:
        index = index * SIZES[d] + spot[d]
    return index


def subsets(dims):
    return [c for n in range(len(dims) + 1) for c in itertools.combinations(dims, n)]


def greet(place, dims, more=()):
    barrier = pltpu.get_barrier_semaphore()
    z = place.at[Z]
    count = jnp.int32(0)
    for d in dims:
        if d == Z:
            @pl.when(z > 0)
            def _():
                pl.semaphore_signal(barrier, inc=1, device_id=place.along(-1), device_id_type=DEV)

            @pl.when(z < NZ - 1)
            def _():
                pl.semaphore_signal(barrier, inc=1, device_id=place.along(1), device_id_type=DEV)

            count = count + jnp.where(z > 0, 1, 0) + jnp.where(z < NZ - 1, 1, 0)
        else:
            pl.semaphore_signal(barrier, inc=1, device_id=place.across(d), device_id_type=DEV)
            count = count + 1
    for device in more:
        pl.semaphore_signal(barrier, inc=1, device_id=device, device_id_type=DEV)
        count = count + 1
    pl.semaphore_wait(barrier, count)


def gather_events(order):
    pairs = [d for d in order if d != Z]
    events = [(k, f) for k in range(NZ) for f in subsets(pairs)]
    return sorted(events, key=lambda e: (e[0] + len(e[1]), len(e[1])))


def gather_sends(order, k, flips):
    z_at = order.index(Z)
    last = max([order.index(d) for d in flips] + ([z_at] if k > 0 else []) + [-1])
    out = []
    for position, d in enumerate(order):
        if position > last:
            out.extend([UP, DOWN] if d == Z else [d])
    if k > 0 and last == z_at:
        out.extend([UP, DOWN])
    return out


def gather_kernel(plans, *refs):
    w_q, w_k, w_v, w_o, router, first_gain, second_gain, first_w, second_w = refs[:9]
    outs, (mine, *others) = refs[9:11], refs[11:14]
    send_sem, recv_sem, own_sem, stage, load_sem, store_sem, pack_one, pack_two = refs[14:]
    ins = pack_one, pack_two
    place = Place()
    held = mine.shape[0]
    split = first_w.shape[2]
    loads = []
    for side in range(2):
        base = (place.at[C] if side == 0 else 1 - place.at[C]) * held
        for e in range(held):
            to = stage.at[side * held + e]
            for w, at in ((first_w, pl.ds(0, split)), (second_w, pl.ds(split, second_w.shape[2]))):
                loads.append(pltpu.make_async_copy(w.at[base + e], to.at[:, at], load_sem.at[len(loads)]))
    for copy in loads:
        copy.start()
    stores = [pltpu.make_async_copy(stage.at[pl.ds(0, held)], mine, store_sem.at[0])] + [
        pltpu.make_async_copy(stage.at[pl.ds(held + e, 1)], out, store_sem.at[1 + e]) for e, out in enumerate(others)
    ]
    at = 0
    for w in (w_q, w_k, w_v):
        pack_one[:, at : at + w.shape[1]] = w[...]
        at += w.shape[1]
    model = w_o.shape[1]
    rows = w_o.shape[0]
    pack_two[:, :model] = w_o[...]
    same = lax.broadcasted_iota(jnp.int32, (rows, rows), 0) == lax.broadcasted_iota(jnp.int32, (rows, rows), 1)
    upright = lambda gain: jnp.sum(jnp.where(same, gain[...].astype(jnp.float32), 0.0), axis=1, keepdims=True)
    lane = lax.broadcasted_iota(jnp.int32, (1, 128), 1)
    count = router.shape[1]
    small = jnp.where(lane == count, upright(first_gain), jnp.where(lane == count + 1, upright(second_gain), 0.0))
    pack_two[:, model:] = small.astype(pack_two.dtype)
    pack_two[:, model : model + count] = router[...]
    z = place.at[Z]
    greet(place, sorted({d for p in plans for d in p.order}))
    pending = []
    slot = 0
    queue = []
    for n, plan in enumerate(plans):
        for rank, event in enumerate(gather_events(plan.order)):
            queue.append((rank / len(gather_events(plan.order)), n, event))
    queue.sort(key=lambda q: (q[0], q[1]))
    bases = [sum(p.blocks for p in plans[:n]) for n in range(len(plans))]
    for turn_at, (_, n, (k, flips)) in enumerate(queue):
        if turn_at == len(queue) // 3:
            for copy in loads:
                copy.wait()
            for copy in stores:
                copy.start()
        plan = plans[n]
        src = ins[plan.ref]
        out = outs[plan.ref]
        rows = plan.rows
        z_from = place.order[k]
        spot = place.coords(z_from, flips)
        index = flat_index(spot, plan.index)
        own = k == 0 and not flips
        if plan.view is not None:
            target = plan.view(out, spot, rows)
            source = src.at[:, pl.ds(rows[0], rows[1])] if own else target
        else:
            target = out.at[index] if rows is None else out.at[index, pl.ds(rows[0], rows[1])]
            source = (src if rows is None else src.at[pl.ds(rows[0], rows[1])]) if own else target
        sem = recv_sem.at[bases[n] + index]
        if not own:
            pltpu.make_async_remote_copy(
                src_ref=target, dst_ref=target, send_sem=own_sem.at[0], recv_sem=sem,
                device_id=place.across(C), device_id_type=DEV,
            ).wait_recv()
        for way in gather_sends(plan.order, k, flips):
            if way in (UP, DOWN):
                step = 1 if way == UP else -1
                go = z < NZ - 1 if way == UP else z > 0
                if k > 0:
                    go = jnp.logical_and(go, z_from < z if way == UP else z_from > z)
                dest = place.device(Z, jnp.clip(z + step, 0, NZ - 1))
            else:
                go, dest = None, place.across(way)
            copy = pltpu.make_async_remote_copy(
                src_ref=source, dst_ref=target, send_sem=send_sem.at[slot], recv_sem=sem,
                device_id=dest, device_id_type=DEV,
            )
            slot += 1
            if go is None:
                copy.start()
            else:
                pl.when(go)(copy.start)
            pending.append((go, copy.wait_send))
        if own:
            copy = pltpu.make_async_copy(source, target, own_sem.at[1 + n])
            copy.start()
            pending.append((None, copy.wait))
    for copy in stores:
        copy.wait()
    for go, wait in pending:
        if go is None:
            wait()
        else:
            pl.when(go)(wait)


def gather_weights(weights, experts, plans, collective_id):
    sends = sum(len(gather_sends(p.order, k, f)) for p in plans for k, f in gather_events(p.order))
    rows = weights[0].shape[0]
    bf = weights[0].dtype
    widths = [sum(w.shape[1] for w in weights[:3]), weights[3].shape[1] + 128]
    held = experts[0].shape[0] // NC
    pack = (experts[0].shape[1], experts[0].shape[2] + experts[1].shape[2])
    apart = pl.BlockSpec(memory_space=pl.ANY)
    dma = pltpu.SemaphoreType.DMA
    return pl.pallas_call(
        functools.partial(gather_kernel, plans),
        out_shape=[jax.ShapeDtypeStruct((plans[0].blocks, rows, w), bf) for w in widths]
        + [jax.ShapeDtypeStruct((n,) + pack, bf) for n in [held] + [1] * held],
        in_specs=[pl.BlockSpec(memory_space=pltpu.VMEM)] * len(weights) + [apart] * 2,
        out_specs=[apart] * (3 + held),
        scratch_shapes=[
            dma((sends,)),
            dma((sum(p.blocks for p in plans),)),
            dma((1 + len(plans),)),
            pltpu.VMEM((NC * held,) + pack, bf),
            dma((2 * NC * held,)),
            dma((1 + held,)),
        ]
        + [pltpu.VMEM((rows, w), bf) for w in widths],
        compiler_params=pltpu.CompilerParams(collective_id=collective_id, has_side_effects=True),
        name="gather_weights",
    )(*weights, *experts)


def add_into(acc, other):
    acc[...] = (acc[...].astype(jnp.float32) + other[...].astype(jnp.float32)).astype(acc.dtype)


class Gather:
    def __init__(self, place, plan, src, out, send_sem, recv_sem, spare_sem, slot, base):
        self.place, self.plan, self.src, self.out = place, plan, src, out
        self.send_sem, self.recv_sem, self.spare_sem = send_sem, recv_sem, spare_sem
        self.slot, self.base = slot, base
        self.pending = []

    @staticmethod
    def sends(plan):
        return sum(len(gather_sends(plan.order, k, f)) for k, f in gather_events(plan.order))

    def goes(self, way, k):
        z, z_from = self.place.at[Z], self.place.order[k]
        if way == UP:
            return z < NZ - 1 if k == 0 else jnp.logical_and(z < NZ - 1, z_from < z)
        return z > 0 if k == 0 else jnp.logical_and(z > 0, z_from > z)

    def part(self, ref):
        rows = self.plan.rows
        return ref if rows is None else ref.at[pl.ds(rows[0], rows[1])]

    def step(self, k, flips):
        place, plan = self.place, self.plan
        index = flat_index(place.coords(place.order[k], flips), plan.index)
        target = self.part(self.out.at[index])
        sem = self.recv_sem.at[self.base + index]
        source = target
        if k == 0 and not flips:
            source = self.part(self.src)
        else:
            pltpu.make_async_remote_copy(
                src_ref=target, dst_ref=target, send_sem=self.spare_sem, recv_sem=sem,
                device_id=place.across(C), device_id_type=DEV,
            ).wait_recv()
        for way in gather_sends(plan.order, k, flips):
            if way in (UP, DOWN):
                dest = place.device(Z, jnp.clip(place.at[Z] + (1 if way == UP else -1), 0, NZ - 1))
            else:
                dest = place.across(way)
            copy = pltpu.make_async_remote_copy(
                src_ref=source, dst_ref=target, send_sem=self.send_sem.at[self.slot], recv_sem=sem,
                device_id=dest, device_id_type=DEV,
            )
            if way in (UP, DOWN):
                pl.when(self.goes(way, k))(copy.start)
            else:
                copy.start()
            self.pending.append((way, k, self.slot))
            self.slot += 1

    def finish(self):
        for way, k, slot in self.pending:
            block = self.part(self.src)
            copy = pltpu.make_async_remote_copy(
                src_ref=block, dst_ref=block, send_sem=self.send_sem.at[slot], recv_sem=self.spare_sem,
                device_id=self.place.across(C), device_id_type=DEV,
            )
            if way in (UP, DOWN):
                pl.when(self.goes(way, k))(copy.wait_send)
            else:
                copy.wait_send()


class Reduce:
    def __init__(self, place, plan, held, levels, chain, send_sem, recv_sem, spare_sem):
        self.place, self.plan, self.held, self.levels, self.chain = place, plan, held, levels, chain
        self.send_sem, self.recv_sem, self.spare_sem = send_sem, recv_sem, spare_sem
        self.order, self.chain_at, self.kept, counts = Reduce.shape(plan)
        self.base = [sum(counts[:p]) for p in range(len(counts))]
        self.slot = 0

    @staticmethod
    def shape(plan):
        order = plan.order if Z in plan.order else plan.order + (Z,)
        at = order.index(Z)
        kept = [subsets(tuple(d for d in order[p + 1 :] if d != Z)) for p in range(len(order))]
        times = [NZ if p < at else NZ + 1 if p == at else 1 for p in range(len(order))]
        return order, at, kept, [n * len(f) for n, f in zip(times, kept)]

    @staticmethod
    def counts(plan):
        _, at, kept, counts = Reduce.shape(plan)
        buffers = counts[:at] + counts[at + 1 :] + [counts[at]]
        return buffers, sum(counts) - 2 * len(kept[at]), sum(counts)

    def level_of(self, p):
        return self.levels[p if p < self.chain_at else p - 1]

    def push(self, source, target, sem, dest):
        copy = pltpu.make_async_remote_copy(
            src_ref=source, dst_ref=target, send_sem=self.send_sem.at[self.slot], recv_sem=sem,
            device_id=dest, device_id_type=DEV,
        )
        self.slot += 1
        copy.start()

    def arrived(self, target, sem):
        pltpu.make_async_remote_copy(
            src_ref=target, dst_ref=target, send_sem=self.spare_sem, recv_sem=sem,
            device_id=self.place.across(C), device_id_type=DEV,
        ).wait_recv()

    def block(self, k, flips):
        return self.held.at[flat_index(self.place.coords(self.place.order[k], flips), self.plan.index)]

    def spot(self, p, k, flips):
        at = self.kept[p].index(flips)
        return at if p > self.chain_at else self.place.order[k] * len(self.kept[p]) + at

    def send(self, p, k, flips):
        dim = self.order[p]
        spot = self.spot(p, k, tuple(d for d in flips if d != dim))
        self.push(
            self.block(k, flips), self.level_of(p).at[spot],
            self.recv_sem.at[self.base[p] + spot], self.place.across(dim),
        )

    def first(self, k):
        for f in self.kept[0]:
            self.send(0, k, (self.order[0],) + f)

    def forward(self, p, k, flips):
        later = p + 1
        if later < len(self.order) and self.order[later] in flips:
            self.send(later, k, flips)

    def level(self, p, k):
        for f in sorted(self.kept[p], key=lambda f: -len(f)):
            spot = self.spot(p, k, f)
            self.arrived(self.level_of(p).at[spot], self.recv_sem.at[self.base[p] + spot])
            add_into(self.block(k, f), self.level_of(p).at[spot])
            self.forward(p, k, f)

    def link(self, spot, n):
        at = spot * len(self.kept[self.chain_at]) + n
        return self.chain.at[at], self.recv_sem.at[self.base[self.chain_at] + at]

    def along(self, k):
        z = self.place.at[Z]
        dest = self.place.order[k]
        up = dest > z
        for n, f in enumerate(self.kept[self.chain_at]):
            mine = self.block(k, f)
            target, sem = self.link(dest + jnp.where(up, 1, 0), n)

            @pl.when(jnp.where(up, z > 0, z < NZ - 1))
            def _():
                self.arrived(target, sem)
                add_into(mine, target)

            self.push(mine, target, sem, self.place.along(jnp.where(up, 1, -1)))

    def settle(self):
        z = self.place.at[Z]
        kept = self.kept[self.chain_at]
        for f in sorted(kept, key=lambda f: -len(f)):
            mine = self.block(0, f)
            for go, spot in ((z > 0, z + 1), (z < NZ - 1, z)):
                target, sem = self.link(spot, kept.index(f))

                @pl.when(go)
                def _():
                    self.arrived(target, sem)
                    add_into(mine, target)

            self.forward(self.chain_at, 0, f)

    def last(self, out, base=None):
        if self.chain_at == len(self.order) - 1:
            self.settle()
        total = self.block(0, ())[...].astype(jnp.float32)
        if base is not None:
            total = base[...] + total
        out[...] = total.astype(out.dtype)

    def at_time(self, t):
        far = list(reversed(range(NZ)))
        at = self.chain_at
        out = [functools.partial(self.level, p, far[t - p]) for p in range(at) if 0 <= t - p < NZ]
        if 0 <= t - at < NZ - 1:
            out.append(functools.partial(self.along, far[t - at]))
        if t - at == NZ - 1 and at < len(self.order) - 1:
            out.append(self.settle)
        out += [functools.partial(self.level, p, 0) for p in range(at + 1, len(self.order)) if t == NZ - 1 + p]
        return out

    def steps(self):
        return [step for t in range(NZ + len(self.order)) for step in self.at_time(t)]

    def finish(self):
        block = self.level_of(0).at[0]
        for slot in range(self.slot):
            pltpu.make_async_remote_copy(
                src_ref=block, dst_ref=block, send_sem=self.send_sem.at[slot], recv_sem=self.spare_sem,
                device_id=self.place.across(C), device_id_type=DEV,
            ).wait_send()


def tile_up(n, m):
    return (n + m - 1) // m * m


def columns_of(width, chunk=512):
    return [(i, min(chunk, width - i)) for i in range(0, width, chunk)]


def moe_kernel(plans, back, width, hidden, cap, *refs):
    payload, cots, w_own, w_x, w_core, w_core_last, w_both, w_send = refs[:8]
    gin_out, part_out = refs[8:10]
    grads = refs[10:14]
    (
        seen, cot_seen, weights, taken, cot_taken, rows_buf, scaled, grad_act, pick, stage,
        lvl_b0, lvl_b1, chain_b, lvl_c0, lvl_c1, chain_c,
        send_sem, recv_sem, spare_sem, send_b, recv_b, send_c, recv_c, load_sem, store_sem, part_sem, piece_sem,
    ) = refs[14:]
    bf, f32 = jnp.bfloat16, jnp.float32
    place = Place()
    count = payload.shape[0]
    pair = 2 * cap
    wide = width + 128
    quarter = width // (NX * NC)
    half = NZ * pair
    lanes = pick.shape[2]
    held = weights.shape[0]
    fsdp = place.at[X] * NC + place.at[C]
    first = (((place.at[Z] * NY + place.at[Y]) * NC) + place.at[C]) * held

    loads = []
    rows_of = lambda owner: pl.ds(pl.multiple_of(owner * quarter, quarter), quarter)
    sources = [(w_own, e, e, 0) for e in range(held)] + [(w_x, e, e, 2) for e in range(held)]
    sources += [(w_core, 0, 0, 1), (w_core_last, 0, held - 1, 1), (w_both, 0, 0, 3)]
    for ref, at, e, j in sources:
        loads.append(pltpu.make_async_copy(ref.at[at], weights.at[e, rows_of(fsdp ^ j)], load_sem.at[len(loads)]))
    there = (place.at[Z] * NY + place.at[Y], (1 - place.at[X]) * NC + 1 - place.at[C])
    piece = pltpu.make_async_remote_copy(
        src_ref=w_send.at[0], dst_ref=weights.at[held - 1, rows_of(fsdp)],
        send_sem=piece_sem.at[0], recv_sem=piece_sem.at[1], device_id=there, device_id_type=DEV,
    )
    base_of = lambda h, k: (jnp.where(h == 0, place.at[C], 1 - place.at[C]) * NZ + place.order[k]) * NY
    cot_loads = {}
    for k in range(NZ):
        for h in range(2):
            at = pl.ds(base_of(h, k), NY)
            cot_loads[(h, k)] = pltpu.make_async_copy(cots.at[at], cot_seen.at[at], load_sem.at[len(loads) + len(cot_loads)])

    greet(place, (Z, Y, C), (there,))
    piece.start()
    ways = []
    send_at = 0
    for n, plan in enumerate(plans):
        ways.append(Gather(place, plan, payload, seen, send_sem, recv_sem, spare_sem, send_at, n * plan.blocks))
        send_at += Gather.sends(plan)
    for way in ways:
        way.step(0, ())
    for key in cot_loads:
        cot_loads[key].start()
    for copy in loads:
        copy.start()
    seen[flat_index(place.at, plans[0].index)] = payload[...]

    row_id = lax.broadcasted_iota(jnp.int32, (NY * count, NY * count), 0)
    col_id = lax.broadcasted_iota(jnp.int32, (NY * count, NY * count), 1)
    earlier = jnp.logical_and(col_id < row_id, col_id // count == row_id // count).astype(bf)
    lane_id = lax.broadcasted_iota(jnp.int32, (1, 128), 1)
    here = [(lane_id == first + e).astype(f32) for e in range(held)]
    pick_lane = lax.broadcasted_iota(jnp.int32, (NY * count, lanes), 1).astype(f32)
    y_shift = (lax.broadcasted_iota(jnp.int32, (NY * count, 1), 0) // count * cap).astype(f32)

    row_of = lambda h, k: (k * NC + h) * pair

    def dispatch(source, target, h, k, cols):
        at = pl.ds(base_of(h, k), NY)
        r = row_of(h, k)
        for c0, cn in cols:
            block = source[at, :, c0 : c0 + cn].reshape(NY * count, cn)
            got = lax.dot_general(
                pick[h * NZ + k], block, (((0,), (0,)), ((), ())), preferred_element_type=f32
            ).astype(bf)
            for e in range(held):
                target[e, r : r + pair, c0 : c0 + cn] = got[e * pair : (e + 1) * pair]

    def cot_chunk(h, k):
        cot_loads[(h, k)].wait()
        at = pl.ds(base_of(h, k), NY)
        chosen = cot_seen[at, :, width:wide].reshape(NY * count, 128)
        before = jnp.dot(earlier, chosen, preferred_element_type=f32)
        picked = None
        for e in range(held):
            is_here = jnp.sum(chosen.astype(f32) * here[e], axis=1, keepdims=True)
            slot = jnp.sum(before * here[e], axis=1, keepdims=True) + y_shift + e * pair
            target = jnp.where(is_here > 0.5, slot, -1.0)
            hit = pick_lane == target
            picked = hit if picked is None else jnp.logical_or(picked, hit)
        pick[h * NZ + k] = picked.astype(f32).astype(bf)
        dispatch(cot_seen, cot_taken, h, k, columns_of(width))

    def hidden_chunk(h, e, n, tile):
        rows = pl.ds(h * half, half)
        tokens_in = taken[e, rows, :width]
        gate = jnp.sum(taken[e, rows, width:wide].astype(f32) * here[e], axis=1, keepdims=True)
        col = n * tile
        g = jnp.dot(tokens_in, weights[e, :, col : col + tile], preferred_element_type=f32)
        u = jnp.dot(tokens_in, weights[e, :, hidden + col : hidden + col + tile], preferred_element_type=f32)
        raw = jnp.dot(
            cot_taken[e, rows, :], weights[e, :, 2 * hidden + col : 2 * hidden + col + tile], preferred_element_type=f32
        )
        s = jax.nn.sigmoid(g)
        gs = g * s
        inner = gs * u
        scaled[e, rows, col : col + tile] = (inner * gate).astype(bf)
        grad_inner = raw * gate
        grad_act[e, rows, col : col + tile] = (grad_inner * u * s * (1.0 + g * (1.0 - s))).astype(bf)
        grad_act[e, rows, hidden + col : hidden + col + tile] = (grad_inner * gs).astype(bf)
        return jnp.sum(raw * inner, axis=1, keepdims=True)

    tile = min(256, hidden)
    found = {}

    def hidden_step(h, e, n):
        got = hidden_chunk(h, e, n, tile)
        found[(h, e)] = got if n == 0 else found[(h, e)] + got
        if n == hidden // tile - 1:
            gate_grad = found.pop((h, e))
            high = gate_grad.astype(bf).astype(f32)
            there = pl.ds(h * half, half)
            apart = (lane_id == EXPERT_COUNT + first + e).astype(f32)
            rows_buf[e, there, width:wide] = (high * here[e] + (gate_grad - high) * apart).astype(bf)

    def hidden_steps(h):
        return [functools.partial(hidden_step, h, e, n) for e in range(held) for n in range(hidden // tile)]

    def project(h, e, left, weight_cols):
        rows = pl.ds(h * half, half)
        lo, n = weight_cols
        for c0, cn in columns_of(width):
            rows_buf[e, rows, c0 : c0 + cn] = lax.dot_general(
                left[e, rows, :], weights[e, c0 : c0 + cn, lo : lo + n], (((1,), (1,)), ((), ())), preferred_element_type=f32
            ).astype(bf)

    def combine(target, h, k, cols):
        at = pl.ds(base_of(h, k), NY)
        r = row_of(h, k)
        for c0, cn in cols:
            parts = [rows_buf[e, r : r + pair, c0 : c0 + cn] for e in range(held)]
            if lanes > held * pair:
                parts.append(jnp.zeros((lanes - held * pair, cn), bf))
            got = jnp.dot(pick[h * NZ + k], jnp.concatenate(parts, axis=0), preferred_element_type=f32)
            target[at, :, c0 : c0 + cn] = got.astype(bf).reshape(NY, count, cn)

    stores = []

    def weight_grad(e, j):
        rows = pl.ds(pl.multiple_of((fsdp ^ j) * quarter, 128), quarter)
        slot = len(stores) % 2
        if len(stores) >= 2:
            stores[-2].wait()
        for c0, cn in columns_of(2 * hidden):
            stage[slot, :, c0 : c0 + cn] = lax.dot_general(
                taken[e, :, rows], grad_act[e, :, c0 : c0 + cn], (((0,), (0,)), ((), ())), preferred_element_type=f32
            ).astype(bf)
        stage[slot, :, 2 * hidden :] = lax.dot_general(
            cot_taken[e, :, rows], scaled[e], (((0,), (0,)), ((), ())), preferred_element_type=f32
        ).astype(bf)
        copy = pltpu.make_async_copy(stage.at[slot], grads[j].at[e], store_sem.at[len(stores)])
        copy.start()
        stores.append(copy)

    work = [functools.partial(cot_chunk, h, k) for h in range(NC) for k in range(NZ)]
    all_cols = columns_of(width) + [(width, 128)]
    ready = {(h, k): 0 for h in range(NC) for k in range(NZ)}
    ready[(0, 0)] = 1
    near_begun = False

    def wait_weights():
        for copy in loads:
            copy.wait()
        arrived = weights.at[held - 1, rows_of(fsdp ^ 3)]
        pltpu.make_async_remote_copy(
            src_ref=arrived, dst_ref=arrived, send_sem=piece_sem.at[0], recv_sem=piece_sem.at[1],
            device_id=there, device_id_type=DEV,
        ).wait_recv()

    for k, flips in gather_events(plans[0].order)[1:]:
        for way in ways:
            way.step(k, flips)
        key = (1 if C in flips else 0, k)
        ready[key] += 1
        if ready[key] == NY:
            work.append(functools.partial(dispatch, seen, taken, *key, all_cols))
            if all(ready[(g, n)] == NY for g in range(NC) for n in range(NZ // 2)) and not near_begun:
                near_begun = True
                work += [wait_weights] + hidden_steps(0)
        for _ in range(min(len(work), 1 if k < NZ - 1 else 2)):
            work.pop(0)()
    for chunk in work:
        chunk()
    for chunk in hidden_steps(1):
        chunk()

    far = list(reversed(range(NZ)))
    spare = spare_sem
    cut = lvl_b0.shape[2]
    in_ways = [
        Reduce(place, back[0], cot_seen.at[:, :, pl.ds(0, cut)], (lvl_b0, lvl_b1), chain_b, send_b, recv_b, spare),
        Reduce(place, back[1], cot_seen.at[:, :, pl.ds(cut, wide - cut)], (lvl_c0, lvl_c1), chain_c, send_c, recv_c, spare),
    ]
    in_steps = [step for t in range(NZ + 3) for way in in_ways for step in way.at_time(t)]
    for e in range(held):
        project(1, e, grad_act, (0, 2 * hidden))
    for k in far[: NZ // 2]:
        combine(cot_seen, 1, k, all_cols)
        for way in in_ways:
            way.first(k)
    for k in far[: NZ // 2]:
        combine(cot_seen, 0, k, all_cols)
    in_steps.pop(0)()
    in_steps.pop(0)()
    for e in range(held):
        project(0, e, grad_act, (0, 2 * hidden))
    in_steps.pop(0)()
    for k in far[NZ // 2 :]:
        combine(cot_seen, 1, k, all_cols)
        for way in in_ways:
            way.first(k)
    for _ in range(3):
        in_steps.pop(0)()
    for k in far[NZ // 2 :]:
        combine(cot_seen, 0, k, all_cols)
    for way in ways:
        way.finish()
    part_copies = []
    work = []

    def out_part(h, k):
        combine(seen, h, k, columns_of(width))
        at = pl.ds(base_of(h, k), NY)
        copy = pltpu.make_async_copy(seen.at[at, :, pl.ds(0, width)], part_out.at[at], part_sem.at[len(part_copies)])
        copy.start()
        part_copies.append(copy)

    for n in range(2):
        for e in range(held):
            work.append(functools.partial(project, n, e, scaled, (2 * hidden, hidden)))
        for k in range(n * NZ // 2, (n + 1) * NZ // 2):
            for h in range(NC):
                work.append(functools.partial(out_part, h, k))
    work += [functools.partial(weight_grad, e, j) for j in reversed(range(NX * NC)) for e in range(held)]
    while in_steps or work:
        for _ in range(2):
            if in_steps:
                in_steps.pop(0)()
        for _ in range(2):
            if work:
                work.pop(0)()
    in_ways[0].last(gin_out.at[:, pl.ds(0, cut)])
    in_ways[1].last(gin_out.at[:, pl.ds(cut, wide - cut)])
    piece.wait_send()
    for copy in stores[-2:] + part_copies:
        copy.wait()
    for way in in_ways:
        way.finish()


def moe(payload, cots, parts, cap, collective_id):
    count, wide = payload.shape
    width = wide - 128
    held, quarter, columns = parts[0].shape
    hidden = columns // 3
    cut = count * 3 // 4
    plans = [
        Plan(0, (Z, Y, C), (C, Z, Y), rows=(0, cut)),
        Plan(0, (Y, Z, C), (C, Z, Y), rows=(cut, count - cut)),
    ]
    back = [Plan(0, (C, Y, Z), (C, Z, Y)), Plan(0, (C, Z, Y), (C, Z, Y))]
    widths = (wide - wide // 4 // 128 * 128, wide // 4 // 128 * 128)
    blocks = NC * NZ * NY
    pair = NY * cap
    rows = blocks // NY * pair
    lanes = tile_up(held * pair, 128)
    bf, f32 = jnp.bfloat16, jnp.float32
    whole = pl.BlockSpec(memory_space=pltpu.VMEM)
    apart = pl.BlockSpec(memory_space=pl.ANY)
    dma = pltpu.SemaphoreType.DMA
    return pl.pallas_call(
        functools.partial(moe_kernel, plans, back, width, hidden, cap),
        out_shape=[
            jax.ShapeDtypeStruct((count, wide), f32),
            jax.ShapeDtypeStruct((blocks, count, width), bf),
        ]
        + [jax.ShapeDtypeStruct((held, quarter, columns), bf)] * (NX * NC),
        in_specs=[whole] + [apart] * 7,
        out_specs=[whole] + [apart] * (1 + NX * NC),
        scratch_shapes=[
            pltpu.VMEM((blocks, count, wide), bf),
            pltpu.VMEM((blocks, count, wide), bf),
            pltpu.VMEM((held, NX * NC * quarter, columns), bf),
            pltpu.VMEM((held, rows, wide), bf),
            pltpu.VMEM((held, rows, width), bf),
            pltpu.VMEM((held, rows, wide), bf),
            pltpu.VMEM((held, rows, hidden), bf),
            pltpu.VMEM((held, rows, 2 * hidden), bf),
            pltpu.VMEM((blocks // NY, NY * count, lanes), bf),
            pltpu.VMEM((2, quarter, columns), bf),
        ]
        + [pltpu.VMEM((n, count, w), bf) for p, w in zip(back, widths) for n in Reduce.counts(p)[0]]
        + [
            dma((sum(Gather.sends(p) for p in plans),)),
            dma((sum(p.blocks for p in plans),)),
            dma(()),
            *[dma((n,)) for p in back for n in Reduce.counts(p)[1:]],
            dma((held * NX * NC + blocks // NY,)),
            dma((held * NX * NC,)),
            dma((blocks // NY,)),
            dma((2,)),
        ],
        compiler_params=pltpu.CompilerParams(
            collective_id=collective_id, has_side_effects=True, vmem_limit_bytes=67043328
        ),
        name="experts",
    )(payload, cots, *parts)


def weights_kernel(plans, gain_at, *refs):
    left_one, right_one, left_two, right_two, left_small, right_small = refs[:6]
    matrix_in, hidden, gain, grad_mixed = refs[6:10]
    n_ways = len(plans)
    outs, grad_input = refs[10:13], refs[13]
    held = refs[14 : 14 + n_ways]
    buffers, refs = refs[14 + n_ways : 14 + 5 * n_ways], refs[14 + 5 * n_ways :]
    matrix, grad_in, halves = refs[:3]
    sems, (spare, matrix_sem) = refs[3 : 3 + 2 * n_ways], refs[3 + 2 * n_ways :]
    bf, f32 = jnp.bfloat16, jnp.float32
    place = Place()
    far = list(reversed(range(NZ)))
    fetch = pltpu.make_async_copy(matrix_in, matrix, matrix_sem)
    fetch.start()
    greet(place, (Z, Y, X, C))
    *ways, small_way = [
        Reduce(place, plan, held[n], buffers[4 * n : 4 * n + 3], buffers[4 * n + 3], sems[2 * n], sems[2 * n + 1], spare)
        for n, plan in enumerate(plans)
    ]
    group = NY * NX * NC
    rows = group * held[0].shape[1]

    def products(pairs, target, k, shift=0):
        at = pl.ds(pl.multiple_of(place.order[k] * rows, 128), rows)
        for c0, cn in columns_of(target.shape[2]):
            got = sum(
                lax.dot_general(
                    left[:, at], right[:, shift + c0 : shift + c0 + cn], (((0,), (0,)), ((), ())),
                    preferred_element_type=f32,
                )
                for left, right in pairs
            )
            target[pl.ds(place.order[k] * group, group), :, c0 : c0 + cn] = got.astype(target.dtype).reshape(
                group, rows // group, cn
            )

    def round_of(some, t):
        for way in some:
            for step in way.at_time(t):
                step()

    for t in range(NZ):
        for n, way in enumerate(ways):
            width = held[n].shape[2]
            products([(left_one, right_one) if n < 2 else (left_two, right_two)], held[n], far[t], n % 2 * width)
            way.first(far[t])
        if t > 0:
            round_of(ways, t - 1)
    fetch.wait()
    for c0, cn in columns_of(grad_in.shape[1]):
        grad_in[:, c0 : c0 + cn] = lax.dot_general(
            right_one[...], matrix[c0 : c0 + cn], (((1,), (1,)), ((), ())), preferred_element_type=f32
        )
    count = grad_in.shape[0]
    wide = hidden[...].astype(f32)
    inverse = lax.rsqrt(jnp.mean(wide * wide, axis=1, keepdims=True) + norm_eps)
    unit = wide * inverse
    factor = grad_in[...] * unit
    high = factor.astype(bf)
    halves[:count] = high
    halves[count:] = (factor - high.astype(f32)).astype(bf)
    scaled = grad_in[...] * gain[...]
    mean = jnp.mean(scaled * unit, axis=1, keepdims=True)
    grad_input[...] = grad_mixed[...] + inverse * (scaled - unit * mean)
    column = (lax.broadcasted_iota(jnp.int32, (2 * count, 128), 1) == gain_at).astype(f32).astype(bf)
    for k in far:
        products([(left_small, right_small), (halves, column)], held[-1], k)
        small_way.first(k)
    late = [(0, 1, 2), (3, 4), (5,), (6,)]
    for n, t in enumerate(range(NZ - 1, NZ + 3)):
        round_of(ways, t)
        for t_small in late[n]:
            round_of([small_way], t_small)
    for n, way in enumerate(ways):
        width = held[n].shape[2]
        way.last(outs[n // 2].at[:, pl.ds(n % 2 * width, width)])
    small_way.last(outs[2])
    for way in ways + [small_way]:
        way.finish()


def return_weights(lefts, rights, matrix, hidden, gain, grad_mixed, gain_at, collective_id):
    width = lefts[0].shape[1]
    rows = width // (NZ * NY * NX * NC)
    widths = [r.shape[1] for r in rights]
    whole = (Z, Y, X, C)
    orders = ((C, Y, Z, X), (C, X, Z, Y), (C, Y, X, Z), (C, X, Y, Z), (C, Y, X, Z))
    plans = [Plan(0, order, whole) for order in orders]
    parts = [widths[0] // 2] * 2 + [widths[1] // 2] * 2 + [widths[2]]
    bf, f32 = jnp.bfloat16, jnp.float32
    dma = pltpu.SemaphoreType.DMA
    vmem = pl.BlockSpec(memory_space=pltpu.VMEM)
    count = hidden.shape[0]
    return pl.pallas_call(
        functools.partial(weights_kernel, plans, gain_at),
        out_shape=[jax.ShapeDtypeStruct((rows, w), f32) for w in widths] + [jax.ShapeDtypeStruct(hidden.shape, f32)],
        in_specs=[vmem] * 6 + [pl.BlockSpec(memory_space=pl.ANY)] + [vmem] * 3,
        out_specs=[vmem] * 4,
        scratch_shapes=[pltpu.VMEM((plans[0].blocks, rows, w), bf) for w in parts]
        + [pltpu.VMEM((n, rows, w), bf) for p, w in zip(plans, parts) for n in Reduce.counts(p)[0]]
        + [pltpu.VMEM(matrix.shape, bf), pltpu.VMEM(hidden.shape, f32), pltpu.VMEM((2 * count, width), bf)]
        + [dma((n,)) for p in plans for n in Reduce.counts(p)[1:]]
        + [dma(()), dma(())],
        compiler_params=pltpu.CompilerParams(
            collective_id=collective_id, has_side_effects=True, vmem_limit_bytes=64 * 1024 * 1024
        ),
        name="return_weights",
    )(*[a for pair in zip(lefts, rights) for a in pair], matrix, hidden, gain, grad_mixed)


def turn(block, cosine, sine):
    lane = lax.broadcasted_iota(jnp.int32, (1, 128), 1)
    half = HEAD_SIZE // 2
    other = jnp.where(lane % HEAD_SIZE < half, pltpu.roll(block, 128 - half, 1), pltpu.roll(block, half, 1))
    return block * cosine + other * sine


def place_heads(read, target, count):
    group = QUERY_HEADS // KEY_VALUE_HEADS
    lane = lax.broadcasted_iota(jnp.int32, (1, 2 * HEAD_SIZE), 1)
    for pair in range(QUERY_HEADS // 2):
        both = read(pair)
        for h in (2 * pair, 2 * pair + 1):
            m, g = h // group, h % group
            block = both if h % 2 == m % 2 else pltpu.roll(both, HEAD_SIZE, 1)
            block = jnp.where(lane // HEAD_SIZE == m % 2, block, 0.0)
            target[m, g * count : (g + 1) * count] = block.astype(target.dtype)


def collect_heads(source, target, count, finish):
    group = QUERY_HEADS // KEY_VALUE_HEADS
    lane = lax.broadcasted_iota(jnp.int32, (1, 2 * HEAD_SIZE), 1)
    for pair in range(QUERY_HEADS // 2):
        sides = []
        for h in (2 * pair, 2 * pair + 1):
            m, g = h // group, h % group
            block = source[m, g * count : (g + 1) * count]
            sides.append(block if h % 2 == m % 2 else pltpu.roll(block, HEAD_SIZE, 1))
        both = finish(jnp.where(lane < HEAD_SIZE, *sides))
        target[:, pair * 128 : pair * 128 + 128] = both.astype(target.dtype)


class Scores:
    def __init__(self, place, queries, keys):
        self.queries, self.keys = queries, keys
        group = QUERY_HEADS // KEY_VALUE_HEADS
        count = keys.shape[1]
        self.total = keys.shape[0] * count
        row = lax.broadcasted_iota(jnp.int32, (group * count, 1), 0) % count
        self.position = row + (place.at[Z] * NY + place.at[Y]) * count
        self.column = lax.broadcasted_iota(jnp.int32, (1, self.total), 1)

    def pair(self, m, shift):
        at = pl.ds(pl.multiple_of(shift + m // 2 * 128, 128), 128)
        return self.keys[:, :, at].reshape(self.total, 128)

    def of(self, m, keys):
        found = lax.dot_general(
            self.queries[m], keys, (((1,), (1,)), ((), ())), preferred_element_type=jnp.float32
        )
        return jnp.where(self.column <= self.position, found * attn_scale, masked_logits)


def attend_kernel(
    plans, linear, cot, routes, cosine, sine, out, log_sums, kv_out, cots, placed, seen, own_kv, own_cots, raw, *sems
):
    send_kv, recv_kv, send_cot, recv_cot, spare, own_sem = sems
    place = Place()
    bf, f32 = jnp.bfloat16, jnp.float32
    count = linear.shape[0]
    width = KEY_VALUE_HEADS * HEAD_SIZE
    q_width = QUERY_HEADS * HEAD_SIZE
    for c0 in range(0, width, 128):
        block = linear[:, q_width + c0 : q_width + c0 + 128]
        own_kv[:, c0 : c0 + 128] = turn(block, cosine[...], sine[...]).astype(bf)
    own_kv[:, width:] = linear[:, q_width + width :].astype(bf)
    model = cot.shape[1]
    own_cots[:, :model] = cot[...].astype(bf)
    expert = lax.broadcasted_iota(jnp.int32, (1, 128), 1)
    routed = routes[:, 0:1] == expert
    for n in range(1, routes.shape[1]):
        routed = jnp.logical_or(routed, routes[:, n : n + 1] == expert)
    own_cots[:, model:] = routed.astype(f32).astype(bf)
    greet(place, (Z, Y, C))
    kv_way = Gather(place, plans[0], own_kv, seen, send_kv, recv_kv, spare, 0, 0)
    cot_ways, at = [], 0
    for n, plan in enumerate(plans[1:]):
        cot_ways.append(Gather(place, plan, own_cots, cots, send_cot, recv_cot, spare, at, n * plan.blocks))
        at += Gather.sends(plan)
    kv_way.step(0, ())
    for way in cot_ways:
        way.step(0, ())
    mine = pltpu.make_async_copy(own_cots, cots.at[flat_index(place.at, plans[1].index)], own_sem.at[0])
    mine.start()
    seen[flat_index(place.at, plans[0].index)] = own_kv[...]
    place_heads(lambda pair: turn(linear[:, pair * 128 : pair * 128 + 128], cosine[...], sine[...]), placed, count)
    log_sums[...] = jnp.zeros(log_sums.shape, f32)
    early = [e for e in gather_events(plans[1].order)[1:]]
    kv_events = gather_events(plans[0].order)[1:]
    for k, flips in kv_events:
        kv_way.step(k, flips)
        if len(early) > 8:
            event = early.pop(0)
            for way in cot_ways:
                way.step(*event)
    keep = pltpu.make_async_copy(seen, kv_out, own_sem.at[1])
    keep.start()
    scores = Scores(place, placed, seen)
    lane = lax.broadcasted_iota(jnp.int32, (1, 128), 1)

    def head(m, carry):
        for i in range(KEY_VALUE_HEADS):
            if early:
                event = early.pop(0)

                @pl.when(m == i)
                def _():
                    for way in cot_ways:
                        way.step(*event)

        s = scores.of(m, scores.pair(m, 0))
        best = jnp.max(s, axis=1, keepdims=True)
        weights = jnp.exp(s - best)
        total = jnp.sum(weights, axis=1, keepdims=True)
        mixed = jnp.dot(weights.astype(bf), scores.pair(m, width), preferred_element_type=f32)
        raw[m] = mixed / total
        log_sums[...] = jnp.where(lane == m, best + jnp.log(total), log_sums[...])
        return carry

    lax.fori_loop(0, KEY_VALUE_HEADS, head, 0)
    collect_heads(raw, out, count, lambda block: block)
    keep.wait()
    mine.wait()
    kv_way.finish()
    for way in cot_ways:
        way.finish()


def attend(linear, cot, routes, cosine, sine, collective_id):
    count = linear.shape[0]
    kv_width = 2 * KEY_VALUE_HEADS * HEAD_SIZE
    cut = count * 3 // 4
    plans = [
        Plan(0, (Z, Y), (Z, Y)),
        Plan(1, (Z, Y, C), (C, Z, Y), rows=(0, cut)),
        Plan(1, (Y, Z, C), (C, Z, Y), rows=(cut, count - cut)),
    ]
    bf, f32 = jnp.bfloat16, jnp.float32
    group = QUERY_HEADS // KEY_VALUE_HEADS
    vmem = pl.BlockSpec(memory_space=pltpu.VMEM)
    apart = pl.BlockSpec(memory_space=pl.ANY)
    dma = pltpu.SemaphoreType.DMA
    kv_shape = (plans[0].blocks, count, kv_width)
    cot_shape = (count, cot.shape[1] + 128)
    heads = (KEY_VALUE_HEADS, group * count, 2 * HEAD_SIZE)
    return pl.pallas_call(
        functools.partial(attend_kernel, plans),
        out_shape=[
            jax.ShapeDtypeStruct((count, QUERY_HEADS * HEAD_SIZE), bf),
            jax.ShapeDtypeStruct((group * count, 128), f32),
            jax.ShapeDtypeStruct(kv_shape, bf),
            jax.ShapeDtypeStruct((plans[1].blocks,) + cot_shape, bf),
            jax.ShapeDtypeStruct(heads, bf),
        ],
        in_specs=[vmem] * 5,
        out_specs=[vmem, vmem, apart, apart, vmem],
        scratch_shapes=[
            pltpu.VMEM(kv_shape, bf),
            pltpu.VMEM((count, kv_width), bf),
            pltpu.VMEM(cot_shape, bf),
            pltpu.VMEM(heads, f32),
        ]
        + [
            dma((Gather.sends(plans[0]),)),
            dma((plans[0].blocks,)),
            dma((Gather.sends(plans[1]) + Gather.sends(plans[2]),)),
            dma((plans[1].blocks + plans[2].blocks,)),
            dma(()),
            dma((2,)),
        ],
        compiler_params=pltpu.CompilerParams(
            collective_id=collective_id, has_side_effects=True, vmem_limit_bytes=56 * 1024 * 1024
        ),
        name="attend",
    )(linear, cot, routes, cosine, sine)


def attend_back_kernel(plans, *refs):
    placed, gin, gate_map, cot, ffn_gain, outputs, log_sums, keys, part, w_o, mixed, cosine, sine = refs[:13]
    back, layer_out, grad_mixed, grad_attn, left_small, right_small = refs[13:19]
    kv_grad, grads_placed, raw, deltas, held, held_out, grads, matrix = refs[19:27]
    level, chain, v_level, v_chain, out_level, out_level_two, out_chain = refs[27:34]
    send_kv, recv_kv, send_v, recv_v, send_out, recv_out, spare, load_sem, matrix_sem = refs[34:]
    place = Place()
    bf, f32 = jnp.bfloat16, jnp.float32
    far = list(reversed(range(NZ)))
    loads = []
    for k in far:
        for h in (1 - place.at[C], place.at[C]):
            at = pl.ds((h * NZ + place.order[k]) * NY, NY)
            loads.append(pltpu.make_async_copy(part.at[at], held_out.at[at], load_sem.at[len(loads)]))
    for copy in loads:
        copy.start()
    fetch = pltpu.make_async_copy(w_o, matrix, matrix_sem)
    fetch.start()
    greet(place, (Z, Y, C))
    width = KEY_VALUE_HEADS * HEAD_SIZE
    k_way = Reduce(place, plans[0], held.at[:, :, pl.ds(0, width)], (level,), chain, send_kv, recv_kv, spare)
    v_way = Reduce(place, plans[1], held.at[:, :, pl.ds(width, width)], (v_level,), v_chain, send_v, recv_v, spare)
    out_way = Reduce(place, plans[2], held_out, (out_level, out_level_two), out_chain, send_out, recv_out, spare)
    for copy in loads:
        copy.wait()
    for k in far:
        out_way.first(k)
    count = grads.shape[0]
    fetch.wait()
    model = cot.shape[1]
    lane = lax.broadcasted_iota(jnp.int32, (1, 128), 1)
    halves = gin[:, model:]
    gate_grad = jnp.where(lane < EXPERT_COUNT, halves + pltpu.roll(halves, 128 - EXPERT_COUNT, 1), 0.0)
    weighted = jnp.sum(gate_map[...] * gate_grad, axis=1, keepdims=True)
    grad_logits = (gate_map[...] * (gate_grad - weighted)).astype(bf)
    over_cols = (((1,), (1,)), ((), ()))
    inverse = lax.rsqrt(jnp.mean(mixed[...] * mixed[...], axis=1, keepdims=True) + norm_eps)
    unit = mixed[...] * inverse
    grad_in = gin[:, :model] + lax.dot_general(
        grad_logits, matrix[:, model:], over_cols, preferred_element_type=f32
    )
    scaled = grad_in * ffn_gain[...]
    grad_mixed[...] = cot[...] + inverse * (scaled - unit * jnp.mean(scaled * unit, axis=1, keepdims=True))
    grad_attn[...] = grad_mixed[...].astype(bf)
    factor = grad_in * unit
    high = factor.astype(bf)
    left_small[:count] = (unit * ffn_gain[...]).astype(bf)
    left_small[count : 2 * count] = high
    left_small[2 * count :] = (factor - high.astype(f32)).astype(bf)
    right_small[:count] = grad_logits
    right_small[count:] = jnp.broadcast_to(jnp.where(lane == EXPERT_COUNT + 1, 1.0, 0.0), (2 * count, 128)).astype(bf)
    for c0, cn in columns_of(grads.shape[1]):
        grads[:, c0 : c0 + cn] = lax.dot_general(
            grad_attn[...], matrix[c0 : c0 + cn, :model], over_cols, preferred_element_type=f32
        ).astype(bf)
    place_heads(lambda pair: grads[:, pair * 128 : pair * 128 + 128].astype(f32), grads_placed, count)
    group = QUERY_HEADS // KEY_VALUE_HEADS
    lane = lax.broadcasted_iota(jnp.int32, (1, 128), 1)
    for g in range(group):
        found = jnp.zeros((count, 128), f32)
        for m in range(KEY_VALUE_HEADS):
            h = m * group + g
            at = slice(h // 2 * 128, h // 2 * 128 + 128)
            both = grads[:, at].astype(f32) * outputs[:, at].astype(f32)
            delta = jnp.sum(jnp.where(lane // HEAD_SIZE == h % 2, both, 0.0), axis=1, keepdims=True)
            found = jnp.where(lane == m, delta, found)
        deltas[g * count : (g + 1) * count] = found
    scores = Scores(place, placed, keys)
    blocks = keys.shape[0]
    turns = KEY_VALUE_HEADS // 2
    early = [[(out_way.level, 0, 3)], [(out_way.level, 0, 2)], [(out_way.level, 1, 3)], [(out_way.level, 1, 2), (out_way.along, 3)]]

    def pair(p, carry):
        for i in range(turns):

            @pl.when(p == i)
            def _():
                for step, *at in early[i]:
                    step(*at)

        key_sum = value_sum = None
        for side in range(2):
            m = 2 * p + side
            k_pair, v_pair = scores.pair(m, 0), scores.pair(m, width)
            of_head = lambda ref: jnp.sum(jnp.where(lane == m, ref[...], 0.0), axis=1, keepdims=True)
            weights = jnp.exp(scores.of(m, k_pair) - of_head(log_sums))
            grad = grads_placed[m]
            grad_probs = lax.dot_general(grad, v_pair, (((1,), (1,)), ((), ())), preferred_element_type=f32)
            grad_scores = (weights * (grad_probs - of_head(deltas))).astype(bf)
            raw[m] = attn_scale * jnp.dot(grad_scores, k_pair, preferred_element_type=f32)
            over_rows = (((0,), (0,)), ((), ()))
            key_part = lax.dot_general(grad_scores, placed[m], over_rows, preferred_element_type=f32)
            value_part = lax.dot_general(weights.astype(bf), grad, over_rows, preferred_element_type=f32)
            key_sum = key_part if key_sum is None else key_sum + key_part
            value_sum = value_part if value_sum is None else value_sum + value_part
        at = pl.multiple_of(p * 128, 128)
        held[:, :, pl.ds(at, 128)] = (attn_scale * key_sum).astype(bf).reshape(blocks, count, 128)
        at = pl.multiple_of(width + p * 128, 128)
        held[:, :, pl.ds(at, 128)] = value_sum.astype(bf).reshape(blocks, count, 128)
        return carry

    lax.fori_loop(0, turns, pair, 0)
    for k in far:
        k_way.first(k)
    v_way.along(3)
    out_way.level(0, 1)
    out_way.level(0, 0)
    collect_heads(raw, back, count, lambda block: turn(block, cosine[...], -sine[...]))
    k_way.level(0, 3)
    v_way.along(2)
    k_way.level(0, 2)
    k_way.along(3)
    v_way.along(1)
    k_way.level(0, 1)
    k_way.along(2)
    out_way.along(2)
    v_way.settle()
    k_way.level(0, 0)
    k_way.along(1)
    k_way.last(kv_grad.at[:, pl.ds(0, width)])
    v_way.level(1, 0)
    v_way.last(kv_grad.at[:, pl.ds(width, width)])
    q_width = QUERY_HEADS * HEAD_SIZE
    for c0 in range(0, width, 128):
        block = turn(kv_grad[:, c0 : c0 + 128], cosine[...], -sine[...])
        back[:, q_width + c0 : q_width + c0 + 128] = block.astype(bf)
    back[:, q_width + width :] = kv_grad[:, width:].astype(bf)
    out_way.level(1, 1)
    out_way.along(1)
    out_way.level(1, 0)
    out_way.last(layer_out, mixed)
    for way in (k_way, v_way, out_way):
        way.finish()


def attend_back(
    placed, gin, gate_map, cot, ffn_gain, outputs, log_sums, keys, part, w_o, mixed, cosine, sine, collective_id
):
    count, kv_width = keys.shape[1:]
    plans = [Plan(0, (Y, Z), (Z, Y)), Plan(0, (Z, Y), (Z, Y)), Plan(1, (C, Y, Z), (C, Z, Y))]
    bf, f32 = jnp.bfloat16, jnp.float32
    group = QUERY_HEADS // KEY_VALUE_HEADS
    vmem = pl.BlockSpec(memory_space=pltpu.VMEM)
    apart = pl.BlockSpec(memory_space=pl.ANY)
    dma = pltpu.SemaphoreType.DMA
    heads = (KEY_VALUE_HEADS, group * count, 2 * HEAD_SIZE)
    blocks = [(count, kv_width // 2)] * 2 + [part.shape[1:]]
    return pl.pallas_call(
        functools.partial(attend_back_kernel, plans),
        out_shape=[
            jax.ShapeDtypeStruct((count, outputs.shape[1] + kv_width), bf),
            jax.ShapeDtypeStruct(mixed.shape, bf),
            jax.ShapeDtypeStruct(mixed.shape, f32),
            jax.ShapeDtypeStruct(mixed.shape, bf),
            jax.ShapeDtypeStruct((3 * count, mixed.shape[1]), bf),
            jax.ShapeDtypeStruct((3 * count, 128), bf),
        ],
        in_specs=[vmem] * 8 + [apart] * 2 + [vmem] * 3,
        out_specs=[vmem] * 6,
        scratch_shapes=[
            pltpu.VMEM((count, kv_width), f32),
            pltpu.VMEM(heads, bf),
            pltpu.VMEM(heads, f32),
            pltpu.VMEM((group * count, 128), f32),
            pltpu.VMEM(keys.shape, bf),
            pltpu.VMEM(part.shape, bf),
            pltpu.VMEM(outputs.shape, bf),
            pltpu.VMEM(w_o.shape, bf),
        ]
        + [pltpu.VMEM((n,) + b, bf) for p, b in zip(plans, blocks) for n in Reduce.counts(p)[0]]
        + [dma((n,)) for p in plans for n in Reduce.counts(p)[1:]]
        + [dma(()), dma((NC * NZ,)), dma(())],
        compiler_params=pltpu.CompilerParams(
            collective_id=collective_id, has_side_effects=True, vmem_limit_bytes=64 * 1024 * 1024
        ),
        name="attend_back",
    )(placed, gin, gate_map, cot, ffn_gain, outputs, log_sums, keys, part, w_o, mixed, cosine, sine)


def last_kernel(core_ref, own, core_part, x_part, both_part, one, two, small, layer, grad, *outs):
    core = core_ref[0]
    in_out, out_out = outs[:2]
    split = in_out.shape[3]
    for at, left, right in ((core, own, x_part), (1 - core, core_part, both_part)):
        total = left[0].astype(jnp.float32) + right[0].astype(jnp.float32)
        in_out[at, 0] = total[:, :split]
        out_out[at, 0] = total[:, split:]

    @pl.when(jnp.logical_and(pl.program_id(0) == 0, pl.program_id(1) == 0))
    def _():
        wq, wk, wv, wo, router, first_gain, second_gain, layer_out, grad_out = outs[2:]
        layer_out[...] = layer[...]
        grad_out[...] = grad[...]
        q, k = wq.shape[1], wk.shape[1]
        wq[...] = one[:, :q]
        wk[...] = one[:, q : q + k]
        wv[...] = one[:, q + k :]
        wo[...] = two[...]
        router[...] = small[:, : router.shape[1]]
        turned = small[...].T
        at = router.shape[1]
        first_gain[...] = turned[at : at + 1]
        second_gain[...] = turned[at + 1 : at + 2]


def last_outputs(pieces, core, split, sums, widths):
    held, quarter, columns = pieces[0].shape
    step = quarter // 4
    rows = sums[0].shape[0]
    spec = pl.BlockSpec((1, step, columns), lambda e, r, c: (e, r, 0))
    fixed = lambda a, b: pl.BlockSpec((a, b), lambda e, r, c: (0, 0))
    outs = (split, columns - split)
    shapes = [(rows, w) for w in widths] + [(1, rows)] * 2 + [a.shape for a in sums[3:]]
    types = [jnp.float32] * 7 + [a.dtype for a in sums[3:]]
    return pl.pallas_call(
        last_kernel,
        grid_spec=pltpu.PrefetchScalarGridSpec(
            num_scalar_prefetch=1,
            grid=(held, 4),
            in_specs=[spec] * 4 + [fixed(*a.shape) for a in sums],
            out_specs=[pl.BlockSpec((NC, 1, step, w), lambda e, r, c: (0, e, r, 0)) for w in outs]
            + [fixed(*s) for s in shapes],
        ),
        out_shape=[jax.ShapeDtypeStruct((NC, held, quarter, w), jnp.float32) for w in outs]
        + [jax.ShapeDtypeStruct(s, d) for s, d in zip(shapes, types)],
        name="last_outputs",
    )(core[None], *pieces, *sums)


MODEL_WIDTH = 1536
QUERY_HEADS = 24
KEY_VALUE_HEADS = 8
HEAD_SIZE = 64
EXPERT_HIDDEN = 512
EXPERT_COUNT = 32
TOP = 8
CAP = 40


norm_eps = 1e-06
attn_scale = 0.015625
rope_base = 10000.0
masked_logits = -1e30


def rope_tables(positions):
    half = HEAD_SIZE // 2
    frequency = jnp.power(
        jnp.float32(rope_base), -2.0 * jnp.arange(half, dtype=jnp.float32) / HEAD_SIZE
    )
    angle = positions.astype(jnp.float32)[:, None] * frequency[None, :]
    return (jnp.cos(angle)[:, None, :], jnp.sin(angle)[:, None, :])


def rotate_pairs(value_tensor, cosine_table, sine_table):
    half = value_tensor.shape[-1] // 2
    first = value_tensor[..., :half]
    second = value_tensor[..., half:]
    return jnp.concatenate(
        [first * cosine_table - second * sine_table, second * cosine_table + first * sine_table],
        axis=-1,
    )


def rms_forward(wide, gain):
    inverse = lax.rsqrt(jnp.mean(wide * wide, axis=-1, keepdims=True) + norm_eps)
    unit = wide * inverse
    return (unit, inverse, (unit * gain.astype(jnp.float32)).astype(jnp.bfloat16))


def rms_backward(grad, unit, inverse, gain):
    scaled = grad * gain.astype(jnp.float32)
    back = inverse * (scaled - unit * jnp.mean(scaled * unit, axis=-1, keepdims=True))
    return (back, jnp.sum(grad * unit, axis=0))


def piece_scores(query_rows, key_section, positions):
    token_count = key_section.shape[0]
    key_tensor = key_section.reshape(token_count, KEY_VALUE_HEADS, HEAD_SIZE)
    scores = (
        jnp.einsum("tkgd,nkd->kgtn", query_rows, key_tensor, preferred_element_type=jnp.float32)
        * attn_scale
    )
    visible = jnp.arange(token_count, dtype=jnp.int32)[None, :] <= positions[:, None]
    return (jnp.where(visible, scores, masked_logits), visible, key_tensor)


def local(
    hidden,
    routes,
    attn_norm,
    ffn_norm,
    w_q,
    key_weight,
    value_weight,
    w_o,
    router,
    expert_in,
    expert_out,
    cotangent,
):
    token_rows = hidden.shape[1]
    query_group = QUERY_HEADS // KEY_VALUE_HEADS
    ctx_size = lax.axis_size(CTX)
    sequence_length = token_rows * ctx_size
    positions = lax.axis_index(CTX) * token_rows + jnp.arange(token_rows, dtype=jnp.int32)
    cosine_table, sine_table = rope_tables(positions)
    contract_rows = (((0,), (0,)), ((), ()))
    contract_cols = (((1,), (1,)), ((), ()))
    layer = (
        lax.all_gather(attn_norm, (CTX, FSDP), axis=0, tiled=True),
        lax.all_gather(ffn_norm, (CTX, FSDP), axis=0, tiled=True),
        lax.all_gather(w_q, (CTX, FSDP), axis=0, tiled=True),
        lax.all_gather(key_weight, (CTX, FSDP), axis=0, tiled=True),
        lax.all_gather(value_weight, (CTX, FSDP), axis=0, tiled=True),
        lax.all_gather(w_o, (CTX, FSDP), axis=0, tiled=True),
        lax.all_gather(router, (CTX, FSDP), axis=0, tiled=True),
    )
    attn_gain, ffn_gain, query_w, key_weight_matrix, value_w, output_w, router_w = layer
    experts = (
        lax.all_gather(expert_in, FSDP, axis=1, tiled=True),
        lax.all_gather(expert_out, FSDP, axis=1, tiled=True),
    )
    weight_in, weight_out = experts
    wide = hidden[0].astype(jnp.float32)
    attn_unit, inverse_one, attention_input = rms_forward(wide, attn_gain)
    query_linear = jnp.dot(attention_input, query_w, preferred_element_type=jnp.float32).reshape(
        token_rows, QUERY_HEADS, HEAD_SIZE
    )
    query_rows = (
        rotate_pairs(query_linear, cosine_table, sine_table)
        .astype(jnp.bfloat16)
        .reshape(token_rows, KEY_VALUE_HEADS, query_group, HEAD_SIZE)
    )
    key_linear = jnp.dot(
        attention_input, key_weight_matrix, preferred_element_type=jnp.float32
    ).reshape(token_rows, KEY_VALUE_HEADS, HEAD_SIZE)
    key_matrix_rows = (
        rotate_pairs(key_linear, cosine_table, sine_table)
        .astype(jnp.bfloat16)
        .reshape(token_rows, KEY_VALUE_HEADS * HEAD_SIZE)
    )
    value_rows = jnp.dot(attention_input, value_w, preferred_element_type=jnp.float32).astype(
        jnp.bfloat16
    )
    init_state = (
        jnp.full((KEY_VALUE_HEADS, query_group, token_rows), masked_logits, jnp.float32),
        jnp.zeros((KEY_VALUE_HEADS, query_group, token_rows), jnp.float32),
        jnp.zeros((KEY_VALUE_HEADS, query_group, token_rows, HEAD_SIZE), jnp.float32),
    )
    key_section = lax.all_gather(key_matrix_rows, CTX, axis=0, tiled=True)
    value_section = lax.all_gather(value_rows, CTX, axis=0, tiled=True)

    def compute(current):
        best, total, weighted = current
        scores, visible, _ = piece_scores(query_rows, key_section, positions)
        value_tensor = value_section.reshape(value_section.shape[0], KEY_VALUE_HEADS, HEAD_SIZE)
        new_best = jnp.maximum(best, jnp.max(scores, axis=-1))
        weights = jnp.where(visible, jnp.exp(scores - new_best[..., None]), 0.0)
        total = jnp.sum(weights, axis=-1)
        weighted = jnp.einsum(
            "kgtn,nkd->kgtd",
            weights.astype(jnp.bfloat16),
            value_tensor,
            preferred_element_type=jnp.float32,
        )
        return (new_best, total, weighted)

    best, total, weighted = lax.cond(
        jnp.int32(0) <= positions[-1], compute, lambda current: current, init_state
    )
    log_sum_rows = best + jnp.log(total)
    attention_output = (
        jnp.transpose(weighted / total[..., None], (2, 0, 1, 3))
        .reshape(token_rows, QUERY_HEADS * HEAD_SIZE)
        .astype(jnp.bfloat16)
    )
    mixed = wide + jnp.dot(attention_output, output_w, preferred_element_type=jnp.float32)
    ffn_unit, inverse_two, ffn_in = rms_forward(mixed, ffn_gain)
    logits = jnp.dot(ffn_in, router_w, preferred_element_type=jnp.float32)
    route = routes[0]
    indicator = (route[:, :, None] == jnp.arange(EXPERT_COUNT, dtype=jnp.int32)).astype(jnp.float32)
    chosen = jnp.sum(indicator * logits[:, None, :], axis=-1)
    gates = jax.nn.softmax(chosen, axis=-1)
    flat_route = route.reshape(-1)
    counter = (flat_route[:, None] == jnp.arange(EXPERT_COUNT, dtype=jnp.int32)).astype(jnp.int32)
    slot = jnp.sum(counter * (jnp.cumsum(counter, axis=0) - 1), axis=1)
    target = flat_route * CAP + slot
    owner = (
        jnp.full((EXPERT_COUNT * CAP,), token_rows * TOP, jnp.int32)
        .at[target]
        .set(jnp.arange(token_rows * TOP, dtype=jnp.int32))
    )
    ffn_pad = jnp.concatenate([ffn_in, jnp.zeros((1, MODEL_WIDTH), jnp.bfloat16)], axis=0)
    local_experts = weight_in.shape[0]
    outgoing = ffn_pad[owner // TOP].reshape(ctx_size, local_experts, CAP, MODEL_WIDTH)
    received = lax.all_to_all(outgoing, CTX, split_axis=0, concat_axis=2, tiled=True)[0]
    act = jnp.einsum("erd,edf->erf", received, weight_in, preferred_element_type=jnp.float32)
    gate_part = act[..., :EXPERT_HIDDEN]
    up_part = act[..., EXPERT_HIDDEN:]
    sigma = jax.nn.sigmoid(gate_part)
    inner = (gate_part * sigma * up_part).astype(jnp.bfloat16)
    produced = jnp.einsum(
        "erf,edf->erd", inner, weight_out, preferred_element_type=jnp.float32
    ).astype(jnp.bfloat16)
    returned = lax.all_to_all(
        produced[None], CTX, split_axis=2, concat_axis=0, tiled=True
    ).reshape(EXPERT_COUNT * CAP, MODEL_WIDTH)
    picked = returned[target].reshape(token_rows, TOP, MODEL_WIDTH)
    layer_out = (mixed + jnp.sum(gates[..., None] * picked, axis=1)).astype(jnp.bfloat16)
    cot = cotangent[0]
    layer = (
        lax.all_gather(attn_norm, (CTX, FSDP), axis=0, tiled=True),
        lax.all_gather(ffn_norm, (CTX, FSDP), axis=0, tiled=True),
        lax.all_gather(w_q, (CTX, FSDP), axis=0, tiled=True),
        lax.all_gather(key_weight, (CTX, FSDP), axis=0, tiled=True),
        lax.all_gather(value_weight, (CTX, FSDP), axis=0, tiled=True),
        lax.all_gather(w_o, (CTX, FSDP), axis=0, tiled=True),
        lax.all_gather(router, (CTX, FSDP), axis=0, tiled=True),
    )
    attn_gain, ffn_gain, query_w, key_weight_matrix, value_w, output_w, router_w = layer
    experts = (
        lax.all_gather(expert_in, FSDP, axis=1, tiled=True),
        lax.all_gather(expert_out, FSDP, axis=1, tiled=True),
    )
    weight_in, weight_out = experts
    grad_gate = jnp.sum(cot[:, None, :] * picked, axis=-1)
    slot_grads = (
        (gates[..., None] * cot[:, None, :])
        .astype(jnp.bfloat16)
        .reshape(token_rows * TOP, MODEL_WIDTH)
    )
    slot_pad = jnp.concatenate([slot_grads, jnp.zeros((1, MODEL_WIDTH), jnp.bfloat16)], axis=0)
    grad_outgoing = slot_pad[owner].reshape(ctx_size, local_experts, CAP, MODEL_WIDTH)
    grad_received = lax.all_to_all(grad_outgoing, CTX, split_axis=0, concat_axis=2, tiled=True)[0]
    grad_w_out = jnp.einsum(
        "erd,erf->edf", grad_received, inner, preferred_element_type=jnp.float32
    )
    grad_inner = jnp.einsum(
        "erd,edf->erf", grad_received, weight_out, preferred_element_type=jnp.float32
    )
    grad_act = jnp.concatenate(
        [
            grad_inner * up_part * sigma * (1.0 + gate_part * (1.0 - sigma)),
            grad_inner * gate_part * sigma,
        ],
        axis=-1,
    ).astype(jnp.bfloat16)
    grad_w_in = jnp.einsum("erd,erf->edf", received, grad_act, preferred_element_type=jnp.float32)
    grad_rows = jnp.einsum(
        "erf,edf->erd", grad_act, weight_in, preferred_element_type=jnp.float32
    ).astype(jnp.bfloat16)
    grad_back = lax.all_to_all(
        grad_rows[None], CTX, split_axis=2, concat_axis=0, tiled=True
    ).reshape(EXPERT_COUNT * CAP, MODEL_WIDTH)
    grad_expert_in, grad_expert_out = (
        lax.psum_scatter(
            grad_w_in.astype(jnp.bfloat16), FSDP, scatter_dimension=1, tiled=True
        ).astype(jnp.float32),
        lax.psum_scatter(
            grad_w_out.astype(jnp.bfloat16), FSDP, scatter_dimension=1, tiled=True
        ).astype(jnp.float32),
    )
    grad_chosen = gates * (grad_gate - jnp.sum(gates * grad_gate, axis=-1, keepdims=True))
    grad_logits = jnp.sum(indicator * grad_chosen[..., None], axis=1).astype(jnp.bfloat16)
    grad_router_part = lax.dot_general(
        ffn_in, grad_logits, contract_rows, preferred_element_type=jnp.float32
    )
    grad_ffn_in = lax.dot_general(
        grad_logits, router_w, contract_cols, preferred_element_type=jnp.float32
    )
    grad_ffn_in = grad_ffn_in + jnp.sum(
        grad_back[target].reshape(token_rows, TOP, MODEL_WIDTH), axis=1, dtype=jnp.float32
    )
    back_two, grad_ffn_gain = rms_backward(grad_ffn_in, ffn_unit, inverse_two, ffn_gain)
    grad_mixed = cot + back_two
    grad_attn = grad_mixed.astype(jnp.bfloat16)
    grad_wo_part = lax.dot_general(
        attention_output, grad_attn, contract_rows, preferred_element_type=jnp.float32
    )
    attention_output_gradient = lax.dot_general(
        grad_attn, output_w, contract_cols, preferred_element_type=jnp.float32
    ).astype(jnp.bfloat16)
    head_gradient = attention_output_gradient.reshape(
        token_rows, KEY_VALUE_HEADS, query_group, HEAD_SIZE
    )
    delta_rows = jnp.sum(
        head_gradient.astype(jnp.float32)
        * attention_output.reshape(token_rows, KEY_VALUE_HEADS, query_group, HEAD_SIZE).astype(
            jnp.float32
        ),
        axis=-1,
    )
    delta_rows = jnp.transpose(delta_rows, (1, 2, 0))
    init_back = (
        jnp.zeros((token_rows, KEY_VALUE_HEADS, query_group, HEAD_SIZE), jnp.float32),
        jnp.zeros((sequence_length, 2 * KEY_VALUE_HEADS * HEAD_SIZE), jnp.float32),
    )
    attend_key_section = lax.all_gather(key_matrix_rows, CTX, axis=0, tiled=True)
    attend_value_section = lax.all_gather(value_rows, CTX, axis=0, tiled=True)

    def compute(current):
        token_count = attend_key_section.shape[0]
        scores, visible, key_tensor = piece_scores(query_rows, attend_key_section, positions)
        value_tensor = attend_value_section.reshape(token_count, KEY_VALUE_HEADS, HEAD_SIZE)
        weights_full = jnp.where(visible, jnp.exp(scores - log_sum_rows[..., None]), 0.0)
        grad_probs = jnp.einsum(
            "tkgd,nkd->kgtn", head_gradient, value_tensor, preferred_element_type=jnp.float32
        )
        grad_scores = (weights_full * (grad_probs - delta_rows[..., None])).astype(jnp.bfloat16)
        grad_query = attn_scale * jnp.einsum(
            "kgtn,nkd->tkgd", grad_scores, key_tensor, preferred_element_type=jnp.float32
        )
        key_portion = attn_scale * jnp.einsum(
            "kgtn,tkgd->nkd", grad_scores, query_rows, preferred_element_type=jnp.float32
        )
        value_portion = jnp.einsum(
            "kgtn,tkgd->nkd",
            weights_full.astype(jnp.bfloat16),
            head_gradient,
            preferred_element_type=jnp.float32,
        )
        update = jnp.concatenate(
            [
                key_portion.reshape(token_count, KEY_VALUE_HEADS * HEAD_SIZE),
                value_portion.reshape(token_count, KEY_VALUE_HEADS * HEAD_SIZE),
            ],
            axis=1,
        )
        return (grad_query, update)

    grad_query, grad_keys_full = lax.cond(
        jnp.int32(0) <= positions[-1], compute, lambda current: current, init_back
    )
    local_gradients = lax.psum_scatter(
        grad_keys_full.astype(jnp.bfloat16), CTX, scatter_dimension=0, tiled=True
    ).astype(jnp.float32)
    query_back = (
        rotate_pairs(
            grad_query.reshape(token_rows, QUERY_HEADS, HEAD_SIZE), cosine_table, -sine_table
        )
        .astype(jnp.bfloat16)
        .reshape(token_rows, QUERY_HEADS * HEAD_SIZE)
    )
    key_backward_rows = (
        rotate_pairs(
            local_gradients[:, : KEY_VALUE_HEADS * HEAD_SIZE].reshape(
                token_rows, KEY_VALUE_HEADS, HEAD_SIZE
            ),
            cosine_table,
            -sine_table,
        )
        .astype(jnp.bfloat16)
        .reshape(token_rows, KEY_VALUE_HEADS * HEAD_SIZE)
    )
    value_backward_rows = local_gradients[:, KEY_VALUE_HEADS * HEAD_SIZE :].astype(jnp.bfloat16)
    grad_wq_part = lax.dot_general(
        attention_input, query_back, contract_rows, preferred_element_type=jnp.float32
    )
    grad_wk_part = lax.dot_general(
        attention_input, key_backward_rows, contract_rows, preferred_element_type=jnp.float32
    )
    grad_wv_part = lax.dot_general(
        attention_input, value_backward_rows, contract_rows, preferred_element_type=jnp.float32
    )
    grad_attn_in = lax.dot_general(
        query_back, query_w, contract_cols, preferred_element_type=jnp.float32
    )
    grad_attn_in = grad_attn_in + lax.dot_general(
        key_backward_rows, key_weight_matrix, contract_cols, preferred_element_type=jnp.float32
    )
    grad_attn_in = grad_attn_in + lax.dot_general(
        value_backward_rows, value_w, contract_cols, preferred_element_type=jnp.float32
    )
    back_one, grad_attn_gain = rms_backward(grad_attn_in, attn_unit, inverse_one, attn_gain)
    grad_input = grad_mixed + back_one
    partial_sums = (
        lax.psum_scatter(
            grad_attn_gain.astype(jnp.bfloat16), CTX, scatter_dimension=0, tiled=True
        ).astype(jnp.float32),
        lax.psum_scatter(
            grad_ffn_gain.astype(jnp.bfloat16), CTX, scatter_dimension=0, tiled=True
        ).astype(jnp.float32),
        lax.psum_scatter(
            grad_wq_part.astype(jnp.bfloat16), CTX, scatter_dimension=0, tiled=True
        ).astype(jnp.float32),
        lax.psum_scatter(
            grad_wk_part.astype(jnp.bfloat16), CTX, scatter_dimension=0, tiled=True
        ).astype(jnp.float32),
        lax.psum_scatter(
            grad_wv_part.astype(jnp.bfloat16), CTX, scatter_dimension=0, tiled=True
        ).astype(jnp.float32),
        lax.psum_scatter(
            grad_wo_part.astype(jnp.bfloat16), CTX, scatter_dimension=0, tiled=True
        ).astype(jnp.float32),
        lax.psum_scatter(
            grad_router_part.astype(jnp.bfloat16), CTX, scatter_dimension=0, tiled=True
        ).astype(jnp.float32),
    )
    summed = (
        lax.psum_scatter(
            partial_sums[0].astype(jnp.bfloat16), FSDP, scatter_dimension=0, tiled=True
        ).astype(jnp.float32),
        lax.psum_scatter(
            partial_sums[1].astype(jnp.bfloat16), FSDP, scatter_dimension=0, tiled=True
        ).astype(jnp.float32),
        lax.psum_scatter(
            partial_sums[2].astype(jnp.bfloat16), FSDP, scatter_dimension=0, tiled=True
        ).astype(jnp.float32),
        lax.psum_scatter(
            partial_sums[3].astype(jnp.bfloat16), FSDP, scatter_dimension=0, tiled=True
        ).astype(jnp.float32),
        lax.psum_scatter(
            partial_sums[4].astype(jnp.bfloat16), FSDP, scatter_dimension=0, tiled=True
        ).astype(jnp.float32),
        lax.psum_scatter(
            partial_sums[5].astype(jnp.bfloat16), FSDP, scatter_dimension=0, tiled=True
        ).astype(jnp.float32),
        lax.psum_scatter(
            partial_sums[6].astype(jnp.bfloat16), FSDP, scatter_dimension=0, tiled=True
        ).astype(jnp.float32),
    )
    return (
        layer_out[None],
        grad_input[None],
        summed[0],
        summed[1],
        summed[2],
        summed[3],
        summed[4],
        summed[5],
        summed[6],
        grad_expert_in,
        grad_expert_out,
    )


def swap(a, flip):
    return lax.ppermute(a, FSDP, [(i, i ^ flip) for i in range(NX * NC)])


def fast_body(
    hidden,
    routes,
    attn_norm,
    ffn_norm,
    w_q,
    key_weight,
    value_weight,
    w_o,
    router,
    expert_in,
    expert_out,
    cotangent,
):
    tokens = hidden.shape[1]
    ctx = lax.axis_index(CTX)
    fsdp = lax.axis_index(FSDP)
    core = fsdp % NC
    rows = w_q.shape[0]
    quarter = expert_in.shape[1]
    kv_width = KEY_VALUE_HEADS * HEAD_SIZE
    q_width = QUERY_HEADS * HEAD_SIZE
    held = expert_in.shape[0] // NC
    bf = jnp.bfloat16
    f32 = jnp.float32
    positions = ctx * tokens + jnp.arange(tokens, dtype=jnp.int32)
    cosine_table, sine_table = (table[:, 0] for table in rope_tables(positions))
    cosine = jnp.concatenate([cosine_table] * 4, axis=1)
    sine = jnp.concatenate([-sine_table, sine_table] * 2, axis=1)
    contract_cols = (((1,), (1,)), ((), ()))
    wide = hidden[0].astype(f32)
    cot = cotangent[0]

    route = routes[0]
    indicator = (route[:, :, None] == jnp.arange(EXPERT_COUNT, dtype=jnp.int32)).astype(f32)
    part = rows // 3
    whole = (Z, Y, X, C)
    one, two, mine, *others = gather_weights(
        [w_q, key_weight, value_weight, w_o, router, attn_norm[None], ffn_norm[None]],
        [expert_in, expert_out],
        [
            Plan(0, (X, Z, Y, C), whole, rows=(2 * part, part)),
            Plan(1, (X, Z, Y, C), whole, rows=(part, part)),
            Plan(1, (X, Y, Z, C), whole, rows=(2 * part, part)),
            Plan(0, (Z, Y, X, C), whole, rows=(0, 2 * part)),
            Plan(1, (Z, Y, X, C), whole, rows=(0, part)),
        ],
        0,
    )
    parts = [mine, swap(mine, 2)] + [swap(other, 1) for other in others] + [swap(others[0], 3)]
    one = one.reshape(MODEL_WIDTH, -1)
    two = two.reshape(MODEL_WIDTH, -1)
    output_w = two[:, :MODEL_WIDTH]
    small = two[:, MODEL_WIDTH:]
    router_w = small[:, :EXPERT_COUNT]
    gains = lax.dot_general(
        jnp.eye(128, dtype=bf), small, contract_cols, preferred_element_type=f32
    )
    attn_gain, ffn_gain = gains[EXPERT_COUNT], gains[EXPERT_COUNT + 1]

    _, _, attention_input = rms_forward(wide, attn_gain)
    linear = jnp.dot(attention_input, one, preferred_element_type=f32)
    attention_output, log_sums, kv, cots, queries = attend(linear, cot, route, cosine, sine, 1)
    mixed = wide + jnp.dot(attention_output, output_w, preferred_element_type=f32)
    _, _, ffn_in = rms_forward(mixed, ffn_gain)
    logits = jnp.dot(ffn_in, router_w, preferred_element_type=f32)
    chosen = jnp.sum(indicator * logits[:, None, :], axis=-1)
    gates = jax.nn.softmax(chosen, axis=-1)
    gate_map = jnp.sum(indicator * gates[..., None], axis=1)
    payload = jnp.concatenate(
        [ffn_in, gate_map.astype(bf), jnp.zeros((tokens, 128 - EXPERT_COUNT), bf)], axis=1
    )
    gin, moe_part, *pieces = moe(payload, cots, parts + others[-1:], CAP, 2)
    across = [swap(pieces[j], j) for j in range(1, NX * NC)]
    gate_wide = jnp.concatenate([gate_map, jnp.zeros((tokens, 128 - EXPERT_COUNT), f32)], axis=1)
    back, layer_out, grad_mixed, grad_attn, left_small, right_small = attend_back(
        queries,
        gin,
        gate_wide,
        cot,
        ffn_gain.astype(f32)[None],
        attention_output,
        log_sums,
        kv,
        moe_part,
        two,
        mixed,
        cosine,
        sine,
        4,
    )
    *sums, grad_input = return_weights(
        [attention_input, attention_output, left_small],
        [back, grad_attn, right_small],
        one,
        hidden[0],
        attn_gain.astype(f32)[None],
        grad_mixed,
        EXPERT_COUNT,
        5,
    )
    grad_expert_in, grad_expert_out, *rest, first_gain, second_gain, layer_out, grad_input = last_outputs(
        [pieces[0]] + across,
        core,
        2 * EXPERT_HIDDEN,
        sums + [layer_out, grad_input],
        (q_width, kv_width, kv_width, MODEL_WIDTH, EXPERT_COUNT),
    )
    return (
        layer_out[None],
        grad_input[None],
        first_gain.reshape(rows),
        second_gain.reshape(rows),
        *rest,
        grad_expert_in.reshape(NC * held, quarter, -1),
        grad_expert_out.reshape(NC * held, quarter, -1),
    )


def fast(*args):
    return fast_body(*args)


def solution(mesh):
    placed = (
        P(FSDP, CTX, None),
        P(FSDP, CTX, None),
        P((CTX, FSDP)),
        P((CTX, FSDP)),
        P((CTX, FSDP), None),
        P((CTX, FSDP), None),
        P((CTX, FSDP), None),
        P((CTX, FSDP), None),
        P((CTX, FSDP), None),
        P(CTX, FSDP, None),
        P(CTX, FSDP, None),
        P(FSDP, CTX, None),
    )
    small = mesh.shape[CTX] == NZ * NY and mesh.shape[FSDP] == NX * NC
    return jax.shard_map(
        fast if small else local,
        mesh=mesh,
        in_specs=placed,
        out_specs=(
            P(FSDP, CTX, None),
            P(FSDP, CTX, None),
            P((CTX, FSDP)),
            P((CTX, FSDP)),
            P((CTX, FSDP), None),
            P((CTX, FSDP), None),
            P((CTX, FSDP), None),
            P((CTX, FSDP), None),
            P((CTX, FSDP), None),
            P(CTX, FSDP, None),
            P(CTX, FSDP, None),
        ),
        check_vma=False,
    )
```

```python
import functools
import itertools

import jax
import jax.numpy as jnp
from jax import lax
from jax.experimental import pallas as pl
from jax.experimental.pallas import tpu as pltpu
from jax.sharding import PartitionSpec as P


NY = 2
NZ = 4
NX = 2
NC = 2
DEV = pl.DeviceIdType.MESH
CTX, FSDP = "ctx", "fsdp"
Z, Y, X, C = 0, 1, 2, 3
SIZES = {Z: NZ, Y: NY, X: NX, C: NC}
UP, DOWN = 4, 5


class Plan:
    def __init__(self, ref, order, index, rows=None, view=None):
        self.ref, self.order, self.index, self.rows, self.view = ref, order, index, rows, view
        self.blocks = 1
        for d in index:
            self.blocks *= SIZES[d]


class Place:
    def __init__(self):
        ctx = lax.axis_index(CTX)
        fsdp = lax.axis_index(FSDP)
        self.at = {Z: ctx // NY, Y: ctx % NY, X: fsdp // NC, C: fsdp % NC}
        z = self.at[Z]
        low = z < NZ // 2
        base = jnp.where(low, z, NZ - 1 - z)
        near = [base, 1 - base, jnp.int32(2), jnp.int32(3)]
        self.order = [z] + [jnp.where(low, k, NZ - 1 - k) for k in near[1:]]

    def device(self, dim, value):
        spot = dict(self.at)
        spot[dim] = value
        return (spot[Z] * NY + spot[Y], spot[X] * NC + spot[C])

    def across(self, dim):
        return self.device(dim, 1 - self.at[dim])

    def along(self, step):
        return self.device(Z, self.at[Z] + step)

    def coords(self, z_from, flips):
        spot = {d: (1 - self.at[d] if d in flips else self.at[d]) for d in (Y, X, C)}
        spot[Z] = z_from
        return spot


def flat_index(spot, dims):
    index = 0
    for d in dims:
        index = index * SIZES[d] + spot[d]
    return index


def subsets(dims):
    return [c for n in range(len(dims) + 1) for c in itertools.combinations(dims, n)]


def hail(place, dims, more=()):
    barrier = pltpu.get_barrier_semaphore()
    z = place.at[Z]
    count = jnp.int32(0)
    for d in dims:
        if d == Z:
            @pl.when(z > 0)
            def _():
                pl.semaphore_signal(barrier, inc=1, device_id=place.along(-1), device_id_type=DEV)

            @pl.when(z < NZ - 1)
            def _():
                pl.semaphore_signal(barrier, inc=1, device_id=place.along(1), device_id_type=DEV)

            count = count + jnp.where(z > 0, 1, 0) + jnp.where(z < NZ - 1, 1, 0)
        else:
            pl.semaphore_signal(barrier, inc=1, device_id=place.across(d), device_id_type=DEV)
            count = count + 1
    for device in more:
        pl.semaphore_signal(barrier, inc=1, device_id=device, device_id_type=DEV)
        count = count + 1
    return count


def meet(count):
    pl.semaphore_wait(pltpu.get_barrier_semaphore(), count)


def gather_events(order):
    pairs = [d for d in order if d != Z]
    events = [(k, f) for k in range(NZ) for f in subsets(pairs)]
    return sorted(events, key=lambda e: (e[0] + len(e[1]), len(e[1])))


def gather_sends(order, k, flips):
    z_at = order.index(Z)
    last = max([order.index(d) for d in flips] + ([z_at] if k > 0 else []) + [-1])
    out = []
    for position, d in enumerate(order):
        if position > last:
            out.extend([UP, DOWN] if d == Z else [d])
    if k > 0 and last == z_at:
        out.extend([UP, DOWN])
    return out


def gather_kernel(plans, *refs):
    w_q, w_k, w_v, w_o, router, first_gain, second_gain, first_w, second_w = refs[:9]
    outs, (mine, *others) = refs[9:11], refs[11:14]
    send_sem, recv_sem, own_sem, stage, load_sem, store_sem, pack_one, pack_two = refs[14:]
    ins = pack_one, pack_two
    place = Place()
    count_here = hail(place, (Z, Y, X, C))
    held = mine.shape[0]
    split = first_w.shape[2]
    loads = []
    for side in range(2):
        base = (place.at[C] if side == 0 else 1 - place.at[C]) * held
        for e in range(held):
            to = stage.at[side * held + e]
            for w, at in ((first_w, pl.ds(0, split)), (second_w, pl.ds(split, second_w.shape[2]))):
                loads.append(pltpu.make_async_copy(w.at[base + e], to.at[:, at], load_sem.at[len(loads)]))
    for copy in loads:
        copy.start()
    stores = [pltpu.make_async_copy(stage.at[pl.ds(0, held)], mine, store_sem.at[0])] + [
        pltpu.make_async_copy(stage.at[pl.ds(held + e, 1)], out, store_sem.at[1 + e]) for e, out in enumerate(others)
    ]
    at = 0
    for w in (w_q, w_k, w_v):
        pack_one[:, at : at + w.shape[1]] = w[...]
        at += w.shape[1]
    model = w_o.shape[1]
    rows = w_o.shape[0]
    pack_two[:, :model] = w_o[...]
    same = lax.broadcasted_iota(jnp.int32, (rows, rows), 0) == lax.broadcasted_iota(jnp.int32, (rows, rows), 1)
    upright = lambda gain: jnp.sum(jnp.where(same, gain[...].astype(jnp.float32), 0.0), axis=1, keepdims=True)
    lane = lax.broadcasted_iota(jnp.int32, (1, 128), 1)
    count = router.shape[0]
    small = jnp.where(lane == count, upright(first_gain), jnp.where(lane == count + 1, upright(second_gain), 0.0))
    pack_two[:, model:] = small.astype(pack_two.dtype)
    pack_two[:, model : model + count] = lax.dot_general(
        same.astype(jnp.float32).astype(router.dtype), router[...], (((1,), (1,)), ((), ())),
        preferred_element_type=jnp.float32,
    ).astype(pack_two.dtype)
    z = place.at[Z]
    meet(count_here)
    pending = []
    slot = 0
    queue = []
    for n, plan in enumerate(plans):
        for rank, event in enumerate(gather_events(plan.order)):
            queue.append((rank / len(gather_events(plan.order)), n, event))
    queue.sort(key=lambda q: (q[0], q[1]))
    bases = [sum(p.blocks for p in plans[:n]) for n in range(len(plans))]
    for turn_at, (_, n, (k, flips)) in enumerate(queue):
        if turn_at == len(queue) // 3:
            for copy in loads:
                copy.wait()
            for copy in stores:
                copy.start()
        plan = plans[n]
        src = ins[plan.ref]
        out = outs[plan.ref]
        rows = plan.rows
        z_from = place.order[k]
        spot = place.coords(z_from, flips)
        index = flat_index(spot, plan.index)
        own = k == 0 and not flips
        if plan.view is not None:
            target = plan.view(out, spot, rows)
            source = src.at[:, pl.ds(rows[0], rows[1])] if own else target
        else:
            target = out.at[index] if rows is None else out.at[index, pl.ds(rows[0], rows[1])]
            source = (src if rows is None else src.at[pl.ds(rows[0], rows[1])]) if own else target
        sem = recv_sem.at[bases[n] + index]
        if not own:
            pltpu.make_async_remote_copy(
                src_ref=target, dst_ref=target, send_sem=own_sem.at[0], recv_sem=sem,
                device_id=place.across(C), device_id_type=DEV,
            ).wait_recv()
        for way in gather_sends(plan.order, k, flips):
            if way in (UP, DOWN):
                step = 1 if way == UP else -1
                go = z < NZ - 1 if way == UP else z > 0
                if k > 0:
                    go = jnp.logical_and(go, z_from < z if way == UP else z_from > z)
                dest = place.device(Z, jnp.clip(z + step, 0, NZ - 1))
            else:
                go, dest = None, place.across(way)
            copy = pltpu.make_async_remote_copy(
                src_ref=source, dst_ref=target, send_sem=send_sem.at[slot], recv_sem=sem,
                device_id=dest, device_id_type=DEV,
            )
            slot += 1
            if go is None:
                copy.start()
            else:
                pl.when(go)(copy.start)
            pending.append((go, copy.wait_send))
        if own:
            copy = pltpu.make_async_copy(source, target, own_sem.at[1 + n])
            copy.start()
            pending.append((None, copy.wait))
    for copy in stores:
        copy.wait()
    for go, wait in pending:
        if go is None:
            wait()
        else:
            pl.when(go)(wait)


def gather_weights(weights, experts, plans, collective_id):
    sends = sum(len(gather_sends(p.order, k, f)) for p in plans for k, f in gather_events(p.order))
    rows = weights[0].shape[0]
    bf = weights[0].dtype
    widths = [sum(w.shape[1] for w in weights[:3]), weights[3].shape[1] + 128]
    held = experts[0].shape[0] // NC
    pack = (experts[0].shape[1], experts[0].shape[2] + experts[1].shape[2])
    apart = pl.BlockSpec(memory_space=pl.ANY)
    dma = pltpu.SemaphoreType.DMA
    return pl.pallas_call(
        functools.partial(gather_kernel, plans),
        out_shape=[jax.ShapeDtypeStruct((plans[0].blocks, rows, w), bf) for w in widths]
        + [jax.ShapeDtypeStruct((n,) + pack, bf) for n in [held] + [1] * held],
        in_specs=[pl.BlockSpec(memory_space=pltpu.VMEM)] * len(weights) + [apart] * 2,
        out_specs=[apart] * (3 + held),
        scratch_shapes=[
            dma((sends,)),
            dma((sum(p.blocks for p in plans),)),
            dma((1 + len(plans),)),
            pltpu.VMEM((NC * held,) + pack, bf),
            dma((2 * NC * held,)),
            dma((1 + held,)),
        ]
        + [pltpu.VMEM((rows, w), bf) for w in widths],
        compiler_params=pltpu.CompilerParams(collective_id=collective_id, has_side_effects=True),
        name="gather_weights",
    )(*weights, *experts)


def add_into(acc, other):
    acc[...] = (acc[...].astype(jnp.float32) + other[...].astype(jnp.float32)).astype(acc.dtype)


class Gather:
    def __init__(self, place, plan, src, out, send_sem, recv_sem, spare_sem, slot, base):
        self.place, self.plan, self.src, self.out = place, plan, src, out
        self.send_sem, self.recv_sem, self.spare_sem = send_sem, recv_sem, spare_sem
        self.slot, self.base = slot, base
        self.pending = []

    @staticmethod
    def sends(plan):
        return sum(len(gather_sends(plan.order, k, f)) for k, f in gather_events(plan.order))

    def goes(self, way, k):
        z, z_from = self.place.at[Z], self.place.order[k]
        if way == UP:
            return z < NZ - 1 if k == 0 else jnp.logical_and(z < NZ - 1, z_from < z)
        return z > 0 if k == 0 else jnp.logical_and(z > 0, z_from > z)

    def part(self, ref):
        rows = self.plan.rows
        return ref if rows is None else ref.at[pl.ds(rows[0], rows[1])]

    def step(self, k, flips):
        place, plan = self.place, self.plan
        index = flat_index(place.coords(place.order[k], flips), plan.index)
        target = self.part(self.out.at[index])
        sem = self.recv_sem.at[self.base + index]
        source = target
        if k == 0 and not flips:
            source = self.part(self.src)
        else:
            pltpu.make_async_remote_copy(
                src_ref=target, dst_ref=target, send_sem=self.spare_sem, recv_sem=sem,
                device_id=place.across(C), device_id_type=DEV,
            ).wait_recv()
        for way in gather_sends(plan.order, k, flips):
            if way in (UP, DOWN):
                dest = place.device(Z, jnp.clip(place.at[Z] + (1 if way == UP else -1), 0, NZ - 1))
            else:
                dest = place.across(way)
            copy = pltpu.make_async_remote_copy(
                src_ref=source, dst_ref=target, send_sem=self.send_sem.at[self.slot], recv_sem=sem,
                device_id=dest, device_id_type=DEV,
            )
            if way in (UP, DOWN):
                pl.when(self.goes(way, k))(copy.start)
            else:
                copy.start()
            self.pending.append((way, k, self.slot))
            self.slot += 1

    def finish(self):
        for way, k, slot in self.pending:
            block = self.part(self.src)
            copy = pltpu.make_async_remote_copy(
                src_ref=block, dst_ref=block, send_sem=self.send_sem.at[slot], recv_sem=self.spare_sem,
                device_id=self.place.across(C), device_id_type=DEV,
            )
            if way in (UP, DOWN):
                pl.when(self.goes(way, k))(copy.wait_send)
            else:
                copy.wait_send()


class Reduce:
    def __init__(self, place, plan, held, levels, chain, send_sem, recv_sem, spare_sem):
        self.place, self.plan, self.held, self.levels, self.chain = place, plan, held, levels, chain
        self.send_sem, self.recv_sem, self.spare_sem = send_sem, recv_sem, spare_sem
        self.order, self.chain_at, self.kept, counts = Reduce.shape(plan)
        self.base = [sum(counts[:p]) for p in range(len(counts))]
        self.slot = 0

    @staticmethod
    def shape(plan):
        order = plan.order if Z in plan.order else plan.order + (Z,)
        at = order.index(Z)
        kept = [subsets(tuple(d for d in order[p + 1 :] if d != Z)) for p in range(len(order))]
        times = [NZ if p < at else NZ + 1 if p == at else 1 for p in range(len(order))]
        return order, at, kept, [n * len(f) for n, f in zip(times, kept)]

    @staticmethod
    def counts(plan):
        _, at, kept, counts = Reduce.shape(plan)
        buffers = counts[:at] + counts[at + 1 :] + [counts[at]]
        return buffers, sum(counts) - 2 * len(kept[at]), sum(counts)

    def level_of(self, p):
        return self.levels[p if p < self.chain_at else p - 1]

    def push(self, source, target, sem, dest):
        copy = pltpu.make_async_remote_copy(
            src_ref=source, dst_ref=target, send_sem=self.send_sem.at[self.slot], recv_sem=sem,
            device_id=dest, device_id_type=DEV,
        )
        self.slot += 1
        copy.start()

    def arrived(self, target, sem):
        pltpu.make_async_remote_copy(
            src_ref=target, dst_ref=target, send_sem=self.spare_sem, recv_sem=sem,
            device_id=self.place.across(C), device_id_type=DEV,
        ).wait_recv()

    def block(self, k, flips):
        return self.held.at[flat_index(self.place.coords(self.place.order[k], flips), self.plan.index)]

    def spot(self, p, k, flips):
        at = self.kept[p].index(flips)
        return at if p > self.chain_at else self.place.order[k] * len(self.kept[p]) + at

    def send(self, p, k, flips):
        dim = self.order[p]
        spot = self.spot(p, k, tuple(d for d in flips if d != dim))
        self.push(
            self.block(k, flips), self.level_of(p).at[spot],
            self.recv_sem.at[self.base[p] + spot], self.place.across(dim),
        )

    def first(self, k):
        for f in self.kept[0]:
            self.send(0, k, (self.order[0],) + f)

    def forward(self, p, k, flips):
        later = p + 1
        if later < len(self.order) and self.order[later] in flips:
            self.send(later, k, flips)

    def level(self, p, k):
        for f in sorted(self.kept[p], key=lambda f: -len(f)):
            spot = self.spot(p, k, f)
            self.arrived(self.level_of(p).at[spot], self.recv_sem.at[self.base[p] + spot])
            add_into(self.block(k, f), self.level_of(p).at[spot])
            self.forward(p, k, f)

    def link(self, spot, n):
        at = spot * len(self.kept[self.chain_at]) + n
        return self.chain.at[at], self.recv_sem.at[self.base[self.chain_at] + at]

    def along(self, k):
        z = self.place.at[Z]
        dest = self.place.order[k]
        up = dest > z
        for n, f in enumerate(self.kept[self.chain_at]):
            mine = self.block(k, f)
            target, sem = self.link(dest + jnp.where(up, 1, 0), n)

            @pl.when(jnp.where(up, z > 0, z < NZ - 1))
            def _():
                self.arrived(target, sem)
                add_into(mine, target)

            self.push(mine, target, sem, self.place.along(jnp.where(up, 1, -1)))

    def settle(self):
        z = self.place.at[Z]
        kept = self.kept[self.chain_at]
        for f in sorted(kept, key=lambda f: -len(f)):
            mine = self.block(0, f)
            for go, spot in ((z > 0, z + 1), (z < NZ - 1, z)):
                target, sem = self.link(spot, kept.index(f))

                @pl.when(go)
                def _():
                    self.arrived(target, sem)
                    add_into(mine, target)

            self.forward(self.chain_at, 0, f)

    def last(self, out, base=None):
        if self.chain_at == len(self.order) - 1:
            self.settle()
        total = self.block(0, ())[...].astype(jnp.float32)
        if base is not None:
            total = base[...] + total
        out[...] = total.astype(out.dtype)

    def at_time(self, t):
        far = list(reversed(range(NZ)))
        at = self.chain_at
        out = [functools.partial(self.level, p, far[t - p]) for p in range(at) if 0 <= t - p < NZ]
        if 0 <= t - at < NZ - 1:
            out.append(functools.partial(self.along, far[t - at]))
        if t - at == NZ - 1 and at < len(self.order) - 1:
            out.append(self.settle)
        out += [functools.partial(self.level, p, 0) for p in range(at + 1, len(self.order)) if t == NZ - 1 + p]
        return out

    def steps(self):
        return [step for t in range(NZ + len(self.order)) for step in self.at_time(t)]

    def finish(self):
        block = self.level_of(0).at[0]
        for slot in range(self.slot):
            pltpu.make_async_remote_copy(
                src_ref=block, dst_ref=block, send_sem=self.send_sem.at[slot], recv_sem=self.spare_sem,
                device_id=self.place.across(C), device_id_type=DEV,
            ).wait_send()


def tile_up(n, m):
    return (n + m - 1) // m * m


def columns_of(width, chunk=512):
    return [(i, min(chunk, width - i)) for i in range(0, width, chunk)]


def moe_kernel(plans, back, width, hidden, cap, *refs):
    payload, cots, w_own, w_x, w_core, w_core_last, w_both, w_send = refs[:8]
    gin_out, part_out = refs[8:10]
    grads = refs[10:14]
    (
        seen, cot_seen, weights, taken, cot_taken, rows_buf, scaled, grad_act, pick, stage,
        lvl_b0, lvl_b1, chain_b, lvl_c0, lvl_c1, chain_c,
        send_sem, recv_sem, spare_sem, send_b, recv_b, send_c, recv_c, load_sem, store_sem, part_sem, piece_sem,
    ) = refs[14:]
    bf, f32 = jnp.bfloat16, jnp.float32
    place = Place()
    count = payload.shape[0]
    pair = 2 * cap
    wide = width + 128
    quarter = width // (NX * NC)
    half = NZ * pair
    lanes = pick.shape[2]
    held = weights.shape[0]
    fsdp = place.at[X] * NC + place.at[C]
    first = (((place.at[Z] * NY + place.at[Y]) * NC) + place.at[C]) * held

    there = (place.at[Z] * NY + place.at[Y], (1 - place.at[X]) * NC + 1 - place.at[C])
    count_here = hail(place, (Z, Y, C), (there,))
    loads = []
    rows_of = lambda owner: pl.ds(pl.multiple_of(owner * quarter, quarter), quarter)
    sources = [(w_own, e, e, 0) for e in range(held)] + [(w_x, e, e, 2) for e in range(held)]
    sources += [(w_core, 0, 0, 1), (w_core_last, 0, held - 1, 1), (w_both, 0, 0, 3)]
    for ref, at, e, j in sources:
        loads.append(pltpu.make_async_copy(ref.at[at], weights.at[e, rows_of(fsdp ^ j)], load_sem.at[len(loads)]))
    piece = pltpu.make_async_remote_copy(
        src_ref=w_send.at[0], dst_ref=weights.at[held - 1, rows_of(fsdp)],
        send_sem=piece_sem.at[0], recv_sem=piece_sem.at[1], device_id=there, device_id_type=DEV,
    )
    base_of = lambda h, k: (jnp.where(h == 0, place.at[C], 1 - place.at[C]) * NZ + place.order[k]) * NY
    cot_loads = {}
    for k in range(NZ):
        for h in range(2):
            at = pl.ds(base_of(h, k), NY)
            cot_loads[(h, k)] = pltpu.make_async_copy(cots.at[at], cot_seen.at[at], load_sem.at[len(loads) + len(cot_loads)])

    meet(count_here)
    piece.start()
    ways = []
    send_at = 0
    for n, plan in enumerate(plans):
        ways.append(Gather(place, plan, payload, seen, send_sem, recv_sem, spare_sem, send_at, n * plan.blocks))
        send_at += Gather.sends(plan)
    for way in ways:
        way.step(0, ())
    for key in cot_loads:
        cot_loads[key].start()
    for copy in loads:
        copy.start()
    seen[flat_index(place.at, plans[0].index)] = payload[...]

    row_id = lax.broadcasted_iota(jnp.int32, (NY * count, NY * count), 0)
    col_id = lax.broadcasted_iota(jnp.int32, (NY * count, NY * count), 1)
    earlier = jnp.logical_and(col_id < row_id, col_id // count == row_id // count).astype(bf)
    lane_id = lax.broadcasted_iota(jnp.int32, (1, 128), 1)
    here = [(lane_id == first + e).astype(f32) for e in range(held)]
    pick_lane = lax.broadcasted_iota(jnp.int32, (NY * count, lanes), 1).astype(f32)
    y_shift = (lax.broadcasted_iota(jnp.int32, (NY * count, 1), 0) // count * cap).astype(f32)

    row_of = lambda h, k: (k * NC + h) * pair

    def dispatch(source, target, h, k, cols):
        at = pl.ds(base_of(h, k), NY)
        r = row_of(h, k)
        for c0, cn in cols:
            block = source[at, :, c0 : c0 + cn].reshape(NY * count, cn)
            got = lax.dot_general(
                pick[h * NZ + k], block, (((0,), (0,)), ((), ())), preferred_element_type=f32
            ).astype(bf)
            for e in range(held):
                target[e, r : r + pair, c0 : c0 + cn] = got[e * pair : (e + 1) * pair]

    def cot_chunk(h, k):
        cot_loads[(h, k)].wait()
        at = pl.ds(base_of(h, k), NY)
        chosen = cot_seen[at, :, width:wide].reshape(NY * count, 128)
        before = jnp.dot(earlier, chosen, preferred_element_type=f32)
        picked = None
        for e in range(held):
            is_here = jnp.sum(chosen.astype(f32) * here[e], axis=1, keepdims=True)
            slot = jnp.sum(before * here[e], axis=1, keepdims=True) + y_shift + e * pair
            target = jnp.where(is_here > 0.5, slot, -1.0)
            hit = pick_lane == target
            picked = hit if picked is None else jnp.logical_or(picked, hit)
        pick[h * NZ + k] = picked.astype(f32).astype(bf)
        dispatch(cot_seen, cot_taken, h, k, columns_of(width))

    def hidden_chunk(h, e, n, tile):
        rows = pl.ds(h * half, half)
        tokens_in = taken[e, rows, :width]
        gate = jnp.sum(taken[e, rows, width:wide].astype(f32) * here[e], axis=1, keepdims=True)
        col = n * tile
        g = jnp.dot(tokens_in, weights[e, :, col : col + tile], preferred_element_type=f32)
        u = jnp.dot(tokens_in, weights[e, :, hidden + col : hidden + col + tile], preferred_element_type=f32)
        raw = jnp.dot(
            cot_taken[e, rows, :], weights[e, :, 2 * hidden + col : 2 * hidden + col + tile], preferred_element_type=f32
        )
        s = jax.nn.sigmoid(g)
        gs = g * s
        inner = gs * u
        scaled[e, rows, col : col + tile] = (inner * gate).astype(bf)
        grad_inner = raw * gate
        grad_act[e, rows, col : col + tile] = (grad_inner * u * s * (1.0 + g * (1.0 - s))).astype(bf)
        grad_act[e, rows, hidden + col : hidden + col + tile] = (grad_inner * gs).astype(bf)
        return jnp.sum(raw * inner, axis=1, keepdims=True)

    tile = min(256, hidden)
    found = {}

    def hidden_step(h, e, n):
        got = hidden_chunk(h, e, n, tile)
        found[(h, e)] = got if n == 0 else found[(h, e)] + got
        if n == hidden // tile - 1:
            gate_grad = found.pop((h, e))
            high = gate_grad.astype(bf).astype(f32)
            there = pl.ds(h * half, half)
            apart = (lane_id == EXPERT_COUNT + first + e).astype(f32)
            rows_buf[e, there, width:wide] = (high * here[e] + (gate_grad - high) * apart).astype(bf)

    def hidden_steps(h):
        return [functools.partial(hidden_step, h, e, n) for e in range(held) for n in range(hidden // tile)]

    def project(h, e, left, weight_cols):
        rows = pl.ds(h * half, half)
        lo, n = weight_cols
        for c0, cn in columns_of(width):
            rows_buf[e, rows, c0 : c0 + cn] = lax.dot_general(
                left[e, rows, :], weights[e, c0 : c0 + cn, lo : lo + n], (((1,), (1,)), ((), ())), preferred_element_type=f32
            ).astype(bf)

    def combine(target, h, k, cols):
        at = pl.ds(base_of(h, k), NY)
        r = row_of(h, k)
        for c0, cn in cols:
            parts = [rows_buf[e, r : r + pair, c0 : c0 + cn] for e in range(held)]
            if lanes > held * pair:
                parts.append(jnp.zeros((lanes - held * pair, cn), bf))
            got = jnp.dot(pick[h * NZ + k], jnp.concatenate(parts, axis=0), preferred_element_type=f32)
            target[at, :, c0 : c0 + cn] = got.astype(bf).reshape(NY, count, cn)

    stores = []

    def weight_grad(e, j):
        rows = pl.ds(pl.multiple_of((fsdp ^ j) * quarter, 128), quarter)
        slot = len(stores) % 2
        if len(stores) >= 2:
            stores[-2].wait()
        for c0, cn in columns_of(2 * hidden):
            stage[slot, :, c0 : c0 + cn] = lax.dot_general(
                taken[e, :, rows], grad_act[e, :, c0 : c0 + cn], (((0,), (0,)), ((), ())), preferred_element_type=f32
            ).astype(bf)
        stage[slot, :, 2 * hidden :] = lax.dot_general(
            cot_taken[e, :, rows], scaled[e], (((0,), (0,)), ((), ())), preferred_element_type=f32
        ).astype(bf)
        copy = pltpu.make_async_copy(stage.at[slot], grads[j].at[e], store_sem.at[len(stores)])
        copy.start()
        stores.append(copy)

    work = [functools.partial(cot_chunk, h, k) for h in range(NC) for k in range(NZ)]
    all_cols = columns_of(width) + [(width, 128)]
    ready = {(h, k): 0 for h in range(NC) for k in range(NZ)}
    ready[(0, 0)] = 1
    near_begun = False

    def wait_weights():
        for copy in loads:
            copy.wait()
        arrived = weights.at[held - 1, rows_of(fsdp ^ 3)]
        pltpu.make_async_remote_copy(
            src_ref=arrived, dst_ref=arrived, send_sem=piece_sem.at[0], recv_sem=piece_sem.at[1],
            device_id=there, device_id_type=DEV,
        ).wait_recv()

    for k, flips in gather_events(plans[0].order)[1:]:
        for way in ways:
            way.step(k, flips)
        key = (1 if C in flips else 0, k)
        ready[key] += 1
        if ready[key] == NY:
            work.append(functools.partial(dispatch, seen, taken, *key, all_cols))
            if all(ready[(g, n)] == NY for g in range(NC) for n in range(NZ // 2)) and not near_begun:
                near_begun = True
                work += [wait_weights] + hidden_steps(0)
        for _ in range(min(len(work), 1 if k < NZ - 1 else 2)):
            work.pop(0)()
    for chunk in work:
        chunk()
    for chunk in hidden_steps(1):
        chunk()

    far = list(reversed(range(NZ)))
    spare = spare_sem
    cut = lvl_b0.shape[2]
    in_ways = [
        Reduce(place, back[0], cot_seen.at[:, :, pl.ds(0, cut)], (lvl_b0, lvl_b1), chain_b, send_b, recv_b, spare),
        Reduce(place, back[1], cot_seen.at[:, :, pl.ds(cut, wide - cut)], (lvl_c0, lvl_c1), chain_c, send_c, recv_c, spare),
    ]
    in_steps = [step for t in range(NZ + 3) for way in in_ways for step in way.at_time(t)]
    for e in range(held):
        project(1, e, grad_act, (0, 2 * hidden))
    for k in far[: NZ // 2]:
        combine(cot_seen, 1, k, all_cols)
        for way in in_ways:
            way.first(k)
    for k in far[: NZ // 2]:
        combine(cot_seen, 0, k, all_cols)
    in_steps.pop(0)()
    in_steps.pop(0)()
    for e in range(held):
        project(0, e, grad_act, (0, 2 * hidden))
    in_steps.pop(0)()
    for k in far[NZ // 2 :]:
        combine(cot_seen, 1, k, all_cols)
        for way in in_ways:
            way.first(k)
    for _ in range(3):
        in_steps.pop(0)()
    for k in far[NZ // 2 :]:
        combine(cot_seen, 0, k, all_cols)
    for way in in_ways:
        way.level(0, 1)
        way.level(0, 0)
    done = ((0, 1), (0, 0))
    in_steps = [step for step in in_steps if not isinstance(step, functools.partial) or step.args not in done]
    for way in ways:
        way.finish()
    part_copies = []
    work = []

    def out_part(h, k):
        combine(seen, h, k, columns_of(width))
        at = pl.ds(base_of(h, k), NY)
        copy = pltpu.make_async_copy(seen.at[at, :, pl.ds(0, width)], part_out.at[at], part_sem.at[len(part_copies)])
        copy.start()
        part_copies.append(copy)

    for n in range(2):
        for e in range(held):
            work.append(functools.partial(project, n, e, scaled, (2 * hidden, hidden)))
        for k in range(n * NZ // 2, (n + 1) * NZ // 2):
            for h in range(NC):
                work.append(functools.partial(out_part, h, k))
    work += [functools.partial(weight_grad, e, j) for j in reversed(range(NX * NC)) for e in range(held)]
    while in_steps or work:
        if in_steps:
            in_steps.pop(0)()
        for _ in range(2):
            if work:
                work.pop(0)()
    in_ways[0].last(gin_out.at[:, pl.ds(0, cut)])
    in_ways[1].last(gin_out.at[:, pl.ds(cut, wide - cut)])
    piece.wait_send()
    for copy in stores[-2:] + part_copies:
        copy.wait()
    for way in in_ways:
        way.finish()


def moe(payload, cots, parts, cap, collective_id):
    count, wide = payload.shape
    width = wide - 128
    held, quarter, columns = parts[0].shape
    hidden = columns // 3
    cut = count * 3 // 4
    plans = [
        Plan(0, (Z, Y, C), (C, Z, Y), rows=(0, cut)),
        Plan(0, (Y, Z, C), (C, Z, Y), rows=(cut, count - cut)),
    ]
    back = [Plan(0, (C, Y, Z), (C, Z, Y)), Plan(0, (C, Z, Y), (C, Z, Y))]
    widths = (wide - wide // 4 // 128 * 128, wide // 4 // 128 * 128)
    blocks = NC * NZ * NY
    pair = NY * cap
    rows = blocks // NY * pair
    lanes = tile_up(held * pair, 128)
    bf, f32 = jnp.bfloat16, jnp.float32
    whole = pl.BlockSpec(memory_space=pltpu.VMEM)
    apart = pl.BlockSpec(memory_space=pl.ANY)
    dma = pltpu.SemaphoreType.DMA
    return pl.pallas_call(
        functools.partial(moe_kernel, plans, back, width, hidden, cap),
        out_shape=[
            jax.ShapeDtypeStruct((count, wide), f32),
            jax.ShapeDtypeStruct((blocks, count, width), bf),
        ]
        + [jax.ShapeDtypeStruct((held, quarter, columns), bf)] * (NX * NC),
        in_specs=[whole] + [apart] * 7,
        out_specs=[whole] + [apart] * (1 + NX * NC),
        scratch_shapes=[
            pltpu.VMEM((blocks, count, wide), bf),
            pltpu.VMEM((blocks, count, wide), bf),
            pltpu.VMEM((held, NX * NC * quarter, columns), bf),
            pltpu.VMEM((held, rows, wide), bf),
            pltpu.VMEM((held, rows, width), bf),
            pltpu.VMEM((held, rows, wide), bf),
            pltpu.VMEM((held, rows, hidden), bf),
            pltpu.VMEM((held, rows, 2 * hidden), bf),
            pltpu.VMEM((blocks // NY, NY * count, lanes), bf),
            pltpu.VMEM((2, quarter, columns), bf),
        ]
        + [pltpu.VMEM((n, count, w), bf) for p, w in zip(back, widths) for n in Reduce.counts(p)[0]]
        + [
            dma((sum(Gather.sends(p) for p in plans),)),
            dma((sum(p.blocks for p in plans),)),
            dma(()),
            *[dma((n,)) for p in back for n in Reduce.counts(p)[1:]],
            dma((held * NX * NC + blocks // NY,)),
            dma((held * NX * NC,)),
            dma((blocks // NY,)),
            dma((2,)),
        ],
        compiler_params=pltpu.CompilerParams(
            collective_id=collective_id, has_side_effects=True, vmem_limit_bytes=67043328
        ),
        name="experts",
    )(payload, cots, *parts)


def weights_kernel(plans, gain_at, *refs):
    left_one, right_one, left_two, right_two, left_small, right_small = refs[:6]
    matrix_in, hidden, gain, grad_mixed = refs[6:10]
    n_ways = len(plans)
    outs, grad_input = refs[10:13], refs[13]
    held = refs[14 : 14 + n_ways]
    buffers, refs = refs[14 + n_ways : 14 + 5 * n_ways], refs[14 + 5 * n_ways :]
    matrix, grad_in, halves = refs[:3]
    sems, (spare, matrix_sem) = refs[3 : 3 + 2 * n_ways], refs[3 + 2 * n_ways :]
    bf, f32 = jnp.bfloat16, jnp.float32
    place = Place()
    far = list(reversed(range(NZ)))
    fetch = pltpu.make_async_copy(matrix_in, matrix, matrix_sem)
    fetch.start()
    count_here = hail(place, (Z, Y, X, C))
    *ways, small_way = [
        Reduce(place, plan, held[n], buffers[4 * n : 4 * n + 3], buffers[4 * n + 3], sems[2 * n], sems[2 * n + 1], spare)
        for n, plan in enumerate(plans)
    ]
    group = NY * NX * NC
    rows = group * held[0].shape[1]

    def products(pairs, target, k, shift=0):
        at = pl.ds(pl.multiple_of(place.order[k] * rows, 128), rows)
        for c0, cn in columns_of(target.shape[2]):
            got = sum(
                lax.dot_general(
                    left[:, at], right[:, shift + c0 : shift + c0 + cn], (((0,), (0,)), ((), ())),
                    preferred_element_type=f32,
                )
                for left, right in pairs
            )
            target[pl.ds(place.order[k] * group, group), :, c0 : c0 + cn] = got.astype(target.dtype).reshape(
                group, rows // group, cn
            )

    def round_of(some, t):
        for way in some:
            for step in way.at_time(t):
                step()

    for t in range(NZ):
        for n, way in enumerate(ways):
            width = held[n].shape[2]
            products([(left_one, right_one) if n < 2 else (left_two, right_two)], held[n], far[t], n % 2 * width)
            if t == n == 0:
                meet(count_here)
            way.first(far[t])
        if t > 0:
            round_of(ways, t - 1)
    fetch.wait()
    for c0, cn in columns_of(grad_in.shape[1]):
        grad_in[:, c0 : c0 + cn] = lax.dot_general(
            right_one[...], matrix[c0 : c0 + cn], (((1,), (1,)), ((), ())), preferred_element_type=f32
        )
    count = grad_in.shape[0]
    wide = hidden[...].astype(f32)
    inverse = lax.rsqrt(jnp.mean(wide * wide, axis=1, keepdims=True) + norm_eps)
    unit = wide * inverse
    factor = grad_in[...] * unit
    high = factor.astype(bf)
    halves[:count] = high
    halves[count:] = (factor - high.astype(f32)).astype(bf)
    scaled = grad_in[...] * gain[...]
    mean = jnp.mean(scaled * unit, axis=1, keepdims=True)
    grad_input[...] = grad_mixed[...] + inverse * (scaled - unit * mean)
    column = (lax.broadcasted_iota(jnp.int32, (2 * count, 128), 1) == gain_at).astype(f32).astype(bf)
    for k in far:
        products([(left_small, right_small), (halves, column)], held[-1], k)
        small_way.first(k)
    late = [(0, 1, 2), (3, 4), (5,), (6,)]
    for n, t in enumerate(range(NZ - 1, NZ + 3)):
        round_of(ways, t)
        for t_small in late[n]:
            round_of([small_way], t_small)
    for n, way in enumerate(ways):
        width = held[n].shape[2]
        way.last(outs[n // 2].at[:, pl.ds(n % 2 * width, width)])
    small_way.last(outs[2])
    for way in ways + [small_way]:
        way.finish()


def return_weights(lefts, rights, matrix, hidden, gain, grad_mixed, gain_at, collective_id):
    width = lefts[0].shape[1]
    rows = width // (NZ * NY * NX * NC)
    widths = [r.shape[1] for r in rights]
    whole = (Z, Y, X, C)
    orders = ((C, Y, Z, X), (C, Y, Z, X), (C, X, Z, Y), (C, X, Y, Z), (C, Y, X, Z))
    plans = [Plan(0, order, whole) for order in orders]
    parts = [widths[0] // 2] * 2 + [widths[1] // 2] * 2 + [widths[2]]
    bf, f32 = jnp.bfloat16, jnp.float32
    dma = pltpu.SemaphoreType.DMA
    vmem = pl.BlockSpec(memory_space=pltpu.VMEM)
    count = hidden.shape[0]
    return pl.pallas_call(
        functools.partial(weights_kernel, plans, gain_at),
        out_shape=[jax.ShapeDtypeStruct((rows, w), f32) for w in widths] + [jax.ShapeDtypeStruct(hidden.shape, f32)],
        in_specs=[vmem] * 6 + [pl.BlockSpec(memory_space=pl.ANY)] + [vmem] * 3,
        out_specs=[vmem] * 4,
        scratch_shapes=[pltpu.VMEM((plans[0].blocks, rows, w), bf) for w in parts]
        + [pltpu.VMEM((n, rows, w), bf) for p, w in zip(plans, parts) for n in Reduce.counts(p)[0]]
        + [pltpu.VMEM(matrix.shape, bf), pltpu.VMEM(hidden.shape, f32), pltpu.VMEM((2 * count, width), bf)]
        + [dma((n,)) for p in plans for n in Reduce.counts(p)[1:]]
        + [dma(()), dma(())],
        compiler_params=pltpu.CompilerParams(
            collective_id=collective_id, has_side_effects=True, vmem_limit_bytes=64 * 1024 * 1024
        ),
        name="return_weights",
    )(*[a for pair in zip(lefts, rights) for a in pair], matrix, hidden, gain, grad_mixed)


def turn(block, cosine, sine):
    lane = lax.broadcasted_iota(jnp.int32, (1, 128), 1)
    half = HEAD_SIZE // 2
    other = jnp.where(lane % HEAD_SIZE < half, pltpu.roll(block, 128 - half, 1), pltpu.roll(block, half, 1))
    return block * cosine + other * sine


def place_heads(read, target, count):
    group = QUERY_HEADS // KEY_VALUE_HEADS
    lane = lax.broadcasted_iota(jnp.int32, (1, 2 * HEAD_SIZE), 1)
    for pair in range(QUERY_HEADS // 2):
        both = read(pair)
        for h in (2 * pair, 2 * pair + 1):
            m, g = h // group, h % group
            block = both if h % 2 == m % 2 else pltpu.roll(both, HEAD_SIZE, 1)
            block = jnp.where(lane // HEAD_SIZE == m % 2, block, 0.0)
            target[m, g * count : (g + 1) * count] = block.astype(target.dtype)


def collect_heads(source, target, count, finish):
    group = QUERY_HEADS // KEY_VALUE_HEADS
    lane = lax.broadcasted_iota(jnp.int32, (1, 2 * HEAD_SIZE), 1)
    for pair in range(QUERY_HEADS // 2):
        sides = []
        for h in (2 * pair, 2 * pair + 1):
            m, g = h // group, h % group
            block = source[m, g * count : (g + 1) * count]
            sides.append(block if h % 2 == m % 2 else pltpu.roll(block, HEAD_SIZE, 1))
        both = finish(jnp.where(lane < HEAD_SIZE, *sides))
        target[:, pair * 128 : pair * 128 + 128] = both.astype(target.dtype)


class Scores:
    def __init__(self, place, queries, keys):
        self.queries, self.keys = queries, keys
        group = QUERY_HEADS // KEY_VALUE_HEADS
        count = keys.shape[1]
        self.total = keys.shape[0] * count
        row = lax.broadcasted_iota(jnp.int32, (group * count, 1), 0) % count
        self.position = row + (place.at[Z] * NY + place.at[Y]) * count
        self.column = lax.broadcasted_iota(jnp.int32, (1, self.total), 1)

    def pair(self, m, shift):
        at = pl.ds(pl.multiple_of(shift + m // 2 * 128, 128), 128)
        return self.keys[:, :, at].reshape(self.total, 128)

    def of(self, m, keys):
        found = lax.dot_general(
            self.queries[m], keys, (((1,), (1,)), ((), ())), preferred_element_type=jnp.float32
        )
        return jnp.where(self.column <= self.position, found * attn_scale, masked_logits)


def attend_kernel(
    plans, linear, cot, routes, cosine, sine, out, log_sums, kv_out, cots, placed, seen, own_kv, own_cots, raw, *sems
):
    send_kv, recv_kv, send_cot, recv_cot, spare, own_sem = sems
    place = Place()
    bf, f32 = jnp.bfloat16, jnp.float32
    count_here = hail(place, (Z, Y, C))
    count = linear.shape[0]
    width = KEY_VALUE_HEADS * HEAD_SIZE
    q_width = QUERY_HEADS * HEAD_SIZE
    for c0 in range(0, width, 128):
        block = linear[:, q_width + c0 : q_width + c0 + 128]
        own_kv[:, c0 : c0 + 128] = turn(block, cosine[...], sine[...]).astype(bf)
    own_kv[:, width:] = linear[:, q_width + width :].astype(bf)
    model = cot.shape[1]
    own_cots[:, :model] = cot[...].astype(bf)
    expert = lax.broadcasted_iota(jnp.int32, (1, 128), 1)
    routed = routes[:, 0:1] == expert
    for n in range(1, routes.shape[1]):
        routed = jnp.logical_or(routed, routes[:, n : n + 1] == expert)
    own_cots[:, model:] = routed.astype(f32).astype(bf)
    meet(count_here)
    kv_way = Gather(place, plans[0], own_kv, seen, send_kv, recv_kv, spare, 0, 0)
    cot_ways, at = [], 0
    for n, plan in enumerate(plans[1:]):
        cot_ways.append(Gather(place, plan, own_cots, cots, send_cot, recv_cot, spare, at, n * plan.blocks))
        at += Gather.sends(plan)
    kv_way.step(0, ())
    for way in cot_ways:
        way.step(0, ())
    mine = pltpu.make_async_copy(own_cots, cots.at[flat_index(place.at, plans[1].index)], own_sem.at[0])
    mine.start()
    seen[flat_index(place.at, plans[0].index)] = own_kv[...]
    place_heads(lambda pair: turn(linear[:, pair * 128 : pair * 128 + 128], cosine[...], sine[...]), placed, count)
    log_sums[...] = jnp.zeros(log_sums.shape, f32)
    early = [e for e in gather_events(plans[1].order)[1:]]
    kv_events = gather_events(plans[0].order)[1:]
    for k, flips in kv_events:
        kv_way.step(k, flips)
        if len(early) > 8:
            event = early.pop(0)
            for way in cot_ways:
                way.step(*event)
    keep = pltpu.make_async_copy(seen, kv_out, own_sem.at[1])
    keep.start()
    scores = Scores(place, placed, seen)
    lane = lax.broadcasted_iota(jnp.int32, (1, 128), 1)

    def head(m, carry):
        for i in range(KEY_VALUE_HEADS):
            if early:
                event = early.pop(0)

                @pl.when(m == i)
                def _():
                    for way in cot_ways:
                        way.step(*event)

        s = scores.of(m, scores.pair(m, 0))
        best = jnp.max(s, axis=1, keepdims=True)
        weights = jnp.exp(s - best)
        total = jnp.sum(weights, axis=1, keepdims=True)
        mixed = jnp.dot(weights.astype(bf), scores.pair(m, width), preferred_element_type=f32)
        raw[m] = mixed / total
        log_sums[...] = jnp.where(lane == m, best + jnp.log(total), log_sums[...])
        return carry

    lax.fori_loop(0, KEY_VALUE_HEADS, head, 0)
    collect_heads(raw, out, count, lambda block: block)
    keep.wait()
    mine.wait()
    kv_way.finish()
    for way in cot_ways:
        way.finish()


def attend(linear, cot, routes, cosine, sine, collective_id):
    count = linear.shape[0]
    kv_width = 2 * KEY_VALUE_HEADS * HEAD_SIZE
    cut = count * 3 // 4
    plans = [
        Plan(0, (Z, Y), (Z, Y)),
        Plan(1, (Z, Y, C), (C, Z, Y), rows=(0, cut)),
        Plan(1, (Y, Z, C), (C, Z, Y), rows=(cut, count - cut)),
    ]
    bf, f32 = jnp.bfloat16, jnp.float32
    group = QUERY_HEADS // KEY_VALUE_HEADS
    vmem = pl.BlockSpec(memory_space=pltpu.VMEM)
    apart = pl.BlockSpec(memory_space=pl.ANY)
    dma = pltpu.SemaphoreType.DMA
    kv_shape = (plans[0].blocks, count, kv_width)
    cot_shape = (count, cot.shape[1] + 128)
    heads = (KEY_VALUE_HEADS, group * count, 2 * HEAD_SIZE)
    return pl.pallas_call(
        functools.partial(attend_kernel, plans),
        out_shape=[
            jax.ShapeDtypeStruct((count, QUERY_HEADS * HEAD_SIZE), bf),
            jax.ShapeDtypeStruct((group * count, 128), f32),
            jax.ShapeDtypeStruct(kv_shape, bf),
            jax.ShapeDtypeStruct((plans[1].blocks,) + cot_shape, bf),
            jax.ShapeDtypeStruct(heads, bf),
        ],
        in_specs=[vmem] * 5,
        out_specs=[vmem, vmem, apart, apart, vmem],
        scratch_shapes=[
            pltpu.VMEM(kv_shape, bf),
            pltpu.VMEM((count, kv_width), bf),
            pltpu.VMEM(cot_shape, bf),
            pltpu.VMEM(heads, f32),
        ]
        + [
            dma((Gather.sends(plans[0]),)),
            dma((plans[0].blocks,)),
            dma((Gather.sends(plans[1]) + Gather.sends(plans[2]),)),
            dma((plans[1].blocks + plans[2].blocks,)),
            dma(()),
            dma((2,)),
        ],
        compiler_params=pltpu.CompilerParams(
            collective_id=collective_id, has_side_effects=True, vmem_limit_bytes=56 * 1024 * 1024
        ),
        name="attend",
    )(linear, cot, routes, cosine, sine)


def attend_back_kernel(plans, *refs):
    placed, gin, gate_map, cot, ffn_gain, outputs, log_sums, keys, part, w_o, mixed, cosine, sine = refs[:13]
    back, layer_out, grad_mixed, grad_attn, left_small, right_small = refs[13:19]
    kv_grad, grads_placed, raw, deltas, held, held_out, grads, matrix = refs[19:27]
    level, chain, v_level, v_chain, out_level, out_level_two, out_chain = refs[27:34]
    send_kv, recv_kv, send_v, recv_v, send_out, recv_out, spare, load_sem, matrix_sem = refs[34:]
    place = Place()
    bf, f32 = jnp.bfloat16, jnp.float32
    far = list(reversed(range(NZ)))
    loads = []
    for k in far:
        for h in (1 - place.at[C], place.at[C]):
            at = pl.ds((h * NZ + place.order[k]) * NY, NY)
            loads.append(pltpu.make_async_copy(part.at[at], held_out.at[at], load_sem.at[len(loads)]))
    for copy in loads:
        copy.start()
    fetch = pltpu.make_async_copy(w_o, matrix, matrix_sem)
    fetch.start()
    meet(hail(place, (Z, Y, C)))
    width = KEY_VALUE_HEADS * HEAD_SIZE
    k_way = Reduce(place, plans[0], held.at[:, :, pl.ds(0, width)], (level,), chain, send_kv, recv_kv, spare)
    v_way = Reduce(place, plans[1], held.at[:, :, pl.ds(width, width)], (v_level,), v_chain, send_v, recv_v, spare)
    out_way = Reduce(place, plans[2], held_out, (out_level, out_level_two), out_chain, send_out, recv_out, spare)
    for copy in loads:
        copy.wait()
    for k in far:
        out_way.first(k)
    count = grads.shape[0]
    fetch.wait()
    out_way.level(0, 3)
    out_way.level(0, 2)
    model = cot.shape[1]
    lane = lax.broadcasted_iota(jnp.int32, (1, 128), 1)
    halves = gin[:, model:]
    gate_grad = jnp.where(lane < EXPERT_COUNT, halves + pltpu.roll(halves, 128 - EXPERT_COUNT, 1), 0.0)
    weighted = jnp.sum(gate_map[...] * gate_grad, axis=1, keepdims=True)
    grad_logits = (gate_map[...] * (gate_grad - weighted)).astype(bf)
    over_cols = (((1,), (1,)), ((), ()))
    inverse = lax.rsqrt(jnp.mean(mixed[...] * mixed[...], axis=1, keepdims=True) + norm_eps)
    unit = mixed[...] * inverse
    grad_in = gin[:, :model] + lax.dot_general(
        grad_logits, matrix[:, model:], over_cols, preferred_element_type=f32
    )
    scaled = grad_in * ffn_gain[...]
    grad_mixed[...] = cot[...] + inverse * (scaled - unit * jnp.mean(scaled * unit, axis=1, keepdims=True))
    grad_attn[...] = grad_mixed[...].astype(bf)
    factor = grad_in * unit
    high = factor.astype(bf)
    left_small[:count] = (unit * ffn_gain[...]).astype(bf)
    left_small[count : 2 * count] = high
    left_small[2 * count :] = (factor - high.astype(f32)).astype(bf)
    right_small[:count] = grad_logits
    right_small[count:] = jnp.broadcast_to(jnp.where(lane == EXPERT_COUNT + 1, 1.0, 0.0), (2 * count, 128)).astype(bf)
    for c0, cn in columns_of(grads.shape[1]):
        grads[:, c0 : c0 + cn] = lax.dot_general(
            grad_attn[...], matrix[c0 : c0 + cn, :model], over_cols, preferred_element_type=f32
        ).astype(bf)
    out_way.level(0, 1)
    place_heads(lambda pair: grads[:, pair * 128 : pair * 128 + 128].astype(f32), grads_placed, count)
    group = QUERY_HEADS // KEY_VALUE_HEADS
    lane = lax.broadcasted_iota(jnp.int32, (1, 128), 1)
    for g in range(group):
        found = jnp.zeros((count, 128), f32)
        for m in range(KEY_VALUE_HEADS):
            h = m * group + g
            at = slice(h // 2 * 128, h // 2 * 128 + 128)
            both = grads[:, at].astype(f32) * outputs[:, at].astype(f32)
            delta = jnp.sum(jnp.where(lane // HEAD_SIZE == h % 2, both, 0.0), axis=1, keepdims=True)
            found = jnp.where(lane == m, delta, found)
        deltas[g * count : (g + 1) * count] = found
    scores = Scores(place, placed, keys)
    blocks = keys.shape[0]
    turns = KEY_VALUE_HEADS // 2
    early = [[(out_way.level, 1, 3)], [(out_way.along, 3), (out_way.level, 1, 2)], [(out_way.along, 2)], []]

    def pair(p, carry):
        for i in range(turns):

            @pl.when(p == i)
            def _():
                for step, *at in early[i]:
                    step(*at)

        key_sum = value_sum = None
        for side in range(2):
            m = 2 * p + side
            k_pair, v_pair = scores.pair(m, 0), scores.pair(m, width)
            of_head = lambda ref: jnp.sum(jnp.where(lane == m, ref[...], 0.0), axis=1, keepdims=True)
            weights = jnp.exp(scores.of(m, k_pair) - of_head(log_sums))
            grad = grads_placed[m]
            grad_probs = lax.dot_general(grad, v_pair, (((1,), (1,)), ((), ())), preferred_element_type=f32)
            grad_scores = (weights * (grad_probs - of_head(deltas))).astype(bf)
            raw[m] = attn_scale * jnp.dot(grad_scores, k_pair, preferred_element_type=f32)
            over_rows = (((0,), (0,)), ((), ()))
            key_part = lax.dot_general(grad_scores, placed[m], over_rows, preferred_element_type=f32)
            value_part = lax.dot_general(weights.astype(bf), grad, over_rows, preferred_element_type=f32)
            key_sum = key_part if key_sum is None else key_sum + key_part
            value_sum = value_part if value_sum is None else value_sum + value_part
        at = pl.multiple_of(p * 128, 128)
        held[:, :, pl.ds(at, 128)] = (attn_scale * key_sum).astype(bf).reshape(blocks, count, 128)
        at = pl.multiple_of(width + p * 128, 128)
        held[:, :, pl.ds(at, 128)] = value_sum.astype(bf).reshape(blocks, count, 128)
        return carry

    lax.fori_loop(0, turns, pair, 0)
    for k in far:
        k_way.first(k)
    v_way.along(3)
    out_way.level(0, 0)
    collect_heads(raw, back, count, lambda block: turn(block, cosine[...], -sine[...]))
    k_way.level(0, 3)
    v_way.along(2)
    k_way.level(0, 2)
    k_way.along(3)
    v_way.along(1)
    k_way.level(0, 1)
    k_way.along(2)
    v_way.settle()
    k_way.level(0, 0)
    k_way.along(1)
    k_way.last(kv_grad.at[:, pl.ds(0, width)])
    v_way.level(1, 0)
    v_way.last(kv_grad.at[:, pl.ds(width, width)])
    q_width = QUERY_HEADS * HEAD_SIZE
    for c0 in range(0, width, 128):
        block = turn(kv_grad[:, c0 : c0 + 128], cosine[...], -sine[...])
        back[:, q_width + c0 : q_width + c0 + 128] = block.astype(bf)
    back[:, q_width + width :] = kv_grad[:, width:].astype(bf)
    out_way.level(1, 1)
    out_way.along(1)
    out_way.level(1, 0)
    out_way.last(layer_out, mixed)
    for way in (k_way, v_way, out_way):
        way.finish()


def attend_back(
    placed, gin, gate_map, cot, ffn_gain, outputs, log_sums, keys, part, w_o, mixed, cosine, sine, collective_id
):
    count, kv_width = keys.shape[1:]
    plans = [Plan(0, (Y, Z), (Z, Y)), Plan(0, (Z, Y), (Z, Y)), Plan(1, (C, Y, Z), (C, Z, Y))]
    bf, f32 = jnp.bfloat16, jnp.float32
    group = QUERY_HEADS // KEY_VALUE_HEADS
    vmem = pl.BlockSpec(memory_space=pltpu.VMEM)
    apart = pl.BlockSpec(memory_space=pl.ANY)
    dma = pltpu.SemaphoreType.DMA
    heads = (KEY_VALUE_HEADS, group * count, 2 * HEAD_SIZE)
    blocks = [(count, kv_width // 2)] * 2 + [part.shape[1:]]
    return pl.pallas_call(
        functools.partial(attend_back_kernel, plans),
        out_shape=[
            jax.ShapeDtypeStruct((count, outputs.shape[1] + kv_width), bf),
            jax.ShapeDtypeStruct(mixed.shape, bf),
            jax.ShapeDtypeStruct(mixed.shape, f32),
            jax.ShapeDtypeStruct(mixed.shape, bf),
            jax.ShapeDtypeStruct((3 * count, mixed.shape[1]), bf),
            jax.ShapeDtypeStruct((3 * count, 128), bf),
        ],
        in_specs=[vmem] * 8 + [apart] * 2 + [vmem] * 3,
        out_specs=[vmem] * 6,
        scratch_shapes=[
            pltpu.VMEM((count, kv_width), f32),
            pltpu.VMEM(heads, bf),
            pltpu.VMEM(heads, f32),
            pltpu.VMEM((group * count, 128), f32),
            pltpu.VMEM(keys.shape, bf),
            pltpu.VMEM(part.shape, bf),
            pltpu.VMEM(outputs.shape, bf),
            pltpu.VMEM(w_o.shape, bf),
        ]
        + [pltpu.VMEM((n,) + b, bf) for p, b in zip(plans, blocks) for n in Reduce.counts(p)[0]]
        + [dma((n,)) for p in plans for n in Reduce.counts(p)[1:]]
        + [dma(()), dma((NC * NZ,)), dma(())],
        compiler_params=pltpu.CompilerParams(
            collective_id=collective_id, has_side_effects=True, vmem_limit_bytes=64 * 1024 * 1024
        ),
        name="attend_back",
    )(placed, gin, gate_map, cot, ffn_gain, outputs, log_sums, keys, part, w_o, mixed, cosine, sine)


def last_kernel(core_ref, own, core_part, x_part, both_part, one, two, small, layer, grad, *outs):
    core = core_ref[0]
    in_out, out_out = outs[:2]
    split = in_out.shape[3]
    for at, left, right in ((core, own, x_part), (1 - core, core_part, both_part)):
        total = left[0].astype(jnp.float32) + right[0].astype(jnp.float32)
        in_out[at, 0] = total[:, :split]
        out_out[at, 0] = total[:, split:]

    @pl.when(jnp.logical_and(pl.program_id(0) == 0, pl.program_id(1) == 0))
    def _():
        wq, wk, wv, wo, router, first_gain, second_gain, layer_out, grad_out = outs[2:]
        layer_out[...] = layer[...]
        grad_out[...] = grad[...]
        q, k = wq.shape[1], wk.shape[1]
        wq[...] = one[:, :q]
        wk[...] = one[:, q : q + k]
        wv[...] = one[:, q + k :]
        wo[...] = two[...]
        turned = small[...].T
        at = router.shape[0]
        router[...] = turned[:at]
        first_gain[...] = turned[at : at + 1]
        second_gain[...] = turned[at + 1 : at + 2]


def last_outputs(pieces, core, split, sums, widths):
    held, quarter, columns = pieces[0].shape
    step = quarter // 2
    rows = sums[0].shape[0]
    spec = pl.BlockSpec((1, step, columns), lambda e, r, c: (e, r, 0))
    fixed = lambda a, b: pl.BlockSpec((a, b), lambda e, r, c: (0, 0))
    outs = (split, columns - split)
    shapes = [(rows, w) for w in widths[:-1]] + [(widths[-1], rows)] + [(1, rows)] * 2 + [a.shape for a in sums[3:]]
    types = [jnp.float32] * 7 + [a.dtype for a in sums[3:]]
    return pl.pallas_call(
        last_kernel,
        grid_spec=pltpu.PrefetchScalarGridSpec(
            num_scalar_prefetch=1,
            grid=(held, 2),
            in_specs=[spec] * 4 + [fixed(*a.shape) for a in sums],
            out_specs=[pl.BlockSpec((NC, 1, step, w), lambda e, r, c: (0, e, r, 0)) for w in outs]
            + [fixed(*s) for s in shapes],
        ),
        out_shape=[jax.ShapeDtypeStruct((NC, held, quarter, w), jnp.float32) for w in outs]
        + [jax.ShapeDtypeStruct(s, d) for s, d in zip(shapes, types)],
        name="last_outputs",
    )(core[None], *pieces, *sums)


MODEL_WIDTH = 1536
QUERY_HEADS = 24
KEY_VALUE_HEADS = 8
HEAD_SIZE = 64
EXPERT_HIDDEN = 512
EXPERT_COUNT = 32
TOP = 8
CAP = 40


norm_eps = 1e-06
attn_scale = 0.015625
rope_base = 10000.0
masked_logits = -1e30


def rope_tables(positions):
    half = HEAD_SIZE // 2
    frequency = jnp.power(
        jnp.float32(rope_base), -2.0 * jnp.arange(half, dtype=jnp.float32) / HEAD_SIZE
    )
    angle = positions.astype(jnp.float32)[:, None] * frequency[None, :]
    return (jnp.cos(angle)[:, None, :], jnp.sin(angle)[:, None, :])


def rotate_pairs(value_tensor, cosine_table, sine_table):
    half = value_tensor.shape[-1] // 2
    first = value_tensor[..., :half]
    second = value_tensor[..., half:]
    return jnp.concatenate(
        [first * cosine_table - second * sine_table, second * cosine_table + first * sine_table],
        axis=-1,
    )


def rms_forward(wide, gain):
    inverse = lax.rsqrt(jnp.mean(wide * wide, axis=-1, keepdims=True) + norm_eps)
    unit = wide * inverse
    return (unit, inverse, (unit * gain.astype(jnp.float32)).astype(jnp.bfloat16))


def rms_backward(grad, unit, inverse, gain):
    scaled = grad * gain.astype(jnp.float32)
    back = inverse * (scaled - unit * jnp.mean(scaled * unit, axis=-1, keepdims=True))
    return (back, jnp.sum(grad * unit, axis=0))


def piece_scores(query_rows, key_section, positions):
    token_count = key_section.shape[0]
    key_tensor = key_section.reshape(token_count, KEY_VALUE_HEADS, HEAD_SIZE)
    scores = (
        jnp.einsum("tkgd,nkd->kgtn", query_rows, key_tensor, preferred_element_type=jnp.float32)
        * attn_scale
    )
    visible = jnp.arange(token_count, dtype=jnp.int32)[None, :] <= positions[:, None]
    return (jnp.where(visible, scores, masked_logits), visible, key_tensor)


def local(
    hidden,
    routes,
    attn_norm,
    ffn_norm,
    w_q,
    key_weight,
    value_weight,
    w_o,
    router,
    expert_in,
    expert_out,
    cotangent,
):
    token_rows = hidden.shape[1]
    query_group = QUERY_HEADS // KEY_VALUE_HEADS
    ctx_size = lax.axis_size(CTX)
    sequence_length = token_rows * ctx_size
    positions = lax.axis_index(CTX) * token_rows + jnp.arange(token_rows, dtype=jnp.int32)
    cosine_table, sine_table = rope_tables(positions)
    contract_rows = (((0,), (0,)), ((), ()))
    contract_cols = (((1,), (1,)), ((), ()))
    layer = (
        lax.all_gather(attn_norm, (CTX, FSDP), axis=0, tiled=True),
        lax.all_gather(ffn_norm, (CTX, FSDP), axis=0, tiled=True),
        lax.all_gather(w_q, (CTX, FSDP), axis=0, tiled=True),
        lax.all_gather(key_weight, (CTX, FSDP), axis=0, tiled=True),
        lax.all_gather(value_weight, (CTX, FSDP), axis=0, tiled=True),
        lax.all_gather(w_o, (CTX, FSDP), axis=0, tiled=True),
        lax.all_gather(router, (CTX, FSDP), axis=0, tiled=True),
    )
    attn_gain, ffn_gain, query_w, key_weight_matrix, value_w, output_w, router_w = layer
    experts = (
        lax.all_gather(expert_in, FSDP, axis=1, tiled=True),
        lax.all_gather(expert_out, FSDP, axis=1, tiled=True),
    )
    weight_in, weight_out = experts
    wide = hidden[0].astype(jnp.float32)
    attn_unit, inverse_one, attention_input = rms_forward(wide, attn_gain)
    query_linear = jnp.dot(attention_input, query_w, preferred_element_type=jnp.float32).reshape(
        token_rows, QUERY_HEADS, HEAD_SIZE
    )
    query_rows = (
        rotate_pairs(query_linear, cosine_table, sine_table)
        .astype(jnp.bfloat16)
        .reshape(token_rows, KEY_VALUE_HEADS, query_group, HEAD_SIZE)
    )
    key_linear = jnp.dot(
        attention_input, key_weight_matrix, preferred_element_type=jnp.float32
    ).reshape(token_rows, KEY_VALUE_HEADS, HEAD_SIZE)
    key_matrix_rows = (
        rotate_pairs(key_linear, cosine_table, sine_table)
        .astype(jnp.bfloat16)
        .reshape(token_rows, KEY_VALUE_HEADS * HEAD_SIZE)
    )
    value_rows = jnp.dot(attention_input, value_w, preferred_element_type=jnp.float32).astype(
        jnp.bfloat16
    )
    init_state = (
        jnp.full((KEY_VALUE_HEADS, query_group, token_rows), masked_logits, jnp.float32),
        jnp.zeros((KEY_VALUE_HEADS, query_group, token_rows), jnp.float32),
        jnp.zeros((KEY_VALUE_HEADS, query_group, token_rows, HEAD_SIZE), jnp.float32),
    )
    key_section = lax.all_gather(key_matrix_rows, CTX, axis=0, tiled=True)
    value_section = lax.all_gather(value_rows, CTX, axis=0, tiled=True)

    def compute(current):
        best, total, weighted = current
        scores, visible, _ = piece_scores(query_rows, key_section, positions)
        value_tensor = value_section.reshape(value_section.shape[0], KEY_VALUE_HEADS, HEAD_SIZE)
        new_best = jnp.maximum(best, jnp.max(scores, axis=-1))
        weights = jnp.where(visible, jnp.exp(scores - new_best[..., None]), 0.0)
        total = jnp.sum(weights, axis=-1)
        weighted = jnp.einsum(
            "kgtn,nkd->kgtd",
            weights.astype(jnp.bfloat16),
            value_tensor,
            preferred_element_type=jnp.float32,
        )
        return (new_best, total, weighted)

    best, total, weighted = lax.cond(
        jnp.int32(0) <= positions[-1], compute, lambda current: current, init_state
    )
    log_sum_rows = best + jnp.log(total)
    attention_output = (
        jnp.transpose(weighted / total[..., None], (2, 0, 1, 3))
        .reshape(token_rows, QUERY_HEADS * HEAD_SIZE)
        .astype(jnp.bfloat16)
    )
    mixed = wide + jnp.dot(attention_output, output_w, preferred_element_type=jnp.float32)
    ffn_unit, inverse_two, ffn_in = rms_forward(mixed, ffn_gain)
    logits = jnp.dot(ffn_in, router_w, preferred_element_type=jnp.float32)
    route = routes[0]
    indicator = (route[:, :, None] == jnp.arange(EXPERT_COUNT, dtype=jnp.int32)).astype(jnp.float32)
    chosen = jnp.sum(indicator * logits[:, None, :], axis=-1)
    gates = jax.nn.softmax(chosen, axis=-1)
    flat_route = route.reshape(-1)
    counter = (flat_route[:, None] == jnp.arange(EXPERT_COUNT, dtype=jnp.int32)).astype(jnp.int32)
    slot = jnp.sum(counter * (jnp.cumsum(counter, axis=0) - 1), axis=1)
    target = flat_route * CAP + slot
    owner = (
        jnp.full((EXPERT_COUNT * CAP,), token_rows * TOP, jnp.int32)
        .at[target]
        .set(jnp.arange(token_rows * TOP, dtype=jnp.int32))
    )
    ffn_pad = jnp.concatenate([ffn_in, jnp.zeros((1, MODEL_WIDTH), jnp.bfloat16)], axis=0)
    local_experts = weight_in.shape[0]
    outgoing = ffn_pad[owner // TOP].reshape(ctx_size, local_experts, CAP, MODEL_WIDTH)
    received = lax.all_to_all(outgoing, CTX, split_axis=0, concat_axis=2, tiled=True)[0]
    act = jnp.einsum("erd,edf->erf", received, weight_in, preferred_element_type=jnp.float32)
    gate_part = act[..., :EXPERT_HIDDEN]
    up_part = act[..., EXPERT_HIDDEN:]
    sigma = jax.nn.sigmoid(gate_part)
    inner = (gate_part * sigma * up_part).astype(jnp.bfloat16)
    produced = jnp.einsum(
        "erf,edf->erd", inner, weight_out, preferred_element_type=jnp.float32
    ).astype(jnp.bfloat16)
    returned = lax.all_to_all(
        produced[None], CTX, split_axis=2, concat_axis=0, tiled=True
    ).reshape(EXPERT_COUNT * CAP, MODEL_WIDTH)
    picked = returned[target].reshape(token_rows, TOP, MODEL_WIDTH)
    layer_out = (mixed + jnp.sum(gates[..., None] * picked, axis=1)).astype(jnp.bfloat16)
    cot = cotangent[0]
    layer = (
        lax.all_gather(attn_norm, (CTX, FSDP), axis=0, tiled=True),
        lax.all_gather(ffn_norm, (CTX, FSDP), axis=0, tiled=True),
        lax.all_gather(w_q, (CTX, FSDP), axis=0, tiled=True),
        lax.all_gather(key_weight, (CTX, FSDP), axis=0, tiled=True),
        lax.all_gather(value_weight, (CTX, FSDP), axis=0, tiled=True),
        lax.all_gather(w_o, (CTX, FSDP), axis=0, tiled=True),
        lax.all_gather(router, (CTX, FSDP), axis=0, tiled=True),
    )
    attn_gain, ffn_gain, query_w, key_weight_matrix, value_w, output_w, router_w = layer
    experts = (
        lax.all_gather(expert_in, FSDP, axis=1, tiled=True),
        lax.all_gather(expert_out, FSDP, axis=1, tiled=True),
    )
    weight_in, weight_out = experts
    grad_gate = jnp.sum(cot[:, None, :] * picked, axis=-1)
    slot_grads = (
        (gates[..., None] * cot[:, None, :])
        .astype(jnp.bfloat16)
        .reshape(token_rows * TOP, MODEL_WIDTH)
    )
    slot_pad = jnp.concatenate([slot_grads, jnp.zeros((1, MODEL_WIDTH), jnp.bfloat16)], axis=0)
    grad_outgoing = slot_pad[owner].reshape(ctx_size, local_experts, CAP, MODEL_WIDTH)
    grad_received = lax.all_to_all(grad_outgoing, CTX, split_axis=0, concat_axis=2, tiled=True)[0]
    grad_w_out = jnp.einsum(
        "erd,erf->edf", grad_received, inner, preferred_element_type=jnp.float32
    )
    grad_inner = jnp.einsum(
        "erd,edf->erf", grad_received, weight_out, preferred_element_type=jnp.float32
    )
    grad_act = jnp.concatenate(
        [
            grad_inner * up_part * sigma * (1.0 + gate_part * (1.0 - sigma)),
            grad_inner * gate_part * sigma,
        ],
        axis=-1,
    ).astype(jnp.bfloat16)
    grad_w_in = jnp.einsum("erd,erf->edf", received, grad_act, preferred_element_type=jnp.float32)
    grad_rows = jnp.einsum(
        "erf,edf->erd", grad_act, weight_in, preferred_element_type=jnp.float32
    ).astype(jnp.bfloat16)
    grad_back = lax.all_to_all(
        grad_rows[None], CTX, split_axis=2, concat_axis=0, tiled=True
    ).reshape(EXPERT_COUNT * CAP, MODEL_WIDTH)
    grad_expert_in, grad_expert_out = (
        lax.psum_scatter(
            grad_w_in.astype(jnp.bfloat16), FSDP, scatter_dimension=1, tiled=True
        ).astype(jnp.float32),
        lax.psum_scatter(
            grad_w_out.astype(jnp.bfloat16), FSDP, scatter_dimension=1, tiled=True
        ).astype(jnp.float32),
    )
    grad_chosen = gates * (grad_gate - jnp.sum(gates * grad_gate, axis=-1, keepdims=True))
    grad_logits = jnp.sum(indicator * grad_chosen[..., None], axis=1).astype(jnp.bfloat16)
    grad_router_part = lax.dot_general(
        ffn_in, grad_logits, contract_rows, preferred_element_type=jnp.float32
    )
    grad_ffn_in = lax.dot_general(
        grad_logits, router_w, contract_cols, preferred_element_type=jnp.float32
    )
    grad_ffn_in = grad_ffn_in + jnp.sum(
        grad_back[target].reshape(token_rows, TOP, MODEL_WIDTH), axis=1, dtype=jnp.float32
    )
    back_two, grad_ffn_gain = rms_backward(grad_ffn_in, ffn_unit, inverse_two, ffn_gain)
    grad_mixed = cot + back_two
    grad_attn = grad_mixed.astype(jnp.bfloat16)
    grad_wo_part = lax.dot_general(
        attention_output, grad_attn, contract_rows, preferred_element_type=jnp.float32
    )
    attention_output_gradient = lax.dot_general(
        grad_attn, output_w, contract_cols, preferred_element_type=jnp.float32
    ).astype(jnp.bfloat16)
    head_gradient = attention_output_gradient.reshape(
        token_rows, KEY_VALUE_HEADS, query_group, HEAD_SIZE
    )
    delta_rows = jnp.sum(
        head_gradient.astype(jnp.float32)
        * attention_output.reshape(token_rows, KEY_VALUE_HEADS, query_group, HEAD_SIZE).astype(
            jnp.float32
        ),
        axis=-1,
    )
    delta_rows = jnp.transpose(delta_rows, (1, 2, 0))
    init_back = (
        jnp.zeros((token_rows, KEY_VALUE_HEADS, query_group, HEAD_SIZE), jnp.float32),
        jnp.zeros((sequence_length, 2 * KEY_VALUE_HEADS * HEAD_SIZE), jnp.float32),
    )
    attend_key_section = lax.all_gather(key_matrix_rows, CTX, axis=0, tiled=True)
    attend_value_section = lax.all_gather(value_rows, CTX, axis=0, tiled=True)

    def compute(current):
        token_count = attend_key_section.shape[0]
        scores, visible, key_tensor = piece_scores(query_rows, attend_key_section, positions)
        value_tensor = attend_value_section.reshape(token_count, KEY_VALUE_HEADS, HEAD_SIZE)
        weights_full = jnp.where(visible, jnp.exp(scores - log_sum_rows[..., None]), 0.0)
        grad_probs = jnp.einsum(
            "tkgd,nkd->kgtn", head_gradient, value_tensor, preferred_element_type=jnp.float32
        )
        grad_scores = (weights_full * (grad_probs - delta_rows[..., None])).astype(jnp.bfloat16)
        grad_query = attn_scale * jnp.einsum(
            "kgtn,nkd->tkgd", grad_scores, key_tensor, preferred_element_type=jnp.float32
        )
        key_portion = attn_scale * jnp.einsum(
            "kgtn,tkgd->nkd", grad_scores, query_rows, preferred_element_type=jnp.float32
        )
        value_portion = jnp.einsum(
            "kgtn,tkgd->nkd",
            weights_full.astype(jnp.bfloat16),
            head_gradient,
            preferred_element_type=jnp.float32,
        )
        update = jnp.concatenate(
            [
                key_portion.reshape(token_count, KEY_VALUE_HEADS * HEAD_SIZE),
                value_portion.reshape(token_count, KEY_VALUE_HEADS * HEAD_SIZE),
            ],
            axis=1,
        )
        return (grad_query, update)

    grad_query, grad_keys_full = lax.cond(
        jnp.int32(0) <= positions[-1], compute, lambda current: current, init_back
    )
    local_gradients = lax.psum_scatter(
        grad_keys_full.astype(jnp.bfloat16), CTX, scatter_dimension=0, tiled=True
    ).astype(jnp.float32)
    query_back = (
        rotate_pairs(
            grad_query.reshape(token_rows, QUERY_HEADS, HEAD_SIZE), cosine_table, -sine_table
        )
        .astype(jnp.bfloat16)
        .reshape(token_rows, QUERY_HEADS * HEAD_SIZE)
    )
    key_backward_rows = (
        rotate_pairs(
            local_gradients[:, : KEY_VALUE_HEADS * HEAD_SIZE].reshape(
                token_rows, KEY_VALUE_HEADS, HEAD_SIZE
            ),
            cosine_table,
            -sine_table,
        )
        .astype(jnp.bfloat16)
        .reshape(token_rows, KEY_VALUE_HEADS * HEAD_SIZE)
    )
    value_backward_rows = local_gradients[:, KEY_VALUE_HEADS * HEAD_SIZE :].astype(jnp.bfloat16)
    grad_wq_part = lax.dot_general(
        attention_input, query_back, contract_rows, preferred_element_type=jnp.float32
    )
    grad_wk_part = lax.dot_general(
        attention_input, key_backward_rows, contract_rows, preferred_element_type=jnp.float32
    )
    grad_wv_part = lax.dot_general(
        attention_input, value_backward_rows, contract_rows, preferred_element_type=jnp.float32
    )
    grad_attn_in = lax.dot_general(
        query_back, query_w, contract_cols, preferred_element_type=jnp.float32
    )
    grad_attn_in = grad_attn_in + lax.dot_general(
        key_backward_rows, key_weight_matrix, contract_cols, preferred_element_type=jnp.float32
    )
    grad_attn_in = grad_attn_in + lax.dot_general(
        value_backward_rows, value_w, contract_cols, preferred_element_type=jnp.float32
    )
    back_one, grad_attn_gain = rms_backward(grad_attn_in, attn_unit, inverse_one, attn_gain)
    grad_input = grad_mixed + back_one
    partial_sums = (
        lax.psum_scatter(
            grad_attn_gain.astype(jnp.bfloat16), CTX, scatter_dimension=0, tiled=True
        ).astype(jnp.float32),
        lax.psum_scatter(
            grad_ffn_gain.astype(jnp.bfloat16), CTX, scatter_dimension=0, tiled=True
        ).astype(jnp.float32),
        lax.psum_scatter(
            grad_wq_part.astype(jnp.bfloat16), CTX, scatter_dimension=0, tiled=True
        ).astype(jnp.float32),
        lax.psum_scatter(
            grad_wk_part.astype(jnp.bfloat16), CTX, scatter_dimension=0, tiled=True
        ).astype(jnp.float32),
        lax.psum_scatter(
            grad_wv_part.astype(jnp.bfloat16), CTX, scatter_dimension=0, tiled=True
        ).astype(jnp.float32),
        lax.psum_scatter(
            grad_wo_part.astype(jnp.bfloat16), CTX, scatter_dimension=0, tiled=True
        ).astype(jnp.float32),
        lax.psum_scatter(
            grad_router_part.astype(jnp.bfloat16), CTX, scatter_dimension=0, tiled=True
        ).astype(jnp.float32),
    )
    summed = (
        lax.psum_scatter(
            partial_sums[0].astype(jnp.bfloat16), FSDP, scatter_dimension=0, tiled=True
        ).astype(jnp.float32),
        lax.psum_scatter(
            partial_sums[1].astype(jnp.bfloat16), FSDP, scatter_dimension=0, tiled=True
        ).astype(jnp.float32),
        lax.psum_scatter(
            partial_sums[2].astype(jnp.bfloat16), FSDP, scatter_dimension=0, tiled=True
        ).astype(jnp.float32),
        lax.psum_scatter(
            partial_sums[3].astype(jnp.bfloat16), FSDP, scatter_dimension=0, tiled=True
        ).astype(jnp.float32),
        lax.psum_scatter(
            partial_sums[4].astype(jnp.bfloat16), FSDP, scatter_dimension=0, tiled=True
        ).astype(jnp.float32),
        lax.psum_scatter(
            partial_sums[5].astype(jnp.bfloat16), FSDP, scatter_dimension=0, tiled=True
        ).astype(jnp.float32),
        lax.psum_scatter(
            partial_sums[6].astype(jnp.bfloat16), FSDP, scatter_dimension=0, tiled=True
        ).astype(jnp.float32),
    )
    return (
        layer_out[None],
        grad_input[None],
        summed[0],
        summed[1],
        summed[2],
        summed[3],
        summed[4],
        summed[5],
        summed[6],
        grad_expert_in,
        grad_expert_out,
    )


def swap(a, flip):
    return lax.ppermute(a, FSDP, [(i, i ^ flip) for i in range(NX * NC)])


def fast_body(
    hidden,
    routes,
    attn_norm,
    ffn_norm,
    w_q,
    key_weight,
    value_weight,
    w_o,
    router,
    expert_in,
    expert_out,
    cotangent,
):
    tokens = hidden.shape[1]
    ctx = lax.axis_index(CTX)
    fsdp = lax.axis_index(FSDP)
    core = fsdp % NC
    rows = w_q.shape[0]
    quarter = expert_in.shape[1]
    kv_width = KEY_VALUE_HEADS * HEAD_SIZE
    q_width = QUERY_HEADS * HEAD_SIZE
    held = expert_in.shape[0] // NC
    bf = jnp.bfloat16
    f32 = jnp.float32
    positions = ctx * tokens + jnp.arange(tokens, dtype=jnp.int32)
    cosine_table, sine_table = (table[:, 0] for table in rope_tables(positions))
    cosine = jnp.concatenate([cosine_table] * 4, axis=1)
    sine = jnp.concatenate([-sine_table, sine_table] * 2, axis=1)
    contract_cols = (((1,), (1,)), ((), ()))
    wide = hidden[0].astype(f32)
    cot = cotangent[0]

    route = routes[0]
    indicator = (route[:, :, None] == jnp.arange(EXPERT_COUNT, dtype=jnp.int32)).astype(f32)
    part = rows // 3
    whole = (Z, Y, X, C)
    one, two, mine, *others = gather_weights(
        [w_q, key_weight, value_weight, w_o, router.T, attn_norm[None], ffn_norm[None]],
        [expert_in, expert_out],
        [
            Plan(0, (X, Z, Y, C), whole, rows=(2 * part, part)),
            Plan(1, (X, Z, Y, C), whole, rows=(part, part)),
            Plan(1, (X, Y, Z, C), whole, rows=(2 * part, part)),
            Plan(0, (Z, Y, X, C), whole, rows=(0, 2 * part)),
            Plan(1, (Z, Y, X, C), whole, rows=(0, part)),
        ],
        0,
    )
    parts = [mine, swap(mine, 2)] + [swap(other, 1) for other in others] + [swap(others[0], 3)]
    one = one.reshape(MODEL_WIDTH, -1)
    two = two.reshape(MODEL_WIDTH, -1)
    output_w = two[:, :MODEL_WIDTH]
    small = two[:, MODEL_WIDTH:]
    router_w = small[:, :EXPERT_COUNT]
    gains = lax.dot_general(
        jnp.eye(128, dtype=bf), small, contract_cols, preferred_element_type=f32
    )
    attn_gain, ffn_gain = gains[EXPERT_COUNT], gains[EXPERT_COUNT + 1]

    _, _, attention_input = rms_forward(wide, attn_gain)
    linear = jnp.dot(attention_input, one, preferred_element_type=f32)
    attention_output, log_sums, kv, cots, queries = attend(linear, cot, route, cosine, sine, 1)
    mixed = wide + jnp.dot(attention_output, output_w, preferred_element_type=f32)
    _, _, ffn_in = rms_forward(mixed, ffn_gain)
    logits = jnp.dot(ffn_in, router_w, preferred_element_type=f32)
    chosen = jnp.sum(indicator * logits[:, None, :], axis=-1)
    gates = jax.nn.softmax(chosen, axis=-1)
    gate_map = jnp.sum(indicator * gates[..., None], axis=1)
    payload = jnp.concatenate(
        [ffn_in, gate_map.astype(bf), jnp.zeros((tokens, 128 - EXPERT_COUNT), bf)], axis=1
    )
    gin, moe_part, *pieces = moe(payload, cots, parts + others[-1:], CAP, 2)
    across = [swap(pieces[j], j) for j in range(1, NX * NC)]
    gate_wide = jnp.concatenate([gate_map, jnp.zeros((tokens, 128 - EXPERT_COUNT), f32)], axis=1)
    back, layer_out, grad_mixed, grad_attn, left_small, right_small = attend_back(
        queries,
        gin,
        gate_wide,
        cot,
        ffn_gain.astype(f32)[None],
        attention_output,
        log_sums,
        kv,
        moe_part,
        two,
        mixed,
        cosine,
        sine,
        4,
    )
    *sums, grad_input = return_weights(
        [attention_input, attention_output, left_small],
        [back, grad_attn, right_small],
        one,
        hidden[0],
        attn_gain.astype(f32)[None],
        grad_mixed,
        EXPERT_COUNT,
        5,
    )
    grad_expert_in, grad_expert_out, *rest, first_gain, second_gain, layer_out, grad_input = last_outputs(
        [pieces[0]] + across,
        core,
        2 * EXPERT_HIDDEN,
        sums + [layer_out, grad_input],
        (q_width, kv_width, kv_width, MODEL_WIDTH, EXPERT_COUNT),
    )
    return (
        layer_out[None],
        grad_input[None],
        first_gain.reshape(rows),
        second_gain.reshape(rows),
        *rest[:-1],
        rest[-1].T,
        grad_expert_in.reshape(NC * held, quarter, -1),
        grad_expert_out.reshape(NC * held, quarter, -1),
    )


def fast(*args):
    return fast_body(*args)


def solution(mesh):
    placed = (
        P(FSDP, CTX, None),
        P(FSDP, CTX, None),
        P((CTX, FSDP)),
        P((CTX, FSDP)),
        P((CTX, FSDP), None),
        P((CTX, FSDP), None),
        P((CTX, FSDP), None),
        P((CTX, FSDP), None),
        P((CTX, FSDP), None),
        P(CTX, FSDP, None),
        P(CTX, FSDP, None),
        P(FSDP, CTX, None),
    )
    small = mesh.shape[CTX] == NZ * NY and mesh.shape[FSDP] == NX * NC
    return jax.shard_map(
        fast if small else local,
        mesh=mesh,
        in_specs=placed,
        out_specs=(
            P(FSDP, CTX, None),
            P(FSDP, CTX, None),
            P((CTX, FSDP)),
            P((CTX, FSDP)),
            P((CTX, FSDP), None),
            P((CTX, FSDP), None),
            P((CTX, FSDP), None),
            P((CTX, FSDP), None),
            P((CTX, FSDP), None),
            P(CTX, FSDP, None),
            P(CTX, FSDP, None),
        ),
        check_vma=False,
    )
```

```python
import functools
import itertools

import jax
import jax.numpy as jnp
from jax import lax
from jax.experimental import pallas as pl
from jax.experimental.pallas import tpu as pltpu
from jax.sharding import PartitionSpec as P


NY = 2
NZ = 4
NX = 2
NC = 2
DEV = pl.DeviceIdType.MESH
CTX, FSDP = "ctx", "fsdp"
Z, Y, X, C = 0, 1, 2, 3
SIZES = {Z: NZ, Y: NY, X: NX, C: NC}
UP, DOWN = 4, 5


class Plan:
    def __init__(self, ref, order, index, rows=None, view=None):
        self.ref, self.order, self.index, self.rows, self.view = ref, order, index, rows, view
        self.blocks = 1
        for d in index:
            self.blocks *= SIZES[d]


class Place:
    def __init__(self):
        ctx = lax.axis_index(CTX)
        fsdp = lax.axis_index(FSDP)
        self.at = {Z: ctx // NY, Y: ctx % NY, X: fsdp // NC, C: fsdp % NC}
        z = self.at[Z]
        low = z < NZ // 2
        base = jnp.where(low, z, NZ - 1 - z)
        near = [base, 1 - base, jnp.int32(2), jnp.int32(3)]
        self.order = [z] + [jnp.where(low, k, NZ - 1 - k) for k in near[1:]]

    def device(self, dim, value):
        spot = dict(self.at)
        spot[dim] = value
        return (spot[Z] * NY + spot[Y], spot[X] * NC + spot[C])

    def across(self, dim):
        return self.device(dim, 1 - self.at[dim])

    def along(self, step):
        return self.device(Z, self.at[Z] + step)

    def coords(self, z_from, flips):
        spot = {d: (1 - self.at[d] if d in flips else self.at[d]) for d in (Y, X, C)}
        spot[Z] = z_from
        return spot


def flat_index(spot, dims):
    index = 0
    for d in dims:
        index = index * SIZES[d] + spot[d]
    return index


def subsets(dims):
    return [c for n in range(len(dims) + 1) for c in itertools.combinations(dims, n)]


def hail(place, dims, more=()):
    barrier = pltpu.get_barrier_semaphore()
    z = place.at[Z]
    count = jnp.int32(0)
    for d in dims:
        if d == Z:
            @pl.when(z > 0)
            def _():
                pl.semaphore_signal(barrier, inc=1, device_id=place.along(-1), device_id_type=DEV)

            @pl.when(z < NZ - 1)
            def _():
                pl.semaphore_signal(barrier, inc=1, device_id=place.along(1), device_id_type=DEV)

            count = count + jnp.where(z > 0, 1, 0) + jnp.where(z < NZ - 1, 1, 0)
        else:
            pl.semaphore_signal(barrier, inc=1, device_id=place.across(d), device_id_type=DEV)
            count = count + 1
    for device in more:
        pl.semaphore_signal(barrier, inc=1, device_id=device, device_id_type=DEV)
        count = count + 1
    return count


def meet(count):
    pl.semaphore_wait(pltpu.get_barrier_semaphore(), count)


def gather_events(order):
    pairs = [d for d in order if d != Z]
    events = [(k, f) for k in range(NZ) for f in subsets(pairs)]
    return sorted(events, key=lambda e: (e[0] + len(e[1]), len(e[1])))


def gather_sends(order, k, flips):
    z_at = order.index(Z)
    last = max([order.index(d) for d in flips] + ([z_at] if k > 0 else []) + [-1])
    out = []
    for position, d in enumerate(order):
        if position > last:
            out.extend([UP, DOWN] if d == Z else [d])
    if k > 0 and last == z_at:
        out.extend([UP, DOWN])
    return out


def gather_kernel(plans, *refs):
    w_q, w_k, w_v, w_o, router, first_gain, second_gain, first_w, second_w = refs[:9]
    outs, (mine, *others) = refs[9:11], refs[11:14]
    send_sem, recv_sem, own_sem, stage, load_sem, store_sem, pack_one, pack_two = refs[14:]
    ins = pack_one, pack_two
    place = Place()
    count_here = hail(place, (Z, Y, X, C))
    held = mine.shape[0]
    split = first_w.shape[2]
    loads = []
    for side in range(2):
        base = (place.at[C] if side == 0 else 1 - place.at[C]) * held
        for e in range(held):
            to = stage.at[side * held + e]
            for w, at in ((first_w, pl.ds(0, split)), (second_w, pl.ds(split, second_w.shape[2]))):
                loads.append(pltpu.make_async_copy(w.at[base + e], to.at[:, at], load_sem.at[len(loads)]))
    for copy in loads:
        copy.start()
    stores = [pltpu.make_async_copy(stage.at[pl.ds(0, held)], mine, store_sem.at[0])] + [
        pltpu.make_async_copy(stage.at[pl.ds(held + e, 1)], out, store_sem.at[1 + e]) for e, out in enumerate(others)
    ]
    at = 0
    for w in (w_q, w_k, w_v):
        pack_one[:, at : at + w.shape[1]] = w[...]
        at += w.shape[1]
    model = w_o.shape[1]
    rows = w_o.shape[0]
    pack_two[:, :model] = w_o[...]
    same = lax.broadcasted_iota(jnp.int32, (rows, rows), 0) == lax.broadcasted_iota(jnp.int32, (rows, rows), 1)
    upright = lambda gain: jnp.sum(jnp.where(same, gain[...].astype(jnp.float32), 0.0), axis=1, keepdims=True)
    lane = lax.broadcasted_iota(jnp.int32, (1, 128), 1)
    count = router.shape[0]
    small = jnp.where(lane == count, upright(first_gain), jnp.where(lane == count + 1, upright(second_gain), 0.0))
    pack_two[:, model:] = small.astype(pack_two.dtype)
    pack_two[:, model : model + count] = lax.dot_general(
        same.astype(jnp.float32).astype(router.dtype), router[...], (((1,), (1,)), ((), ())),
        preferred_element_type=jnp.float32,
    ).astype(pack_two.dtype)
    z = place.at[Z]
    meet(count_here)
    pending = []
    slot = 0
    queue = []
    for n, plan in enumerate(plans):
        for rank, event in enumerate(gather_events(plan.order)):
            queue.append((rank / len(gather_events(plan.order)), n, event))
    queue.sort(key=lambda q: (q[0], q[1]))
    bases = [sum(p.blocks for p in plans[:n]) for n in range(len(plans))]
    for turn_at, (_, n, (k, flips)) in enumerate(queue):
        if turn_at == len(queue) // 3:
            for copy in loads:
                copy.wait()
            for copy in stores:
                copy.start()
        plan = plans[n]
        src = ins[plan.ref]
        out = outs[plan.ref]
        rows = plan.rows
        z_from = place.order[k]
        spot = place.coords(z_from, flips)
        index = flat_index(spot, plan.index)
        own = k == 0 and not flips
        if plan.view is not None:
            target = plan.view(out, spot, rows)
            source = src.at[:, pl.ds(rows[0], rows[1])] if own else target
        else:
            target = out.at[index] if rows is None else out.at[index, pl.ds(rows[0], rows[1])]
            source = (src if rows is None else src.at[pl.ds(rows[0], rows[1])]) if own else target
        sem = recv_sem.at[bases[n] + index]
        if not own:
            pltpu.make_async_remote_copy(
                src_ref=target, dst_ref=target, send_sem=own_sem.at[0], recv_sem=sem,
                device_id=place.across(C), device_id_type=DEV,
            ).wait_recv()
        for way in gather_sends(plan.order, k, flips):
            if way in (UP, DOWN):
                step = 1 if way == UP else -1
                go = z < NZ - 1 if way == UP else z > 0
                if k > 0:
                    go = jnp.logical_and(go, z_from < z if way == UP else z_from > z)
                dest = place.device(Z, jnp.clip(z + step, 0, NZ - 1))
            else:
                go, dest = None, place.across(way)
            copy = pltpu.make_async_remote_copy(
                src_ref=source, dst_ref=target, send_sem=send_sem.at[slot], recv_sem=sem,
                device_id=dest, device_id_type=DEV,
            )
            slot += 1
            if go is None:
                copy.start()
            else:
                pl.when(go)(copy.start)
            pending.append((go, copy.wait_send))
        if own:
            copy = pltpu.make_async_copy(source, target, own_sem.at[1 + n])
            copy.start()
            pending.append((None, copy.wait))
    for copy in stores:
        copy.wait()
    for go, wait in pending:
        if go is None:
            wait()
        else:
            pl.when(go)(wait)


def gather_weights(weights, experts, plans, collective_id):
    sends = sum(len(gather_sends(p.order, k, f)) for p in plans for k, f in gather_events(p.order))
    rows = weights[0].shape[0]
    bf = weights[0].dtype
    widths = [sum(w.shape[1] for w in weights[:3]), weights[3].shape[1] + 128]
    held = experts[0].shape[0] // NC
    pack = (experts[0].shape[1], experts[0].shape[2] + experts[1].shape[2])
    apart = pl.BlockSpec(memory_space=pl.ANY)
    dma = pltpu.SemaphoreType.DMA
    return pl.pallas_call(
        functools.partial(gather_kernel, plans),
        out_shape=[jax.ShapeDtypeStruct((plans[0].blocks, rows, w), bf) for w in widths]
        + [jax.ShapeDtypeStruct((n,) + pack, bf) for n in [held] + [1] * held],
        in_specs=[pl.BlockSpec(memory_space=pltpu.VMEM)] * len(weights) + [apart] * 2,
        out_specs=[apart] * (3 + held),
        scratch_shapes=[
            dma((sends,)),
            dma((sum(p.blocks for p in plans),)),
            dma((1 + len(plans),)),
            pltpu.VMEM((NC * held,) + pack, bf),
            dma((2 * NC * held,)),
            dma((1 + held,)),
        ]
        + [pltpu.VMEM((rows, w), bf) for w in widths],
        compiler_params=pltpu.CompilerParams(collective_id=collective_id, has_side_effects=True),
        name="gather_weights",
    )(*weights, *experts)


def add_into(acc, other):
    acc[...] = (acc[...].astype(jnp.float32) + other[...].astype(jnp.float32)).astype(acc.dtype)


class Gather:
    def __init__(self, place, plan, src, out, send_sem, recv_sem, spare_sem, slot, base):
        self.place, self.plan, self.src, self.out = place, plan, src, out
        self.send_sem, self.recv_sem, self.spare_sem = send_sem, recv_sem, spare_sem
        self.slot, self.base = slot, base
        self.pending = []

    @staticmethod
    def sends(plan):
        return sum(len(gather_sends(plan.order, k, f)) for k, f in gather_events(plan.order))

    def goes(self, way, k):
        z, z_from = self.place.at[Z], self.place.order[k]
        if way == UP:
            return z < NZ - 1 if k == 0 else jnp.logical_and(z < NZ - 1, z_from < z)
        return z > 0 if k == 0 else jnp.logical_and(z > 0, z_from > z)

    def part(self, ref):
        rows = self.plan.rows
        return ref if rows is None else ref.at[pl.ds(rows[0], rows[1])]

    def step(self, k, flips):
        place, plan = self.place, self.plan
        index = flat_index(place.coords(place.order[k], flips), plan.index)
        target = self.part(self.out.at[index])
        sem = self.recv_sem.at[self.base + index]
        source = target
        if k == 0 and not flips:
            source = self.part(self.src)
        else:
            pltpu.make_async_remote_copy(
                src_ref=target, dst_ref=target, send_sem=self.spare_sem, recv_sem=sem,
                device_id=place.across(C), device_id_type=DEV,
            ).wait_recv()
        for way in gather_sends(plan.order, k, flips):
            if way in (UP, DOWN):
                dest = place.device(Z, jnp.clip(place.at[Z] + (1 if way == UP else -1), 0, NZ - 1))
            else:
                dest = place.across(way)
            copy = pltpu.make_async_remote_copy(
                src_ref=source, dst_ref=target, send_sem=self.send_sem.at[self.slot], recv_sem=sem,
                device_id=dest, device_id_type=DEV,
            )
            if way in (UP, DOWN):
                pl.when(self.goes(way, k))(copy.start)
            else:
                copy.start()
            self.pending.append((way, k, self.slot))
            self.slot += 1

    def finish(self):
        for way, k, slot in self.pending:
            block = self.part(self.src)
            copy = pltpu.make_async_remote_copy(
                src_ref=block, dst_ref=block, send_sem=self.send_sem.at[slot], recv_sem=self.spare_sem,
                device_id=self.place.across(C), device_id_type=DEV,
            )
            if way in (UP, DOWN):
                pl.when(self.goes(way, k))(copy.wait_send)
            else:
                copy.wait_send()


class Reduce:
    def __init__(self, place, plan, held, levels, chain, send_sem, recv_sem, spare_sem):
        self.place, self.plan, self.held, self.levels, self.chain = place, plan, held, levels, chain
        self.send_sem, self.recv_sem, self.spare_sem = send_sem, recv_sem, spare_sem
        self.order, self.chain_at, self.kept, counts = Reduce.shape(plan)
        self.base = [sum(counts[:p]) for p in range(len(counts))]
        self.slot = 0

    @staticmethod
    def shape(plan):
        order = plan.order if Z in plan.order else plan.order + (Z,)
        at = order.index(Z)
        kept = [subsets(tuple(d for d in order[p + 1 :] if d != Z)) for p in range(len(order))]
        times = [NZ if p < at else NZ + 1 if p == at else 1 for p in range(len(order))]
        return order, at, kept, [n * len(f) for n, f in zip(times, kept)]

    @staticmethod
    def counts(plan):
        _, at, kept, counts = Reduce.shape(plan)
        buffers = counts[:at] + counts[at + 1 :] + [counts[at]]
        return buffers, sum(counts) - 2 * len(kept[at]), sum(counts)

    def level_of(self, p):
        return self.levels[p if p < self.chain_at else p - 1]

    def push(self, source, target, sem, dest):
        copy = pltpu.make_async_remote_copy(
            src_ref=source, dst_ref=target, send_sem=self.send_sem.at[self.slot], recv_sem=sem,
            device_id=dest, device_id_type=DEV,
        )
        self.slot += 1
        copy.start()

    def arrived(self, target, sem):
        pltpu.make_async_remote_copy(
            src_ref=target, dst_ref=target, send_sem=self.spare_sem, recv_sem=sem,
            device_id=self.place.across(C), device_id_type=DEV,
        ).wait_recv()

    def block(self, k, flips):
        return self.held.at[flat_index(self.place.coords(self.place.order[k], flips), self.plan.index)]

    def spot(self, p, k, flips):
        at = self.kept[p].index(flips)
        return at if p > self.chain_at else self.place.order[k] * len(self.kept[p]) + at

    def send(self, p, k, flips):
        dim = self.order[p]
        spot = self.spot(p, k, tuple(d for d in flips if d != dim))
        self.push(
            self.block(k, flips), self.level_of(p).at[spot],
            self.recv_sem.at[self.base[p] + spot], self.place.across(dim),
        )

    def first(self, k):
        for f in self.kept[0]:
            self.send(0, k, (self.order[0],) + f)

    def forward(self, p, k, flips):
        later = p + 1
        if later < len(self.order) and self.order[later] in flips:
            self.send(later, k, flips)

    def level(self, p, k):
        for f in sorted(self.kept[p], key=lambda f: -len(f)):
            spot = self.spot(p, k, f)
            self.arrived(self.level_of(p).at[spot], self.recv_sem.at[self.base[p] + spot])
            add_into(self.block(k, f), self.level_of(p).at[spot])
            self.forward(p, k, f)

    def link(self, spot, n):
        at = spot * len(self.kept[self.chain_at]) + n
        return self.chain.at[at], self.recv_sem.at[self.base[self.chain_at] + at]

    def along(self, k):
        z = self.place.at[Z]
        dest = self.place.order[k]
        up = dest > z
        for n, f in enumerate(self.kept[self.chain_at]):
            mine = self.block(k, f)
            target, sem = self.link(dest + jnp.where(up, 1, 0), n)

            @pl.when(jnp.where(up, z > 0, z < NZ - 1))
            def _():
                self.arrived(target, sem)
                add_into(mine, target)

            self.push(mine, target, sem, self.place.along(jnp.where(up, 1, -1)))

    def settle(self):
        z = self.place.at[Z]
        kept = self.kept[self.chain_at]
        for f in sorted(kept, key=lambda f: -len(f)):
            mine = self.block(0, f)
            for go, spot in ((z > 0, z + 1), (z < NZ - 1, z)):
                target, sem = self.link(spot, kept.index(f))

                @pl.when(go)
                def _():
                    self.arrived(target, sem)
                    add_into(mine, target)

            self.forward(self.chain_at, 0, f)

    def last(self, out, base=None):
        if self.chain_at == len(self.order) - 1:
            self.settle()
        total = self.block(0, ())[...].astype(jnp.float32)
        if base is not None:
            total = base[...] + total
        out[...] = total.astype(out.dtype)

    def at_time(self, t):
        far = list(reversed(range(NZ)))
        at = self.chain_at
        out = [functools.partial(self.level, p, far[t - p]) for p in range(at) if 0 <= t - p < NZ]
        if 0 <= t - at < NZ - 1:
            out.append(functools.partial(self.along, far[t - at]))
        if t - at == NZ - 1 and at < len(self.order) - 1:
            out.append(self.settle)
        out += [functools.partial(self.level, p, 0) for p in range(at + 1, len(self.order)) if t == NZ - 1 + p]
        return out

    def steps(self):
        return [step for t in range(NZ + len(self.order)) for step in self.at_time(t)]

    def finish(self):
        block = self.level_of(0).at[0]
        for slot in range(self.slot):
            pltpu.make_async_remote_copy(
                src_ref=block, dst_ref=block, send_sem=self.send_sem.at[slot], recv_sem=self.spare_sem,
                device_id=self.place.across(C), device_id_type=DEV,
            ).wait_send()


def tile_up(n, m):
    return (n + m - 1) // m * m


def columns_of(width, chunk=512):
    return [(i, min(chunk, width - i)) for i in range(0, width, chunk)]


def moe_kernel(plans, back, width, hidden, cap, *refs):
    payload, cots, w_own, w_x, w_core, w_core_last, w_both, w_send = refs[:8]
    gin_out, part_out = refs[8:10]
    grads = refs[10:14]
    (
        seen, cot_seen, weights, taken, cot_taken, rows_buf, scaled, grad_act, pick, stage,
        lvl_b0, lvl_b1, chain_b, lvl_c0, lvl_c1, chain_c,
        send_sem, recv_sem, spare_sem, send_b, recv_b, send_c, recv_c, load_sem, store_sem, part_sem, piece_sem,
    ) = refs[14:]
    bf, f32 = jnp.bfloat16, jnp.float32
    place = Place()
    count = payload.shape[0]
    pair = 2 * cap
    wide = width + 128
    quarter = width // (NX * NC)
    half = NZ * pair
    lanes = pick.shape[2]
    held = weights.shape[0]
    fsdp = place.at[X] * NC + place.at[C]
    first = (((place.at[Z] * NY + place.at[Y]) * NC) + place.at[C]) * held

    there = (place.at[Z] * NY + place.at[Y], (1 - place.at[X]) * NC + 1 - place.at[C])
    count_here = hail(place, (Z, Y, C), (there,))
    loads = []
    rows_of = lambda owner: pl.ds(pl.multiple_of(owner * quarter, quarter), quarter)
    sources = [(w_own, e, e, 0) for e in range(held)] + [(w_x, e, e, 2) for e in range(held)]
    sources += [(w_core, 0, 0, 1), (w_core_last, 0, held - 1, 1), (w_both, 0, 0, 3)]
    for ref, at, e, j in sources:
        loads.append(pltpu.make_async_copy(ref.at[at], weights.at[e, rows_of(fsdp ^ j)], load_sem.at[len(loads)]))
    piece = pltpu.make_async_remote_copy(
        src_ref=w_send.at[0], dst_ref=weights.at[held - 1, rows_of(fsdp)],
        send_sem=piece_sem.at[0], recv_sem=piece_sem.at[1], device_id=there, device_id_type=DEV,
    )
    base_of = lambda h, k: (jnp.where(h == 0, place.at[C], 1 - place.at[C]) * NZ + place.order[k]) * NY
    cot_loads = {}
    for k in range(NZ):
        for h in range(2):
            at = pl.ds(base_of(h, k), NY)
            cot_loads[(h, k)] = pltpu.make_async_copy(cots.at[at], cot_seen.at[at], load_sem.at[len(loads) + len(cot_loads)])

    meet(count_here)
    piece.start()
    ways = []
    send_at = 0
    for n, plan in enumerate(plans):
        ways.append(Gather(place, plan, payload, seen, send_sem, recv_sem, spare_sem, send_at, n * plan.blocks))
        send_at += Gather.sends(plan)
    for way in ways:
        way.step(0, ())
    for key in cot_loads:
        cot_loads[key].start()
    for copy in loads:
        copy.start()
    seen[flat_index(place.at, plans[0].index)] = payload[...]

    row_id = lax.broadcasted_iota(jnp.int32, (NY * count, NY * count), 0)
    col_id = lax.broadcasted_iota(jnp.int32, (NY * count, NY * count), 1)
    earlier = jnp.logical_and(col_id < row_id, col_id // count == row_id // count).astype(bf)
    lane_id = lax.broadcasted_iota(jnp.int32, (1, 128), 1)
    here = [(lane_id == first + e).astype(f32) for e in range(held)]
    pick_lane = lax.broadcasted_iota(jnp.int32, (NY * count, lanes), 1).astype(f32)
    y_shift = (lax.broadcasted_iota(jnp.int32, (NY * count, 1), 0) // count * cap).astype(f32)

    row_of = lambda h, k: (k * NC + h) * pair

    def dispatch(source, target, h, k, cols):
        at = pl.ds(base_of(h, k), NY)
        r = row_of(h, k)
        for c0, cn in cols:
            block = source[at, :, c0 : c0 + cn].reshape(NY * count, cn)
            got = lax.dot_general(
                pick[h * NZ + k], block, (((0,), (0,)), ((), ())), preferred_element_type=f32
            ).astype(bf)
            for e in range(held):
                target[e, r : r + pair, c0 : c0 + cn] = got[e * pair : (e + 1) * pair]

    def cot_chunk(h, k):
        cot_loads[(h, k)].wait()
        at = pl.ds(base_of(h, k), NY)
        chosen = cot_seen[at, :, width:wide].reshape(NY * count, 128)
        before = jnp.dot(earlier, chosen, preferred_element_type=f32)
        picked = None
        for e in range(held):
            is_here = jnp.sum(chosen.astype(f32) * here[e], axis=1, keepdims=True)
            slot = jnp.sum(before * here[e], axis=1, keepdims=True) + y_shift + e * pair
            target = jnp.where(is_here > 0.5, slot, -1.0)
            hit = pick_lane == target
            picked = hit if picked is None else jnp.logical_or(picked, hit)
        pick[h * NZ + k] = picked.astype(f32).astype(bf)
        dispatch(cot_seen, cot_taken, h, k, columns_of(width))

    def hidden_chunk(h, e, n, tile):
        rows = pl.ds(h * half, half)
        tokens_in = taken[e, rows, :width]
        gate = jnp.sum(taken[e, rows, width:wide].astype(f32) * here[e], axis=1, keepdims=True)
        col = n * tile
        g = jnp.dot(tokens_in, weights[e, :, col : col + tile], preferred_element_type=f32)
        u = jnp.dot(tokens_in, weights[e, :, hidden + col : hidden + col + tile], preferred_element_type=f32)
        raw = jnp.dot(
            cot_taken[e, rows, :], weights[e, :, 2 * hidden + col : 2 * hidden + col + tile], preferred_element_type=f32
        )
        s = jax.nn.sigmoid(g)
        gs = g * s
        inner = gs * u
        scaled[e, rows, col : col + tile] = (inner * gate).astype(bf)
        grad_inner = raw * gate
        grad_act[e, rows, col : col + tile] = (grad_inner * u * s * (1.0 + g * (1.0 - s))).astype(bf)
        grad_act[e, rows, hidden + col : hidden + col + tile] = (grad_inner * gs).astype(bf)
        return jnp.sum(raw * inner, axis=1, keepdims=True)

    tile = min(256, hidden)
    found = {}

    def hidden_step(h, e, n):
        got = hidden_chunk(h, e, n, tile)
        found[(h, e)] = got if n == 0 else found[(h, e)] + got
        if n == hidden // tile - 1:
            gate_grad = found.pop((h, e))
            high = gate_grad.astype(bf).astype(f32)
            there = pl.ds(h * half, half)
            apart = (lane_id == EXPERT_COUNT + first + e).astype(f32)
            rows_buf[e, there, width:wide] = (high * here[e] + (gate_grad - high) * apart).astype(bf)

    def hidden_steps(h):
        return [functools.partial(hidden_step, h, e, n) for e in range(held) for n in range(hidden // tile)]

    def project(h, e, left, weight_cols):
        rows = pl.ds(h * half, half)
        lo, n = weight_cols
        for c0, cn in columns_of(width):
            rows_buf[e, rows, c0 : c0 + cn] = lax.dot_general(
                left[e, rows, :], weights[e, c0 : c0 + cn, lo : lo + n], (((1,), (1,)), ((), ())), preferred_element_type=f32
            ).astype(bf)

    def combine(target, h, k, cols):
        at = pl.ds(base_of(h, k), NY)
        r = row_of(h, k)
        for c0, cn in cols:
            parts = [rows_buf[e, r : r + pair, c0 : c0 + cn] for e in range(held)]
            if lanes > held * pair:
                parts.append(jnp.zeros((lanes - held * pair, cn), bf))
            got = jnp.dot(pick[h * NZ + k], jnp.concatenate(parts, axis=0), preferred_element_type=f32)
            target[at, :, c0 : c0 + cn] = got.astype(bf).reshape(NY, count, cn)

    stores = []

    def weight_grad(e, j):
        rows = pl.ds(pl.multiple_of((fsdp ^ j) * quarter, 128), quarter)
        slot = len(stores) % 2
        if len(stores) >= 2:
            stores[-2].wait()
        for c0, cn in columns_of(2 * hidden):
            stage[slot, :, c0 : c0 + cn] = lax.dot_general(
                taken[e, :, rows], grad_act[e, :, c0 : c0 + cn], (((0,), (0,)), ((), ())), preferred_element_type=f32
            ).astype(bf)
        stage[slot, :, 2 * hidden :] = lax.dot_general(
            cot_taken[e, :, rows], scaled[e], (((0,), (0,)), ((), ())), preferred_element_type=f32
        ).astype(bf)
        copy = pltpu.make_async_copy(stage.at[slot], grads[j].at[e], store_sem.at[len(stores)])
        copy.start()
        stores.append(copy)

    work = [functools.partial(cot_chunk, h, k) for h in range(NC) for k in range(NZ)]
    all_cols = columns_of(width) + [(width, 128)]
    ready = {(h, k): 0 for h in range(NC) for k in range(NZ)}
    ready[(0, 0)] = 1
    near_begun = False

    def wait_weights():
        for copy in loads:
            copy.wait()
        arrived = weights.at[held - 1, rows_of(fsdp ^ 3)]
        pltpu.make_async_remote_copy(
            src_ref=arrived, dst_ref=arrived, send_sem=piece_sem.at[0], recv_sem=piece_sem.at[1],
            device_id=there, device_id_type=DEV,
        ).wait_recv()

    for k, flips in gather_events(plans[0].order)[1:]:
        for way in ways:
            way.step(k, flips)
        key = (1 if C in flips else 0, k)
        ready[key] += 1
        if ready[key] == NY:
            work.append(functools.partial(dispatch, seen, taken, *key, all_cols))
            if all(ready[(g, n)] == NY for g in range(NC) for n in range(NZ // 2)) and not near_begun:
                near_begun = True
                work += [wait_weights] + hidden_steps(0)
        for _ in range(min(len(work), 1 if k < NZ - 1 else 2)):
            work.pop(0)()
    for chunk in work:
        chunk()
    for chunk in hidden_steps(1):
        chunk()

    far = list(reversed(range(NZ)))
    spare = spare_sem
    cut = lvl_b0.shape[2]
    in_ways = [
        Reduce(place, back[0], cot_seen.at[:, :, pl.ds(0, cut)], (lvl_b0, lvl_b1), chain_b, send_b, recv_b, spare),
        Reduce(place, back[1], cot_seen.at[:, :, pl.ds(cut, wide - cut)], (lvl_c0, lvl_c1), chain_c, send_c, recv_c, spare),
    ]
    in_steps = [step for t in range(NZ + 3) for way in in_ways for step in way.at_time(t)]
    for e in range(held):
        project(1, e, grad_act, (0, 2 * hidden))
    for k in far[: NZ // 2]:
        combine(cot_seen, 1, k, all_cols)
        for way in in_ways:
            way.first(k)
    for k in far[: NZ // 2]:
        combine(cot_seen, 0, k, all_cols)
    in_steps.pop(0)()
    in_steps.pop(0)()
    for e in range(held):
        project(0, e, grad_act, (0, 2 * hidden))
    in_steps.pop(0)()
    for k in far[NZ // 2 :]:
        combine(cot_seen, 1, k, all_cols)
        for way in in_ways:
            way.first(k)
    for _ in range(3):
        in_steps.pop(0)()
    for k in far[NZ // 2 :]:
        combine(cot_seen, 0, k, all_cols)
    for way in in_ways:
        way.level(0, 1)
        way.level(0, 0)
    done = ((0, 1), (0, 0))
    in_steps = [step for step in in_steps if not isinstance(step, functools.partial) or step.args not in done]
    for way in ways:
        way.finish()
    part_copies = []
    work = []

    def out_part(h, k):
        combine(seen, h, k, columns_of(width))
        at = pl.ds(base_of(h, k), NY)
        copy = pltpu.make_async_copy(seen.at[at, :, pl.ds(0, width)], part_out.at[at], part_sem.at[len(part_copies)])
        copy.start()
        part_copies.append(copy)

    for n in range(2):
        for e in range(held):
            work.append(functools.partial(project, n, e, scaled, (2 * hidden, hidden)))
        for k in range(n * NZ // 2, (n + 1) * NZ // 2):
            for h in range(NC):
                work.append(functools.partial(out_part, h, k))
    work += [functools.partial(weight_grad, e, j) for j in reversed(range(NX * NC)) for e in range(held)]
    while in_steps or work:
        if in_steps:
            in_steps.pop(0)()
        for _ in range(2):
            if work:
                work.pop(0)()
    in_ways[0].last(gin_out.at[:, pl.ds(0, cut)])
    in_ways[1].last(gin_out.at[:, pl.ds(cut, wide - cut)])
    piece.wait_send()
    for copy in stores[-2:] + part_copies:
        copy.wait()
    for way in in_ways:
        way.finish()


def moe(payload, cots, parts, cap, collective_id):
    count, wide = payload.shape
    width = wide - 128
    held, quarter, columns = parts[0].shape
    hidden = columns // 3
    cut = count * 3 // 4
    plans = [
        Plan(0, (Z, Y, C), (C, Z, Y), rows=(0, cut)),
        Plan(0, (Y, Z, C), (C, Z, Y), rows=(cut, count - cut)),
    ]
    back = [Plan(0, (C, Y, Z), (C, Z, Y)), Plan(0, (C, Z, Y), (C, Z, Y))]
    widths = (wide - wide // 4 // 128 * 128, wide // 4 // 128 * 128)
    blocks = NC * NZ * NY
    pair = NY * cap
    rows = blocks // NY * pair
    lanes = tile_up(held * pair, 128)
    bf, f32 = jnp.bfloat16, jnp.float32
    whole = pl.BlockSpec(memory_space=pltpu.VMEM)
    apart = pl.BlockSpec(memory_space=pl.ANY)
    dma = pltpu.SemaphoreType.DMA
    return pl.pallas_call(
        functools.partial(moe_kernel, plans, back, width, hidden, cap),
        out_shape=[
            jax.ShapeDtypeStruct((count, wide), f32),
            jax.ShapeDtypeStruct((blocks, count, width), bf),
        ]
        + [jax.ShapeDtypeStruct((held, quarter, columns), bf)] * (NX * NC),
        in_specs=[whole] + [apart] * 7,
        out_specs=[whole] + [apart] * (1 + NX * NC),
        scratch_shapes=[
            pltpu.VMEM((blocks, count, wide), bf),
            pltpu.VMEM((blocks, count, wide), bf),
            pltpu.VMEM((held, NX * NC * quarter, columns), bf),
            pltpu.VMEM((held, rows, wide), bf),
            pltpu.VMEM((held, rows, width), bf),
            pltpu.VMEM((held, rows, wide), bf),
            pltpu.VMEM((held, rows, hidden), bf),
            pltpu.VMEM((held, rows, 2 * hidden), bf),
            pltpu.VMEM((blocks // NY, NY * count, lanes), bf),
            pltpu.VMEM((2, quarter, columns), bf),
        ]
        + [pltpu.VMEM((n, count, w), bf) for p, w in zip(back, widths) for n in Reduce.counts(p)[0]]
        + [
            dma((sum(Gather.sends(p) for p in plans),)),
            dma((sum(p.blocks for p in plans),)),
            dma(()),
            *[dma((n,)) for p in back for n in Reduce.counts(p)[1:]],
            dma((held * NX * NC + blocks // NY,)),
            dma((held * NX * NC,)),
            dma((blocks // NY,)),
            dma((2,)),
        ],
        compiler_params=pltpu.CompilerParams(
            collective_id=collective_id, has_side_effects=True, vmem_limit_bytes=67043328
        ),
        name="experts",
    )(payload, cots, *parts)


def weights_kernel(plans, gain_at, *refs):
    left_one, right_one, left_two, right_two, left_small, right_small = refs[:6]
    matrix_in, hidden, gain, grad_mixed = refs[6:10]
    n_ways = len(plans)
    outs, grad_input = refs[10:13], refs[13]
    held = refs[14 : 14 + n_ways]
    buffers, refs = refs[14 + n_ways : 14 + 5 * n_ways], refs[14 + 5 * n_ways :]
    matrix, grad_in, halves = refs[:3]
    sems, (spare, matrix_sem) = refs[3 : 3 + 2 * n_ways], refs[3 + 2 * n_ways :]
    bf, f32 = jnp.bfloat16, jnp.float32
    place = Place()
    far = list(reversed(range(NZ)))
    fetch = pltpu.make_async_copy(matrix_in, matrix, matrix_sem)
    fetch.start()
    count_here = hail(place, (Z, Y, X, C))
    *ways, small_way = [
        Reduce(place, plan, held[n], buffers[4 * n : 4 * n + 3], buffers[4 * n + 3], sems[2 * n], sems[2 * n + 1], spare)
        for n, plan in enumerate(plans)
    ]
    group = NY * NX * NC
    rows = group * held[0].shape[1]

    def products(pairs, target, k, shift=0):
        at = pl.ds(pl.multiple_of(place.order[k] * rows, 128), rows)
        for c0, cn in columns_of(target.shape[2]):
            got = sum(
                lax.dot_general(
                    left[:, at], right[:, shift + c0 : shift + c0 + cn], (((0,), (0,)), ((), ())),
                    preferred_element_type=f32,
                )
                for left, right in pairs
            )
            target[pl.ds(place.order[k] * group, group), :, c0 : c0 + cn] = got.astype(target.dtype).reshape(
                group, rows // group, cn
            )

    def late(some, t):
        for way in some:
            for step in way.at_time(t):
                if not (isinstance(step, functools.partial) and len(step.args) == 2 and step.args[0] == 0):
                    step()

    for t in range(NZ):
        for n, way in enumerate(ways):
            width = held[n].shape[2]
            products([(left_one, right_one) if n < 2 else (left_two, right_two)], held[n], far[t], n % 2 * width)
            if t == n == 0:
                meet(count_here)
            way.first(far[t])
        if t > 0:
            for way in ways:
                way.level(0, far[t - 1])
    for way in ways:
        way.level(0, far[-1])
    fetch.wait()
    for c0, cn in columns_of(grad_in.shape[1]):
        grad_in[:, c0 : c0 + cn] = lax.dot_general(
            right_one[...], matrix[c0 : c0 + cn], (((1,), (1,)), ((), ())), preferred_element_type=f32
        )
    count = grad_in.shape[0]
    wide = hidden[...].astype(f32)
    inverse = lax.rsqrt(jnp.mean(wide * wide, axis=1, keepdims=True) + norm_eps)
    unit = wide * inverse
    factor = grad_in[...] * unit
    high = factor.astype(bf)
    halves[:count] = high
    halves[count:] = (factor - high.astype(f32)).astype(bf)
    scaled = grad_in[...] * gain[...]
    mean = jnp.mean(scaled * unit, axis=1, keepdims=True)
    grad_input[...] = grad_mixed[...] + inverse * (scaled - unit * mean)
    column = (lax.broadcasted_iota(jnp.int32, (2 * count, 128), 1) == gain_at).astype(f32).astype(bf)
    for k in far:
        products([(left_small, right_small), (halves, column)], held[-1], k)
        small_way.first(k)
    for k in far:
        small_way.level(0, k)
    y_first, x_first, small = ways[:2], ways[2:], [small_way]
    for some, t in (
        (y_first, 1), (y_first, 2), (x_first, 1), (x_first, 2), (y_first, 3), (x_first, 3), (small, 1), (x_first, 4),
        (y_first, 4), (small, 2), (small, 3), (y_first, 5), (x_first, 5), (small, 4), (y_first, 6), (x_first, 6),
        (small, 5), (small, 6),
    ):
        late(some, t)
    for n, way in enumerate(ways):
        width = held[n].shape[2]
        way.last(outs[n // 2].at[:, pl.ds(n % 2 * width, width)])
    small_way.last(outs[2])
    for way in ways + [small_way]:
        way.finish()


def return_weights(lefts, rights, matrix, hidden, gain, grad_mixed, gain_at, collective_id):
    width = lefts[0].shape[1]
    rows = width // (NZ * NY * NX * NC)
    widths = [r.shape[1] for r in rights]
    whole = (Z, Y, X, C)
    orders = ((C, Y, Z, X), (C, Y, Z, X), (C, X, Z, Y), (C, X, Y, Z), (C, Y, X, Z))
    plans = [Plan(0, order, whole) for order in orders]
    parts = [widths[0] // 2] * 2 + [widths[1] // 2] * 2 + [widths[2]]
    bf, f32 = jnp.bfloat16, jnp.float32
    dma = pltpu.SemaphoreType.DMA
    vmem = pl.BlockSpec(memory_space=pltpu.VMEM)
    count = hidden.shape[0]
    return pl.pallas_call(
        functools.partial(weights_kernel, plans, gain_at),
        out_shape=[jax.ShapeDtypeStruct((rows, w), f32) for w in widths] + [jax.ShapeDtypeStruct(hidden.shape, f32)],
        in_specs=[vmem] * 6 + [pl.BlockSpec(memory_space=pl.ANY)] + [vmem] * 3,
        out_specs=[vmem] * 4,
        scratch_shapes=[pltpu.VMEM((plans[0].blocks, rows, w), bf) for w in parts]
        + [pltpu.VMEM((n, rows, w), bf) for p, w in zip(plans, parts) for n in Reduce.counts(p)[0]]
        + [pltpu.VMEM(matrix.shape, bf), pltpu.VMEM(hidden.shape, f32), pltpu.VMEM((2 * count, width), bf)]
        + [dma((n,)) for p in plans for n in Reduce.counts(p)[1:]]
        + [dma(()), dma(())],
        compiler_params=pltpu.CompilerParams(
            collective_id=collective_id, has_side_effects=True, vmem_limit_bytes=64 * 1024 * 1024
        ),
        name="return_weights",
    )(*[a for pair in zip(lefts, rights) for a in pair], matrix, hidden, gain, grad_mixed)


def turn(block, cosine, sine):
    lane = lax.broadcasted_iota(jnp.int32, (1, 128), 1)
    half = HEAD_SIZE // 2
    other = jnp.where(lane % HEAD_SIZE < half, pltpu.roll(block, 128 - half, 1), pltpu.roll(block, half, 1))
    return block * cosine + other * sine


def place_heads(read, target, count):
    group = QUERY_HEADS // KEY_VALUE_HEADS
    lane = lax.broadcasted_iota(jnp.int32, (1, 2 * HEAD_SIZE), 1)
    for pair in range(QUERY_HEADS // 2):
        both = read(pair)
        for h in (2 * pair, 2 * pair + 1):
            m, g = h // group, h % group
            block = both if h % 2 == m % 2 else pltpu.roll(both, HEAD_SIZE, 1)
            block = jnp.where(lane // HEAD_SIZE == m % 2, block, 0.0)
            target[m, g * count : (g + 1) * count] = block.astype(target.dtype)


def collect_heads(source, target, count, finish):
    group = QUERY_HEADS // KEY_VALUE_HEADS
    lane = lax.broadcasted_iota(jnp.int32, (1, 2 * HEAD_SIZE), 1)
    for pair in range(QUERY_HEADS // 2):
        sides = []
        for h in (2 * pair, 2 * pair + 1):
            m, g = h // group, h % group
            block = source[m, g * count : (g + 1) * count]
            sides.append(block if h % 2 == m % 2 else pltpu.roll(block, HEAD_SIZE, 1))
        both = finish(jnp.where(lane < HEAD_SIZE, *sides))
        target[:, pair * 128 : pair * 128 + 128] = both.astype(target.dtype)


class Scores:
    def __init__(self, place, queries, keys):
        self.queries, self.keys = queries, keys
        group = QUERY_HEADS // KEY_VALUE_HEADS
        count = keys.shape[1]
        self.total = keys.shape[0] * count
        row = lax.broadcasted_iota(jnp.int32, (group * count, 1), 0) % count
        self.position = row + (place.at[Z] * NY + place.at[Y]) * count
        self.column = lax.broadcasted_iota(jnp.int32, (1, self.total), 1)

    def pair(self, m, shift):
        at = pl.ds(pl.multiple_of(shift + m // 2 * 128, 128), 128)
        return self.keys[:, :, at].reshape(self.total, 128)

    def of(self, m, keys):
        found = lax.dot_general(
            self.queries[m], keys, (((1,), (1,)), ((), ())), preferred_element_type=jnp.float32
        )
        return jnp.where(self.column <= self.position, found * attn_scale, masked_logits)


def attend_kernel(
    plans, linear, cot, routes, cosine, sine, out, log_sums, kv_out, cots, placed, seen, own_kv, own_cots, raw, *sems
):
    send_kv, recv_kv, send_cot, recv_cot, spare, own_sem = sems
    place = Place()
    bf, f32 = jnp.bfloat16, jnp.float32
    count_here = hail(place, (Z, Y, C))
    count = linear.shape[0]
    width = KEY_VALUE_HEADS * HEAD_SIZE
    q_width = QUERY_HEADS * HEAD_SIZE
    for c0 in range(0, width, 128):
        block = linear[:, q_width + c0 : q_width + c0 + 128]
        own_kv[:, c0 : c0 + 128] = turn(block, cosine[...], sine[...]).astype(bf)
    own_kv[:, width:] = linear[:, q_width + width :].astype(bf)
    model = cot.shape[1]
    own_cots[:, :model] = cot[...].astype(bf)
    expert = lax.broadcasted_iota(jnp.int32, (1, 128), 1)
    routed = routes[:, 0:1] == expert
    for n in range(1, routes.shape[1]):
        routed = jnp.logical_or(routed, routes[:, n : n + 1] == expert)
    own_cots[:, model:] = routed.astype(f32).astype(bf)
    meet(count_here)
    kv_way = Gather(place, plans[0], own_kv, seen, send_kv, recv_kv, spare, 0, 0)
    cot_ways, at = [], 0
    for n, plan in enumerate(plans[1:]):
        cot_ways.append(Gather(place, plan, own_cots, cots, send_cot, recv_cot, spare, at, n * plan.blocks))
        at += Gather.sends(plan)
    kv_way.step(0, ())
    for way in cot_ways:
        way.step(0, ())
    mine = pltpu.make_async_copy(own_cots, cots.at[flat_index(place.at, plans[1].index)], own_sem.at[0])
    mine.start()
    seen[flat_index(place.at, plans[0].index)] = own_kv[...]
    place_heads(lambda pair: turn(linear[:, pair * 128 : pair * 128 + 128], cosine[...], sine[...]), placed, count)
    log_sums[...] = jnp.zeros(log_sums.shape, f32)
    early = [e for e in gather_events(plans[1].order)[1:]]
    kv_events = gather_events(plans[0].order)[1:]
    for k, flips in kv_events:
        kv_way.step(k, flips)
        if len(early) > 8:
            event = early.pop(0)
            for way in cot_ways:
                way.step(*event)
    keep = pltpu.make_async_copy(seen, kv_out, own_sem.at[1])
    keep.start()
    scores = Scores(place, placed, seen)
    lane = lax.broadcasted_iota(jnp.int32, (1, 128), 1)

    def head(m, carry):
        for i in range(KEY_VALUE_HEADS):
            if early:
                event = early.pop(0)

                @pl.when(m == i)
                def _():
                    for way in cot_ways:
                        way.step(*event)

        s = scores.of(m, scores.pair(m, 0))
        best = jnp.max(s, axis=1, keepdims=True)
        weights = jnp.exp(s - best)
        total = jnp.sum(weights, axis=1, keepdims=True)
        mixed = jnp.dot(weights.astype(bf), scores.pair(m, width), preferred_element_type=f32)
        raw[m] = mixed / total
        log_sums[...] = jnp.where(lane == m, best + jnp.log(total), log_sums[...])
        return carry

    lax.fori_loop(0, KEY_VALUE_HEADS, head, 0)
    collect_heads(raw, out, count, lambda block: block)
    keep.wait()
    mine.wait()
    kv_way.finish()
    for way in cot_ways:
        way.finish()


def attend(linear, cot, routes, cosine, sine, collective_id):
    count = linear.shape[0]
    kv_width = 2 * KEY_VALUE_HEADS * HEAD_SIZE
    cut = count * 3 // 4
    plans = [
        Plan(0, (Z, Y), (Z, Y)),
        Plan(1, (Z, Y, C), (C, Z, Y), rows=(0, cut)),
        Plan(1, (Y, Z, C), (C, Z, Y), rows=(cut, count - cut)),
    ]
    bf, f32 = jnp.bfloat16, jnp.float32
    group = QUERY_HEADS // KEY_VALUE_HEADS
    vmem = pl.BlockSpec(memory_space=pltpu.VMEM)
    apart = pl.BlockSpec(memory_space=pl.ANY)
    dma = pltpu.SemaphoreType.DMA
    kv_shape = (plans[0].blocks, count, kv_width)
    cot_shape = (count, cot.shape[1] + 128)
    heads = (KEY_VALUE_HEADS, group * count, 2 * HEAD_SIZE)
    return pl.pallas_call(
        functools.partial(attend_kernel, plans),
        out_shape=[
            jax.ShapeDtypeStruct((count, QUERY_HEADS * HEAD_SIZE), bf),
            jax.ShapeDtypeStruct((group * count, 128), f32),
            jax.ShapeDtypeStruct(kv_shape, bf),
            jax.ShapeDtypeStruct((plans[1].blocks,) + cot_shape, bf),
            jax.ShapeDtypeStruct(heads, bf),
        ],
        in_specs=[vmem] * 5,
        out_specs=[vmem, vmem, apart, apart, vmem],
        scratch_shapes=[
            pltpu.VMEM(kv_shape, bf),
            pltpu.VMEM((count, kv_width), bf),
            pltpu.VMEM(cot_shape, bf),
            pltpu.VMEM(heads, f32),
        ]
        + [
            dma((Gather.sends(plans[0]),)),
            dma((plans[0].blocks,)),
            dma((Gather.sends(plans[1]) + Gather.sends(plans[2]),)),
            dma((plans[1].blocks + plans[2].blocks,)),
            dma(()),
            dma((2,)),
        ],
        compiler_params=pltpu.CompilerParams(
            collective_id=collective_id, has_side_effects=True, vmem_limit_bytes=56 * 1024 * 1024
        ),
        name="attend",
    )(linear, cot, routes, cosine, sine)


def attend_back_kernel(plans, *refs):
    placed, gin, gate_map, cot, ffn_gain, outputs, log_sums, keys, part, w_o, mixed, cosine, sine = refs[:13]
    back, layer_out, grad_mixed, grad_attn, left_small, right_small = refs[13:19]
    kv_grad, grads_placed, raw, deltas, held, held_out, grads, matrix = refs[19:27]
    level, chain, v_level, v_chain, out_level, out_level_two, out_chain = refs[27:34]
    send_kv, recv_kv, send_v, recv_v, send_out, recv_out, spare, load_sem, matrix_sem = refs[34:]
    place = Place()
    bf, f32 = jnp.bfloat16, jnp.float32
    far = list(reversed(range(NZ)))
    loads = []
    for k in far:
        for h in (1 - place.at[C], place.at[C]):
            at = pl.ds((h * NZ + place.order[k]) * NY, NY)
            loads.append(pltpu.make_async_copy(part.at[at], held_out.at[at], load_sem.at[len(loads)]))
    for copy in loads:
        copy.start()
    fetch = pltpu.make_async_copy(w_o, matrix, matrix_sem)
    fetch.start()
    meet(hail(place, (Z, Y, C)))
    width = KEY_VALUE_HEADS * HEAD_SIZE
    k_way = Reduce(place, plans[0], held.at[:, :, pl.ds(0, width)], (level,), chain, send_kv, recv_kv, spare)
    v_way = Reduce(place, plans[1], held.at[:, :, pl.ds(width, width)], (v_level,), v_chain, send_v, recv_v, spare)
    out_way = Reduce(place, plans[2], held_out, (out_level, out_level_two), out_chain, send_out, recv_out, spare)
    for copy in loads:
        copy.wait()
    for k in far:
        out_way.first(k)
    count = grads.shape[0]
    fetch.wait()
    out_way.level(0, 3)
    out_way.level(0, 2)
    model = cot.shape[1]
    lane = lax.broadcasted_iota(jnp.int32, (1, 128), 1)
    halves = gin[:, model:]
    gate_grad = jnp.where(lane < EXPERT_COUNT, halves + pltpu.roll(halves, 128 - EXPERT_COUNT, 1), 0.0)
    weighted = jnp.sum(gate_map[...] * gate_grad, axis=1, keepdims=True)
    grad_logits = (gate_map[...] * (gate_grad - weighted)).astype(bf)
    over_cols = (((1,), (1,)), ((), ()))
    inverse = lax.rsqrt(jnp.mean(mixed[...] * mixed[...], axis=1, keepdims=True) + norm_eps)
    unit = mixed[...] * inverse
    grad_in = gin[:, :model] + lax.dot_general(
        grad_logits, matrix[:, model:], over_cols, preferred_element_type=f32
    )
    scaled = grad_in * ffn_gain[...]
    grad_mixed[...] = cot[...] + inverse * (scaled - unit * jnp.mean(scaled * unit, axis=1, keepdims=True))
    grad_attn[...] = grad_mixed[...].astype(bf)
    factor = grad_in * unit
    high = factor.astype(bf)
    left_small[:count] = (unit * ffn_gain[...]).astype(bf)
    left_small[count : 2 * count] = high
    left_small[2 * count :] = (factor - high.astype(f32)).astype(bf)
    right_small[:count] = grad_logits
    right_small[count:] = jnp.broadcast_to(jnp.where(lane == EXPERT_COUNT + 1, 1.0, 0.0), (2 * count, 128)).astype(bf)
    for c0, cn in columns_of(grads.shape[1]):
        grads[:, c0 : c0 + cn] = lax.dot_general(
            grad_attn[...], matrix[c0 : c0 + cn, :model], over_cols, preferred_element_type=f32
        ).astype(bf)
    out_way.level(0, 1)
    place_heads(lambda pair: grads[:, pair * 128 : pair * 128 + 128].astype(f32), grads_placed, count)
    group = QUERY_HEADS // KEY_VALUE_HEADS
    lane = lax.broadcasted_iota(jnp.int32, (1, 128), 1)
    for g in range(group):
        found = jnp.zeros((count, 128), f32)
        for m in range(KEY_VALUE_HEADS):
            h = m * group + g
            at = slice(h // 2 * 128, h // 2 * 128 + 128)
            both = grads[:, at].astype(f32) * outputs[:, at].astype(f32)
            delta = jnp.sum(jnp.where(lane // HEAD_SIZE == h % 2, both, 0.0), axis=1, keepdims=True)
            found = jnp.where(lane == m, delta, found)
        deltas[g * count : (g + 1) * count] = found
    scores = Scores(place, placed, keys)
    blocks = keys.shape[0]
    turns = KEY_VALUE_HEADS // 2
    early = [[(out_way.level, 1, 3)], [(out_way.along, 3), (out_way.level, 1, 2)], [(out_way.along, 2)], []]

    def pair(p, carry):
        for i in range(turns):

            @pl.when(p == i)
            def _():
                for step, *at in early[i]:
                    step(*at)

        key_sum = value_sum = None
        for side in range(2):
            m = 2 * p + side
            k_pair, v_pair = scores.pair(m, 0), scores.pair(m, width)
            of_head = lambda ref: jnp.sum(jnp.where(lane == m, ref[...], 0.0), axis=1, keepdims=True)
            weights = jnp.exp(scores.of(m, k_pair) - of_head(log_sums))
            grad = grads_placed[m]
            grad_probs = lax.dot_general(grad, v_pair, (((1,), (1,)), ((), ())), preferred_element_type=f32)
            grad_scores = (weights * (grad_probs - of_head(deltas))).astype(bf)
            raw[m] = attn_scale * jnp.dot(grad_scores, k_pair, preferred_element_type=f32)
            over_rows = (((0,), (0,)), ((), ()))
            key_part = lax.dot_general(grad_scores, placed[m], over_rows, preferred_element_type=f32)
            value_part = lax.dot_general(weights.astype(bf), grad, over_rows, preferred_element_type=f32)
            key_sum = key_part if key_sum is None else key_sum + key_part
            value_sum = value_part if value_sum is None else value_sum + value_part
        at = pl.multiple_of(p * 128, 128)
        held[:, :, pl.ds(at, 128)] = (attn_scale * key_sum).astype(bf).reshape(blocks, count, 128)
        at = pl.multiple_of(width + p * 128, 128)
        held[:, :, pl.ds(at, 128)] = value_sum.astype(bf).reshape(blocks, count, 128)
        return carry

    lax.fori_loop(0, turns, pair, 0)
    for k in far:
        k_way.first(k)
    v_way.along(3)
    out_way.level(0, 0)
    collect_heads(raw, back, count, lambda block: turn(block, cosine[...], -sine[...]))
    k_way.level(0, 3)
    v_way.along(2)
    k_way.level(0, 2)
    k_way.along(3)
    v_way.along(1)
    k_way.level(0, 1)
    k_way.along(2)
    v_way.settle()
    k_way.level(0, 0)
    k_way.along(1)
    k_way.last(kv_grad.at[:, pl.ds(0, width)])
    v_way.level(1, 0)
    v_way.last(kv_grad.at[:, pl.ds(width, width)])
    q_width = QUERY_HEADS * HEAD_SIZE
    for c0 in range(0, width, 128):
        block = turn(kv_grad[:, c0 : c0 + 128], cosine[...], -sine[...])
        back[:, q_width + c0 : q_width + c0 + 128] = block.astype(bf)
    back[:, q_width + width :] = kv_grad[:, width:].astype(bf)
    out_way.level(1, 1)
    out_way.along(1)
    out_way.level(1, 0)
    out_way.last(layer_out, mixed)
    for way in (k_way, v_way, out_way):
        way.finish()


def attend_back(
    placed, gin, gate_map, cot, ffn_gain, outputs, log_sums, keys, part, w_o, mixed, cosine, sine, collective_id
):
    count, kv_width = keys.shape[1:]
    plans = [Plan(0, (Y, Z), (Z, Y)), Plan(0, (Z, Y), (Z, Y)), Plan(1, (C, Y, Z), (C, Z, Y))]
    bf, f32 = jnp.bfloat16, jnp.float32
    group = QUERY_HEADS // KEY_VALUE_HEADS
    vmem = pl.BlockSpec(memory_space=pltpu.VMEM)
    apart = pl.BlockSpec(memory_space=pl.ANY)
    dma = pltpu.SemaphoreType.DMA
    heads = (KEY_VALUE_HEADS, group * count, 2 * HEAD_SIZE)
    blocks = [(count, kv_width // 2)] * 2 + [part.shape[1:]]
    return pl.pallas_call(
        functools.partial(attend_back_kernel, plans),
        out_shape=[
            jax.ShapeDtypeStruct((count, outputs.shape[1] + kv_width), bf),
            jax.ShapeDtypeStruct(mixed.shape, bf),
            jax.ShapeDtypeStruct(mixed.shape, f32),
            jax.ShapeDtypeStruct(mixed.shape, bf),
            jax.ShapeDtypeStruct((3 * count, mixed.shape[1]), bf),
            jax.ShapeDtypeStruct((3 * count, 128), bf),
        ],
        in_specs=[vmem] * 8 + [apart] * 2 + [vmem] * 3,
        out_specs=[vmem] * 6,
        scratch_shapes=[
            pltpu.VMEM((count, kv_width), f32),
            pltpu.VMEM(heads, bf),
            pltpu.VMEM(heads, f32),
            pltpu.VMEM((group * count, 128), f32),
            pltpu.VMEM(keys.shape, bf),
            pltpu.VMEM(part.shape, bf),
            pltpu.VMEM(outputs.shape, bf),
            pltpu.VMEM(w_o.shape, bf),
        ]
        + [pltpu.VMEM((n,) + b, bf) for p, b in zip(plans, blocks) for n in Reduce.counts(p)[0]]
        + [dma((n,)) for p in plans for n in Reduce.counts(p)[1:]]
        + [dma(()), dma((NC * NZ,)), dma(())],
        compiler_params=pltpu.CompilerParams(
            collective_id=collective_id, has_side_effects=True, vmem_limit_bytes=64 * 1024 * 1024
        ),
        name="attend_back",
    )(placed, gin, gate_map, cot, ffn_gain, outputs, log_sums, keys, part, w_o, mixed, cosine, sine)


def last_kernel(core_ref, own, core_part, x_part, both_part, one, two, small, layer, grad, *outs):
    core = core_ref[0]
    in_out, out_out = outs[:2]
    split = in_out.shape[3]
    for at, left, right in ((core, own, x_part), (1 - core, core_part, both_part)):
        total = left[0].astype(jnp.float32) + right[0].astype(jnp.float32)
        in_out[at, 0] = total[:, :split]
        out_out[at, 0] = total[:, split:]

    @pl.when(jnp.logical_and(pl.program_id(0) == 0, pl.program_id(1) == 0))
    def _():
        wq, wk, wv, wo, router, first_gain, second_gain, layer_out, grad_out = outs[2:]
        layer_out[...] = layer[...]
        grad_out[...] = grad[...]
        q, k = wq.shape[1], wk.shape[1]
        wq[...] = one[:, :q]
        wk[...] = one[:, q : q + k]
        wv[...] = one[:, q + k :]
        wo[...] = two[...]
        turned = small[...].T
        at = router.shape[0]
        router[...] = turned[:at]
        first_gain[...] = turned[at : at + 1]
        second_gain[...] = turned[at + 1 : at + 2]


def last_outputs(pieces, core, split, sums, widths):
    held, quarter, columns = pieces[0].shape
    step = quarter // 2
    rows = sums[0].shape[0]
    spec = pl.BlockSpec((1, step, columns), lambda e, r, c: (e, r, 0))
    fixed = lambda a, b: pl.BlockSpec((a, b), lambda e, r, c: (0, 0))
    outs = (split, columns - split)
    shapes = [(rows, w) for w in widths[:-1]] + [(widths[-1], rows)] + [(1, rows)] * 2 + [a.shape for a in sums[3:]]
    types = [jnp.float32] * 7 + [a.dtype for a in sums[3:]]
    return pl.pallas_call(
        last_kernel,
        grid_spec=pltpu.PrefetchScalarGridSpec(
            num_scalar_prefetch=1,
            grid=(held, 2),
            in_specs=[spec] * 4 + [fixed(*a.shape) for a in sums],
            out_specs=[pl.BlockSpec((NC, 1, step, w), lambda e, r, c: (0, e, r, 0)) for w in outs]
            + [fixed(*s) for s in shapes],
        ),
        out_shape=[jax.ShapeDtypeStruct((NC, held, quarter, w), jnp.float32) for w in outs]
        + [jax.ShapeDtypeStruct(s, d) for s, d in zip(shapes, types)],
        name="last_outputs",
    )(core[None], *pieces, *sums)


MODEL_WIDTH = 1536
QUERY_HEADS = 24
KEY_VALUE_HEADS = 8
HEAD_SIZE = 64
EXPERT_HIDDEN = 512
EXPERT_COUNT = 32
TOP = 8
CAP = 40


norm_eps = 1e-06
attn_scale = 0.015625
rope_base = 10000.0
masked_logits = -1e30


def rope_tables(positions):
    half = HEAD_SIZE // 2
    frequency = jnp.power(
        jnp.float32(rope_base), -2.0 * jnp.arange(half, dtype=jnp.float32) / HEAD_SIZE
    )
    angle = positions.astype(jnp.float32)[:, None] * frequency[None, :]
    return (jnp.cos(angle)[:, None, :], jnp.sin(angle)[:, None, :])


def rotate_pairs(value_tensor, cosine_table, sine_table):
    half = value_tensor.shape[-1] // 2
    first = value_tensor[..., :half]
    second = value_tensor[..., half:]
    return jnp.concatenate(
        [first * cosine_table - second * sine_table, second * cosine_table + first * sine_table],
        axis=-1,
    )


def rms_forward(wide, gain):
    inverse = lax.rsqrt(jnp.mean(wide * wide, axis=-1, keepdims=True) + norm_eps)
    unit = wide * inverse
    return (unit, inverse, (unit * gain.astype(jnp.float32)).astype(jnp.bfloat16))


def rms_backward(grad, unit, inverse, gain):
    scaled = grad * gain.astype(jnp.float32)
    back = inverse * (scaled - unit * jnp.mean(scaled * unit, axis=-1, keepdims=True))
    return (back, jnp.sum(grad * unit, axis=0))


def piece_scores(query_rows, key_section, positions):
    token_count = key_section.shape[0]
    key_tensor = key_section.reshape(token_count, KEY_VALUE_HEADS, HEAD_SIZE)
    scores = (
        jnp.einsum("tkgd,nkd->kgtn", query_rows, key_tensor, preferred_element_type=jnp.float32)
        * attn_scale
    )
    visible = jnp.arange(token_count, dtype=jnp.int32)[None, :] <= positions[:, None]
    return (jnp.where(visible, scores, masked_logits), visible, key_tensor)


def local(
    hidden,
    routes,
    attn_norm,
    ffn_norm,
    w_q,
    key_weight,
    value_weight,
    w_o,
    router,
    expert_in,
    expert_out,
    cotangent,
):
    token_rows = hidden.shape[1]
    query_group = QUERY_HEADS // KEY_VALUE_HEADS
    ctx_size = lax.axis_size(CTX)
    sequence_length = token_rows * ctx_size
    positions = lax.axis_index(CTX) * token_rows + jnp.arange(token_rows, dtype=jnp.int32)
    cosine_table, sine_table = rope_tables(positions)
    contract_rows = (((0,), (0,)), ((), ()))
    contract_cols = (((1,), (1,)), ((), ()))
    layer = (
        lax.all_gather(attn_norm, (CTX, FSDP), axis=0, tiled=True),
        lax.all_gather(ffn_norm, (CTX, FSDP), axis=0, tiled=True),
        lax.all_gather(w_q, (CTX, FSDP), axis=0, tiled=True),
        lax.all_gather(key_weight, (CTX, FSDP), axis=0, tiled=True),
        lax.all_gather(value_weight, (CTX, FSDP), axis=0, tiled=True),
        lax.all_gather(w_o, (CTX, FSDP), axis=0, tiled=True),
        lax.all_gather(router, (CTX, FSDP), axis=0, tiled=True),
    )
    attn_gain, ffn_gain, query_w, key_weight_matrix, value_w, output_w, router_w = layer
    experts = (
        lax.all_gather(expert_in, FSDP, axis=1, tiled=True),
        lax.all_gather(expert_out, FSDP, axis=1, tiled=True),
    )
    weight_in, weight_out = experts
    wide = hidden[0].astype(jnp.float32)
    attn_unit, inverse_one, attention_input = rms_forward(wide, attn_gain)
    query_linear = jnp.dot(attention_input, query_w, preferred_element_type=jnp.float32).reshape(
        token_rows, QUERY_HEADS, HEAD_SIZE
    )
    query_rows = (
        rotate_pairs(query_linear, cosine_table, sine_table)
        .astype(jnp.bfloat16)
        .reshape(token_rows, KEY_VALUE_HEADS, query_group, HEAD_SIZE)
    )
    key_linear = jnp.dot(
        attention_input, key_weight_matrix, preferred_element_type=jnp.float32
    ).reshape(token_rows, KEY_VALUE_HEADS, HEAD_SIZE)
    key_matrix_rows = (
        rotate_pairs(key_linear, cosine_table, sine_table)
        .astype(jnp.bfloat16)
        .reshape(token_rows, KEY_VALUE_HEADS * HEAD_SIZE)
    )
    value_rows = jnp.dot(attention_input, value_w, preferred_element_type=jnp.float32).astype(
        jnp.bfloat16
    )
    init_state = (
        jnp.full((KEY_VALUE_HEADS, query_group, token_rows), masked_logits, jnp.float32),
        jnp.zeros((KEY_VALUE_HEADS, query_group, token_rows), jnp.float32),
        jnp.zeros((KEY_VALUE_HEADS, query_group, token_rows, HEAD_SIZE), jnp.float32),
    )
    key_section = lax.all_gather(key_matrix_rows, CTX, axis=0, tiled=True)
    value_section = lax.all_gather(value_rows, CTX, axis=0, tiled=True)

    def compute(current):
        best, total, weighted = current
        scores, visible, _ = piece_scores(query_rows, key_section, positions)
        value_tensor = value_section.reshape(value_section.shape[0], KEY_VALUE_HEADS, HEAD_SIZE)
        new_best = jnp.maximum(best, jnp.max(scores, axis=-1))
        weights = jnp.where(visible, jnp.exp(scores - new_best[..., None]), 0.0)
        total = jnp.sum(weights, axis=-1)
        weighted = jnp.einsum(
            "kgtn,nkd->kgtd",
            weights.astype(jnp.bfloat16),
            value_tensor,
            preferred_element_type=jnp.float32,
        )
        return (new_best, total, weighted)

    best, total, weighted = lax.cond(
        jnp.int32(0) <= positions[-1], compute, lambda current: current, init_state
    )
    log_sum_rows = best + jnp.log(total)
    attention_output = (
        jnp.transpose(weighted / total[..., None], (2, 0, 1, 3))
        .reshape(token_rows, QUERY_HEADS * HEAD_SIZE)
        .astype(jnp.bfloat16)
    )
    mixed = wide + jnp.dot(attention_output, output_w, preferred_element_type=jnp.float32)
    ffn_unit, inverse_two, ffn_in = rms_forward(mixed, ffn_gain)
    logits = jnp.dot(ffn_in, router_w, preferred_element_type=jnp.float32)
    route = routes[0]
    indicator = (route[:, :, None] == jnp.arange(EXPERT_COUNT, dtype=jnp.int32)).astype(jnp.float32)
    chosen = jnp.sum(indicator * logits[:, None, :], axis=-1)
    gates = jax.nn.softmax(chosen, axis=-1)
    flat_route = route.reshape(-1)
    counter = (flat_route[:, None] == jnp.arange(EXPERT_COUNT, dtype=jnp.int32)).astype(jnp.int32)
    slot = jnp.sum(counter * (jnp.cumsum(counter, axis=0) - 1), axis=1)
    target = flat_route * CAP + slot
    owner = (
        jnp.full((EXPERT_COUNT * CAP,), token_rows * TOP, jnp.int32)
        .at[target]
        .set(jnp.arange(token_rows * TOP, dtype=jnp.int32))
    )
    ffn_pad = jnp.concatenate([ffn_in, jnp.zeros((1, MODEL_WIDTH), jnp.bfloat16)], axis=0)
    local_experts = weight_in.shape[0]
    outgoing = ffn_pad[owner // TOP].reshape(ctx_size, local_experts, CAP, MODEL_WIDTH)
    received = lax.all_to_all(outgoing, CTX, split_axis=0, concat_axis=2, tiled=True)[0]
    act = jnp.einsum("erd,edf->erf", received, weight_in, preferred_element_type=jnp.float32)
    gate_part = act[..., :EXPERT_HIDDEN]
    up_part = act[..., EXPERT_HIDDEN:]
    sigma = jax.nn.sigmoid(gate_part)
    inner = (gate_part * sigma * up_part).astype(jnp.bfloat16)
    produced = jnp.einsum(
        "erf,edf->erd", inner, weight_out, preferred_element_type=jnp.float32
    ).astype(jnp.bfloat16)
    returned = lax.all_to_all(
        produced[None], CTX, split_axis=2, concat_axis=0, tiled=True
    ).reshape(EXPERT_COUNT * CAP, MODEL_WIDTH)
    picked = returned[target].reshape(token_rows, TOP, MODEL_WIDTH)
    layer_out = (mixed + jnp.sum(gates[..., None] * picked, axis=1)).astype(jnp.bfloat16)
    cot = cotangent[0]
    layer = (
        lax.all_gather(attn_norm, (CTX, FSDP), axis=0, tiled=True),
        lax.all_gather(ffn_norm, (CTX, FSDP), axis=0, tiled=True),
        lax.all_gather(w_q, (CTX, FSDP), axis=0, tiled=True),
        lax.all_gather(key_weight, (CTX, FSDP), axis=0, tiled=True),
        lax.all_gather(value_weight, (CTX, FSDP), axis=0, tiled=True),
        lax.all_gather(w_o, (CTX, FSDP), axis=0, tiled=True),
        lax.all_gather(router, (CTX, FSDP), axis=0, tiled=True),
    )
    attn_gain, ffn_gain, query_w, key_weight_matrix, value_w, output_w, router_w = layer
    experts = (
        lax.all_gather(expert_in, FSDP, axis=1, tiled=True),
        lax.all_gather(expert_out, FSDP, axis=1, tiled=True),
    )
    weight_in, weight_out = experts
    grad_gate = jnp.sum(cot[:, None, :] * picked, axis=-1)
    slot_grads = (
        (gates[..., None] * cot[:, None, :])
        .astype(jnp.bfloat16)
        .reshape(token_rows * TOP, MODEL_WIDTH)
    )
    slot_pad = jnp.concatenate([slot_grads, jnp.zeros((1, MODEL_WIDTH), jnp.bfloat16)], axis=0)
    grad_outgoing = slot_pad[owner].reshape(ctx_size, local_experts, CAP, MODEL_WIDTH)
    grad_received = lax.all_to_all(grad_outgoing, CTX, split_axis=0, concat_axis=2, tiled=True)[0]
    grad_w_out = jnp.einsum(
        "erd,erf->edf", grad_received, inner, preferred_element_type=jnp.float32
    )
    grad_inner = jnp.einsum(
        "erd,edf->erf", grad_received, weight_out, preferred_element_type=jnp.float32
    )
    grad_act = jnp.concatenate(
        [
            grad_inner * up_part * sigma * (1.0 + gate_part * (1.0 - sigma)),
            grad_inner * gate_part * sigma,
        ],
        axis=-1,
    ).astype(jnp.bfloat16)
    grad_w_in = jnp.einsum("erd,erf->edf", received, grad_act, preferred_element_type=jnp.float32)
    grad_rows = jnp.einsum(
        "erf,edf->erd", grad_act, weight_in, preferred_element_type=jnp.float32
    ).astype(jnp.bfloat16)
    grad_back = lax.all_to_all(
        grad_rows[None], CTX, split_axis=2, concat_axis=0, tiled=True
    ).reshape(EXPERT_COUNT * CAP, MODEL_WIDTH)
    grad_expert_in, grad_expert_out = (
        lax.psum_scatter(
            grad_w_in.astype(jnp.bfloat16), FSDP, scatter_dimension=1, tiled=True
        ).astype(jnp.float32),
        lax.psum_scatter(
            grad_w_out.astype(jnp.bfloat16), FSDP, scatter_dimension=1, tiled=True
        ).astype(jnp.float32),
    )
    grad_chosen = gates * (grad_gate - jnp.sum(gates * grad_gate, axis=-1, keepdims=True))
    grad_logits = jnp.sum(indicator * grad_chosen[..., None], axis=1).astype(jnp.bfloat16)
    grad_router_part = lax.dot_general(
        ffn_in, grad_logits, contract_rows, preferred_element_type=jnp.float32
    )
    grad_ffn_in = lax.dot_general(
        grad_logits, router_w, contract_cols, preferred_element_type=jnp.float32
    )
    grad_ffn_in = grad_ffn_in + jnp.sum(
        grad_back[target].reshape(token_rows, TOP, MODEL_WIDTH), axis=1, dtype=jnp.float32
    )
    back_two, grad_ffn_gain = rms_backward(grad_ffn_in, ffn_unit, inverse_two, ffn_gain)
    grad_mixed = cot + back_two
    grad_attn = grad_mixed.astype(jnp.bfloat16)
    grad_wo_part = lax.dot_general(
        attention_output, grad_attn, contract_rows, preferred_element_type=jnp.float32
    )
    attention_output_gradient = lax.dot_general(
        grad_attn, output_w, contract_cols, preferred_element_type=jnp.float32
    ).astype(jnp.bfloat16)
    head_gradient = attention_output_gradient.reshape(
        token_rows, KEY_VALUE_HEADS, query_group, HEAD_SIZE
    )
    delta_rows = jnp.sum(
        head_gradient.astype(jnp.float32)
        * attention_output.reshape(token_rows, KEY_VALUE_HEADS, query_group, HEAD_SIZE).astype(
            jnp.float32
        ),
        axis=-1,
    )
    delta_rows = jnp.transpose(delta_rows, (1, 2, 0))
    init_back = (
        jnp.zeros((token_rows, KEY_VALUE_HEADS, query_group, HEAD_SIZE), jnp.float32),
        jnp.zeros((sequence_length, 2 * KEY_VALUE_HEADS * HEAD_SIZE), jnp.float32),
    )
    attend_key_section = lax.all_gather(key_matrix_rows, CTX, axis=0, tiled=True)
    attend_value_section = lax.all_gather(value_rows, CTX, axis=0, tiled=True)

    def compute(current):
        token_count = attend_key_section.shape[0]
        scores, visible, key_tensor = piece_scores(query_rows, attend_key_section, positions)
        value_tensor = attend_value_section.reshape(token_count, KEY_VALUE_HEADS, HEAD_SIZE)
        weights_full = jnp.where(visible, jnp.exp(scores - log_sum_rows[..., None]), 0.0)
        grad_probs = jnp.einsum(
            "tkgd,nkd->kgtn", head_gradient, value_tensor, preferred_element_type=jnp.float32
        )
        grad_scores = (weights_full * (grad_probs - delta_rows[..., None])).astype(jnp.bfloat16)
        grad_query = attn_scale * jnp.einsum(
            "kgtn,nkd->tkgd", grad_scores, key_tensor, preferred_element_type=jnp.float32
        )
        key_portion = attn_scale * jnp.einsum(
            "kgtn,tkgd->nkd", grad_scores, query_rows, preferred_element_type=jnp.float32
        )
        value_portion = jnp.einsum(
            "kgtn,tkgd->nkd",
            weights_full.astype(jnp.bfloat16),
            head_gradient,
            preferred_element_type=jnp.float32,
        )
        update = jnp.concatenate(
            [
                key_portion.reshape(token_count, KEY_VALUE_HEADS * HEAD_SIZE),
                value_portion.reshape(token_count, KEY_VALUE_HEADS * HEAD_SIZE),
            ],
            axis=1,
        )
        return (grad_query, update)

    grad_query, grad_keys_full = lax.cond(
        jnp.int32(0) <= positions[-1], compute, lambda current: current, init_back
    )
    local_gradients = lax.psum_scatter(
        grad_keys_full.astype(jnp.bfloat16), CTX, scatter_dimension=0, tiled=True
    ).astype(jnp.float32)
    query_back = (
        rotate_pairs(
            grad_query.reshape(token_rows, QUERY_HEADS, HEAD_SIZE), cosine_table, -sine_table
        )
        .astype(jnp.bfloat16)
        .reshape(token_rows, QUERY_HEADS * HEAD_SIZE)
    )
    key_backward_rows = (
        rotate_pairs(
            local_gradients[:, : KEY_VALUE_HEADS * HEAD_SIZE].reshape(
                token_rows, KEY_VALUE_HEADS, HEAD_SIZE
            ),
            cosine_table,
            -sine_table,
        )
        .astype(jnp.bfloat16)
        .reshape(token_rows, KEY_VALUE_HEADS * HEAD_SIZE)
    )
    value_backward_rows = local_gradients[:, KEY_VALUE_HEADS * HEAD_SIZE :].astype(jnp.bfloat16)
    grad_wq_part = lax.dot_general(
        attention_input, query_back, contract_rows, preferred_element_type=jnp.float32
    )
    grad_wk_part = lax.dot_general(
        attention_input, key_backward_rows, contract_rows, preferred_element_type=jnp.float32
    )
    grad_wv_part = lax.dot_general(
        attention_input, value_backward_rows, contract_rows, preferred_element_type=jnp.float32
    )
    grad_attn_in = lax.dot_general(
        query_back, query_w, contract_cols, preferred_element_type=jnp.float32
    )
    grad_attn_in = grad_attn_in + lax.dot_general(
        key_backward_rows, key_weight_matrix, contract_cols, preferred_element_type=jnp.float32
    )
    grad_attn_in = grad_attn_in + lax.dot_general(
        value_backward_rows, value_w, contract_cols, preferred_element_type=jnp.float32
    )
    back_one, grad_attn_gain = rms_backward(grad_attn_in, attn_unit, inverse_one, attn_gain)
    grad_input = grad_mixed + back_one
    partial_sums = (
        lax.psum_scatter(
            grad_attn_gain.astype(jnp.bfloat16), CTX, scatter_dimension=0, tiled=True
        ).astype(jnp.float32),
        lax.psum_scatter(
            grad_ffn_gain.astype(jnp.bfloat16), CTX, scatter_dimension=0, tiled=True
        ).astype(jnp.float32),
        lax.psum_scatter(
            grad_wq_part.astype(jnp.bfloat16), CTX, scatter_dimension=0, tiled=True
        ).astype(jnp.float32),
        lax.psum_scatter(
            grad_wk_part.astype(jnp.bfloat16), CTX, scatter_dimension=0, tiled=True
        ).astype(jnp.float32),
        lax.psum_scatter(
            grad_wv_part.astype(jnp.bfloat16), CTX, scatter_dimension=0, tiled=True
        ).astype(jnp.float32),
        lax.psum_scatter(
            grad_wo_part.astype(jnp.bfloat16), CTX, scatter_dimension=0, tiled=True
        ).astype(jnp.float32),
        lax.psum_scatter(
            grad_router_part.astype(jnp.bfloat16), CTX, scatter_dimension=0, tiled=True
        ).astype(jnp.float32),
    )
    summed = (
        lax.psum_scatter(
            partial_sums[0].astype(jnp.bfloat16), FSDP, scatter_dimension=0, tiled=True
        ).astype(jnp.float32),
        lax.psum_scatter(
            partial_sums[1].astype(jnp.bfloat16), FSDP, scatter_dimension=0, tiled=True
        ).astype(jnp.float32),
        lax.psum_scatter(
            partial_sums[2].astype(jnp.bfloat16), FSDP, scatter_dimension=0, tiled=True
        ).astype(jnp.float32),
        lax.psum_scatter(
            partial_sums[3].astype(jnp.bfloat16), FSDP, scatter_dimension=0, tiled=True
        ).astype(jnp.float32),
        lax.psum_scatter(
            partial_sums[4].astype(jnp.bfloat16), FSDP, scatter_dimension=0, tiled=True
        ).astype(jnp.float32),
        lax.psum_scatter(
            partial_sums[5].astype(jnp.bfloat16), FSDP, scatter_dimension=0, tiled=True
        ).astype(jnp.float32),
        lax.psum_scatter(
            partial_sums[6].astype(jnp.bfloat16), FSDP, scatter_dimension=0, tiled=True
        ).astype(jnp.float32),
    )
    return (
        layer_out[None],
        grad_input[None],
        summed[0],
        summed[1],
        summed[2],
        summed[3],
        summed[4],
        summed[5],
        summed[6],
        grad_expert_in,
        grad_expert_out,
    )


def swap(a, flip):
    return lax.ppermute(a, FSDP, [(i, i ^ flip) for i in range(NX * NC)])


def fast_body(
    hidden,
    routes,
    attn_norm,
    ffn_norm,
    w_q,
    key_weight,
    value_weight,
    w_o,
    router,
    expert_in,
    expert_out,
    cotangent,
):
    tokens = hidden.shape[1]
    ctx = lax.axis_index(CTX)
    fsdp = lax.axis_index(FSDP)
    core = fsdp % NC
    rows = w_q.shape[0]
    quarter = expert_in.shape[1]
    kv_width = KEY_VALUE_HEADS * HEAD_SIZE
    q_width = QUERY_HEADS * HEAD_SIZE
    held = expert_in.shape[0] // NC
    bf = jnp.bfloat16
    f32 = jnp.float32
    positions = ctx * tokens + jnp.arange(tokens, dtype=jnp.int32)
    cosine_table, sine_table = (table[:, 0] for table in rope_tables(positions))
    cosine = jnp.concatenate([cosine_table] * 4, axis=1)
    sine = jnp.concatenate([-sine_table, sine_table] * 2, axis=1)
    contract_cols = (((1,), (1,)), ((), ()))
    wide = hidden[0].astype(f32)
    cot = cotangent[0]

    route = routes[0]
    indicator = (route[:, :, None] == jnp.arange(EXPERT_COUNT, dtype=jnp.int32)).astype(f32)
    part = rows // 3
    whole = (Z, Y, X, C)
    one, two, mine, *others = gather_weights(
        [w_q, key_weight, value_weight, w_o, router.T, attn_norm[None], ffn_norm[None]],
        [expert_in, expert_out],
        [
            Plan(0, (X, Z, Y, C), whole, rows=(2 * part, part)),
            Plan(1, (X, Z, Y, C), whole, rows=(part, part)),
            Plan(1, (X, Y, Z, C), whole, rows=(2 * part, part)),
            Plan(0, (Z, Y, X, C), whole, rows=(0, 2 * part)),
            Plan(1, (Z, Y, X, C), whole, rows=(0, part)),
        ],
        0,
    )
    parts = [mine, swap(mine, 2)] + [swap(other, 1) for other in others] + [swap(others[0], 3)]
    one = one.reshape(MODEL_WIDTH, -1)
    two = two.reshape(MODEL_WIDTH, -1)
    output_w = two[:, :MODEL_WIDTH]
    small = two[:, MODEL_WIDTH:]
    router_w = small[:, :EXPERT_COUNT]
    gains = lax.dot_general(
        jnp.eye(128, dtype=bf), small, contract_cols, preferred_element_type=f32
    )
    attn_gain, ffn_gain = gains[EXPERT_COUNT], gains[EXPERT_COUNT + 1]

    _, _, attention_input = rms_forward(wide, attn_gain)
    linear = jnp.dot(attention_input, one, preferred_element_type=f32)
    attention_output, log_sums, kv, cots, queries = attend(linear, cot, route, cosine, sine, 1)
    mixed = wide + jnp.dot(attention_output, output_w, preferred_element_type=f32)
    _, _, ffn_in = rms_forward(mixed, ffn_gain)
    logits = jnp.dot(ffn_in, router_w, preferred_element_type=f32)
    chosen = jnp.sum(indicator * logits[:, None, :], axis=-1)
    gates = jax.nn.softmax(chosen, axis=-1)
    gate_map = jnp.sum(indicator * gates[..., None], axis=1)
    payload = jnp.concatenate(
        [ffn_in, gate_map.astype(bf), jnp.zeros((tokens, 128 - EXPERT_COUNT), bf)], axis=1
    )
    gin, moe_part, *pieces = moe(payload, cots, parts + others[-1:], CAP, 2)
    across = [swap(pieces[j], j) for j in range(1, NX * NC)]
    gate_wide = jnp.concatenate([gate_map, jnp.zeros((tokens, 128 - EXPERT_COUNT), f32)], axis=1)
    back, layer_out, grad_mixed, grad_attn, left_small, right_small = attend_back(
        queries,
        gin,
        gate_wide,
        cot,
        ffn_gain.astype(f32)[None],
        attention_output,
        log_sums,
        kv,
        moe_part,
        two,
        mixed,
        cosine,
        sine,
        4,
    )
    *sums, grad_input = return_weights(
        [attention_input, attention_output, left_small],
        [back, grad_attn, right_small],
        one,
        hidden[0],
        attn_gain.astype(f32)[None],
        grad_mixed,
        EXPERT_COUNT,
        5,
    )
    grad_expert_in, grad_expert_out, *rest, first_gain, second_gain, layer_out, grad_input = last_outputs(
        [pieces[0]] + across,
        core,
        2 * EXPERT_HIDDEN,
        sums + [layer_out, grad_input],
        (q_width, kv_width, kv_width, MODEL_WIDTH, EXPERT_COUNT),
    )
    return (
        layer_out[None],
        grad_input[None],
        first_gain.reshape(rows),
        second_gain.reshape(rows),
        *rest[:-1],
        rest[-1].T,
        grad_expert_in.reshape(NC * held, quarter, -1),
        grad_expert_out.reshape(NC * held, quarter, -1),
    )


def fast(*args):
    return fast_body(*args)


def solution(mesh):
    placed = (
        P(FSDP, CTX, None),
        P(FSDP, CTX, None),
        P((CTX, FSDP)),
        P((CTX, FSDP)),
        P((CTX, FSDP), None),
        P((CTX, FSDP), None),
        P((CTX, FSDP), None),
        P((CTX, FSDP), None),
        P((CTX, FSDP), None),
        P(CTX, FSDP, None),
        P(CTX, FSDP, None),
        P(FSDP, CTX, None),
    )
    small = mesh.shape[CTX] == NZ * NY and mesh.shape[FSDP] == NX * NC
    return jax.shard_map(
        fast if small else local,
        mesh=mesh,
        in_specs=placed,
        out_specs=(
            P(FSDP, CTX, None),
            P(FSDP, CTX, None),
            P((CTX, FSDP)),
            P((CTX, FSDP)),
            P((CTX, FSDP), None),
            P((CTX, FSDP), None),
            P((CTX, FSDP), None),
            P((CTX, FSDP), None),
            P((CTX, FSDP), None),
            P(CTX, FSDP, None),
            P(CTX, FSDP, None),
        ),
        check_vma=False,
    )
```
